32 devices in a mesh: data: 1 (over z), cols: 4 (over y), model: 8 (over x, core).
Axes of the slice: x: 4, y: 4, z: 1, core: 2. Of those that a mesh axis runs over, the one named last changes fastest.
The devices are a block of a 4x4x8 slice.
Arguments:
- x_in: bfloat16 [64, 56, 56, 64], P('data', None, None, ('model', 'cols'))
- w_conv1: bfloat16 [3, 3, 64, 64], P(None, None, ('model', 'cols'))
- b_conv1: float32 [64], replicated
- w_conv2: bfloat16 [3, 3, 64, 64], replicated
- b_conv2: float32 [64], replicated
Outputs:
- output: float32 [64, 56, 56, 64], P('data', 'model', 'cols')
All inputs are finite; a program needn't handle non-finite values.
Results may differ from the reference program's by a relative error of at most 0.001.
Values are sent between devices in bfloat16 or wider.
A program may use at most 768 MiB of HBM per device.

```python
import jax
import jax.numpy as jnp
from jax import lax

IMAGES = 64
HEIGHT = 56
WIDTH = 56
IN_CHANS = 64
MID_CHANS = 64
OUT_CHANS = 64

CONV_DIMS = ("NHWC", "HWIO", "NHWC")


def setup_inputs(seed: int = 0, part: int = 0) -> dict:
    base_key = jax.random.key(seed)
    part_key = jax.random.fold_in(base_key, part)
    key_w1, key_b1, key_w2, key_b2 = jax.random.split(jax.random.fold_in(base_key, 1000), 4)
    x_in = jax.random.normal(part_key, (IMAGES, HEIGHT, WIDTH, IN_CHANS), jnp.float32)
    w_conv1 = jax.random.normal(key_w1, (3, 3, IN_CHANS, MID_CHANS), jnp.float32) * (9 * IN_CHANS) ** -0.5
    b_conv1 = 0.5 * jax.random.normal(key_b1, (MID_CHANS,), jnp.float32)
    w_conv2 = jax.random.normal(key_w2, (3, 3, MID_CHANS, OUT_CHANS), jnp.float32) * (4.5 * MID_CHANS) ** -0.5
    b_conv2 = 0.5 * jax.random.normal(key_b2, (OUT_CHANS,), jnp.float32)
    return {"x_in": x_in.astype(jnp.bfloat16), "w_conv1": w_conv1.astype(jnp.bfloat16), "b_conv1": b_conv1, "w_conv2": w_conv2.astype(jnp.bfloat16), "b_conv2": b_conv2}


def reference(x_in, w_conv1, b_conv1, w_conv2, b_conv2):
    kernel_one = w_conv1.astype(jnp.float32)
    kernel_two = w_conv2.astype(jnp.float32)

    def one_image(image):
        z_sum = lax.conv_general_dilated(image[None].astype(jnp.float32), kernel_one, (1, 1), "SAME", dimension_numbers=CONV_DIMS)
        act_map = jnp.maximum(z_sum + b_conv1, 0.0).astype(jnp.bfloat16)
        out_map = lax.conv_general_dilated(act_map.astype(jnp.float32), kernel_two, (1, 1), "SAME", dimension_numbers=CONV_DIMS)
        return out_map[0] + b_conv2

    return lax.map(one_image, x_in)
```

```python
import functools

import jax
import jax.numpy as jnp
from jax import lax
from jax.experimental import pallas as pl
from jax.experimental.pallas import tpu as pltpu
from jax.sharding import PartitionSpec as P

MESH = pl.DeviceIdType.MESH
BF16 = jnp.bfloat16
F32 = jnp.float32
FIRST_ROWS = 3
AHEAD = (1, 0)
COLUMN_FIRST = (2, 3)
CHIPS_ALONG = (1, 3, 2, 0)
CHIP_ORDER = tuple((other, dy) for other in (0, 1) for dy in (1, -1, 0, 2))


def turn(recv, i, put):
    sources, _, win_j, own_chans, lanes = recv.shape
    chans = sources * own_chans
    for j in range(win_j):
        top = recv[:, 2 * i, j].reshape(chans, lanes)
        under = recv[:, 2 * i + 1, j].reshape(chans, lanes)
        put(j, jnp.concatenate([top, under], axis=0).T.reshape(2, lanes // 2, 2 * chans))


def blocks(pairs, weights, count):
    acc = None
    for dw in range(4):
        parts = [view[dw // 2 : dw // 2 + count, dw % 2] for view in pairs]
        lhs = jnp.concatenate([p.reshape(count * p.shape[1], p.shape[2]) for p in parts], axis=1)
        term = jnp.dot(lhs, weights(dw), preferred_element_type=F32)
        acc = term if acc is None else acc + term
    return acc


def first(pairs, weights, bias, y_row, blank_a):
    count, _, images, lanes = y_row.shape
    c = lax.axis_index("cols")
    row = lax.rem(lax.broadcasted_iota(jnp.int32, (1, 2 * lanes), 1), lanes) // (lanes // 2)
    act = jnp.maximum(blocks(pairs, weights, count) + bias, 0.0)
    act = jnp.where(row != blank_a, act, 0.0).astype(BF16)
    for b in range(2):
        y_row[:, b] = act[:, b * lanes : (b + 1) * lanes].reshape(count, images, lanes)
    blank = jnp.zeros((images, lanes), BF16)

    @pl.when(c == 0)
    def _():
        y_row[0, 0] = blank

    @pl.when(c == lax.axis_size("cols") - 1)
    def _():
        y_row[count - 1, 1] = blank


def second(pairs, weights, bias, out_pair):
    _, count, _, images, chans = out_pair.shape
    res = blocks(pairs, weights, count) + bias
    for b in range(2):
        for a in range(2):
            at = (2 * b + a) * chans
            out_pair[a, :, b] = res[:, at : at + chans].reshape(count, images, chans)


def conv_kernel(
    n_rows,
    n_cols,
    x_hbm,
    w1_hbm,
    b1_hbm,
    w2_hbm,
    b2_hbm,
    out,
    ymat,
    wt2,
    bias2,
    recv,
    xmat,
    wt1,
    bias1,
    xs,
    packed,
    w1s,
    w1own,
    w1all,
    w2s,
    b1s,
    b2s,
    load_sem,
    par_sem,
    send_sem,
    recv_sem,
    wsend_sem,
    wrecv_sem,
    swap_send_sem,
    swap_recv_sem,
    wswap_send_sem,
    wswap_recv_sem,
):
    chip_h, pairs = xs.shape[1:3]
    images = xs.shape[-1]
    tile_h, tile_j = chip_h // 2, pairs // n_cols
    win_j = tile_j + 2
    sources = n_rows * n_cols
    r, c = lax.axis_index("model"), lax.axis_index("cols")
    par = lax.rem(r, 2)
    me = r * n_cols + c
    chans = recv.shape[0] * 2

    near = tile_h - FIRST_ROWS
    groups = (((near, chip_h - near),), *(((k, k + 2), (chip_h - k - 2, chip_h - k)) for k in range(near - 2, -1, -2)))
    loads = []
    for g, spans in enumerate(groups):
        loads.append(
            [
                pltpu.make_async_copy(x_hbm.at[:, lo:hi], xs.at[:, lo:hi], load_sem.at[g, n])
                for n, (lo, hi) in enumerate(spans)
            ]
        )
    for copies in loads:
        for copy in copies:
            copy.start()
    params = [
        pltpu.make_async_copy(src, dst, par_sem.at[s])
        for s, (src, dst) in enumerate(((w1_hbm, w1s), (w2_hbm, w2s), (b1_hbm, b1s), (b2_hbm, b2s)))
    ]
    for copy in params:
        copy.start()

    barrier = pltpu.get_barrier_semaphore()
    to_cs = [lax.rem(c + k, n_cols) for k in range(n_cols)]

    def device(to_r, to_c):
        return {"model": to_r, "cols": to_c}

    to_rs = [lax.rem(r + k, n_rows) for k in range(n_rows)]
    for kr, kc in sorted(
        ((kr, kc) for kr in range(n_rows) for kc in range(n_cols) if kr or kc),
        key=lambda k: (not (k[0] in (2, 3) and k[1] == 1), -(min(k[0], n_rows - k[0]) // 2 + min(k[1], n_cols - k[1]))),
    ):
        pl.semaphore_signal(barrier, inc=1, device_id=device(to_rs[kr], to_cs[kc]), device_id_type=MESH)

    def pack_rows(x, lo, hi):
        rows = hi - lo
        left, right = (xs[x, lo:hi, :, p].reshape(rows * pairs * 2, images) for p in range(2))
        both = jnp.concatenate([left, right], axis=1)
        packed[pl.ds(chip_h * x + lo, rows)] = both.reshape(rows, pairs, 2, 2 * images)

    def pack(g):
        for copy in loads[g]:
            copy.wait()

        def body(x, carry):
            for lo, hi in groups[g]:
                pack_rows(x, lo, hi)
            return carry

        lax.fori_loop(0, n_rows // 2, body, 0)

    last = tile_h + 4

    def rows_of(offset, count):
        def where(to_r):
            q = lax.rem(to_r, 2)
            src = tile_h * to_r + offset + (tile_h - count - 2 * offset) * q
            dst = offset + 2 + (last - count - 2 * offset - 3) * q
            return src, dst

        return where

    chunks = (
        (FIRST_ROWS, rows_of(near, FIRST_ROWS), False),
        *((2, rows_of(k, 2), False) for k in range(near - 2, -1, -2)),
        (2, rows_of(-2, 2), True),
    )
    no_outer = (r == 0) | (r == n_rows - 1)
    at_edge = (c == 0) | (c == n_cols - 1)
    own_j = c == 0
    own_j = own_j.astype(jnp.int32)

    def send_tile(chunk, to_r, to_c, there):
        rows, where, is_outer = chunks[chunk]
        src, dst = where(to_r)
        skip = (to_c == 0).astype(jnp.int32)
        edge = (to_c == 0) | (to_c == n_cols - 1)
        if is_outer:
            there = there & (to_r > 0) & (to_r < n_rows - 1)

        def copy(count, src_j, dst_j):
            pltpu.make_async_remote_copy(
                src_ref=packed.at[pl.ds(src, rows), pl.ds(src_j, count)],
                dst_ref=recv.at[me, pl.ds(dst, rows), pl.ds(dst_j, count)],
                send_sem=send_sem.at[chunk],
                recv_sem=recv_sem.at[chunk],
                device_id=device(to_r, to_c),
                device_id_type=MESH,
            ).start()

        pl.when(there & edge)(lambda: copy(win_j - 1, tile_j * to_c - 1 + skip, skip))
        pl.when(there & jnp.logical_not(edge))(lambda: copy(win_j, tile_j * to_c - 1, 0))

    chips = n_rows // 2
    ahead_r, ahead_c = AHEAD

    def step(t, table):
        value = jnp.int32(table[-1])
        for k, entry in enumerate(table[:-1]):
            value = jnp.where(t == k, entry, value)
        return value

    def turn_to(t):
        dx = step(t, CHIPS_ALONG)
        return lax.rem(r // 2 + dx, chips), dx

    def send_chip(chunk, t, rest, where=None):
        x, dx = turn_to(t)
        way = 1 - 2 * lax.rem(par + t, 2)
        for other, dy in CHIP_ORDER:
            to_r = 2 * x + (1 - par if other else par)
            to_c = lax.rem(c + way * dy + n_cols, n_cols)
            there = True
            if not other and dy == 0:
                there = dx > 0
            if rest:
                there = there & jnp.logical_not((to_r == ahead_r) & (to_c == ahead_c))
            if where is not None:
                there = there & where(to_c)
            send_tile(chunk, to_r, to_c, there)

    def send_ahead(chunk):
        send_tile(chunk, jnp.int32(ahead_r), jnp.int32(ahead_c), (r != ahead_r) | (c != ahead_c))

    def send_chunk(chunk):

        def first_column(t, carry):
            x, _ = turn_to(t)
            for other in range(2):
                to_r = 2 * x + (1 - par if other else par)
                there = ((to_r != r) | (c != 0)) & (to_r != ahead_r)
                send_tile(chunk, to_r, jnp.int32(0), there)
            return carry

        where = None
        if chunk in COLUMN_FIRST:
            lax.fori_loop(0, chips, first_column, 0)
            where = lambda to_c: to_c > 0

        def body(t, carry):
            send_chip(chunk, t, chunk > 1, where)
            return carry

        lax.fori_loop(0, chips, body, 0)

    params[0].wait()
    for dw in range(3):
        w1own[dw] = jnp.concatenate([w1s[1, dw], w1s[0, dw]], axis=1)
    w1own[3] = jnp.concatenate([w1s[2, 0], w1s[2, 1]], axis=1)
    w1own[4] = jnp.concatenate([w1s[2, 2], jnp.zeros_like(w1s[2, 2])], axis=1)
    w1all[r // 2, par, c] = w1own[...]

    for copy in loads[0]:
        copy.wait()
    pack_rows(turn_to(0)[0], *groups[0][0])
    pl.semaphore_wait(barrier, sources - 1)

    def send_weights():
        for kr in range(0, n_rows, 2):
            for kc in range(n_cols):
                if kr or kc:
                    pltpu.make_async_remote_copy(
                        src_ref=w1own,
                        dst_ref=w1all.at[r // 2, par, c],
                        send_sem=wsend_sem,
                        recv_sem=wrecv_sem,
                        device_id=device(to_rs[kr], to_cs[kc]),
                        device_id_type=MESH,
                    ).start()

    def pack_and_send(t, carry):
        pl.when(t < chips - 1)(lambda: pack_rows(turn_to(t + 1)[0], *groups[0][0]))
        send_chip(0, t, False)
        pl.when(t == 0)(send_weights)
        return carry

    lax.fori_loop(0, chips, pack_and_send, 0)

    pack(1)
    send_chunk(1)
    pack(2)
    send_ahead(2)
    send_ahead(3)
    send_chunk(2)
    send_chunk(3)

    def own_rows(chunk):
        rows, where, _ = chunks[chunk]
        src, dst = where(r)

        def copy(count, src_j, dst_j):
            for h in range(rows):
                recv[me, dst + h, pl.ds(dst_j, count)] = packed[src + h, pl.ds(src_j, count)]

        pl.when(at_edge)(lambda: copy(win_j - 1, tile_j * c - 1 + own_j, own_j))
        pl.when(jnp.logical_not(at_edge))(lambda: copy(win_j, tile_j * c - 1, 0))

    for chunk in range(3):
        own_rows(chunk)
    pl.when(jnp.logical_not(no_outer))(lambda: own_rows(3))

    zero_row = jnp.zeros((win_j, 2, 2 * images), BF16)
    zero_col = jnp.zeros((tile_h + 2, 2, 2 * images), BF16)

    def clear(s, carry):
        recv[s, last * (1 - par)] = zero_row
        return carry

    def clear_outer(s, carry):
        recv[s, (last - 1) * par] = zero_row
        recv[s, (last - 1) * par + 1] = zero_row
        return carry

    def clear_edge(s, carry):
        recv[s, pl.ds(3 * par, tile_h + 2), (win_j - 1) * (1 - own_j)] = zero_col
        return carry

    lax.fori_loop(0, sources, clear, 0)
    pl.when(no_outer)(lambda: (lax.fori_loop(0, sources, clear_outer, 0), None)[1])
    pl.when(at_edge)(lambda: (lax.fori_loop(0, sources, clear_edge, 0), None)[1])

    low = lax.broadcasted_iota(jnp.int32, (chans, 2 * chans), 1) < chans

    def spread(wt, u, v, dw):
        ur, vr = pltpu.roll(u, chans, 1), pltpu.roll(v, chans, 1)
        zero = jnp.zeros_like(u)
        tiles = (jnp.where(low, ur, zero), u, jnp.where(low, v, ur), jnp.where(low, zero, vr))
        for k, tile in enumerate(tiles):
            tile = tile.astype(BF16)
            for b in range(2):
                wt[dw + b, k * chans : (k + 1) * chans, b * 2 * chans : (b + 1) * 2 * chans] = tile

    def blank(wt):
        zero = jnp.zeros((4 * chans, 2 * chans), BF16)
        wt[3, :, 0 : 2 * chans] = zero
        wt[0, :, 2 * chans : 4 * chans] = zero

    for copy in params[1:]:
        copy.wait()
    blank(wt1)
    blank(wt2)
    for dw in range(3):
        w = [w2s[dh, dw].astype(F32) for dh in range(3)]
        spread(
            wt2,
            jnp.concatenate([w[1], w[0]], axis=1),
            jnp.concatenate([w[2], jnp.zeros_like(w[2])], axis=1),
            dw,
        )
    bias1[...] = jnp.concatenate([b1s[...]] * 4, axis=1)
    bias2[...] = jnp.concatenate([b2s[...]] * 4, axis=1)

    def wait_bytes(ref, sem):
        pltpu.make_async_copy(ref, ref, sem).wait()

    w1_bytes = recv.at[0 : sources // 2 - 1, 0, 0:5]
    wait_bytes(w1_bytes, wrecv_sem)
    wait_bytes(w1_bytes, wsend_sem)
    partner = device(r + 1 - 2 * par, c)
    w_swap = pltpu.make_async_remote_copy(
        src_ref=w1all.at[:, par],
        dst_ref=w1all.at[:, par],
        send_sem=wswap_send_sem,
        recv_sem=wswap_recv_sem,
        device_id=partner,
        device_id_type=MESH,
    )
    w_swap.start()

    def arrived(chunk):
        def wait(count):
            wait_bytes(recv.at[0 : sources - 1, 0 : chunks[chunk][0], 0:count], recv_sem.at[chunk])

        pl.when(at_edge)(lambda: wait(win_j - 1))
        pl.when(jnp.logical_not(at_edge))(lambda: wait(win_j))

    arrived(0)
    give = tile_h - (tile_h - 3) * par
    land = tile_h + 2 - (tile_h + 1) * (1 - par)
    swap = pltpu.make_async_remote_copy(
        src_ref=recv.at[:, pl.ds(give, 2)],
        dst_ref=recv.at[:, pl.ds(land, 2)],
        send_sem=swap_send_sem,
        recv_sem=swap_recv_sem,
        device_id=partner,
        device_id_type=MESH,
    )
    swap.start()

    w_swap.wait()
    u = [w1all[:, :, :, k].reshape(chans, 2 * chans).astype(F32) for k in range(5)]
    for dw in range(3):
        v = (u[3], pltpu.roll(u[3], chans, 1), u[4])[dw]
        spread(wt1, u[dw], jnp.where(low, v, 0.0), dw)

    x_pairs, z_pairs = xmat.shape[0], ymat.shape[0]
    o_pairs = z_pairs - 1

    def nth(n, count):
        return (count - 1) * (1 - par) + n * (2 * par - 1)

    def turn_one(n, carry):
        i = nth(n, x_pairs)

        def put(j, value):
            xmat[i, j] = value

        turn(recv, i, put)
        return carry

    def first_one(n, carry):
        i = nth(n, z_pairs)
        fill = jnp.where(n == 0, 1 - par, 2)
        out_of = jnp.where(n == z_pairs - 1, jnp.where(r == 0, 0, jnp.where(r == n_rows - 1, 1, 2)), 2)
        blank_a = jnp.where(fill < 2, fill, out_of)
        first((xmat.at[i], xmat.at[i + 1]), lambda dw: wt1[dw], bias1[...], ymat.at[i], blank_a)
        return carry

    def second_one(n, carry):
        i = nth(n, o_pairs)
        second((ymat.at[i], ymat.at[i + 1]), lambda dw: wt2[dw], bias2[...], out.at[pl.ds(2 * i, 2)])
        return carry

    def stage(s, carry):
        @pl.when(s == 0)
        def _():
            swap.wait()

        for k in range(1, 4):
            there = s == k
            if k == 3:
                there = there & jnp.logical_not(no_outer)
            pl.when(there)(lambda k=k: arrived(k))

        later = (s + 3) // 4
        lax.fori_loop((2 + s) * later, 3 + s, turn_one, 0)
        lax.fori_loop((1 + s) * later, 2 + s, first_one, 0)
        lax.fori_loop(s, 1 + s - s // 3, second_one, 0)
        return carry

    lax.fori_loop(0, 4, stage, 0)

    per_edge = n_rows * 2
    for chunk in range(4):
        rows = chunks[chunk][0]
        n_r = n_rows - 2 if chunk == 3 else n_rows
        counts = (n_r * 2, n_r * (n_cols - 2))

        def drain(edge_n, inner_n, rows=rows, chunk=chunk):
            wait_bytes(recv.at[0:edge_n, 0:rows, 0 : win_j - 1], send_sem.at[chunk])
            wait_bytes(recv.at[0:inner_n, 0:rows, 0:win_j], send_sem.at[chunk])

        def drain_own(chunk=chunk, counts=counts, drain=drain):
            pl.when(at_edge)(lambda: drain(counts[0] - 1, counts[1]))
            pl.when(jnp.logical_not(at_edge))(lambda: drain(counts[0], counts[1] - 1))

        if chunk == 3:
            pl.when(no_outer)(lambda: drain(*counts))
            pl.when(jnp.logical_not(no_outer))(drain_own)
        else:
            drain_own()


def tail_kernel(tile, ymat, wt2, bias2, out_hbm, o_new, sem):
    par = lax.rem(lax.axis_index("model"), 2)
    rows = out_hbm.shape[0]
    o_pairs = ymat.shape[0] - 1
    late = (rows - 2) * par
    here = 2 * (1 - par)

    def start(k, carry):
        pltpu.make_async_copy(tile.at[par + k], out_hbm.at[k], sem.at[0]).start()
        return carry

    lax.fori_loop(here, here + rows - 2, start, 0)
    i = (o_pairs - 1) * par
    second((ymat.at[i], ymat.at[i + 1]), lambda dw: wt2[dw], bias2[...], o_new)
    last = pltpu.make_async_copy(o_new, out_hbm.at[pl.ds(late, 2)], sem.at[1])
    last.start()
    pltpu.make_async_copy(tile.at[0 : rows - 2], out_hbm.at[0 : rows - 2], sem.at[0]).wait()
    last.wait()


def solution(mesh):
    n_rows = mesh.shape["model"]
    n_cols = mesh.shape["cols"]

    def run_local(x_in, w_conv1, b_conv1, w_conv2, b_conv2):
        images, height, width, own_chans = x_in.shape
        sources = n_rows * n_cols
        chans = own_chans * sources
        pairs = width // 2
        tile_h, tile_j = height // n_rows, pairs // n_cols
        win_j = tile_j + 2
        x_pairs, z_pairs = (tile_h + 5) // 2, (tile_h + 3) // 2
        x_t = jnp.transpose(x_in, (1, 2, 3, 0)).reshape(n_rows // 2, 2 * tile_h, pairs, 2, own_chans, images)
        args = (x_t, w_conv1, b_conv1.reshape(1, chans), w_conv2, b_conv2.reshape(1, chans))
        hbm = pl.BlockSpec(memory_space=pltpu.HBM)
        vmem = pl.BlockSpec(memory_space=pltpu.VMEM)
        kept = (
            pltpu.VMEM((2 * (z_pairs - 1), tile_j, 2, images, chans), F32),
            pltpu.VMEM((z_pairs, win_j - 1, 2, images, 2 * chans), BF16),
            pltpu.VMEM((4, 4 * chans, 4 * chans), BF16),
            pltpu.VMEM((1, 4 * chans), F32),
        )
        state = pl.pallas_call(
            functools.partial(conv_kernel, n_rows, n_cols),
            out_shape=kept,
            in_specs=[hbm] * 5,
            out_specs=[vmem] * len(kept),
            scratch_shapes=[
                pltpu.VMEM((sources, 2 * x_pairs, win_j, own_chans, 2 * images), BF16),
                pltpu.VMEM((x_pairs, win_j, 2, images, 2 * chans), BF16),
                pltpu.VMEM((4, 4 * chans, 4 * chans), BF16),
                pltpu.VMEM((1, 4 * chans), F32),
                pltpu.VMEM((n_rows // 2, 2 * tile_h, pairs, 2, own_chans, images), BF16),
                pltpu.VMEM((height, pairs, own_chans, 2 * images), BF16),
                pltpu.VMEM((3, 3, own_chans, chans), BF16),
                pltpu.VMEM((5, own_chans, 2 * chans), BF16),
                pltpu.VMEM((n_rows // 2, 2, n_cols, 5, own_chans, 2 * chans), BF16),
                pltpu.VMEM((3, 3, chans, chans), BF16),
                pltpu.VMEM((1, chans), F32),
                pltpu.VMEM((1, chans), F32),
                pltpu.SemaphoreType.DMA((3, 2)),
                pltpu.SemaphoreType.DMA((4,)),
                pltpu.SemaphoreType.DMA((4,)),
                pltpu.SemaphoreType.DMA((4,)),
            ]
            + [pltpu.SemaphoreType.DMA] * 6,
            compiler_params=pltpu.CompilerParams(
                collective_id=0, has_side_effects=True, vmem_limit_bytes=24 << 20
            ),
            name="conv",
        )(*(pltpu.with_memory_space_constraint(a, pltpu.HBM) for a in args))
        out = pl.pallas_call(
            tail_kernel,
            out_shape=jax.ShapeDtypeStruct((tile_h, tile_j, 2, images, chans), F32),
            in_specs=[vmem] * len(kept),
            out_specs=pl.BlockSpec(memory_space=pl.ANY),
            scratch_shapes=[
                pltpu.VMEM((2, tile_j, 2, images, chans), F32),
                pltpu.SemaphoreType.DMA((2,)),
            ],
            compiler_params=pltpu.CompilerParams(vmem_limit_bytes=8 << 20),
            name="tail",
        )(*state)
        out = out.reshape(tile_h, 2 * tile_j, images, chans)
        return jnp.transpose(out, (2, 0, 1, 3))

    group = ("model", "cols")
    return jax.shard_map(
        run_local,
        mesh=mesh,
        in_specs=(P("data", None, None, group), P(None, None, group, None), P(), P(), P()),
        out_specs=P("data", "model", "cols", None),
        check_vma=False,
    )
```

```python
import functools

import jax
import jax.numpy as jnp
from jax import lax
from jax.experimental import pallas as pl
from jax.experimental.pallas import tpu as pltpu
from jax.sharding import PartitionSpec as P

MESH = pl.DeviceIdType.MESH
BF16 = jnp.bfloat16
F32 = jnp.float32
FIRST_ROWS = 3
AHEAD = (1, 0)
COLUMN_FIRST = (2, 3)
CHIPS_ALONG = (3, 1, 2, 0)
CHIP_ORDER = tuple((other, dy) for other in (0, 1) for dy in (1, -1, 0, 2))


def turn(recv, i, put):
    sources, _, win_j, own_chans, lanes = recv.shape
    chans = sources * own_chans
    for j in range(win_j):
        top = recv[:, 2 * i, j].reshape(chans, lanes)
        under = recv[:, 2 * i + 1, j].reshape(chans, lanes)
        put(j, jnp.concatenate([top, under], axis=0).T.reshape(2, lanes // 2, 2 * chans))


def blocks(pairs, weights, count):
    acc = None
    for dw in range(4):
        parts = [view[dw // 2 : dw // 2 + count, dw % 2] for view in pairs]
        lhs = jnp.concatenate([p.reshape(count * p.shape[1], p.shape[2]) for p in parts], axis=1)
        term = jnp.dot(lhs, weights(dw), preferred_element_type=F32)
        acc = term if acc is None else acc + term
    return acc


def first(pairs, weights, bias, y_row, blank_a):
    count, _, images, lanes = y_row.shape
    c = lax.axis_index("cols")
    row = lax.rem(lax.broadcasted_iota(jnp.int32, (1, 2 * lanes), 1), lanes) // (lanes // 2)
    act = jnp.maximum(blocks(pairs, weights, count) + bias, 0.0)
    act = jnp.where(row != blank_a, act, 0.0).astype(BF16)
    for b in range(2):
        y_row[:, b] = act[:, b * lanes : (b + 1) * lanes].reshape(count, images, lanes)
    blank = jnp.zeros((images, lanes), BF16)

    @pl.when(c == 0)
    def _():
        y_row[0, 0] = blank

    @pl.when(c == lax.axis_size("cols") - 1)
    def _():
        y_row[count - 1, 1] = blank


def second(pairs, weights, bias, out_pair):
    _, count, _, images, chans = out_pair.shape
    res = blocks(pairs, weights, count) + bias
    for b in range(2):
        for a in range(2):
            at = (2 * b + a) * chans
            out_pair[a, :, b] = res[:, at : at + chans].reshape(count, images, chans)


def conv_kernel(
    n_rows,
    n_cols,
    x_hbm,
    w1_hbm,
    b1_hbm,
    w2_hbm,
    b2_hbm,
    out,
    ymat,
    wt2,
    bias2,
    recv,
    xmat,
    wt1,
    bias1,
    xs,
    packed,
    w1s,
    w1own,
    w1all,
    w2s,
    b1s,
    b2s,
    load_sem,
    par_sem,
    send_sem,
    recv_sem,
    wsend_sem,
    wrecv_sem,
    swap_send_sem,
    swap_recv_sem,
    wswap_send_sem,
    wswap_recv_sem,
):
    chip_h, pairs = xs.shape[1:3]
    images = xs.shape[-1]
    tile_h, tile_j = chip_h // 2, pairs // n_cols
    win_j = tile_j + 2
    sources = n_rows * n_cols
    r, c = lax.axis_index("model"), lax.axis_index("cols")
    par = lax.rem(r, 2)
    me = r * n_cols + c
    chans = recv.shape[0] * 2

    near = tile_h - FIRST_ROWS
    groups = (((near, chip_h - near),), *(((k, k + 2), (chip_h - k - 2, chip_h - k)) for k in range(near - 2, -1, -2)))
    loads = []
    for g, spans in enumerate(groups):
        loads.append(
            [
                pltpu.make_async_copy(x_hbm.at[:, lo:hi], xs.at[:, lo:hi], load_sem.at[g, n])
                for n, (lo, hi) in enumerate(spans)
            ]
        )
    for copies in loads:
        for copy in copies:
            copy.start()
    params = [
        pltpu.make_async_copy(src, dst, par_sem.at[s])
        for s, (src, dst) in enumerate(((w1_hbm, w1s), (w2_hbm, w2s), (b1_hbm, b1s), (b2_hbm, b2s)))
    ]
    for copy in params:
        copy.start()

    barrier = pltpu.get_barrier_semaphore()
    to_cs = [lax.rem(c + k, n_cols) for k in range(n_cols)]

    def device(to_r, to_c):
        return {"model": to_r, "cols": to_c}

    to_rs = [lax.rem(r + k, n_rows) for k in range(n_rows)]
    for kr, kc in sorted(
        ((kr, kc) for kr in range(n_rows) for kc in range(n_cols) if kr or kc),
        key=lambda k: (not (k[0] in (2, 3) and k[1] == 1), -(min(k[0], n_rows - k[0]) // 2 + min(k[1], n_cols - k[1]))),
    ):
        pl.semaphore_signal(barrier, inc=1, device_id=device(to_rs[kr], to_cs[kc]), device_id_type=MESH)

    def pack_rows(x, lo, hi):
        rows = hi - lo
        left, right = (xs[x, lo:hi, :, p].reshape(rows * pairs * 2, images) for p in range(2))
        both = jnp.concatenate([left, right], axis=1)
        packed[pl.ds(chip_h * x + lo, rows)] = both.reshape(rows, pairs, 2, 2 * images)

    def pack(g):
        for copy in loads[g]:
            copy.wait()

        def body(x, carry):
            for lo, hi in groups[g]:
                pack_rows(x, lo, hi)
            return carry

        lax.fori_loop(0, n_rows // 2, body, 0)

    last = tile_h + 4

    def rows_of(offset, count):
        def where(to_r):
            q = lax.rem(to_r, 2)
            src = tile_h * to_r + offset + (tile_h - count - 2 * offset) * q
            dst = offset + 2 + (last - count - 2 * offset - 3) * q
            return src, dst

        return where

    chunks = (
        (FIRST_ROWS, rows_of(near, FIRST_ROWS), False),
        *((2, rows_of(k, 2), False) for k in range(near - 2, -1, -2)),
        (2, rows_of(-2, 2), True),
    )
    no_outer = (r == 0) | (r == n_rows - 1)
    at_edge = (c == 0) | (c == n_cols - 1)
    own_j = c == 0
    own_j = own_j.astype(jnp.int32)

    def send_tile(chunk, to_r, to_c, there):
        rows, where, is_outer = chunks[chunk]
        src, dst = where(to_r)
        skip = (to_c == 0).astype(jnp.int32)
        edge = (to_c == 0) | (to_c == n_cols - 1)
        if is_outer:
            there = there & (to_r > 0) & (to_r < n_rows - 1)

        def copy(count, src_j, dst_j):
            pltpu.make_async_remote_copy(
                src_ref=packed.at[pl.ds(src, rows), pl.ds(src_j, count)],
                dst_ref=recv.at[me, pl.ds(dst, rows), pl.ds(dst_j, count)],
                send_sem=send_sem.at[chunk],
                recv_sem=recv_sem.at[chunk],
                device_id=device(to_r, to_c),
                device_id_type=MESH,
            ).start()

        pl.when(there & edge)(lambda: copy(win_j - 1, tile_j * to_c - 1 + skip, skip))
        pl.when(there & jnp.logical_not(edge))(lambda: copy(win_j, tile_j * to_c - 1, 0))

    chips = n_rows // 2
    ahead_r, ahead_c = AHEAD

    def step(t, table):
        value = jnp.int32(table[-1])
        for k, entry in enumerate(table[:-1]):
            value = jnp.where(t == k, entry, value)
        return value

    def turn_to(t):
        dx = step(t, CHIPS_ALONG)
        return lax.rem(r // 2 + dx, chips), dx

    def send_chip(chunk, t, rest, where=None):
        x, dx = turn_to(t)
        way = 1 - 2 * lax.rem(par + t, 2)
        for other, dy in CHIP_ORDER:
            to_r = 2 * x + (1 - par if other else par)
            to_c = lax.rem(c + way * dy + n_cols, n_cols)
            there = True
            if not other and dy == 0:
                there = dx > 0
            if rest:
                there = there & jnp.logical_not((to_r == ahead_r) & (to_c == ahead_c))
            if where is not None:
                there = there & where(to_c)
            send_tile(chunk, to_r, to_c, there)

    def send_ahead(chunk):
        send_tile(chunk, jnp.int32(ahead_r), jnp.int32(ahead_c), (r != ahead_r) | (c != ahead_c))

    def send_chunk(chunk):

        def first_column(t, carry):
            x, _ = turn_to(t)
            for other in range(2):
                to_r = 2 * x + (1 - par if other else par)
                there = ((to_r != r) | (c != 0)) & (to_r != ahead_r)
                send_tile(chunk, to_r, jnp.int32(0), there)
            return carry

        where = None
        if chunk in COLUMN_FIRST:
            lax.fori_loop(0, chips, first_column, 0)
            where = lambda to_c: to_c > 0

        def body(t, carry):
            send_chip(chunk, t, True, where)
            return carry

        lax.fori_loop(0, chips, body, 0)

    params[0].wait()
    for dw in range(3):
        w1own[dw] = jnp.concatenate([w1s[1, dw], w1s[0, dw]], axis=1)
    w1own[3] = jnp.concatenate([w1s[2, 0], w1s[2, 1]], axis=1)
    w1own[4] = jnp.concatenate([w1s[2, 2], jnp.zeros_like(w1s[2, 2])], axis=1)
    w1all[r // 2, par, c] = w1own[...]

    for copy in loads[0]:
        copy.wait()
    pack_rows(turn_to(0)[0], *groups[0][0])
    pl.semaphore_wait(barrier, sources - 1)

    def send_weights():
        for kr in range(0, n_rows, 2):
            for kc in range(n_cols):
                if kr or kc:
                    pltpu.make_async_remote_copy(
                        src_ref=w1own,
                        dst_ref=w1all.at[r // 2, par, c],
                        send_sem=wsend_sem,
                        recv_sem=wrecv_sem,
                        device_id=device(to_rs[kr], to_cs[kc]),
                        device_id_type=MESH,
                    ).start()

    def pack_and_send(t, carry):
        pl.when(t < chips - 1)(lambda: pack_rows(turn_to(t + 1)[0], *groups[0][0]))
        send_chip(0, t, False)
        pl.when(t == 0)(send_weights)
        return carry

    lax.fori_loop(0, chips, pack_and_send, 0)

    pack(1)
    send_ahead(1)
    send_chunk(1)
    pack(2)
    send_ahead(2)
    send_ahead(3)
    send_chunk(2)
    send_chunk(3)

    def own_rows(chunk):
        rows, where, _ = chunks[chunk]
        src, dst = where(r)

        def copy(count, src_j, dst_j):
            for h in range(rows):
                recv[me, dst + h, pl.ds(dst_j, count)] = packed[src + h, pl.ds(src_j, count)]

        pl.when(at_edge)(lambda: copy(win_j - 1, tile_j * c - 1 + own_j, own_j))
        pl.when(jnp.logical_not(at_edge))(lambda: copy(win_j, tile_j * c - 1, 0))

    for chunk in range(3):
        own_rows(chunk)
    pl.when(jnp.logical_not(no_outer))(lambda: own_rows(3))

    zero_row = jnp.zeros((win_j, 2, 2 * images), BF16)
    zero_col = jnp.zeros((tile_h + 2, 2, 2 * images), BF16)

    def clear(s, carry):
        recv[s, last * (1 - par)] = zero_row
        return carry

    def clear_outer(s, carry):
        recv[s, (last - 1) * par] = zero_row
        recv[s, (last - 1) * par + 1] = zero_row
        return carry

    def clear_edge(s, carry):
        recv[s, pl.ds(3 * par, tile_h + 2), (win_j - 1) * (1 - own_j)] = zero_col
        return carry

    lax.fori_loop(0, sources, clear, 0)
    pl.when(no_outer)(lambda: (lax.fori_loop(0, sources, clear_outer, 0), None)[1])
    pl.when(at_edge)(lambda: (lax.fori_loop(0, sources, clear_edge, 0), None)[1])

    low = lax.broadcasted_iota(jnp.int32, (chans, 2 * chans), 1) < chans

    def spread(wt, u, v, dw):
        ur, vr = pltpu.roll(u, chans, 1), pltpu.roll(v, chans, 1)
        zero = jnp.zeros_like(u)
        tiles = (jnp.where(low, ur, zero), u, jnp.where(low, v, ur), jnp.where(low, zero, vr))
        for k, tile in enumerate(tiles):
            tile = tile.astype(BF16)
            for b in range(2):
                wt[dw + b, k * chans : (k + 1) * chans, b * 2 * chans : (b + 1) * 2 * chans] = tile

    def blank(wt):
        zero = jnp.zeros((4 * chans, 2 * chans), BF16)
        wt[3, :, 0 : 2 * chans] = zero
        wt[0, :, 2 * chans : 4 * chans] = zero

    for copy in params[1:]:
        copy.wait()
    blank(wt1)
    blank(wt2)
    for dw in range(3):
        w = [w2s[dh, dw].astype(F32) for dh in range(3)]
        spread(
            wt2,
            jnp.concatenate([w[1], w[0]], axis=1),
            jnp.concatenate([w[2], jnp.zeros_like(w[2])], axis=1),
            dw,
        )
    bias1[...] = jnp.concatenate([b1s[...]] * 4, axis=1)
    bias2[...] = jnp.concatenate([b2s[...]] * 4, axis=1)

    def wait_bytes(ref, sem):
        pltpu.make_async_copy(ref, ref, sem).wait()

    w1_bytes = recv.at[0 : sources // 2 - 1, 0, 0:5]
    wait_bytes(w1_bytes, wrecv_sem)
    wait_bytes(w1_bytes, wsend_sem)
    partner = device(r + 1 - 2 * par, c)
    w_swap = pltpu.make_async_remote_copy(
        src_ref=w1all.at[:, par],
        dst_ref=w1all.at[:, par],
        send_sem=wswap_send_sem,
        recv_sem=wswap_recv_sem,
        device_id=partner,
        device_id_type=MESH,
    )
    w_swap.start()

    def arrived(chunk):
        def wait(count):
            wait_bytes(recv.at[0 : sources - 1, 0 : chunks[chunk][0], 0:count], recv_sem.at[chunk])

        pl.when(at_edge)(lambda: wait(win_j - 1))
        pl.when(jnp.logical_not(at_edge))(lambda: wait(win_j))

    arrived(0)
    give = tile_h - (tile_h - 3) * par
    land = tile_h + 2 - (tile_h + 1) * (1 - par)
    swap = pltpu.make_async_remote_copy(
        src_ref=recv.at[:, pl.ds(give, 2)],
        dst_ref=recv.at[:, pl.ds(land, 2)],
        send_sem=swap_send_sem,
        recv_sem=swap_recv_sem,
        device_id=partner,
        device_id_type=MESH,
    )
    swap.start()

    w_swap.wait()
    u = [w1all[:, :, :, k].reshape(chans, 2 * chans).astype(F32) for k in range(5)]
    for dw in range(3):
        v = (u[3], pltpu.roll(u[3], chans, 1), u[4])[dw]
        spread(wt1, u[dw], jnp.where(low, v, 0.0), dw)

    x_pairs, z_pairs = xmat.shape[0], ymat.shape[0]
    o_pairs = z_pairs - 1

    def nth(n, count):
        return (count - 1) * (1 - par) + n * (2 * par - 1)

    def turn_one(n, carry):
        i = nth(n, x_pairs)

        def put(j, value):
            xmat[i, j] = value

        turn(recv, i, put)
        return carry

    def first_one(n, carry):
        i = nth(n, z_pairs)
        fill = jnp.where(n == 0, 1 - par, 2)
        out_of = jnp.where(n == z_pairs - 1, jnp.where(r == 0, 0, jnp.where(r == n_rows - 1, 1, 2)), 2)
        blank_a = jnp.where(fill < 2, fill, out_of)
        first((xmat.at[i], xmat.at[i + 1]), lambda dw: wt1[dw], bias1[...], ymat.at[i], blank_a)
        return carry

    def second_one(n, carry):
        i = nth(n, o_pairs)
        second((ymat.at[i], ymat.at[i + 1]), lambda dw: wt2[dw], bias2[...], out.at[pl.ds(2 * i, 2)])
        return carry

    def stage(s, carry):
        @pl.when(s == 0)
        def _():
            swap.wait()

        for k in range(1, 4):
            there = s == k
            if k == 3:
                there = there & jnp.logical_not(no_outer)
            pl.when(there)(lambda k=k: arrived(k))

        later = (s + 3) // 4
        lax.fori_loop((2 + s) * later, 3 + s, turn_one, 0)
        lax.fori_loop((1 + s) * later, 2 + s, first_one, 0)
        lax.fori_loop(s, 1 + s - s // 3, second_one, 0)
        return carry

    lax.fori_loop(0, 4, stage, 0)

    per_edge = n_rows * 2
    for chunk in range(4):
        rows = chunks[chunk][0]
        n_r = n_rows - 2 if chunk == 3 else n_rows
        counts = (n_r * 2, n_r * (n_cols - 2))

        def drain(edge_n, inner_n, rows=rows, chunk=chunk):
            wait_bytes(recv.at[0:edge_n, 0:rows, 0 : win_j - 1], send_sem.at[chunk])
            wait_bytes(recv.at[0:inner_n, 0:rows, 0:win_j], send_sem.at[chunk])

        def drain_own(chunk=chunk, counts=counts, drain=drain):
            pl.when(at_edge)(lambda: drain(counts[0] - 1, counts[1]))
            pl.when(jnp.logical_not(at_edge))(lambda: drain(counts[0], counts[1] - 1))

        if chunk == 3:
            pl.when(no_outer)(lambda: drain(*counts))
            pl.when(jnp.logical_not(no_outer))(drain_own)
        else:
            drain_own()


def tail_kernel(tile, ymat, wt2, bias2, out_hbm, o_new, sem):
    par = lax.rem(lax.axis_index("model"), 2)
    rows = out_hbm.shape[0]
    o_pairs = ymat.shape[0] - 1
    late = (rows - 2) * par
    here = 2 * (1 - par)

    def start(k, carry):
        pltpu.make_async_copy(tile.at[par + k], out_hbm.at[k], sem.at[0]).start()
        return carry

    lax.fori_loop(here, here + rows - 2, start, 0)
    i = (o_pairs - 1) * par
    second((ymat.at[i], ymat.at[i + 1]), lambda dw: wt2[dw], bias2[...], o_new)
    last = pltpu.make_async_copy(o_new, out_hbm.at[pl.ds(late, 2)], sem.at[1])
    last.start()
    pltpu.make_async_copy(tile.at[0 : rows - 2], out_hbm.at[0 : rows - 2], sem.at[0]).wait()
    last.wait()


def solution(mesh):
    n_rows = mesh.shape["model"]
    n_cols = mesh.shape["cols"]

    def run_local(x_in, w_conv1, b_conv1, w_conv2, b_conv2):
        images, height, width, own_chans = x_in.shape
        sources = n_rows * n_cols
        chans = own_chans * sources
        pairs = width // 2
        tile_h, tile_j = height // n_rows, pairs // n_cols
        win_j = tile_j + 2
        x_pairs, z_pairs = (tile_h + 5) // 2, (tile_h + 3) // 2
        x_t = jnp.transpose(x_in, (1, 2, 3, 0)).reshape(n_rows // 2, 2 * tile_h, pairs, 2, own_chans, images)
        args = (x_t, w_conv1, b_conv1.reshape(1, chans), w_conv2, b_conv2.reshape(1, chans))
        hbm = pl.BlockSpec(memory_space=pltpu.HBM)
        vmem = pl.BlockSpec(memory_space=pltpu.VMEM)
        kept = (
            pltpu.VMEM((2 * (z_pairs - 1), tile_j, 2, images, chans), F32),
            pltpu.VMEM((z_pairs, win_j - 1, 2, images, 2 * chans), BF16),
            pltpu.VMEM((4, 4 * chans, 4 * chans), BF16),
            pltpu.VMEM((1, 4 * chans), F32),
        )
        state = pl.pallas_call(
            functools.partial(conv_kernel, n_rows, n_cols),
            out_shape=kept,
            in_specs=[hbm] * 5,
            out_specs=[vmem] * len(kept),
            scratch_shapes=[
                pltpu.VMEM((sources, 2 * x_pairs, win_j, own_chans, 2 * images), BF16),
                pltpu.VMEM((x_pairs, win_j, 2, images, 2 * chans), BF16),
                pltpu.VMEM((4, 4 * chans, 4 * chans), BF16),
                pltpu.VMEM((1, 4 * chans), F32),
                pltpu.VMEM((n_rows // 2, 2 * tile_h, pairs, 2, own_chans, images), BF16),
                pltpu.VMEM((height, pairs, own_chans, 2 * images), BF16),
                pltpu.VMEM((3, 3, own_chans, chans), BF16),
                pltpu.VMEM((5, own_chans, 2 * chans), BF16),
                pltpu.VMEM((n_rows // 2, 2, n_cols, 5, own_chans, 2 * chans), BF16),
                pltpu.VMEM((3, 3, chans, chans), BF16),
                pltpu.VMEM((1, chans), F32),
                pltpu.VMEM((1, chans), F32),
                pltpu.SemaphoreType.DMA((3, 2)),
                pltpu.SemaphoreType.DMA((4,)),
                pltpu.SemaphoreType.DMA((4,)),
                pltpu.SemaphoreType.DMA((4,)),
            ]
            + [pltpu.SemaphoreType.DMA] * 6,
            compiler_params=pltpu.CompilerParams(
                collective_id=0, has_side_effects=True, vmem_limit_bytes=24 << 20
            ),
            name="conv",
        )(*(pltpu.with_memory_space_constraint(a, pltpu.HBM) for a in args))
        out = pl.pallas_call(
            tail_kernel,
            out_shape=jax.ShapeDtypeStruct((tile_h, tile_j, 2, images, chans), F32),
            in_specs=[vmem] * len(kept),
            out_specs=pl.BlockSpec(memory_space=pl.ANY),
            scratch_shapes=[
                pltpu.VMEM((2, tile_j, 2, images, chans), F32),
                pltpu.SemaphoreType.DMA((2,)),
            ],
            compiler_params=pltpu.CompilerParams(vmem_limit_bytes=8 << 20),
            name="tail",
        )(*state)
        out = out.reshape(tile_h, 2 * tile_j, images, chans)
        return jnp.transpose(out, (2, 0, 1, 3))

    group = ("model", "cols")
    return jax.shard_map(
        run_local,
        mesh=mesh,
        in_specs=(P("data", None, None, group), P(None, None, group, None), P(), P(), P()),
        out_specs=P("data", "model", "cols", None),
        check_vma=False,
    )
```

```python
import functools

import jax
import jax.numpy as jnp
from jax import lax
from jax.experimental import pallas as pl
from jax.experimental.pallas import tpu as pltpu
from jax.sharding import PartitionSpec as P

MESH = pl.DeviceIdType.MESH
BF16 = jnp.bfloat16
F32 = jnp.float32
FIRST_ROWS = 3
AHEAD = (1, 0)
COLUMN_FIRST = (2, 3)
CHIPS_ALONG = (1, 3, 2, 0)
CHIP_ORDER = tuple((other, dy) for other in (0, 1) for dy in (1, -1, 0, 2))


def turn(recv, i, put):
    sources, _, win_j, own_chans, lanes = recv.shape
    chans = sources * own_chans
    for j in range(win_j):
        top = recv[:, 2 * i, j].reshape(chans, lanes)
        under = recv[:, 2 * i + 1, j].reshape(chans, lanes)
        put(j, jnp.concatenate([top, under], axis=0).T.reshape(2, lanes // 2, 2 * chans))


def blocks(pairs, weights, count):
    acc = None
    for dw in range(4):
        parts = [view[dw // 2 : dw // 2 + count, dw % 2] for view in pairs]
        lhs = jnp.concatenate([p.reshape(count * p.shape[1], p.shape[2]) for p in parts], axis=1)
        term = jnp.dot(lhs, weights(dw), preferred_element_type=F32)
        acc = term if acc is None else acc + term
    return acc


def first(pairs, weights, bias, y_row, blank_a):
    count, _, images, lanes = y_row.shape
    c = lax.axis_index("cols")
    row = lax.rem(lax.broadcasted_iota(jnp.int32, (1, 2 * lanes), 1), lanes) // (lanes // 2)
    act = jnp.maximum(blocks(pairs, weights, count) + bias, 0.0)
    act = jnp.where(row != blank_a, act, 0.0).astype(BF16)
    for b in range(2):
        y_row[:, b] = act[:, b * lanes : (b + 1) * lanes].reshape(count, images, lanes)
    blank = jnp.zeros((images, lanes), BF16)

    @pl.when(c == 0)
    def _():
        y_row[0, 0] = blank

    @pl.when(c == lax.axis_size("cols") - 1)
    def _():
        y_row[count - 1, 1] = blank


def second(pairs, weights, bias, out_pair):
    _, count, _, images, chans = out_pair.shape
    res = blocks(pairs, weights, count) + bias
    for b in range(2):
        for a in range(2):
            at = (2 * b + a) * chans
            out_pair[a, :, b] = res[:, at : at + chans].reshape(count, images, chans)


def conv_kernel(
    n_rows,
    n_cols,
    x_hbm,
    w1_hbm,
    b1_hbm,
    w2_hbm,
    b2_hbm,
    out,
    ymat,
    wt2,
    bias2,
    recv,
    xmat,
    wt1,
    bias1,
    xs,
    packed,
    w1s,
    w1own,
    w1all,
    w2s,
    b1s,
    b2s,
    load_sem,
    par_sem,
    send_sem,
    recv_sem,
    wsend_sem,
    wrecv_sem,
    swap_send_sem,
    swap_recv_sem,
    wswap_send_sem,
    wswap_recv_sem,
):
    chip_h, pairs = xs.shape[1:3]
    images = xs.shape[-1]
    tile_h, tile_j = chip_h // 2, pairs // n_cols
    win_j = tile_j + 2
    sources = n_rows * n_cols
    r, c = lax.axis_index("model"), lax.axis_index("cols")
    par = lax.rem(r, 2)
    me = r * n_cols + c
    chans = recv.shape[0] * 2

    near = tile_h - FIRST_ROWS
    groups = (((near, chip_h - near),), *(((k, k + 2), (chip_h - k - 2, chip_h - k)) for k in range(near - 2, -1, -2)))
    loads = []
    for g, spans in enumerate(groups):
        loads.append(
            [
                pltpu.make_async_copy(x_hbm.at[:, lo:hi], xs.at[:, lo:hi], load_sem.at[g, n])
                for n, (lo, hi) in enumerate(spans)
            ]
        )
    for copies in loads:
        for copy in copies:
            copy.start()
    params = [
        pltpu.make_async_copy(src, dst, par_sem.at[s])
        for s, (src, dst) in enumerate(((w1_hbm, w1s), (w2_hbm, w2s), (b1_hbm, b1s), (b2_hbm, b2s)))
    ]
    for copy in params:
        copy.start()

    barrier = pltpu.get_barrier_semaphore()
    to_cs = [lax.rem(c + k, n_cols) for k in range(n_cols)]

    def device(to_r, to_c):
        return {"model": to_r, "cols": to_c}

    to_rs = [lax.rem(r + k, n_rows) for k in range(n_rows)]
    for kr, kc in sorted(
        ((kr, kc) for kr in range(n_rows) for kc in range(n_cols) if kr or kc),
        key=lambda k: (not (k[0] in (2, 3) and k[1] == 1), -(min(k[0], n_rows - k[0]) // 2 + min(k[1], n_cols - k[1]))),
    ):
        pl.semaphore_signal(barrier, inc=1, device_id=device(to_rs[kr], to_cs[kc]), device_id_type=MESH)

    def pack_rows(x, lo, hi):
        rows = hi - lo
        left, right = (xs[x, lo:hi, :, p].reshape(rows * pairs * 2, images) for p in range(2))
        both = jnp.concatenate([left, right], axis=1)
        packed[pl.ds(chip_h * x + lo, rows)] = both.reshape(rows, pairs, 2, 2 * images)

    def pack(g):
        for copy in loads[g]:
            copy.wait()

        def body(x, carry):
            for lo, hi in groups[g]:
                pack_rows(x, lo, hi)
            return carry

        lax.fori_loop(0, n_rows // 2, body, 0)

    last = tile_h + 4

    def rows_of(offset, count):
        def where(to_r):
            q = lax.rem(to_r, 2)
            src = tile_h * to_r + offset + (tile_h - count - 2 * offset) * q
            dst = offset + 2 + (last - count - 2 * offset - 3) * q
            return src, dst

        return where

    chunks = (
        (FIRST_ROWS, rows_of(near, FIRST_ROWS), False),
        *((2, rows_of(k, 2), False) for k in range(near - 2, -1, -2)),
        (2, rows_of(-2, 2), True),
    )
    no_outer = (r == 0) | (r == n_rows - 1)
    at_edge = (c == 0) | (c == n_cols - 1)
    own_j = c == 0
    own_j = own_j.astype(jnp.int32)

    def send_tile(chunk, to_r, to_c, there):
        rows, where, is_outer = chunks[chunk]
        src, dst = where(to_r)
        skip = (to_c == 0).astype(jnp.int32)
        edge = (to_c == 0) | (to_c == n_cols - 1)
        if is_outer:
            there = there & (to_r > 0) & (to_r < n_rows - 1)

        def copy(count, src_j, dst_j):
            pltpu.make_async_remote_copy(
                src_ref=packed.at[pl.ds(src, rows), pl.ds(src_j, count)],
                dst_ref=recv.at[me, pl.ds(dst, rows), pl.ds(dst_j, count)],
                send_sem=send_sem.at[chunk],
                recv_sem=recv_sem.at[chunk],
                device_id=device(to_r, to_c),
                device_id_type=MESH,
            ).start()

        pl.when(there & edge)(lambda: copy(win_j - 1, tile_j * to_c - 1 + skip, skip))
        pl.when(there & jnp.logical_not(edge))(lambda: copy(win_j, tile_j * to_c - 1, 0))

    chips = n_rows // 2
    ahead_r, ahead_c = AHEAD

    def step(t, table):
        value = jnp.int32(table[-1])
        for k, entry in enumerate(table[:-1]):
            value = jnp.where(t == k, entry, value)
        return value

    def turn_to(t):
        dx = step(t, CHIPS_ALONG)
        return lax.rem(r // 2 + dx, chips), dx

    def send_chip(chunk, t, rest, where=None):
        x, dx = turn_to(t)
        way = 1 - 2 * par
        for other, dy in CHIP_ORDER:
            to_r = 2 * x + (1 - par if other else par)
            to_c = lax.rem(c + way * dy + n_cols, n_cols)
            there = True
            if not other and dy == 0:
                there = dx > 0
            if rest:
                there = there & jnp.logical_not((to_r == ahead_r) & (to_c == ahead_c))
            if where is not None:
                there = there & where(to_c)
            send_tile(chunk, to_r, to_c, there)

    def send_ahead(chunk):
        send_tile(chunk, jnp.int32(ahead_r), jnp.int32(ahead_c), (r != ahead_r) | (c != ahead_c))

    def send_chunk(chunk):

        def first_column(t, carry):
            x, _ = turn_to(t)
            for other in range(2):
                to_r = 2 * x + (1 - par if other else par)
                there = ((to_r != r) | (c != 0)) & (to_r != ahead_r)
                send_tile(chunk, to_r, jnp.int32(0), there)
            return carry

        where = None
        if chunk in COLUMN_FIRST:
            lax.fori_loop(0, chips, first_column, 0)
            where = lambda to_c: to_c > 0

        def body(t, carry):
            send_chip(chunk, t, True, where)
            return carry

        lax.fori_loop(0, chips, body, 0)

    params[0].wait()
    for dw in range(3):
        w1own[dw] = jnp.concatenate([w1s[1, dw], w1s[0, dw]], axis=1)
    w1own[3] = jnp.concatenate([w1s[2, 0], w1s[2, 1]], axis=1)
    w1own[4] = jnp.concatenate([w1s[2, 2], jnp.zeros_like(w1s[2, 2])], axis=1)
    w1all[r // 2, par, c] = w1own[...]

    for copy in loads[0]:
        copy.wait()
    pack_rows(turn_to(0)[0], *groups[0][0])
    pl.semaphore_wait(barrier, sources - 1)

    def send_weights():
        for kr in range(0, n_rows, 2):
            for kc in range(n_cols):
                if kr or kc:
                    pltpu.make_async_remote_copy(
                        src_ref=w1own,
                        dst_ref=w1all.at[r // 2, par, c],
                        send_sem=wsend_sem,
                        recv_sem=wrecv_sem,
                        device_id=device(to_rs[kr], to_cs[kc]),
                        device_id_type=MESH,
                    ).start()

    def pack_and_send(t, carry):
        pl.when(t < chips - 1)(lambda: pack_rows(turn_to(t + 1)[0], *groups[0][0]))
        send_chip(0, t, False)
        pl.when(t == 0)(send_weights)
        return carry

    lax.fori_loop(0, chips, pack_and_send, 0)

    pack(1)
    send_ahead(1)
    send_chunk(1)
    pack(2)
    send_ahead(2)
    send_ahead(3)
    send_chunk(2)
    send_chunk(3)

    def own_rows(chunk):
        rows, where, _ = chunks[chunk]
        src, dst = where(r)

        def copy(count, src_j, dst_j):
            for h in range(rows):
                recv[me, dst + h, pl.ds(dst_j, count)] = packed[src + h, pl.ds(src_j, count)]

        pl.when(at_edge)(lambda: copy(win_j - 1, tile_j * c - 1 + own_j, own_j))
        pl.when(jnp.logical_not(at_edge))(lambda: copy(win_j, tile_j * c - 1, 0))

    for chunk in range(3):
        own_rows(chunk)
    pl.when(jnp.logical_not(no_outer))(lambda: own_rows(3))

    zero_row = jnp.zeros((win_j, 2, 2 * images), BF16)
    zero_col = jnp.zeros((tile_h + 2, 2, 2 * images), BF16)

    def clear(s, carry):
        recv[s, last * (1 - par)] = zero_row
        return carry

    def clear_outer(s, carry):
        recv[s, (last - 1) * par] = zero_row
        recv[s, (last - 1) * par + 1] = zero_row
        return carry

    def clear_edge(s, carry):
        recv[s, pl.ds(3 * par, tile_h + 2), (win_j - 1) * (1 - own_j)] = zero_col
        return carry

    lax.fori_loop(0, sources, clear, 0)
    pl.when(no_outer)(lambda: (lax.fori_loop(0, sources, clear_outer, 0), None)[1])
    pl.when(at_edge)(lambda: (lax.fori_loop(0, sources, clear_edge, 0), None)[1])

    low = lax.broadcasted_iota(jnp.int32, (chans, 2 * chans), 1) < chans

    def spread(wt, u, v, dw):
        ur, vr = pltpu.roll(u, chans, 1), pltpu.roll(v, chans, 1)
        zero = jnp.zeros_like(u)
        tiles = (jnp.where(low, ur, zero), u, jnp.where(low, v, ur), jnp.where(low, zero, vr))
        for k, tile in enumerate(tiles):
            tile = tile.astype(BF16)
            for b in range(2):
                wt[dw + b, k * chans : (k + 1) * chans, b * 2 * chans : (b + 1) * 2 * chans] = tile

    def blank(wt):
        zero = jnp.zeros((4 * chans, 2 * chans), BF16)
        wt[3, :, 0 : 2 * chans] = zero
        wt[0, :, 2 * chans : 4 * chans] = zero

    for copy in params[1:]:
        copy.wait()
    blank(wt1)
    blank(wt2)
    for dw in range(3):
        w = [w2s[dh, dw].astype(F32) for dh in range(3)]
        spread(
            wt2,
            jnp.concatenate([w[1], w[0]], axis=1),
            jnp.concatenate([w[2], jnp.zeros_like(w[2])], axis=1),
            dw,
        )
    bias1[...] = jnp.concatenate([b1s[...]] * 4, axis=1)
    bias2[...] = jnp.concatenate([b2s[...]] * 4, axis=1)

    def wait_bytes(ref, sem):
        pltpu.make_async_copy(ref, ref, sem).wait()

    w1_bytes = recv.at[0 : sources // 2 - 1, 0, 0:5]
    wait_bytes(w1_bytes, wrecv_sem)
    wait_bytes(w1_bytes, wsend_sem)
    partner = device(r + 1 - 2 * par, c)
    w_swap = pltpu.make_async_remote_copy(
        src_ref=w1all.at[:, par],
        dst_ref=w1all.at[:, par],
        send_sem=wswap_send_sem,
        recv_sem=wswap_recv_sem,
        device_id=partner,
        device_id_type=MESH,
    )
    w_swap.start()

    def arrived(chunk):
        def wait(count):
            wait_bytes(recv.at[0 : sources - 1, 0 : chunks[chunk][0], 0:count], recv_sem.at[chunk])

        pl.when(at_edge)(lambda: wait(win_j - 1))
        pl.when(jnp.logical_not(at_edge))(lambda: wait(win_j))

    arrived(0)
    give = tile_h - (tile_h - 3) * par
    land = tile_h + 2 - (tile_h + 1) * (1 - par)
    swap = pltpu.make_async_remote_copy(
        src_ref=recv.at[:, pl.ds(give, 2)],
        dst_ref=recv.at[:, pl.ds(land, 2)],
        send_sem=swap_send_sem,
        recv_sem=swap_recv_sem,
        device_id=partner,
        device_id_type=MESH,
    )
    swap.start()

    w_swap.wait()
    u = [w1all[:, :, :, k].reshape(chans, 2 * chans).astype(F32) for k in range(5)]
    for dw in range(3):
        v = (u[3], pltpu.roll(u[3], chans, 1), u[4])[dw]
        spread(wt1, u[dw], jnp.where(low, v, 0.0), dw)

    x_pairs, z_pairs = xmat.shape[0], ymat.shape[0]
    o_pairs = z_pairs - 1

    def nth(n, count):
        return (count - 1) * (1 - par) + n * (2 * par - 1)

    def turn_one(n, carry):
        i = nth(n, x_pairs)

        def put(j, value):
            xmat[i, j] = value

        turn(recv, i, put)
        return carry

    def first_one(n, carry):
        i = nth(n, z_pairs)
        fill = jnp.where(n == 0, 1 - par, 2)
        out_of = jnp.where(n == z_pairs - 1, jnp.where(r == 0, 0, jnp.where(r == n_rows - 1, 1, 2)), 2)
        blank_a = jnp.where(fill < 2, fill, out_of)
        first((xmat.at[i], xmat.at[i + 1]), lambda dw: wt1[dw], bias1[...], ymat.at[i], blank_a)
        return carry

    def second_one(n, carry):
        i = nth(n, o_pairs)
        second((ymat.at[i], ymat.at[i + 1]), lambda dw: wt2[dw], bias2[...], out.at[pl.ds(2 * i, 2)])
        return carry

    def stage(s, carry):
        @pl.when(s == 0)
        def _():
            swap.wait()

        for k in range(1, 4):
            there = s == k
            if k == 3:
                there = there & jnp.logical_not(no_outer)
            pl.when(there)(lambda k=k: arrived(k))

        later = (s + 3) // 4
        lax.fori_loop((2 + s) * later, 3 + s, turn_one, 0)
        lax.fori_loop((1 + s) * later, 2 + s, first_one, 0)
        lax.fori_loop(s, 1 + s - s // 3, second_one, 0)
        return carry

    lax.fori_loop(0, 4, stage, 0)

    per_edge = n_rows * 2
    for chunk in range(4):
        rows = chunks[chunk][0]
        n_r = n_rows - 2 if chunk == 3 else n_rows
        counts = (n_r * 2, n_r * (n_cols - 2))

        def drain(edge_n, inner_n, rows=rows, chunk=chunk):
            wait_bytes(recv.at[0:edge_n, 0:rows, 0 : win_j - 1], send_sem.at[chunk])
            wait_bytes(recv.at[0:inner_n, 0:rows, 0:win_j], send_sem.at[chunk])

        def drain_own(chunk=chunk, counts=counts, drain=drain):
            pl.when(at_edge)(lambda: drain(counts[0] - 1, counts[1]))
            pl.when(jnp.logical_not(at_edge))(lambda: drain(counts[0], counts[1] - 1))

        if chunk == 3:
            pl.when(no_outer)(lambda: drain(*counts))
            pl.when(jnp.logical_not(no_outer))(drain_own)
        else:
            drain_own()


def tail_kernel(tile, ymat, wt2, bias2, out_hbm, o_new, sem):
    par = lax.rem(lax.axis_index("model"), 2)
    rows = out_hbm.shape[0]
    o_pairs = ymat.shape[0] - 1
    late = (rows - 2) * par
    here = 2 * (1 - par)

    def start(k, carry):
        pltpu.make_async_copy(tile.at[par + k], out_hbm.at[k], sem.at[0]).start()
        return carry

    lax.fori_loop(here, here + rows - 2, start, 0)
    i = (o_pairs - 1) * par
    second((ymat.at[i], ymat.at[i + 1]), lambda dw: wt2[dw], bias2[...], o_new)
    last = pltpu.make_async_copy(o_new, out_hbm.at[pl.ds(late, 2)], sem.at[1])
    last.start()
    pltpu.make_async_copy(tile.at[0 : rows - 2], out_hbm.at[0 : rows - 2], sem.at[0]).wait()
    last.wait()


def solution(mesh):
    n_rows = mesh.shape["model"]
    n_cols = mesh.shape["cols"]

    def run_local(x_in, w_conv1, b_conv1, w_conv2, b_conv2):
        images, height, width, own_chans = x_in.shape
        sources = n_rows * n_cols
        chans = own_chans * sources
        pairs = width // 2
        tile_h, tile_j = height // n_rows, pairs // n_cols
        win_j = tile_j + 2
        x_pairs, z_pairs = (tile_h + 5) // 2, (tile_h + 3) // 2
        x_t = jnp.transpose(x_in, (1, 2, 3, 0)).reshape(n_rows // 2, 2 * tile_h, pairs, 2, own_chans, images)
        args = (x_t, w_conv1, b_conv1.reshape(1, chans), w_conv2, b_conv2.reshape(1, chans))
        hbm = pl.BlockSpec(memory_space=pltpu.HBM)
        vmem = pl.BlockSpec(memory_space=pltpu.VMEM)
        kept = (
            pltpu.VMEM((2 * (z_pairs - 1), tile_j, 2, images, chans), F32),
            pltpu.VMEM((z_pairs, win_j - 1, 2, images, 2 * chans), BF16),
            pltpu.VMEM((4, 4 * chans, 4 * chans), BF16),
            pltpu.VMEM((1, 4 * chans), F32),
        )
        state = pl.pallas_call(
            functools.partial(conv_kernel, n_rows, n_cols),
            out_shape=kept,
            in_specs=[hbm] * 5,
            out_specs=[vmem] * len(kept),
            scratch_shapes=[
                pltpu.VMEM((sources, 2 * x_pairs, win_j, own_chans, 2 * images), BF16),
                pltpu.VMEM((x_pairs, win_j, 2, images, 2 * chans), BF16),
                pltpu.VMEM((4, 4 * chans, 4 * chans), BF16),
                pltpu.VMEM((1, 4 * chans), F32),
                pltpu.VMEM((n_rows // 2, 2 * tile_h, pairs, 2, own_chans, images), BF16),
                pltpu.VMEM((height, pairs, own_chans, 2 * images), BF16),
                pltpu.VMEM((3, 3, own_chans, chans), BF16),
                pltpu.VMEM((5, own_chans, 2 * chans), BF16),
                pltpu.VMEM((n_rows // 2, 2, n_cols, 5, own_chans, 2 * chans), BF16),
                pltpu.VMEM((3, 3, chans, chans), BF16),
                pltpu.VMEM((1, chans), F32),
                pltpu.VMEM((1, chans), F32),
                pltpu.SemaphoreType.DMA((3, 2)),
                pltpu.SemaphoreType.DMA((4,)),
                pltpu.SemaphoreType.DMA((4,)),
                pltpu.SemaphoreType.DMA((4,)),
            ]
            + [pltpu.SemaphoreType.DMA] * 6,
            compiler_params=pltpu.CompilerParams(
                collective_id=0, has_side_effects=True, vmem_limit_bytes=24 << 20
            ),
            name="conv",
        )(*(pltpu.with_memory_space_constraint(a, pltpu.HBM) for a in args))
        out = pl.pallas_call(
            tail_kernel,
            out_shape=jax.ShapeDtypeStruct((tile_h, tile_j, 2, images, chans), F32),
            in_specs=[vmem] * len(kept),
            out_specs=pl.BlockSpec(memory_space=pl.ANY),
            scratch_shapes=[
                pltpu.VMEM((2, tile_j, 2, images, chans), F32),
                pltpu.SemaphoreType.DMA((2,)),
            ],
            compiler_params=pltpu.CompilerParams(vmem_limit_bytes=8 << 20),
            name="tail",
        )(*state)
        out = out.reshape(tile_h, 2 * tile_j, images, chans)
        return jnp.transpose(out, (2, 0, 1, 3))

    group = ("model", "cols")
    return jax.shard_map(
        run_local,
        mesh=mesh,
        in_specs=(P("data", None, None, group), P(None, None, group, None), P(), P(), P()),
        out_specs=P("data", "model", "cols", None),
        check_vma=False,
    )
```

```python
import functools

import jax
import jax.numpy as jnp
from jax import lax
from jax.experimental import pallas as pl
from jax.experimental.pallas import tpu as pltpu
from jax.sharding import PartitionSpec as P

MESH = pl.DeviceIdType.MESH
BF16 = jnp.bfloat16
F32 = jnp.float32
CHUNK_ROWS = (2, 3, 2)
TURNS, FIRSTS, SECONDS = (2, 4, 5, 6), (1, 3, 4, 5), (0, 2, 3, 3)
AHEAD = (1, 0)
COLUMN_FIRST = (2, 3)
CHIPS_ALONG = (3, 1, 2, 0)
CHIP_ORDER = tuple((other, dy) for other in (0, 1) for dy in (1, -1, 0, 2))


def turn(recv, i, put):
    sources, _, win_j, own_chans, lanes = recv.shape
    chans = sources * own_chans
    for j in range(win_j):
        top = recv[:, 2 * i, j].reshape(chans, lanes)
        under = recv[:, 2 * i + 1, j].reshape(chans, lanes)
        put(j, jnp.concatenate([top, under], axis=0).T.reshape(2, lanes // 2, 2 * chans))


def blocks(pairs, weights, count):
    acc = None
    for dw in range(4):
        parts = [view[dw // 2 : dw // 2 + count, dw % 2] for view in pairs]
        lhs = jnp.concatenate([p.reshape(count * p.shape[1], p.shape[2]) for p in parts], axis=1)
        term = jnp.dot(lhs, weights(dw), preferred_element_type=F32)
        acc = term if acc is None else acc + term
    return acc


def first(pairs, weights, bias, y_row, blank_a):
    count, _, images, lanes = y_row.shape
    c = lax.axis_index("cols")
    row = lax.rem(lax.broadcasted_iota(jnp.int32, (1, 2 * lanes), 1), lanes) // (lanes // 2)
    act = jnp.maximum(blocks(pairs, weights, count) + bias, 0.0)
    act = jnp.where(row != blank_a, act, 0.0).astype(BF16)
    for b in range(2):
        y_row[:, b] = act[:, b * lanes : (b + 1) * lanes].reshape(count, images, lanes)
    blank = jnp.zeros((images, lanes), BF16)

    @pl.when(c == 0)
    def _():
        y_row[0, 0] = blank

    @pl.when(c == lax.axis_size("cols") - 1)
    def _():
        y_row[count - 1, 1] = blank


def second(pairs, weights, bias, out_pair):
    _, count, _, images, chans = out_pair.shape
    res = blocks(pairs, weights, count) + bias
    for b in range(2):
        for a in range(2):
            at = (2 * b + a) * chans
            out_pair[a, :, b] = res[:, at : at + chans].reshape(count, images, chans)


def conv_kernel(
    n_rows,
    n_cols,
    x_hbm,
    w1_hbm,
    b1_hbm,
    w2_hbm,
    b2_hbm,
    out,
    ymat,
    wt2,
    bias2,
    recv,
    xmat,
    wt1,
    bias1,
    xs,
    packed,
    w1s,
    w1own,
    w1all,
    w2s,
    b1s,
    b2s,
    load_sem,
    par_sem,
    send_sem,
    recv_sem,
    wsend_sem,
    wrecv_sem,
    swap_send_sem,
    swap_recv_sem,
    wswap_send_sem,
    wswap_recv_sem,
):
    chip_h, pairs = xs.shape[1:3]
    images = xs.shape[-1]
    tile_h, tile_j = chip_h // 2, pairs // n_cols
    win_j = tile_j + 2
    sources = n_rows * n_cols
    r, c = lax.axis_index("model"), lax.axis_index("cols")
    par = lax.rem(r, 2)
    me = r * n_cols + c
    chans = recv.shape[0] * 2

    tops = [tile_h - sum(CHUNK_ROWS[: k + 1]) for k in range(len(CHUNK_ROWS))]
    groups = (
        ((tops[0], chip_h - tops[0]),),
        *(((k, k + n), (chip_h - k - n, chip_h - k)) for k, n in zip(tops[1:], CHUNK_ROWS[1:])),
    )
    loads = []
    for g, spans in enumerate(groups):
        loads.append(
            [
                pltpu.make_async_copy(x_hbm.at[:, lo:hi], xs.at[:, lo:hi], load_sem.at[g, n])
                for n, (lo, hi) in enumerate(spans)
            ]
        )
    for copies in loads:
        for copy in copies:
            copy.start()
    params = [
        pltpu.make_async_copy(src, dst, par_sem.at[s])
        for s, (src, dst) in enumerate(((w1_hbm, w1s), (w2_hbm, w2s), (b1_hbm, b1s), (b2_hbm, b2s)))
    ]
    for copy in params:
        copy.start()

    barrier = pltpu.get_barrier_semaphore()
    to_cs = [lax.rem(c + k, n_cols) for k in range(n_cols)]

    def device(to_r, to_c):
        return {"model": to_r, "cols": to_c}

    to_rs = [lax.rem(r + k, n_rows) for k in range(n_rows)]
    for kr, kc in sorted(
        ((kr, kc) for kr in range(n_rows) for kc in range(n_cols) if kr or kc),
        key=lambda k: (not (k[0] in (2, 3) and k[1] == 1), -(min(k[0], n_rows - k[0]) // 2 + min(k[1], n_cols - k[1]))),
    ):
        pl.semaphore_signal(barrier, inc=1, device_id=device(to_rs[kr], to_cs[kc]), device_id_type=MESH)

    def pack_rows(x, lo, hi):
        rows = hi - lo
        left, right = (xs[x, lo:hi, :, p].reshape(rows * pairs * 2, images) for p in range(2))
        both = jnp.concatenate([left, right], axis=1)
        packed[pl.ds(chip_h * x + lo, rows)] = both.reshape(rows, pairs, 2, 2 * images)

    def pack(g):
        for copy in loads[g]:
            copy.wait()

        def body(x, carry):
            for lo, hi in groups[g]:
                pack_rows(x, lo, hi)
            return carry

        lax.fori_loop(0, n_rows // 2, body, 0)

    last = tile_h + 4

    def rows_of(offset, count):
        def where(to_r):
            q = lax.rem(to_r, 2)
            src = tile_h * to_r + offset + (tile_h - count - 2 * offset) * q
            dst = offset + 2 + (last - count - 2 * offset - 3) * q
            return src, dst

        return where

    chunks = (
        *((n, rows_of(k, n), False) for k, n in zip(tops, CHUNK_ROWS)),
        (2, rows_of(-2, 2), True),
    )
    no_outer = (r == 0) | (r == n_rows - 1)
    at_edge = (c == 0) | (c == n_cols - 1)
    own_j = c == 0
    own_j = own_j.astype(jnp.int32)

    def send_tile(chunk, to_r, to_c, there):
        rows, where, is_outer = chunks[chunk]
        src, dst = where(to_r)
        skip = (to_c == 0).astype(jnp.int32)
        edge = (to_c == 0) | (to_c == n_cols - 1)
        if is_outer:
            there = there & (to_r > 0) & (to_r < n_rows - 1)

        def copy(count, src_j, dst_j):
            pltpu.make_async_remote_copy(
                src_ref=packed.at[pl.ds(src, rows), pl.ds(src_j, count)],
                dst_ref=recv.at[me, pl.ds(dst, rows), pl.ds(dst_j, count)],
                send_sem=send_sem.at[chunk],
                recv_sem=recv_sem.at[chunk],
                device_id=device(to_r, to_c),
                device_id_type=MESH,
            ).start()

        pl.when(there & edge)(lambda: copy(win_j - 1, tile_j * to_c - 1 + skip, skip))
        pl.when(there & jnp.logical_not(edge))(lambda: copy(win_j, tile_j * to_c - 1, 0))

    chips = n_rows // 2
    ahead_r, ahead_c = AHEAD

    def step(t, table):
        value = jnp.int32(table[-1])
        for k, entry in enumerate(table[:-1]):
            value = jnp.where(t == k, entry, value)
        return value

    def turn_to(t):
        dx = step(t, CHIPS_ALONG)
        return lax.rem(r // 2 + dx, chips), dx

    def send_chip(chunk, t, rest, where=None):
        x, dx = turn_to(t)
        way = 1 - 2 * lax.rem(par + t, 2)
        for other, dy in CHIP_ORDER:
            to_r = 2 * x + (1 - par if other else par)
            to_c = lax.rem(c + way * dy + n_cols, n_cols)
            there = True
            if not other and dy == 0:
                there = dx > 0
            if rest:
                there = there & jnp.logical_not((to_r == ahead_r) & (to_c == ahead_c))
            if where is not None:
                there = there & where(to_c)
            send_tile(chunk, to_r, to_c, there)

    def send_ahead(chunk):
        send_tile(chunk, jnp.int32(ahead_r), jnp.int32(ahead_c), (r != ahead_r) | (c != ahead_c))

    def send_chunk(chunk):

        def first_column(t, carry):
            x, _ = turn_to(t)
            for other in range(2):
                to_r = 2 * x + (1 - par if other else par)
                there = ((to_r != r) | (c != 0)) & (to_r != ahead_r)
                send_tile(chunk, to_r, jnp.int32(0), there)
            return carry

        where = None
        if chunk in COLUMN_FIRST:
            lax.fori_loop(0, chips, first_column, 0)
            where = lambda to_c: to_c > 0

        def body(t, carry):
            send_chip(chunk, t, True, where)
            return carry

        lax.fori_loop(0, chips, body, 0)

    params[0].wait()
    for dw in range(3):
        w1own[dw] = jnp.concatenate([w1s[1, dw], w1s[0, dw]], axis=1)
    w1own[3] = jnp.concatenate([w1s[2, 0], w1s[2, 1]], axis=1)
    w1own[4] = jnp.concatenate([w1s[2, 2], jnp.zeros_like(w1s[2, 2])], axis=1)
    w1all[r // 2, par, c] = w1own[...]

    for copy in loads[0]:
        copy.wait()
    pack_rows(turn_to(0)[0], *groups[0][0])
    pl.semaphore_wait(barrier, sources - 1)

    def send_weights():
        for kr in range(0, n_rows, 2):
            for kc in range(n_cols):
                if kr or kc:
                    pltpu.make_async_remote_copy(
                        src_ref=w1own,
                        dst_ref=w1all.at[r // 2, par, c],
                        send_sem=wsend_sem,
                        recv_sem=wrecv_sem,
                        device_id=device(to_rs[kr], to_cs[kc]),
                        device_id_type=MESH,
                    ).start()

    def pack_and_send(t, carry):
        pl.when(t < chips - 1)(lambda: pack_rows(turn_to(t + 1)[0], *groups[0][0]))
        send_chip(0, t, False)
        pl.when(t == 0)(send_weights)
        return carry

    lax.fori_loop(0, chips, pack_and_send, 0)

    pack(1)
    send_ahead(1)
    send_chunk(1)
    pack(2)
    send_ahead(2)
    send_ahead(3)
    send_chunk(2)
    send_chunk(3)

    def own_rows(chunk):
        rows, where, _ = chunks[chunk]
        src, dst = where(r)

        def copy(count, src_j, dst_j):
            for h in range(rows):
                recv[me, dst + h, pl.ds(dst_j, count)] = packed[src + h, pl.ds(src_j, count)]

        pl.when(at_edge)(lambda: copy(win_j - 1, tile_j * c - 1 + own_j, own_j))
        pl.when(jnp.logical_not(at_edge))(lambda: copy(win_j, tile_j * c - 1, 0))

    for chunk in range(3):
        own_rows(chunk)
    pl.when(jnp.logical_not(no_outer))(lambda: own_rows(3))

    zero_row = jnp.zeros((win_j, 2, 2 * images), BF16)
    zero_col = jnp.zeros((tile_h + 2, 2, 2 * images), BF16)

    def clear(s, carry):
        recv[s, last * (1 - par)] = zero_row
        return carry

    def clear_outer(s, carry):
        recv[s, (last - 1) * par] = zero_row
        recv[s, (last - 1) * par + 1] = zero_row
        return carry

    def clear_edge(s, carry):
        recv[s, pl.ds(3 * par, tile_h + 2), (win_j - 1) * (1 - own_j)] = zero_col
        return carry

    lax.fori_loop(0, sources, clear, 0)
    pl.when(no_outer)(lambda: (lax.fori_loop(0, sources, clear_outer, 0), None)[1])
    pl.when(at_edge)(lambda: (lax.fori_loop(0, sources, clear_edge, 0), None)[1])

    low = lax.broadcasted_iota(jnp.int32, (chans, 2 * chans), 1) < chans

    def spread(wt, u, v, dw):
        ur, vr = pltpu.roll(u, chans, 1), pltpu.roll(v, chans, 1)
        zero = jnp.zeros_like(u)
        tiles = (jnp.where(low, ur, zero), u, jnp.where(low, v, ur), jnp.where(low, zero, vr))
        for k, tile in enumerate(tiles):
            tile = tile.astype(BF16)
            for b in range(2):
                wt[dw + b, k * chans : (k + 1) * chans, b * 2 * chans : (b + 1) * 2 * chans] = tile

    def blank(wt):
        zero = jnp.zeros((4 * chans, 2 * chans), BF16)
        wt[3, :, 0 : 2 * chans] = zero
        wt[0, :, 2 * chans : 4 * chans] = zero

    for copy in params[1:]:
        copy.wait()
    blank(wt1)
    blank(wt2)
    for dw in range(3):
        w = [w2s[dh, dw].astype(F32) for dh in range(3)]
        spread(
            wt2,
            jnp.concatenate([w[1], w[0]], axis=1),
            jnp.concatenate([w[2], jnp.zeros_like(w[2])], axis=1),
            dw,
        )
    bias1[...] = jnp.concatenate([b1s[...]] * 4, axis=1)
    bias2[...] = jnp.concatenate([b2s[...]] * 4, axis=1)

    def wait_bytes(ref, sem):
        pltpu.make_async_copy(ref, ref, sem).wait()

    w1_bytes = recv.at[0 : sources // 2 - 1, 0, 0:5]
    wait_bytes(w1_bytes, wrecv_sem)
    wait_bytes(w1_bytes, wsend_sem)
    partner = device(r + 1 - 2 * par, c)
    w_swap = pltpu.make_async_remote_copy(
        src_ref=w1all.at[:, par],
        dst_ref=w1all.at[:, par],
        send_sem=wswap_send_sem,
        recv_sem=wswap_recv_sem,
        device_id=partner,
        device_id_type=MESH,
    )
    w_swap.start()

    def arrived(chunk):
        def wait(count):
            wait_bytes(recv.at[0 : sources - 1, 0 : chunks[chunk][0], 0:count], recv_sem.at[chunk])

        pl.when(at_edge)(lambda: wait(win_j - 1))
        pl.when(jnp.logical_not(at_edge))(lambda: wait(win_j))

    arrived(0)
    give = tile_h - (tile_h - 3) * par
    land = tile_h + 2 - (tile_h + 1) * (1 - par)
    swap = pltpu.make_async_remote_copy(
        src_ref=recv.at[:, pl.ds(give, 2)],
        dst_ref=recv.at[:, pl.ds(land, 2)],
        send_sem=swap_send_sem,
        recv_sem=swap_recv_sem,
        device_id=partner,
        device_id_type=MESH,
    )
    swap.start()

    w_swap.wait()
    u = [w1all[:, :, :, k].reshape(chans, 2 * chans).astype(F32) for k in range(5)]
    for dw in range(3):
        v = (u[3], pltpu.roll(u[3], chans, 1), u[4])[dw]
        spread(wt1, u[dw], jnp.where(low, v, 0.0), dw)

    x_pairs, z_pairs = xmat.shape[0], ymat.shape[0]
    o_pairs = z_pairs - 1

    def nth(n, count):
        return (count - 1) * (1 - par) + n * (2 * par - 1)

    def turn_one(n, carry):
        i = nth(n, x_pairs)

        def put(j, value):
            xmat[i, j] = value

        turn(recv, i, put)
        return carry

    def first_one(n, carry):
        i = nth(n, z_pairs)
        fill = jnp.where(n == 0, 1 - par, 2)
        out_of = jnp.where(n == z_pairs - 1, jnp.where(r == 0, 0, jnp.where(r == n_rows - 1, 1, 2)), 2)
        blank_a = jnp.where(fill < 2, fill, out_of)
        first((xmat.at[i], xmat.at[i + 1]), lambda dw: wt1[dw], bias1[...], ymat.at[i], blank_a)
        return carry

    def second_one(n, carry):
        i = nth(n, o_pairs)
        second((ymat.at[i], ymat.at[i + 1]), lambda dw: wt2[dw], bias2[...], out.at[pl.ds(2 * i, 2)])
        return carry

    def stage(s, carry):
        @pl.when(s == 0)
        def _():
            swap.wait()

        for k in range(1, 4):
            there = s == k
            if k == 3:
                there = there & jnp.logical_not(no_outer)
            pl.when(there)(lambda k=k: arrived(k))

        for ends, one in ((TURNS, turn_one), (FIRSTS, first_one), (SECONDS, second_one)):
            lax.fori_loop(step(s, (0, *ends[:-1])), step(s, ends), one, 0)
        return carry

    lax.fori_loop(0, 4, stage, 0)

    per_edge = n_rows * 2
    for chunk in range(4):
        rows = chunks[chunk][0]
        n_r = n_rows - 2 if chunk == 3 else n_rows
        counts = (n_r * 2, n_r * (n_cols - 2))

        def drain(edge_n, inner_n, rows=rows, chunk=chunk):
            wait_bytes(recv.at[0:edge_n, 0:rows, 0 : win_j - 1], send_sem.at[chunk])
            wait_bytes(recv.at[0:inner_n, 0:rows, 0:win_j], send_sem.at[chunk])

        def drain_own(chunk=chunk, counts=counts, drain=drain):
            pl.when(at_edge)(lambda: drain(counts[0] - 1, counts[1]))
            pl.when(jnp.logical_not(at_edge))(lambda: drain(counts[0], counts[1] - 1))

        if chunk == 3:
            pl.when(no_outer)(lambda: drain(*counts))
            pl.when(jnp.logical_not(no_outer))(drain_own)
        else:
            drain_own()


def tail_kernel(tile, ymat, wt2, bias2, out_hbm, o_new, sem):
    par = lax.rem(lax.axis_index("model"), 2)
    rows = out_hbm.shape[0]
    o_pairs = ymat.shape[0] - 1
    late = (rows - 2) * par
    here = 2 * (1 - par)

    def start(k, carry):
        pltpu.make_async_copy(tile.at[par + k], out_hbm.at[k], sem.at[0]).start()
        return carry

    lax.fori_loop(here, here + rows - 2, start, 0)
    i = (o_pairs - 1) * par
    second((ymat.at[i], ymat.at[i + 1]), lambda dw: wt2[dw], bias2[...], o_new)
    last = pltpu.make_async_copy(o_new, out_hbm.at[pl.ds(late, 2)], sem.at[1])
    last.start()
    pltpu.make_async_copy(tile.at[0 : rows - 2], out_hbm.at[0 : rows - 2], sem.at[0]).wait()
    last.wait()


def solution(mesh):
    n_rows = mesh.shape["model"]
    n_cols = mesh.shape["cols"]

    def run_local(x_in, w_conv1, b_conv1, w_conv2, b_conv2):
        images, height, width, own_chans = x_in.shape
        sources = n_rows * n_cols
        chans = own_chans * sources
        pairs = width // 2
        tile_h, tile_j = height // n_rows, pairs // n_cols
        win_j = tile_j + 2
        x_pairs, z_pairs = (tile_h + 5) // 2, (tile_h + 3) // 2
        x_t = jnp.transpose(x_in, (1, 2, 3, 0)).reshape(n_rows // 2, 2 * tile_h, pairs, 2, own_chans, images)
        args = (x_t, w_conv1, b_conv1.reshape(1, chans), w_conv2, b_conv2.reshape(1, chans))
        hbm = pl.BlockSpec(memory_space=pltpu.HBM)
        vmem = pl.BlockSpec(memory_space=pltpu.VMEM)
        kept = (
            pltpu.VMEM((2 * (z_pairs - 1), tile_j, 2, images, chans), F32),
            pltpu.VMEM((z_pairs, win_j - 1, 2, images, 2 * chans), BF16),
            pltpu.VMEM((4, 4 * chans, 4 * chans), BF16),
            pltpu.VMEM((1, 4 * chans), F32),
        )
        state = pl.pallas_call(
            functools.partial(conv_kernel, n_rows, n_cols),
            out_shape=kept,
            in_specs=[hbm] * 5,
            out_specs=[vmem] * len(kept),
            scratch_shapes=[
                pltpu.VMEM((sources, 2 * x_pairs, win_j, own_chans, 2 * images), BF16),
                pltpu.VMEM((x_pairs, win_j, 2, images, 2 * chans), BF16),
                pltpu.VMEM((4, 4 * chans, 4 * chans), BF16),
                pltpu.VMEM((1, 4 * chans), F32),
                pltpu.VMEM((n_rows // 2, 2 * tile_h, pairs, 2, own_chans, images), BF16),
                pltpu.VMEM((height, pairs, own_chans, 2 * images), BF16),
                pltpu.VMEM((3, 3, own_chans, chans), BF16),
                pltpu.VMEM((5, own_chans, 2 * chans), BF16),
                pltpu.VMEM((n_rows // 2, 2, n_cols, 5, own_chans, 2 * chans), BF16),
                pltpu.VMEM((3, 3, chans, chans), BF16),
                pltpu.VMEM((1, chans), F32),
                pltpu.VMEM((1, chans), F32),
                pltpu.SemaphoreType.DMA((3, 2)),
                pltpu.SemaphoreType.DMA((4,)),
                pltpu.SemaphoreType.DMA((4,)),
                pltpu.SemaphoreType.DMA((4,)),
            ]
            + [pltpu.SemaphoreType.DMA] * 6,
            compiler_params=pltpu.CompilerParams(
                collective_id=0, has_side_effects=True, vmem_limit_bytes=24 << 20
            ),
            name="conv",
        )(*(pltpu.with_memory_space_constraint(a, pltpu.HBM) for a in args))
        out = pl.pallas_call(
            tail_kernel,
            out_shape=jax.ShapeDtypeStruct((tile_h, tile_j, 2, images, chans), F32),
            in_specs=[vmem] * len(kept),
            out_specs=pl.BlockSpec(memory_space=pl.ANY),
            scratch_shapes=[
                pltpu.VMEM((2, tile_j, 2, images, chans), F32),
                pltpu.SemaphoreType.DMA((2,)),
            ],
            compiler_params=pltpu.CompilerParams(vmem_limit_bytes=8 << 20),
            name="tail",
        )(*state)
        out = out.reshape(tile_h, 2 * tile_j, images, chans)
        return jnp.transpose(out, (2, 0, 1, 3))

    group = ("model", "cols")
    return jax.shard_map(
        run_local,
        mesh=mesh,
        in_specs=(P("data", None, None, group), P(None, None, group, None), P(), P(), P()),
        out_specs=P("data", "model", "cols", None),
        check_vma=False,
    )
```

```python
import functools

import jax
import jax.numpy as jnp
from jax import lax
from jax.experimental import pallas as pl
from jax.experimental.pallas import tpu as pltpu
from jax.sharding import PartitionSpec as P

MESH = pl.DeviceIdType.MESH
BF16 = jnp.bfloat16
F32 = jnp.float32
CHUNK_ROWS = (2, 3, 2)
TURNS, FIRSTS, SECONDS = (2, 4, 5, 6), (1, 3, 4, 5), (0, 2, 3, 3)
AHEAD = (1, 0)
COLUMN_FIRST = (2, 3)
CHIPS_ALONG = (3, 1, 2, 0)
CHIP_ORDER = tuple((other, dy) for other in (0, 1) for dy in (1, -1, 0, 2))


def turn(recv, i, put):
    sources, _, win_j, own_chans, lanes = recv.shape
    chans = sources * own_chans
    for j in range(win_j):
        top = recv[:, 2 * i, j].reshape(chans, lanes)
        under = recv[:, 2 * i + 1, j].reshape(chans, lanes)
        put(j, jnp.concatenate([top, under], axis=0).T.reshape(2, lanes // 2, 2 * chans))


def blocks(pairs, weights, count):
    acc = None
    for dw in range(4):
        parts = [view[dw // 2 : dw // 2 + count, dw % 2] for view in pairs]
        lhs = jnp.concatenate([p.reshape(count * p.shape[1], p.shape[2]) for p in parts], axis=1)
        term = jnp.dot(lhs, weights(dw), preferred_element_type=F32)
        acc = term if acc is None else acc + term
    return acc


def first(pairs, weights, bias, y_row, blank_a):
    count, _, images, lanes = y_row.shape
    c = lax.axis_index("cols")
    row = lax.rem(lax.broadcasted_iota(jnp.int32, (1, 2 * lanes), 1), lanes) // (lanes // 2)
    act = jnp.maximum(blocks(pairs, weights, count) + bias, 0.0)
    act = jnp.where(row != blank_a, act, 0.0).astype(BF16)
    for b in range(2):
        y_row[:, b] = act[:, b * lanes : (b + 1) * lanes].reshape(count, images, lanes)
    blank = jnp.zeros((images, lanes), BF16)

    @pl.when(c == 0)
    def _():
        y_row[0, 0] = blank

    @pl.when(c == lax.axis_size("cols") - 1)
    def _():
        y_row[count - 1, 1] = blank


def second(pairs, weights, bias, out_pair):
    _, count, _, images, chans = out_pair.shape
    res = blocks(pairs, weights, count) + bias
    for b in range(2):
        for a in range(2):
            at = (2 * b + a) * chans
            out_pair[a, :, b] = res[:, at : at + chans].reshape(count, images, chans)


def conv_kernel(
    n_rows,
    n_cols,
    x_hbm,
    w1_hbm,
    b1_hbm,
    w2_hbm,
    b2_hbm,
    out,
    ymat,
    wt2,
    bias2,
    recv,
    xmat,
    wt1,
    bias1,
    xs,
    packed,
    w1s,
    w1own,
    w1all,
    w2s,
    b1s,
    b2s,
    load_sem,
    par_sem,
    send_sem,
    recv_sem,
    wsend_sem,
    wrecv_sem,
    swap_send_sem,
    swap_recv_sem,
    wswap_send_sem,
    wswap_recv_sem,
):
    chip_h, pairs = xs.shape[1:3]
    images = xs.shape[-1]
    tile_h, tile_j = chip_h // 2, pairs // n_cols
    win_j = tile_j + 2
    sources = n_rows * n_cols
    r, c = lax.axis_index("model"), lax.axis_index("cols")
    par = lax.rem(r, 2)
    me = r * n_cols + c
    chans = recv.shape[0] * 2

    tops = [tile_h - sum(CHUNK_ROWS[: k + 1]) for k in range(len(CHUNK_ROWS))]
    groups = (
        ((tops[0], chip_h - tops[0]),),
        *(((k, k + n), (chip_h - k - n, chip_h - k)) for k, n in zip(tops[1:], CHUNK_ROWS[1:])),
    )
    loads = []
    for g, spans in enumerate(groups):
        loads.append(
            [
                pltpu.make_async_copy(x_hbm.at[:, lo:hi], xs.at[:, lo:hi], load_sem.at[g, n])
                for n, (lo, hi) in enumerate(spans)
            ]
        )
    for copies in loads:
        for copy in copies:
            copy.start()
    params = [
        pltpu.make_async_copy(src, dst, par_sem.at[s])
        for s, (src, dst) in enumerate(((w1_hbm, w1s), (w2_hbm, w2s), (b1_hbm, b1s), (b2_hbm, b2s)))
    ]
    for copy in params:
        copy.start()

    barrier = pltpu.get_barrier_semaphore()
    to_cs = [lax.rem(c + k, n_cols) for k in range(n_cols)]

    def device(to_r, to_c):
        return {"model": to_r, "cols": to_c}

    to_rs = [lax.rem(r + k, n_rows) for k in range(n_rows)]
    for kr, kc in sorted(
        ((kr, kc) for kr in range(n_rows) for kc in range(n_cols) if kr or kc),
        key=lambda k: (not (k[0] in (2, 3) and k[1] == 1), -(min(k[0], n_rows - k[0]) // 2 + min(k[1], n_cols - k[1]))),
    ):
        pl.semaphore_signal(barrier, inc=1, device_id=device(to_rs[kr], to_cs[kc]), device_id_type=MESH)

    def pack_rows(x, lo, hi):
        rows = hi - lo
        left, right = (xs[x, lo:hi, :, p].reshape(rows * pairs * 2, images) for p in range(2))
        both = jnp.concatenate([left, right], axis=1)
        packed[pl.ds(chip_h * x + lo, rows)] = both.reshape(rows, pairs, 2, 2 * images)

    def pack(g):
        for copy in loads[g]:
            copy.wait()

        def body(x, carry):
            for lo, hi in groups[g]:
                pack_rows(x, lo, hi)
            return carry

        lax.fori_loop(0, n_rows // 2, body, 0)

    last = tile_h + 4

    def rows_of(offset, count):
        def where(to_r):
            q = lax.rem(to_r, 2)
            src = tile_h * to_r + offset + (tile_h - count - 2 * offset) * q
            dst = offset + 2 + (last - count - 2 * offset - 3) * q
            return src, dst

        return where

    chunks = (
        *((n, rows_of(k, n), False) for k, n in zip(tops, CHUNK_ROWS)),
        (2, rows_of(-2, 2), True),
    )
    no_outer = (r == 0) | (r == n_rows - 1)
    at_edge = (c == 0) | (c == n_cols - 1)
    own_j = c == 0
    own_j = own_j.astype(jnp.int32)

    def send_tile(chunk, to_r, to_c, there):
        rows, where, is_outer = chunks[chunk]
        src, dst = where(to_r)
        skip = (to_c == 0).astype(jnp.int32)
        edge = (to_c == 0) | (to_c == n_cols - 1)
        if is_outer:
            there = there & (to_r > 0) & (to_r < n_rows - 1)

        def copy(count, src_j, dst_j):
            pltpu.make_async_remote_copy(
                src_ref=packed.at[pl.ds(src, rows), pl.ds(src_j, count)],
                dst_ref=recv.at[me, pl.ds(dst, rows), pl.ds(dst_j, count)],
                send_sem=send_sem.at[chunk],
                recv_sem=recv_sem.at[chunk],
                device_id=device(to_r, to_c),
                device_id_type=MESH,
            ).start()

        pl.when(there & edge)(lambda: copy(win_j - 1, tile_j * to_c - 1 + skip, skip))
        pl.when(there & jnp.logical_not(edge))(lambda: copy(win_j, tile_j * to_c - 1, 0))

    chips = n_rows // 2
    ahead_r, ahead_c = AHEAD

    def step(t, table):
        value = jnp.int32(table[-1])
        for k, entry in enumerate(table[:-1]):
            value = jnp.where(t == k, entry, value)
        return value

    def turn_to(t):
        dx = step(t, CHIPS_ALONG)
        return lax.rem(r // 2 + dx, chips), dx

    def send_chip(chunk, t, rest, where=None):
        x, dx = turn_to(t)
        way = 1 - 2 * par
        for other, dy in CHIP_ORDER:
            to_r = 2 * x + (1 - par if other else par)
            to_c = lax.rem(c + way * dy + n_cols, n_cols)
            there = True
            if not other and dy == 0:
                there = dx > 0
            if rest:
                there = there & jnp.logical_not((to_r == ahead_r) & (to_c == ahead_c))
            if where is not None:
                there = there & where(to_c)
            send_tile(chunk, to_r, to_c, there)

    def send_ahead(chunk):
        send_tile(chunk, jnp.int32(ahead_r), jnp.int32(ahead_c), (r != ahead_r) | (c != ahead_c))

    def send_chunk(chunk):

        def first_column(t, carry):
            x, _ = turn_to(t)
            for other in range(2):
                to_r = 2 * x + (1 - par if other else par)
                there = ((to_r != r) | (c != 0)) & (to_r != ahead_r)
                send_tile(chunk, to_r, jnp.int32(0), there)
            return carry

        where = None
        if chunk in COLUMN_FIRST:
            lax.fori_loop(0, chips, first_column, 0)
            where = lambda to_c: to_c > 0

        def body(t, carry):
            send_chip(chunk, t, True, where)
            return carry

        lax.fori_loop(0, chips, body, 0)

    params[0].wait()
    for dw in range(3):
        w1own[dw] = jnp.concatenate([w1s[1, dw], w1s[0, dw]], axis=1)
    w1own[3] = jnp.concatenate([w1s[2, 0], w1s[2, 1]], axis=1)
    w1own[4] = jnp.concatenate([w1s[2, 2], jnp.zeros_like(w1s[2, 2])], axis=1)
    w1all[r // 2, par, c] = w1own[...]

    for copy in loads[0]:
        copy.wait()
    pack_rows(turn_to(0)[0], *groups[0][0])
    pl.semaphore_wait(barrier, sources - 1)

    def send_weights():
        for kr in range(0, n_rows, 2):
            for kc in range(n_cols):
                if kr or kc:
                    pltpu.make_async_remote_copy(
                        src_ref=w1own,
                        dst_ref=w1all.at[r // 2, par, c],
                        send_sem=wsend_sem,
                        recv_sem=wrecv_sem,
                        device_id=device(to_rs[kr], to_cs[kc]),
                        device_id_type=MESH,
                    ).start()

    def pack_and_send(t, carry):
        pl.when(t < chips - 1)(lambda: pack_rows(turn_to(t + 1)[0], *groups[0][0]))
        send_chip(0, t, False)
        pl.when(t == 0)(send_weights)
        return carry

    lax.fori_loop(0, chips, pack_and_send, 0)

    pack(1)
    send_ahead(1)
    send_chunk(1)
    pack(2)
    send_ahead(2)
    send_ahead(3)
    send_chunk(2)
    send_chunk(3)

    def own_rows(chunk):
        rows, where, _ = chunks[chunk]
        src, dst = where(r)

        def copy(count, src_j, dst_j):
            for h in range(rows):
                recv[me, dst + h, pl.ds(dst_j, count)] = packed[src + h, pl.ds(src_j, count)]

        pl.when(at_edge)(lambda: copy(win_j - 1, tile_j * c - 1 + own_j, own_j))
        pl.when(jnp.logical_not(at_edge))(lambda: copy(win_j, tile_j * c - 1, 0))

    for chunk in range(3):
        own_rows(chunk)
    pl.when(jnp.logical_not(no_outer))(lambda: own_rows(3))

    zero_row = jnp.zeros((win_j, 2, 2 * images), BF16)
    zero_col = jnp.zeros((tile_h + 2, 2, 2 * images), BF16)

    def clear(s, carry):
        recv[s, last * (1 - par)] = zero_row
        return carry

    def clear_outer(s, carry):
        recv[s, (last - 1) * par] = zero_row
        recv[s, (last - 1) * par + 1] = zero_row
        return carry

    def clear_edge(s, carry):
        recv[s, pl.ds(3 * par, tile_h + 2), (win_j - 1) * (1 - own_j)] = zero_col
        return carry

    lax.fori_loop(0, sources, clear, 0)
    pl.when(no_outer)(lambda: (lax.fori_loop(0, sources, clear_outer, 0), None)[1])
    pl.when(at_edge)(lambda: (lax.fori_loop(0, sources, clear_edge, 0), None)[1])

    low = lax.broadcasted_iota(jnp.int32, (chans, 2 * chans), 1) < chans

    def spread(wt, u, v, dw):
        ur, vr = pltpu.roll(u, chans, 1), pltpu.roll(v, chans, 1)
        zero = jnp.zeros_like(u)
        tiles = (jnp.where(low, ur, zero), u, jnp.where(low, v, ur), jnp.where(low, zero, vr))
        for k, tile in enumerate(tiles):
            tile = tile.astype(BF16)
            for b in range(2):
                wt[dw + b, k * chans : (k + 1) * chans, b * 2 * chans : (b + 1) * 2 * chans] = tile

    def blank(wt):
        zero = jnp.zeros((4 * chans, 2 * chans), BF16)
        wt[3, :, 0 : 2 * chans] = zero
        wt[0, :, 2 * chans : 4 * chans] = zero

    for copy in params[1:]:
        copy.wait()
    blank(wt1)
    blank(wt2)
    for dw in range(3):
        w = [w2s[dh, dw].astype(F32) for dh in range(3)]
        spread(
            wt2,
            jnp.concatenate([w[1], w[0]], axis=1),
            jnp.concatenate([w[2], jnp.zeros_like(w[2])], axis=1),
            dw,
        )
    bias1[...] = jnp.concatenate([b1s[...]] * 4, axis=1)
    bias2[...] = jnp.concatenate([b2s[...]] * 4, axis=1)

    def wait_bytes(ref, sem):
        pltpu.make_async_copy(ref, ref, sem).wait()

    w1_bytes = recv.at[0 : sources // 2 - 1, 0, 0:5]
    wait_bytes(w1_bytes, wrecv_sem)
    wait_bytes(w1_bytes, wsend_sem)
    partner = device(r + 1 - 2 * par, c)
    w_swap = pltpu.make_async_remote_copy(
        src_ref=w1all.at[:, par],
        dst_ref=w1all.at[:, par],
        send_sem=wswap_send_sem,
        recv_sem=wswap_recv_sem,
        device_id=partner,
        device_id_type=MESH,
    )
    w_swap.start()

    def arrived(chunk):
        def wait(count):
            wait_bytes(recv.at[0 : sources - 1, 0 : chunks[chunk][0], 0:count], recv_sem.at[chunk])

        pl.when(at_edge)(lambda: wait(win_j - 1))
        pl.when(jnp.logical_not(at_edge))(lambda: wait(win_j))

    arrived(0)
    give = tile_h - (tile_h - 3) * par
    land = tile_h + 2 - (tile_h + 1) * (1 - par)
    swap = pltpu.make_async_remote_copy(
        src_ref=recv.at[:, pl.ds(give, 2)],
        dst_ref=recv.at[:, pl.ds(land, 2)],
        send_sem=swap_send_sem,
        recv_sem=swap_recv_sem,
        device_id=partner,
        device_id_type=MESH,
    )
    swap.start()

    w_swap.wait()
    u = [w1all[:, :, :, k].reshape(chans, 2 * chans).astype(F32) for k in range(5)]
    for dw in range(3):
        v = (u[3], pltpu.roll(u[3], chans, 1), u[4])[dw]
        spread(wt1, u[dw], jnp.where(low, v, 0.0), dw)

    x_pairs, z_pairs = xmat.shape[0], ymat.shape[0]
    o_pairs = z_pairs - 1

    def nth(n, count):
        return (count - 1) * (1 - par) + n * (2 * par - 1)

    def turn_one(n, carry):
        i = nth(n, x_pairs)

        def put(j, value):
            xmat[i, j] = value

        turn(recv, i, put)
        return carry

    def first_one(n, carry):
        i = nth(n, z_pairs)
        fill = jnp.where(n == 0, 1 - par, 2)
        out_of = jnp.where(n == z_pairs - 1, jnp.where(r == 0, 0, jnp.where(r == n_rows - 1, 1, 2)), 2)
        blank_a = jnp.where(fill < 2, fill, out_of)
        first((xmat.at[i], xmat.at[i + 1]), lambda dw: wt1[dw], bias1[...], ymat.at[i], blank_a)
        return carry

    def second_one(n, carry):
        i = nth(n, o_pairs)
        second((ymat.at[i], ymat.at[i + 1]), lambda dw: wt2[dw], bias2[...], out.at[pl.ds(2 * i, 2)])
        return carry

    def stage(s, carry):
        @pl.when(s == 0)
        def _():
            swap.wait()

        for k in range(1, 4):
            there = s == k
            if k == 3:
                there = there & jnp.logical_not(no_outer)
            pl.when(there)(lambda k=k: arrived(k))

        for ends, one in ((TURNS, turn_one), (FIRSTS, first_one), (SECONDS, second_one)):
            lax.fori_loop(step(s, (0, *ends[:-1])), step(s, ends), one, 0)
        return carry

    lax.fori_loop(0, 4, stage, 0)

    per_edge = n_rows * 2
    for chunk in range(4):
        rows = chunks[chunk][0]
        n_r = n_rows - 2 if chunk == 3 else n_rows
        counts = (n_r * 2, n_r * (n_cols - 2))

        def drain(edge_n, inner_n, rows=rows, chunk=chunk):
            wait_bytes(recv.at[0:edge_n, 0:rows, 0 : win_j - 1], send_sem.at[chunk])
            wait_bytes(recv.at[0:inner_n, 0:rows, 0:win_j], send_sem.at[chunk])

        def drain_own(chunk=chunk, counts=counts, drain=drain):
            pl.when(at_edge)(lambda: drain(counts[0] - 1, counts[1]))
            pl.when(jnp.logical_not(at_edge))(lambda: drain(counts[0], counts[1] - 1))

        if chunk == 3:
            pl.when(no_outer)(lambda: drain(*counts))
            pl.when(jnp.logical_not(no_outer))(drain_own)
        else:
            drain_own()


def tail_kernel(tile, ymat, wt2, bias2, out_hbm, o_new, sem):
    par = lax.rem(lax.axis_index("model"), 2)
    rows = out_hbm.shape[0]
    o_pairs = ymat.shape[0] - 1
    late = (rows - 2) * par
    here = 2 * (1 - par)

    def start(k, carry):
        pltpu.make_async_copy(tile.at[par + k], out_hbm.at[k], sem.at[0]).start()
        return carry

    lax.fori_loop(here, here + rows - 2, start, 0)
    i = (o_pairs - 1) * par
    second((ymat.at[i], ymat.at[i + 1]), lambda dw: wt2[dw], bias2[...], o_new)
    last = pltpu.make_async_copy(o_new, out_hbm.at[pl.ds(late, 2)], sem.at[1])
    last.start()
    pltpu.make_async_copy(tile.at[0 : rows - 2], out_hbm.at[0 : rows - 2], sem.at[0]).wait()
    last.wait()


def solution(mesh):
    n_rows = mesh.shape["model"]
    n_cols = mesh.shape["cols"]

    def run_local(x_in, w_conv1, b_conv1, w_conv2, b_conv2):
        images, height, width, own_chans = x_in.shape
        sources = n_rows * n_cols
        chans = own_chans * sources
        pairs = width // 2
        tile_h, tile_j = height // n_rows, pairs // n_cols
        win_j = tile_j + 2
        x_pairs, z_pairs = (tile_h + 5) // 2, (tile_h + 3) // 2
        x_t = jnp.transpose(x_in, (1, 2, 3, 0)).reshape(n_rows // 2, 2 * tile_h, pairs, 2, own_chans, images)
        args = (x_t, w_conv1, b_conv1.reshape(1, chans), w_conv2, b_conv2.reshape(1, chans))
        hbm = pl.BlockSpec(memory_space=pltpu.HBM)
        vmem = pl.BlockSpec(memory_space=pltpu.VMEM)
        kept = (
            pltpu.VMEM((2 * (z_pairs - 1), tile_j, 2, images, chans), F32),
            pltpu.VMEM((z_pairs, win_j - 1, 2, images, 2 * chans), BF16),
            pltpu.VMEM((4, 4 * chans, 4 * chans), BF16),
            pltpu.VMEM((1, 4 * chans), F32),
        )
        state = pl.pallas_call(
            functools.partial(conv_kernel, n_rows, n_cols),
            out_shape=kept,
            in_specs=[hbm] * 5,
            out_specs=[vmem] * len(kept),
            scratch_shapes=[
                pltpu.VMEM((sources, 2 * x_pairs, win_j, own_chans, 2 * images), BF16),
                pltpu.VMEM((x_pairs, win_j, 2, images, 2 * chans), BF16),
                pltpu.VMEM((4, 4 * chans, 4 * chans), BF16),
                pltpu.VMEM((1, 4 * chans), F32),
                pltpu.VMEM((n_rows // 2, 2 * tile_h, pairs, 2, own_chans, images), BF16),
                pltpu.VMEM((height, pairs, own_chans, 2 * images), BF16),
                pltpu.VMEM((3, 3, own_chans, chans), BF16),
                pltpu.VMEM((5, own_chans, 2 * chans), BF16),
                pltpu.VMEM((n_rows // 2, 2, n_cols, 5, own_chans, 2 * chans), BF16),
                pltpu.VMEM((3, 3, chans, chans), BF16),
                pltpu.VMEM((1, chans), F32),
                pltpu.VMEM((1, chans), F32),
                pltpu.SemaphoreType.DMA((3, 2)),
                pltpu.SemaphoreType.DMA((4,)),
                pltpu.SemaphoreType.DMA((4,)),
                pltpu.SemaphoreType.DMA((4,)),
            ]
            + [pltpu.SemaphoreType.DMA] * 6,
            compiler_params=pltpu.CompilerParams(
                collective_id=0, has_side_effects=True, vmem_limit_bytes=24 << 20
            ),
            name="conv",
        )(*(pltpu.with_memory_space_constraint(a, pltpu.HBM) for a in args))
        out = pl.pallas_call(
            tail_kernel,
            out_shape=jax.ShapeDtypeStruct((tile_h, tile_j, 2, images, chans), F32),
            in_specs=[vmem] * len(kept),
            out_specs=pl.BlockSpec(memory_space=pl.ANY),
            scratch_shapes=[
                pltpu.VMEM((2, tile_j, 2, images, chans), F32),
                pltpu.SemaphoreType.DMA((2,)),
            ],
            compiler_params=pltpu.CompilerParams(vmem_limit_bytes=8 << 20),
            name="tail",
        )(*state)
        out = out.reshape(tile_h, 2 * tile_j, images, chans)
        return jnp.transpose(out, (2, 0, 1, 3))

    group = ("model", "cols")
    return jax.shard_map(
        run_local,
        mesh=mesh,
        in_specs=(P("data", None, None, group), P(None, None, group, None), P(), P(), P()),
        out_specs=P("data", "model", "cols", None),
        check_vma=False,
    )
```

```python
import functools

import jax
import jax.numpy as jnp
from jax import lax
from jax.experimental import pallas as pl
from jax.experimental.pallas import tpu as pltpu
from jax.sharding import PartitionSpec as P

MESH = pl.DeviceIdType.MESH
BF16 = jnp.bfloat16
F32 = jnp.float32
CHUNK_ROWS = (2, 3, 2)
TURNS, FIRSTS, SECONDS = (2, 4, 5, 6), (1, 3, 4, 5), (0, 2, 3, 3)
AHEAD = (1, 0)
COLUMN_FIRST = (2, 3)
CHIPS_ALONG = (3, 1, 2, 0)
CHIP_ORDER = tuple((other, dy) for other in (0, 1) for dy in (1, -1, 0, 2))


def turn(recv, i, put):
    sources, _, win_j, own_chans, lanes = recv.shape
    chans = sources * own_chans
    for j in range(win_j):
        top = recv[:, 2 * i, j].reshape(chans, lanes)
        under = recv[:, 2 * i + 1, j].reshape(chans, lanes)
        put(j, jnp.concatenate([top, under], axis=0).T.reshape(2, lanes // 2, 2 * chans))


def blocks(pairs, weights, count):
    acc = None
    for dw in range(4):
        parts = [view[dw // 2 : dw // 2 + count, dw % 2] for view in pairs]
        lhs = jnp.concatenate([p.reshape(count * p.shape[1], p.shape[2]) for p in parts], axis=1)
        term = jnp.dot(lhs, weights(dw), preferred_element_type=F32)
        acc = term if acc is None else acc + term
    return acc


def first(pairs, weights, bias, y_row, blank_a):
    count, _, images, lanes = y_row.shape
    c = lax.axis_index("cols")
    row = lax.rem(lax.broadcasted_iota(jnp.int32, (1, 2 * lanes), 1), lanes) // (lanes // 2)
    act = jnp.maximum(blocks(pairs, weights, count) + bias, 0.0)
    act = jnp.where(row != blank_a, act, 0.0).astype(BF16)
    for b in range(2):
        y_row[:, b] = act[:, b * lanes : (b + 1) * lanes].reshape(count, images, lanes)
    blank = jnp.zeros((images, lanes), BF16)

    @pl.when(c == 0)
    def _():
        y_row[0, 0] = blank

    @pl.when(c == lax.axis_size("cols") - 1)
    def _():
        y_row[count - 1, 1] = blank


def second(pairs, weights, bias, out_pair):
    _, count, _, images, chans = out_pair.shape
    res = blocks(pairs, weights, count) + bias
    for b in range(2):
        for a in range(2):
            at = (2 * b + a) * chans
            out_pair[a, :, b] = res[:, at : at + chans].reshape(count, images, chans)


def conv_kernel(
    n_rows,
    n_cols,
    x_hbm,
    w1_hbm,
    b1_hbm,
    w2_hbm,
    b2_hbm,
    out,
    ymat,
    wt2,
    bias2,
    recv,
    xmat,
    wt1,
    bias1,
    xs,
    packed,
    w1s,
    w1own,
    w1all,
    w2s,
    b1s,
    b2s,
    load_sem,
    par_sem,
    send_sem,
    recv_sem,
    wsend_sem,
    wrecv_sem,
    swap_send_sem,
    swap_recv_sem,
    wswap_send_sem,
    wswap_recv_sem,
):
    chip_h, pairs = xs.shape[1:3]
    images = xs.shape[-1]
    tile_h, tile_j = chip_h // 2, pairs // n_cols
    win_j = tile_j + 2
    sources = n_rows * n_cols
    r, c = lax.axis_index("model"), lax.axis_index("cols")
    par = lax.rem(r, 2)
    me = r * n_cols + c
    chans = recv.shape[0] * 2

    tops = [tile_h - sum(CHUNK_ROWS[: k + 1]) for k in range(len(CHUNK_ROWS))]
    groups = (
        ((tops[0], chip_h - tops[0]),),
        *(((k, k + n), (chip_h - k - n, chip_h - k)) for k, n in zip(tops[1:], CHUNK_ROWS[1:])),
    )
    loads = []
    for g, spans in enumerate(groups):
        loads.append(
            [
                pltpu.make_async_copy(x_hbm.at[:, lo:hi], xs.at[:, lo:hi], load_sem.at[g, n])
                for n, (lo, hi) in enumerate(spans)
            ]
        )
    for copies in loads:
        for copy in copies:
            copy.start()
    params = [
        pltpu.make_async_copy(src, dst, par_sem.at[s])
        for s, (src, dst) in enumerate(((w1_hbm, w1s), (w2_hbm, w2s), (b1_hbm, b1s), (b2_hbm, b2s)))
    ]
    for copy in params:
        copy.start()

    barrier = pltpu.get_barrier_semaphore()
    to_cs = [lax.rem(c + k, n_cols) for k in range(n_cols)]

    def device(to_r, to_c):
        return {"model": to_r, "cols": to_c}

    to_rs = [lax.rem(r + k, n_rows) for k in range(n_rows)]
    for kr, kc in sorted(
        ((kr, kc) for kr in range(n_rows) for kc in range(n_cols) if kr or kc),
        key=lambda k: (not (k[0] in (2, 3) and k[1] == 1), -(min(k[0], n_rows - k[0]) // 2 + min(k[1], n_cols - k[1]))),
    ):
        pl.semaphore_signal(barrier, inc=1, device_id=device(to_rs[kr], to_cs[kc]), device_id_type=MESH)

    def pack_rows(x, lo, hi):
        rows = hi - lo
        left, right = (xs[x, lo:hi, :, p].reshape(rows * pairs * 2, images) for p in range(2))
        both = jnp.concatenate([left, right], axis=1)
        packed[pl.ds(chip_h * x + lo, rows)] = both.reshape(rows, pairs, 2, 2 * images)

    def pack(g):
        for copy in loads[g]:
            copy.wait()

        def body(x, carry):
            for lo, hi in groups[g]:
                pack_rows(x, lo, hi)
            return carry

        lax.fori_loop(0, n_rows // 2, body, 0)

    last = tile_h + 4

    def rows_of(offset, count):
        def where(to_r):
            q = lax.rem(to_r, 2)
            src = tile_h * to_r + offset + (tile_h - count - 2 * offset) * q
            dst = offset + 2 + (last - count - 2 * offset - 3) * q
            return src, dst

        return where

    chunks = (
        *((n, rows_of(k, n), False) for k, n in zip(tops, CHUNK_ROWS)),
        (2, rows_of(-2, 2), True),
    )
    no_outer = (r == 0) | (r == n_rows - 1)
    at_edge = (c == 0) | (c == n_cols - 1)
    own_j = c == 0
    own_j = own_j.astype(jnp.int32)

    def send_tile(chunk, to_r, to_c, there):
        rows, where, is_outer = chunks[chunk]
        src, dst = where(to_r)
        skip = (to_c == 0).astype(jnp.int32)
        edge = (to_c == 0) | (to_c == n_cols - 1)
        if is_outer:
            there = there & (to_r > 0) & (to_r < n_rows - 1)

        def copy(count, src_j, dst_j):
            pltpu.make_async_remote_copy(
                src_ref=packed.at[pl.ds(src, rows), pl.ds(src_j, count)],
                dst_ref=recv.at[me, pl.ds(dst, rows), pl.ds(dst_j, count)],
                send_sem=send_sem.at[chunk],
                recv_sem=recv_sem.at[chunk],
                device_id=device(to_r, to_c),
                device_id_type=MESH,
            ).start()

        pl.when(there & edge)(lambda: copy(win_j - 1, tile_j * to_c - 1 + skip, skip))
        pl.when(there & jnp.logical_not(edge))(lambda: copy(win_j, tile_j * to_c - 1, 0))

    chips = n_rows // 2
    ahead_r, ahead_c = AHEAD

    def step(t, table):
        value = jnp.int32(table[-1])
        for k, entry in enumerate(table[:-1]):
            value = jnp.where(t == k, entry, value)
        return value

    def turn_to(t):
        dx = step(t, CHIPS_ALONG)
        return lax.rem(r // 2 + dx, chips), dx

    def send_chip(chunk, t, rest, where=None):
        x, dx = turn_to(t)
        way = 1 - 2 * lax.rem(par + t, 2)
        for other, dy in CHIP_ORDER:
            to_r = 2 * x + (1 - par if other else par)
            to_c = lax.rem(c + way * dy + n_cols, n_cols)
            there = True
            if not other and dy == 0:
                there = dx > 0
            if rest:
                there = there & jnp.logical_not((to_r == ahead_r) & (to_c == ahead_c))
            if where is not None:
                there = there & where(to_c)
            send_tile(chunk, to_r, to_c, there)

    def send_ahead(chunk):
        send_tile(chunk, jnp.int32(ahead_r), jnp.int32(ahead_c), (r != ahead_r) | (c != ahead_c))

    def send_chunk(chunk):

        def first_column(t, carry):
            x, _ = turn_to(t)
            for other in range(2):
                to_r = 2 * x + (1 - par if other else par)
                there = ((to_r != r) | (c != 0)) & (to_r != ahead_r)
                send_tile(chunk, to_r, jnp.int32(0), there)
            return carry

        where = None
        if chunk in COLUMN_FIRST:
            lax.fori_loop(0, chips, first_column, 0)
            where = lambda to_c: to_c > 0

        def body(t, carry):
            send_chip(chunk, t, True, where)
            return carry

        lax.fori_loop(0, chips, body, 0)

    params[0].wait()
    for dw in range(3):
        w1own[dw] = jnp.concatenate([w1s[1, dw], w1s[0, dw]], axis=1)
    w1own[3] = jnp.concatenate([w1s[2, 0], w1s[2, 1]], axis=1)
    w1own[4] = jnp.concatenate([w1s[2, 2], jnp.zeros_like(w1s[2, 2])], axis=1)
    w1all[r // 2, par, c] = w1own[...]

    for copy in loads[0]:
        copy.wait()
    pack_rows(turn_to(0)[0], *groups[0][0])
    pl.semaphore_wait(barrier, sources - 1)

    def send_weights():
        for kr in range(0, n_rows, 2):
            for kc in range(n_cols):
                if kr or kc:
                    pltpu.make_async_remote_copy(
                        src_ref=w1own,
                        dst_ref=w1all.at[r // 2, par, c],
                        send_sem=wsend_sem,
                        recv_sem=wrecv_sem,
                        device_id=device(to_rs[kr], to_cs[kc]),
                        device_id_type=MESH,
                    ).start()

    def pack_and_send(t, carry):
        pl.when(t < chips - 1)(lambda: pack_rows(turn_to(t + 1)[0], *groups[0][0]))
        send_chip(0, t, False)
        pl.when(t == 0)(send_weights)
        return carry

    lax.fori_loop(0, chips, pack_and_send, 0)

    pack(1)
    pack(2)
    send_ahead(1)
    send_ahead(2)
    send_chunk(1)
    send_ahead(3)
    send_chunk(2)
    send_chunk(3)

    def wait_bytes(ref, sem):
        pltpu.make_async_copy(ref, ref, sem).wait()

    w1_bytes = recv.at[0 : sources // 2 - 1, 0, 0:5]
    wait_bytes(w1_bytes, wrecv_sem)
    wait_bytes(w1_bytes, wsend_sem)
    partner = device(r + 1 - 2 * par, c)
    w_swap = pltpu.make_async_remote_copy(
        src_ref=w1all.at[:, par],
        dst_ref=w1all.at[:, par],
        send_sem=wswap_send_sem,
        recv_sem=wswap_recv_sem,
        device_id=partner,
        device_id_type=MESH,
    )
    w_swap.start()

    def own_rows(chunk):
        rows, where, _ = chunks[chunk]
        src, dst = where(r)

        def copy(count, src_j, dst_j):
            for h in range(rows):
                recv[me, dst + h, pl.ds(dst_j, count)] = packed[src + h, pl.ds(src_j, count)]

        pl.when(at_edge)(lambda: copy(win_j - 1, tile_j * c - 1 + own_j, own_j))
        pl.when(jnp.logical_not(at_edge))(lambda: copy(win_j, tile_j * c - 1, 0))

    for chunk in range(3):
        own_rows(chunk)
    pl.when(jnp.logical_not(no_outer))(lambda: own_rows(3))

    zero_row = jnp.zeros((win_j, 2, 2 * images), BF16)
    zero_col = jnp.zeros((tile_h + 2, 2, 2 * images), BF16)

    def clear(s, carry):
        recv[s, last * (1 - par)] = zero_row
        return carry

    def clear_outer(s, carry):
        recv[s, (last - 1) * par] = zero_row
        recv[s, (last - 1) * par + 1] = zero_row
        return carry

    def clear_edge(s, carry):
        recv[s, pl.ds(3 * par, tile_h + 2), (win_j - 1) * (1 - own_j)] = zero_col
        return carry

    lax.fori_loop(0, sources, clear, 0)
    pl.when(no_outer)(lambda: (lax.fori_loop(0, sources, clear_outer, 0), None)[1])
    pl.when(at_edge)(lambda: (lax.fori_loop(0, sources, clear_edge, 0), None)[1])

    low = lax.broadcasted_iota(jnp.int32, (chans, 2 * chans), 1) < chans

    def spread(wt, u, v, dw):
        ur, vr = pltpu.roll(u, chans, 1), pltpu.roll(v, chans, 1)
        zero = jnp.zeros_like(u)
        tiles = (jnp.where(low, ur, zero), u, jnp.where(low, v, ur), jnp.where(low, zero, vr))
        for k, tile in enumerate(tiles):
            tile = tile.astype(BF16)
            for b in range(2):
                wt[dw + b, k * chans : (k + 1) * chans, b * 2 * chans : (b + 1) * 2 * chans] = tile

    def blank(wt):
        zero = jnp.zeros((4 * chans, 2 * chans), BF16)
        wt[3, :, 0 : 2 * chans] = zero
        wt[0, :, 2 * chans : 4 * chans] = zero

    for copy in params[1:]:
        copy.wait()
    blank(wt1)
    blank(wt2)
    for dw in range(3):
        w = [w2s[dh, dw].astype(F32) for dh in range(3)]
        spread(
            wt2,
            jnp.concatenate([w[1], w[0]], axis=1),
            jnp.concatenate([w[2], jnp.zeros_like(w[2])], axis=1),
            dw,
        )
    bias1[...] = jnp.concatenate([b1s[...]] * 4, axis=1)
    bias2[...] = jnp.concatenate([b2s[...]] * 4, axis=1)

    def arrived(chunk):
        def wait(count):
            wait_bytes(recv.at[0 : sources - 1, 0 : chunks[chunk][0], 0:count], recv_sem.at[chunk])

        pl.when(at_edge)(lambda: wait(win_j - 1))
        pl.when(jnp.logical_not(at_edge))(lambda: wait(win_j))

    arrived(0)
    give = tile_h - (tile_h - 3) * par
    land = tile_h + 2 - (tile_h + 1) * (1 - par)
    swap = pltpu.make_async_remote_copy(
        src_ref=recv.at[:, pl.ds(give, 2)],
        dst_ref=recv.at[:, pl.ds(land, 2)],
        send_sem=swap_send_sem,
        recv_sem=swap_recv_sem,
        device_id=partner,
        device_id_type=MESH,
    )
    swap.start()

    w_swap.wait()
    u = [w1all[:, :, :, k].reshape(chans, 2 * chans).astype(F32) for k in range(5)]
    for dw in range(3):
        v = (u[3], pltpu.roll(u[3], chans, 1), u[4])[dw]
        spread(wt1, u[dw], jnp.where(low, v, 0.0), dw)

    x_pairs, z_pairs = xmat.shape[0], ymat.shape[0]
    o_pairs = z_pairs - 1

    def nth(n, count):
        return (count - 1) * (1 - par) + n * (2 * par - 1)

    def turn_one(n, carry):
        i = nth(n, x_pairs)

        def put(j, value):
            xmat[i, j] = value

        turn(recv, i, put)
        return carry

    def first_one(n, carry):
        i = nth(n, z_pairs)
        fill = jnp.where(n == 0, 1 - par, 2)
        out_of = jnp.where(n == z_pairs - 1, jnp.where(r == 0, 0, jnp.where(r == n_rows - 1, 1, 2)), 2)
        blank_a = jnp.where(fill < 2, fill, out_of)
        first((xmat.at[i], xmat.at[i + 1]), lambda dw: wt1[dw], bias1[...], ymat.at[i], blank_a)
        return carry

    def second_one(n, carry):
        i = nth(n, o_pairs)
        second((ymat.at[i], ymat.at[i + 1]), lambda dw: wt2[dw], bias2[...], out.at[pl.ds(2 * i, 2)])
        return carry

    def stage(s, carry):
        @pl.when(s == 0)
        def _():
            swap.wait()

        for k in range(1, 4):
            there = s == k
            if k == 3:
                there = there & jnp.logical_not(no_outer)
            pl.when(there)(lambda k=k: arrived(k))

        for ends, one in ((TURNS, turn_one), (FIRSTS, first_one), (SECONDS, second_one)):
            lax.fori_loop(step(s, (0, *ends[:-1])), step(s, ends), one, 0)
        return carry

    lax.fori_loop(0, 4, stage, 0)

    per_edge = n_rows * 2
    for chunk in range(4):
        rows = chunks[chunk][0]
        n_r = n_rows - 2 if chunk == 3 else n_rows
        counts = (n_r * 2, n_r * (n_cols - 2))

        def drain(edge_n, inner_n, rows=rows, chunk=chunk):
            wait_bytes(recv.at[0:edge_n, 0:rows, 0 : win_j - 1], send_sem.at[chunk])
            wait_bytes(recv.at[0:inner_n, 0:rows, 0:win_j], send_sem.at[chunk])

        def drain_own(chunk=chunk, counts=counts, drain=drain):
            pl.when(at_edge)(lambda: drain(counts[0] - 1, counts[1]))
            pl.when(jnp.logical_not(at_edge))(lambda: drain(counts[0], counts[1] - 1))

        if chunk == 3:
            pl.when(no_outer)(lambda: drain(*counts))
            pl.when(jnp.logical_not(no_outer))(drain_own)
        else:
            drain_own()


def tail_kernel(tile, ymat, wt2, bias2, out_hbm, o_new, sem):
    par = lax.rem(lax.axis_index("model"), 2)
    rows = out_hbm.shape[0]
    o_pairs = ymat.shape[0] - 1
    late = (rows - 2) * par
    here = 2 * (1 - par)

    def start(k, carry):
        pltpu.make_async_copy(tile.at[par + k], out_hbm.at[k], sem.at[0]).start()
        return carry

    lax.fori_loop(here, here + rows - 2, start, 0)
    i = (o_pairs - 1) * par
    second((ymat.at[i], ymat.at[i + 1]), lambda dw: wt2[dw], bias2[...], o_new)
    last = pltpu.make_async_copy(o_new, out_hbm.at[pl.ds(late, 2)], sem.at[1])
    last.start()
    pltpu.make_async_copy(tile.at[0 : rows - 2], out_hbm.at[0 : rows - 2], sem.at[0]).wait()
    last.wait()


def solution(mesh):
    n_rows = mesh.shape["model"]
    n_cols = mesh.shape["cols"]

    def run_local(x_in, w_conv1, b_conv1, w_conv2, b_conv2):
        images, height, width, own_chans = x_in.shape
        sources = n_rows * n_cols
        chans = own_chans * sources
        pairs = width // 2
        tile_h, tile_j = height // n_rows, pairs // n_cols
        win_j = tile_j + 2
        x_pairs, z_pairs = (tile_h + 5) // 2, (tile_h + 3) // 2
        x_t = jnp.transpose(x_in, (1, 2, 3, 0)).reshape(n_rows // 2, 2 * tile_h, pairs, 2, own_chans, images)
        args = (x_t, w_conv1, b_conv1.reshape(1, chans), w_conv2, b_conv2.reshape(1, chans))
        hbm = pl.BlockSpec(memory_space=pltpu.HBM)
        vmem = pl.BlockSpec(memory_space=pltpu.VMEM)
        kept = (
            pltpu.VMEM((2 * (z_pairs - 1), tile_j, 2, images, chans), F32),
            pltpu.VMEM((z_pairs, win_j - 1, 2, images, 2 * chans), BF16),
            pltpu.VMEM((4, 4 * chans, 4 * chans), BF16),
            pltpu.VMEM((1, 4 * chans), F32),
        )
        state = pl.pallas_call(
            functools.partial(conv_kernel, n_rows, n_cols),
            out_shape=kept,
            in_specs=[hbm] * 5,
            out_specs=[vmem] * len(kept),
            scratch_shapes=[
                pltpu.VMEM((sources, 2 * x_pairs, win_j, own_chans, 2 * images), BF16),
                pltpu.VMEM((x_pairs, win_j, 2, images, 2 * chans), BF16),
                pltpu.VMEM((4, 4 * chans, 4 * chans), BF16),
                pltpu.VMEM((1, 4 * chans), F32),
                pltpu.VMEM((n_rows // 2, 2 * tile_h, pairs, 2, own_chans, images), BF16),
                pltpu.VMEM((height, pairs, own_chans, 2 * images), BF16),
                pltpu.VMEM((3, 3, own_chans, chans), BF16),
                pltpu.VMEM((5, own_chans, 2 * chans), BF16),
                pltpu.VMEM((n_rows // 2, 2, n_cols, 5, own_chans, 2 * chans), BF16),
                pltpu.VMEM((3, 3, chans, chans), BF16),
                pltpu.VMEM((1, chans), F32),
                pltpu.VMEM((1, chans), F32),
                pltpu.SemaphoreType.DMA((3, 2)),
                pltpu.SemaphoreType.DMA((4,)),
                pltpu.SemaphoreType.DMA((4,)),
                pltpu.SemaphoreType.DMA((4,)),
            ]
            + [pltpu.SemaphoreType.DMA] * 6,
            compiler_params=pltpu.CompilerParams(
                collective_id=0, has_side_effects=True, vmem_limit_bytes=24 << 20
            ),
            name="conv",
        )(*(pltpu.with_memory_space_constraint(a, pltpu.HBM) for a in args))
        out = pl.pallas_call(
            tail_kernel,
            out_shape=jax.ShapeDtypeStruct((tile_h, tile_j, 2, images, chans), F32),
            in_specs=[vmem] * len(kept),
            out_specs=pl.BlockSpec(memory_space=pl.ANY),
            scratch_shapes=[
                pltpu.VMEM((2, tile_j, 2, images, chans), F32),
                pltpu.SemaphoreType.DMA((2,)),
            ],
            compiler_params=pltpu.CompilerParams(vmem_limit_bytes=8 << 20),
            name="tail",
        )(*state)
        out = out.reshape(tile_h, 2 * tile_j, images, chans)
        return jnp.transpose(out, (2, 0, 1, 3))

    group = ("model", "cols")
    return jax.shard_map(
        run_local,
        mesh=mesh,
        in_specs=(P("data", None, None, group), P(None, None, group, None), P(), P(), P()),
        out_specs=P("data", "model", "cols", None),
        check_vma=False,
    )
```

```python
import functools

import jax
import jax.numpy as jnp
from jax import lax
from jax.experimental import pallas as pl
from jax.experimental.pallas import tpu as pltpu
from jax.sharding import PartitionSpec as P

MESH = pl.DeviceIdType.MESH
BF16 = jnp.bfloat16
F32 = jnp.float32
CHUNK_ROWS = (2, 3, 2)
TURNS, FIRSTS, SECONDS = (2, 4, 5, 6), (1, 3, 4, 5), (0, 2, 3, 3)
AHEAD = (1, 0)
COLUMN_FIRST = (2, 3)
CHIPS_ALONG = (3, 1, 2, 0)
CHIP_ORDER = tuple((other, dy) for other in (0, 1) for dy in (1, -1, 0, 2))


def turn(recv, i, put):
    sources, _, win_j, own_chans, lanes = recv.shape
    chans = sources * own_chans
    for j in range(win_j):
        top = recv[:, 2 * i, j].reshape(chans, lanes)
        under = recv[:, 2 * i + 1, j].reshape(chans, lanes)
        put(j, jnp.concatenate([top, under], axis=0).T.reshape(2, lanes // 2, 2 * chans))


def blocks(pairs, weights, count):
    acc = None
    for dw in range(4):
        parts = [view[dw // 2 : dw // 2 + count, dw % 2] for view in pairs]
        lhs = jnp.concatenate([p.reshape(count * p.shape[1], p.shape[2]) for p in parts], axis=1)
        term = jnp.dot(lhs, weights(dw), preferred_element_type=F32)
        acc = term if acc is None else acc + term
    return acc


def first(pairs, weights, bias, y_row, blank_a):
    count, _, images, lanes = y_row.shape
    c = lax.axis_index("cols")
    row = lax.rem(lax.broadcasted_iota(jnp.int32, (1, 2 * lanes), 1), lanes) // (lanes // 2)
    act = jnp.maximum(blocks(pairs, weights, count) + bias, 0.0)
    act = jnp.where(row != blank_a, act, 0.0).astype(BF16)
    for b in range(2):
        y_row[:, b] = act[:, b * lanes : (b + 1) * lanes].reshape(count, images, lanes)
    blank = jnp.zeros((images, lanes), BF16)

    @pl.when(c == 0)
    def _():
        y_row[0, 0] = blank

    @pl.when(c == lax.axis_size("cols") - 1)
    def _():
        y_row[count - 1, 1] = blank


def second(pairs, weights, bias, out_pair):
    _, count, _, images, chans = out_pair.shape
    res = blocks(pairs, weights, count) + bias
    for b in range(2):
        for a in range(2):
            at = (2 * b + a) * chans
            out_pair[a, :, b] = res[:, at : at + chans].reshape(count, images, chans)


def conv_kernel(
    n_rows,
    n_cols,
    x_hbm,
    w1_hbm,
    b1_hbm,
    w2_hbm,
    b2_hbm,
    out,
    ymat,
    wt2,
    bias2,
    recv,
    xmat,
    wt1,
    bias1,
    xs,
    packed,
    w1s,
    w1own,
    w1all,
    w2s,
    b1s,
    b2s,
    load_sem,
    par_sem,
    send_sem,
    recv_sem,
    wsend_sem,
    wrecv_sem,
    swap_send_sem,
    swap_recv_sem,
    wswap_send_sem,
    wswap_recv_sem,
):
    chip_h, pairs = xs.shape[1:3]
    images = xs.shape[-1]
    tile_h, tile_j = chip_h // 2, pairs // n_cols
    win_j = tile_j + 2
    sources = n_rows * n_cols
    r, c = lax.axis_index("model"), lax.axis_index("cols")
    par = lax.rem(r, 2)
    me = r * n_cols + c
    chans = recv.shape[0] * 2

    tops = [tile_h - sum(CHUNK_ROWS[: k + 1]) for k in range(len(CHUNK_ROWS))]
    groups = (
        ((tops[0], chip_h - tops[0]),),
        *(((k, k + n), (chip_h - k - n, chip_h - k)) for k, n in zip(tops[1:], CHUNK_ROWS[1:])),
    )
    loads = []
    for g, spans in enumerate(groups):
        loads.append(
            [
                pltpu.make_async_copy(x_hbm.at[:, lo:hi], xs.at[:, lo:hi], load_sem.at[g, n])
                for n, (lo, hi) in enumerate(spans)
            ]
        )
    for copies in loads:
        for copy in copies:
            copy.start()
    params = [
        pltpu.make_async_copy(src, dst, par_sem.at[s])
        for s, (src, dst) in enumerate(((w1_hbm, w1s), (w2_hbm, w2s), (b1_hbm, b1s), (b2_hbm, b2s)))
    ]
    for copy in params:
        copy.start()

    barrier = pltpu.get_barrier_semaphore()
    to_cs = [lax.rem(c + k, n_cols) for k in range(n_cols)]

    def device(to_r, to_c):
        return {"model": to_r, "cols": to_c}

    to_rs = [lax.rem(r + k, n_rows) for k in range(n_rows)]
    for kr, kc in sorted(
        ((kr, kc) for kr in range(n_rows) for kc in range(n_cols) if kr or kc),
        key=lambda k: (not (k[0] in (2, 3) and k[1] == 1), -(min(k[0], n_rows - k[0]) // 2 + min(k[1], n_cols - k[1]))),
    ):
        pl.semaphore_signal(barrier, inc=1, device_id=device(to_rs[kr], to_cs[kc]), device_id_type=MESH)

    def pack_rows(x, lo, hi):
        rows = hi - lo
        left, right = (xs[x, lo:hi, :, p].reshape(rows * pairs * 2, images) for p in range(2))
        both = jnp.concatenate([left, right], axis=1)
        packed[pl.ds(chip_h * x + lo, rows)] = both.reshape(rows, pairs, 2, 2 * images)

    def pack(g):
        for copy in loads[g]:
            copy.wait()

        def body(x, carry):
            for lo, hi in groups[g]:
                pack_rows(x, lo, hi)
            return carry

        lax.fori_loop(0, n_rows // 2, body, 0)

    last = tile_h + 4

    def rows_of(offset, count):
        def where(to_r):
            q = lax.rem(to_r, 2)
            src = tile_h * to_r + offset + (tile_h - count - 2 * offset) * q
            dst = offset + 2 + (last - count - 2 * offset - 3) * q
            return src, dst

        return where

    chunks = (
        *((n, rows_of(k, n), False) for k, n in zip(tops, CHUNK_ROWS)),
        (2, rows_of(-2, 2), True),
    )
    no_outer = (r == 0) | (r == n_rows - 1)
    at_edge = (c == 0) | (c == n_cols - 1)
    own_j = c == 0
    own_j = own_j.astype(jnp.int32)

    def send_tile(chunk, to_r, to_c, there):
        rows, where, is_outer = chunks[chunk]
        src, dst = where(to_r)
        skip = (to_c == 0).astype(jnp.int32)
        edge = (to_c == 0) | (to_c == n_cols - 1)
        if is_outer:
            there = there & (to_r > 0) & (to_r < n_rows - 1)

        def copy(count, src_j, dst_j):
            pltpu.make_async_remote_copy(
                src_ref=packed.at[pl.ds(src, rows), pl.ds(src_j, count)],
                dst_ref=recv.at[me, pl.ds(dst, rows), pl.ds(dst_j, count)],
                send_sem=send_sem.at[chunk],
                recv_sem=recv_sem.at[chunk],
                device_id=device(to_r, to_c),
                device_id_type=MESH,
            ).start()

        pl.when(there & edge)(lambda: copy(win_j - 1, tile_j * to_c - 1 + skip, skip))
        pl.when(there & jnp.logical_not(edge))(lambda: copy(win_j, tile_j * to_c - 1, 0))

    chips = n_rows // 2
    ahead_r, ahead_c = AHEAD

    def step(t, table):
        value = jnp.int32(table[-1])
        for k, entry in enumerate(table[:-1]):
            value = jnp.where(t == k, entry, value)
        return value

    def turn_to(t):
        dx = step(t, CHIPS_ALONG)
        return lax.rem(r // 2 + dx, chips), dx

    def send_chip(chunk, t, rest, where=None):
        x, dx = turn_to(t)
        way = 1 - 2 * lax.rem(par + t, 2)
        for other, dy in CHIP_ORDER:
            to_r = 2 * x + (1 - par if other else par)
            to_c = lax.rem(c + way * dy + n_cols, n_cols)
            there = True
            if not other and dy == 0:
                there = dx > 0
            if rest:
                there = there & jnp.logical_not((to_r == ahead_r) & (to_c == ahead_c))
            if where is not None:
                there = there & where(to_c)
            send_tile(chunk, to_r, to_c, there)

    def send_ahead(chunk):
        send_tile(chunk, jnp.int32(ahead_r), jnp.int32(ahead_c), (r != ahead_r) | (c != ahead_c))

    def send_chunk(chunk):

        def first_column(t, carry):
            x, _ = turn_to(t)
            for other in range(2):
                to_r = 2 * x + (1 - par if other else par)
                there = ((to_r != r) | (c != 0)) & (to_r != ahead_r)
                send_tile(chunk, to_r, jnp.int32(0), there)
            return carry

        where = None
        if chunk in COLUMN_FIRST:
            lax.fori_loop(0, chips, first_column, 0)
            where = lambda to_c: to_c > 0

        def body(t, carry):
            send_chip(chunk, t, True, where)
            return carry

        lax.fori_loop(0, chips, body, 0)

    params[0].wait()
    for dw in range(3):
        w1own[dw] = jnp.concatenate([w1s[1, dw], w1s[0, dw]], axis=1)
    w1own[3] = jnp.concatenate([w1s[2, 0], w1s[2, 1]], axis=1)
    w1own[4] = jnp.concatenate([w1s[2, 2], jnp.zeros_like(w1s[2, 2])], axis=1)
    w1all[r // 2, par, c] = w1own[...]

    for copy in loads[0]:
        copy.wait()
    pack_rows(turn_to(0)[0], *groups[0][0])
    pl.semaphore_wait(barrier, sources - 1)

    def send_weights():
        for kr in range(0, n_rows, 2):
            for kc in range(n_cols):
                if kr or kc:
                    pltpu.make_async_remote_copy(
                        src_ref=w1own,
                        dst_ref=w1all.at[r // 2, par, c],
                        send_sem=wsend_sem,
                        recv_sem=wrecv_sem,
                        device_id=device(to_rs[kr], to_cs[kc]),
                        device_id_type=MESH,
                    ).start()

    def pack_and_send(t, carry):
        pl.when(t < chips - 1)(lambda: pack_rows(turn_to(t + 1)[0], *groups[0][0]))
        send_chip(0, t, False)
        pl.when(t == 0)(send_weights)
        return carry

    lax.fori_loop(0, chips, pack_and_send, 0)

    pack(1)
    send_ahead(1)
    send_chunk(1)
    pack(2)
    send_ahead(2)
    send_ahead(3)
    send_chunk(2)
    send_chunk(3)

    def wait_bytes(ref, sem):
        pltpu.make_async_copy(ref, ref, sem).wait()

    w1_bytes = recv.at[0 : sources // 2 - 1, 0, 0:5]
    wait_bytes(w1_bytes, wrecv_sem)
    wait_bytes(w1_bytes, wsend_sem)
    partner = device(r + 1 - 2 * par, c)
    w_swap = pltpu.make_async_remote_copy(
        src_ref=w1all.at[:, par],
        dst_ref=w1all.at[:, par],
        send_sem=wswap_send_sem,
        recv_sem=wswap_recv_sem,
        device_id=partner,
        device_id_type=MESH,
    )
    w_swap.start()

    def own_rows(chunk):
        rows, where, _ = chunks[chunk]
        src, dst = where(r)

        def copy(count, src_j, dst_j):
            for h in range(rows):
                recv[me, dst + h, pl.ds(dst_j, count)] = packed[src + h, pl.ds(src_j, count)]

        pl.when(at_edge)(lambda: copy(win_j - 1, tile_j * c - 1 + own_j, own_j))
        pl.when(jnp.logical_not(at_edge))(lambda: copy(win_j, tile_j * c - 1, 0))

    for chunk in range(3):
        own_rows(chunk)
    pl.when(jnp.logical_not(no_outer))(lambda: own_rows(3))

    zero_row = jnp.zeros((win_j, 2, 2 * images), BF16)
    zero_col = jnp.zeros((tile_h + 2, 2, 2 * images), BF16)

    def clear(s, carry):
        recv[s, last * (1 - par)] = zero_row
        return carry

    def clear_outer(s, carry):
        recv[s, (last - 1) * par] = zero_row
        recv[s, (last - 1) * par + 1] = zero_row
        return carry

    def clear_edge(s, carry):
        recv[s, pl.ds(3 * par, tile_h + 2), (win_j - 1) * (1 - own_j)] = zero_col
        return carry

    lax.fori_loop(0, sources, clear, 0)
    pl.when(no_outer)(lambda: (lax.fori_loop(0, sources, clear_outer, 0), None)[1])
    pl.when(at_edge)(lambda: (lax.fori_loop(0, sources, clear_edge, 0), None)[1])

    low = lax.broadcasted_iota(jnp.int32, (chans, 2 * chans), 1) < chans

    def spread(wt, u, v, dw):
        ur, vr = pltpu.roll(u, chans, 1), pltpu.roll(v, chans, 1)
        zero = jnp.zeros_like(u)
        tiles = (jnp.where(low, ur, zero), u, jnp.where(low, v, ur), jnp.where(low, zero, vr))
        for k, tile in enumerate(tiles):
            tile = tile.astype(BF16)
            for b in range(2):
                wt[dw + b, k * chans : (k + 1) * chans, b * 2 * chans : (b + 1) * 2 * chans] = tile

    def blank(wt):
        zero = jnp.zeros((4 * chans, 2 * chans), BF16)
        wt[3, :, 0 : 2 * chans] = zero
        wt[0, :, 2 * chans : 4 * chans] = zero

    for copy in params[1:]:
        copy.wait()
    blank(wt1)
    blank(wt2)
    for dw in range(3):
        w = [w2s[dh, dw].astype(F32) for dh in range(3)]
        spread(
            wt2,
            jnp.concatenate([w[1], w[0]], axis=1),
            jnp.concatenate([w[2], jnp.zeros_like(w[2])], axis=1),
            dw,
        )
    bias1[...] = jnp.concatenate([b1s[...]] * 4, axis=1)
    bias2[...] = jnp.concatenate([b2s[...]] * 4, axis=1)

    def arrived(chunk):
        def wait(count):
            wait_bytes(recv.at[0 : sources - 1, 0 : chunks[chunk][0], 0:count], recv_sem.at[chunk])

        pl.when(at_edge)(lambda: wait(win_j - 1))
        pl.when(jnp.logical_not(at_edge))(lambda: wait(win_j))

    arrived(0)
    give = tile_h - (tile_h - 3) * par
    land = tile_h + 2 - (tile_h + 1) * (1 - par)
    swap = pltpu.make_async_remote_copy(
        src_ref=recv.at[:, pl.ds(give, 2)],
        dst_ref=recv.at[:, pl.ds(land, 2)],
        send_sem=swap_send_sem,
        recv_sem=swap_recv_sem,
        device_id=partner,
        device_id_type=MESH,
    )
    swap.start()

    w_swap.wait()
    u = [w1all[:, :, :, k].reshape(chans, 2 * chans).astype(F32) for k in range(5)]
    for dw in range(3):
        v = (u[3], pltpu.roll(u[3], chans, 1), u[4])[dw]
        spread(wt1, u[dw], jnp.where(low, v, 0.0), dw)

    x_pairs, z_pairs = xmat.shape[0], ymat.shape[0]
    o_pairs = z_pairs - 1

    def nth(n, count):
        return (count - 1) * (1 - par) + n * (2 * par - 1)

    def turn_one(n, carry):
        i = nth(n, x_pairs)

        def put(j, value):
            xmat[i, j] = value

        turn(recv, i, put)
        return carry

    def first_one(n, carry):
        i = nth(n, z_pairs)
        fill = jnp.where(n == 0, 1 - par, 2)
        out_of = jnp.where(n == z_pairs - 1, jnp.where(r == 0, 0, jnp.where(r == n_rows - 1, 1, 2)), 2)
        blank_a = jnp.where(fill < 2, fill, out_of)
        first((xmat.at[i], xmat.at[i + 1]), lambda dw: wt1[dw], bias1[...], ymat.at[i], blank_a)
        return carry

    def second_one(n, carry):
        i = nth(n, o_pairs)
        second((ymat.at[i], ymat.at[i + 1]), lambda dw: wt2[dw], bias2[...], out.at[pl.ds(2 * i, 2)])
        return carry

    def stage(s, carry):
        @pl.when(s == 0)
        def _():
            swap.wait()

        for k in range(1, 4):
            there = s == k
            if k == 3:
                there = there & jnp.logical_not(no_outer)
            pl.when(there)(lambda k=k: arrived(k))

        for ends, one in ((TURNS, turn_one), (FIRSTS, first_one), (SECONDS, second_one)):
            lax.fori_loop(step(s, (0, *ends[:-1])), step(s, ends), one, 0)
        return carry

    lax.fori_loop(0, 4, stage, 0)

    per_edge = n_rows * 2
    for chunk in range(4):
        rows = chunks[chunk][0]
        n_r = n_rows - 2 if chunk == 3 else n_rows
        counts = (n_r * 2, n_r * (n_cols - 2))

        def drain(edge_n, inner_n, rows=rows, chunk=chunk):
            wait_bytes(recv.at[0:edge_n, 0:rows, 0 : win_j - 1], send_sem.at[chunk])
            wait_bytes(recv.at[0:inner_n, 0:rows, 0:win_j], send_sem.at[chunk])

        def drain_own(chunk=chunk, counts=counts, drain=drain):
            pl.when(at_edge)(lambda: drain(counts[0] - 1, counts[1]))
            pl.when(jnp.logical_not(at_edge))(lambda: drain(counts[0], counts[1] - 1))

        if chunk == 3:
            pl.when(no_outer)(lambda: drain(*counts))
            pl.when(jnp.logical_not(no_outer))(drain_own)
        else:
            drain_own()


def tail_kernel(tile, ymat, wt2, bias2, out_hbm, o_new, sem):
    par = lax.rem(lax.axis_index("model"), 2)
    rows = out_hbm.shape[0]
    o_pairs = ymat.shape[0] - 1
    late = (rows - 2) * par
    here = 2 * (1 - par)

    def start(k, carry):
        pltpu.make_async_copy(tile.at[par + k], out_hbm.at[k], sem.at[0]).start()
        return carry

    lax.fori_loop(here, here + rows - 2, start, 0)
    i = (o_pairs - 1) * par
    second((ymat.at[i], ymat.at[i + 1]), lambda dw: wt2[dw], bias2[...], o_new)
    last = pltpu.make_async_copy(o_new, out_hbm.at[pl.ds(late, 2)], sem.at[1])
    last.start()
    pltpu.make_async_copy(tile.at[0 : rows - 2], out_hbm.at[0 : rows - 2], sem.at[0]).wait()
    last.wait()


def solution(mesh):
    n_rows = mesh.shape["model"]
    n_cols = mesh.shape["cols"]

    def run_local(x_in, w_conv1, b_conv1, w_conv2, b_conv2):
        images, height, width, own_chans = x_in.shape
        sources = n_rows * n_cols
        chans = own_chans * sources
        pairs = width // 2
        tile_h, tile_j = height // n_rows, pairs // n_cols
        win_j = tile_j + 2
        x_pairs, z_pairs = (tile_h + 5) // 2, (tile_h + 3) // 2
        x_t = jnp.transpose(x_in, (1, 2, 3, 0)).reshape(n_rows // 2, 2 * tile_h, pairs, 2, own_chans, images)
        args = (x_t, w_conv1, b_conv1.reshape(1, chans), w_conv2, b_conv2.reshape(1, chans))
        hbm = pl.BlockSpec(memory_space=pltpu.HBM)
        vmem = pl.BlockSpec(memory_space=pltpu.VMEM)
        kept = (
            pltpu.VMEM((2 * (z_pairs - 1), tile_j, 2, images, chans), F32),
            pltpu.VMEM((z_pairs, win_j - 1, 2, images, 2 * chans), BF16),
            pltpu.VMEM((4, 4 * chans, 4 * chans), BF16),
            pltpu.VMEM((1, 4 * chans), F32),
        )
        state = pl.pallas_call(
            functools.partial(conv_kernel, n_rows, n_cols),
            out_shape=kept,
            in_specs=[hbm] * 5,
            out_specs=[vmem] * len(kept),
            scratch_shapes=[
                pltpu.VMEM((sources, 2 * x_pairs, win_j, own_chans, 2 * images), BF16),
                pltpu.VMEM((x_pairs, win_j, 2, images, 2 * chans), BF16),
                pltpu.VMEM((4, 4 * chans, 4 * chans), BF16),
                pltpu.VMEM((1, 4 * chans), F32),
                pltpu.VMEM((n_rows // 2, 2 * tile_h, pairs, 2, own_chans, images), BF16),
                pltpu.VMEM((height, pairs, own_chans, 2 * images), BF16),
                pltpu.VMEM((3, 3, own_chans, chans), BF16),
                pltpu.VMEM((5, own_chans, 2 * chans), BF16),
                pltpu.VMEM((n_rows // 2, 2, n_cols, 5, own_chans, 2 * chans), BF16),
                pltpu.VMEM((3, 3, chans, chans), BF16),
                pltpu.VMEM((1, chans), F32),
                pltpu.VMEM((1, chans), F32),
                pltpu.SemaphoreType.DMA((3, 2)),
                pltpu.SemaphoreType.DMA((4,)),
                pltpu.SemaphoreType.DMA((4,)),
                pltpu.SemaphoreType.DMA((4,)),
            ]
            + [pltpu.SemaphoreType.DMA] * 6,
            compiler_params=pltpu.CompilerParams(
                collective_id=0, has_side_effects=True, vmem_limit_bytes=24 << 20
            ),
            name="conv",
        )(*(pltpu.with_memory_space_constraint(a, pltpu.HBM) for a in args))
        out = pl.pallas_call(
            tail_kernel,
            out_shape=jax.ShapeDtypeStruct((tile_h, tile_j, 2, images, chans), F32),
            in_specs=[vmem] * len(kept),
            out_specs=pl.BlockSpec(memory_space=pl.ANY),
            scratch_shapes=[
                pltpu.VMEM((2, tile_j, 2, images, chans), F32),
                pltpu.SemaphoreType.DMA((2,)),
            ],
            compiler_params=pltpu.CompilerParams(vmem_limit_bytes=8 << 20),
            name="tail",
        )(*state)
        out = out.reshape(tile_h, 2 * tile_j, images, chans)
        return jnp.transpose(out, (2, 0, 1, 3))

    group = ("model", "cols")
    return jax.shard_map(
        run_local,
        mesh=mesh,
        in_specs=(P("data", None, None, group), P(None, None, group, None), P(), P(), P()),
        out_specs=P("data", "model", "cols", None),
        check_vma=False,
    )
```

```python
import functools

import jax
import jax.numpy as jnp
from jax import lax
from jax.experimental import pallas as pl
from jax.experimental.pallas import tpu as pltpu
from jax.sharding import PartitionSpec as P

MESH = pl.DeviceIdType.MESH
BF16 = jnp.bfloat16
F32 = jnp.float32
CHUNK_ROWS = (2, 3, 2)
TURNS, FIRSTS, SECONDS = (2, 4, 5, 6), (1, 3, 4, 5), (0, 2, 3, 3)
AHEAD = (1, 0)
COLUMN_FIRST = (2, 3)
CHIPS_ALONG = (3, 1, 2, 0)
CHIP_ORDER = tuple((other, dy) for other in (0, 1) for dy in (1, -1, 0, 2))


def turn(recv, i, put):
    sources, _, win_j, own_chans, lanes = recv.shape
    chans = sources * own_chans
    for j in range(win_j):
        top = recv[:, 2 * i, j].reshape(chans, lanes)
        under = recv[:, 2 * i + 1, j].reshape(chans, lanes)
        put(j, jnp.concatenate([top, under], axis=0).T.reshape(2, lanes // 2, 2 * chans))


def blocks(pairs, weights, count):
    acc = None
    for dw in range(4):
        parts = [view[dw // 2 : dw // 2 + count, dw % 2] for view in pairs]
        lhs = jnp.concatenate([p.reshape(count * p.shape[1], p.shape[2]) for p in parts], axis=1)
        term = jnp.dot(lhs, weights(dw), preferred_element_type=F32)
        acc = term if acc is None else acc + term
    return acc


def first(pairs, weights, bias, y_row, blank_a):
    count, _, images, lanes = y_row.shape
    c = lax.axis_index("cols")
    row = lax.rem(lax.broadcasted_iota(jnp.int32, (1, 2 * lanes), 1), lanes) // (lanes // 2)
    act = jnp.maximum(blocks(pairs, weights, count) + bias, 0.0)
    act = jnp.where(row != blank_a, act, 0.0).astype(BF16)
    for b in range(2):
        y_row[:, b] = act[:, b * lanes : (b + 1) * lanes].reshape(count, images, lanes)
    blank = jnp.zeros((images, lanes), BF16)

    @pl.when(c == 0)
    def _():
        y_row[0, 0] = blank

    @pl.when(c == lax.axis_size("cols") - 1)
    def _():
        y_row[count - 1, 1] = blank


def second(pairs, weights, bias, out_pair):
    _, count, _, images, chans = out_pair.shape
    res = blocks(pairs, weights, count) + bias
    for b in range(2):
        for a in range(2):
            at = (2 * b + a) * chans
            out_pair[a, :, b] = res[:, at : at + chans].reshape(count, images, chans)


def conv_kernel(
    n_rows,
    n_cols,
    x_hbm,
    w1_hbm,
    b1_hbm,
    w2_hbm,
    b2_hbm,
    out,
    ymat,
    wt2,
    bias2,
    recv,
    xmat,
    wt1,
    bias1,
    xs,
    packed,
    w1s,
    w1own,
    w1all,
    w2s,
    b1s,
    b2s,
    load_sem,
    par_sem,
    send_sem,
    recv_sem,
    wsend_sem,
    wrecv_sem,
    swap_send_sem,
    swap_recv_sem,
    wswap_send_sem,
    wswap_recv_sem,
):
    chip_h, pairs = xs.shape[1:3]
    images = xs.shape[-1]
    tile_h, tile_j = chip_h // 2, pairs // n_cols
    win_j = tile_j + 2
    sources = n_rows * n_cols
    r, c = lax.axis_index("model"), lax.axis_index("cols")
    par = lax.rem(r, 2)
    me = r * n_cols + c
    chans = recv.shape[0] * 2

    tops = [tile_h - sum(CHUNK_ROWS[: k + 1]) for k in range(len(CHUNK_ROWS))]
    groups = (
        ((tops[0], chip_h - tops[0]),),
        *(((k, k + n), (chip_h - k - n, chip_h - k)) for k, n in zip(tops[1:], CHUNK_ROWS[1:])),
    )
    loads = []
    for g, spans in enumerate(groups):
        loads.append(
            [
                pltpu.make_async_copy(x_hbm.at[:, lo:hi], xs.at[:, lo:hi], load_sem.at[g, n])
                for n, (lo, hi) in enumerate(spans)
            ]
        )
    for copies in loads:
        for copy in copies:
            copy.start()
    params = [
        pltpu.make_async_copy(src, dst, par_sem.at[s])
        for s, (src, dst) in enumerate(((w1_hbm, w1s), (w2_hbm, w2s), (b1_hbm, b1s), (b2_hbm, b2s)))
    ]
    for copy in params:
        copy.start()

    barrier = pltpu.get_barrier_semaphore()
    to_cs = [lax.rem(c + k, n_cols) for k in range(n_cols)]

    def device(to_r, to_c):
        return {"model": to_r, "cols": to_c}

    to_rs = [lax.rem(r + k, n_rows) for k in range(n_rows)]
    for kr, kc in sorted(
        ((kr, kc) for kr in range(n_rows) for kc in range(n_cols) if kr or kc),
        key=lambda k: (not (k[0] in (2, 3) and k[1] == 1), -(min(k[0], n_rows - k[0]) // 2 + min(k[1], n_cols - k[1]))),
    ):
        pl.semaphore_signal(barrier, inc=1, device_id=device(to_rs[kr], to_cs[kc]), device_id_type=MESH)

    def pack_rows(x, lo, hi):
        rows = hi - lo
        left, right = (xs[x, lo:hi, :, p].reshape(rows * pairs * 2, images) for p in range(2))
        both = jnp.concatenate([left, right], axis=1)
        packed[pl.ds(chip_h * x + lo, rows)] = both.reshape(rows, pairs, 2, 2 * images)

    def pack(g):
        for copy in loads[g]:
            copy.wait()

        def body(x, carry):
            for lo, hi in groups[g]:
                pack_rows(x, lo, hi)
            return carry

        lax.fori_loop(0, n_rows // 2, body, 0)

    last = tile_h + 4

    def rows_of(offset, count):
        def where(to_r):
            q = lax.rem(to_r, 2)
            src = tile_h * to_r + offset + (tile_h - count - 2 * offset) * q
            dst = offset + 2 + (last - count - 2 * offset - 3) * q
            return src, dst

        return where

    chunks = (
        *((n, rows_of(k, n), False) for k, n in zip(tops, CHUNK_ROWS)),
        (2, rows_of(-2, 2), True),
    )
    no_outer = (r == 0) | (r == n_rows - 1)
    at_edge = (c == 0) | (c == n_cols - 1)
    own_j = c == 0
    own_j = own_j.astype(jnp.int32)

    def send_tile(chunk, to_r, to_c, there):
        rows, where, is_outer = chunks[chunk]
        src, dst = where(to_r)
        skip = (to_c == 0).astype(jnp.int32)
        edge = (to_c == 0) | (to_c == n_cols - 1)
        if is_outer:
            there = there & (to_r > 0) & (to_r < n_rows - 1)

        def copy(count, src_j, dst_j):
            pltpu.make_async_remote_copy(
                src_ref=packed.at[pl.ds(src, rows), pl.ds(src_j, count)],
                dst_ref=recv.at[me, pl.ds(dst, rows), pl.ds(dst_j, count)],
                send_sem=send_sem.at[chunk],
                recv_sem=recv_sem.at[chunk],
                device_id=device(to_r, to_c),
                device_id_type=MESH,
            ).start()

        pl.when(there & edge)(lambda: copy(win_j - 1, tile_j * to_c - 1 + skip, skip))
        pl.when(there & jnp.logical_not(edge))(lambda: copy(win_j, tile_j * to_c - 1, 0))

    chips = n_rows // 2
    ahead_r, ahead_c = AHEAD

    def step(t, table):
        value = jnp.int32(table[-1])
        for k, entry in enumerate(table[:-1]):
            value = jnp.where(t == k, entry, value)
        return value

    def turn_to(t):
        dx = step(t, CHIPS_ALONG)
        return lax.rem(r // 2 + dx, chips), dx

    def send_chip(chunk, t, rest, where=None):
        x, dx = turn_to(t)
        way = 1 - 2 * lax.rem(par + t, 2)
        for other, dy in CHIP_ORDER:
            to_r = 2 * x + (1 - par if other else par)
            to_c = lax.rem(c + way * dy + n_cols, n_cols)
            there = True
            if not other and dy == 0:
                there = dx > 0
            if rest:
                there = there & jnp.logical_not((to_r == ahead_r) & (to_c == ahead_c))
            if where is not None:
                there = there & where(to_c)
            send_tile(chunk, to_r, to_c, there)

    def send_ahead(chunk):
        send_tile(chunk, jnp.int32(ahead_r), jnp.int32(ahead_c), (r != ahead_r) | (c != ahead_c))

    def send_chunk(chunk):

        def first_column(t, carry):
            x, _ = turn_to(t)
            for other in range(2):
                to_r = 2 * x + (1 - par if other else par)
                there = ((to_r != r) | (c != 0)) & (to_r != ahead_r)
                send_tile(chunk, to_r, jnp.int32(0), there)
            return carry

        where = None
        if chunk in COLUMN_FIRST:
            lax.fori_loop(0, chips, first_column, 0)
            where = lambda to_c: to_c > 0

        def body(t, carry):
            send_chip(chunk, t, chunk > 1, where)
            return carry

        lax.fori_loop(0, chips, body, 0)

    params[0].wait()
    for dw in range(3):
        w1own[dw] = jnp.concatenate([w1s[1, dw], w1s[0, dw]], axis=1)
    w1own[3] = jnp.concatenate([w1s[2, 0], w1s[2, 1]], axis=1)
    w1own[4] = jnp.concatenate([w1s[2, 2], jnp.zeros_like(w1s[2, 2])], axis=1)
    w1all[r // 2, par, c] = w1own[...]

    for copy in loads[0]:
        copy.wait()
    pack_rows(turn_to(0)[0], *groups[0][0])
    pl.semaphore_wait(barrier, sources - 1)

    def send_weights():
        for kr in range(0, n_rows, 2):
            for kc in range(n_cols):
                if kr or kc:
                    pltpu.make_async_remote_copy(
                        src_ref=w1own,
                        dst_ref=w1all.at[r // 2, par, c],
                        send_sem=wsend_sem,
                        recv_sem=wrecv_sem,
                        device_id=device(to_rs[kr], to_cs[kc]),
                        device_id_type=MESH,
                    ).start()

    def pack_and_send(t, carry):
        pl.when(t < chips - 1)(lambda: pack_rows(turn_to(t + 1)[0], *groups[0][0]))
        send_chip(0, t, False)
        pl.when(t == 0)(send_weights)
        return carry

    lax.fori_loop(0, chips, pack_and_send, 0)

    pack(1)
    send_chunk(1)
    pack(2)
    send_ahead(2)
    send_ahead(3)
    send_chunk(2)
    send_chunk(3)

    def wait_bytes(ref, sem):
        pltpu.make_async_copy(ref, ref, sem).wait()

    w1_bytes = recv.at[0 : sources // 2 - 1, 0, 0:5]
    wait_bytes(w1_bytes, wrecv_sem)
    wait_bytes(w1_bytes, wsend_sem)
    partner = device(r + 1 - 2 * par, c)
    w_swap = pltpu.make_async_remote_copy(
        src_ref=w1all.at[:, par],
        dst_ref=w1all.at[:, par],
        send_sem=wswap_send_sem,
        recv_sem=wswap_recv_sem,
        device_id=partner,
        device_id_type=MESH,
    )
    w_swap.start()

    def own_rows(chunk):
        rows, where, _ = chunks[chunk]
        src, dst = where(r)

        def copy(count, src_j, dst_j):
            for h in range(rows):
                recv[me, dst + h, pl.ds(dst_j, count)] = packed[src + h, pl.ds(src_j, count)]

        pl.when(at_edge)(lambda: copy(win_j - 1, tile_j * c - 1 + own_j, own_j))
        pl.when(jnp.logical_not(at_edge))(lambda: copy(win_j, tile_j * c - 1, 0))

    for chunk in range(3):
        own_rows(chunk)
    pl.when(jnp.logical_not(no_outer))(lambda: own_rows(3))

    zero_row = jnp.zeros((win_j, 2, 2 * images), BF16)
    zero_col = jnp.zeros((tile_h + 2, 2, 2 * images), BF16)

    def clear(s, carry):
        recv[s, last * (1 - par)] = zero_row
        return carry

    def clear_outer(s, carry):
        recv[s, (last - 1) * par] = zero_row
        recv[s, (last - 1) * par + 1] = zero_row
        return carry

    def clear_edge(s, carry):
        recv[s, pl.ds(3 * par, tile_h + 2), (win_j - 1) * (1 - own_j)] = zero_col
        return carry

    lax.fori_loop(0, sources, clear, 0)
    pl.when(no_outer)(lambda: (lax.fori_loop(0, sources, clear_outer, 0), None)[1])
    pl.when(at_edge)(lambda: (lax.fori_loop(0, sources, clear_edge, 0), None)[1])

    low = lax.broadcasted_iota(jnp.int32, (chans, 2 * chans), 1) < chans

    def spread(wt, u, v, dw):
        ur, vr = pltpu.roll(u, chans, 1), pltpu.roll(v, chans, 1)
        zero = jnp.zeros_like(u)
        tiles = (jnp.where(low, ur, zero), u, jnp.where(low, v, ur), jnp.where(low, zero, vr))
        for k, tile in enumerate(tiles):
            tile = tile.astype(BF16)
            for b in range(2):
                wt[dw + b, k * chans : (k + 1) * chans, b * 2 * chans : (b + 1) * 2 * chans] = tile

    def blank(wt):
        zero = jnp.zeros((4 * chans, 2 * chans), BF16)
        wt[3, :, 0 : 2 * chans] = zero
        wt[0, :, 2 * chans : 4 * chans] = zero

    for copy in params[1:]:
        copy.wait()
    blank(wt1)
    blank(wt2)
    for dw in range(3):
        w = [w2s[dh, dw].astype(F32) for dh in range(3)]
        spread(
            wt2,
            jnp.concatenate([w[1], w[0]], axis=1),
            jnp.concatenate([w[2], jnp.zeros_like(w[2])], axis=1),
            dw,
        )
    bias1[...] = jnp.concatenate([b1s[...]] * 4, axis=1)
    bias2[...] = jnp.concatenate([b2s[...]] * 4, axis=1)

    def arrived(chunk):
        def wait(count):
            wait_bytes(recv.at[0 : sources - 1, 0 : chunks[chunk][0], 0:count], recv_sem.at[chunk])

        pl.when(at_edge)(lambda: wait(win_j - 1))
        pl.when(jnp.logical_not(at_edge))(lambda: wait(win_j))

    arrived(0)
    give = tile_h - (tile_h - 3) * par
    land = tile_h + 2 - (tile_h + 1) * (1 - par)
    swap = pltpu.make_async_remote_copy(
        src_ref=recv.at[:, pl.ds(give, 2)],
        dst_ref=recv.at[:, pl.ds(land, 2)],
        send_sem=swap_send_sem,
        recv_sem=swap_recv_sem,
        device_id=partner,
        device_id_type=MESH,
    )
    swap.start()

    w_swap.wait()
    u = [w1all[:, :, :, k].reshape(chans, 2 * chans).astype(F32) for k in range(5)]
    for dw in range(3):
        v = (u[3], pltpu.roll(u[3], chans, 1), u[4])[dw]
        spread(wt1, u[dw], jnp.where(low, v, 0.0), dw)

    x_pairs, z_pairs = xmat.shape[0], ymat.shape[0]
    o_pairs = z_pairs - 1

    def nth(n, count):
        return (count - 1) * (1 - par) + n * (2 * par - 1)

    def turn_one(n, carry):
        i = nth(n, x_pairs)

        def put(j, value):
            xmat[i, j] = value

        turn(recv, i, put)
        return carry

    def first_one(n, carry):
        i = nth(n, z_pairs)
        fill = jnp.where(n == 0, 1 - par, 2)
        out_of = jnp.where(n == z_pairs - 1, jnp.where(r == 0, 0, jnp.where(r == n_rows - 1, 1, 2)), 2)
        blank_a = jnp.where(fill < 2, fill, out_of)
        first((xmat.at[i], xmat.at[i + 1]), lambda dw: wt1[dw], bias1[...], ymat.at[i], blank_a)
        return carry

    def second_one(n, carry):
        i = nth(n, o_pairs)
        second((ymat.at[i], ymat.at[i + 1]), lambda dw: wt2[dw], bias2[...], out.at[pl.ds(2 * i, 2)])
        return carry

    def stage(s, carry):
        @pl.when(s == 0)
        def _():
            swap.wait()

        for k in range(1, 4):
            there = s == k
            if k == 3:
                there = there & jnp.logical_not(no_outer)
            pl.when(there)(lambda k=k: arrived(k))

        for ends, one in ((TURNS, turn_one), (FIRSTS, first_one), (SECONDS, second_one)):
            lax.fori_loop(step(s, (0, *ends[:-1])), step(s, ends), one, 0)
        return carry

    lax.fori_loop(0, 4, stage, 0)

    per_edge = n_rows * 2
    for chunk in range(4):
        rows = chunks[chunk][0]
        n_r = n_rows - 2 if chunk == 3 else n_rows
        counts = (n_r * 2, n_r * (n_cols - 2))

        def drain(edge_n, inner_n, rows=rows, chunk=chunk):
            wait_bytes(recv.at[0:edge_n, 0:rows, 0 : win_j - 1], send_sem.at[chunk])
            wait_bytes(recv.at[0:inner_n, 0:rows, 0:win_j], send_sem.at[chunk])

        def drain_own(chunk=chunk, counts=counts, drain=drain):
            pl.when(at_edge)(lambda: drain(counts[0] - 1, counts[1]))
            pl.when(jnp.logical_not(at_edge))(lambda: drain(counts[0], counts[1] - 1))

        if chunk == 3:
            pl.when(no_outer)(lambda: drain(*counts))
            pl.when(jnp.logical_not(no_outer))(drain_own)
        else:
            drain_own()


def tail_kernel(tile, ymat, wt2, bias2, out_hbm, o_new, sem):
    par = lax.rem(lax.axis_index("model"), 2)
    rows = out_hbm.shape[0]
    o_pairs = ymat.shape[0] - 1
    late = (rows - 2) * par
    here = 2 * (1 - par)

    def start(k, carry):
        pltpu.make_async_copy(tile.at[par + k], out_hbm.at[k], sem.at[0]).start()
        return carry

    lax.fori_loop(here, here + rows - 2, start, 0)
    i = (o_pairs - 1) * par
    second((ymat.at[i], ymat.at[i + 1]), lambda dw: wt2[dw], bias2[...], o_new)
    last = pltpu.make_async_copy(o_new, out_hbm.at[pl.ds(late, 2)], sem.at[1])
    last.start()
    pltpu.make_async_copy(tile.at[0 : rows - 2], out_hbm.at[0 : rows - 2], sem.at[0]).wait()
    last.wait()


def solution(mesh):
    n_rows = mesh.shape["model"]
    n_cols = mesh.shape["cols"]

    def run_local(x_in, w_conv1, b_conv1, w_conv2, b_conv2):
        images, height, width, own_chans = x_in.shape
        sources = n_rows * n_cols
        chans = own_chans * sources
        pairs = width // 2
        tile_h, tile_j = height // n_rows, pairs // n_cols
        win_j = tile_j + 2
        x_pairs, z_pairs = (tile_h + 5) // 2, (tile_h + 3) // 2
        x_t = jnp.transpose(x_in, (1, 2, 3, 0)).reshape(n_rows // 2, 2 * tile_h, pairs, 2, own_chans, images)
        args = (x_t, w_conv1, b_conv1.reshape(1, chans), w_conv2, b_conv2.reshape(1, chans))
        hbm = pl.BlockSpec(memory_space=pltpu.HBM)
        vmem = pl.BlockSpec(memory_space=pltpu.VMEM)
        kept = (
            pltpu.VMEM((2 * (z_pairs - 1), tile_j, 2, images, chans), F32),
            pltpu.VMEM((z_pairs, win_j - 1, 2, images, 2 * chans), BF16),
            pltpu.VMEM((4, 4 * chans, 4 * chans), BF16),
            pltpu.VMEM((1, 4 * chans), F32),
        )
        state = pl.pallas_call(
            functools.partial(conv_kernel, n_rows, n_cols),
            out_shape=kept,
            in_specs=[hbm] * 5,
            out_specs=[vmem] * len(kept),
            scratch_shapes=[
                pltpu.VMEM((sources, 2 * x_pairs, win_j, own_chans, 2 * images), BF16),
                pltpu.VMEM((x_pairs, win_j, 2, images, 2 * chans), BF16),
                pltpu.VMEM((4, 4 * chans, 4 * chans), BF16),
                pltpu.VMEM((1, 4 * chans), F32),
                pltpu.VMEM((n_rows // 2, 2 * tile_h, pairs, 2, own_chans, images), BF16),
                pltpu.VMEM((height, pairs, own_chans, 2 * images), BF16),
                pltpu.VMEM((3, 3, own_chans, chans), BF16),
                pltpu.VMEM((5, own_chans, 2 * chans), BF16),
                pltpu.VMEM((n_rows // 2, 2, n_cols, 5, own_chans, 2 * chans), BF16),
                pltpu.VMEM((3, 3, chans, chans), BF16),
                pltpu.VMEM((1, chans), F32),
                pltpu.VMEM((1, chans), F32),
                pltpu.SemaphoreType.DMA((3, 2)),
                pltpu.SemaphoreType.DMA((4,)),
                pltpu.SemaphoreType.DMA((4,)),
                pltpu.SemaphoreType.DMA((4,)),
            ]
            + [pltpu.SemaphoreType.DMA] * 6,
            compiler_params=pltpu.CompilerParams(
                collective_id=0, has_side_effects=True, vmem_limit_bytes=24 << 20
            ),
            name="conv",
        )(*(pltpu.with_memory_space_constraint(a, pltpu.HBM) for a in args))
        out = pl.pallas_call(
            tail_kernel,
            out_shape=jax.ShapeDtypeStruct((tile_h, tile_j, 2, images, chans), F32),
            in_specs=[vmem] * len(kept),
            out_specs=pl.BlockSpec(memory_space=pl.ANY),
            scratch_shapes=[
                pltpu.VMEM((2, tile_j, 2, images, chans), F32),
                pltpu.SemaphoreType.DMA((2,)),
            ],
            compiler_params=pltpu.CompilerParams(vmem_limit_bytes=8 << 20),
            name="tail",
        )(*state)
        out = out.reshape(tile_h, 2 * tile_j, images, chans)
        return jnp.transpose(out, (2, 0, 1, 3))

    group = ("model", "cols")
    return jax.shard_map(
        run_local,
        mesh=mesh,
        in_specs=(P("data", None, None, group), P(None, None, group, None), P(), P(), P()),
        out_specs=P("data", "model", "cols", None),
        check_vma=False,
    )
```

```python
import functools

import jax
import jax.numpy as jnp
from jax import lax
from jax.experimental import pallas as pl
from jax.experimental.pallas import tpu as pltpu
from jax.sharding import PartitionSpec as P

MESH = pl.DeviceIdType.MESH
BF16 = jnp.bfloat16
F32 = jnp.float32
CHUNK_ROWS = (2, 3, 2)
TURNS, FIRSTS, SECONDS = (2, 4, 5, 6), (1, 3, 4, 5), (0, 2, 3, 3)
AHEAD = (1, 0)
COLUMN_FIRST = (2, 3)
CHIPS_ALONG = (3, 1, 2, 0)
CHIP_ORDER = tuple((other, dy) for other in (0, 1) for dy in (0, 1, -1, 2))


def turn(recv, i, put):
    sources, _, win_j, own_chans, lanes = recv.shape
    chans = sources * own_chans
    for j in range(win_j):
        top = recv[:, 2 * i, j].reshape(chans, lanes)
        under = recv[:, 2 * i + 1, j].reshape(chans, lanes)
        put(j, jnp.concatenate([top, under], axis=0).T.reshape(2, lanes // 2, 2 * chans))


def blocks(pairs, weights, count):
    acc = None
    for dw in range(4):
        parts = [view[dw // 2 : dw // 2 + count, dw % 2] for view in pairs]
        lhs = jnp.concatenate([p.reshape(count * p.shape[1], p.shape[2]) for p in parts], axis=1)
        term = jnp.dot(lhs, weights(dw), preferred_element_type=F32)
        acc = term if acc is None else acc + term
    return acc


def first(pairs, weights, bias, y_row, blank_a):
    count, _, images, lanes = y_row.shape
    c = lax.axis_index("cols")
    row = lax.rem(lax.broadcasted_iota(jnp.int32, (1, 2 * lanes), 1), lanes) // (lanes // 2)
    act = jnp.maximum(blocks(pairs, weights, count) + bias, 0.0)
    act = jnp.where(row != blank_a, act, 0.0).astype(BF16)
    for b in range(2):
        y_row[:, b] = act[:, b * lanes : (b + 1) * lanes].reshape(count, images, lanes)
    blank = jnp.zeros((images, lanes), BF16)

    @pl.when(c == 0)
    def _():
        y_row[0, 0] = blank

    @pl.when(c == lax.axis_size("cols") - 1)
    def _():
        y_row[count - 1, 1] = blank


def second(pairs, weights, bias, out_pair):
    _, count, _, images, chans = out_pair.shape
    res = blocks(pairs, weights, count) + bias
    for b in range(2):
        for a in range(2):
            at = (2 * b + a) * chans
            out_pair[a, :, b] = res[:, at : at + chans].reshape(count, images, chans)


def conv_kernel(
    n_rows,
    n_cols,
    x_hbm,
    w1_hbm,
    b1_hbm,
    w2_hbm,
    b2_hbm,
    out,
    ymat,
    wt2,
    bias2,
    recv,
    xmat,
    wt1,
    bias1,
    xs,
    packed,
    w1s,
    w1own,
    w1all,
    w2s,
    b1s,
    b2s,
    load_sem,
    par_sem,
    send_sem,
    recv_sem,
    wsend_sem,
    wrecv_sem,
    swap_send_sem,
    swap_recv_sem,
    wswap_send_sem,
    wswap_recv_sem,
):
    chip_h, pairs = xs.shape[1:3]
    images = xs.shape[-1]
    tile_h, tile_j = chip_h // 2, pairs // n_cols
    win_j = tile_j + 2
    sources = n_rows * n_cols
    r, c = lax.axis_index("model"), lax.axis_index("cols")
    par = lax.rem(r, 2)
    me = r * n_cols + c
    chans = recv.shape[0] * 2

    tops = [tile_h - sum(CHUNK_ROWS[: k + 1]) for k in range(len(CHUNK_ROWS))]
    groups = (
        ((tops[0], chip_h - tops[0]),),
        *(((k, k + n), (chip_h - k - n, chip_h - k)) for k, n in zip(tops[1:], CHUNK_ROWS[1:])),
    )
    loads = []
    for g, spans in enumerate(groups):
        loads.append(
            [
                pltpu.make_async_copy(x_hbm.at[:, lo:hi], xs.at[:, lo:hi], load_sem.at[g, n])
                for n, (lo, hi) in enumerate(spans)
            ]
        )
    for copies in loads:
        for copy in copies:
            copy.start()
    params = [
        pltpu.make_async_copy(src, dst, par_sem.at[s])
        for s, (src, dst) in enumerate(((w1_hbm, w1s), (w2_hbm, w2s), (b1_hbm, b1s), (b2_hbm, b2s)))
    ]
    for copy in params:
        copy.start()

    barrier = pltpu.get_barrier_semaphore()
    to_cs = [lax.rem(c + k, n_cols) for k in range(n_cols)]

    def device(to_r, to_c):
        return {"model": to_r, "cols": to_c}

    to_rs = [lax.rem(r + k, n_rows) for k in range(n_rows)]
    for kr, kc in sorted(
        ((kr, kc) for kr in range(n_rows) for kc in range(n_cols) if kr or kc),
        key=lambda k: (not (k[0] in (2, 3) and k[1] == 1), -(min(k[0], n_rows - k[0]) // 2 + min(k[1], n_cols - k[1]))),
    ):
        pl.semaphore_signal(barrier, inc=1, device_id=device(to_rs[kr], to_cs[kc]), device_id_type=MESH)

    def pack_rows(x, lo, hi):
        rows = hi - lo
        left, right = (xs[x, lo:hi, :, p].reshape(rows * pairs * 2, images) for p in range(2))
        both = jnp.concatenate([left, right], axis=1)
        packed[pl.ds(chip_h * x + lo, rows)] = both.reshape(rows, pairs, 2, 2 * images)

    def pack(g):
        for copy in loads[g]:
            copy.wait()

        def body(x, carry):
            for lo, hi in groups[g]:
                pack_rows(x, lo, hi)
            return carry

        lax.fori_loop(0, n_rows // 2, body, 0)

    last = tile_h + 4

    def rows_of(offset, count):
        def where(to_r):
            q = lax.rem(to_r, 2)
            src = tile_h * to_r + offset + (tile_h - count - 2 * offset) * q
            dst = offset + 2 + (last - count - 2 * offset - 3) * q
            return src, dst

        return where

    chunks = (
        *((n, rows_of(k, n), False) for k, n in zip(tops, CHUNK_ROWS)),
        (2, rows_of(-2, 2), True),
    )
    no_outer = (r == 0) | (r == n_rows - 1)
    at_edge = (c == 0) | (c == n_cols - 1)
    own_j = c == 0
    own_j = own_j.astype(jnp.int32)

    def send_tile(chunk, to_r, to_c, there):
        rows, where, is_outer = chunks[chunk]
        src, dst = where(to_r)
        skip = (to_c == 0).astype(jnp.int32)
        edge = (to_c == 0) | (to_c == n_cols - 1)
        if is_outer:
            there = there & (to_r > 0) & (to_r < n_rows - 1)

        def copy(count, src_j, dst_j):
            pltpu.make_async_remote_copy(
                src_ref=packed.at[pl.ds(src, rows), pl.ds(src_j, count)],
                dst_ref=recv.at[me, pl.ds(dst, rows), pl.ds(dst_j, count)],
                send_sem=send_sem.at[chunk],
                recv_sem=recv_sem.at[chunk],
                device_id=device(to_r, to_c),
                device_id_type=MESH,
            ).start()

        pl.when(there & edge)(lambda: copy(win_j - 1, tile_j * to_c - 1 + skip, skip))
        pl.when(there & jnp.logical_not(edge))(lambda: copy(win_j, tile_j * to_c - 1, 0))

    chips = n_rows // 2
    ahead_r, ahead_c = AHEAD

    def step(t, table):
        value = jnp.int32(table[-1])
        for k, entry in enumerate(table[:-1]):
            value = jnp.where(t == k, entry, value)
        return value

    def turn_to(t):
        dx = step(t, CHIPS_ALONG)
        return lax.rem(r // 2 + dx, chips), dx

    def send_chip(chunk, t, rest, where=None):
        x, dx = turn_to(t)
        way = 1 - 2 * lax.rem(par + t, 2)
        for other, dy in CHIP_ORDER:
            to_r = 2 * x + (1 - par if other else par)
            to_c = lax.rem(c + way * dy + n_cols, n_cols)
            there = True
            if not other and dy == 0:
                there = dx > 0
            if rest:
                there = there & jnp.logical_not((to_r == ahead_r) & (to_c == ahead_c))
            if where is not None:
                there = there & where(to_c)
            send_tile(chunk, to_r, to_c, there)

    def send_ahead(chunk):
        send_tile(chunk, jnp.int32(ahead_r), jnp.int32(ahead_c), (r != ahead_r) | (c != ahead_c))

    def send_chunk(chunk):

        def first_column(t, carry):
            x, _ = turn_to(t)
            for other in range(2):
                to_r = 2 * x + (1 - par if other else par)
                there = ((to_r != r) | (c != 0)) & (to_r != ahead_r)
                send_tile(chunk, to_r, jnp.int32(0), there)
            return carry

        where = None
        if chunk in COLUMN_FIRST:
            lax.fori_loop(0, chips, first_column, 0)
            where = lambda to_c: to_c > 0

        def body(t, carry):
            send_chip(chunk, t, True, where)
            return carry

        lax.fori_loop(0, chips, body, 0)

    params[0].wait()
    for dw in range(3):
        w1own[dw] = jnp.concatenate([w1s[1, dw], w1s[0, dw]], axis=1)
    w1own[3] = jnp.concatenate([w1s[2, 0], w1s[2, 1]], axis=1)
    w1own[4] = jnp.concatenate([w1s[2, 2], jnp.zeros_like(w1s[2, 2])], axis=1)
    w1all[r // 2, par, c] = w1own[...]

    for copy in loads[0]:
        copy.wait()
    pack_rows(turn_to(0)[0], *groups[0][0])
    pl.semaphore_wait(barrier, sources - 1)

    def send_weights():
        for kr in range(0, n_rows, 2):
            for kc in range(n_cols):
                if kr or kc:
                    pltpu.make_async_remote_copy(
                        src_ref=w1own,
                        dst_ref=w1all.at[r // 2, par, c],
                        send_sem=wsend_sem,
                        recv_sem=wrecv_sem,
                        device_id=device(to_rs[kr], to_cs[kc]),
                        device_id_type=MESH,
                    ).start()

    def pack_and_send(t, carry):
        pl.when(t < chips - 1)(lambda: pack_rows(turn_to(t + 1)[0], *groups[0][0]))
        send_chip(0, t, False)
        pl.when(t == 0)(send_weights)
        return carry

    lax.fori_loop(0, chips, pack_and_send, 0)

    pack(1)
    send_ahead(1)
    send_chunk(1)
    pack(2)
    send_ahead(2)
    send_ahead(3)
    send_chunk(2)
    send_chunk(3)

    def wait_bytes(ref, sem):
        pltpu.make_async_copy(ref, ref, sem).wait()

    w1_bytes = recv.at[0 : sources // 2 - 1, 0, 0:5]
    wait_bytes(w1_bytes, wrecv_sem)
    wait_bytes(w1_bytes, wsend_sem)
    partner = device(r + 1 - 2 * par, c)
    w_swap = pltpu.make_async_remote_copy(
        src_ref=w1all.at[:, par],
        dst_ref=w1all.at[:, par],
        send_sem=wswap_send_sem,
        recv_sem=wswap_recv_sem,
        device_id=partner,
        device_id_type=MESH,
    )
    w_swap.start()

    def own_rows(chunk):
        rows, where, _ = chunks[chunk]
        src, dst = where(r)

        def copy(count, src_j, dst_j):
            for h in range(rows):
                recv[me, dst + h, pl.ds(dst_j, count)] = packed[src + h, pl.ds(src_j, count)]

        pl.when(at_edge)(lambda: copy(win_j - 1, tile_j * c - 1 + own_j, own_j))
        pl.when(jnp.logical_not(at_edge))(lambda: copy(win_j, tile_j * c - 1, 0))

    for chunk in range(3):
        own_rows(chunk)
    pl.when(jnp.logical_not(no_outer))(lambda: own_rows(3))

    zero_row = jnp.zeros((win_j, 2, 2 * images), BF16)
    zero_col = jnp.zeros((tile_h + 2, 2, 2 * images), BF16)

    def clear(s, carry):
        recv[s, last * (1 - par)] = zero_row
        return carry

    def clear_outer(s, carry):
        recv[s, (last - 1) * par] = zero_row
        recv[s, (last - 1) * par + 1] = zero_row
        return carry

    def clear_edge(s, carry):
        recv[s, pl.ds(3 * par, tile_h + 2), (win_j - 1) * (1 - own_j)] = zero_col
        return carry

    lax.fori_loop(0, sources, clear, 0)
    pl.when(no_outer)(lambda: (lax.fori_loop(0, sources, clear_outer, 0), None)[1])
    pl.when(at_edge)(lambda: (lax.fori_loop(0, sources, clear_edge, 0), None)[1])

    low = lax.broadcasted_iota(jnp.int32, (chans, 2 * chans), 1) < chans

    def spread(wt, u, v, dw):
        ur, vr = pltpu.roll(u, chans, 1), pltpu.roll(v, chans, 1)
        zero = jnp.zeros_like(u)
        tiles = (jnp.where(low, ur, zero), u, jnp.where(low, v, ur), jnp.where(low, zero, vr))
        for k, tile in enumerate(tiles):
            tile = tile.astype(BF16)
            for b in range(2):
                wt[dw + b, k * chans : (k + 1) * chans, b * 2 * chans : (b + 1) * 2 * chans] = tile

    def blank(wt):
        zero = jnp.zeros((4 * chans, 2 * chans), BF16)
        wt[3, :, 0 : 2 * chans] = zero
        wt[0, :, 2 * chans : 4 * chans] = zero

    for copy in params[1:]:
        copy.wait()
    blank(wt1)
    blank(wt2)
    for dw in range(3):
        w = [w2s[dh, dw].astype(F32) for dh in range(3)]
        spread(
            wt2,
            jnp.concatenate([w[1], w[0]], axis=1),
            jnp.concatenate([w[2], jnp.zeros_like(w[2])], axis=1),
            dw,
        )
    bias1[...] = jnp.concatenate([b1s[...]] * 4, axis=1)
    bias2[...] = jnp.concatenate([b2s[...]] * 4, axis=1)

    def arrived(chunk):
        def wait(count):
            wait_bytes(recv.at[0 : sources - 1, 0 : chunks[chunk][0], 0:count], recv_sem.at[chunk])

        pl.when(at_edge)(lambda: wait(win_j - 1))
        pl.when(jnp.logical_not(at_edge))(lambda: wait(win_j))

    arrived(0)
    give = tile_h - (tile_h - 3) * par
    land = tile_h + 2 - (tile_h + 1) * (1 - par)
    swap = pltpu.make_async_remote_copy(
        src_ref=recv.at[:, pl.ds(give, 2)],
        dst_ref=recv.at[:, pl.ds(land, 2)],
        send_sem=swap_send_sem,
        recv_sem=swap_recv_sem,
        device_id=partner,
        device_id_type=MESH,
    )
    swap.start()

    w_swap.wait()
    u = [w1all[:, :, :, k].reshape(chans, 2 * chans).astype(F32) for k in range(5)]
    for dw in range(3):
        v = (u[3], pltpu.roll(u[3], chans, 1), u[4])[dw]
        spread(wt1, u[dw], jnp.where(low, v, 0.0), dw)

    x_pairs, z_pairs = xmat.shape[0], ymat.shape[0]
    o_pairs = z_pairs - 1

    def nth(n, count):
        return (count - 1) * (1 - par) + n * (2 * par - 1)

    def turn_one(n, carry):
        i = nth(n, x_pairs)

        def put(j, value):
            xmat[i, j] = value

        turn(recv, i, put)
        return carry

    def first_one(n, carry):
        i = nth(n, z_pairs)
        fill = jnp.where(n == 0, 1 - par, 2)
        out_of = jnp.where(n == z_pairs - 1, jnp.where(r == 0, 0, jnp.where(r == n_rows - 1, 1, 2)), 2)
        blank_a = jnp.where(fill < 2, fill, out_of)
        first((xmat.at[i], xmat.at[i + 1]), lambda dw: wt1[dw], bias1[...], ymat.at[i], blank_a)
        return carry

    def second_one(n, carry):
        i = nth(n, o_pairs)
        second((ymat.at[i], ymat.at[i + 1]), lambda dw: wt2[dw], bias2[...], out.at[pl.ds(2 * i, 2)])
        return carry

    def stage(s, carry):
        @pl.when(s == 0)
        def _():
            swap.wait()

        for k in range(1, 4):
            there = s == k
            if k == 3:
                there = there & jnp.logical_not(no_outer)
            pl.when(there)(lambda k=k: arrived(k))

        for ends, one in ((TURNS, turn_one), (FIRSTS, first_one), (SECONDS, second_one)):
            lax.fori_loop(step(s, (0, *ends[:-1])), step(s, ends), one, 0)
        return carry

    lax.fori_loop(0, 4, stage, 0)

    per_edge = n_rows * 2
    for chunk in range(4):
        rows = chunks[chunk][0]
        n_r = n_rows - 2 if chunk == 3 else n_rows
        counts = (n_r * 2, n_r * (n_cols - 2))

        def drain(edge_n, inner_n, rows=rows, chunk=chunk):
            wait_bytes(recv.at[0:edge_n, 0:rows, 0 : win_j - 1], send_sem.at[chunk])
            wait_bytes(recv.at[0:inner_n, 0:rows, 0:win_j], send_sem.at[chunk])

        def drain_own(chunk=chunk, counts=counts, drain=drain):
            pl.when(at_edge)(lambda: drain(counts[0] - 1, counts[1]))
            pl.when(jnp.logical_not(at_edge))(lambda: drain(counts[0], counts[1] - 1))

        if chunk == 3:
            pl.when(no_outer)(lambda: drain(*counts))
            pl.when(jnp.logical_not(no_outer))(drain_own)
        else:
            drain_own()


def tail_kernel(tile, ymat, wt2, bias2, out_hbm, o_new, sem):
    par = lax.rem(lax.axis_index("model"), 2)
    rows = out_hbm.shape[0]
    o_pairs = ymat.shape[0] - 1
    late = (rows - 2) * par
    here = 2 * (1 - par)

    def start(k, carry):
        pltpu.make_async_copy(tile.at[par + k], out_hbm.at[k], sem.at[0]).start()
        return carry

    lax.fori_loop(here, here + rows - 2, start, 0)
    i = (o_pairs - 1) * par
    second((ymat.at[i], ymat.at[i + 1]), lambda dw: wt2[dw], bias2[...], o_new)
    last = pltpu.make_async_copy(o_new, out_hbm.at[pl.ds(late, 2)], sem.at[1])
    last.start()
    pltpu.make_async_copy(tile.at[0 : rows - 2], out_hbm.at[0 : rows - 2], sem.at[0]).wait()
    last.wait()


def solution(mesh):
    n_rows = mesh.shape["model"]
    n_cols = mesh.shape["cols"]

    def run_local(x_in, w_conv1, b_conv1, w_conv2, b_conv2):
        images, height, width, own_chans = x_in.shape
        sources = n_rows * n_cols
        chans = own_chans * sources
        pairs = width // 2
        tile_h, tile_j = height // n_rows, pairs // n_cols
        win_j = tile_j + 2
        x_pairs, z_pairs = (tile_h + 5) // 2, (tile_h + 3) // 2
        x_t = jnp.transpose(x_in, (1, 2, 3, 0)).reshape(n_rows // 2, 2 * tile_h, pairs, 2, own_chans, images)
        args = (x_t, w_conv1, b_conv1.reshape(1, chans), w_conv2, b_conv2.reshape(1, chans))
        hbm = pl.BlockSpec(memory_space=pltpu.HBM)
        vmem = pl.BlockSpec(memory_space=pltpu.VMEM)
        kept = (
            pltpu.VMEM((2 * (z_pairs - 1), tile_j, 2, images, chans), F32),
            pltpu.VMEM((z_pairs, win_j - 1, 2, images, 2 * chans), BF16),
            pltpu.VMEM((4, 4 * chans, 4 * chans), BF16),
            pltpu.VMEM((1, 4 * chans), F32),
        )
        state = pl.pallas_call(
            functools.partial(conv_kernel, n_rows, n_cols),
            out_shape=kept,
            in_specs=[hbm] * 5,
            out_specs=[vmem] * len(kept),
            scratch_shapes=[
                pltpu.VMEM((sources, 2 * x_pairs, win_j, own_chans, 2 * images), BF16),
                pltpu.VMEM((x_pairs, win_j, 2, images, 2 * chans), BF16),
                pltpu.VMEM((4, 4 * chans, 4 * chans), BF16),
                pltpu.VMEM((1, 4 * chans), F32),
                pltpu.VMEM((n_rows // 2, 2 * tile_h, pairs, 2, own_chans, images), BF16),
                pltpu.VMEM((height, pairs, own_chans, 2 * images), BF16),
                pltpu.VMEM((3, 3, own_chans, chans), BF16),
                pltpu.VMEM((5, own_chans, 2 * chans), BF16),
                pltpu.VMEM((n_rows // 2, 2, n_cols, 5, own_chans, 2 * chans), BF16),
                pltpu.VMEM((3, 3, chans, chans), BF16),
                pltpu.VMEM((1, chans), F32),
                pltpu.VMEM((1, chans), F32),
                pltpu.SemaphoreType.DMA((3, 2)),
                pltpu.SemaphoreType.DMA((4,)),
                pltpu.SemaphoreType.DMA((4,)),
                pltpu.SemaphoreType.DMA((4,)),
            ]
            + [pltpu.SemaphoreType.DMA] * 6,
            compiler_params=pltpu.CompilerParams(
                collective_id=0, has_side_effects=True, vmem_limit_bytes=24 << 20
            ),
            name="conv",
        )(*(pltpu.with_memory_space_constraint(a, pltpu.HBM) for a in args))
        out = pl.pallas_call(
            tail_kernel,
            out_shape=jax.ShapeDtypeStruct((tile_h, tile_j, 2, images, chans), F32),
            in_specs=[vmem] * len(kept),
            out_specs=pl.BlockSpec(memory_space=pl.ANY),
            scratch_shapes=[
                pltpu.VMEM((2, tile_j, 2, images, chans), F32),
                pltpu.SemaphoreType.DMA((2,)),
            ],
            compiler_params=pltpu.CompilerParams(vmem_limit_bytes=8 << 20),
            name="tail",
        )(*state)
        out = out.reshape(tile_h, 2 * tile_j, images, chans)
        return jnp.transpose(out, (2, 0, 1, 3))

    group = ("model", "cols")
    return jax.shard_map(
        run_local,
        mesh=mesh,
        in_specs=(P("data", None, None, group), P(None, None, group, None), P(), P(), P()),
        out_specs=P("data", "model", "cols", None),
        check_vma=False,
    )
```

```python
import functools

import jax
import jax.numpy as jnp
from jax import lax
from jax.experimental import pallas as pl
from jax.experimental.pallas import tpu as pltpu
from jax.sharding import PartitionSpec as P

MESH = pl.DeviceIdType.MESH
BF16 = jnp.bfloat16
F32 = jnp.float32
CHUNK_ROWS = (2, 3, 2)
TURNS, FIRSTS, SECONDS = (2, 4, 5, 6), (1, 3, 4, 5), (0, 2, 3, 3)
AHEAD = (1, 0)
COLUMN_FIRST = (2, 3)
CHIPS_ALONG = (3, 1, 2, 0)
CHIP_ORDER = tuple((other, dy) for other in (0, 1) for dy in (-1, 1, 0, 2))


def turn(recv, i, put):
    sources, _, win_j, own_chans, lanes = recv.shape
    chans = sources * own_chans
    for j in range(win_j):
        top = recv[:, 2 * i, j].reshape(chans, lanes)
        under = recv[:, 2 * i + 1, j].reshape(chans, lanes)
        put(j, jnp.concatenate([top, under], axis=0).T.reshape(2, lanes // 2, 2 * chans))


def blocks(pairs, weights, count):
    acc = None
    for dw in range(4):
        parts = [view[dw // 2 : dw // 2 + count, dw % 2] for view in pairs]
        lhs = jnp.concatenate([p.reshape(count * p.shape[1], p.shape[2]) for p in parts], axis=1)
        term = jnp.dot(lhs, weights(dw), preferred_element_type=F32)
        acc = term if acc is None else acc + term
    return acc


def first(pairs, weights, bias, y_row, blank_a):
    count, _, images, lanes = y_row.shape
    c = lax.axis_index("cols")
    row = lax.rem(lax.broadcasted_iota(jnp.int32, (1, 2 * lanes), 1), lanes) // (lanes // 2)
    act = jnp.maximum(blocks(pairs, weights, count) + bias, 0.0)
    act = jnp.where(row != blank_a, act, 0.0).astype(BF16)
    for b in range(2):
        y_row[:, b] = act[:, b * lanes : (b + 1) * lanes].reshape(count, images, lanes)
    blank = jnp.zeros((images, lanes), BF16)

    @pl.when(c == 0)
    def _():
        y_row[0, 0] = blank

    @pl.when(c == lax.axis_size("cols") - 1)
    def _():
        y_row[count - 1, 1] = blank


def second(pairs, weights, bias, out_pair):
    _, count, _, images, chans = out_pair.shape
    res = blocks(pairs, weights, count) + bias
    for b in range(2):
        for a in range(2):
            at = (2 * b + a) * chans
            out_pair[a, :, b] = res[:, at : at + chans].reshape(count, images, chans)


def conv_kernel(
    n_rows,
    n_cols,
    x_hbm,
    w1_hbm,
    b1_hbm,
    w2_hbm,
    b2_hbm,
    out,
    ymat,
    wt2,
    bias2,
    recv,
    xmat,
    wt1,
    bias1,
    xs,
    packed,
    w1s,
    w1own,
    w1all,
    w2s,
    b1s,
    b2s,
    load_sem,
    par_sem,
    send_sem,
    recv_sem,
    wsend_sem,
    wrecv_sem,
    swap_send_sem,
    swap_recv_sem,
    wswap_send_sem,
    wswap_recv_sem,
):
    chip_h, pairs = xs.shape[1:3]
    images = xs.shape[-1]
    tile_h, tile_j = chip_h // 2, pairs // n_cols
    win_j = tile_j + 2
    sources = n_rows * n_cols
    r, c = lax.axis_index("model"), lax.axis_index("cols")
    par = lax.rem(r, 2)
    me = r * n_cols + c
    chans = recv.shape[0] * 2

    tops = [tile_h - sum(CHUNK_ROWS[: k + 1]) for k in range(len(CHUNK_ROWS))]
    groups = (
        ((tops[0], chip_h - tops[0]),),
        *(((k, k + n), (chip_h - k - n, chip_h - k)) for k, n in zip(tops[1:], CHUNK_ROWS[1:])),
    )
    loads = []
    for g, spans in enumerate(groups):
        loads.append(
            [
                pltpu.make_async_copy(x_hbm.at[:, lo:hi], xs.at[:, lo:hi], load_sem.at[g, n])
                for n, (lo, hi) in enumerate(spans)
            ]
        )
    for copies in loads:
        for copy in copies:
            copy.start()
    params = [
        pltpu.make_async_copy(src, dst, par_sem.at[s])
        for s, (src, dst) in enumerate(((w1_hbm, w1s), (w2_hbm, w2s), (b1_hbm, b1s), (b2_hbm, b2s)))
    ]
    for copy in params:
        copy.start()

    barrier = pltpu.get_barrier_semaphore()
    to_cs = [lax.rem(c + k, n_cols) for k in range(n_cols)]

    def device(to_r, to_c):
        return {"model": to_r, "cols": to_c}

    to_rs = [lax.rem(r + k, n_rows) for k in range(n_rows)]
    for kr, kc in sorted(
        ((kr, kc) for kr in range(n_rows) for kc in range(n_cols) if kr or kc),
        key=lambda k: (not (k[0] in (2, 3) and k[1] == 1), -(min(k[0], n_rows - k[0]) // 2 + min(k[1], n_cols - k[1]))),
    ):
        pl.semaphore_signal(barrier, inc=1, device_id=device(to_rs[kr], to_cs[kc]), device_id_type=MESH)

    def pack_rows(x, lo, hi):
        rows = hi - lo
        left, right = (xs[x, lo:hi, :, p].reshape(rows * pairs * 2, images) for p in range(2))
        both = jnp.concatenate([left, right], axis=1)
        packed[pl.ds(chip_h * x + lo, rows)] = both.reshape(rows, pairs, 2, 2 * images)

    def pack(g):
        for copy in loads[g]:
            copy.wait()

        def body(x, carry):
            for lo, hi in groups[g]:
                pack_rows(x, lo, hi)
            return carry

        lax.fori_loop(0, n_rows // 2, body, 0)

    last = tile_h + 4

    def rows_of(offset, count):
        def where(to_r):
            q = lax.rem(to_r, 2)
            src = tile_h * to_r + offset + (tile_h - count - 2 * offset) * q
            dst = offset + 2 + (last - count - 2 * offset - 3) * q
            return src, dst

        return where

    chunks = (
        *((n, rows_of(k, n), False) for k, n in zip(tops, CHUNK_ROWS)),
        (2, rows_of(-2, 2), True),
    )
    no_outer = (r == 0) | (r == n_rows - 1)
    at_edge = (c == 0) | (c == n_cols - 1)
    own_j = c == 0
    own_j = own_j.astype(jnp.int32)

    def send_tile(chunk, to_r, to_c, there):
        rows, where, is_outer = chunks[chunk]
        src, dst = where(to_r)
        skip = (to_c == 0).astype(jnp.int32)
        edge = (to_c == 0) | (to_c == n_cols - 1)
        if is_outer:
            there = there & (to_r > 0) & (to_r < n_rows - 1)

        def copy(count, src_j, dst_j):
            pltpu.make_async_remote_copy(
                src_ref=packed.at[pl.ds(src, rows), pl.ds(src_j, count)],
                dst_ref=recv.at[me, pl.ds(dst, rows), pl.ds(dst_j, count)],
                send_sem=send_sem.at[chunk],
                recv_sem=recv_sem.at[chunk],
                device_id=device(to_r, to_c),
                device_id_type=MESH,
            ).start()

        pl.when(there & edge)(lambda: copy(win_j - 1, tile_j * to_c - 1 + skip, skip))
        pl.when(there & jnp.logical_not(edge))(lambda: copy(win_j, tile_j * to_c - 1, 0))

    chips = n_rows // 2
    ahead_r, ahead_c = AHEAD

    def step(t, table):
        value = jnp.int32(table[-1])
        for k, entry in enumerate(table[:-1]):
            value = jnp.where(t == k, entry, value)
        return value

    def turn_to(t):
        dx = step(t, CHIPS_ALONG)
        return lax.rem(r // 2 + dx, chips), dx

    def send_chip(chunk, t, rest, where=None):
        x, dx = turn_to(t)
        way = 1 - 2 * lax.rem(par + t, 2)
        for other, dy in CHIP_ORDER:
            to_r = 2 * x + (1 - par if other else par)
            to_c = lax.rem(c + way * dy + n_cols, n_cols)
            there = True
            if not other and dy == 0:
                there = dx > 0
            if rest:
                there = there & jnp.logical_not((to_r == ahead_r) & (to_c == ahead_c))
            if where is not None:
                there = there & where(to_c)
            send_tile(chunk, to_r, to_c, there)

    def send_ahead(chunk):
        send_tile(chunk, jnp.int32(ahead_r), jnp.int32(ahead_c), (r != ahead_r) | (c != ahead_c))

    def send_chunk(chunk):

        def first_column(t, carry):
            x, _ = turn_to(t)
            for other in range(2):
                to_r = 2 * x + (1 - par if other else par)
                there = ((to_r != r) | (c != 0)) & (to_r != ahead_r)
                send_tile(chunk, to_r, jnp.int32(0), there)
            return carry

        where = None
        if chunk in COLUMN_FIRST:
            lax.fori_loop(0, chips, first_column, 0)
            where = lambda to_c: to_c > 0

        def body(t, carry):
            send_chip(chunk, t, True, where)
            return carry

        lax.fori_loop(0, chips, body, 0)

    params[0].wait()
    for dw in range(3):
        w1own[dw] = jnp.concatenate([w1s[1, dw], w1s[0, dw]], axis=1)
    w1own[3] = jnp.concatenate([w1s[2, 0], w1s[2, 1]], axis=1)
    w1own[4] = jnp.concatenate([w1s[2, 2], jnp.zeros_like(w1s[2, 2])], axis=1)
    w1all[r // 2, par, c] = w1own[...]

    for copy in loads[0]:
        copy.wait()
    pack_rows(turn_to(0)[0], *groups[0][0])
    pl.semaphore_wait(barrier, sources - 1)

    def send_weights():
        for kr in range(0, n_rows, 2):
            for kc in range(n_cols):
                if kr or kc:
                    pltpu.make_async_remote_copy(
                        src_ref=w1own,
                        dst_ref=w1all.at[r // 2, par, c],
                        send_sem=wsend_sem,
                        recv_sem=wrecv_sem,
                        device_id=device(to_rs[kr], to_cs[kc]),
                        device_id_type=MESH,
                    ).start()

    def pack_and_send(t, carry):
        pl.when(t < chips - 1)(lambda: pack_rows(turn_to(t + 1)[0], *groups[0][0]))
        send_chip(0, t, False)
        pl.when(t == 0)(send_weights)
        return carry

    lax.fori_loop(0, chips, pack_and_send, 0)

    pack(1)
    send_ahead(1)
    send_chunk(1)
    pack(2)
    send_ahead(2)
    send_ahead(3)
    send_chunk(2)
    send_chunk(3)

    def wait_bytes(ref, sem):
        pltpu.make_async_copy(ref, ref, sem).wait()

    w1_bytes = recv.at[0 : sources // 2 - 1, 0, 0:5]
    wait_bytes(w1_bytes, wrecv_sem)
    wait_bytes(w1_bytes, wsend_sem)
    partner = device(r + 1 - 2 * par, c)
    w_swap = pltpu.make_async_remote_copy(
        src_ref=w1all.at[:, par],
        dst_ref=w1all.at[:, par],
        send_sem=wswap_send_sem,
        recv_sem=wswap_recv_sem,
        device_id=partner,
        device_id_type=MESH,
    )
    w_swap.start()

    def own_rows(chunk):
        rows, where, _ = chunks[chunk]
        src, dst = where(r)

        def copy(count, src_j, dst_j):
            for h in range(rows):
                recv[me, dst + h, pl.ds(dst_j, count)] = packed[src + h, pl.ds(src_j, count)]

        pl.when(at_edge)(lambda: copy(win_j - 1, tile_j * c - 1 + own_j, own_j))
        pl.when(jnp.logical_not(at_edge))(lambda: copy(win_j, tile_j * c - 1, 0))

    for chunk in range(3):
        own_rows(chunk)
    pl.when(jnp.logical_not(no_outer))(lambda: own_rows(3))

    zero_row = jnp.zeros((win_j, 2, 2 * images), BF16)
    zero_col = jnp.zeros((tile_h + 2, 2, 2 * images), BF16)

    def clear(s, carry):
        recv[s, last * (1 - par)] = zero_row
        return carry

    def clear_outer(s, carry):
        recv[s, (last - 1) * par] = zero_row
        recv[s, (last - 1) * par + 1] = zero_row
        return carry

    def clear_edge(s, carry):
        recv[s, pl.ds(3 * par, tile_h + 2), (win_j - 1) * (1 - own_j)] = zero_col
        return carry

    lax.fori_loop(0, sources, clear, 0)
    pl.when(no_outer)(lambda: (lax.fori_loop(0, sources, clear_outer, 0), None)[1])
    pl.when(at_edge)(lambda: (lax.fori_loop(0, sources, clear_edge, 0), None)[1])

    low = lax.broadcasted_iota(jnp.int32, (chans, 2 * chans), 1) < chans

    def spread(wt, u, v, dw):
        ur, vr = pltpu.roll(u, chans, 1), pltpu.roll(v, chans, 1)
        zero = jnp.zeros_like(u)
        tiles = (jnp.where(low, ur, zero), u, jnp.where(low, v, ur), jnp.where(low, zero, vr))
        for k, tile in enumerate(tiles):
            tile = tile.astype(BF16)
            for b in range(2):
                wt[dw + b, k * chans : (k + 1) * chans, b * 2 * chans : (b + 1) * 2 * chans] = tile

    def blank(wt):
        zero = jnp.zeros((4 * chans, 2 * chans), BF16)
        wt[3, :, 0 : 2 * chans] = zero
        wt[0, :, 2 * chans : 4 * chans] = zero

    for copy in params[1:]:
        copy.wait()
    blank(wt1)
    blank(wt2)
    for dw in range(3):
        w = [w2s[dh, dw].astype(F32) for dh in range(3)]
        spread(
            wt2,
            jnp.concatenate([w[1], w[0]], axis=1),
            jnp.concatenate([w[2], jnp.zeros_like(w[2])], axis=1),
            dw,
        )
    bias1[...] = jnp.concatenate([b1s[...]] * 4, axis=1)
    bias2[...] = jnp.concatenate([b2s[...]] * 4, axis=1)

    def arrived(chunk):
        def wait(count):
            wait_bytes(recv.at[0 : sources - 1, 0 : chunks[chunk][0], 0:count], recv_sem.at[chunk])

        pl.when(at_edge)(lambda: wait(win_j - 1))
        pl.when(jnp.logical_not(at_edge))(lambda: wait(win_j))

    arrived(0)
    give = tile_h - (tile_h - 3) * par
    land = tile_h + 2 - (tile_h + 1) * (1 - par)
    swap = pltpu.make_async_remote_copy(
        src_ref=recv.at[:, pl.ds(give, 2)],
        dst_ref=recv.at[:, pl.ds(land, 2)],
        send_sem=swap_send_sem,
        recv_sem=swap_recv_sem,
        device_id=partner,
        device_id_type=MESH,
    )
    swap.start()

    w_swap.wait()
    u = [w1all[:, :, :, k].reshape(chans, 2 * chans).astype(F32) for k in range(5)]
    for dw in range(3):
        v = (u[3], pltpu.roll(u[3], chans, 1), u[4])[dw]
        spread(wt1, u[dw], jnp.where(low, v, 0.0), dw)

    x_pairs, z_pairs = xmat.shape[0], ymat.shape[0]
    o_pairs = z_pairs - 1

    def nth(n, count):
        return (count - 1) * (1 - par) + n * (2 * par - 1)

    def turn_one(n, carry):
        i = nth(n, x_pairs)

        def put(j, value):
            xmat[i, j] = value

        turn(recv, i, put)
        return carry

    def first_one(n, carry):
        i = nth(n, z_pairs)
        fill = jnp.where(n == 0, 1 - par, 2)
        out_of = jnp.where(n == z_pairs - 1, jnp.where(r == 0, 0, jnp.where(r == n_rows - 1, 1, 2)), 2)
        blank_a = jnp.where(fill < 2, fill, out_of)
        first((xmat.at[i], xmat.at[i + 1]), lambda dw: wt1[dw], bias1[...], ymat.at[i], blank_a)
        return carry

    def second_one(n, carry):
        i = nth(n, o_pairs)
        second((ymat.at[i], ymat.at[i + 1]), lambda dw: wt2[dw], bias2[...], out.at[pl.ds(2 * i, 2)])
        return carry

    def stage(s, carry):
        @pl.when(s == 0)
        def _():
            swap.wait()

        for k in range(1, 4):
            there = s == k
            if k == 3:
                there = there & jnp.logical_not(no_outer)
            pl.when(there)(lambda k=k: arrived(k))

        for ends, one in ((TURNS, turn_one), (FIRSTS, first_one), (SECONDS, second_one)):
            lax.fori_loop(step(s, (0, *ends[:-1])), step(s, ends), one, 0)
        return carry

    lax.fori_loop(0, 4, stage, 0)

    per_edge = n_rows * 2
    for chunk in range(4):
        rows = chunks[chunk][0]
        n_r = n_rows - 2 if chunk == 3 else n_rows
        counts = (n_r * 2, n_r * (n_cols - 2))

        def drain(edge_n, inner_n, rows=rows, chunk=chunk):
            wait_bytes(recv.at[0:edge_n, 0:rows, 0 : win_j - 1], send_sem.at[chunk])
            wait_bytes(recv.at[0:inner_n, 0:rows, 0:win_j], send_sem.at[chunk])

        def drain_own(chunk=chunk, counts=counts, drain=drain):
            pl.when(at_edge)(lambda: drain(counts[0] - 1, counts[1]))
            pl.when(jnp.logical_not(at_edge))(lambda: drain(counts[0], counts[1] - 1))

        if chunk == 3:
            pl.when(no_outer)(lambda: drain(*counts))
            pl.when(jnp.logical_not(no_outer))(drain_own)
        else:
            drain_own()


def tail_kernel(tile, ymat, wt2, bias2, out_hbm, o_new, sem):
    par = lax.rem(lax.axis_index("model"), 2)
    rows = out_hbm.shape[0]
    o_pairs = ymat.shape[0] - 1
    late = (rows - 2) * par
    here = 2 * (1 - par)

    def start(k, carry):
        pltpu.make_async_copy(tile.at[par + k], out_hbm.at[k], sem.at[0]).start()
        return carry

    lax.fori_loop(here, here + rows - 2, start, 0)
    i = (o_pairs - 1) * par
    second((ymat.at[i], ymat.at[i + 1]), lambda dw: wt2[dw], bias2[...], o_new)
    last = pltpu.make_async_copy(o_new, out_hbm.at[pl.ds(late, 2)], sem.at[1])
    last.start()
    pltpu.make_async_copy(tile.at[0 : rows - 2], out_hbm.at[0 : rows - 2], sem.at[0]).wait()
    last.wait()


def solution(mesh):
    n_rows = mesh.shape["model"]
    n_cols = mesh.shape["cols"]

    def run_local(x_in, w_conv1, b_conv1, w_conv2, b_conv2):
        images, height, width, own_chans = x_in.shape
        sources = n_rows * n_cols
        chans = own_chans * sources
        pairs = width // 2
        tile_h, tile_j = height // n_rows, pairs // n_cols
        win_j = tile_j + 2
        x_pairs, z_pairs = (tile_h + 5) // 2, (tile_h + 3) // 2
        x_t = jnp.transpose(x_in, (1, 2, 3, 0)).reshape(n_rows // 2, 2 * tile_h, pairs, 2, own_chans, images)
        args = (x_t, w_conv1, b_conv1.reshape(1, chans), w_conv2, b_conv2.reshape(1, chans))
        hbm = pl.BlockSpec(memory_space=pltpu.HBM)
        vmem = pl.BlockSpec(memory_space=pltpu.VMEM)
        kept = (
            pltpu.VMEM((2 * (z_pairs - 1), tile_j, 2, images, chans), F32),
            pltpu.VMEM((z_pairs, win_j - 1, 2, images, 2 * chans), BF16),
            pltpu.VMEM((4, 4 * chans, 4 * chans), BF16),
            pltpu.VMEM((1, 4 * chans), F32),
        )
        state = pl.pallas_call(
            functools.partial(conv_kernel, n_rows, n_cols),
            out_shape=kept,
            in_specs=[hbm] * 5,
            out_specs=[vmem] * len(kept),
            scratch_shapes=[
                pltpu.VMEM((sources, 2 * x_pairs, win_j, own_chans, 2 * images), BF16),
                pltpu.VMEM((x_pairs, win_j, 2, images, 2 * chans), BF16),
                pltpu.VMEM((4, 4 * chans, 4 * chans), BF16),
                pltpu.VMEM((1, 4 * chans), F32),
                pltpu.VMEM((n_rows // 2, 2 * tile_h, pairs, 2, own_chans, images), BF16),
                pltpu.VMEM((height, pairs, own_chans, 2 * images), BF16),
                pltpu.VMEM((3, 3, own_chans, chans), BF16),
                pltpu.VMEM((5, own_chans, 2 * chans), BF16),
                pltpu.VMEM((n_rows // 2, 2, n_cols, 5, own_chans, 2 * chans), BF16),
                pltpu.VMEM((3, 3, chans, chans), BF16),
                pltpu.VMEM((1, chans), F32),
                pltpu.VMEM((1, chans), F32),
                pltpu.SemaphoreType.DMA((3, 2)),
                pltpu.SemaphoreType.DMA((4,)),
                pltpu.SemaphoreType.DMA((4,)),
                pltpu.SemaphoreType.DMA((4,)),
            ]
            + [pltpu.SemaphoreType.DMA] * 6,
            compiler_params=pltpu.CompilerParams(
                collective_id=0, has_side_effects=True, vmem_limit_bytes=24 << 20
            ),
            name="conv",
        )(*(pltpu.with_memory_space_constraint(a, pltpu.HBM) for a in args))
        out = pl.pallas_call(
            tail_kernel,
            out_shape=jax.ShapeDtypeStruct((tile_h, tile_j, 2, images, chans), F32),
            in_specs=[vmem] * len(kept),
            out_specs=pl.BlockSpec(memory_space=pl.ANY),
            scratch_shapes=[
                pltpu.VMEM((2, tile_j, 2, images, chans), F32),
                pltpu.SemaphoreType.DMA((2,)),
            ],
            compiler_params=pltpu.CompilerParams(vmem_limit_bytes=8 << 20),
            name="tail",
        )(*state)
        out = out.reshape(tile_h, 2 * tile_j, images, chans)
        return jnp.transpose(out, (2, 0, 1, 3))

    group = ("model", "cols")
    return jax.shard_map(
        run_local,
        mesh=mesh,
        in_specs=(P("data", None, None, group), P(None, None, group, None), P(), P(), P()),
        out_specs=P("data", "model", "cols", None),
        check_vma=False,
    )
```

```python
import functools

import jax
import jax.numpy as jnp
from jax import lax
from jax.experimental import pallas as pl
from jax.experimental.pallas import tpu as pltpu
from jax.sharding import PartitionSpec as P

MESH = pl.DeviceIdType.MESH
BF16 = jnp.bfloat16
F32 = jnp.float32
CHUNK_ROWS = (2, 3, 2)
TURNS, FIRSTS, SECONDS = (2, 4, 5, 6), (1, 3, 4, 5), (0, 2, 3, 3)
AHEAD = (1, 0)
COLUMN_FIRST = (2, 3)
CHIPS_ALONG = (3, 1, 2, 0)
CHIP_ORDER = tuple((other, dy) for other in (1, 0) for dy in (1, -1, 0, 2))


def turn(recv, i, put):
    sources, _, win_j, own_chans, lanes = recv.shape
    chans = sources * own_chans
    for j in range(win_j):
        top = recv[:, 2 * i, j].reshape(chans, lanes)
        under = recv[:, 2 * i + 1, j].reshape(chans, lanes)
        put(j, jnp.concatenate([top, under], axis=0).T.reshape(2, lanes // 2, 2 * chans))


def blocks(pairs, weights, count):
    acc = None
    for dw in range(4):
        parts = [view[dw // 2 : dw // 2 + count, dw % 2] for view in pairs]
        lhs = jnp.concatenate([p.reshape(count * p.shape[1], p.shape[2]) for p in parts], axis=1)
        term = jnp.dot(lhs, weights(dw), preferred_element_type=F32)
        acc = term if acc is None else acc + term
    return acc


def first(pairs, weights, bias, y_row, blank_a):
    count, _, images, lanes = y_row.shape
    c = lax.axis_index("cols")
    row = lax.rem(lax.broadcasted_iota(jnp.int32, (1, 2 * lanes), 1), lanes) // (lanes // 2)
    act = jnp.maximum(blocks(pairs, weights, count) + bias, 0.0)
    act = jnp.where(row != blank_a, act, 0.0).astype(BF16)
    for b in range(2):
        y_row[:, b] = act[:, b * lanes : (b + 1) * lanes].reshape(count, images, lanes)
    blank = jnp.zeros((images, lanes), BF16)

    @pl.when(c == 0)
    def _():
        y_row[0, 0] = blank

    @pl.when(c == lax.axis_size("cols") - 1)
    def _():
        y_row[count - 1, 1] = blank


def second(pairs, weights, bias, out_pair):
    _, count, _, images, chans = out_pair.shape
    res = blocks(pairs, weights, count) + bias
    for b in range(2):
        for a in range(2):
            at = (2 * b + a) * chans
            out_pair[a, :, b] = res[:, at : at + chans].reshape(count, images, chans)


def conv_kernel(
    n_rows,
    n_cols,
    x_hbm,
    w1_hbm,
    b1_hbm,
    w2_hbm,
    b2_hbm,
    out,
    ymat,
    wt2,
    bias2,
    recv,
    xmat,
    wt1,
    bias1,
    xs,
    packed,
    w1s,
    w1own,
    w1all,
    w2s,
    b1s,
    b2s,
    load_sem,
    par_sem,
    send_sem,
    recv_sem,
    wsend_sem,
    wrecv_sem,
    swap_send_sem,
    swap_recv_sem,
    wswap_send_sem,
    wswap_recv_sem,
):
    chip_h, pairs = xs.shape[1:3]
    images = xs.shape[-1]
    tile_h, tile_j = chip_h // 2, pairs // n_cols
    win_j = tile_j + 2
    sources = n_rows * n_cols
    r, c = lax.axis_index("model"), lax.axis_index("cols")
    par = lax.rem(r, 2)
    me = r * n_cols + c
    chans = recv.shape[0] * 2

    tops = [tile_h - sum(CHUNK_ROWS[: k + 1]) for k in range(len(CHUNK_ROWS))]
    groups = (
        ((tops[0], chip_h - tops[0]),),
        *(((k, k + n), (chip_h - k - n, chip_h - k)) for k, n in zip(tops[1:], CHUNK_ROWS[1:])),
    )
    loads = []
    for g, spans in enumerate(groups):
        loads.append(
            [
                pltpu.make_async_copy(x_hbm.at[:, lo:hi], xs.at[:, lo:hi], load_sem.at[g, n])
                for n, (lo, hi) in enumerate(spans)
            ]
        )
    for copies in loads:
        for copy in copies:
            copy.start()
    params = [
        pltpu.make_async_copy(src, dst, par_sem.at[s])
        for s, (src, dst) in enumerate(((w1_hbm, w1s), (w2_hbm, w2s), (b1_hbm, b1s), (b2_hbm, b2s)))
    ]
    for copy in params:
        copy.start()

    barrier = pltpu.get_barrier_semaphore()
    to_cs = [lax.rem(c + k, n_cols) for k in range(n_cols)]

    def device(to_r, to_c):
        return {"model": to_r, "cols": to_c}

    to_rs = [lax.rem(r + k, n_rows) for k in range(n_rows)]
    for kr, kc in sorted(
        ((kr, kc) for kr in range(n_rows) for kc in range(n_cols) if kr or kc),
        key=lambda k: (not (k[0] in (2, 3) and k[1] == 1), -(min(k[0], n_rows - k[0]) // 2 + min(k[1], n_cols - k[1]))),
    ):
        pl.semaphore_signal(barrier, inc=1, device_id=device(to_rs[kr], to_cs[kc]), device_id_type=MESH)

    def pack_rows(x, lo, hi):
        rows = hi - lo
        left, right = (xs[x, lo:hi, :, p].reshape(rows * pairs * 2, images) for p in range(2))
        both = jnp.concatenate([left, right], axis=1)
        packed[pl.ds(chip_h * x + lo, rows)] = both.reshape(rows, pairs, 2, 2 * images)

    def pack(g):
        for copy in loads[g]:
            copy.wait()

        def body(x, carry):
            for lo, hi in groups[g]:
                pack_rows(x, lo, hi)
            return carry

        lax.fori_loop(0, n_rows // 2, body, 0)

    last = tile_h + 4

    def rows_of(offset, count):
        def where(to_r):
            q = lax.rem(to_r, 2)
            src = tile_h * to_r + offset + (tile_h - count - 2 * offset) * q
            dst = offset + 2 + (last - count - 2 * offset - 3) * q
            return src, dst

        return where

    chunks = (
        *((n, rows_of(k, n), False) for k, n in zip(tops, CHUNK_ROWS)),
        (2, rows_of(-2, 2), True),
    )
    no_outer = (r == 0) | (r == n_rows - 1)
    at_edge = (c == 0) | (c == n_cols - 1)
    own_j = c == 0
    own_j = own_j.astype(jnp.int32)

    def send_tile(chunk, to_r, to_c, there):
        rows, where, is_outer = chunks[chunk]
        src, dst = where(to_r)
        skip = (to_c == 0).astype(jnp.int32)
        edge = (to_c == 0) | (to_c == n_cols - 1)
        if is_outer:
            there = there & (to_r > 0) & (to_r < n_rows - 1)

        def copy(count, src_j, dst_j):
            pltpu.make_async_remote_copy(
                src_ref=packed.at[pl.ds(src, rows), pl.ds(src_j, count)],
                dst_ref=recv.at[me, pl.ds(dst, rows), pl.ds(dst_j, count)],
                send_sem=send_sem.at[chunk],
                recv_sem=recv_sem.at[chunk],
                device_id=device(to_r, to_c),
                device_id_type=MESH,
            ).start()

        pl.when(there & edge)(lambda: copy(win_j - 1, tile_j * to_c - 1 + skip, skip))
        pl.when(there & jnp.logical_not(edge))(lambda: copy(win_j, tile_j * to_c - 1, 0))

    chips = n_rows // 2
    ahead_r, ahead_c = AHEAD

    def step(t, table):
        value = jnp.int32(table[-1])
        for k, entry in enumerate(table[:-1]):
            value = jnp.where(t == k, entry, value)
        return value

    def turn_to(t):
        dx = step(t, CHIPS_ALONG)
        return lax.rem(r // 2 + dx, chips), dx

    def send_chip(chunk, t, rest, where=None):
        x, dx = turn_to(t)
        way = 1 - 2 * lax.rem(par + t, 2)
        for other, dy in CHIP_ORDER:
            to_r = 2 * x + (1 - par if other else par)
            to_c = lax.rem(c + way * dy + n_cols, n_cols)
            there = True
            if not other and dy == 0:
                there = dx > 0
            if rest:
                there = there & jnp.logical_not((to_r == ahead_r) & (to_c == ahead_c))
            if where is not None:
                there = there & where(to_c)
            send_tile(chunk, to_r, to_c, there)

    def send_ahead(chunk):
        send_tile(chunk, jnp.int32(ahead_r), jnp.int32(ahead_c), (r != ahead_r) | (c != ahead_c))

    def send_chunk(chunk):

        def first_column(t, carry):
            x, _ = turn_to(t)
            for other in range(2):
                to_r = 2 * x + (1 - par if other else par)
                there = ((to_r != r) | (c != 0)) & (to_r != ahead_r)
                send_tile(chunk, to_r, jnp.int32(0), there)
            return carry

        where = None
        if chunk in COLUMN_FIRST:
            lax.fori_loop(0, chips, first_column, 0)
            where = lambda to_c: to_c > 0

        def body(t, carry):
            send_chip(chunk, t, True, where)
            return carry

        lax.fori_loop(0, chips, body, 0)

    params[0].wait()
    for dw in range(3):
        w1own[dw] = jnp.concatenate([w1s[1, dw], w1s[0, dw]], axis=1)
    w1own[3] = jnp.concatenate([w1s[2, 0], w1s[2, 1]], axis=1)
    w1own[4] = jnp.concatenate([w1s[2, 2], jnp.zeros_like(w1s[2, 2])], axis=1)
    w1all[r // 2, par, c] = w1own[...]

    for copy in loads[0]:
        copy.wait()
    pack_rows(turn_to(0)[0], *groups[0][0])
    pl.semaphore_wait(barrier, sources - 1)

    def send_weights():
        for kr in range(0, n_rows, 2):
            for kc in range(n_cols):
                if kr or kc:
                    pltpu.make_async_remote_copy(
                        src_ref=w1own,
                        dst_ref=w1all.at[r // 2, par, c],
                        send_sem=wsend_sem,
                        recv_sem=wrecv_sem,
                        device_id=device(to_rs[kr], to_cs[kc]),
                        device_id_type=MESH,
                    ).start()

    def pack_and_send(t, carry):
        pl.when(t < chips - 1)(lambda: pack_rows(turn_to(t + 1)[0], *groups[0][0]))
        send_chip(0, t, False)
        pl.when(t == 0)(send_weights)
        return carry

    lax.fori_loop(0, chips, pack_and_send, 0)

    pack(1)
    send_ahead(1)
    send_chunk(1)
    pack(2)
    send_ahead(2)
    send_ahead(3)
    send_chunk(2)
    send_chunk(3)

    def wait_bytes(ref, sem):
        pltpu.make_async_copy(ref, ref, sem).wait()

    w1_bytes = recv.at[0 : sources // 2 - 1, 0, 0:5]
    wait_bytes(w1_bytes, wrecv_sem)
    wait_bytes(w1_bytes, wsend_sem)
    partner = device(r + 1 - 2 * par, c)
    w_swap = pltpu.make_async_remote_copy(
        src_ref=w1all.at[:, par],
        dst_ref=w1all.at[:, par],
        send_sem=wswap_send_sem,
        recv_sem=wswap_recv_sem,
        device_id=partner,
        device_id_type=MESH,
    )
    w_swap.start()

    def own_rows(chunk):
        rows, where, _ = chunks[chunk]
        src, dst = where(r)

        def copy(count, src_j, dst_j):
            for h in range(rows):
                recv[me, dst + h, pl.ds(dst_j, count)] = packed[src + h, pl.ds(src_j, count)]

        pl.when(at_edge)(lambda: copy(win_j - 1, tile_j * c - 1 + own_j, own_j))
        pl.when(jnp.logical_not(at_edge))(lambda: copy(win_j, tile_j * c - 1, 0))

    for chunk in range(3):
        own_rows(chunk)
    pl.when(jnp.logical_not(no_outer))(lambda: own_rows(3))

    zero_row = jnp.zeros((win_j, 2, 2 * images), BF16)
    zero_col = jnp.zeros((tile_h + 2, 2, 2 * images), BF16)

    def clear(s, carry):
        recv[s, last * (1 - par)] = zero_row
        return carry

    def clear_outer(s, carry):
        recv[s, (last - 1) * par] = zero_row
        recv[s, (last - 1) * par + 1] = zero_row
        return carry

    def clear_edge(s, carry):
        recv[s, pl.ds(3 * par, tile_h + 2), (win_j - 1) * (1 - own_j)] = zero_col
        return carry

    lax.fori_loop(0, sources, clear, 0)
    pl.when(no_outer)(lambda: (lax.fori_loop(0, sources, clear_outer, 0), None)[1])
    pl.when(at_edge)(lambda: (lax.fori_loop(0, sources, clear_edge, 0), None)[1])

    low = lax.broadcasted_iota(jnp.int32, (chans, 2 * chans), 1) < chans

    def spread(wt, u, v, dw):
        ur, vr = pltpu.roll(u, chans, 1), pltpu.roll(v, chans, 1)
        zero = jnp.zeros_like(u)
        tiles = (jnp.where(low, ur, zero), u, jnp.where(low, v, ur), jnp.where(low, zero, vr))
        for k, tile in enumerate(tiles):
            tile = tile.astype(BF16)
            for b in range(2):
                wt[dw + b, k * chans : (k + 1) * chans, b * 2 * chans : (b + 1) * 2 * chans] = tile

    def blank(wt):
        zero = jnp.zeros((4 * chans, 2 * chans), BF16)
        wt[3, :, 0 : 2 * chans] = zero
        wt[0, :, 2 * chans : 4 * chans] = zero

    for copy in params[1:]:
        copy.wait()
    blank(wt1)
    blank(wt2)
    for dw in range(3):
        w = [w2s[dh, dw].astype(F32) for dh in range(3)]
        spread(
            wt2,
            jnp.concatenate([w[1], w[0]], axis=1),
            jnp.concatenate([w[2], jnp.zeros_like(w[2])], axis=1),
            dw,
        )
    bias1[...] = jnp.concatenate([b1s[...]] * 4, axis=1)
    bias2[...] = jnp.concatenate([b2s[...]] * 4, axis=1)

    def arrived(chunk):
        def wait(count):
            wait_bytes(recv.at[0 : sources - 1, 0 : chunks[chunk][0], 0:count], recv_sem.at[chunk])

        pl.when(at_edge)(lambda: wait(win_j - 1))
        pl.when(jnp.logical_not(at_edge))(lambda: wait(win_j))

    arrived(0)
    give = tile_h - (tile_h - 3) * par
    land = tile_h + 2 - (tile_h + 1) * (1 - par)
    swap = pltpu.make_async_remote_copy(
        src_ref=recv.at[:, pl.ds(give, 2)],
        dst_ref=recv.at[:, pl.ds(land, 2)],
        send_sem=swap_send_sem,
        recv_sem=swap_recv_sem,
        device_id=partner,
        device_id_type=MESH,
    )
    swap.start()

    w_swap.wait()
    u = [w1all[:, :, :, k].reshape(chans, 2 * chans).astype(F32) for k in range(5)]
    for dw in range(3):
        v = (u[3], pltpu.roll(u[3], chans, 1), u[4])[dw]
        spread(wt1, u[dw], jnp.where(low, v, 0.0), dw)

    x_pairs, z_pairs = xmat.shape[0], ymat.shape[0]
    o_pairs = z_pairs - 1

    def nth(n, count):
        return (count - 1) * (1 - par) + n * (2 * par - 1)

    def turn_one(n, carry):
        i = nth(n, x_pairs)

        def put(j, value):
            xmat[i, j] = value

        turn(recv, i, put)
        return carry

    def first_one(n, carry):
        i = nth(n, z_pairs)
        fill = jnp.where(n == 0, 1 - par, 2)
        out_of = jnp.where(n == z_pairs - 1, jnp.where(r == 0, 0, jnp.where(r == n_rows - 1, 1, 2)), 2)
        blank_a = jnp.where(fill < 2, fill, out_of)
        first((xmat.at[i], xmat.at[i + 1]), lambda dw: wt1[dw], bias1[...], ymat.at[i], blank_a)
        return carry

    def second_one(n, carry):
        i = nth(n, o_pairs)
        second((ymat.at[i], ymat.at[i + 1]), lambda dw: wt2[dw], bias2[...], out.at[pl.ds(2 * i, 2)])
        return carry

    def stage(s, carry):
        @pl.when(s == 0)
        def _():
            swap.wait()

        for k in range(1, 4):
            there = s == k
            if k == 3:
                there = there & jnp.logical_not(no_outer)
            pl.when(there)(lambda k=k: arrived(k))

        for ends, one in ((TURNS, turn_one), (FIRSTS, first_one), (SECONDS, second_one)):
            lax.fori_loop(step(s, (0, *ends[:-1])), step(s, ends), one, 0)
        return carry

    lax.fori_loop(0, 4, stage, 0)

    per_edge = n_rows * 2
    for chunk in range(4):
        rows = chunks[chunk][0]
        n_r = n_rows - 2 if chunk == 3 else n_rows
        counts = (n_r * 2, n_r * (n_cols - 2))

        def drain(edge_n, inner_n, rows=rows, chunk=chunk):
            wait_bytes(recv.at[0:edge_n, 0:rows, 0 : win_j - 1], send_sem.at[chunk])
            wait_bytes(recv.at[0:inner_n, 0:rows, 0:win_j], send_sem.at[chunk])

        def drain_own(chunk=chunk, counts=counts, drain=drain):
            pl.when(at_edge)(lambda: drain(counts[0] - 1, counts[1]))
            pl.when(jnp.logical_not(at_edge))(lambda: drain(counts[0], counts[1] - 1))

        if chunk == 3:
            pl.when(no_outer)(lambda: drain(*counts))
            pl.when(jnp.logical_not(no_outer))(drain_own)
        else:
            drain_own()


def tail_kernel(tile, ymat, wt2, bias2, out_hbm, o_new, sem):
    par = lax.rem(lax.axis_index("model"), 2)
    rows = out_hbm.shape[0]
    o_pairs = ymat.shape[0] - 1
    late = (rows - 2) * par
    here = 2 * (1 - par)

    def start(k, carry):
        pltpu.make_async_copy(tile.at[par + k], out_hbm.at[k], sem.at[0]).start()
        return carry

    lax.fori_loop(here, here + rows - 2, start, 0)
    i = (o_pairs - 1) * par
    second((ymat.at[i], ymat.at[i + 1]), lambda dw: wt2[dw], bias2[...], o_new)
    last = pltpu.make_async_copy(o_new, out_hbm.at[pl.ds(late, 2)], sem.at[1])
    last.start()
    pltpu.make_async_copy(tile.at[0 : rows - 2], out_hbm.at[0 : rows - 2], sem.at[0]).wait()
    last.wait()


def solution(mesh):
    n_rows = mesh.shape["model"]
    n_cols = mesh.shape["cols"]

    def run_local(x_in, w_conv1, b_conv1, w_conv2, b_conv2):
        images, height, width, own_chans = x_in.shape
        sources = n_rows * n_cols
        chans = own_chans * sources
        pairs = width // 2
        tile_h, tile_j = height // n_rows, pairs // n_cols
        win_j = tile_j + 2
        x_pairs, z_pairs = (tile_h + 5) // 2, (tile_h + 3) // 2
        x_t = jnp.transpose(x_in, (1, 2, 3, 0)).reshape(n_rows // 2, 2 * tile_h, pairs, 2, own_chans, images)
        args = (x_t, w_conv1, b_conv1.reshape(1, chans), w_conv2, b_conv2.reshape(1, chans))
        hbm = pl.BlockSpec(memory_space=pltpu.HBM)
        vmem = pl.BlockSpec(memory_space=pltpu.VMEM)
        kept = (
            pltpu.VMEM((2 * (z_pairs - 1), tile_j, 2, images, chans), F32),
            pltpu.VMEM((z_pairs, win_j - 1, 2, images, 2 * chans), BF16),
            pltpu.VMEM((4, 4 * chans, 4 * chans), BF16),
            pltpu.VMEM((1, 4 * chans), F32),
        )
        state = pl.pallas_call(
            functools.partial(conv_kernel, n_rows, n_cols),
            out_shape=kept,
            in_specs=[hbm] * 5,
            out_specs=[vmem] * len(kept),
            scratch_shapes=[
                pltpu.VMEM((sources, 2 * x_pairs, win_j, own_chans, 2 * images), BF16),
                pltpu.VMEM((x_pairs, win_j, 2, images, 2 * chans), BF16),
                pltpu.VMEM((4, 4 * chans, 4 * chans), BF16),
                pltpu.VMEM((1, 4 * chans), F32),
                pltpu.VMEM((n_rows // 2, 2 * tile_h, pairs, 2, own_chans, images), BF16),
                pltpu.VMEM((height, pairs, own_chans, 2 * images), BF16),
                pltpu.VMEM((3, 3, own_chans, chans), BF16),
                pltpu.VMEM((5, own_chans, 2 * chans), BF16),
                pltpu.VMEM((n_rows // 2, 2, n_cols, 5, own_chans, 2 * chans), BF16),
                pltpu.VMEM((3, 3, chans, chans), BF16),
                pltpu.VMEM((1, chans), F32),
                pltpu.VMEM((1, chans), F32),
                pltpu.SemaphoreType.DMA((3, 2)),
                pltpu.SemaphoreType.DMA((4,)),
                pltpu.SemaphoreType.DMA((4,)),
                pltpu.SemaphoreType.DMA((4,)),
            ]
            + [pltpu.SemaphoreType.DMA] * 6,
            compiler_params=pltpu.CompilerParams(
                collective_id=0, has_side_effects=True, vmem_limit_bytes=24 << 20
            ),
            name="conv",
        )(*(pltpu.with_memory_space_constraint(a, pltpu.HBM) for a in args))
        out = pl.pallas_call(
            tail_kernel,
            out_shape=jax.ShapeDtypeStruct((tile_h, tile_j, 2, images, chans), F32),
            in_specs=[vmem] * len(kept),
            out_specs=pl.BlockSpec(memory_space=pl.ANY),
            scratch_shapes=[
                pltpu.VMEM((2, tile_j, 2, images, chans), F32),
                pltpu.SemaphoreType.DMA((2,)),
            ],
            compiler_params=pltpu.CompilerParams(vmem_limit_bytes=8 << 20),
            name="tail",
        )(*state)
        out = out.reshape(tile_h, 2 * tile_j, images, chans)
        return jnp.transpose(out, (2, 0, 1, 3))

    group = ("model", "cols")
    return jax.shard_map(
        run_local,
        mesh=mesh,
        in_specs=(P("data", None, None, group), P(None, None, group, None), P(), P(), P()),
        out_specs=P("data", "model", "cols", None),
        check_vma=False,
    )
```

```python
import functools

import jax
import jax.numpy as jnp
from jax import lax
from jax.experimental import pallas as pl
from jax.experimental.pallas import tpu as pltpu
from jax.sharding import PartitionSpec as P

MESH = pl.DeviceIdType.MESH
BF16 = jnp.bfloat16
F32 = jnp.float32
CHUNK_ROWS = (2, 3, 2)
TURNS, FIRSTS, SECONDS = (2, 4, 5, 6), (1, 3, 4, 5), (0, 2, 3, 3)
AHEAD = (1, 0)
COLUMN_FIRST = (3,)
CHIPS_ALONG = (3, 1, 2, 0)
CHIP_ORDER = tuple((other, dy) for other in (0, 1) for dy in (1, -1, 0, 2))


def turn(recv, i, put):
    sources, _, win_j, own_chans, lanes = recv.shape
    chans = sources * own_chans
    for j in range(win_j):
        top = recv[:, 2 * i, j].reshape(chans, lanes)
        under = recv[:, 2 * i + 1, j].reshape(chans, lanes)
        put(j, jnp.concatenate([top, under], axis=0).T.reshape(2, lanes // 2, 2 * chans))


def blocks(pairs, weights, count):
    acc = None
    for dw in range(4):
        parts = [view[dw // 2 : dw // 2 + count, dw % 2] for view in pairs]
        lhs = jnp.concatenate([p.reshape(count * p.shape[1], p.shape[2]) for p in parts], axis=1)
        term = jnp.dot(lhs, weights(dw), preferred_element_type=F32)
        acc = term if acc is None else acc + term
    return acc


def first(pairs, weights, bias, y_row, blank_a):
    count, _, images, lanes = y_row.shape
    c = lax.axis_index("cols")
    row = lax.rem(lax.broadcasted_iota(jnp.int32, (1, 2 * lanes), 1), lanes) // (lanes // 2)
    act = jnp.maximum(blocks(pairs, weights, count) + bias, 0.0)
    act = jnp.where(row != blank_a, act, 0.0).astype(BF16)
    for b in range(2):
        y_row[:, b] = act[:, b * lanes : (b + 1) * lanes].reshape(count, images, lanes)
    blank = jnp.zeros((images, lanes), BF16)

    @pl.when(c == 0)
    def _():
        y_row[0, 0] = blank

    @pl.when(c == lax.axis_size("cols") - 1)
    def _():
        y_row[count - 1, 1] = blank


def second(pairs, weights, bias, out_pair):
    _, count, _, images, chans = out_pair.shape
    res = blocks(pairs, weights, count) + bias
    for b in range(2):
        for a in range(2):
            at = (2 * b + a) * chans
            out_pair[a, :, b] = res[:, at : at + chans].reshape(count, images, chans)


def conv_kernel(
    n_rows,
    n_cols,
    x_hbm,
    w1_hbm,
    b1_hbm,
    w2_hbm,
    b2_hbm,
    out,
    ymat,
    wt2,
    bias2,
    recv,
    xmat,
    wt1,
    bias1,
    xs,
    packed,
    w1s,
    w1own,
    w1all,
    w2s,
    b1s,
    b2s,
    load_sem,
    par_sem,
    send_sem,
    recv_sem,
    wsend_sem,
    wrecv_sem,
    swap_send_sem,
    swap_recv_sem,
    wswap_send_sem,
    wswap_recv_sem,
):
    chip_h, pairs = xs.shape[1:3]
    images = xs.shape[-1]
    tile_h, tile_j = chip_h // 2, pairs // n_cols
    win_j = tile_j + 2
    sources = n_rows * n_cols
    r, c = lax.axis_index("model"), lax.axis_index("cols")
    par = lax.rem(r, 2)
    me = r * n_cols + c
    chans = recv.shape[0] * 2

    tops = [tile_h - sum(CHUNK_ROWS[: k + 1]) for k in range(len(CHUNK_ROWS))]
    groups = (
        ((tops[0], chip_h - tops[0]),),
        *(((k, k + n), (chip_h - k - n, chip_h - k)) for k, n in zip(tops[1:], CHUNK_ROWS[1:])),
    )
    loads = []
    for g, spans in enumerate(groups):
        loads.append(
            [
                pltpu.make_async_copy(x_hbm.at[:, lo:hi], xs.at[:, lo:hi], load_sem.at[g, n])
                for n, (lo, hi) in enumerate(spans)
            ]
        )
    for copies in loads:
        for copy in copies:
            copy.start()
    params = [
        pltpu.make_async_copy(src, dst, par_sem.at[s])
        for s, (src, dst) in enumerate(((w1_hbm, w1s), (w2_hbm, w2s), (b1_hbm, b1s), (b2_hbm, b2s)))
    ]
    for copy in params:
        copy.start()

    barrier = pltpu.get_barrier_semaphore()
    to_cs = [lax.rem(c + k, n_cols) for k in range(n_cols)]

    def device(to_r, to_c):
        return {"model": to_r, "cols": to_c}

    to_rs = [lax.rem(r + k, n_rows) for k in range(n_rows)]
    for kr, kc in sorted(
        ((kr, kc) for kr in range(n_rows) for kc in range(n_cols) if kr or kc),
        key=lambda k: (not (k[0] in (2, 3) and k[1] == 1), -(min(k[0], n_rows - k[0]) // 2 + min(k[1], n_cols - k[1]))),
    ):
        pl.semaphore_signal(barrier, inc=1, device_id=device(to_rs[kr], to_cs[kc]), device_id_type=MESH)

    def pack_rows(x, lo, hi):
        rows = hi - lo
        left, right = (xs[x, lo:hi, :, p].reshape(rows * pairs * 2, images) for p in range(2))
        both = jnp.concatenate([left, right], axis=1)
        packed[pl.ds(chip_h * x + lo, rows)] = both.reshape(rows, pairs, 2, 2 * images)

    def pack(g):
        for copy in loads[g]:
            copy.wait()

        def body(x, carry):
            for lo, hi in groups[g]:
                pack_rows(x, lo, hi)
            return carry

        lax.fori_loop(0, n_rows // 2, body, 0)

    last = tile_h + 4

    def rows_of(offset, count):
        def where(to_r):
            q = lax.rem(to_r, 2)
            src = tile_h * to_r + offset + (tile_h - count - 2 * offset) * q
            dst = offset + 2 + (last - count - 2 * offset - 3) * q
            return src, dst

        return where

    chunks = (
        *((n, rows_of(k, n), False) for k, n in zip(tops, CHUNK_ROWS)),
        (2, rows_of(-2, 2), True),
    )
    no_outer = (r == 0) | (r == n_rows - 1)
    at_edge = (c == 0) | (c == n_cols - 1)
    own_j = c == 0
    own_j = own_j.astype(jnp.int32)

    def send_tile(chunk, to_r, to_c, there):
        rows, where, is_outer = chunks[chunk]
        src, dst = where(to_r)
        skip = (to_c == 0).astype(jnp.int32)
        edge = (to_c == 0) | (to_c == n_cols - 1)
        if is_outer:
            there = there & (to_r > 0) & (to_r < n_rows - 1)

        def copy(count, src_j, dst_j):
            pltpu.make_async_remote_copy(
                src_ref=packed.at[pl.ds(src, rows), pl.ds(src_j, count)],
                dst_ref=recv.at[me, pl.ds(dst, rows), pl.ds(dst_j, count)],
                send_sem=send_sem.at[chunk],
                recv_sem=recv_sem.at[chunk],
                device_id=device(to_r, to_c),
                device_id_type=MESH,
            ).start()

        pl.when(there & edge)(lambda: copy(win_j - 1, tile_j * to_c - 1 + skip, skip))
        pl.when(there & jnp.logical_not(edge))(lambda: copy(win_j, tile_j * to_c - 1, 0))

    chips = n_rows // 2
    ahead_r, ahead_c = AHEAD

    def step(t, table):
        value = jnp.int32(table[-1])
        for k, entry in enumerate(table[:-1]):
            value = jnp.where(t == k, entry, value)
        return value

    def turn_to(t):
        dx = step(t, CHIPS_ALONG)
        return lax.rem(r // 2 + dx, chips), dx

    def send_chip(chunk, t, rest, where=None):
        x, dx = turn_to(t)
        way = 1 - 2 * lax.rem(par + t, 2)
        for other, dy in CHIP_ORDER:
            to_r = 2 * x + (1 - par if other else par)
            to_c = lax.rem(c + way * dy + n_cols, n_cols)
            there = True
            if not other and dy == 0:
                there = dx > 0
            if rest:
                there = there & jnp.logical_not((to_r == ahead_r) & (to_c == ahead_c))
            if where is not None:
                there = there & where(to_c)
            send_tile(chunk, to_r, to_c, there)

    def send_ahead(chunk):
        send_tile(chunk, jnp.int32(ahead_r), jnp.int32(ahead_c), (r != ahead_r) | (c != ahead_c))

    def send_chunk(chunk):

        def first_column(t, carry):
            x, _ = turn_to(t)
            for other in range(2):
                to_r = 2 * x + (1 - par if other else par)
                there = ((to_r != r) | (c != 0)) & (to_r != ahead_r)
                send_tile(chunk, to_r, jnp.int32(0), there)
            return carry

        where = None
        if chunk in COLUMN_FIRST:
            lax.fori_loop(0, chips, first_column, 0)
            where = lambda to_c: to_c > 0

        def body(t, carry):
            send_chip(chunk, t, True, where)
            return carry

        lax.fori_loop(0, chips, body, 0)

    params[0].wait()
    for dw in range(3):
        w1own[dw] = jnp.concatenate([w1s[1, dw], w1s[0, dw]], axis=1)
    w1own[3] = jnp.concatenate([w1s[2, 0], w1s[2, 1]], axis=1)
    w1own[4] = jnp.concatenate([w1s[2, 2], jnp.zeros_like(w1s[2, 2])], axis=1)
    w1all[r // 2, par, c] = w1own[...]

    for copy in loads[0]:
        copy.wait()
    pack_rows(turn_to(0)[0], *groups[0][0])
    pl.semaphore_wait(barrier, sources - 1)

    def send_weights():
        for kr in range(0, n_rows, 2):
            for kc in range(n_cols):
                if kr or kc:
                    pltpu.make_async_remote_copy(
                        src_ref=w1own,
                        dst_ref=w1all.at[r // 2, par, c],
                        send_sem=wsend_sem,
                        recv_sem=wrecv_sem,
                        device_id=device(to_rs[kr], to_cs[kc]),
                        device_id_type=MESH,
                    ).start()

    def pack_and_send(t, carry):
        pl.when(t < chips - 1)(lambda: pack_rows(turn_to(t + 1)[0], *groups[0][0]))
        send_chip(0, t, False)
        pl.when(t == 0)(send_weights)
        return carry

    lax.fori_loop(0, chips, pack_and_send, 0)

    pack(1)
    send_ahead(1)
    send_chunk(1)
    pack(2)
    send_ahead(2)
    send_ahead(3)
    send_chunk(2)
    send_chunk(3)

    def wait_bytes(ref, sem):
        pltpu.make_async_copy(ref, ref, sem).wait()

    w1_bytes = recv.at[0 : sources // 2 - 1, 0, 0:5]
    wait_bytes(w1_bytes, wrecv_sem)
    wait_bytes(w1_bytes, wsend_sem)
    partner = device(r + 1 - 2 * par, c)
    w_swap = pltpu.make_async_remote_copy(
        src_ref=w1all.at[:, par],
        dst_ref=w1all.at[:, par],
        send_sem=wswap_send_sem,
        recv_sem=wswap_recv_sem,
        device_id=partner,
        device_id_type=MESH,
    )
    w_swap.start()

    def own_rows(chunk):
        rows, where, _ = chunks[chunk]
        src, dst = where(r)

        def copy(count, src_j, dst_j):
            for h in range(rows):
                recv[me, dst + h, pl.ds(dst_j, count)] = packed[src + h, pl.ds(src_j, count)]

        pl.when(at_edge)(lambda: copy(win_j - 1, tile_j * c - 1 + own_j, own_j))
        pl.when(jnp.logical_not(at_edge))(lambda: copy(win_j, tile_j * c - 1, 0))

    for chunk in range(3):
        own_rows(chunk)
    pl.when(jnp.logical_not(no_outer))(lambda: own_rows(3))

    zero_row = jnp.zeros((win_j, 2, 2 * images), BF16)
    zero_col = jnp.zeros((tile_h + 2, 2, 2 * images), BF16)

    def clear(s, carry):
        recv[s, last * (1 - par)] = zero_row
        return carry

    def clear_outer(s, carry):
        recv[s, (last - 1) * par] = zero_row
        recv[s, (last - 1) * par + 1] = zero_row
        return carry

    def clear_edge(s, carry):
        recv[s, pl.ds(3 * par, tile_h + 2), (win_j - 1) * (1 - own_j)] = zero_col
        return carry

    lax.fori_loop(0, sources, clear, 0)
    pl.when(no_outer)(lambda: (lax.fori_loop(0, sources, clear_outer, 0), None)[1])
    pl.when(at_edge)(lambda: (lax.fori_loop(0, sources, clear_edge, 0), None)[1])

    low = lax.broadcasted_iota(jnp.int32, (chans, 2 * chans), 1) < chans

    def spread(wt, u, v, dw):
        ur, vr = pltpu.roll(u, chans, 1), pltpu.roll(v, chans, 1)
        zero = jnp.zeros_like(u)
        tiles = (jnp.where(low, ur, zero), u, jnp.where(low, v, ur), jnp.where(low, zero, vr))
        for k, tile in enumerate(tiles):
            tile = tile.astype(BF16)
            for b in range(2):
                wt[dw + b, k * chans : (k + 1) * chans, b * 2 * chans : (b + 1) * 2 * chans] = tile

    def blank(wt):
        zero = jnp.zeros((4 * chans, 2 * chans), BF16)
        wt[3, :, 0 : 2 * chans] = zero
        wt[0, :, 2 * chans : 4 * chans] = zero

    for copy in params[1:]:
        copy.wait()
    blank(wt1)
    blank(wt2)
    for dw in range(3):
        w = [w2s[dh, dw].astype(F32) for dh in range(3)]
        spread(
            wt2,
            jnp.concatenate([w[1], w[0]], axis=1),
            jnp.concatenate([w[2], jnp.zeros_like(w[2])], axis=1),
            dw,
        )
    bias1[...] = jnp.concatenate([b1s[...]] * 4, axis=1)
    bias2[...] = jnp.concatenate([b2s[...]] * 4, axis=1)

    def arrived(chunk):
        def wait(count):
            wait_bytes(recv.at[0 : sources - 1, 0 : chunks[chunk][0], 0:count], recv_sem.at[chunk])

        pl.when(at_edge)(lambda: wait(win_j - 1))
        pl.when(jnp.logical_not(at_edge))(lambda: wait(win_j))

    arrived(0)
    give = tile_h - (tile_h - 3) * par
    land = tile_h + 2 - (tile_h + 1) * (1 - par)
    swap = pltpu.make_async_remote_copy(
        src_ref=recv.at[:, pl.ds(give, 2)],
        dst_ref=recv.at[:, pl.ds(land, 2)],
        send_sem=swap_send_sem,
        recv_sem=swap_recv_sem,
        device_id=partner,
        device_id_type=MESH,
    )
    swap.start()

    w_swap.wait()
    u = [w1all[:, :, :, k].reshape(chans, 2 * chans).astype(F32) for k in range(5)]
    for dw in range(3):
        v = (u[3], pltpu.roll(u[3], chans, 1), u[4])[dw]
        spread(wt1, u[dw], jnp.where(low, v, 0.0), dw)

    x_pairs, z_pairs = xmat.shape[0], ymat.shape[0]
    o_pairs = z_pairs - 1

    def nth(n, count):
        return (count - 1) * (1 - par) + n * (2 * par - 1)

    def turn_one(n, carry):
        i = nth(n, x_pairs)

        def put(j, value):
            xmat[i, j] = value

        turn(recv, i, put)
        return carry

    def first_one(n, carry):
        i = nth(n, z_pairs)
        fill = jnp.where(n == 0, 1 - par, 2)
        out_of = jnp.where(n == z_pairs - 1, jnp.where(r == 0, 0, jnp.where(r == n_rows - 1, 1, 2)), 2)
        blank_a = jnp.where(fill < 2, fill, out_of)
        first((xmat.at[i], xmat.at[i + 1]), lambda dw: wt1[dw], bias1[...], ymat.at[i], blank_a)
        return carry

    def second_one(n, carry):
        i = nth(n, o_pairs)
        second((ymat.at[i], ymat.at[i + 1]), lambda dw: wt2[dw], bias2[...], out.at[pl.ds(2 * i, 2)])
        return carry

    def stage(s, carry):
        @pl.when(s == 0)
        def _():
            swap.wait()

        for k in range(1, 4):
            there = s == k
            if k == 3:
                there = there & jnp.logical_not(no_outer)
            pl.when(there)(lambda k=k: arrived(k))

        for ends, one in ((TURNS, turn_one), (FIRSTS, first_one), (SECONDS, second_one)):
            lax.fori_loop(step(s, (0, *ends[:-1])), step(s, ends), one, 0)
        return carry

    lax.fori_loop(0, 4, stage, 0)

    per_edge = n_rows * 2
    for chunk in range(4):
        rows = chunks[chunk][0]
        n_r = n_rows - 2 if chunk == 3 else n_rows
        counts = (n_r * 2, n_r * (n_cols - 2))

        def drain(edge_n, inner_n, rows=rows, chunk=chunk):
            wait_bytes(recv.at[0:edge_n, 0:rows, 0 : win_j - 1], send_sem.at[chunk])
            wait_bytes(recv.at[0:inner_n, 0:rows, 0:win_j], send_sem.at[chunk])

        def drain_own(chunk=chunk, counts=counts, drain=drain):
            pl.when(at_edge)(lambda: drain(counts[0] - 1, counts[1]))
            pl.when(jnp.logical_not(at_edge))(lambda: drain(counts[0], counts[1] - 1))

        if chunk == 3:
            pl.when(no_outer)(lambda: drain(*counts))
            pl.when(jnp.logical_not(no_outer))(drain_own)
        else:
            drain_own()


def tail_kernel(tile, ymat, wt2, bias2, out_hbm, o_new, sem):
    par = lax.rem(lax.axis_index("model"), 2)
    rows = out_hbm.shape[0]
    o_pairs = ymat.shape[0] - 1
    late = (rows - 2) * par
    here = 2 * (1 - par)

    def start(k, carry):
        pltpu.make_async_copy(tile.at[par + k], out_hbm.at[k], sem.at[0]).start()
        return carry

    lax.fori_loop(here, here + rows - 2, start, 0)
    i = (o_pairs - 1) * par
    second((ymat.at[i], ymat.at[i + 1]), lambda dw: wt2[dw], bias2[...], o_new)
    last = pltpu.make_async_copy(o_new, out_hbm.at[pl.ds(late, 2)], sem.at[1])
    last.start()
    pltpu.make_async_copy(tile.at[0 : rows - 2], out_hbm.at[0 : rows - 2], sem.at[0]).wait()
    last.wait()


def solution(mesh):
    n_rows = mesh.shape["model"]
    n_cols = mesh.shape["cols"]

    def run_local(x_in, w_conv1, b_conv1, w_conv2, b_conv2):
        images, height, width, own_chans = x_in.shape
        sources = n_rows * n_cols
        chans = own_chans * sources
        pairs = width // 2
        tile_h, tile_j = height // n_rows, pairs // n_cols
        win_j = tile_j + 2
        x_pairs, z_pairs = (tile_h + 5) // 2, (tile_h + 3) // 2
        x_t = jnp.transpose(x_in, (1, 2, 3, 0)).reshape(n_rows // 2, 2 * tile_h, pairs, 2, own_chans, images)
        args = (x_t, w_conv1, b_conv1.reshape(1, chans), w_conv2, b_conv2.reshape(1, chans))
        hbm = pl.BlockSpec(memory_space=pltpu.HBM)
        vmem = pl.BlockSpec(memory_space=pltpu.VMEM)
        kept = (
            pltpu.VMEM((2 * (z_pairs - 1), tile_j, 2, images, chans), F32),
            pltpu.VMEM((z_pairs, win_j - 1, 2, images, 2 * chans), BF16),
            pltpu.VMEM((4, 4 * chans, 4 * chans), BF16),
            pltpu.VMEM((1, 4 * chans), F32),
        )
        state = pl.pallas_call(
            functools.partial(conv_kernel, n_rows, n_cols),
            out_shape=kept,
            in_specs=[hbm] * 5,
            out_specs=[vmem] * len(kept),
            scratch_shapes=[
                pltpu.VMEM((sources, 2 * x_pairs, win_j, own_chans, 2 * images), BF16),
                pltpu.VMEM((x_pairs, win_j, 2, images, 2 * chans), BF16),
                pltpu.VMEM((4, 4 * chans, 4 * chans), BF16),
                pltpu.VMEM((1, 4 * chans), F32),
                pltpu.VMEM((n_rows // 2, 2 * tile_h, pairs, 2, own_chans, images), BF16),
                pltpu.VMEM((height, pairs, own_chans, 2 * images), BF16),
                pltpu.VMEM((3, 3, own_chans, chans), BF16),
                pltpu.VMEM((5, own_chans, 2 * chans), BF16),
                pltpu.VMEM((n_rows // 2, 2, n_cols, 5, own_chans, 2 * chans), BF16),
                pltpu.VMEM((3, 3, chans, chans), BF16),
                pltpu.VMEM((1, chans), F32),
                pltpu.VMEM((1, chans), F32),
                pltpu.SemaphoreType.DMA((3, 2)),
                pltpu.SemaphoreType.DMA((4,)),
                pltpu.SemaphoreType.DMA((4,)),
                pltpu.SemaphoreType.DMA((4,)),
            ]
            + [pltpu.SemaphoreType.DMA] * 6,
            compiler_params=pltpu.CompilerParams(
                collective_id=0, has_side_effects=True, vmem_limit_bytes=24 << 20
            ),
            name="conv",
        )(*(pltpu.with_memory_space_constraint(a, pltpu.HBM) for a in args))
        out = pl.pallas_call(
            tail_kernel,
            out_shape=jax.ShapeDtypeStruct((tile_h, tile_j, 2, images, chans), F32),
            in_specs=[vmem] * len(kept),
            out_specs=pl.BlockSpec(memory_space=pl.ANY),
            scratch_shapes=[
                pltpu.VMEM((2, tile_j, 2, images, chans), F32),
                pltpu.SemaphoreType.DMA((2,)),
            ],
            compiler_params=pltpu.CompilerParams(vmem_limit_bytes=8 << 20),
            name="tail",
        )(*state)
        out = out.reshape(tile_h, 2 * tile_j, images, chans)
        return jnp.transpose(out, (2, 0, 1, 3))

    group = ("model", "cols")
    return jax.shard_map(
        run_local,
        mesh=mesh,
        in_specs=(P("data", None, None, group), P(None, None, group, None), P(), P(), P()),
        out_specs=P("data", "model", "cols", None),
        check_vma=False,
    )
```

```python
import functools

import jax
import jax.numpy as jnp
from jax import lax
from jax.experimental import pallas as pl
from jax.experimental.pallas import tpu as pltpu
from jax.sharding import PartitionSpec as P

MESH = pl.DeviceIdType.MESH
BF16 = jnp.bfloat16
F32 = jnp.float32
CHUNK_ROWS = (2, 3, 2)
TURNS, FIRSTS, SECONDS = (2, 4, 5, 6), (1, 3, 4, 4), (0, 2, 3, 3)
AHEAD = (1, 0)
COLUMN_FIRST = (2, 3)
CHIPS_ALONG = (3, 1, 2, 0)
CHIP_ORDER = tuple((other, dy) for other in (0, 1) for dy in (0, 1, -1, 2))


def turn(recv, i, put):
    sources, _, win_j, own_chans, lanes = recv.shape
    chans = sources * own_chans
    for j in range(win_j):
        top = recv[:, 2 * i, j].reshape(chans, lanes)
        under = recv[:, 2 * i + 1, j].reshape(chans, lanes)
        put(j, jnp.concatenate([top, under], axis=0).T.reshape(2, lanes // 2, 2 * chans))


def blocks(pairs, weights, lo, count):
    acc = None
    for dw in range(4):
        parts = [view[pl.ds(dw // 2 + lo, count), dw % 2] for view in pairs]
        lhs = jnp.concatenate([p.reshape(count * p.shape[1], p.shape[2]) for p in parts], axis=1)
        term = jnp.dot(lhs, weights(dw), preferred_element_type=F32)
        acc = term if acc is None else acc + term
    return acc


def first(pairs, weights, bias, y_row, blank_a, lo, count):
    images, lanes = y_row.shape[2:]
    row = lax.rem(lax.broadcasted_iota(jnp.int32, (1, 2 * lanes), 1), lanes) // (lanes // 2)
    act = jnp.maximum(blocks(pairs, weights, lo, count) + bias, 0.0)
    act = jnp.where(row != blank_a, act, 0.0).astype(BF16)
    for b in range(2):
        y_row[pl.ds(lo, count), b] = act[:, b * lanes : (b + 1) * lanes].reshape(count, images, lanes)


def blank_edges(y_row):
    count, _, images, lanes = y_row.shape
    c = lax.axis_index("cols")
    blank = jnp.zeros((images, lanes), BF16)

    @pl.when(c == 0)
    def _():
        y_row[0, 0] = blank

    @pl.when(c == lax.axis_size("cols") - 1)
    def _():
        y_row[count - 1, 1] = blank


def second(pairs, weights, bias, out_pair, lo, count):
    images, chans = out_pair.shape[3:]
    res = blocks(pairs, weights, lo, count) + bias
    for b in range(2):
        for a in range(2):
            at = (2 * b + a) * chans
            out_pair[a, pl.ds(lo, count), b] = res[:, at : at + chans].reshape(count, images, chans)


def conv_kernel(
    n_rows,
    n_cols,
    x_hbm,
    w1_hbm,
    b1_hbm,
    w2_hbm,
    b2_hbm,
    out,
    xmat,
    ymat,
    wt1,
    wt2,
    bias1,
    bias2,
    recv,
    xs,
    packed,
    w1s,
    w1own,
    w1all,
    w2s,
    b1s,
    b2s,
    load_sem,
    par_sem,
    send_sem,
    recv_sem,
    wsend_sem,
    wrecv_sem,
    swap_send_sem,
    swap_recv_sem,
    wswap_send_sem,
    wswap_recv_sem,
):
    chip_h, pairs = xs.shape[1:3]
    images = xs.shape[-1]
    tile_h, tile_j = chip_h // 2, pairs // n_cols
    win_j = tile_j + 2
    sources = n_rows * n_cols
    r, c = lax.axis_index("model"), lax.axis_index("cols")
    par = lax.rem(r, 2)
    me = r * n_cols + c
    chans = recv.shape[0] * 2

    tops = [tile_h - sum(CHUNK_ROWS[: k + 1]) for k in range(len(CHUNK_ROWS))]
    groups = (
        ((tops[0], chip_h - tops[0]),),
        *(((k, k + n), (chip_h - k - n, chip_h - k)) for k, n in zip(tops[1:], CHUNK_ROWS[1:])),
    )
    loads = []
    for g, spans in enumerate(groups):
        loads.append(
            [
                pltpu.make_async_copy(x_hbm.at[:, lo:hi], xs.at[:, lo:hi], load_sem.at[g, n])
                for n, (lo, hi) in enumerate(spans)
            ]
        )
    for copies in loads:
        for copy in copies:
            copy.start()
    params = [
        pltpu.make_async_copy(src, dst, par_sem.at[s])
        for s, (src, dst) in enumerate(((w1_hbm, w1s), (w2_hbm, w2s), (b1_hbm, b1s), (b2_hbm, b2s)))
    ]
    for copy in params:
        copy.start()

    barrier = pltpu.get_barrier_semaphore()
    to_cs = [lax.rem(c + k, n_cols) for k in range(n_cols)]

    def device(to_r, to_c):
        return {"model": to_r, "cols": to_c}

    to_rs = [lax.rem(r + k, n_rows) for k in range(n_rows)]
    for kr, kc in sorted(
        ((kr, kc) for kr in range(n_rows) for kc in range(n_cols) if kr or kc),
        key=lambda k: (not (k[0] in (2, 3) and k[1] == 1), -(min(k[0], n_rows - k[0]) // 2 + min(k[1], n_cols - k[1]))),
    ):
        pl.semaphore_signal(barrier, inc=1, device_id=device(to_rs[kr], to_cs[kc]), device_id_type=MESH)

    def pack_rows(x, lo, hi):
        rows = hi - lo
        left, right = (xs[x, lo:hi, :, p].reshape(rows * pairs * 2, images) for p in range(2))
        both = jnp.concatenate([left, right], axis=1)
        packed[pl.ds(chip_h * x + lo, rows)] = both.reshape(rows, pairs, 2, 2 * images)

    def pack(g):
        for copy in loads[g]:
            copy.wait()

        def body(x, carry):
            for lo, hi in groups[g]:
                pack_rows(x, lo, hi)
            return carry

        lax.fori_loop(0, n_rows // 2, body, 0)

    last = tile_h + 4

    def rows_of(offset, count):
        def where(to_r):
            q = lax.rem(to_r, 2)
            src = tile_h * to_r + offset + (tile_h - count - 2 * offset) * q
            dst = offset + 2 + (last - count - 2 * offset - 3) * q
            return src, dst

        return where

    chunks = (
        *((n, rows_of(k, n), False) for k, n in zip(tops, CHUNK_ROWS)),
        (2, rows_of(-2, 2), True),
    )
    no_outer = (r == 0) | (r == n_rows - 1)
    at_edge = (c == 0) | (c == n_cols - 1)
    own_j = c == 0
    own_j = own_j.astype(jnp.int32)

    def send_tile(chunk, to_r, to_c, there):
        rows, where, is_outer = chunks[chunk]
        src, dst = where(to_r)
        skip = (to_c == 0).astype(jnp.int32)
        edge = (to_c == 0) | (to_c == n_cols - 1)
        if is_outer:
            there = there & (to_r > 0) & (to_r < n_rows - 1)

        def copy(count, src_j, dst_j):
            pltpu.make_async_remote_copy(
                src_ref=packed.at[pl.ds(src, rows), pl.ds(src_j, count)],
                dst_ref=recv.at[me, pl.ds(dst, rows), pl.ds(dst_j, count)],
                send_sem=send_sem.at[chunk],
                recv_sem=recv_sem.at[chunk],
                device_id=device(to_r, to_c),
                device_id_type=MESH,
            ).start()

        pl.when(there & edge)(lambda: copy(win_j - 1, tile_j * to_c - 1 + skip, skip))
        pl.when(there & jnp.logical_not(edge))(lambda: copy(win_j, tile_j * to_c - 1, 0))

    chips = n_rows // 2
    ahead_r, ahead_c = AHEAD

    def step(t, table):
        value = jnp.int32(table[-1])
        for k, entry in enumerate(table[:-1]):
            value = jnp.where(t == k, entry, value)
        return value

    def turn_to(t):
        dx = step(t, CHIPS_ALONG)
        return lax.rem(r // 2 + dx, chips), dx

    def send_chip(chunk, t, rest, where=None):
        x, dx = turn_to(t)
        way = 1 - 2 * lax.rem(par + t, 2)
        for other, dy in CHIP_ORDER:
            to_r = 2 * x + (1 - par if other else par)
            to_c = lax.rem(c + way * dy + n_cols, n_cols)
            there = True
            if not other and dy == 0:
                there = dx > 0
            if rest:
                there = there & jnp.logical_not((to_r == ahead_r) & (to_c == ahead_c))
            if where is not None:
                there = there & where(to_c)
            send_tile(chunk, to_r, to_c, there)

    def send_ahead(chunk):
        send_tile(chunk, jnp.int32(ahead_r), jnp.int32(ahead_c), (r != ahead_r) | (c != ahead_c))

    def send_chunk(chunk):

        def first_column(t, carry):
            x, _ = turn_to(t)
            for other in range(2):
                to_r = 2 * x + (1 - par if other else par)
                there = ((to_r != r) | (c != 0)) & (to_r != ahead_r)
                send_tile(chunk, to_r, jnp.int32(0), there)
            return carry

        where = None
        if chunk in COLUMN_FIRST:
            lax.fori_loop(0, chips, first_column, 0)
            where = lambda to_c: to_c > 0

        def body(t, carry):
            send_chip(chunk, t, True, where)
            return carry

        lax.fori_loop(0, chips, body, 0)

    params[0].wait()
    for dw in range(3):
        w1own[dw] = jnp.concatenate([w1s[1, dw], w1s[0, dw]], axis=1)
    w1own[3] = jnp.concatenate([w1s[2, 0], w1s[2, 1]], axis=1)
    w1own[4] = jnp.concatenate([w1s[2, 2], jnp.zeros_like(w1s[2, 2])], axis=1)
    w1all[r // 2, par, c] = w1own[...]

    for copy in loads[0]:
        copy.wait()
    pack_rows(turn_to(0)[0], *groups[0][0])
    pl.semaphore_wait(barrier, sources - 1)

    def send_weights():
        for kr in range(0, n_rows, 2):
            for kc in range(n_cols):
                if kr or kc:
                    pltpu.make_async_remote_copy(
                        src_ref=w1own,
                        dst_ref=w1all.at[r // 2, par, c],
                        send_sem=wsend_sem,
                        recv_sem=wrecv_sem,
                        device_id=device(to_rs[kr], to_cs[kc]),
                        device_id_type=MESH,
                    ).start()

    def pack_and_send(t, carry):
        pl.when(t < chips - 1)(lambda: pack_rows(turn_to(t + 1)[0], *groups[0][0]))
        send_chip(0, t, False)
        pl.when(t == 0)(send_weights)
        return carry

    lax.fori_loop(0, chips, pack_and_send, 0)

    pack(1)
    send_ahead(1)
    send_chunk(1)
    pack(2)
    send_ahead(2)
    send_ahead(3)
    send_chunk(2)
    send_chunk(3)

    def wait_bytes(ref, sem):
        pltpu.make_async_copy(ref, ref, sem).wait()

    w1_bytes = recv.at[0 : sources // 2 - 1, 0, 0:5]
    wait_bytes(w1_bytes, wrecv_sem)
    wait_bytes(w1_bytes, wsend_sem)
    partner = device(r + 1 - 2 * par, c)
    w_swap = pltpu.make_async_remote_copy(
        src_ref=w1all.at[:, par],
        dst_ref=w1all.at[:, par],
        send_sem=wswap_send_sem,
        recv_sem=wswap_recv_sem,
        device_id=partner,
        device_id_type=MESH,
    )
    w_swap.start()

    def own_rows(chunk):
        rows, where, _ = chunks[chunk]
        src, dst = where(r)

        def copy(count, src_j, dst_j):
            for h in range(rows):
                recv[me, dst + h, pl.ds(dst_j, count)] = packed[src + h, pl.ds(src_j, count)]

        pl.when(at_edge)(lambda: copy(win_j - 1, tile_j * c - 1 + own_j, own_j))
        pl.when(jnp.logical_not(at_edge))(lambda: copy(win_j, tile_j * c - 1, 0))

    for chunk in range(3):
        own_rows(chunk)
    pl.when(jnp.logical_not(no_outer))(lambda: own_rows(3))

    zero_row = jnp.zeros((win_j, 2, 2 * images), BF16)
    zero_col = jnp.zeros((tile_h + 2, 2, 2 * images), BF16)

    def clear(s, carry):
        recv[s, last * (1 - par)] = zero_row
        return carry

    def clear_outer(s, carry):
        recv[s, (last - 1) * par] = zero_row
        recv[s, (last - 1) * par + 1] = zero_row
        return carry

    def clear_edge(s, carry):
        recv[s, pl.ds(3 * par, tile_h + 2), (win_j - 1) * (1 - own_j)] = zero_col
        return carry

    lax.fori_loop(0, sources, clear, 0)
    pl.when(no_outer)(lambda: (lax.fori_loop(0, sources, clear_outer, 0), None)[1])
    pl.when(at_edge)(lambda: (lax.fori_loop(0, sources, clear_edge, 0), None)[1])

    low = lax.broadcasted_iota(jnp.int32, (chans, 2 * chans), 1) < chans

    def spread(wt, u, v, dw):
        ur, vr = pltpu.roll(u, chans, 1), pltpu.roll(v, chans, 1)
        zero = jnp.zeros_like(u)
        tiles = (jnp.where(low, ur, zero), u, jnp.where(low, v, ur), jnp.where(low, zero, vr))
        for k, tile in enumerate(tiles):
            tile = tile.astype(BF16)
            for b in range(2):
                wt[dw + b, k * chans : (k + 1) * chans, b * 2 * chans : (b + 1) * 2 * chans] = tile

    def blank(wt):
        zero = jnp.zeros((4 * chans, 2 * chans), BF16)
        wt[3, :, 0 : 2 * chans] = zero
        wt[0, :, 2 * chans : 4 * chans] = zero

    for copy in params[1:]:
        copy.wait()
    blank(wt1)
    blank(wt2)
    for dw in range(3):
        w = [w2s[dh, dw].astype(F32) for dh in range(3)]
        spread(
            wt2,
            jnp.concatenate([w[1], w[0]], axis=1),
            jnp.concatenate([w[2], jnp.zeros_like(w[2])], axis=1),
            dw,
        )
    bias1[...] = jnp.concatenate([b1s[...]] * 4, axis=1)
    bias2[...] = jnp.concatenate([b2s[...]] * 4, axis=1)

    def arrived(chunk):
        def wait(count):
            wait_bytes(recv.at[0 : sources - 1, 0 : chunks[chunk][0], 0:count], recv_sem.at[chunk])

        pl.when(at_edge)(lambda: wait(win_j - 1))
        pl.when(jnp.logical_not(at_edge))(lambda: wait(win_j))

    arrived(0)
    give = tile_h - (tile_h - 3) * par
    land = tile_h + 2 - (tile_h + 1) * (1 - par)
    swap = pltpu.make_async_remote_copy(
        src_ref=recv.at[:, pl.ds(give, 2)],
        dst_ref=recv.at[:, pl.ds(land, 2)],
        send_sem=swap_send_sem,
        recv_sem=swap_recv_sem,
        device_id=partner,
        device_id_type=MESH,
    )
    swap.start()

    w_swap.wait()
    u = [w1all[:, :, :, k].reshape(chans, 2 * chans).astype(F32) for k in range(5)]
    for dw in range(3):
        v = (u[3], pltpu.roll(u[3], chans, 1), u[4])[dw]
        spread(wt1, u[dw], jnp.where(low, v, 0.0), dw)

    x_pairs, z_pairs = xmat.shape[0], ymat.shape[0]
    o_pairs = z_pairs - 1

    def nth(n, count):
        return (count - 1) * (1 - par) + n * (2 * par - 1)

    def turn_one(n, carry):
        i = nth(n, x_pairs)

        def put(j, value):
            xmat[i, j] = value

        turn(recv, i, put)
        return carry

    def first_one(n, carry):
        i = nth(n, z_pairs)
        blank_a = jnp.where(n == 0, 1 - par, 2)
        pairs = (xmat.at[i], xmat.at[i + 1])
        first(pairs, lambda dw: wt1[dw], bias1[...], ymat.at[i], blank_a, 0, win_j - 1)
        blank_edges(ymat.at[i])
        return carry

    def second_one(n, carry):
        i = nth(n, o_pairs)
        pairs = (ymat.at[i], ymat.at[i + 1])
        second(pairs, lambda dw: wt2[dw], bias2[...], out.at[pl.ds(2 * i, 2)], 0, tile_j)
        return carry

    def stage(s, carry):
        @pl.when(s == 0)
        def _():
            swap.wait()

        for k in range(1, 4):
            there = s == k
            if k == 3:
                there = there & jnp.logical_not(no_outer)
            pl.when(there)(lambda k=k: arrived(k))

        for ends, one in ((TURNS, turn_one), (FIRSTS, first_one), (SECONDS, second_one)):
            lax.fori_loop(step(s, (0, *ends[:-1])), step(s, ends), one, 0)
        return carry

    lax.fori_loop(0, 4, stage, 0)

    per_edge = n_rows * 2
    for chunk in range(4):
        rows = chunks[chunk][0]
        n_r = n_rows - 2 if chunk == 3 else n_rows
        counts = (n_r * 2, n_r * (n_cols - 2))

        def drain(edge_n, inner_n, rows=rows, chunk=chunk):
            wait_bytes(recv.at[0:edge_n, 0:rows, 0 : win_j - 1], send_sem.at[chunk])
            wait_bytes(recv.at[0:inner_n, 0:rows, 0:win_j], send_sem.at[chunk])

        def drain_own(chunk=chunk, counts=counts, drain=drain):
            pl.when(at_edge)(lambda: drain(counts[0] - 1, counts[1]))
            pl.when(jnp.logical_not(at_edge))(lambda: drain(counts[0], counts[1] - 1))

        if chunk == 3:
            pl.when(no_outer)(lambda: drain(*counts))
            pl.when(jnp.logical_not(no_outer))(drain_own)
        else:
            drain_own()


def tail_kernel(tile, xmat, ymat, wt1, wt2, bias1, bias2, out_hbm, y_new, o_new, sem):
    r = lax.axis_index("model")
    par = lax.rem(r, 2)
    rows = out_hbm.shape[0]
    x_pairs, z_pairs = xmat.shape[0], ymat.shape[0]
    late = (rows - 2) * par
    here = 2 * (1 - par)

    def start(k, carry):
        pltpu.make_async_copy(tile.at[par + k], out_hbm.at[k], sem.at[0]).start()
        return carry

    lax.fori_loop(here, here + rows - 2, start, 0)
    i = (x_pairs - 2) * par
    blank_a = jnp.where(r == 0, 0, jnp.where(r == lax.axis_size("model") - 1, 1, 2))
    half = y_new.shape[0] // 2

    def first_half(h, carry):
        first((xmat.at[i], xmat.at[i + 1]), lambda dw: wt1[dw], bias1[...], y_new, blank_a, half * h, half)
        return carry

    lax.fori_loop(0, 2, first_half, 0)
    blank_edges(y_new)
    depth = wt2.shape[1] // 2

    def weights(dw):
        new, old = wt2[dw, pl.ds(depth * par, depth)], wt2[dw, pl.ds(depth * (1 - par), depth)]
        return jnp.concatenate([new, old], axis=0)

    old = ymat.at[1 + (z_pairs - 3) * par]
    count = o_new.shape[1]
    step = count - half

    def part(lo, hi, k):
        return pltpu.make_async_copy(o_new.at[:, lo:hi], out_hbm.at[pl.ds(late, 2), lo:hi], sem.at[k])

    def second_half(h, carry):
        second((y_new, old), weights, bias2[...], o_new, step * h, half)
        pl.when(h == 0)(lambda: part(0, step, 1).start())
        return carry

    lax.fori_loop(0, 2, second_half, 0)
    part(step, count, 2).start()
    pltpu.make_async_copy(tile.at[0 : rows - 2], out_hbm.at[0 : rows - 2], sem.at[0]).wait()
    part(0, step, 1).wait()
    part(step, count, 2).wait()


def solution(mesh):
    n_rows = mesh.shape["model"]
    n_cols = mesh.shape["cols"]

    def run_local(x_in, w_conv1, b_conv1, w_conv2, b_conv2):
        images, height, width, own_chans = x_in.shape
        sources = n_rows * n_cols
        chans = own_chans * sources
        pairs = width // 2
        tile_h, tile_j = height // n_rows, pairs // n_cols
        win_j = tile_j + 2
        x_pairs, z_pairs = (tile_h + 5) // 2, (tile_h + 3) // 2
        x_t = jnp.transpose(x_in, (1, 2, 3, 0)).reshape(n_rows // 2, 2 * tile_h, pairs, 2, own_chans, images)
        args = (x_t, w_conv1, b_conv1.reshape(1, chans), w_conv2, b_conv2.reshape(1, chans))
        hbm = pl.BlockSpec(memory_space=pltpu.HBM)
        vmem = pl.BlockSpec(memory_space=pltpu.VMEM)
        kept = (
            pltpu.VMEM((2 * (z_pairs - 1), tile_j, 2, images, chans), F32),
            pltpu.VMEM((x_pairs, win_j, 2, images, 2 * chans), BF16),
            pltpu.VMEM((z_pairs, win_j - 1, 2, images, 2 * chans), BF16),
            pltpu.VMEM((4, 4 * chans, 4 * chans), BF16),
            pltpu.VMEM((4, 4 * chans, 4 * chans), BF16),
            pltpu.VMEM((1, 4 * chans), F32),
            pltpu.VMEM((1, 4 * chans), F32),
        )
        state = pl.pallas_call(
            functools.partial(conv_kernel, n_rows, n_cols),
            out_shape=kept,
            in_specs=[hbm] * 5,
            out_specs=[vmem] * len(kept),
            scratch_shapes=[
                pltpu.VMEM((sources, 2 * x_pairs, win_j, own_chans, 2 * images), BF16),
                pltpu.VMEM((n_rows // 2, 2 * tile_h, pairs, 2, own_chans, images), BF16),
                pltpu.VMEM((height, pairs, own_chans, 2 * images), BF16),
                pltpu.VMEM((3, 3, own_chans, chans), BF16),
                pltpu.VMEM((5, own_chans, 2 * chans), BF16),
                pltpu.VMEM((n_rows // 2, 2, n_cols, 5, own_chans, 2 * chans), BF16),
                pltpu.VMEM((3, 3, chans, chans), BF16),
                pltpu.VMEM((1, chans), F32),
                pltpu.VMEM((1, chans), F32),
                pltpu.SemaphoreType.DMA((3, 2)),
                pltpu.SemaphoreType.DMA((4,)),
                pltpu.SemaphoreType.DMA((4,)),
                pltpu.SemaphoreType.DMA((4,)),
            ]
            + [pltpu.SemaphoreType.DMA] * 6,
            compiler_params=pltpu.CompilerParams(
                collective_id=0, has_side_effects=True, vmem_limit_bytes=24 << 20
            ),
            name="conv",
        )(*(pltpu.with_memory_space_constraint(a, pltpu.HBM) for a in args))
        out = pl.pallas_call(
            tail_kernel,
            out_shape=jax.ShapeDtypeStruct((tile_h, tile_j, 2, images, chans), F32),
            in_specs=[vmem] * len(kept),
            out_specs=pl.BlockSpec(memory_space=pl.ANY),
            scratch_shapes=[
                pltpu.VMEM((win_j - 1, 2, images, 2 * chans), BF16),
                pltpu.VMEM((2, tile_j, 2, images, chans), F32),
                pltpu.SemaphoreType.DMA((3,)),
            ],
            compiler_params=pltpu.CompilerParams(vmem_limit_bytes=8 << 20),
            name="tail",
        )(*state)
        out = out.reshape(tile_h, 2 * tile_j, images, chans)
        return jnp.transpose(out, (2, 0, 1, 3))

    group = ("model", "cols")
    return jax.shard_map(
        run_local,
        mesh=mesh,
        in_specs=(P("data", None, None, group), P(None, None, group, None), P(), P(), P()),
        out_specs=P("data", "model", "cols", None),
        check_vma=False,
    )
```

```python
import functools

import jax
import jax.numpy as jnp
from jax import lax
from jax.experimental import pallas as pl
from jax.experimental.pallas import tpu as pltpu
from jax.sharding import PartitionSpec as P

MESH = pl.DeviceIdType.MESH
BF16 = jnp.bfloat16
F32 = jnp.float32
CHUNK_ROWS = (2, 3, 2)
TURNS, FIRSTS, SECONDS = (2, 4, 5, 6), (1, 3, 4, 5), (0, 2, 3, 3)
AHEAD = (1, 0)
COLUMN_FIRST = (2, 3)
CHIPS_ALONG = (3, 1, 2, 0)
CHIP_ORDER = tuple((other, dy) for other in (0, 1) for dy in (0, 1, -1, 2))


def turn(recv, i, put):
    sources, _, win_j, own_chans, lanes = recv.shape
    chans = sources * own_chans
    for j in range(win_j):
        top = recv[:, 2 * i, j].reshape(chans, lanes)
        under = recv[:, 2 * i + 1, j].reshape(chans, lanes)
        put(j, jnp.concatenate([top, under], axis=0).T.reshape(2, lanes // 2, 2 * chans))


def blocks(pairs, weights, count):
    acc = None
    for dw in range(4):
        parts = [view[dw // 2 : dw // 2 + count, dw % 2] for view in pairs]
        lhs = jnp.concatenate([p.reshape(count * p.shape[1], p.shape[2]) for p in parts], axis=1)
        term = jnp.dot(lhs, weights(dw), preferred_element_type=F32)
        acc = term if acc is None else acc + term
    return acc


def first(pairs, weights, bias, y_row, blank_a):
    count, _, images, lanes = y_row.shape
    c = lax.axis_index("cols")
    row = lax.rem(lax.broadcasted_iota(jnp.int32, (1, 2 * lanes), 1), lanes) // (lanes // 2)
    act = jnp.maximum(blocks(pairs, weights, count) + bias, 0.0)
    act = jnp.where(row != blank_a, act, 0.0).astype(BF16)
    for b in range(2):
        y_row[:, b] = act[:, b * lanes : (b + 1) * lanes].reshape(count, images, lanes)
    blank = jnp.zeros((images, lanes), BF16)

    @pl.when(c == 0)
    def _():
        y_row[0, 0] = blank

    @pl.when(c == lax.axis_size("cols") - 1)
    def _():
        y_row[count - 1, 1] = blank


def second(pairs, weights, bias, out_pair):
    _, count, _, images, chans = out_pair.shape
    res = blocks(pairs, weights, count) + bias
    for b in range(2):
        for a in range(2):
            at = (2 * b + a) * chans
            out_pair[a, :, b] = res[:, at : at + chans].reshape(count, images, chans)


def conv_kernel(
    n_rows,
    n_cols,
    x_hbm,
    w1_hbm,
    b1_hbm,
    w2_hbm,
    b2_hbm,
    out,
    ymat,
    wt2,
    bias2,
    recv,
    xmat,
    wt1,
    bias1,
    xs,
    packed,
    w1s,
    w1own,
    w1all,
    w2s,
    b1s,
    b2s,
    load_sem,
    par_sem,
    send_sem,
    recv_sem,
    wsend_sem,
    wrecv_sem,
    swap_send_sem,
    swap_recv_sem,
    wswap_send_sem,
    wswap_recv_sem,
):
    chip_h, pairs = xs.shape[1:3]
    images = xs.shape[-1]
    tile_h, tile_j = chip_h // 2, pairs // n_cols
    win_j = tile_j + 2
    sources = n_rows * n_cols
    r, c = lax.axis_index("model"), lax.axis_index("cols")
    par = lax.rem(r, 2)
    me = r * n_cols + c
    chans = recv.shape[0] * 2

    tops = [tile_h - sum(CHUNK_ROWS[: k + 1]) for k in range(len(CHUNK_ROWS))]
    groups = (
        ((tops[0], chip_h - tops[0]),),
        *(((k, k + n), (chip_h - k - n, chip_h - k)) for k, n in zip(tops[1:], CHUNK_ROWS[1:])),
    )
    loads = []
    for g, spans in enumerate(groups):
        loads.append(
            [
                pltpu.make_async_copy(x_hbm.at[:, lo:hi], xs.at[:, lo:hi], load_sem.at[g, n])
                for n, (lo, hi) in enumerate(spans)
            ]
        )
    for copies in loads:
        for copy in copies:
            copy.start()
    params = [
        pltpu.make_async_copy(src, dst, par_sem.at[s])
        for s, (src, dst) in enumerate(((w1_hbm, w1s), (w2_hbm, w2s), (b1_hbm, b1s), (b2_hbm, b2s)))
    ]
    for copy in params:
        copy.start()

    barrier = pltpu.get_barrier_semaphore()
    to_cs = [lax.rem(c + k, n_cols) for k in range(n_cols)]

    def device(to_r, to_c):
        return {"model": to_r, "cols": to_c}

    to_rs = [lax.rem(r + k, n_rows) for k in range(n_rows)]
    for kr, kc in sorted(
        ((kr, kc) for kr in range(n_rows) for kc in range(n_cols) if kr or kc),
        key=lambda k: (k[1] not in (1, 2), k[0] not in (2, 3, 4, 5), k[1] == 2, k[0] < 4, -min(k[0], n_rows - k[0])),
    ):
        pl.semaphore_signal(barrier, inc=1, device_id=device(to_rs[kr], to_cs[kc]), device_id_type=MESH)

    def pack_rows(x, lo, hi):
        rows = hi - lo
        left, right = (xs[x, lo:hi, :, p].reshape(rows * pairs * 2, images) for p in range(2))
        both = jnp.concatenate([left, right], axis=1)
        packed[pl.ds(chip_h * x + lo, rows)] = both.reshape(rows, pairs, 2, 2 * images)

    def pack(g):
        for copy in loads[g]:
            copy.wait()

        def body(x, carry):
            for lo, hi in groups[g]:
                pack_rows(x, lo, hi)
            return carry

        lax.fori_loop(0, n_rows // 2, body, 0)

    last = tile_h + 4

    def rows_of(offset, count):
        def where(to_r):
            q = lax.rem(to_r, 2)
            src = tile_h * to_r + offset + (tile_h - count - 2 * offset) * q
            dst = offset + 2 + (last - count - 2 * offset - 3) * q
            return src, dst

        return where

    chunks = (
        *((n, rows_of(k, n), False) for k, n in zip(tops, CHUNK_ROWS)),
        (2, rows_of(-2, 2), True),
    )
    no_outer = (r == 0) | (r == n_rows - 1)
    at_edge = (c == 0) | (c == n_cols - 1)
    own_j = c == 0
    own_j = own_j.astype(jnp.int32)

    def send_tile(chunk, to_r, to_c, there):
        rows, where, is_outer = chunks[chunk]
        src, dst = where(to_r)
        skip = (to_c == 0).astype(jnp.int32)
        edge = (to_c == 0) | (to_c == n_cols - 1)
        if is_outer:
            there = there & (to_r > 0) & (to_r < n_rows - 1)

        def copy(count, src_j, dst_j):
            pltpu.make_async_remote_copy(
                src_ref=packed.at[pl.ds(src, rows), pl.ds(src_j, count)],
                dst_ref=recv.at[me, pl.ds(dst, rows), pl.ds(dst_j, count)],
                send_sem=send_sem.at[chunk],
                recv_sem=recv_sem.at[chunk],
                device_id=device(to_r, to_c),
                device_id_type=MESH,
            ).start()

        pl.when(there & edge)(lambda: copy(win_j - 1, tile_j * to_c - 1 + skip, skip))
        pl.when(there & jnp.logical_not(edge))(lambda: copy(win_j, tile_j * to_c - 1, 0))

    chips = n_rows // 2
    ahead_r, ahead_c = AHEAD

    def step(t, table):
        value = jnp.int32(table[-1])
        for k, entry in enumerate(table[:-1]):
            value = jnp.where(t == k, entry, value)
        return value

    def turn_to(t):
        dx = step(t, CHIPS_ALONG)
        return lax.rem(r // 2 + dx, chips), dx

    def send_chip(chunk, t, rest, where=None):
        x, dx = turn_to(t)
        way = 1 - 2 * lax.rem(par + t, 2)
        for other, dy in CHIP_ORDER:
            to_r = 2 * x + (1 - par if other else par)
            to_c = lax.rem(c + way * dy + n_cols, n_cols)
            there = True
            if not other and dy == 0:
                there = dx > 0
            if rest:
                there = there & jnp.logical_not((to_r == ahead_r) & (to_c == ahead_c))
            if where is not None:
                there = there & where(to_c)
            send_tile(chunk, to_r, to_c, there)

    def send_ahead(chunk):
        send_tile(chunk, jnp.int32(ahead_r), jnp.int32(ahead_c), (r != ahead_r) | (c != ahead_c))

    def send_chunk(chunk):

        def first_column(t, carry):
            x, _ = turn_to(t)
            for other in range(2):
                to_r = 2 * x + (1 - par if other else par)
                there = ((to_r != r) | (c != 0)) & (to_r != ahead_r)
                send_tile(chunk, to_r, jnp.int32(0), there)
            return carry

        where = None
        if chunk in COLUMN_FIRST:
            lax.fori_loop(0, chips, first_column, 0)
            where = lambda to_c: to_c > 0

        def body(t, carry):
            send_chip(chunk, t, True, where)
            return carry

        lax.fori_loop(0, chips, body, 0)

    params[0].wait()
    for dw in range(3):
        w1own[dw] = jnp.concatenate([w1s[1, dw], w1s[0, dw]], axis=1)
    w1own[3] = jnp.concatenate([w1s[2, 0], w1s[2, 1]], axis=1)
    w1own[4] = jnp.concatenate([w1s[2, 2], jnp.zeros_like(w1s[2, 2])], axis=1)
    w1all[r // 2, par, c] = w1own[...]

    for copy in loads[0]:
        copy.wait()
    pack_rows(turn_to(0)[0], *groups[0][0])
    pl.semaphore_wait(barrier, sources - 1)

    def send_weights():
        for kr in range(0, n_rows, 2):
            for kc in range(n_cols):
                if kr or kc:
                    pltpu.make_async_remote_copy(
                        src_ref=w1own,
                        dst_ref=w1all.at[r // 2, par, c],
                        send_sem=wsend_sem,
                        recv_sem=wrecv_sem,
                        device_id=device(to_rs[kr], to_cs[kc]),
                        device_id_type=MESH,
                    ).start()

    def pack_and_send(t, carry):
        pl.when(t < chips - 1)(lambda: pack_rows(turn_to(t + 1)[0], *groups[0][0]))
        send_chip(0, t, False)
        pl.when(t == 0)(send_weights)
        return carry

    lax.fori_loop(0, chips, pack_and_send, 0)

    pack(1)
    send_ahead(1)
    send_chunk(1)
    pack(2)
    send_ahead(2)
    send_ahead(3)
    send_chunk(2)
    send_chunk(3)

    def wait_bytes(ref, sem):
        pltpu.make_async_copy(ref, ref, sem).wait()

    w1_bytes = recv.at[0 : sources // 2 - 1, 0, 0:5]
    wait_bytes(w1_bytes, wrecv_sem)
    wait_bytes(w1_bytes, wsend_sem)
    partner = device(r + 1 - 2 * par, c)
    w_swap = pltpu.make_async_remote_copy(
        src_ref=w1all.at[:, par],
        dst_ref=w1all.at[:, par],
        send_sem=wswap_send_sem,
        recv_sem=wswap_recv_sem,
        device_id=partner,
        device_id_type=MESH,
    )
    w_swap.start()

    def own_rows(chunk):
        rows, where, _ = chunks[chunk]
        src, dst = where(r)

        def copy(count, src_j, dst_j):
            for h in range(rows):
                recv[me, dst + h, pl.ds(dst_j, count)] = packed[src + h, pl.ds(src_j, count)]

        pl.when(at_edge)(lambda: copy(win_j - 1, tile_j * c - 1 + own_j, own_j))
        pl.when(jnp.logical_not(at_edge))(lambda: copy(win_j, tile_j * c - 1, 0))

    for chunk in range(3):
        own_rows(chunk)
    pl.when(jnp.logical_not(no_outer))(lambda: own_rows(3))

    zero_row = jnp.zeros((win_j, 2, 2 * images), BF16)
    zero_col = jnp.zeros((tile_h + 2, 2, 2 * images), BF16)

    def clear(s, carry):
        recv[s, last * (1 - par)] = zero_row
        return carry

    def clear_outer(s, carry):
        recv[s, (last - 1) * par] = zero_row
        recv[s, (last - 1) * par + 1] = zero_row
        return carry

    def clear_edge(s, carry):
        recv[s, pl.ds(3 * par, tile_h + 2), (win_j - 1) * (1 - own_j)] = zero_col
        return carry

    lax.fori_loop(0, sources, clear, 0)
    pl.when(no_outer)(lambda: (lax.fori_loop(0, sources, clear_outer, 0), None)[1])
    pl.when(at_edge)(lambda: (lax.fori_loop(0, sources, clear_edge, 0), None)[1])

    low = lax.broadcasted_iota(jnp.int32, (chans, 2 * chans), 1) < chans

    def spread(wt, u, v, dw):
        ur, vr = pltpu.roll(u, chans, 1), pltpu.roll(v, chans, 1)
        zero = jnp.zeros_like(u)
        tiles = (jnp.where(low, ur, zero), u, jnp.where(low, v, ur), jnp.where(low, zero, vr))
        for k, tile in enumerate(tiles):
            tile = tile.astype(BF16)
            for b in range(2):
                wt[dw + b, k * chans : (k + 1) * chans, b * 2 * chans : (b + 1) * 2 * chans] = tile

    def blank(wt):
        zero = jnp.zeros((4 * chans, 2 * chans), BF16)
        wt[3, :, 0 : 2 * chans] = zero
        wt[0, :, 2 * chans : 4 * chans] = zero

    for copy in params[1:]:
        copy.wait()
    blank(wt1)
    blank(wt2)
    for dw in range(3):
        w = [w2s[dh, dw].astype(F32) for dh in range(3)]
        spread(
            wt2,
            jnp.concatenate([w[1], w[0]], axis=1),
            jnp.concatenate([w[2], jnp.zeros_like(w[2])], axis=1),
            dw,
        )
    bias1[...] = jnp.concatenate([b1s[...]] * 4, axis=1)
    bias2[...] = jnp.concatenate([b2s[...]] * 4, axis=1)

    def arrived(chunk):
        def wait(count):
            wait_bytes(recv.at[0 : sources - 1, 0 : chunks[chunk][0], 0:count], recv_sem.at[chunk])

        pl.when(at_edge)(lambda: wait(win_j - 1))
        pl.when(jnp.logical_not(at_edge))(lambda: wait(win_j))

    arrived(0)
    give = tile_h - (tile_h - 3) * par
    land = tile_h + 2 - (tile_h + 1) * (1 - par)
    swap = pltpu.make_async_remote_copy(
        src_ref=recv.at[:, pl.ds(give, 2)],
        dst_ref=recv.at[:, pl.ds(land, 2)],
        send_sem=swap_send_sem,
        recv_sem=swap_recv_sem,
        device_id=partner,
        device_id_type=MESH,
    )
    swap.start()

    w_swap.wait()
    u = [w1all[:, :, :, k].reshape(chans, 2 * chans).astype(F32) for k in range(5)]
    for dw in range(3):
        v = (u[3], pltpu.roll(u[3], chans, 1), u[4])[dw]
        spread(wt1, u[dw], jnp.where(low, v, 0.0), dw)

    x_pairs, z_pairs = xmat.shape[0], ymat.shape[0]
    o_pairs = z_pairs - 1

    def nth(n, count):
        return (count - 1) * (1 - par) + n * (2 * par - 1)

    def turn_one(n, carry):
        i = nth(n, x_pairs)

        def put(j, value):
            xmat[i, j] = value

        turn(recv, i, put)
        return carry

    def first_one(n, carry):
        i = nth(n, z_pairs)
        fill = jnp.where(n == 0, 1 - par, 2)
        out_of = jnp.where(n == z_pairs - 1, jnp.where(r == 0, 0, jnp.where(r == n_rows - 1, 1, 2)), 2)
        blank_a = jnp.where(fill < 2, fill, out_of)
        first((xmat.at[i], xmat.at[i + 1]), lambda dw: wt1[dw], bias1[...], ymat.at[i], blank_a)
        return carry

    def second_one(n, carry):
        i = nth(n, o_pairs)
        second((ymat.at[i], ymat.at[i + 1]), lambda dw: wt2[dw], bias2[...], out.at[pl.ds(2 * i, 2)])
        return carry

    def stage(s, carry):
        @pl.when(s == 0)
        def _():
            swap.wait()

        for k in range(1, 4):
            there = s == k
            if k == 3:
                there = there & jnp.logical_not(no_outer)
            pl.when(there)(lambda k=k: arrived(k))

        for ends, one in ((TURNS, turn_one), (FIRSTS, first_one), (SECONDS, second_one)):
            lax.fori_loop(step(s, (0, *ends[:-1])), step(s, ends), one, 0)
        return carry

    lax.fori_loop(0, 4, stage, 0)

    per_edge = n_rows * 2
    for chunk in range(4):
        rows = chunks[chunk][0]
        n_r = n_rows - 2 if chunk == 3 else n_rows
        counts = (n_r * 2, n_r * (n_cols - 2))

        def drain(edge_n, inner_n, rows=rows, chunk=chunk):
            wait_bytes(recv.at[0:edge_n, 0:rows, 0 : win_j - 1], send_sem.at[chunk])
            wait_bytes(recv.at[0:inner_n, 0:rows, 0:win_j], send_sem.at[chunk])

        def drain_own(chunk=chunk, counts=counts, drain=drain):
            pl.when(at_edge)(lambda: drain(counts[0] - 1, counts[1]))
            pl.when(jnp.logical_not(at_edge))(lambda: drain(counts[0], counts[1] - 1))

        if chunk == 3:
            pl.when(no_outer)(lambda: drain(*counts))
            pl.when(jnp.logical_not(no_outer))(drain_own)
        else:
            drain_own()


def tail_kernel(tile, ymat, wt2, bias2, out_hbm, o_new, sem):
    par = lax.rem(lax.axis_index("model"), 2)
    rows = out_hbm.shape[0]
    o_pairs = ymat.shape[0] - 1
    late = (rows - 2) * par
    here = 2 * (1 - par)

    def start(k, carry):
        pltpu.make_async_copy(tile.at[par + k], out_hbm.at[k], sem.at[0]).start()
        return carry

    lax.fori_loop(here, here + rows - 2, start, 0)
    i = (o_pairs - 1) * par
    second((ymat.at[i], ymat.at[i + 1]), lambda dw: wt2[dw], bias2[...], o_new)
    last = pltpu.make_async_copy(o_new, out_hbm.at[pl.ds(late, 2)], sem.at[1])
    last.start()
    pltpu.make_async_copy(tile.at[0 : rows - 2], out_hbm.at[0 : rows - 2], sem.at[0]).wait()
    last.wait()


def solution(mesh):
    n_rows = mesh.shape["model"]
    n_cols = mesh.shape["cols"]

    def run_local(x_in, w_conv1, b_conv1, w_conv2, b_conv2):
        images, height, width, own_chans = x_in.shape
        sources = n_rows * n_cols
        chans = own_chans * sources
        pairs = width // 2
        tile_h, tile_j = height // n_rows, pairs // n_cols
        win_j = tile_j + 2
        x_pairs, z_pairs = (tile_h + 5) // 2, (tile_h + 3) // 2
        x_t = jnp.transpose(x_in, (1, 2, 3, 0)).reshape(n_rows // 2, 2 * tile_h, pairs, 2, own_chans, images)
        args = (x_t, w_conv1, b_conv1.reshape(1, chans), w_conv2, b_conv2.reshape(1, chans))
        hbm = pl.BlockSpec(memory_space=pltpu.HBM)
        vmem = pl.BlockSpec(memory_space=pltpu.VMEM)
        kept = (
            pltpu.VMEM((2 * (z_pairs - 1), tile_j, 2, images, chans), F32),
            pltpu.VMEM((z_pairs, win_j - 1, 2, images, 2 * chans), BF16),
            pltpu.VMEM((4, 4 * chans, 4 * chans), BF16),
            pltpu.VMEM((1, 4 * chans), F32),
        )
        state = pl.pallas_call(
            functools.partial(conv_kernel, n_rows, n_cols),
            out_shape=kept,
            in_specs=[hbm] * 5,
            out_specs=[vmem] * len(kept),
            scratch_shapes=[
                pltpu.VMEM((sources, 2 * x_pairs, win_j, own_chans, 2 * images), BF16),
                pltpu.VMEM((x_pairs, win_j, 2, images, 2 * chans), BF16),
                pltpu.VMEM((4, 4 * chans, 4 * chans), BF16),
                pltpu.VMEM((1, 4 * chans), F32),
                pltpu.VMEM((n_rows // 2, 2 * tile_h, pairs, 2, own_chans, images), BF16),
                pltpu.VMEM((height, pairs, own_chans, 2 * images), BF16),
                pltpu.VMEM((3, 3, own_chans, chans), BF16),
                pltpu.VMEM((5, own_chans, 2 * chans), BF16),
                pltpu.VMEM((n_rows // 2, 2, n_cols, 5, own_chans, 2 * chans), BF16),
                pltpu.VMEM((3, 3, chans, chans), BF16),
                pltpu.VMEM((1, chans), F32),
                pltpu.VMEM((1, chans), F32),
                pltpu.SemaphoreType.DMA((3, 2)),
                pltpu.SemaphoreType.DMA((4,)),
                pltpu.SemaphoreType.DMA((4,)),
                pltpu.SemaphoreType.DMA((4,)),
            ]
            + [pltpu.SemaphoreType.DMA] * 6,
            compiler_params=pltpu.CompilerParams(
                collective_id=0, has_side_effects=True, vmem_limit_bytes=24 << 20
            ),
            name="conv",
        )(*(pltpu.with_memory_space_constraint(a, pltpu.HBM) for a in args))
        out = pl.pallas_call(
            tail_kernel,
            out_shape=jax.ShapeDtypeStruct((tile_h, tile_j, 2, images, chans), F32),
            in_specs=[vmem] * len(kept),
            out_specs=pl.BlockSpec(memory_space=pl.ANY),
            scratch_shapes=[
                pltpu.VMEM((2, tile_j, 2, images, chans), F32),
                pltpu.SemaphoreType.DMA((2,)),
            ],
            compiler_params=pltpu.CompilerParams(vmem_limit_bytes=8 << 20),
            name="tail",
        )(*state)
        out = out.reshape(tile_h, 2 * tile_j, images, chans)
        return jnp.transpose(out, (2, 0, 1, 3))

    group = ("model", "cols")
    return jax.shard_map(
        run_local,
        mesh=mesh,
        in_specs=(P("data", None, None, group), P(None, None, group, None), P(), P(), P()),
        out_specs=P("data", "model", "cols", None),
        check_vma=False,
    )
```

```python
import functools

import jax
import jax.numpy as jnp
from jax import lax
from jax.experimental import pallas as pl
from jax.experimental.pallas import tpu as pltpu
from jax.sharding import PartitionSpec as P

MESH = pl.DeviceIdType.MESH
BF16 = jnp.bfloat16
F32 = jnp.float32
CHUNK_ROWS = (2, 3, 2)
TURNS, FIRSTS, SECONDS = (2, 4, 5, 6), (1, 3, 4, 5), (0, 2, 3, 3)
AHEAD = (1, 0)
COLUMN_FIRST = (2, 3)
CHIPS_ALONG = (3, 1, 2, 0)
CHIP_ORDER = tuple((other, dy) for other in (0, 1) for dy in (1, -1, 0, 2))


def turn(recv, i, put):
    sources, _, win_j, own_chans, lanes = recv.shape
    chans = sources * own_chans
    for j in range(win_j):
        top = recv[:, 2 * i, j].reshape(chans, lanes)
        under = recv[:, 2 * i + 1, j].reshape(chans, lanes)
        put(j, jnp.concatenate([top, under], axis=0).T.reshape(2, lanes // 2, 2 * chans))


def blocks(pairs, weights, count):
    acc = None
    for dw in range(4):
        parts = [view[dw // 2 : dw // 2 + count, dw % 2] for view in pairs]
        lhs = jnp.concatenate([p.reshape(count * p.shape[1], p.shape[2]) for p in parts], axis=1)
        term = jnp.dot(lhs, weights(dw), preferred_element_type=F32)
        acc = term if acc is None else acc + term
    return acc


def first(pairs, weights, bias, y_row, blank_a):
    count, _, images, lanes = y_row.shape
    c = lax.axis_index("cols")
    row = lax.rem(lax.broadcasted_iota(jnp.int32, (1, 2 * lanes), 1), lanes) // (lanes // 2)
    act = jnp.maximum(blocks(pairs, weights, count) + bias, 0.0)
    act = jnp.where(row != blank_a, act, 0.0).astype(BF16)
    for b in range(2):
        y_row[:, b] = act[:, b * lanes : (b + 1) * lanes].reshape(count, images, lanes)
    blank = jnp.zeros((images, lanes), BF16)

    @pl.when(c == 0)
    def _():
        y_row[0, 0] = blank

    @pl.when(c == lax.axis_size("cols") - 1)
    def _():
        y_row[count - 1, 1] = blank


def second(pairs, weights, bias, out_pair):
    _, count, _, images, chans = out_pair.shape
    res = blocks(pairs, weights, count) + bias
    for b in range(2):
        for a in range(2):
            at = (2 * b + a) * chans
            out_pair[a, :, b] = res[:, at : at + chans].reshape(count, images, chans)


def conv_kernel(
    n_rows,
    n_cols,
    x_hbm,
    w1_hbm,
    b1_hbm,
    w2_hbm,
    b2_hbm,
    out,
    ymat,
    wt2,
    bias2,
    recv,
    xmat,
    wt1,
    bias1,
    xs,
    packed,
    w1s,
    w1own,
    w1all,
    w2s,
    b1s,
    b2s,
    load_sem,
    par_sem,
    send_sem,
    recv_sem,
    wsend_sem,
    wrecv_sem,
    swap_send_sem,
    swap_recv_sem,
    wswap_send_sem,
    wswap_recv_sem,
):
    chip_h, pairs = xs.shape[1:3]
    images = xs.shape[-1]
    tile_h, tile_j = chip_h // 2, pairs // n_cols
    win_j = tile_j + 2
    sources = n_rows * n_cols
    r, c = lax.axis_index("model"), lax.axis_index("cols")
    par = lax.rem(r, 2)
    me = r * n_cols + c
    chans = recv.shape[0] * 2

    tops = [tile_h - sum(CHUNK_ROWS[: k + 1]) for k in range(len(CHUNK_ROWS))]
    groups = (
        ((tops[0], chip_h - tops[0]),),
        *(((k, k + n), (chip_h - k - n, chip_h - k)) for k, n in zip(tops[1:], CHUNK_ROWS[1:])),
    )
    loads = []
    for g, spans in enumerate(groups):
        loads.append(
            [
                pltpu.make_async_copy(x_hbm.at[:, lo:hi], xs.at[:, lo:hi], load_sem.at[g, n])
                for n, (lo, hi) in enumerate(spans)
            ]
        )
    for copies in loads:
        for copy in copies:
            copy.start()
    params = [
        pltpu.make_async_copy(src, dst, par_sem.at[s])
        for s, (src, dst) in enumerate(((w1_hbm, w1s), (w2_hbm, w2s), (b1_hbm, b1s), (b2_hbm, b2s)))
    ]
    for copy in params:
        copy.start()

    barrier = pltpu.get_barrier_semaphore()
    to_cs = [lax.rem(c + k, n_cols) for k in range(n_cols)]

    def device(to_r, to_c):
        return {"model": to_r, "cols": to_c}

    to_rs = [lax.rem(r + k, n_rows) for k in range(n_rows)]
    for kr, kc in sorted(
        ((kr, kc) for kr in range(n_rows) for kc in range(n_cols) if kr or kc),
        key=lambda k: (k[1] not in (1, 2), k[0] not in (2, 3, 4, 5), k[1] == 2, k[0] < 4, -min(k[0], n_rows - k[0])),
    ):
        pl.semaphore_signal(barrier, inc=1, device_id=device(to_rs[kr], to_cs[kc]), device_id_type=MESH)

    def pack_rows(x, lo, hi):
        rows = hi - lo
        left, right = (xs[x, lo:hi, :, p].reshape(rows * pairs * 2, images) for p in range(2))
        both = jnp.concatenate([left, right], axis=1)
        packed[pl.ds(chip_h * x + lo, rows)] = both.reshape(rows, pairs, 2, 2 * images)

    def pack(g):
        for copy in loads[g]:
            copy.wait()

        def body(x, carry):
            for lo, hi in groups[g]:
                pack_rows(x, lo, hi)
            return carry

        lax.fori_loop(0, n_rows // 2, body, 0)

    last = tile_h + 4

    def rows_of(offset, count):
        def where(to_r):
            q = lax.rem(to_r, 2)
            src = tile_h * to_r + offset + (tile_h - count - 2 * offset) * q
            dst = offset + 2 + (last - count - 2 * offset - 3) * q
            return src, dst

        return where

    chunks = (
        *((n, rows_of(k, n), False) for k, n in zip(tops, CHUNK_ROWS)),
        (2, rows_of(-2, 2), True),
    )
    no_outer = (r == 0) | (r == n_rows - 1)
    at_edge = (c == 0) | (c == n_cols - 1)
    own_j = c == 0
    own_j = own_j.astype(jnp.int32)

    def send_tile(chunk, to_r, to_c, there):
        rows, where, is_outer = chunks[chunk]
        src, dst = where(to_r)
        skip = (to_c == 0).astype(jnp.int32)
        edge = (to_c == 0) | (to_c == n_cols - 1)
        if is_outer:
            there = there & (to_r > 0) & (to_r < n_rows - 1)

        def copy(count, src_j, dst_j):
            pltpu.make_async_remote_copy(
                src_ref=packed.at[pl.ds(src, rows), pl.ds(src_j, count)],
                dst_ref=recv.at[me, pl.ds(dst, rows), pl.ds(dst_j, count)],
                send_sem=send_sem.at[chunk],
                recv_sem=recv_sem.at[chunk],
                device_id=device(to_r, to_c),
                device_id_type=MESH,
            ).start()

        pl.when(there & edge)(lambda: copy(win_j - 1, tile_j * to_c - 1 + skip, skip))
        pl.when(there & jnp.logical_not(edge))(lambda: copy(win_j, tile_j * to_c - 1, 0))

    chips = n_rows // 2
    ahead_r, ahead_c = AHEAD

    def step(t, table):
        value = jnp.int32(table[-1])
        for k, entry in enumerate(table[:-1]):
            value = jnp.where(t == k, entry, value)
        return value

    def turn_to(t):
        dx = step(t, CHIPS_ALONG)
        return lax.rem(r // 2 + dx, chips), dx

    def send_chip(chunk, t, rest, where=None):
        x, dx = turn_to(t)
        way = 1 - 2 * lax.rem(par + t, 2)
        for other, dy in CHIP_ORDER:
            to_r = 2 * x + (1 - par if other else par)
            to_c = lax.rem(c + way * dy + n_cols, n_cols)
            there = True
            if not other and dy == 0:
                there = dx > 0
            if rest:
                there = there & jnp.logical_not((to_r == ahead_r) & (to_c == ahead_c))
            if where is not None:
                there = there & where(to_c)
            send_tile(chunk, to_r, to_c, there)

    def send_ahead(chunk):
        send_tile(chunk, jnp.int32(ahead_r), jnp.int32(ahead_c), (r != ahead_r) | (c != ahead_c))

    def send_chunk(chunk):

        def first_column(t, carry):
            x, _ = turn_to(t)
            for other in range(2):
                to_r = 2 * x + (1 - par if other else par)
                there = ((to_r != r) | (c != 0)) & (to_r != ahead_r)
                send_tile(chunk, to_r, jnp.int32(0), there)
            return carry

        where = None
        if chunk in COLUMN_FIRST:
            lax.fori_loop(0, chips, first_column, 0)
            where = lambda to_c: to_c > 0

        def body(t, carry):
            send_chip(chunk, t, True, where)
            return carry

        lax.fori_loop(0, chips, body, 0)

    params[0].wait()
    for dw in range(3):
        w1own[dw] = jnp.concatenate([w1s[1, dw], w1s[0, dw]], axis=1)
    w1own[3] = jnp.concatenate([w1s[2, 0], w1s[2, 1]], axis=1)
    w1own[4] = jnp.concatenate([w1s[2, 2], jnp.zeros_like(w1s[2, 2])], axis=1)
    w1all[r // 2, par, c] = w1own[...]

    for copy in loads[0]:
        copy.wait()
    pack_rows(turn_to(0)[0], *groups[0][0])
    pl.semaphore_wait(barrier, sources - 1)

    def send_weights():
        for kr in range(0, n_rows, 2):
            for kc in range(n_cols):
                if kr or kc:
                    pltpu.make_async_remote_copy(
                        src_ref=w1own,
                        dst_ref=w1all.at[r // 2, par, c],
                        send_sem=wsend_sem,
                        recv_sem=wrecv_sem,
                        device_id=device(to_rs[kr], to_cs[kc]),
                        device_id_type=MESH,
                    ).start()

    def pack_and_send(t, carry):
        pl.when(t < chips - 1)(lambda: pack_rows(turn_to(t + 1)[0], *groups[0][0]))
        send_chip(0, t, False)
        pl.when(t == 0)(send_weights)
        return carry

    lax.fori_loop(0, chips, pack_and_send, 0)

    pack(1)
    send_ahead(1)
    send_chunk(1)
    pack(2)
    send_ahead(2)
    send_ahead(3)
    send_chunk(2)
    send_chunk(3)

    def wait_bytes(ref, sem):
        pltpu.make_async_copy(ref, ref, sem).wait()

    w1_bytes = recv.at[0 : sources // 2 - 1, 0, 0:5]
    wait_bytes(w1_bytes, wrecv_sem)
    wait_bytes(w1_bytes, wsend_sem)
    partner = device(r + 1 - 2 * par, c)
    w_swap = pltpu.make_async_remote_copy(
        src_ref=w1all.at[:, par],
        dst_ref=w1all.at[:, par],
        send_sem=wswap_send_sem,
        recv_sem=wswap_recv_sem,
        device_id=partner,
        device_id_type=MESH,
    )
    w_swap.start()

    def own_rows(chunk):
        rows, where, _ = chunks[chunk]
        src, dst = where(r)

        def copy(count, src_j, dst_j):
            for h in range(rows):
                recv[me, dst + h, pl.ds(dst_j, count)] = packed[src + h, pl.ds(src_j, count)]

        pl.when(at_edge)(lambda: copy(win_j - 1, tile_j * c - 1 + own_j, own_j))
        pl.when(jnp.logical_not(at_edge))(lambda: copy(win_j, tile_j * c - 1, 0))

    for chunk in range(3):
        own_rows(chunk)
    pl.when(jnp.logical_not(no_outer))(lambda: own_rows(3))

    zero_row = jnp.zeros((win_j, 2, 2 * images), BF16)
    zero_col = jnp.zeros((tile_h + 2, 2, 2 * images), BF16)

    def clear(s, carry):
        recv[s, last * (1 - par)] = zero_row
        return carry

    def clear_outer(s, carry):
        recv[s, (last - 1) * par] = zero_row
        recv[s, (last - 1) * par + 1] = zero_row
        return carry

    def clear_edge(s, carry):
        recv[s, pl.ds(3 * par, tile_h + 2), (win_j - 1) * (1 - own_j)] = zero_col
        return carry

    lax.fori_loop(0, sources, clear, 0)
    pl.when(no_outer)(lambda: (lax.fori_loop(0, sources, clear_outer, 0), None)[1])
    pl.when(at_edge)(lambda: (lax.fori_loop(0, sources, clear_edge, 0), None)[1])

    low = lax.broadcasted_iota(jnp.int32, (chans, 2 * chans), 1) < chans

    def spread(wt, u, v, dw):
        ur, vr = pltpu.roll(u, chans, 1), pltpu.roll(v, chans, 1)
        zero = jnp.zeros_like(u)
        tiles = (jnp.where(low, ur, zero), u, jnp.where(low, v, ur), jnp.where(low, zero, vr))
        for k, tile in enumerate(tiles):
            tile = tile.astype(BF16)
            for b in range(2):
                wt[dw + b, k * chans : (k + 1) * chans, b * 2 * chans : (b + 1) * 2 * chans] = tile

    def blank(wt):
        zero = jnp.zeros((4 * chans, 2 * chans), BF16)
        wt[3, :, 0 : 2 * chans] = zero
        wt[0, :, 2 * chans : 4 * chans] = zero

    for copy in params[1:]:
        copy.wait()
    blank(wt1)
    blank(wt2)
    for dw in range(3):
        w = [w2s[dh, dw].astype(F32) for dh in range(3)]
        spread(
            wt2,
            jnp.concatenate([w[1], w[0]], axis=1),
            jnp.concatenate([w[2], jnp.zeros_like(w[2])], axis=1),
            dw,
        )
    bias1[...] = jnp.concatenate([b1s[...]] * 4, axis=1)
    bias2[...] = jnp.concatenate([b2s[...]] * 4, axis=1)

    def arrived(chunk):
        def wait(count):
            wait_bytes(recv.at[0 : sources - 1, 0 : chunks[chunk][0], 0:count], recv_sem.at[chunk])

        pl.when(at_edge)(lambda: wait(win_j - 1))
        pl.when(jnp.logical_not(at_edge))(lambda: wait(win_j))

    arrived(0)
    give = tile_h - (tile_h - 3) * par
    land = tile_h + 2 - (tile_h + 1) * (1 - par)
    swap = pltpu.make_async_remote_copy(
        src_ref=recv.at[:, pl.ds(give, 2)],
        dst_ref=recv.at[:, pl.ds(land, 2)],
        send_sem=swap_send_sem,
        recv_sem=swap_recv_sem,
        device_id=partner,
        device_id_type=MESH,
    )
    swap.start()

    w_swap.wait()
    u = [w1all[:, :, :, k].reshape(chans, 2 * chans).astype(F32) for k in range(5)]
    for dw in range(3):
        v = (u[3], pltpu.roll(u[3], chans, 1), u[4])[dw]
        spread(wt1, u[dw], jnp.where(low, v, 0.0), dw)

    x_pairs, z_pairs = xmat.shape[0], ymat.shape[0]
    o_pairs = z_pairs - 1

    def nth(n, count):
        return (count - 1) * (1 - par) + n * (2 * par - 1)

    def turn_one(n, carry):
        i = nth(n, x_pairs)

        def put(j, value):
            xmat[i, j] = value

        turn(recv, i, put)
        return carry

    def first_one(n, carry):
        i = nth(n, z_pairs)
        fill = jnp.where(n == 0, 1 - par, 2)
        out_of = jnp.where(n == z_pairs - 1, jnp.where(r == 0, 0, jnp.where(r == n_rows - 1, 1, 2)), 2)
        blank_a = jnp.where(fill < 2, fill, out_of)
        first((xmat.at[i], xmat.at[i + 1]), lambda dw: wt1[dw], bias1[...], ymat.at[i], blank_a)
        return carry

    def second_one(n, carry):
        i = nth(n, o_pairs)
        second((ymat.at[i], ymat.at[i + 1]), lambda dw: wt2[dw], bias2[...], out.at[pl.ds(2 * i, 2)])
        return carry

    def stage(s, carry):
        @pl.when(s == 0)
        def _():
            swap.wait()

        for k in range(1, 4):
            there = s == k
            if k == 3:
                there = there & jnp.logical_not(no_outer)
            pl.when(there)(lambda k=k: arrived(k))

        for ends, one in ((TURNS, turn_one), (FIRSTS, first_one), (SECONDS, second_one)):
            lax.fori_loop(step(s, (0, *ends[:-1])), step(s, ends), one, 0)
        return carry

    lax.fori_loop(0, 4, stage, 0)

    per_edge = n_rows * 2
    for chunk in range(4):
        rows = chunks[chunk][0]
        n_r = n_rows - 2 if chunk == 3 else n_rows
        counts = (n_r * 2, n_r * (n_cols - 2))

        def drain(edge_n, inner_n, rows=rows, chunk=chunk):
            wait_bytes(recv.at[0:edge_n, 0:rows, 0 : win_j - 1], send_sem.at[chunk])
            wait_bytes(recv.at[0:inner_n, 0:rows, 0:win_j], send_sem.at[chunk])

        def drain_own(chunk=chunk, counts=counts, drain=drain):
            pl.when(at_edge)(lambda: drain(counts[0] - 1, counts[1]))
            pl.when(jnp.logical_not(at_edge))(lambda: drain(counts[0], counts[1] - 1))

        if chunk == 3:
            pl.when(no_outer)(lambda: drain(*counts))
            pl.when(jnp.logical_not(no_outer))(drain_own)
        else:
            drain_own()


def tail_kernel(tile, ymat, wt2, bias2, out_hbm, o_new, sem):
    par = lax.rem(lax.axis_index("model"), 2)
    rows = out_hbm.shape[0]
    o_pairs = ymat.shape[0] - 1
    late = (rows - 2) * par
    here = 2 * (1 - par)

    def start(k, carry):
        pltpu.make_async_copy(tile.at[par + k], out_hbm.at[k], sem.at[0]).start()
        return carry

    lax.fori_loop(here, here + rows - 2, start, 0)
    i = (o_pairs - 1) * par
    second((ymat.at[i], ymat.at[i + 1]), lambda dw: wt2[dw], bias2[...], o_new)
    last = pltpu.make_async_copy(o_new, out_hbm.at[pl.ds(late, 2)], sem.at[1])
    last.start()
    pltpu.make_async_copy(tile.at[0 : rows - 2], out_hbm.at[0 : rows - 2], sem.at[0]).wait()
    last.wait()


def solution(mesh):
    n_rows = mesh.shape["model"]
    n_cols = mesh.shape["cols"]

    def run_local(x_in, w_conv1, b_conv1, w_conv2, b_conv2):
        images, height, width, own_chans = x_in.shape
        sources = n_rows * n_cols
        chans = own_chans * sources
        pairs = width // 2
        tile_h, tile_j = height // n_rows, pairs // n_cols
        win_j = tile_j + 2
        x_pairs, z_pairs = (tile_h + 5) // 2, (tile_h + 3) // 2
        x_t = jnp.transpose(x_in, (1, 2, 3, 0)).reshape(n_rows // 2, 2 * tile_h, pairs, 2, own_chans, images)
        args = (x_t, w_conv1, b_conv1.reshape(1, chans), w_conv2, b_conv2.reshape(1, chans))
        hbm = pl.BlockSpec(memory_space=pltpu.HBM)
        vmem = pl.BlockSpec(memory_space=pltpu.VMEM)
        kept = (
            pltpu.VMEM((2 * (z_pairs - 1), tile_j, 2, images, chans), F32),
            pltpu.VMEM((z_pairs, win_j - 1, 2, images, 2 * chans), BF16),
            pltpu.VMEM((4, 4 * chans, 4 * chans), BF16),
            pltpu.VMEM((1, 4 * chans), F32),
        )
        state = pl.pallas_call(
            functools.partial(conv_kernel, n_rows, n_cols),
            out_shape=kept,
            in_specs=[hbm] * 5,
            out_specs=[vmem] * len(kept),
            scratch_shapes=[
                pltpu.VMEM((sources, 2 * x_pairs, win_j, own_chans, 2 * images), BF16),
                pltpu.VMEM((x_pairs, win_j, 2, images, 2 * chans), BF16),
                pltpu.VMEM((4, 4 * chans, 4 * chans), BF16),
                pltpu.VMEM((1, 4 * chans), F32),
                pltpu.VMEM((n_rows // 2, 2 * tile_h, pairs, 2, own_chans, images), BF16),
                pltpu.VMEM((height, pairs, own_chans, 2 * images), BF16),
                pltpu.VMEM((3, 3, own_chans, chans), BF16),
                pltpu.VMEM((5, own_chans, 2 * chans), BF16),
                pltpu.VMEM((n_rows // 2, 2, n_cols, 5, own_chans, 2 * chans), BF16),
                pltpu.VMEM((3, 3, chans, chans), BF16),
                pltpu.VMEM((1, chans), F32),
                pltpu.VMEM((1, chans), F32),
                pltpu.SemaphoreType.DMA((3, 2)),
                pltpu.SemaphoreType.DMA((4,)),
                pltpu.SemaphoreType.DMA((4,)),
                pltpu.SemaphoreType.DMA((4,)),
            ]
            + [pltpu.SemaphoreType.DMA] * 6,
            compiler_params=pltpu.CompilerParams(
                collective_id=0, has_side_effects=True, vmem_limit_bytes=24 << 20
            ),
            name="conv",
        )(*(pltpu.with_memory_space_constraint(a, pltpu.HBM) for a in args))
        out = pl.pallas_call(
            tail_kernel,
            out_shape=jax.ShapeDtypeStruct((tile_h, tile_j, 2, images, chans), F32),
            in_specs=[vmem] * len(kept),
            out_specs=pl.BlockSpec(memory_space=pl.ANY),
            scratch_shapes=[
                pltpu.VMEM((2, tile_j, 2, images, chans), F32),
                pltpu.SemaphoreType.DMA((2,)),
            ],
            compiler_params=pltpu.CompilerParams(vmem_limit_bytes=8 << 20),
            name="tail",
        )(*state)
        out = out.reshape(tile_h, 2 * tile_j, images, chans)
        return jnp.transpose(out, (2, 0, 1, 3))

    group = ("model", "cols")
    return jax.shard_map(
        run_local,
        mesh=mesh,
        in_specs=(P("data", None, None, group), P(None, None, group, None), P(), P(), P()),
        out_specs=P("data", "model", "cols", None),
        check_vma=False,
    )
```

```python
import functools

import jax
import jax.numpy as jnp
from jax import lax
from jax.experimental import pallas as pl
from jax.experimental.pallas import tpu as pltpu
from jax.sharding import PartitionSpec as P

MESH = pl.DeviceIdType.MESH
BF16 = jnp.bfloat16
F32 = jnp.float32
CHUNK_ROWS = (2, 3, 2)
TURNS, FIRSTS, SECONDS = (2, 4, 5, 6), (1, 3, 4, 5), (0, 2, 3, 3)
AHEAD = (1, 0)
COLUMN_FIRST = (3,)
CHIPS_ALONG = (3, 1, 2, 0)
CHIP_ORDER = tuple((other, dy) for other in (0, 1) for dy in (0, 1, -1, 2))


def turn(recv, i, put):
    sources, _, win_j, own_chans, lanes = recv.shape
    chans = sources * own_chans
    for j in range(win_j):
        top = recv[:, 2 * i, j].reshape(chans, lanes)
        under = recv[:, 2 * i + 1, j].reshape(chans, lanes)
        put(j, jnp.concatenate([top, under], axis=0).T.reshape(2, lanes // 2, 2 * chans))


def blocks(pairs, weights, count):
    acc = None
    for dw in range(4):
        parts = [view[dw // 2 : dw // 2 + count, dw % 2] for view in pairs]
        lhs = jnp.concatenate([p.reshape(count * p.shape[1], p.shape[2]) for p in parts], axis=1)
        term = jnp.dot(lhs, weights(dw), preferred_element_type=F32)
        acc = term if acc is None else acc + term
    return acc


def first(pairs, weights, bias, y_row, blank_a):
    count, _, images, lanes = y_row.shape
    c = lax.axis_index("cols")
    row = lax.rem(lax.broadcasted_iota(jnp.int32, (1, 2 * lanes), 1), lanes) // (lanes // 2)
    act = jnp.maximum(blocks(pairs, weights, count) + bias, 0.0)
    act = jnp.where(row != blank_a, act, 0.0).astype(BF16)
    for b in range(2):
        y_row[:, b] = act[:, b * lanes : (b + 1) * lanes].reshape(count, images, lanes)
    blank = jnp.zeros((images, lanes), BF16)

    @pl.when(c == 0)
    def _():
        y_row[0, 0] = blank

    @pl.when(c == lax.axis_size("cols") - 1)
    def _():
        y_row[count - 1, 1] = blank


def second(pairs, weights, bias, out_pair):
    _, count, _, images, chans = out_pair.shape
    res = blocks(pairs, weights, count) + bias
    for b in range(2):
        for a in range(2):
            at = (2 * b + a) * chans
            out_pair[a, :, b] = res[:, at : at + chans].reshape(count, images, chans)


def conv_kernel(
    n_rows,
    n_cols,
    x_hbm,
    w1_hbm,
    b1_hbm,
    w2_hbm,
    b2_hbm,
    out,
    ymat,
    wt2,
    bias2,
    recv,
    xmat,
    wt1,
    bias1,
    xs,
    packed,
    w1s,
    w1own,
    w1all,
    w2s,
    b1s,
    b2s,
    load_sem,
    par_sem,
    send_sem,
    recv_sem,
    wsend_sem,
    wrecv_sem,
    swap_send_sem,
    swap_recv_sem,
    wswap_send_sem,
    wswap_recv_sem,
):
    chip_h, pairs = xs.shape[1:3]
    images = xs.shape[-1]
    tile_h, tile_j = chip_h // 2, pairs // n_cols
    win_j = tile_j + 2
    sources = n_rows * n_cols
    r, c = lax.axis_index("model"), lax.axis_index("cols")
    par = lax.rem(r, 2)
    me = r * n_cols + c
    chans = recv.shape[0] * 2

    tops = [tile_h - sum(CHUNK_ROWS[: k + 1]) for k in range(len(CHUNK_ROWS))]
    groups = (
        ((tops[0], chip_h - tops[0]),),
        *(((k, k + n), (chip_h - k - n, chip_h - k)) for k, n in zip(tops[1:], CHUNK_ROWS[1:])),
    )
    loads = []
    for g, spans in enumerate(groups):
        loads.append(
            [
                pltpu.make_async_copy(x_hbm.at[:, lo:hi], xs.at[:, lo:hi], load_sem.at[g, n])
                for n, (lo, hi) in enumerate(spans)
            ]
        )
    for copies in loads:
        for copy in copies:
            copy.start()
    params = [
        pltpu.make_async_copy(src, dst, par_sem.at[s])
        for s, (src, dst) in enumerate(((w1_hbm, w1s), (w2_hbm, w2s), (b1_hbm, b1s), (b2_hbm, b2s)))
    ]
    for copy in params:
        copy.start()

    barrier = pltpu.get_barrier_semaphore()
    to_cs = [lax.rem(c + k, n_cols) for k in range(n_cols)]

    def device(to_r, to_c):
        return {"model": to_r, "cols": to_c}

    to_rs = [lax.rem(r + k, n_rows) for k in range(n_rows)]
    for kr, kc in sorted(
        ((kr, kc) for kr in range(n_rows) for kc in range(n_cols) if kr or kc),
        key=lambda k: (k[1] not in (1, 2), k[0] not in (2, 3, 4, 5), k[1] == 2, k[0] < 4, -min(k[0], n_rows - k[0])),
    ):
        pl.semaphore_signal(barrier, inc=1, device_id=device(to_rs[kr], to_cs[kc]), device_id_type=MESH)

    def pack_rows(x, lo, hi):
        rows = hi - lo
        left, right = (xs[x, lo:hi, :, p].reshape(rows * pairs * 2, images) for p in range(2))
        both = jnp.concatenate([left, right], axis=1)
        packed[pl.ds(chip_h * x + lo, rows)] = both.reshape(rows, pairs, 2, 2 * images)

    def pack(g):
        for copy in loads[g]:
            copy.wait()

        def body(x, carry):
            for lo, hi in groups[g]:
                pack_rows(x, lo, hi)
            return carry

        lax.fori_loop(0, n_rows // 2, body, 0)

    last = tile_h + 4

    def rows_of(offset, count):
        def where(to_r):
            q = lax.rem(to_r, 2)
            src = tile_h * to_r + offset + (tile_h - count - 2 * offset) * q
            dst = offset + 2 + (last - count - 2 * offset - 3) * q
            return src, dst

        return where

    chunks = (
        *((n, rows_of(k, n), False) for k, n in zip(tops, CHUNK_ROWS)),
        (2, rows_of(-2, 2), True),
    )
    no_outer = (r == 0) | (r == n_rows - 1)
    at_edge = (c == 0) | (c == n_cols - 1)
    own_j = c == 0
    own_j = own_j.astype(jnp.int32)

    def send_tile(chunk, to_r, to_c, there):
        rows, where, is_outer = chunks[chunk]
        src, dst = where(to_r)
        skip = (to_c == 0).astype(jnp.int32)
        edge = (to_c == 0) | (to_c == n_cols - 1)
        if is_outer:
            there = there & (to_r > 0) & (to_r < n_rows - 1)

        def copy(count, src_j, dst_j):
            pltpu.make_async_remote_copy(
                src_ref=packed.at[pl.ds(src, rows), pl.ds(src_j, count)],
                dst_ref=recv.at[me, pl.ds(dst, rows), pl.ds(dst_j, count)],
                send_sem=send_sem.at[chunk],
                recv_sem=recv_sem.at[chunk],
                device_id=device(to_r, to_c),
                device_id_type=MESH,
            ).start()

        pl.when(there & edge)(lambda: copy(win_j - 1, tile_j * to_c - 1 + skip, skip))
        pl.when(there & jnp.logical_not(edge))(lambda: copy(win_j, tile_j * to_c - 1, 0))

    chips = n_rows // 2
    ahead_r, ahead_c = AHEAD

    def step(t, table):
        value = jnp.int32(table[-1])
        for k, entry in enumerate(table[:-1]):
            value = jnp.where(t == k, entry, value)
        return value

    def turn_to(t):
        dx = step(t, CHIPS_ALONG)
        return lax.rem(r // 2 + dx, chips), dx

    def send_chip(chunk, t, rest, where=None):
        x, dx = turn_to(t)
        way = 1 - 2 * lax.rem(par + t, 2)
        for other, dy in CHIP_ORDER:
            to_r = 2 * x + (1 - par if other else par)
            to_c = lax.rem(c + way * dy + n_cols, n_cols)
            there = True
            if not other and dy == 0:
                there = dx > 0
            if rest:
                there = there & jnp.logical_not((to_r == ahead_r) & (to_c == ahead_c))
            if where is not None:
                there = there & where(to_c)
            send_tile(chunk, to_r, to_c, there)

    def send_ahead(chunk):
        send_tile(chunk, jnp.int32(ahead_r), jnp.int32(ahead_c), (r != ahead_r) | (c != ahead_c))

    def send_chunk(chunk):

        def first_column(t, carry):
            x, _ = turn_to(t)
            for other in range(2):
                to_r = 2 * x + (1 - par if other else par)
                there = ((to_r != r) | (c != 0)) & (to_r != ahead_r)
                send_tile(chunk, to_r, jnp.int32(0), there)
            return carry

        where = None
        if chunk in COLUMN_FIRST:
            lax.fori_loop(0, chips, first_column, 0)
            where = lambda to_c: to_c > 0

        def body(t, carry):
            send_chip(chunk, t, True, where)
            return carry

        lax.fori_loop(0, chips, body, 0)

    params[0].wait()
    for dw in range(3):
        w1own[dw] = jnp.concatenate([w1s[1, dw], w1s[0, dw]], axis=1)
    w1own[3] = jnp.concatenate([w1s[2, 0], w1s[2, 1]], axis=1)
    w1own[4] = jnp.concatenate([w1s[2, 2], jnp.zeros_like(w1s[2, 2])], axis=1)
    w1all[r // 2, par, c] = w1own[...]

    for copy in loads[0]:
        copy.wait()
    pack_rows(turn_to(0)[0], *groups[0][0])
    pl.semaphore_wait(barrier, sources - 1)

    def send_weights():
        for kr in range(0, n_rows, 2):
            for kc in range(n_cols):
                if kr or kc:
                    pltpu.make_async_remote_copy(
                        src_ref=w1own,
                        dst_ref=w1all.at[r // 2, par, c],
                        send_sem=wsend_sem,
                        recv_sem=wrecv_sem,
                        device_id=device(to_rs[kr], to_cs[kc]),
                        device_id_type=MESH,
                    ).start()

    def pack_and_send(t, carry):
        pl.when(t < chips - 1)(lambda: pack_rows(turn_to(t + 1)[0], *groups[0][0]))
        send_chip(0, t, False)
        pl.when(t == 0)(send_weights)
        return carry

    lax.fori_loop(0, chips, pack_and_send, 0)

    pack(1)
    send_ahead(1)
    send_chunk(1)
    pack(2)
    send_ahead(2)
    send_ahead(3)
    send_chunk(2)
    send_chunk(3)

    def wait_bytes(ref, sem):
        pltpu.make_async_copy(ref, ref, sem).wait()

    w1_bytes = recv.at[0 : sources // 2 - 1, 0, 0:5]
    wait_bytes(w1_bytes, wrecv_sem)
    wait_bytes(w1_bytes, wsend_sem)
    partner = device(r + 1 - 2 * par, c)
    w_swap = pltpu.make_async_remote_copy(
        src_ref=w1all.at[:, par],
        dst_ref=w1all.at[:, par],
        send_sem=wswap_send_sem,
        recv_sem=wswap_recv_sem,
        device_id=partner,
        device_id_type=MESH,
    )
    w_swap.start()

    def own_rows(chunk):
        rows, where, _ = chunks[chunk]
        src, dst = where(r)

        def copy(count, src_j, dst_j):
            for h in range(rows):
                recv[me, dst + h, pl.ds(dst_j, count)] = packed[src + h, pl.ds(src_j, count)]

        pl.when(at_edge)(lambda: copy(win_j - 1, tile_j * c - 1 + own_j, own_j))
        pl.when(jnp.logical_not(at_edge))(lambda: copy(win_j, tile_j * c - 1, 0))

    for chunk in range(3):
        own_rows(chunk)
    pl.when(jnp.logical_not(no_outer))(lambda: own_rows(3))

    zero_row = jnp.zeros((win_j, 2, 2 * images), BF16)
    zero_col = jnp.zeros((tile_h + 2, 2, 2 * images), BF16)

    def clear(s, carry):
        recv[s, last * (1 - par)] = zero_row
        return carry

    def clear_outer(s, carry):
        recv[s, (last - 1) * par] = zero_row
        recv[s, (last - 1) * par + 1] = zero_row
        return carry

    def clear_edge(s, carry):
        recv[s, pl.ds(3 * par, tile_h + 2), (win_j - 1) * (1 - own_j)] = zero_col
        return carry

    lax.fori_loop(0, sources, clear, 0)
    pl.when(no_outer)(lambda: (lax.fori_loop(0, sources, clear_outer, 0), None)[1])
    pl.when(at_edge)(lambda: (lax.fori_loop(0, sources, clear_edge, 0), None)[1])

    low = lax.broadcasted_iota(jnp.int32, (chans, 2 * chans), 1) < chans

    def spread(wt, u, v, dw):
        ur, vr = pltpu.roll(u, chans, 1), pltpu.roll(v, chans, 1)
        zero = jnp.zeros_like(u)
        tiles = (jnp.where(low, ur, zero), u, jnp.where(low, v, ur), jnp.where(low, zero, vr))
        for k, tile in enumerate(tiles):
            tile = tile.astype(BF16)
            for b in range(2):
                wt[dw + b, k * chans : (k + 1) * chans, b * 2 * chans : (b + 1) * 2 * chans] = tile

    def blank(wt):
        zero = jnp.zeros((4 * chans, 2 * chans), BF16)
        wt[3, :, 0 : 2 * chans] = zero
        wt[0, :, 2 * chans : 4 * chans] = zero

    for copy in params[1:]:
        copy.wait()
    blank(wt1)
    blank(wt2)
    for dw in range(3):
        w = [w2s[dh, dw].astype(F32) for dh in range(3)]
        spread(
            wt2,
            jnp.concatenate([w[1], w[0]], axis=1),
            jnp.concatenate([w[2], jnp.zeros_like(w[2])], axis=1),
            dw,
        )
    bias1[...] = jnp.concatenate([b1s[...]] * 4, axis=1)
    bias2[...] = jnp.concatenate([b2s[...]] * 4, axis=1)

    def arrived(chunk):
        def wait(count):
            wait_bytes(recv.at[0 : sources - 1, 0 : chunks[chunk][0], 0:count], recv_sem.at[chunk])

        pl.when(at_edge)(lambda: wait(win_j - 1))
        pl.when(jnp.logical_not(at_edge))(lambda: wait(win_j))

    arrived(0)
    give = tile_h - (tile_h - 3) * par
    land = tile_h + 2 - (tile_h + 1) * (1 - par)
    swap = pltpu.make_async_remote_copy(
        src_ref=recv.at[:, pl.ds(give, 2)],
        dst_ref=recv.at[:, pl.ds(land, 2)],
        send_sem=swap_send_sem,
        recv_sem=swap_recv_sem,
        device_id=partner,
        device_id_type=MESH,
    )
    swap.start()

    w_swap.wait()
    u = [w1all[:, :, :, k].reshape(chans, 2 * chans).astype(F32) for k in range(5)]
    for dw in range(3):
        v = (u[3], pltpu.roll(u[3], chans, 1), u[4])[dw]
        spread(wt1, u[dw], jnp.where(low, v, 0.0), dw)

    x_pairs, z_pairs = xmat.shape[0], ymat.shape[0]
    o_pairs = z_pairs - 1

    def nth(n, count):
        return (count - 1) * (1 - par) + n * (2 * par - 1)

    def turn_one(n, carry):
        i = nth(n, x_pairs)

        def put(j, value):
            xmat[i, j] = value

        turn(recv, i, put)
        return carry

    def first_one(n, carry):
        i = nth(n, z_pairs)
        fill = jnp.where(n == 0, 1 - par, 2)
        out_of = jnp.where(n == z_pairs - 1, jnp.where(r == 0, 0, jnp.where(r == n_rows - 1, 1, 2)), 2)
        blank_a = jnp.where(fill < 2, fill, out_of)
        first((xmat.at[i], xmat.at[i + 1]), lambda dw: wt1[dw], bias1[...], ymat.at[i], blank_a)
        return carry

    def second_one(n, carry):
        i = nth(n, o_pairs)
        second((ymat.at[i], ymat.at[i + 1]), lambda dw: wt2[dw], bias2[...], out.at[pl.ds(2 * i, 2)])
        return carry

    def stage(s, carry):
        @pl.when(s == 0)
        def _():
            swap.wait()

        for k in range(1, 4):
            there = s == k
            if k == 3:
                there = there & jnp.logical_not(no_outer)
            pl.when(there)(lambda k=k: arrived(k))

        for ends, one in ((TURNS, turn_one), (FIRSTS, first_one), (SECONDS, second_one)):
            lax.fori_loop(step(s, (0, *ends[:-1])), step(s, ends), one, 0)
        return carry

    lax.fori_loop(0, 4, stage, 0)

    per_edge = n_rows * 2
    for chunk in range(4):
        rows = chunks[chunk][0]
        n_r = n_rows - 2 if chunk == 3 else n_rows
        counts = (n_r * 2, n_r * (n_cols - 2))

        def drain(edge_n, inner_n, rows=rows, chunk=chunk):
            wait_bytes(recv.at[0:edge_n, 0:rows, 0 : win_j - 1], send_sem.at[chunk])
            wait_bytes(recv.at[0:inner_n, 0:rows, 0:win_j], send_sem.at[chunk])

        def drain_own(chunk=chunk, counts=counts, drain=drain):
            pl.when(at_edge)(lambda: drain(counts[0] - 1, counts[1]))
            pl.when(jnp.logical_not(at_edge))(lambda: drain(counts[0], counts[1] - 1))

        if chunk == 3:
            pl.when(no_outer)(lambda: drain(*counts))
            pl.when(jnp.logical_not(no_outer))(drain_own)
        else:
            drain_own()


def tail_kernel(tile, ymat, wt2, bias2, out_hbm, o_new, sem):
    par = lax.rem(lax.axis_index("model"), 2)
    rows = out_hbm.shape[0]
    o_pairs = ymat.shape[0] - 1
    late = (rows - 2) * par
    here = 2 * (1 - par)

    def start(k, carry):
        pltpu.make_async_copy(tile.at[par + k], out_hbm.at[k], sem.at[0]).start()
        return carry

    lax.fori_loop(here, here + rows - 2, start, 0)
    i = (o_pairs - 1) * par
    second((ymat.at[i], ymat.at[i + 1]), lambda dw: wt2[dw], bias2[...], o_new)
    last = pltpu.make_async_copy(o_new, out_hbm.at[pl.ds(late, 2)], sem.at[1])
    last.start()
    pltpu.make_async_copy(tile.at[0 : rows - 2], out_hbm.at[0 : rows - 2], sem.at[0]).wait()
    last.wait()


def solution(mesh):
    n_rows = mesh.shape["model"]
    n_cols = mesh.shape["cols"]

    def run_local(x_in, w_conv1, b_conv1, w_conv2, b_conv2):
        images, height, width, own_chans = x_in.shape
        sources = n_rows * n_cols
        chans = own_chans * sources
        pairs = width // 2
        tile_h, tile_j = height // n_rows, pairs // n_cols
        win_j = tile_j + 2
        x_pairs, z_pairs = (tile_h + 5) // 2, (tile_h + 3) // 2
        x_t = jnp.transpose(x_in, (1, 2, 3, 0)).reshape(n_rows // 2, 2 * tile_h, pairs, 2, own_chans, images)
        args = (x_t, w_conv1, b_conv1.reshape(1, chans), w_conv2, b_conv2.reshape(1, chans))
        hbm = pl.BlockSpec(memory_space=pltpu.HBM)
        vmem = pl.BlockSpec(memory_space=pltpu.VMEM)
        kept = (
            pltpu.VMEM((2 * (z_pairs - 1), tile_j, 2, images, chans), F32),
            pltpu.VMEM((z_pairs, win_j - 1, 2, images, 2 * chans), BF16),
            pltpu.VMEM((4, 4 * chans, 4 * chans), BF16),
            pltpu.VMEM((1, 4 * chans), F32),
        )
        state = pl.pallas_call(
            functools.partial(conv_kernel, n_rows, n_cols),
            out_shape=kept,
            in_specs=[hbm] * 5,
            out_specs=[vmem] * len(kept),
            scratch_shapes=[
                pltpu.VMEM((sources, 2 * x_pairs, win_j, own_chans, 2 * images), BF16),
                pltpu.VMEM((x_pairs, win_j, 2, images, 2 * chans), BF16),
                pltpu.VMEM((4, 4 * chans, 4 * chans), BF16),
                pltpu.VMEM((1, 4 * chans), F32),
                pltpu.VMEM((n_rows // 2, 2 * tile_h, pairs, 2, own_chans, images), BF16),
                pltpu.VMEM((height, pairs, own_chans, 2 * images), BF16),
                pltpu.VMEM((3, 3, own_chans, chans), BF16),
                pltpu.VMEM((5, own_chans, 2 * chans), BF16),
                pltpu.VMEM((n_rows // 2, 2, n_cols, 5, own_chans, 2 * chans), BF16),
                pltpu.VMEM((3, 3, chans, chans), BF16),
                pltpu.VMEM((1, chans), F32),
                pltpu.VMEM((1, chans), F32),
                pltpu.SemaphoreType.DMA((3, 2)),
                pltpu.SemaphoreType.DMA((4,)),
                pltpu.SemaphoreType.DMA((4,)),
                pltpu.SemaphoreType.DMA((4,)),
            ]
            + [pltpu.SemaphoreType.DMA] * 6,
            compiler_params=pltpu.CompilerParams(
                collective_id=0, has_side_effects=True, vmem_limit_bytes=24 << 20
            ),
            name="conv",
        )(*(pltpu.with_memory_space_constraint(a, pltpu.HBM) for a in args))
        out = pl.pallas_call(
            tail_kernel,
            out_shape=jax.ShapeDtypeStruct((tile_h, tile_j, 2, images, chans), F32),
            in_specs=[vmem] * len(kept),
            out_specs=pl.BlockSpec(memory_space=pl.ANY),
            scratch_shapes=[
                pltpu.VMEM((2, tile_j, 2, images, chans), F32),
                pltpu.SemaphoreType.DMA((2,)),
            ],
            compiler_params=pltpu.CompilerParams(vmem_limit_bytes=8 << 20),
            name="tail",
        )(*state)
        out = out.reshape(tile_h, 2 * tile_j, images, chans)
        return jnp.transpose(out, (2, 0, 1, 3))

    group = ("model", "cols")
    return jax.shard_map(
        run_local,
        mesh=mesh,
        in_specs=(P("data", None, None, group), P(None, None, group, None), P(), P(), P()),
        out_specs=P("data", "model", "cols", None),
        check_vma=False,
    )
```

```python
import functools

import jax
import jax.numpy as jnp
from jax import lax
from jax.experimental import pallas as pl
from jax.experimental.pallas import tpu as pltpu
from jax.sharding import PartitionSpec as P

MESH = pl.DeviceIdType.MESH
BF16 = jnp.bfloat16
F32 = jnp.float32
CHUNK_ROWS = (2, 3, 2)
TURNS, FIRSTS, SECONDS = (2, 4, 5, 6), (1, 3, 4, 5), (0, 2, 3, 3)
AHEAD = (1, 0)
COLUMN_FIRST = (3,)
CHIPS_ALONG = (3, 1, 2, 0)
CHIP_ORDER = tuple((other, dy) for other in (0, 1) for dy in (1, -1, 0, 2))


def turn(recv, i, put):
    sources, _, win_j, own_chans, lanes = recv.shape
    chans = sources * own_chans
    for j in range(win_j):
        top = recv[:, 2 * i, j].reshape(chans, lanes)
        under = recv[:, 2 * i + 1, j].reshape(chans, lanes)
        put(j, jnp.concatenate([top, under], axis=0).T.reshape(2, lanes // 2, 2 * chans))


def blocks(pairs, weights, count):
    acc = None
    for dw in range(4):
        parts = [view[dw // 2 : dw // 2 + count, dw % 2] for view in pairs]
        lhs = jnp.concatenate([p.reshape(count * p.shape[1], p.shape[2]) for p in parts], axis=1)
        term = jnp.dot(lhs, weights(dw), preferred_element_type=F32)
        acc = term if acc is None else acc + term
    return acc


def first(pairs, weights, bias, y_row, blank_a):
    count, _, images, lanes = y_row.shape
    c = lax.axis_index("cols")
    row = lax.rem(lax.broadcasted_iota(jnp.int32, (1, 2 * lanes), 1), lanes) // (lanes // 2)
    act = jnp.maximum(blocks(pairs, weights, count) + bias, 0.0)
    act = jnp.where(row != blank_a, act, 0.0).astype(BF16)
    for b in range(2):
        y_row[:, b] = act[:, b * lanes : (b + 1) * lanes].reshape(count, images, lanes)
    blank = jnp.zeros((images, lanes), BF16)

    @pl.when(c == 0)
    def _():
        y_row[0, 0] = blank

    @pl.when(c == lax.axis_size("cols") - 1)
    def _():
        y_row[count - 1, 1] = blank


def second(pairs, weights, bias, out_pair):
    _, count, _, images, chans = out_pair.shape
    res = blocks(pairs, weights, count) + bias
    for b in range(2):
        for a in range(2):
            at = (2 * b + a) * chans
            out_pair[a, :, b] = res[:, at : at + chans].reshape(count, images, chans)


def conv_kernel(
    n_rows,
    n_cols,
    x_hbm,
    w1_hbm,
    b1_hbm,
    w2_hbm,
    b2_hbm,
    out,
    ymat,
    wt2,
    bias2,
    recv,
    xmat,
    wt1,
    bias1,
    xs,
    packed,
    w1s,
    w1own,
    w1all,
    w2s,
    b1s,
    b2s,
    load_sem,
    par_sem,
    send_sem,
    recv_sem,
    wsend_sem,
    wrecv_sem,
    swap_send_sem,
    swap_recv_sem,
    wswap_send_sem,
    wswap_recv_sem,
):
    chip_h, pairs = xs.shape[1:3]
    images = xs.shape[-1]
    tile_h, tile_j = chip_h // 2, pairs // n_cols
    win_j = tile_j + 2
    sources = n_rows * n_cols
    r, c = lax.axis_index("model"), lax.axis_index("cols")
    par = lax.rem(r, 2)
    me = r * n_cols + c
    chans = recv.shape[0] * 2

    tops = [tile_h - sum(CHUNK_ROWS[: k + 1]) for k in range(len(CHUNK_ROWS))]
    groups = (
        ((tops[0], chip_h - tops[0]),),
        *(((k, k + n), (chip_h - k - n, chip_h - k)) for k, n in zip(tops[1:], CHUNK_ROWS[1:])),
    )
    loads = []
    for g, spans in enumerate(groups):
        loads.append(
            [
                pltpu.make_async_copy(x_hbm.at[:, lo:hi], xs.at[:, lo:hi], load_sem.at[g, n])
                for n, (lo, hi) in enumerate(spans)
            ]
        )
    for copies in loads:
        for copy in copies:
            copy.start()
    params = [
        pltpu.make_async_copy(src, dst, par_sem.at[s])
        for s, (src, dst) in enumerate(((w1_hbm, w1s), (w2_hbm, w2s), (b1_hbm, b1s), (b2_hbm, b2s)))
    ]
    for copy in params:
        copy.start()

    barrier = pltpu.get_barrier_semaphore()
    to_cs = [lax.rem(c + k, n_cols) for k in range(n_cols)]

    def device(to_r, to_c):
        return {"model": to_r, "cols": to_c}

    to_rs = [lax.rem(r + k, n_rows) for k in range(n_rows)]
    for kr, kc in sorted(
        ((kr, kc) for kr in range(n_rows) for kc in range(n_cols) if kr or kc),
        key=lambda k: (k[1] not in (1, 2), k[0] not in (2, 3, 4, 5), k[1] == 2, k[0] < 4, -min(k[0], n_rows - k[0])),
    ):
        pl.semaphore_signal(barrier, inc=1, device_id=device(to_rs[kr], to_cs[kc]), device_id_type=MESH)

    def pack_rows(x, lo, hi):
        rows = hi - lo
        left, right = (xs[x, lo:hi, :, p].reshape(rows * pairs * 2, images) for p in range(2))
        both = jnp.concatenate([left, right], axis=1)
        packed[pl.ds(chip_h * x + lo, rows)] = both.reshape(rows, pairs, 2, 2 * images)

    def pack(g):
        for copy in loads[g]:
            copy.wait()

        def body(x, carry):
            for lo, hi in groups[g]:
                pack_rows(x, lo, hi)
            return carry

        lax.fori_loop(0, n_rows // 2, body, 0)

    last = tile_h + 4

    def rows_of(offset, count):
        def where(to_r):
            q = lax.rem(to_r, 2)
            src = tile_h * to_r + offset + (tile_h - count - 2 * offset) * q
            dst = offset + 2 + (last - count - 2 * offset - 3) * q
            return src, dst

        return where

    chunks = (
        *((n, rows_of(k, n), False) for k, n in zip(tops, CHUNK_ROWS)),
        (2, rows_of(-2, 2), True),
    )
    no_outer = (r == 0) | (r == n_rows - 1)
    at_edge = (c == 0) | (c == n_cols - 1)
    own_j = c == 0
    own_j = own_j.astype(jnp.int32)

    def send_tile(chunk, to_r, to_c, there):
        rows, where, is_outer = chunks[chunk]
        src, dst = where(to_r)
        skip = (to_c == 0).astype(jnp.int32)
        edge = (to_c == 0) | (to_c == n_cols - 1)
        if is_outer:
            there = there & (to_r > 0) & (to_r < n_rows - 1)

        def copy(count, src_j, dst_j):
            pltpu.make_async_remote_copy(
                src_ref=packed.at[pl.ds(src, rows), pl.ds(src_j, count)],
                dst_ref=recv.at[me, pl.ds(dst, rows), pl.ds(dst_j, count)],
                send_sem=send_sem.at[chunk],
                recv_sem=recv_sem.at[chunk],
                device_id=device(to_r, to_c),
                device_id_type=MESH,
            ).start()

        pl.when(there & edge)(lambda: copy(win_j - 1, tile_j * to_c - 1 + skip, skip))
        pl.when(there & jnp.logical_not(edge))(lambda: copy(win_j, tile_j * to_c - 1, 0))

    chips = n_rows // 2
    ahead_r, ahead_c = AHEAD

    def step(t, table):
        value = jnp.int32(table[-1])
        for k, entry in enumerate(table[:-1]):
            value = jnp.where(t == k, entry, value)
        return value

    def turn_to(t):
        dx = step(t, CHIPS_ALONG)
        return lax.rem(r // 2 + dx, chips), dx

    def send_chip(chunk, t, rest, where=None):
        x, dx = turn_to(t)
        way = 1 - 2 * lax.rem(par + t, 2)
        for other, dy in CHIP_ORDER:
            to_r = 2 * x + (1 - par if other else par)
            to_c = lax.rem(c + way * dy + n_cols, n_cols)
            there = True
            if not other and dy == 0:
                there = dx > 0
            if rest:
                there = there & jnp.logical_not((to_r == ahead_r) & (to_c == ahead_c))
            if where is not None:
                there = there & where(to_c)
            send_tile(chunk, to_r, to_c, there)

    def send_ahead(chunk):
        send_tile(chunk, jnp.int32(ahead_r), jnp.int32(ahead_c), (r != ahead_r) | (c != ahead_c))

    def send_chunk(chunk):

        def first_column(t, carry):
            x, _ = turn_to(t)
            for other in range(2):
                to_r = 2 * x + (1 - par if other else par)
                there = ((to_r != r) | (c != 0)) & (to_r != ahead_r)
                send_tile(chunk, to_r, jnp.int32(0), there)
            return carry

        where = None
        if chunk in COLUMN_FIRST:
            lax.fori_loop(0, chips, first_column, 0)
            where = lambda to_c: to_c > 0

        def body(t, carry):
            send_chip(chunk, t, True, where)
            return carry

        lax.fori_loop(0, chips, body, 0)

    params[0].wait()
    for dw in range(3):
        w1own[dw] = jnp.concatenate([w1s[1, dw], w1s[0, dw]], axis=1)
    w1own[3] = jnp.concatenate([w1s[2, 0], w1s[2, 1]], axis=1)
    w1own[4] = jnp.concatenate([w1s[2, 2], jnp.zeros_like(w1s[2, 2])], axis=1)
    w1all[r // 2, par, c] = w1own[...]

    for copy in loads[0]:
        copy.wait()
    pack_rows(turn_to(0)[0], *groups[0][0])
    pl.semaphore_wait(barrier, sources - 1)

    def send_weights():
        for kr in range(0, n_rows, 2):
            for kc in range(n_cols):
                if kr or kc:
                    pltpu.make_async_remote_copy(
                        src_ref=w1own,
                        dst_ref=w1all.at[r // 2, par, c],
                        send_sem=wsend_sem,
                        recv_sem=wrecv_sem,
                        device_id=device(to_rs[kr], to_cs[kc]),
                        device_id_type=MESH,
                    ).start()

    def pack_and_send(t, carry):
        pl.when(t < chips - 1)(lambda: pack_rows(turn_to(t + 1)[0], *groups[0][0]))
        send_chip(0, t, False)
        pl.when(t == 0)(send_weights)
        return carry

    lax.fori_loop(0, chips, pack_and_send, 0)

    pack(1)
    send_ahead(1)
    send_chunk(1)
    pack(2)
    send_ahead(2)
    send_ahead(3)
    send_chunk(2)
    send_chunk(3)

    def wait_bytes(ref, sem):
        pltpu.make_async_copy(ref, ref, sem).wait()

    w1_bytes = recv.at[0 : sources // 2 - 1, 0, 0:5]
    wait_bytes(w1_bytes, wrecv_sem)
    wait_bytes(w1_bytes, wsend_sem)
    partner = device(r + 1 - 2 * par, c)
    w_swap = pltpu.make_async_remote_copy(
        src_ref=w1all.at[:, par],
        dst_ref=w1all.at[:, par],
        send_sem=wswap_send_sem,
        recv_sem=wswap_recv_sem,
        device_id=partner,
        device_id_type=MESH,
    )
    w_swap.start()

    def own_rows(chunk):
        rows, where, _ = chunks[chunk]
        src, dst = where(r)

        def copy(count, src_j, dst_j):
            for h in range(rows):
                recv[me, dst + h, pl.ds(dst_j, count)] = packed[src + h, pl.ds(src_j, count)]

        pl.when(at_edge)(lambda: copy(win_j - 1, tile_j * c - 1 + own_j, own_j))
        pl.when(jnp.logical_not(at_edge))(lambda: copy(win_j, tile_j * c - 1, 0))

    for chunk in range(3):
        own_rows(chunk)
    pl.when(jnp.logical_not(no_outer))(lambda: own_rows(3))

    zero_row = jnp.zeros((win_j, 2, 2 * images), BF16)
    zero_col = jnp.zeros((tile_h + 2, 2, 2 * images), BF16)

    def clear(s, carry):
        recv[s, last * (1 - par)] = zero_row
        return carry

    def clear_outer(s, carry):
        recv[s, (last - 1) * par] = zero_row
        recv[s, (last - 1) * par + 1] = zero_row
        return carry

    def clear_edge(s, carry):
        recv[s, pl.ds(3 * par, tile_h + 2), (win_j - 1) * (1 - own_j)] = zero_col
        return carry

    lax.fori_loop(0, sources, clear, 0)
    pl.when(no_outer)(lambda: (lax.fori_loop(0, sources, clear_outer, 0), None)[1])
    pl.when(at_edge)(lambda: (lax.fori_loop(0, sources, clear_edge, 0), None)[1])

    low = lax.broadcasted_iota(jnp.int32, (chans, 2 * chans), 1) < chans

    def spread(wt, u, v, dw):
        ur, vr = pltpu.roll(u, chans, 1), pltpu.roll(v, chans, 1)
        zero = jnp.zeros_like(u)
        tiles = (jnp.where(low, ur, zero), u, jnp.where(low, v, ur), jnp.where(low, zero, vr))
        for k, tile in enumerate(tiles):
            tile = tile.astype(BF16)
            for b in range(2):
                wt[dw + b, k * chans : (k + 1) * chans, b * 2 * chans : (b + 1) * 2 * chans] = tile

    def blank(wt):
        zero = jnp.zeros((4 * chans, 2 * chans), BF16)
        wt[3, :, 0 : 2 * chans] = zero
        wt[0, :, 2 * chans : 4 * chans] = zero

    for copy in params[1:]:
        copy.wait()
    blank(wt1)
    blank(wt2)
    for dw in range(3):
        w = [w2s[dh, dw].astype(F32) for dh in range(3)]
        spread(
            wt2,
            jnp.concatenate([w[1], w[0]], axis=1),
            jnp.concatenate([w[2], jnp.zeros_like(w[2])], axis=1),
            dw,
        )
    bias1[...] = jnp.concatenate([b1s[...]] * 4, axis=1)
    bias2[...] = jnp.concatenate([b2s[...]] * 4, axis=1)

    def arrived(chunk):
        def wait(count):
            wait_bytes(recv.at[0 : sources - 1, 0 : chunks[chunk][0], 0:count], recv_sem.at[chunk])

        pl.when(at_edge)(lambda: wait(win_j - 1))
        pl.when(jnp.logical_not(at_edge))(lambda: wait(win_j))

    arrived(0)
    give = tile_h - (tile_h - 3) * par
    land = tile_h + 2 - (tile_h + 1) * (1 - par)
    swap = pltpu.make_async_remote_copy(
        src_ref=recv.at[:, pl.ds(give, 2)],
        dst_ref=recv.at[:, pl.ds(land, 2)],
        send_sem=swap_send_sem,
        recv_sem=swap_recv_sem,
        device_id=partner,
        device_id_type=MESH,
    )
    swap.start()

    w_swap.wait()
    u = [w1all[:, :, :, k].reshape(chans, 2 * chans).astype(F32) for k in range(5)]
    for dw in range(3):
        v = (u[3], pltpu.roll(u[3], chans, 1), u[4])[dw]
        spread(wt1, u[dw], jnp.where(low, v, 0.0), dw)

    x_pairs, z_pairs = xmat.shape[0], ymat.shape[0]
    o_pairs = z_pairs - 1

    def nth(n, count):
        return (count - 1) * (1 - par) + n * (2 * par - 1)

    def turn_one(n, carry):
        i = nth(n, x_pairs)

        def put(j, value):
            xmat[i, j] = value

        turn(recv, i, put)
        return carry

    def first_one(n, carry):
        i = nth(n, z_pairs)
        fill = jnp.where(n == 0, 1 - par, 2)
        out_of = jnp.where(n == z_pairs - 1, jnp.where(r == 0, 0, jnp.where(r == n_rows - 1, 1, 2)), 2)
        blank_a = jnp.where(fill < 2, fill, out_of)
        first((xmat.at[i], xmat.at[i + 1]), lambda dw: wt1[dw], bias1[...], ymat.at[i], blank_a)
        return carry

    def second_one(n, carry):
        i = nth(n, o_pairs)
        second((ymat.at[i], ymat.at[i + 1]), lambda dw: wt2[dw], bias2[...], out.at[pl.ds(2 * i, 2)])
        return carry

    def stage(s, carry):
        @pl.when(s == 0)
        def _():
            swap.wait()

        for k in range(1, 4):
            there = s == k
            if k == 3:
                there = there & jnp.logical_not(no_outer)
            pl.when(there)(lambda k=k: arrived(k))

        for ends, one in ((TURNS, turn_one), (FIRSTS, first_one), (SECONDS, second_one)):
            lax.fori_loop(step(s, (0, *ends[:-1])), step(s, ends), one, 0)
        return carry

    lax.fori_loop(0, 4, stage, 0)

    per_edge = n_rows * 2
    for chunk in range(4):
        rows = chunks[chunk][0]
        n_r = n_rows - 2 if chunk == 3 else n_rows
        counts = (n_r * 2, n_r * (n_cols - 2))

        def drain(edge_n, inner_n, rows=rows, chunk=chunk):
            wait_bytes(recv.at[0:edge_n, 0:rows, 0 : win_j - 1], send_sem.at[chunk])
            wait_bytes(recv.at[0:inner_n, 0:rows, 0:win_j], send_sem.at[chunk])

        def drain_own(chunk=chunk, counts=counts, drain=drain):
            pl.when(at_edge)(lambda: drain(counts[0] - 1, counts[1]))
            pl.when(jnp.logical_not(at_edge))(lambda: drain(counts[0], counts[1] - 1))

        if chunk == 3:
            pl.when(no_outer)(lambda: drain(*counts))
            pl.when(jnp.logical_not(no_outer))(drain_own)
        else:
            drain_own()


def tail_kernel(tile, ymat, wt2, bias2, out_hbm, o_new, sem):
    par = lax.rem(lax.axis_index("model"), 2)
    rows = out_hbm.shape[0]
    o_pairs = ymat.shape[0] - 1
    late = (rows - 2) * par
    here = 2 * (1 - par)

    def start(k, carry):
        pltpu.make_async_copy(tile.at[par + k], out_hbm.at[k], sem.at[0]).start()
        return carry

    lax.fori_loop(here, here + rows - 2, start, 0)
    i = (o_pairs - 1) * par
    second((ymat.at[i], ymat.at[i + 1]), lambda dw: wt2[dw], bias2[...], o_new)
    last = pltpu.make_async_copy(o_new, out_hbm.at[pl.ds(late, 2)], sem.at[1])
    last.start()
    pltpu.make_async_copy(tile.at[0 : rows - 2], out_hbm.at[0 : rows - 2], sem.at[0]).wait()
    last.wait()


def solution(mesh):
    n_rows = mesh.shape["model"]
    n_cols = mesh.shape["cols"]

    def run_local(x_in, w_conv1, b_conv1, w_conv2, b_conv2):
        images, height, width, own_chans = x_in.shape
        sources = n_rows * n_cols
        chans = own_chans * sources
        pairs = width // 2
        tile_h, tile_j = height // n_rows, pairs // n_cols
        win_j = tile_j + 2
        x_pairs, z_pairs = (tile_h + 5) // 2, (tile_h + 3) // 2
        x_t = jnp.transpose(x_in, (1, 2, 3, 0)).reshape(n_rows // 2, 2 * tile_h, pairs, 2, own_chans, images)
        args = (x_t, w_conv1, b_conv1.reshape(1, chans), w_conv2, b_conv2.reshape(1, chans))
        hbm = pl.BlockSpec(memory_space=pltpu.HBM)
        vmem = pl.BlockSpec(memory_space=pltpu.VMEM)
        kept = (
            pltpu.VMEM((2 * (z_pairs - 1), tile_j, 2, images, chans), F32),
            pltpu.VMEM((z_pairs, win_j - 1, 2, images, 2 * chans), BF16),
            pltpu.VMEM((4, 4 * chans, 4 * chans), BF16),
            pltpu.VMEM((1, 4 * chans), F32),
        )
        state = pl.pallas_call(
            functools.partial(conv_kernel, n_rows, n_cols),
            out_shape=kept,
            in_specs=[hbm] * 5,
            out_specs=[vmem] * len(kept),
            scratch_shapes=[
                pltpu.VMEM((sources, 2 * x_pairs, win_j, own_chans, 2 * images), BF16),
                pltpu.VMEM((x_pairs, win_j, 2, images, 2 * chans), BF16),
                pltpu.VMEM((4, 4 * chans, 4 * chans), BF16),
                pltpu.VMEM((1, 4 * chans), F32),
                pltpu.VMEM((n_rows // 2, 2 * tile_h, pairs, 2, own_chans, images), BF16),
                pltpu.VMEM((height, pairs, own_chans, 2 * images), BF16),
                pltpu.VMEM((3, 3, own_chans, chans), BF16),
                pltpu.VMEM((5, own_chans, 2 * chans), BF16),
                pltpu.VMEM((n_rows // 2, 2, n_cols, 5, own_chans, 2 * chans), BF16),
                pltpu.VMEM((3, 3, chans, chans), BF16),
                pltpu.VMEM((1, chans), F32),
                pltpu.VMEM((1, chans), F32),
                pltpu.SemaphoreType.DMA((3, 2)),
                pltpu.SemaphoreType.DMA((4,)),
                pltpu.SemaphoreType.DMA((4,)),
                pltpu.SemaphoreType.DMA((4,)),
            ]
            + [pltpu.SemaphoreType.DMA] * 6,
            compiler_params=pltpu.CompilerParams(
                collective_id=0, has_side_effects=True, vmem_limit_bytes=24 << 20
            ),
            name="conv",
        )(*(pltpu.with_memory_space_constraint(a, pltpu.HBM) for a in args))
        out = pl.pallas_call(
            tail_kernel,
            out_shape=jax.ShapeDtypeStruct((tile_h, tile_j, 2, images, chans), F32),
            in_specs=[vmem] * len(kept),
            out_specs=pl.BlockSpec(memory_space=pl.ANY),
            scratch_shapes=[
                pltpu.VMEM((2, tile_j, 2, images, chans), F32),
                pltpu.SemaphoreType.DMA((2,)),
            ],
            compiler_params=pltpu.CompilerParams(vmem_limit_bytes=8 << 20),
            name="tail",
        )(*state)
        out = out.reshape(tile_h, 2 * tile_j, images, chans)
        return jnp.transpose(out, (2, 0, 1, 3))

    group = ("model", "cols")
    return jax.shard_map(
        run_local,
        mesh=mesh,
        in_specs=(P("data", None, None, group), P(None, None, group, None), P(), P(), P()),
        out_specs=P("data", "model", "cols", None),
        check_vma=False,
    )
```

```python
import functools

import jax
import jax.numpy as jnp
from jax import lax
from jax.experimental import pallas as pl
from jax.experimental.pallas import tpu as pltpu
from jax.sharding import PartitionSpec as P

MESH = pl.DeviceIdType.MESH
BF16 = jnp.bfloat16
F32 = jnp.float32
CHUNK_ROWS = (2, 3, 2)
TURNS, FIRSTS, SECONDS = (2, 4, 5, 6), (1, 3, 4, 5), (0, 2, 3, 3)
AHEAD = (1, 0)
COLUMN_FIRST = (2, 3)
CHIPS_ALONG = (1, 3, 2, 0)
CHIP_ORDER = tuple((other, dy) for other in (0, 1) for dy in (1, -1, 0, 2))


def turn(recv, i, put):
    sources, _, win_j, own_chans, lanes = recv.shape
    chans = sources * own_chans
    for j in range(win_j):
        top = recv[:, 2 * i, j].reshape(chans, lanes)
        under = recv[:, 2 * i + 1, j].reshape(chans, lanes)
        put(j, jnp.concatenate([top, under], axis=0).T.reshape(2, lanes // 2, 2 * chans))


def blocks(pairs, weights, count):
    acc = None
    for dw in range(4):
        parts = [view[dw // 2 : dw // 2 + count, dw % 2] for view in pairs]
        lhs = jnp.concatenate([p.reshape(count * p.shape[1], p.shape[2]) for p in parts], axis=1)
        term = jnp.dot(lhs, weights(dw), preferred_element_type=F32)
        acc = term if acc is None else acc + term
    return acc


def first(pairs, weights, bias, y_row, blank_a):
    count, _, images, lanes = y_row.shape
    c = lax.axis_index("cols")
    row = lax.rem(lax.broadcasted_iota(jnp.int32, (1, 2 * lanes), 1), lanes) // (lanes // 2)
    act = jnp.maximum(blocks(pairs, weights, count) + bias, 0.0)
    act = jnp.where(row != blank_a, act, 0.0).astype(BF16)
    for b in range(2):
        y_row[:, b] = act[:, b * lanes : (b + 1) * lanes].reshape(count, images, lanes)
    blank = jnp.zeros((images, lanes), BF16)

    @pl.when(c == 0)
    def _():
        y_row[0, 0] = blank

    @pl.when(c == lax.axis_size("cols") - 1)
    def _():
        y_row[count - 1, 1] = blank


def second(pairs, weights, bias, out_pair):
    _, count, _, images, chans = out_pair.shape
    res = blocks(pairs, weights, count) + bias
    for b in range(2):
        for a in range(2):
            at = (2 * b + a) * chans
            out_pair[a, :, b] = res[:, at : at + chans].reshape(count, images, chans)


def conv_kernel(
    n_rows,
    n_cols,
    x_hbm,
    w1_hbm,
    b1_hbm,
    w2_hbm,
    b2_hbm,
    out,
    ymat,
    wt2,
    bias2,
    recv,
    xmat,
    wt1,
    bias1,
    xs,
    packed,
    w1s,
    w1own,
    w1all,
    w2s,
    b1s,
    b2s,
    load_sem,
    par_sem,
    send_sem,
    recv_sem,
    wsend_sem,
    wrecv_sem,
    swap_send_sem,
    swap_recv_sem,
    wswap_send_sem,
    wswap_recv_sem,
):
    chip_h, pairs = xs.shape[1:3]
    images = xs.shape[-1]
    tile_h, tile_j = chip_h // 2, pairs // n_cols
    win_j = tile_j + 2
    sources = n_rows * n_cols
    r, c = lax.axis_index("model"), lax.axis_index("cols")
    par = lax.rem(r, 2)
    me = r * n_cols + c
    chans = recv.shape[0] * 2

    tops = [tile_h - sum(CHUNK_ROWS[: k + 1]) for k in range(len(CHUNK_ROWS))]
    groups = (
        ((tops[0], chip_h - tops[0]),),
        *(((k, k + n), (chip_h - k - n, chip_h - k)) for k, n in zip(tops[1:], CHUNK_ROWS[1:])),
    )
    loads = []
    for g, spans in enumerate(groups):
        loads.append(
            [
                pltpu.make_async_copy(x_hbm.at[:, lo:hi], xs.at[:, lo:hi], load_sem.at[g, n])
                for n, (lo, hi) in enumerate(spans)
            ]
        )
    for copies in loads:
        for copy in copies:
            copy.start()
    params = [
        pltpu.make_async_copy(src, dst, par_sem.at[s])
        for s, (src, dst) in enumerate(((w1_hbm, w1s), (w2_hbm, w2s), (b1_hbm, b1s), (b2_hbm, b2s)))
    ]
    for copy in params:
        copy.start()

    barrier = pltpu.get_barrier_semaphore()
    to_cs = [lax.rem(c + k, n_cols) for k in range(n_cols)]

    def device(to_r, to_c):
        return {"model": to_r, "cols": to_c}

    to_rs = [lax.rem(r + k, n_rows) for k in range(n_rows)]
    for kr, kc in sorted(
        ((kr, kc) for kr in range(n_rows) for kc in range(n_cols) if kr or kc),
        key=lambda k: (k[1] not in (1, 2), k[0] not in (2, 3, 4, 5), k[1] == 2, k[0] < 4, -min(k[0], n_rows - k[0])),
    ):
        pl.semaphore_signal(barrier, inc=1, device_id=device(to_rs[kr], to_cs[kc]), device_id_type=MESH)

    def pack_rows(x, lo, hi):
        rows = hi - lo
        left, right = (xs[x, lo:hi, :, p].reshape(rows * pairs * 2, images) for p in range(2))
        both = jnp.concatenate([left, right], axis=1)
        packed[pl.ds(chip_h * x + lo, rows)] = both.reshape(rows, pairs, 2, 2 * images)

    def pack(g):
        for copy in loads[g]:
            copy.wait()

        def body(x, carry):
            for lo, hi in groups[g]:
                pack_rows(x, lo, hi)
            return carry

        lax.fori_loop(0, n_rows // 2, body, 0)

    last = tile_h + 4

    def rows_of(offset, count):
        def where(to_r):
            q = lax.rem(to_r, 2)
            src = tile_h * to_r + offset + (tile_h - count - 2 * offset) * q
            dst = offset + 2 + (last - count - 2 * offset - 3) * q
            return src, dst

        return where

    chunks = (
        *((n, rows_of(k, n), False) for k, n in zip(tops, CHUNK_ROWS)),
        (2, rows_of(-2, 2), True),
    )
    no_outer = (r == 0) | (r == n_rows - 1)
    at_edge = (c == 0) | (c == n_cols - 1)
    own_j = c == 0
    own_j = own_j.astype(jnp.int32)

    def send_tile(chunk, to_r, to_c, there):
        rows, where, is_outer = chunks[chunk]
        src, dst = where(to_r)
        skip = (to_c == 0).astype(jnp.int32)
        edge = (to_c == 0) | (to_c == n_cols - 1)
        if is_outer:
            there = there & (to_r > 0) & (to_r < n_rows - 1)

        def copy(count, src_j, dst_j):
            pltpu.make_async_remote_copy(
                src_ref=packed.at[pl.ds(src, rows), pl.ds(src_j, count)],
                dst_ref=recv.at[me, pl.ds(dst, rows), pl.ds(dst_j, count)],
                send_sem=send_sem.at[chunk],
                recv_sem=recv_sem.at[chunk],
                device_id=device(to_r, to_c),
                device_id_type=MESH,
            ).start()

        pl.when(there & edge)(lambda: copy(win_j - 1, tile_j * to_c - 1 + skip, skip))
        pl.when(there & jnp.logical_not(edge))(lambda: copy(win_j, tile_j * to_c - 1, 0))

    chips = n_rows // 2
    ahead_r, ahead_c = AHEAD

    def step(t, table):
        value = jnp.int32(table[-1])
        for k, entry in enumerate(table[:-1]):
            value = jnp.where(t == k, entry, value)
        return value

    def turn_to(t):
        dx = step(t, CHIPS_ALONG)
        return lax.rem(r // 2 + dx, chips), dx

    def send_chip(chunk, t, rest, where=None):
        x, dx = turn_to(t)
        way = 1 - 2 * lax.rem(par + t, 2)
        for other, dy in CHIP_ORDER:
            to_r = 2 * x + (1 - par if other else par)
            to_c = lax.rem(c + way * dy + n_cols, n_cols)
            there = True
            if not other and dy == 0:
                there = dx > 0
            if rest:
                there = there & jnp.logical_not((to_r == ahead_r) & (to_c == ahead_c))
            if where is not None:
                there = there & where(to_c)
            send_tile(chunk, to_r, to_c, there)

    def send_ahead(chunk):
        send_tile(chunk, jnp.int32(ahead_r), jnp.int32(ahead_c), (r != ahead_r) | (c != ahead_c))

    def send_chunk(chunk):

        def first_column(t, carry):
            x, _ = turn_to(t)
            for other in range(2):
                to_r = 2 * x + (1 - par if other else par)
                there = ((to_r != r) | (c != 0)) & (to_r != ahead_r)
                send_tile(chunk, to_r, jnp.int32(0), there)
            return carry

        where = None
        if chunk in COLUMN_FIRST:
            lax.fori_loop(0, chips, first_column, 0)
            where = lambda to_c: to_c > 0

        def body(t, carry):
            send_chip(chunk, t, True, where)
            return carry

        lax.fori_loop(0, chips, body, 0)

    params[0].wait()
    for dw in range(3):
        w1own[dw] = jnp.concatenate([w1s[1, dw], w1s[0, dw]], axis=1)
    w1own[3] = jnp.concatenate([w1s[2, 0], w1s[2, 1]], axis=1)
    w1own[4] = jnp.concatenate([w1s[2, 2], jnp.zeros_like(w1s[2, 2])], axis=1)
    w1all[r // 2, par, c] = w1own[...]

    for copy in loads[0]:
        copy.wait()
    pack_rows(turn_to(0)[0], *groups[0][0])
    pl.semaphore_wait(barrier, sources - 1)

    def send_weights():
        for kr in range(0, n_rows, 2):
            for kc in range(n_cols):
                if kr or kc:
                    pltpu.make_async_remote_copy(
                        src_ref=w1own,
                        dst_ref=w1all.at[r // 2, par, c],
                        send_sem=wsend_sem,
                        recv_sem=wrecv_sem,
                        device_id=device(to_rs[kr], to_cs[kc]),
                        device_id_type=MESH,
                    ).start()

    def pack_and_send(t, carry):
        pl.when(t < chips - 1)(lambda: pack_rows(turn_to(t + 1)[0], *groups[0][0]))
        send_chip(0, t, False)
        pl.when(t == 0)(send_weights)
        return carry

    lax.fori_loop(0, chips, pack_and_send, 0)

    pack(1)
    send_ahead(1)
    send_chunk(1)
    pack(2)
    send_ahead(2)
    send_ahead(3)
    send_chunk(2)
    send_chunk(3)

    def wait_bytes(ref, sem):
        pltpu.make_async_copy(ref, ref, sem).wait()

    w1_bytes = recv.at[0 : sources // 2 - 1, 0, 0:5]
    wait_bytes(w1_bytes, wrecv_sem)
    wait_bytes(w1_bytes, wsend_sem)
    partner = device(r + 1 - 2 * par, c)
    w_swap = pltpu.make_async_remote_copy(
        src_ref=w1all.at[:, par],
        dst_ref=w1all.at[:, par],
        send_sem=wswap_send_sem,
        recv_sem=wswap_recv_sem,
        device_id=partner,
        device_id_type=MESH,
    )
    w_swap.start()

    def own_rows(chunk):
        rows, where, _ = chunks[chunk]
        src, dst = where(r)

        def copy(count, src_j, dst_j):
            for h in range(rows):
                recv[me, dst + h, pl.ds(dst_j, count)] = packed[src + h, pl.ds(src_j, count)]

        pl.when(at_edge)(lambda: copy(win_j - 1, tile_j * c - 1 + own_j, own_j))
        pl.when(jnp.logical_not(at_edge))(lambda: copy(win_j, tile_j * c - 1, 0))

    for chunk in range(3):
        own_rows(chunk)
    pl.when(jnp.logical_not(no_outer))(lambda: own_rows(3))

    zero_row = jnp.zeros((win_j, 2, 2 * images), BF16)
    zero_col = jnp.zeros((tile_h + 2, 2, 2 * images), BF16)

    def clear(s, carry):
        recv[s, last * (1 - par)] = zero_row
        return carry

    def clear_outer(s, carry):
        recv[s, (last - 1) * par] = zero_row
        recv[s, (last - 1) * par + 1] = zero_row
        return carry

    def clear_edge(s, carry):
        recv[s, pl.ds(3 * par, tile_h + 2), (win_j - 1) * (1 - own_j)] = zero_col
        return carry

    lax.fori_loop(0, sources, clear, 0)
    pl.when(no_outer)(lambda: (lax.fori_loop(0, sources, clear_outer, 0), None)[1])
    pl.when(at_edge)(lambda: (lax.fori_loop(0, sources, clear_edge, 0), None)[1])

    low = lax.broadcasted_iota(jnp.int32, (chans, 2 * chans), 1) < chans

    def spread(wt, u, v, dw):
        ur, vr = pltpu.roll(u, chans, 1), pltpu.roll(v, chans, 1)
        zero = jnp.zeros_like(u)
        tiles = (jnp.where(low, ur, zero), u, jnp.where(low, v, ur), jnp.where(low, zero, vr))
        for k, tile in enumerate(tiles):
            tile = tile.astype(BF16)
            for b in range(2):
                wt[dw + b, k * chans : (k + 1) * chans, b * 2 * chans : (b + 1) * 2 * chans] = tile

    def blank(wt):
        zero = jnp.zeros((4 * chans, 2 * chans), BF16)
        wt[3, :, 0 : 2 * chans] = zero
        wt[0, :, 2 * chans : 4 * chans] = zero

    for copy in params[1:]:
        copy.wait()
    blank(wt1)
    blank(wt2)
    for dw in range(3):
        w = [w2s[dh, dw].astype(F32) for dh in range(3)]
        spread(
            wt2,
            jnp.concatenate([w[1], w[0]], axis=1),
            jnp.concatenate([w[2], jnp.zeros_like(w[2])], axis=1),
            dw,
        )
    bias1[...] = jnp.concatenate([b1s[...]] * 4, axis=1)
    bias2[...] = jnp.concatenate([b2s[...]] * 4, axis=1)

    def arrived(chunk):
        def wait(count):
            wait_bytes(recv.at[0 : sources - 1, 0 : chunks[chunk][0], 0:count], recv_sem.at[chunk])

        pl.when(at_edge)(lambda: wait(win_j - 1))
        pl.when(jnp.logical_not(at_edge))(lambda: wait(win_j))

    arrived(0)
    give = tile_h - (tile_h - 3) * par
    land = tile_h + 2 - (tile_h + 1) * (1 - par)
    swap = pltpu.make_async_remote_copy(
        src_ref=recv.at[:, pl.ds(give, 2)],
        dst_ref=recv.at[:, pl.ds(land, 2)],
        send_sem=swap_send_sem,
        recv_sem=swap_recv_sem,
        device_id=partner,
        device_id_type=MESH,
    )
    swap.start()

    w_swap.wait()
    u = [w1all[:, :, :, k].reshape(chans, 2 * chans).astype(F32) for k in range(5)]
    for dw in range(3):
        v = (u[3], pltpu.roll(u[3], chans, 1), u[4])[dw]
        spread(wt1, u[dw], jnp.where(low, v, 0.0), dw)

    x_pairs, z_pairs = xmat.shape[0], ymat.shape[0]
    o_pairs = z_pairs - 1

    def nth(n, count):
        return (count - 1) * (1 - par) + n * (2 * par - 1)

    def turn_one(n, carry):
        i = nth(n, x_pairs)

        def put(j, value):
            xmat[i, j] = value

        turn(recv, i, put)
        return carry

    def first_one(n, carry):
        i = nth(n, z_pairs)
        fill = jnp.where(n == 0, 1 - par, 2)
        out_of = jnp.where(n == z_pairs - 1, jnp.where(r == 0, 0, jnp.where(r == n_rows - 1, 1, 2)), 2)
        blank_a = jnp.where(fill < 2, fill, out_of)
        first((xmat.at[i], xmat.at[i + 1]), lambda dw: wt1[dw], bias1[...], ymat.at[i], blank_a)
        return carry

    def second_one(n, carry):
        i = nth(n, o_pairs)
        second((ymat.at[i], ymat.at[i + 1]), lambda dw: wt2[dw], bias2[...], out.at[pl.ds(2 * i, 2)])
        return carry

    def stage(s, carry):
        @pl.when(s == 0)
        def _():
            swap.wait()

        for k in range(1, 4):
            there = s == k
            if k == 3:
                there = there & jnp.logical_not(no_outer)
            pl.when(there)(lambda k=k: arrived(k))

        for ends, one in ((TURNS, turn_one), (FIRSTS, first_one), (SECONDS, second_one)):
            lax.fori_loop(step(s, (0, *ends[:-1])), step(s, ends), one, 0)
        return carry

    lax.fori_loop(0, 4, stage, 0)

    per_edge = n_rows * 2
    for chunk in range(4):
        rows = chunks[chunk][0]
        n_r = n_rows - 2 if chunk == 3 else n_rows
        counts = (n_r * 2, n_r * (n_cols - 2))

        def drain(edge_n, inner_n, rows=rows, chunk=chunk):
            wait_bytes(recv.at[0:edge_n, 0:rows, 0 : win_j - 1], send_sem.at[chunk])
            wait_bytes(recv.at[0:inner_n, 0:rows, 0:win_j], send_sem.at[chunk])

        def drain_own(chunk=chunk, counts=counts, drain=drain):
            pl.when(at_edge)(lambda: drain(counts[0] - 1, counts[1]))
            pl.when(jnp.logical_not(at_edge))(lambda: drain(counts[0], counts[1] - 1))

        if chunk == 3:
            pl.when(no_outer)(lambda: drain(*counts))
            pl.when(jnp.logical_not(no_outer))(drain_own)
        else:
            drain_own()


def tail_kernel(tile, ymat, wt2, bias2, out_hbm, o_new, sem):
    par = lax.rem(lax.axis_index("model"), 2)
    rows = out_hbm.shape[0]
    o_pairs = ymat.shape[0] - 1
    late = (rows - 2) * par
    here = 2 * (1 - par)

    def start(k, carry):
        pltpu.make_async_copy(tile.at[par + k], out_hbm.at[k], sem.at[0]).start()
        return carry

    lax.fori_loop(here, here + rows - 2, start, 0)
    i = (o_pairs - 1) * par
    second((ymat.at[i], ymat.at[i + 1]), lambda dw: wt2[dw], bias2[...], o_new)
    last = pltpu.make_async_copy(o_new, out_hbm.at[pl.ds(late, 2)], sem.at[1])
    last.start()
    pltpu.make_async_copy(tile.at[0 : rows - 2], out_hbm.at[0 : rows - 2], sem.at[0]).wait()
    last.wait()


def solution(mesh):
    n_rows = mesh.shape["model"]
    n_cols = mesh.shape["cols"]

    def run_local(x_in, w_conv1, b_conv1, w_conv2, b_conv2):
        images, height, width, own_chans = x_in.shape
        sources = n_rows * n_cols
        chans = own_chans * sources
        pairs = width // 2
        tile_h, tile_j = height // n_rows, pairs // n_cols
        win_j = tile_j + 2
        x_pairs, z_pairs = (tile_h + 5) // 2, (tile_h + 3) // 2
        x_t = jnp.transpose(x_in, (1, 2, 3, 0)).reshape(n_rows // 2, 2 * tile_h, pairs, 2, own_chans, images)
        args = (x_t, w_conv1, b_conv1.reshape(1, chans), w_conv2, b_conv2.reshape(1, chans))
        hbm = pl.BlockSpec(memory_space=pltpu.HBM)
        vmem = pl.BlockSpec(memory_space=pltpu.VMEM)
        kept = (
            pltpu.VMEM((2 * (z_pairs - 1), tile_j, 2, images, chans), F32),
            pltpu.VMEM((z_pairs, win_j - 1, 2, images, 2 * chans), BF16),
            pltpu.VMEM((4, 4 * chans, 4 * chans), BF16),
            pltpu.VMEM((1, 4 * chans), F32),
        )
        state = pl.pallas_call(
            functools.partial(conv_kernel, n_rows, n_cols),
            out_shape=kept,
            in_specs=[hbm] * 5,
            out_specs=[vmem] * len(kept),
            scratch_shapes=[
                pltpu.VMEM((sources, 2 * x_pairs, win_j, own_chans, 2 * images), BF16),
                pltpu.VMEM((x_pairs, win_j, 2, images, 2 * chans), BF16),
                pltpu.VMEM((4, 4 * chans, 4 * chans), BF16),
                pltpu.VMEM((1, 4 * chans), F32),
                pltpu.VMEM((n_rows // 2, 2 * tile_h, pairs, 2, own_chans, images), BF16),
                pltpu.VMEM((height, pairs, own_chans, 2 * images), BF16),
                pltpu.VMEM((3, 3, own_chans, chans), BF16),
                pltpu.VMEM((5, own_chans, 2 * chans), BF16),
                pltpu.VMEM((n_rows // 2, 2, n_cols, 5, own_chans, 2 * chans), BF16),
                pltpu.VMEM((3, 3, chans, chans), BF16),
                pltpu.VMEM((1, chans), F32),
                pltpu.VMEM((1, chans), F32),
                pltpu.SemaphoreType.DMA((3, 2)),
                pltpu.SemaphoreType.DMA((4,)),
                pltpu.SemaphoreType.DMA((4,)),
                pltpu.SemaphoreType.DMA((4,)),
            ]
            + [pltpu.SemaphoreType.DMA] * 6,
            compiler_params=pltpu.CompilerParams(
                collective_id=0, has_side_effects=True, vmem_limit_bytes=24 << 20
            ),
            name="conv",
        )(*(pltpu.with_memory_space_constraint(a, pltpu.HBM) for a in args))
        out = pl.pallas_call(
            tail_kernel,
            out_shape=jax.ShapeDtypeStruct((tile_h, tile_j, 2, images, chans), F32),
            in_specs=[vmem] * len(kept),
            out_specs=pl.BlockSpec(memory_space=pl.ANY),
            scratch_shapes=[
                pltpu.VMEM((2, tile_j, 2, images, chans), F32),
                pltpu.SemaphoreType.DMA((2,)),
            ],
            compiler_params=pltpu.CompilerParams(vmem_limit_bytes=8 << 20),
            name="tail",
        )(*state)
        out = out.reshape(tile_h, 2 * tile_j, images, chans)
        return jnp.transpose(out, (2, 0, 1, 3))

    group = ("model", "cols")
    return jax.shard_map(
        run_local,
        mesh=mesh,
        in_specs=(P("data", None, None, group), P(None, None, group, None), P(), P(), P()),
        out_specs=P("data", "model", "cols", None),
        check_vma=False,
    )
```

```python
import functools

import jax
import jax.numpy as jnp
from jax import lax
from jax.experimental import pallas as pl
from jax.experimental.pallas import tpu as pltpu
from jax.sharding import PartitionSpec as P

MESH = pl.DeviceIdType.MESH
BF16 = jnp.bfloat16
F32 = jnp.float32
CHUNK_ROWS = (2, 3, 2)
TURNS, FIRSTS, SECONDS = (2, 4, 5, 6), (1, 3, 4, 5), (0, 2, 3, 3)
AHEAD = (1, 0)
COLUMN_FIRST = (2, 3)
CHIPS_ALONG = (1, 3, 2, 0)
CHIP_ORDER = tuple((other, dy) for other in (0, 1) for dy in (0, 1, -1, 2))


def turn(recv, i, put):
    sources, _, win_j, own_chans, lanes = recv.shape
    chans = sources * own_chans
    for j in range(win_j):
        top = recv[:, 2 * i, j].reshape(chans, lanes)
        under = recv[:, 2 * i + 1, j].reshape(chans, lanes)
        put(j, jnp.concatenate([top, under], axis=0).T.reshape(2, lanes // 2, 2 * chans))


def blocks(pairs, weights, count):
    acc = None
    for dw in range(4):
        parts = [view[dw // 2 : dw // 2 + count, dw % 2] for view in pairs]
        lhs = jnp.concatenate([p.reshape(count * p.shape[1], p.shape[2]) for p in parts], axis=1)
        term = jnp.dot(lhs, weights(dw), preferred_element_type=F32)
        acc = term if acc is None else acc + term
    return acc


def first(pairs, weights, bias, y_row, blank_a):
    count, _, images, lanes = y_row.shape
    c = lax.axis_index("cols")
    row = lax.rem(lax.broadcasted_iota(jnp.int32, (1, 2 * lanes), 1), lanes) // (lanes // 2)
    act = jnp.maximum(blocks(pairs, weights, count) + bias, 0.0)
    act = jnp.where(row != blank_a, act, 0.0).astype(BF16)
    for b in range(2):
        y_row[:, b] = act[:, b * lanes : (b + 1) * lanes].reshape(count, images, lanes)
    blank = jnp.zeros((images, lanes), BF16)

    @pl.when(c == 0)
    def _():
        y_row[0, 0] = blank

    @pl.when(c == lax.axis_size("cols") - 1)
    def _():
        y_row[count - 1, 1] = blank


def second(pairs, weights, bias, out_pair):
    _, count, _, images, chans = out_pair.shape
    res = blocks(pairs, weights, count) + bias
    for b in range(2):
        for a in range(2):
            at = (2 * b + a) * chans
            out_pair[a, :, b] = res[:, at : at + chans].reshape(count, images, chans)


def conv_kernel(
    n_rows,
    n_cols,
    x_hbm,
    w1_hbm,
    b1_hbm,
    w2_hbm,
    b2_hbm,
    out,
    ymat,
    wt2,
    bias2,
    recv,
    xmat,
    wt1,
    bias1,
    xs,
    packed,
    w1s,
    w1own,
    w1all,
    w2s,
    b1s,
    b2s,
    load_sem,
    par_sem,
    send_sem,
    recv_sem,
    wsend_sem,
    wrecv_sem,
    swap_send_sem,
    swap_recv_sem,
    wswap_send_sem,
    wswap_recv_sem,
):
    chip_h, pairs = xs.shape[1:3]
    images = xs.shape[-1]
    tile_h, tile_j = chip_h // 2, pairs // n_cols
    win_j = tile_j + 2
    sources = n_rows * n_cols
    r, c = lax.axis_index("model"), lax.axis_index("cols")
    par = lax.rem(r, 2)
    me = r * n_cols + c
    chans = recv.shape[0] * 2

    tops = [tile_h - sum(CHUNK_ROWS[: k + 1]) for k in range(len(CHUNK_ROWS))]
    groups = (
        ((tops[0], chip_h - tops[0]),),
        *(((k, k + n), (chip_h - k - n, chip_h - k)) for k, n in zip(tops[1:], CHUNK_ROWS[1:])),
    )
    loads = []
    for g, spans in enumerate(groups):
        loads.append(
            [
                pltpu.make_async_copy(x_hbm.at[:, lo:hi], xs.at[:, lo:hi], load_sem.at[g, n])
                for n, (lo, hi) in enumerate(spans)
            ]
        )
    for copies in loads:
        for copy in copies:
            copy.start()
    params = [
        pltpu.make_async_copy(src, dst, par_sem.at[s])
        for s, (src, dst) in enumerate(((w1_hbm, w1s), (w2_hbm, w2s), (b1_hbm, b1s), (b2_hbm, b2s)))
    ]
    for copy in params:
        copy.start()

    barrier = pltpu.get_barrier_semaphore()
    to_cs = [lax.rem(c + k, n_cols) for k in range(n_cols)]

    def device(to_r, to_c):
        return {"model": to_r, "cols": to_c}

    to_rs = [lax.rem(r + k, n_rows) for k in range(n_rows)]
    for kr, kc in sorted(
        ((kr, kc) for kr in range(n_rows) for kc in range(n_cols) if kr or kc),
        key=lambda k: (k[1] not in (1, 2), k[0] not in (2, 3, 4, 5), k[1] == 2, k[0] < 4, -min(k[0], n_rows - k[0])),
    ):
        pl.semaphore_signal(barrier, inc=1, device_id=device(to_rs[kr], to_cs[kc]), device_id_type=MESH)

    def pack_rows(x, lo, hi):
        rows = hi - lo
        left, right = (xs[x, lo:hi, :, p].reshape(rows * pairs * 2, images) for p in range(2))
        both = jnp.concatenate([left, right], axis=1)
        packed[pl.ds(chip_h * x + lo, rows)] = both.reshape(rows, pairs, 2, 2 * images)

    def pack(g):
        for copy in loads[g]:
            copy.wait()

        def body(x, carry):
            for lo, hi in groups[g]:
                pack_rows(x, lo, hi)
            return carry

        lax.fori_loop(0, n_rows // 2, body, 0)

    last = tile_h + 4

    def rows_of(offset, count):
        def where(to_r):
            q = lax.rem(to_r, 2)
            src = tile_h * to_r + offset + (tile_h - count - 2 * offset) * q
            dst = offset + 2 + (last - count - 2 * offset - 3) * q
            return src, dst

        return where

    chunks = (
        *((n, rows_of(k, n), False) for k, n in zip(tops, CHUNK_ROWS)),
        (2, rows_of(-2, 2), True),
    )
    no_outer = (r == 0) | (r == n_rows - 1)
    at_edge = (c == 0) | (c == n_cols - 1)
    own_j = c == 0
    own_j = own_j.astype(jnp.int32)

    def send_tile(chunk, to_r, to_c, there):
        rows, where, is_outer = chunks[chunk]
        src, dst = where(to_r)
        skip = (to_c == 0).astype(jnp.int32)
        edge = (to_c == 0) | (to_c == n_cols - 1)
        if is_outer:
            there = there & (to_r > 0) & (to_r < n_rows - 1)

        def copy(count, src_j, dst_j):
            pltpu.make_async_remote_copy(
                src_ref=packed.at[pl.ds(src, rows), pl.ds(src_j, count)],
                dst_ref=recv.at[me, pl.ds(dst, rows), pl.ds(dst_j, count)],
                send_sem=send_sem.at[chunk],
                recv_sem=recv_sem.at[chunk],
                device_id=device(to_r, to_c),
                device_id_type=MESH,
            ).start()

        pl.when(there & edge)(lambda: copy(win_j - 1, tile_j * to_c - 1 + skip, skip))
        pl.when(there & jnp.logical_not(edge))(lambda: copy(win_j, tile_j * to_c - 1, 0))

    chips = n_rows // 2
    ahead_r, ahead_c = AHEAD

    def step(t, table):
        value = jnp.int32(table[-1])
        for k, entry in enumerate(table[:-1]):
            value = jnp.where(t == k, entry, value)
        return value

    def turn_to(t):
        dx = step(t, CHIPS_ALONG)
        return lax.rem(r // 2 + dx, chips), dx

    def send_chip(chunk, t, rest, where=None):
        x, dx = turn_to(t)
        way = 1 - 2 * lax.rem(par + t, 2)
        for other, dy in CHIP_ORDER:
            to_r = 2 * x + (1 - par if other else par)
            to_c = lax.rem(c + way * dy + n_cols, n_cols)
            there = True
            if not other and dy == 0:
                there = dx > 0
            if rest:
                there = there & jnp.logical_not((to_r == ahead_r) & (to_c == ahead_c))
            if where is not None:
                there = there & where(to_c)
            send_tile(chunk, to_r, to_c, there)

    def send_ahead(chunk):
        send_tile(chunk, jnp.int32(ahead_r), jnp.int32(ahead_c), (r != ahead_r) | (c != ahead_c))

    def send_chunk(chunk):

        def first_column(t, carry):
            x, _ = turn_to(t)
            for other in range(2):
                to_r = 2 * x + (1 - par if other else par)
                there = ((to_r != r) | (c != 0)) & (to_r != ahead_r)
                send_tile(chunk, to_r, jnp.int32(0), there)
            return carry

        where = None
        if chunk in COLUMN_FIRST:
            lax.fori_loop(0, chips, first_column, 0)
            where = lambda to_c: to_c > 0

        def body(t, carry):
            send_chip(chunk, t, True, where)
            return carry

        lax.fori_loop(0, chips, body, 0)

    params[0].wait()
    for dw in range(3):
        w1own[dw] = jnp.concatenate([w1s[1, dw], w1s[0, dw]], axis=1)
    w1own[3] = jnp.concatenate([w1s[2, 0], w1s[2, 1]], axis=1)
    w1own[4] = jnp.concatenate([w1s[2, 2], jnp.zeros_like(w1s[2, 2])], axis=1)
    w1all[r // 2, par, c] = w1own[...]

    for copy in loads[0]:
        copy.wait()
    pack_rows(turn_to(0)[0], *groups[0][0])
    pl.semaphore_wait(barrier, sources - 1)

    def send_weights():
        for kr in range(0, n_rows, 2):
            for kc in range(n_cols):
                if kr or kc:
                    pltpu.make_async_remote_copy(
                        src_ref=w1own,
                        dst_ref=w1all.at[r // 2, par, c],
                        send_sem=wsend_sem,
                        recv_sem=wrecv_sem,
                        device_id=device(to_rs[kr], to_cs[kc]),
                        device_id_type=MESH,
                    ).start()

    def pack_and_send(t, carry):
        pl.when(t < chips - 1)(lambda: pack_rows(turn_to(t + 1)[0], *groups[0][0]))
        send_chip(0, t, False)
        pl.when(t == 0)(send_weights)
        return carry

    lax.fori_loop(0, chips, pack_and_send, 0)

    pack(1)
    send_ahead(1)
    send_chunk(1)
    pack(2)
    send_ahead(2)
    send_ahead(3)
    send_chunk(2)
    send_chunk(3)

    def wait_bytes(ref, sem):
        pltpu.make_async_copy(ref, ref, sem).wait()

    w1_bytes = recv.at[0 : sources // 2 - 1, 0, 0:5]
    wait_bytes(w1_bytes, wrecv_sem)
    wait_bytes(w1_bytes, wsend_sem)
    partner = device(r + 1 - 2 * par, c)
    w_swap = pltpu.make_async_remote_copy(
        src_ref=w1all.at[:, par],
        dst_ref=w1all.at[:, par],
        send_sem=wswap_send_sem,
        recv_sem=wswap_recv_sem,
        device_id=partner,
        device_id_type=MESH,
    )
    w_swap.start()

    def own_rows(chunk):
        rows, where, _ = chunks[chunk]
        src, dst = where(r)

        def copy(count, src_j, dst_j):
            for h in range(rows):
                recv[me, dst + h, pl.ds(dst_j, count)] = packed[src + h, pl.ds(src_j, count)]

        pl.when(at_edge)(lambda: copy(win_j - 1, tile_j * c - 1 + own_j, own_j))
        pl.when(jnp.logical_not(at_edge))(lambda: copy(win_j, tile_j * c - 1, 0))

    for chunk in range(3):
        own_rows(chunk)
    pl.when(jnp.logical_not(no_outer))(lambda: own_rows(3))

    zero_row = jnp.zeros((win_j, 2, 2 * images), BF16)
    zero_col = jnp.zeros((tile_h + 2, 2, 2 * images), BF16)

    def clear(s, carry):
        recv[s, last * (1 - par)] = zero_row
        return carry

    def clear_outer(s, carry):
        recv[s, (last - 1) * par] = zero_row
        recv[s, (last - 1) * par + 1] = zero_row
        return carry

    def clear_edge(s, carry):
        recv[s, pl.ds(3 * par, tile_h + 2), (win_j - 1) * (1 - own_j)] = zero_col
        return carry

    lax.fori_loop(0, sources, clear, 0)
    pl.when(no_outer)(lambda: (lax.fori_loop(0, sources, clear_outer, 0), None)[1])
    pl.when(at_edge)(lambda: (lax.fori_loop(0, sources, clear_edge, 0), None)[1])

    low = lax.broadcasted_iota(jnp.int32, (chans, 2 * chans), 1) < chans

    def spread(wt, u, v, dw):
        ur, vr = pltpu.roll(u, chans, 1), pltpu.roll(v, chans, 1)
        zero = jnp.zeros_like(u)
        tiles = (jnp.where(low, ur, zero), u, jnp.where(low, v, ur), jnp.where(low, zero, vr))
        for k, tile in enumerate(tiles):
            tile = tile.astype(BF16)
            for b in range(2):
                wt[dw + b, k * chans : (k + 1) * chans, b * 2 * chans : (b + 1) * 2 * chans] = tile

    def blank(wt):
        zero = jnp.zeros((4 * chans, 2 * chans), BF16)
        wt[3, :, 0 : 2 * chans] = zero
        wt[0, :, 2 * chans : 4 * chans] = zero

    for copy in params[1:]:
        copy.wait()
    blank(wt1)
    blank(wt2)
    for dw in range(3):
        w = [w2s[dh, dw].astype(F32) for dh in range(3)]
        spread(
            wt2,
            jnp.concatenate([w[1], w[0]], axis=1),
            jnp.concatenate([w[2], jnp.zeros_like(w[2])], axis=1),
            dw,
        )
    bias1[...] = jnp.concatenate([b1s[...]] * 4, axis=1)
    bias2[...] = jnp.concatenate([b2s[...]] * 4, axis=1)

    def arrived(chunk):
        def wait(count):
            wait_bytes(recv.at[0 : sources - 1, 0 : chunks[chunk][0], 0:count], recv_sem.at[chunk])

        pl.when(at_edge)(lambda: wait(win_j - 1))
        pl.when(jnp.logical_not(at_edge))(lambda: wait(win_j))

    arrived(0)
    give = tile_h - (tile_h - 3) * par
    land = tile_h + 2 - (tile_h + 1) * (1 - par)
    swap = pltpu.make_async_remote_copy(
        src_ref=recv.at[:, pl.ds(give, 2)],
        dst_ref=recv.at[:, pl.ds(land, 2)],
        send_sem=swap_send_sem,
        recv_sem=swap_recv_sem,
        device_id=partner,
        device_id_type=MESH,
    )
    swap.start()

    w_swap.wait()
    u = [w1all[:, :, :, k].reshape(chans, 2 * chans).astype(F32) for k in range(5)]
    for dw in range(3):
        v = (u[3], pltpu.roll(u[3], chans, 1), u[4])[dw]
        spread(wt1, u[dw], jnp.where(low, v, 0.0), dw)

    x_pairs, z_pairs = xmat.shape[0], ymat.shape[0]
    o_pairs = z_pairs - 1

    def nth(n, count):
        return (count - 1) * (1 - par) + n * (2 * par - 1)

    def turn_one(n, carry):
        i = nth(n, x_pairs)

        def put(j, value):
            xmat[i, j] = value

        turn(recv, i, put)
        return carry

    def first_one(n, carry):
        i = nth(n, z_pairs)
        fill = jnp.where(n == 0, 1 - par, 2)
        out_of = jnp.where(n == z_pairs - 1, jnp.where(r == 0, 0, jnp.where(r == n_rows - 1, 1, 2)), 2)
        blank_a = jnp.where(fill < 2, fill, out_of)
        first((xmat.at[i], xmat.at[i + 1]), lambda dw: wt1[dw], bias1[...], ymat.at[i], blank_a)
        return carry

    def second_one(n, carry):
        i = nth(n, o_pairs)
        second((ymat.at[i], ymat.at[i + 1]), lambda dw: wt2[dw], bias2[...], out.at[pl.ds(2 * i, 2)])
        return carry

    def stage(s, carry):
        @pl.when(s == 0)
        def _():
            swap.wait()

        for k in range(1, 4):
            there = s == k
            if k == 3:
                there = there & jnp.logical_not(no_outer)
            pl.when(there)(lambda k=k: arrived(k))

        for ends, one in ((TURNS, turn_one), (FIRSTS, first_one), (SECONDS, second_one)):
            lax.fori_loop(step(s, (0, *ends[:-1])), step(s, ends), one, 0)
        return carry

    lax.fori_loop(0, 4, stage, 0)

    per_edge = n_rows * 2
    for chunk in range(4):
        rows = chunks[chunk][0]
        n_r = n_rows - 2 if chunk == 3 else n_rows
        counts = (n_r * 2, n_r * (n_cols - 2))

        def drain(edge_n, inner_n, rows=rows, chunk=chunk):
            wait_bytes(recv.at[0:edge_n, 0:rows, 0 : win_j - 1], send_sem.at[chunk])
            wait_bytes(recv.at[0:inner_n, 0:rows, 0:win_j], send_sem.at[chunk])

        def drain_own(chunk=chunk, counts=counts, drain=drain):
            pl.when(at_edge)(lambda: drain(counts[0] - 1, counts[1]))
            pl.when(jnp.logical_not(at_edge))(lambda: drain(counts[0], counts[1] - 1))

        if chunk == 3:
            pl.when(no_outer)(lambda: drain(*counts))
            pl.when(jnp.logical_not(no_outer))(drain_own)
        else:
            drain_own()


def tail_kernel(tile, ymat, wt2, bias2, out_hbm, o_new, sem):
    par = lax.rem(lax.axis_index("model"), 2)
    rows = out_hbm.shape[0]
    o_pairs = ymat.shape[0] - 1
    late = (rows - 2) * par
    here = 2 * (1 - par)

    def start(k, carry):
        pltpu.make_async_copy(tile.at[par + k], out_hbm.at[k], sem.at[0]).start()
        return carry

    lax.fori_loop(here, here + rows - 2, start, 0)
    i = (o_pairs - 1) * par
    second((ymat.at[i], ymat.at[i + 1]), lambda dw: wt2[dw], bias2[...], o_new)
    last = pltpu.make_async_copy(o_new, out_hbm.at[pl.ds(late, 2)], sem.at[1])
    last.start()
    pltpu.make_async_copy(tile.at[0 : rows - 2], out_hbm.at[0 : rows - 2], sem.at[0]).wait()
    last.wait()


def solution(mesh):
    n_rows = mesh.shape["model"]
    n_cols = mesh.shape["cols"]

    def run_local(x_in, w_conv1, b_conv1, w_conv2, b_conv2):
        images, height, width, own_chans = x_in.shape
        sources = n_rows * n_cols
        chans = own_chans * sources
        pairs = width // 2
        tile_h, tile_j = height // n_rows, pairs // n_cols
        win_j = tile_j + 2
        x_pairs, z_pairs = (tile_h + 5) // 2, (tile_h + 3) // 2
        x_t = jnp.transpose(x_in, (1, 2, 3, 0)).reshape(n_rows // 2, 2 * tile_h, pairs, 2, own_chans, images)
        args = (x_t, w_conv1, b_conv1.reshape(1, chans), w_conv2, b_conv2.reshape(1, chans))
        hbm = pl.BlockSpec(memory_space=pltpu.HBM)
        vmem = pl.BlockSpec(memory_space=pltpu.VMEM)
        kept = (
            pltpu.VMEM((2 * (z_pairs - 1), tile_j, 2, images, chans), F32),
            pltpu.VMEM((z_pairs, win_j - 1, 2, images, 2 * chans), BF16),
            pltpu.VMEM((4, 4 * chans, 4 * chans), BF16),
            pltpu.VMEM((1, 4 * chans), F32),
        )
        state = pl.pallas_call(
            functools.partial(conv_kernel, n_rows, n_cols),
            out_shape=kept,
            in_specs=[hbm] * 5,
            out_specs=[vmem] * len(kept),
            scratch_shapes=[
                pltpu.VMEM((sources, 2 * x_pairs, win_j, own_chans, 2 * images), BF16),
                pltpu.VMEM((x_pairs, win_j, 2, images, 2 * chans), BF16),
                pltpu.VMEM((4, 4 * chans, 4 * chans), BF16),
                pltpu.VMEM((1, 4 * chans), F32),
                pltpu.VMEM((n_rows // 2, 2 * tile_h, pairs, 2, own_chans, images), BF16),
                pltpu.VMEM((height, pairs, own_chans, 2 * images), BF16),
                pltpu.VMEM((3, 3, own_chans, chans), BF16),
                pltpu.VMEM((5, own_chans, 2 * chans), BF16),
                pltpu.VMEM((n_rows // 2, 2, n_cols, 5, own_chans, 2 * chans), BF16),
                pltpu.VMEM((3, 3, chans, chans), BF16),
                pltpu.VMEM((1, chans), F32),
                pltpu.VMEM((1, chans), F32),
                pltpu.SemaphoreType.DMA((3, 2)),
                pltpu.SemaphoreType.DMA((4,)),
                pltpu.SemaphoreType.DMA((4,)),
                pltpu.SemaphoreType.DMA((4,)),
            ]
            + [pltpu.SemaphoreType.DMA] * 6,
            compiler_params=pltpu.CompilerParams(
                collective_id=0, has_side_effects=True, vmem_limit_bytes=24 << 20
            ),
            name="conv",
        )(*(pltpu.with_memory_space_constraint(a, pltpu.HBM) for a in args))
        out = pl.pallas_call(
            tail_kernel,
            out_shape=jax.ShapeDtypeStruct((tile_h, tile_j, 2, images, chans), F32),
            in_specs=[vmem] * len(kept),
            out_specs=pl.BlockSpec(memory_space=pl.ANY),
            scratch_shapes=[
                pltpu.VMEM((2, tile_j, 2, images, chans), F32),
                pltpu.SemaphoreType.DMA((2,)),
            ],
            compiler_params=pltpu.CompilerParams(vmem_limit_bytes=8 << 20),
            name="tail",
        )(*state)
        out = out.reshape(tile_h, 2 * tile_j, images, chans)
        return jnp.transpose(out, (2, 0, 1, 3))

    group = ("model", "cols")
    return jax.shard_map(
        run_local,
        mesh=mesh,
        in_specs=(P("data", None, None, group), P(None, None, group, None), P(), P(), P()),
        out_specs=P("data", "model", "cols", None),
        check_vma=False,
    )
```

```python
import functools

import jax
import jax.numpy as jnp
from jax import lax
from jax.experimental import pallas as pl
from jax.experimental.pallas import tpu as pltpu
from jax.sharding import PartitionSpec as P

MESH = pl.DeviceIdType.MESH
BF16 = jnp.bfloat16
F32 = jnp.float32
CHUNK_ROWS = (2, 3, 2)
TURNS, FIRSTS, SECONDS = (2, 4, 5, 6), (1, 3, 4, 5), (0, 2, 3, 3)
AHEAD = (1, 0)
COLUMN_FIRST = (2, 3)
CHIPS_ALONG = (3, 1, 2, 0)
CHIP_ORDER = tuple((other, dy) for other in (0, 1) for dy in (1, -1, 0, 2))


def turn(recv, i, put):
    sources, _, win_j, own_chans, lanes = recv.shape
    chans = sources * own_chans
    for j in range(win_j):
        top = recv[:, 2 * i, j].reshape(chans, lanes)
        under = recv[:, 2 * i + 1, j].reshape(chans, lanes)
        put(j, jnp.concatenate([top, under], axis=0).T.reshape(2, lanes // 2, 2 * chans))


def blocks(pairs, weights, count):
    acc = None
    for dw in range(4):
        parts = [view[dw // 2 : dw // 2 + count, dw % 2] for view in pairs]
        lhs = jnp.concatenate([p.reshape(count * p.shape[1], p.shape[2]) for p in parts], axis=1)
        term = jnp.dot(lhs, weights(dw), preferred_element_type=F32)
        acc = term if acc is None else acc + term
    return acc


def first(pairs, weights, bias, y_row, blank_a):
    count, _, images, lanes = y_row.shape
    c = lax.axis_index("cols")
    row = lax.rem(lax.broadcasted_iota(jnp.int32, (1, 2 * lanes), 1), lanes) // (lanes // 2)
    act = jnp.maximum(blocks(pairs, weights, count) + bias, 0.0)
    act = jnp.where(row != blank_a, act, 0.0).astype(BF16)
    for b in range(2):
        y_row[:, b] = act[:, b * lanes : (b + 1) * lanes].reshape(count, images, lanes)
    blank = jnp.zeros((images, lanes), BF16)

    @pl.when(c == 0)
    def _():
        y_row[0, 0] = blank

    @pl.when(c == lax.axis_size("cols") - 1)
    def _():
        y_row[count - 1, 1] = blank


def second(pairs, weights, bias, out_pair):
    _, count, _, images, chans = out_pair.shape
    res = blocks(pairs, weights, count) + bias
    for b in range(2):
        for a in range(2):
            at = (2 * b + a) * chans
            out_pair[a, :, b] = res[:, at : at + chans].reshape(count, images, chans)


def conv_kernel(
    n_rows,
    n_cols,
    x_hbm,
    w1_hbm,
    b1_hbm,
    w2_hbm,
    b2_hbm,
    out,
    ymat,
    wt2,
    bias2,
    recv,
    xmat,
    wt1,
    bias1,
    xs,
    packed,
    w1s,
    w1own,
    w1all,
    w2s,
    b1s,
    b2s,
    load_sem,
    par_sem,
    send_sem,
    recv_sem,
    wsend_sem,
    wrecv_sem,
    swap_send_sem,
    swap_recv_sem,
    wswap_send_sem,
    wswap_recv_sem,
):
    chip_h, pairs = xs.shape[1:3]
    images = xs.shape[-1]
    tile_h, tile_j = chip_h // 2, pairs // n_cols
    win_j = tile_j + 2
    sources = n_rows * n_cols
    r, c = lax.axis_index("model"), lax.axis_index("cols")
    par = lax.rem(r, 2)
    me = r * n_cols + c
    chans = recv.shape[0] * 2

    tops = [tile_h - sum(CHUNK_ROWS[: k + 1]) for k in range(len(CHUNK_ROWS))]
    groups = (
        ((tops[0], chip_h - tops[0]),),
        *(((k, k + n), (chip_h - k - n, chip_h - k)) for k, n in zip(tops[1:], CHUNK_ROWS[1:])),
    )
    loads = []
    for g, spans in enumerate(groups):
        loads.append(
            [
                pltpu.make_async_copy(x_hbm.at[:, lo:hi], xs.at[:, lo:hi], load_sem.at[g, n])
                for n, (lo, hi) in enumerate(spans)
            ]
        )
    for copies in loads:
        for copy in copies:
            copy.start()
    params = [
        pltpu.make_async_copy(src, dst, par_sem.at[s])
        for s, (src, dst) in enumerate(((w1_hbm, w1s), (w2_hbm, w2s), (b1_hbm, b1s), (b2_hbm, b2s)))
    ]
    for copy in params:
        copy.start()

    barrier = pltpu.get_barrier_semaphore()
    to_cs = [lax.rem(c + k, n_cols) for k in range(n_cols)]

    def device(to_r, to_c):
        return {"model": to_r, "cols": to_c}

    to_rs = [lax.rem(r + k, n_rows) for k in range(n_rows)]
    for kr, kc in sorted(
        ((kr, kc) for kr in range(n_rows) for kc in range(n_cols) if kr or kc),
        key=lambda k: (k[1] not in (1, 2), k[0] not in (2, 3, 4, 5), k[1] == 2, k[0] < 4, -min(k[0], n_rows - k[0])),
    ):
        pl.semaphore_signal(barrier, inc=1, device_id=device(to_rs[kr], to_cs[kc]), device_id_type=MESH)

    def pack_rows(x, lo, hi):
        rows = hi - lo
        left, right = (xs[x, lo:hi, :, p].reshape(rows * pairs * 2, images) for p in range(2))
        both = jnp.concatenate([left, right], axis=1)
        packed[pl.ds(chip_h * x + lo, rows)] = both.reshape(rows, pairs, 2, 2 * images)

    def pack(g):
        for copy in loads[g]:
            copy.wait()

        def body(x, carry):
            for lo, hi in groups[g]:
                pack_rows(x, lo, hi)
            return carry

        lax.fori_loop(0, n_rows // 2, body, 0)

    last = tile_h + 4

    def rows_of(offset, count):
        def where(to_r):
            q = lax.rem(to_r, 2)
            src = tile_h * to_r + offset + (tile_h - count - 2 * offset) * q
            dst = offset + 2 + (last - count - 2 * offset - 3) * q
            return src, dst

        return where

    chunks = (
        *((n, rows_of(k, n), False) for k, n in zip(tops, CHUNK_ROWS)),
        (2, rows_of(-2, 2), True),
    )
    no_outer = (r == 0) | (r == n_rows - 1)
    at_edge = (c == 0) | (c == n_cols - 1)
    own_j = c == 0
    own_j = own_j.astype(jnp.int32)

    def send_tile(chunk, to_r, to_c, there):
        rows, where, is_outer = chunks[chunk]
        src, dst = where(to_r)
        skip = (to_c == 0).astype(jnp.int32)
        edge = (to_c == 0) | (to_c == n_cols - 1)
        if is_outer:
            there = there & (to_r > 0) & (to_r < n_rows - 1)

        def copy(count, src_j, dst_j):
            pltpu.make_async_remote_copy(
                src_ref=packed.at[pl.ds(src, rows), pl.ds(src_j, count)],
                dst_ref=recv.at[me, pl.ds(dst, rows), pl.ds(dst_j, count)],
                send_sem=send_sem.at[chunk],
                recv_sem=recv_sem.at[chunk],
                device_id=device(to_r, to_c),
                device_id_type=MESH,
            ).start()

        pl.when(there & edge)(lambda: copy(win_j - 1, tile_j * to_c - 1 + skip, skip))
        pl.when(there & jnp.logical_not(edge))(lambda: copy(win_j, tile_j * to_c - 1, 0))

    chips = n_rows // 2
    ahead_r, ahead_c = AHEAD

    def step(t, table):
        value = jnp.int32(table[-1])
        for k, entry in enumerate(table[:-1]):
            value = jnp.where(t == k, entry, value)
        return value

    def turn_to(t):
        dx = step(t, CHIPS_ALONG)
        return lax.rem(r // 2 + dx, chips), dx

    def send_chip(chunk, t, rest, where=None):
        x, dx = turn_to(t)
        way = 1 - 2 * lax.rem(par + t, 2)
        for other, dy in CHIP_ORDER:
            to_r = 2 * x + (1 - par if other else par)
            to_c = lax.rem(c + way * dy + n_cols, n_cols)
            there = True
            if not other and dy == 0:
                there = dx > 0
            if rest:
                there = there & jnp.logical_not((to_r == ahead_r) & (to_c == ahead_c))
            if where is not None:
                there = there & where(to_c)
            send_tile(chunk, to_r, to_c, there)

    def send_ahead(chunk):
        send_tile(chunk, jnp.int32(ahead_r), jnp.int32(ahead_c), (r != ahead_r) | (c != ahead_c))

    def send_chunk(chunk):

        def first_column(t, carry):
            x, _ = turn_to(t)
            for other in range(2):
                to_r = 2 * x + (1 - par if other else par)
                there = ((to_r != r) | (c != 0)) & (to_r != ahead_r)
                send_tile(chunk, to_r, jnp.int32(0), there)
            return carry

        where = None
        if chunk in COLUMN_FIRST:
            lax.fori_loop(0, chips, first_column, 0)
            where = lambda to_c: to_c > 0

        def body(t, carry):
            send_chip(chunk, t, True, where)
            return carry

        lax.fori_loop(0, chips, body, 0)

    params[0].wait()
    for dw in range(3):
        w1own[dw] = jnp.concatenate([w1s[1, dw], w1s[0, dw]], axis=1)
    w1own[3] = jnp.concatenate([w1s[2, 0], w1s[2, 1]], axis=1)
    w1own[4] = jnp.concatenate([w1s[2, 2], jnp.zeros_like(w1s[2, 2])], axis=1)
    w1all[r // 2, par, c] = w1own[...]

    for copy in loads[0]:
        copy.wait()
    pack_rows(turn_to(0)[0], *groups[0][0])
    pl.semaphore_wait(barrier, sources - 1)

    def send_weights():
        for kr in range(0, n_rows, 2):
            for kc in range(n_cols):
                if kr or kc:
                    pltpu.make_async_remote_copy(
                        src_ref=w1own,
                        dst_ref=w1all.at[r // 2, par, c],
                        send_sem=wsend_sem,
                        recv_sem=wrecv_sem,
                        device_id=device(to_rs[kr], to_cs[kc]),
                        device_id_type=MESH,
                    ).start()

    def pack_and_send(t, carry):
        pl.when(t < chips - 1)(lambda: pack_rows(turn_to(t + 1)[0], *groups[0][0]))
        send_chip(0, t, False)
        pl.when(t == chips - 1)(send_weights)
        return carry

    lax.fori_loop(0, chips, pack_and_send, 0)

    pack(1)
    send_ahead(1)
    send_chunk(1)
    pack(2)
    send_ahead(2)
    send_ahead(3)
    send_chunk(2)
    send_chunk(3)

    def wait_bytes(ref, sem):
        pltpu.make_async_copy(ref, ref, sem).wait()

    w1_bytes = recv.at[0 : sources // 2 - 1, 0, 0:5]
    wait_bytes(w1_bytes, wrecv_sem)
    wait_bytes(w1_bytes, wsend_sem)
    partner = device(r + 1 - 2 * par, c)
    w_swap = pltpu.make_async_remote_copy(
        src_ref=w1all.at[:, par],
        dst_ref=w1all.at[:, par],
        send_sem=wswap_send_sem,
        recv_sem=wswap_recv_sem,
        device_id=partner,
        device_id_type=MESH,
    )
    w_swap.start()

    def own_rows(chunk):
        rows, where, _ = chunks[chunk]
        src, dst = where(r)

        def copy(count, src_j, dst_j):
            for h in range(rows):
                recv[me, dst + h, pl.ds(dst_j, count)] = packed[src + h, pl.ds(src_j, count)]

        pl.when(at_edge)(lambda: copy(win_j - 1, tile_j * c - 1 + own_j, own_j))
        pl.when(jnp.logical_not(at_edge))(lambda: copy(win_j, tile_j * c - 1, 0))

    for chunk in range(3):
        own_rows(chunk)
    pl.when(jnp.logical_not(no_outer))(lambda: own_rows(3))

    zero_row = jnp.zeros((win_j, 2, 2 * images), BF16)
    zero_col = jnp.zeros((tile_h + 2, 2, 2 * images), BF16)

    def clear(s, carry):
        recv[s, last * (1 - par)] = zero_row
        return carry

    def clear_outer(s, carry):
        recv[s, (last - 1) * par] = zero_row
        recv[s, (last - 1) * par + 1] = zero_row
        return carry

    def clear_edge(s, carry):
        recv[s, pl.ds(3 * par, tile_h + 2), (win_j - 1) * (1 - own_j)] = zero_col
        return carry

    lax.fori_loop(0, sources, clear, 0)
    pl.when(no_outer)(lambda: (lax.fori_loop(0, sources, clear_outer, 0), None)[1])
    pl.when(at_edge)(lambda: (lax.fori_loop(0, sources, clear_edge, 0), None)[1])

    low = lax.broadcasted_iota(jnp.int32, (chans, 2 * chans), 1) < chans

    def spread(wt, u, v, dw):
        ur, vr = pltpu.roll(u, chans, 1), pltpu.roll(v, chans, 1)
        zero = jnp.zeros_like(u)
        tiles = (jnp.where(low, ur, zero), u, jnp.where(low, v, ur), jnp.where(low, zero, vr))
        for k, tile in enumerate(tiles):
            tile = tile.astype(BF16)
            for b in range(2):
                wt[dw + b, k * chans : (k + 1) * chans, b * 2 * chans : (b + 1) * 2 * chans] = tile

    def blank(wt):
        zero = jnp.zeros((4 * chans, 2 * chans), BF16)
        wt[3, :, 0 : 2 * chans] = zero
        wt[0, :, 2 * chans : 4 * chans] = zero

    for copy in params[1:]:
        copy.wait()
    blank(wt1)
    blank(wt2)
    for dw in range(3):
        w = [w2s[dh, dw].astype(F32) for dh in range(3)]
        spread(
            wt2,
            jnp.concatenate([w[1], w[0]], axis=1),
            jnp.concatenate([w[2], jnp.zeros_like(w[2])], axis=1),
            dw,
        )
    bias1[...] = jnp.concatenate([b1s[...]] * 4, axis=1)
    bias2[...] = jnp.concatenate([b2s[...]] * 4, axis=1)

    def arrived(chunk):
        def wait(count):
            wait_bytes(recv.at[0 : sources - 1, 0 : chunks[chunk][0], 0:count], recv_sem.at[chunk])

        pl.when(at_edge)(lambda: wait(win_j - 1))
        pl.when(jnp.logical_not(at_edge))(lambda: wait(win_j))

    arrived(0)
    give = tile_h - (tile_h - 3) * par
    land = tile_h + 2 - (tile_h + 1) * (1 - par)
    swap = pltpu.make_async_remote_copy(
        src_ref=recv.at[:, pl.ds(give, 2)],
        dst_ref=recv.at[:, pl.ds(land, 2)],
        send_sem=swap_send_sem,
        recv_sem=swap_recv_sem,
        device_id=partner,
        device_id_type=MESH,
    )
    swap.start()

    w_swap.wait()
    u = [w1all[:, :, :, k].reshape(chans, 2 * chans).astype(F32) for k in range(5)]
    for dw in range(3):
        v = (u[3], pltpu.roll(u[3], chans, 1), u[4])[dw]
        spread(wt1, u[dw], jnp.where(low, v, 0.0), dw)

    x_pairs, z_pairs = xmat.shape[0], ymat.shape[0]
    o_pairs = z_pairs - 1

    def nth(n, count):
        return (count - 1) * (1 - par) + n * (2 * par - 1)

    def turn_one(n, carry):
        i = nth(n, x_pairs)

        def put(j, value):
            xmat[i, j] = value

        turn(recv, i, put)
        return carry

    def first_one(n, carry):
        i = nth(n, z_pairs)
        fill = jnp.where(n == 0, 1 - par, 2)
        out_of = jnp.where(n == z_pairs - 1, jnp.where(r == 0, 0, jnp.where(r == n_rows - 1, 1, 2)), 2)
        blank_a = jnp.where(fill < 2, fill, out_of)
        first((xmat.at[i], xmat.at[i + 1]), lambda dw: wt1[dw], bias1[...], ymat.at[i], blank_a)
        return carry

    def second_one(n, carry):
        i = nth(n, o_pairs)
        second((ymat.at[i], ymat.at[i + 1]), lambda dw: wt2[dw], bias2[...], out.at[pl.ds(2 * i, 2)])
        return carry

    def stage(s, carry):
        @pl.when(s == 0)
        def _():
            swap.wait()

        for k in range(1, 4):
            there = s == k
            if k == 3:
                there = there & jnp.logical_not(no_outer)
            pl.when(there)(lambda k=k: arrived(k))

        for ends, one in ((TURNS, turn_one), (FIRSTS, first_one), (SECONDS, second_one)):
            lax.fori_loop(step(s, (0, *ends[:-1])), step(s, ends), one, 0)
        return carry

    lax.fori_loop(0, 4, stage, 0)

    per_edge = n_rows * 2
    for chunk in range(4):
        rows = chunks[chunk][0]
        n_r = n_rows - 2 if chunk == 3 else n_rows
        counts = (n_r * 2, n_r * (n_cols - 2))

        def drain(edge_n, inner_n, rows=rows, chunk=chunk):
            wait_bytes(recv.at[0:edge_n, 0:rows, 0 : win_j - 1], send_sem.at[chunk])
            wait_bytes(recv.at[0:inner_n, 0:rows, 0:win_j], send_sem.at[chunk])

        def drain_own(chunk=chunk, counts=counts, drain=drain):
            pl.when(at_edge)(lambda: drain(counts[0] - 1, counts[1]))
            pl.when(jnp.logical_not(at_edge))(lambda: drain(counts[0], counts[1] - 1))

        if chunk == 3:
            pl.when(no_outer)(lambda: drain(*counts))
            pl.when(jnp.logical_not(no_outer))(drain_own)
        else:
            drain_own()


def tail_kernel(tile, ymat, wt2, bias2, out_hbm, o_new, sem):
    par = lax.rem(lax.axis_index("model"), 2)
    rows = out_hbm.shape[0]
    o_pairs = ymat.shape[0] - 1
    late = (rows - 2) * par
    here = 2 * (1 - par)

    def start(k, carry):
        pltpu.make_async_copy(tile.at[par + k], out_hbm.at[k], sem.at[0]).start()
        return carry

    lax.fori_loop(here, here + rows - 2, start, 0)
    i = (o_pairs - 1) * par
    second((ymat.at[i], ymat.at[i + 1]), lambda dw: wt2[dw], bias2[...], o_new)
    last = pltpu.make_async_copy(o_new, out_hbm.at[pl.ds(late, 2)], sem.at[1])
    last.start()
    pltpu.make_async_copy(tile.at[0 : rows - 2], out_hbm.at[0 : rows - 2], sem.at[0]).wait()
    last.wait()


def solution(mesh):
    n_rows = mesh.shape["model"]
    n_cols = mesh.shape["cols"]

    def run_local(x_in, w_conv1, b_conv1, w_conv2, b_conv2):
        images, height, width, own_chans = x_in.shape
        sources = n_rows * n_cols
        chans = own_chans * sources
        pairs = width // 2
        tile_h, tile_j = height // n_rows, pairs // n_cols
        win_j = tile_j + 2
        x_pairs, z_pairs = (tile_h + 5) // 2, (tile_h + 3) // 2
        x_t = jnp.transpose(x_in, (1, 2, 3, 0)).reshape(n_rows // 2, 2 * tile_h, pairs, 2, own_chans, images)
        args = (x_t, w_conv1, b_conv1.reshape(1, chans), w_conv2, b_conv2.reshape(1, chans))
        hbm = pl.BlockSpec(memory_space=pltpu.HBM)
        vmem = pl.BlockSpec(memory_space=pltpu.VMEM)
        kept = (
            pltpu.VMEM((2 * (z_pairs - 1), tile_j, 2, images, chans), F32),
            pltpu.VMEM((z_pairs, win_j - 1, 2, images, 2 * chans), BF16),
            pltpu.VMEM((4, 4 * chans, 4 * chans), BF16),
            pltpu.VMEM((1, 4 * chans), F32),
        )
        state = pl.pallas_call(
            functools.partial(conv_kernel, n_rows, n_cols),
            out_shape=kept,
            in_specs=[hbm] * 5,
            out_specs=[vmem] * len(kept),
            scratch_shapes=[
                pltpu.VMEM((sources, 2 * x_pairs, win_j, own_chans, 2 * images), BF16),
                pltpu.VMEM((x_pairs, win_j, 2, images, 2 * chans), BF16),
                pltpu.VMEM((4, 4 * chans, 4 * chans), BF16),
                pltpu.VMEM((1, 4 * chans), F32),
                pltpu.VMEM((n_rows // 2, 2 * tile_h, pairs, 2, own_chans, images), BF16),
                pltpu.VMEM((height, pairs, own_chans, 2 * images), BF16),
                pltpu.VMEM((3, 3, own_chans, chans), BF16),
                pltpu.VMEM((5, own_chans, 2 * chans), BF16),
                pltpu.VMEM((n_rows // 2, 2, n_cols, 5, own_chans, 2 * chans), BF16),
                pltpu.VMEM((3, 3, chans, chans), BF16),
                pltpu.VMEM((1, chans), F32),
                pltpu.VMEM((1, chans), F32),
                pltpu.SemaphoreType.DMA((3, 2)),
                pltpu.SemaphoreType.DMA((4,)),
                pltpu.SemaphoreType.DMA((4,)),
                pltpu.SemaphoreType.DMA((4,)),
            ]
            + [pltpu.SemaphoreType.DMA] * 6,
            compiler_params=pltpu.CompilerParams(
                collective_id=0, has_side_effects=True, vmem_limit_bytes=24 << 20
            ),
            name="conv",
        )(*(pltpu.with_memory_space_constraint(a, pltpu.HBM) for a in args))
        out = pl.pallas_call(
            tail_kernel,
            out_shape=jax.ShapeDtypeStruct((tile_h, tile_j, 2, images, chans), F32),
            in_specs=[vmem] * len(kept),
            out_specs=pl.BlockSpec(memory_space=pl.ANY),
            scratch_shapes=[
                pltpu.VMEM((2, tile_j, 2, images, chans), F32),
                pltpu.SemaphoreType.DMA((2,)),
            ],
            compiler_params=pltpu.CompilerParams(vmem_limit_bytes=8 << 20),
            name="tail",
        )(*state)
        out = out.reshape(tile_h, 2 * tile_j, images, chans)
        return jnp.transpose(out, (2, 0, 1, 3))

    group = ("model", "cols")
    return jax.shard_map(
        run_local,
        mesh=mesh,
        in_specs=(P("data", None, None, group), P(None, None, group, None), P(), P(), P()),
        out_specs=P("data", "model", "cols", None),
        check_vma=False,
    )
```

```python
import functools

import jax
import jax.numpy as jnp
from jax import lax
from jax.experimental import pallas as pl
from jax.experimental.pallas import tpu as pltpu
from jax.sharding import PartitionSpec as P

MESH = pl.DeviceIdType.MESH
BF16 = jnp.bfloat16
F32 = jnp.float32
CHUNK_ROWS = (2, 3, 2)
TURNS, FIRSTS, SECONDS = (2, 4, 5, 6), (1, 3, 4, 5), (0, 2, 3, 3)
EARLY_FROM = 1
CHIPS_ALONG = (3, 1, 2, 0)
CHIP_ORDER = tuple((other, dy) for other in (0, 1) for dy in (0, 1, -1, 2))


def turn(recv, i, put):
    sources, _, win_j, own_chans, lanes = recv.shape
    chans = sources * own_chans
    for j in range(win_j):
        top = recv[:, 2 * i, j].reshape(chans, lanes)
        under = recv[:, 2 * i + 1, j].reshape(chans, lanes)
        put(j, jnp.concatenate([top, under], axis=0).T.reshape(2, lanes // 2, 2 * chans))


def blocks(pairs, weights, count):
    acc = None
    for dw in range(4):
        parts = [view[dw // 2 : dw // 2 + count, dw % 2] for view in pairs]
        lhs = jnp.concatenate([p.reshape(count * p.shape[1], p.shape[2]) for p in parts], axis=1)
        term = jnp.dot(lhs, weights(dw), preferred_element_type=F32)
        acc = term if acc is None else acc + term
    return acc


def first(pairs, weights, bias, y_row, blank_a):
    count, _, images, lanes = y_row.shape
    c = lax.axis_index("cols")
    row = lax.rem(lax.broadcasted_iota(jnp.int32, (1, 2 * lanes), 1), lanes) // (lanes // 2)
    act = jnp.maximum(blocks(pairs, weights, count) + bias, 0.0)
    act = jnp.where(row != blank_a, act, 0.0).astype(BF16)
    for b in range(2):
        y_row[:, b] = act[:, b * lanes : (b + 1) * lanes].reshape(count, images, lanes)
    blank = jnp.zeros((images, lanes), BF16)

    @pl.when(c == 0)
    def _():
        y_row[0, 0] = blank

    @pl.when(c == lax.axis_size("cols") - 1)
    def _():
        y_row[count - 1, 1] = blank


def second(pairs, weights, bias, out_pair):
    _, count, _, images, chans = out_pair.shape
    res = blocks(pairs, weights, count) + bias
    for b in range(2):
        for a in range(2):
            at = (2 * b + a) * chans
            out_pair[a, :, b] = res[:, at : at + chans].reshape(count, images, chans)


def conv_kernel(
    n_rows,
    n_cols,
    x_hbm,
    w1_hbm,
    b1_hbm,
    w2_hbm,
    b2_hbm,
    out,
    ymat,
    wt2,
    bias2,
    recv,
    xmat,
    wt1,
    bias1,
    xs,
    packed,
    w1s,
    w1own,
    w1all,
    w2s,
    b1s,
    b2s,
    load_sem,
    par_sem,
    send_sem,
    recv_sem,
    wsend_sem,
    wrecv_sem,
    swap_send_sem,
    swap_recv_sem,
    wswap_send_sem,
    wswap_recv_sem,
):
    chip_h, pairs = xs.shape[1:3]
    images = xs.shape[-1]
    tile_h, tile_j = chip_h // 2, pairs // n_cols
    win_j = tile_j + 2
    sources = n_rows * n_cols
    r, c = lax.axis_index("model"), lax.axis_index("cols")
    par = lax.rem(r, 2)
    me = r * n_cols + c
    chans = recv.shape[0] * 2

    tops = [tile_h - sum(CHUNK_ROWS[: k + 1]) for k in range(len(CHUNK_ROWS))]
    groups = (
        ((tops[0], chip_h - tops[0]),),
        *(((k, k + n), (chip_h - k - n, chip_h - k)) for k, n in zip(tops[1:], CHUNK_ROWS[1:])),
    )
    loads = []
    for g, spans in enumerate(groups):
        loads.append(
            [
                pltpu.make_async_copy(x_hbm.at[:, lo:hi], xs.at[:, lo:hi], load_sem.at[g, n])
                for n, (lo, hi) in enumerate(spans)
            ]
        )
    for copies in loads:
        for copy in copies:
            copy.start()
    params = [
        pltpu.make_async_copy(src, dst, par_sem.at[s])
        for s, (src, dst) in enumerate(((w1_hbm, w1s), (w2_hbm, w2s), (b1_hbm, b1s), (b2_hbm, b2s)))
    ]
    for copy in params:
        copy.start()

    barrier = pltpu.get_barrier_semaphore()
    to_cs = [lax.rem(c + k, n_cols) for k in range(n_cols)]

    def device(to_r, to_c):
        return {"model": to_r, "cols": to_c}

    to_rs = [lax.rem(r + k, n_rows) for k in range(n_rows)]
    for kr, kc in sorted(
        ((kr, kc) for kr in range(n_rows) for kc in range(n_cols) if kr or kc),
        key=lambda k: (not (k[0] in (2, 3) and k[1] == 1), -(min(k[0], n_rows - k[0]) // 2 + min(k[1], n_cols - k[1]))),
    ):
        pl.semaphore_signal(barrier, inc=1, device_id=device(to_rs[kr], to_cs[kc]), device_id_type=MESH)

    def pack_rows(x, lo, hi):
        rows = hi - lo
        left, right = (xs[x, lo:hi, :, p].reshape(rows * pairs * 2, images) for p in range(2))
        both = jnp.concatenate([left, right], axis=1)
        packed[pl.ds(chip_h * x + lo, rows)] = both.reshape(rows, pairs, 2, 2 * images)

    def pack(g):
        for copy in loads[g]:
            copy.wait()

        def body(x, carry):
            for lo, hi in groups[g]:
                pack_rows(x, lo, hi)
            return carry

        lax.fori_loop(0, n_rows // 2, body, 0)

    last = tile_h + 4

    def rows_of(offset, count):
        def where(to_r):
            q = lax.rem(to_r, 2)
            src = tile_h * to_r + offset + (tile_h - count - 2 * offset) * q
            dst = offset + 2 + (last - count - 2 * offset - 3) * q
            return src, dst

        return where

    chunks = (
        *((n, rows_of(k, n), False) for k, n in zip(tops, CHUNK_ROWS)),
        (2, rows_of(-2, 2), True),
    )
    no_outer = (r == 0) | (r == n_rows - 1)
    at_edge = (c == 0) | (c == n_cols - 1)
    own_j = c == 0
    own_j = own_j.astype(jnp.int32)

    def send_tile(chunk, to_r, to_c, there):
        rows, where, is_outer = chunks[chunk]
        src, dst = where(to_r)
        skip = (to_c == 0).astype(jnp.int32)
        edge = (to_c == 0) | (to_c == n_cols - 1)
        if is_outer:
            there = there & (to_r > 0) & (to_r < n_rows - 1)

        def copy(count, src_j, dst_j):
            pltpu.make_async_remote_copy(
                src_ref=packed.at[pl.ds(src, rows), pl.ds(src_j, count)],
                dst_ref=recv.at[me, pl.ds(dst, rows), pl.ds(dst_j, count)],
                send_sem=send_sem.at[chunk],
                recv_sem=recv_sem.at[chunk],
                device_id=device(to_r, to_c),
                device_id_type=MESH,
            ).start()

        pl.when(there & edge)(lambda: copy(win_j - 1, tile_j * to_c - 1 + skip, skip))
        pl.when(there & jnp.logical_not(edge))(lambda: copy(win_j, tile_j * to_c - 1, 0))

    chips = n_rows // 2

    def step(t, table):
        value = jnp.int32(table[-1])
        for k, entry in enumerate(table[:-1]):
            value = jnp.where(t == k, entry, value)
        return value

    def turn_to(t):
        dx = step(t, CHIPS_ALONG)
        return lax.rem(r // 2 + dx, chips), dx

    def send_chip(chunk, t, where=None):
        x, dx = turn_to(t)
        way = 1 - 2 * lax.rem(par + t, 2)
        for other, dy in CHIP_ORDER:
            to_r = 2 * x + (1 - par if other else par)
            to_c = lax.rem(c + way * dy + n_cols, n_cols)
            there = True
            if not other and dy == 0:
                there = dx > 0
            if where is not None:
                there = there & where(to_c)
            send_tile(chunk, to_r, to_c, there)

    def send_chunk(chunk):
        early = EARLY_FROM <= chunk

        def body(t, carry):
            send_chip(chunk, t, (lambda to_c: to_c > 0) if early and chunk > EARLY_FROM else None)
            if early and chunk + 1 < len(chunks):
                x, dx = turn_to(t)
                for other in range(2):
                    to_r = 2 * x + (1 - par if other else par)
                    send_tile(chunk + 1, to_r, jnp.int32(0), (to_r != r) | (c != 0))
            return carry

        lax.fori_loop(0, chips, body, 0)

    params[0].wait()
    for dw in range(3):
        w1own[dw] = jnp.concatenate([w1s[1, dw], w1s[0, dw]], axis=1)
    w1own[3] = jnp.concatenate([w1s[2, 0], w1s[2, 1]], axis=1)
    w1own[4] = jnp.concatenate([w1s[2, 2], jnp.zeros_like(w1s[2, 2])], axis=1)
    w1all[r // 2, par, c] = w1own[...]

    for copy in loads[0]:
        copy.wait()
    pack_rows(turn_to(0)[0], *groups[0][0])
    pl.semaphore_wait(barrier, sources - 1)

    def send_weights():
        for kr in range(0, n_rows, 2):
            for kc in range(n_cols):
                if kr or kc:
                    pltpu.make_async_remote_copy(
                        src_ref=w1own,
                        dst_ref=w1all.at[r // 2, par, c],
                        send_sem=wsend_sem,
                        recv_sem=wrecv_sem,
                        device_id=device(to_rs[kr], to_cs[kc]),
                        device_id_type=MESH,
                    ).start()

    def pack_and_send(t, carry):
        pl.when(t < chips - 1)(lambda: pack_rows(turn_to(t + 1)[0], *groups[0][0]))
        send_chip(0, t)
        pl.when(t == 0)(send_weights)
        return carry

    lax.fori_loop(0, chips, pack_and_send, 0)

    for g in range(1, EARLY_FROM + 1):
        pack(g)
    for chunk in range(1, len(chunks)):
        if chunk >= EARLY_FROM and chunk + 1 < len(groups):
            pack(chunk + 1)
        send_chunk(chunk)

    def wait_bytes(ref, sem):
        pltpu.make_async_copy(ref, ref, sem).wait()

    w1_bytes = recv.at[0 : sources // 2 - 1, 0, 0:5]
    wait_bytes(w1_bytes, wrecv_sem)
    wait_bytes(w1_bytes, wsend_sem)
    partner = device(r + 1 - 2 * par, c)
    w_swap = pltpu.make_async_remote_copy(
        src_ref=w1all.at[:, par],
        dst_ref=w1all.at[:, par],
        send_sem=wswap_send_sem,
        recv_sem=wswap_recv_sem,
        device_id=partner,
        device_id_type=MESH,
    )
    w_swap.start()

    def own_rows(chunk):
        rows, where, _ = chunks[chunk]
        src, dst = where(r)

        def copy(count, src_j, dst_j):
            for h in range(rows):
                recv[me, dst + h, pl.ds(dst_j, count)] = packed[src + h, pl.ds(src_j, count)]

        pl.when(at_edge)(lambda: copy(win_j - 1, tile_j * c - 1 + own_j, own_j))
        pl.when(jnp.logical_not(at_edge))(lambda: copy(win_j, tile_j * c - 1, 0))

    for chunk in range(3):
        own_rows(chunk)
    pl.when(jnp.logical_not(no_outer))(lambda: own_rows(3))

    zero_row = jnp.zeros((win_j, 2, 2 * images), BF16)
    zero_col = jnp.zeros((tile_h + 2, 2, 2 * images), BF16)

    def clear(s, carry):
        recv[s, last * (1 - par)] = zero_row
        return carry

    def clear_outer(s, carry):
        recv[s, (last - 1) * par] = zero_row
        recv[s, (last - 1) * par + 1] = zero_row
        return carry

    def clear_edge(s, carry):
        recv[s, pl.ds(3 * par, tile_h + 2), (win_j - 1) * (1 - own_j)] = zero_col
        return carry

    lax.fori_loop(0, sources, clear, 0)
    pl.when(no_outer)(lambda: (lax.fori_loop(0, sources, clear_outer, 0), None)[1])
    pl.when(at_edge)(lambda: (lax.fori_loop(0, sources, clear_edge, 0), None)[1])

    low = lax.broadcasted_iota(jnp.int32, (chans, 2 * chans), 1) < chans

    def spread(wt, u, v, dw):
        ur, vr = pltpu.roll(u, chans, 1), pltpu.roll(v, chans, 1)
        zero = jnp.zeros_like(u)
        tiles = (jnp.where(low, ur, zero), u, jnp.where(low, v, ur), jnp.where(low, zero, vr))
        for k, tile in enumerate(tiles):
            tile = tile.astype(BF16)
            for b in range(2):
                wt[dw + b, k * chans : (k + 1) * chans, b * 2 * chans : (b + 1) * 2 * chans] = tile

    def blank(wt):
        zero = jnp.zeros((4 * chans, 2 * chans), BF16)
        wt[3, :, 0 : 2 * chans] = zero
        wt[0, :, 2 * chans : 4 * chans] = zero

    for copy in params[1:]:
        copy.wait()
    blank(wt1)
    blank(wt2)
    for dw in range(3):
        w = [w2s[dh, dw].astype(F32) for dh in range(3)]
        spread(
            wt2,
            jnp.concatenate([w[1], w[0]], axis=1),
            jnp.concatenate([w[2], jnp.zeros_like(w[2])], axis=1),
            dw,
        )
    bias1[...] = jnp.concatenate([b1s[...]] * 4, axis=1)
    bias2[...] = jnp.concatenate([b2s[...]] * 4, axis=1)

    def arrived(chunk):
        def wait(count):
            wait_bytes(recv.at[0 : sources - 1, 0 : chunks[chunk][0], 0:count], recv_sem.at[chunk])

        pl.when(at_edge)(lambda: wait(win_j - 1))
        pl.when(jnp.logical_not(at_edge))(lambda: wait(win_j))

    arrived(0)
    give = tile_h - (tile_h - 3) * par
    land = tile_h + 2 - (tile_h + 1) * (1 - par)
    swap = pltpu.make_async_remote_copy(
        src_ref=recv.at[:, pl.ds(give, 2)],
        dst_ref=recv.at[:, pl.ds(land, 2)],
        send_sem=swap_send_sem,
        recv_sem=swap_recv_sem,
        device_id=partner,
        device_id_type=MESH,
    )
    swap.start()

    w_swap.wait()
    u = [w1all[:, :, :, k].reshape(chans, 2 * chans).astype(F32) for k in range(5)]
    for dw in range(3):
        v = (u[3], pltpu.roll(u[3], chans, 1), u[4])[dw]
        spread(wt1, u[dw], jnp.where(low, v, 0.0), dw)

    x_pairs, z_pairs = xmat.shape[0], ymat.shape[0]
    o_pairs = z_pairs - 1

    def nth(n, count):
        return (count - 1) * (1 - par) + n * (2 * par - 1)

    def turn_one(n, carry):
        i = nth(n, x_pairs)

        def put(j, value):
            xmat[i, j] = value

        turn(recv, i, put)
        return carry

    def first_one(n, carry):
        i = nth(n, z_pairs)
        fill = jnp.where(n == 0, 1 - par, 2)
        out_of = jnp.where(n == z_pairs - 1, jnp.where(r == 0, 0, jnp.where(r == n_rows - 1, 1, 2)), 2)
        blank_a = jnp.where(fill < 2, fill, out_of)
        first((xmat.at[i], xmat.at[i + 1]), lambda dw: wt1[dw], bias1[...], ymat.at[i], blank_a)
        return carry

    def second_one(n, carry):
        i = nth(n, o_pairs)
        second((ymat.at[i], ymat.at[i + 1]), lambda dw: wt2[dw], bias2[...], out.at[pl.ds(2 * i, 2)])
        return carry

    def stage(s, carry):
        @pl.when(s == 0)
        def _():
            swap.wait()

        for k in range(1, 4):
            there = s == k
            if k == 3:
                there = there & jnp.logical_not(no_outer)
            pl.when(there)(lambda k=k: arrived(k))

        for ends, one in ((TURNS, turn_one), (FIRSTS, first_one), (SECONDS, second_one)):
            lax.fori_loop(step(s, (0, *ends[:-1])), step(s, ends), one, 0)
        return carry

    lax.fori_loop(0, 4, stage, 0)

    per_edge = n_rows * 2
    for chunk in range(4):
        rows = chunks[chunk][0]
        n_r = n_rows - 2 if chunk == 3 else n_rows
        counts = (n_r * 2, n_r * (n_cols - 2))

        def drain(edge_n, inner_n, rows=rows, chunk=chunk):
            wait_bytes(recv.at[0:edge_n, 0:rows, 0 : win_j - 1], send_sem.at[chunk])
            wait_bytes(recv.at[0:inner_n, 0:rows, 0:win_j], send_sem.at[chunk])

        def drain_own(chunk=chunk, counts=counts, drain=drain):
            pl.when(at_edge)(lambda: drain(counts[0] - 1, counts[1]))
            pl.when(jnp.logical_not(at_edge))(lambda: drain(counts[0], counts[1] - 1))

        if chunk == 3:
            pl.when(no_outer)(lambda: drain(*counts))
            pl.when(jnp.logical_not(no_outer))(drain_own)
        else:
            drain_own()


def tail_kernel(tile, ymat, wt2, bias2, out_hbm, o_new, sem):
    par = lax.rem(lax.axis_index("model"), 2)
    rows = out_hbm.shape[0]
    o_pairs = ymat.shape[0] - 1
    late = (rows - 2) * par
    here = 2 * (1 - par)

    def start(k, carry):
        pltpu.make_async_copy(tile.at[par + k], out_hbm.at[k], sem.at[0]).start()
        return carry

    lax.fori_loop(here, here + rows - 2, start, 0)
    i = (o_pairs - 1) * par
    second((ymat.at[i], ymat.at[i + 1]), lambda dw: wt2[dw], bias2[...], o_new)
    last = pltpu.make_async_copy(o_new, out_hbm.at[pl.ds(late, 2)], sem.at[1])
    last.start()
    pltpu.make_async_copy(tile.at[0 : rows - 2], out_hbm.at[0 : rows - 2], sem.at[0]).wait()
    last.wait()


def solution(mesh):
    n_rows = mesh.shape["model"]
    n_cols = mesh.shape["cols"]

    def run_local(x_in, w_conv1, b_conv1, w_conv2, b_conv2):
        images, height, width, own_chans = x_in.shape
        sources = n_rows * n_cols
        chans = own_chans * sources
        pairs = width // 2
        tile_h, tile_j = height // n_rows, pairs // n_cols
        win_j = tile_j + 2
        x_pairs, z_pairs = (tile_h + 5) // 2, (tile_h + 3) // 2
        x_t = jnp.transpose(x_in, (1, 2, 3, 0)).reshape(n_rows // 2, 2 * tile_h, pairs, 2, own_chans, images)
        args = (x_t, w_conv1, b_conv1.reshape(1, chans), w_conv2, b_conv2.reshape(1, chans))
        hbm = pl.BlockSpec(memory_space=pltpu.HBM)
        vmem = pl.BlockSpec(memory_space=pltpu.VMEM)
        kept = (
            pltpu.VMEM((2 * (z_pairs - 1), tile_j, 2, images, chans), F32),
            pltpu.VMEM((z_pairs, win_j - 1, 2, images, 2 * chans), BF16),
            pltpu.VMEM((4, 4 * chans, 4 * chans), BF16),
            pltpu.VMEM((1, 4 * chans), F32),
        )
        state = pl.pallas_call(
            functools.partial(conv_kernel, n_rows, n_cols),
            out_shape=kept,
            in_specs=[hbm] * 5,
            out_specs=[vmem] * len(kept),
            scratch_shapes=[
                pltpu.VMEM((sources, 2 * x_pairs, win_j, own_chans, 2 * images), BF16),
                pltpu.VMEM((x_pairs, win_j, 2, images, 2 * chans), BF16),
                pltpu.VMEM((4, 4 * chans, 4 * chans), BF16),
                pltpu.VMEM((1, 4 * chans), F32),
                pltpu.VMEM((n_rows // 2, 2 * tile_h, pairs, 2, own_chans, images), BF16),
                pltpu.VMEM((height, pairs, own_chans, 2 * images), BF16),
                pltpu.VMEM((3, 3, own_chans, chans), BF16),
                pltpu.VMEM((5, own_chans, 2 * chans), BF16),
                pltpu.VMEM((n_rows // 2, 2, n_cols, 5, own_chans, 2 * chans), BF16),
                pltpu.VMEM((3, 3, chans, chans), BF16),
                pltpu.VMEM((1, chans), F32),
                pltpu.VMEM((1, chans), F32),
                pltpu.SemaphoreType.DMA((3, 2)),
                pltpu.SemaphoreType.DMA((4,)),
                pltpu.SemaphoreType.DMA((4,)),
                pltpu.SemaphoreType.DMA((4,)),
            ]
            + [pltpu.SemaphoreType.DMA] * 6,
            compiler_params=pltpu.CompilerParams(
                collective_id=0, has_side_effects=True, vmem_limit_bytes=24 << 20
            ),
            name="conv",
        )(*(pltpu.with_memory_space_constraint(a, pltpu.HBM) for a in args))
        out = pl.pallas_call(
            tail_kernel,
            out_shape=jax.ShapeDtypeStruct((tile_h, tile_j, 2, images, chans), F32),
            in_specs=[vmem] * len(kept),
            out_specs=pl.BlockSpec(memory_space=pl.ANY),
            scratch_shapes=[
                pltpu.VMEM((2, tile_j, 2, images, chans), F32),
                pltpu.SemaphoreType.DMA((2,)),
            ],
            compiler_params=pltpu.CompilerParams(vmem_limit_bytes=8 << 20),
            name="tail",
        )(*state)
        out = out.reshape(tile_h, 2 * tile_j, images, chans)
        return jnp.transpose(out, (2, 0, 1, 3))

    group = ("model", "cols")
    return jax.shard_map(
        run_local,
        mesh=mesh,
        in_specs=(P("data", None, None, group), P(None, None, group, None), P(), P(), P()),
        out_specs=P("data", "model", "cols", None),
        check_vma=False,
    )
```

```python
import functools

import jax
import jax.numpy as jnp
from jax import lax
from jax.experimental import pallas as pl
from jax.experimental.pallas import tpu as pltpu
from jax.sharding import PartitionSpec as P

MESH = pl.DeviceIdType.MESH
BF16 = jnp.bfloat16
F32 = jnp.float32
CHUNK_ROWS = (2, 3, 2)
TURNS, FIRSTS, SECONDS = (2, 4, 5, 6), (1, 3, 4, 5), (0, 2, 3, 3)
EARLY_FROM = 2
CHIPS_ALONG = (3, 1, 2, 0)
CHIP_ORDER = tuple((other, dy) for other in (0, 1) for dy in (0, 1, -1, 2))


def turn(recv, i, put):
    sources, _, win_j, own_chans, lanes = recv.shape
    chans = sources * own_chans
    for j in range(win_j):
        top = recv[:, 2 * i, j].reshape(chans, lanes)
        under = recv[:, 2 * i + 1, j].reshape(chans, lanes)
        put(j, jnp.concatenate([top, under], axis=0).T.reshape(2, lanes // 2, 2 * chans))


def blocks(pairs, weights, count):
    acc = None
    for dw in range(4):
        parts = [view[dw // 2 : dw // 2 + count, dw % 2] for view in pairs]
        lhs = jnp.concatenate([p.reshape(count * p.shape[1], p.shape[2]) for p in parts], axis=1)
        term = jnp.dot(lhs, weights(dw), preferred_element_type=F32)
        acc = term if acc is None else acc + term
    return acc


def first(pairs, weights, bias, y_row, blank_a):
    count, _, images, lanes = y_row.shape
    c = lax.axis_index("cols")
    row = lax.rem(lax.broadcasted_iota(jnp.int32, (1, 2 * lanes), 1), lanes) // (lanes // 2)
    act = jnp.maximum(blocks(pairs, weights, count) + bias, 0.0)
    act = jnp.where(row != blank_a, act, 0.0).astype(BF16)
    for b in range(2):
        y_row[:, b] = act[:, b * lanes : (b + 1) * lanes].reshape(count, images, lanes)
    blank = jnp.zeros((images, lanes), BF16)

    @pl.when(c == 0)
    def _():
        y_row[0, 0] = blank

    @pl.when(c == lax.axis_size("cols") - 1)
    def _():
        y_row[count - 1, 1] = blank


def second(pairs, weights, bias, out_pair):
    _, count, _, images, chans = out_pair.shape
    res = blocks(pairs, weights, count) + bias
    for b in range(2):
        for a in range(2):
            at = (2 * b + a) * chans
            out_pair[a, :, b] = res[:, at : at + chans].reshape(count, images, chans)


def conv_kernel(
    n_rows,
    n_cols,
    x_hbm,
    w1_hbm,
    b1_hbm,
    w2_hbm,
    b2_hbm,
    out,
    ymat,
    wt2,
    bias2,
    recv,
    xmat,
    wt1,
    bias1,
    xs,
    packed,
    w1s,
    w1own,
    w1all,
    w2s,
    b1s,
    b2s,
    load_sem,
    par_sem,
    send_sem,
    recv_sem,
    wsend_sem,
    wrecv_sem,
    swap_send_sem,
    swap_recv_sem,
    wswap_send_sem,
    wswap_recv_sem,
):
    chip_h, pairs = xs.shape[1:3]
    images = xs.shape[-1]
    tile_h, tile_j = chip_h // 2, pairs // n_cols
    win_j = tile_j + 2
    sources = n_rows * n_cols
    r, c = lax.axis_index("model"), lax.axis_index("cols")
    par = lax.rem(r, 2)
    me = r * n_cols + c
    chans = recv.shape[0] * 2

    tops = [tile_h - sum(CHUNK_ROWS[: k + 1]) for k in range(len(CHUNK_ROWS))]
    groups = (
        ((tops[0], chip_h - tops[0]),),
        *(((k, k + n), (chip_h - k - n, chip_h - k)) for k, n in zip(tops[1:], CHUNK_ROWS[1:])),
    )
    loads = []
    for g, spans in enumerate(groups):
        loads.append(
            [
                pltpu.make_async_copy(x_hbm.at[:, lo:hi], xs.at[:, lo:hi], load_sem.at[g, n])
                for n, (lo, hi) in enumerate(spans)
            ]
        )
    for copies in loads:
        for copy in copies:
            copy.start()
    params = [
        pltpu.make_async_copy(src, dst, par_sem.at[s])
        for s, (src, dst) in enumerate(((w1_hbm, w1s), (w2_hbm, w2s), (b1_hbm, b1s), (b2_hbm, b2s)))
    ]
    for copy in params:
        copy.start()

    barrier = pltpu.get_barrier_semaphore()
    to_cs = [lax.rem(c + k, n_cols) for k in range(n_cols)]

    def device(to_r, to_c):
        return {"model": to_r, "cols": to_c}

    to_rs = [lax.rem(r + k, n_rows) for k in range(n_rows)]
    for kr, kc in sorted(
        ((kr, kc) for kr in range(n_rows) for kc in range(n_cols) if kr or kc),
        key=lambda k: (not (k[0] in (2, 3) and k[1] == 1), -(min(k[0], n_rows - k[0]) // 2 + min(k[1], n_cols - k[1]))),
    ):
        pl.semaphore_signal(barrier, inc=1, device_id=device(to_rs[kr], to_cs[kc]), device_id_type=MESH)

    def pack_rows(x, lo, hi):
        rows = hi - lo
        left, right = (xs[x, lo:hi, :, p].reshape(rows * pairs * 2, images) for p in range(2))
        both = jnp.concatenate([left, right], axis=1)
        packed[pl.ds(chip_h * x + lo, rows)] = both.reshape(rows, pairs, 2, 2 * images)

    def pack(g):
        for copy in loads[g]:
            copy.wait()

        def body(x, carry):
            for lo, hi in groups[g]:
                pack_rows(x, lo, hi)
            return carry

        lax.fori_loop(0, n_rows // 2, body, 0)

    last = tile_h + 4

    def rows_of(offset, count):
        def where(to_r):
            q = lax.rem(to_r, 2)
            src = tile_h * to_r + offset + (tile_h - count - 2 * offset) * q
            dst = offset + 2 + (last - count - 2 * offset - 3) * q
            return src, dst

        return where

    chunks = (
        *((n, rows_of(k, n), False) for k, n in zip(tops, CHUNK_ROWS)),
        (2, rows_of(-2, 2), True),
    )
    no_outer = (r == 0) | (r == n_rows - 1)
    at_edge = (c == 0) | (c == n_cols - 1)
    own_j = c == 0
    own_j = own_j.astype(jnp.int32)

    def send_tile(chunk, to_r, to_c, there):
        rows, where, is_outer = chunks[chunk]
        src, dst = where(to_r)
        skip = (to_c == 0).astype(jnp.int32)
        edge = (to_c == 0) | (to_c == n_cols - 1)
        if is_outer:
            there = there & (to_r > 0) & (to_r < n_rows - 1)

        def copy(count, src_j, dst_j):
            pltpu.make_async_remote_copy(
                src_ref=packed.at[pl.ds(src, rows), pl.ds(src_j, count)],
                dst_ref=recv.at[me, pl.ds(dst, rows), pl.ds(dst_j, count)],
                send_sem=send_sem.at[chunk],
                recv_sem=recv_sem.at[chunk],
                device_id=device(to_r, to_c),
                device_id_type=MESH,
            ).start()

        pl.when(there & edge)(lambda: copy(win_j - 1, tile_j * to_c - 1 + skip, skip))
        pl.when(there & jnp.logical_not(edge))(lambda: copy(win_j, tile_j * to_c - 1, 0))

    chips = n_rows // 2

    def step(t, table):
        value = jnp.int32(table[-1])
        for k, entry in enumerate(table[:-1]):
            value = jnp.where(t == k, entry, value)
        return value

    def turn_to(t):
        dx = step(t, CHIPS_ALONG)
        return lax.rem(r // 2 + dx, chips), dx

    def send_chip(chunk, t, where=None):
        x, dx = turn_to(t)
        way = 1 - 2 * lax.rem(par + t, 2)
        for other, dy in CHIP_ORDER:
            to_r = 2 * x + (1 - par if other else par)
            to_c = lax.rem(c + way * dy + n_cols, n_cols)
            there = True
            if not other and dy == 0:
                there = dx > 0
            if where is not None:
                there = there & where(to_c)
            send_tile(chunk, to_r, to_c, there)

    def send_chunk(chunk):
        early = EARLY_FROM <= chunk

        def body(t, carry):
            send_chip(chunk, t, (lambda to_c: to_c > 0) if early and chunk > EARLY_FROM else None)
            if early and chunk + 1 < len(chunks):
                x, dx = turn_to(t)
                for other in range(2):
                    to_r = 2 * x + (1 - par if other else par)
                    send_tile(chunk + 1, to_r, jnp.int32(0), (to_r != r) | (c != 0))
            return carry

        lax.fori_loop(0, chips, body, 0)

    params[0].wait()
    for dw in range(3):
        w1own[dw] = jnp.concatenate([w1s[1, dw], w1s[0, dw]], axis=1)
    w1own[3] = jnp.concatenate([w1s[2, 0], w1s[2, 1]], axis=1)
    w1own[4] = jnp.concatenate([w1s[2, 2], jnp.zeros_like(w1s[2, 2])], axis=1)
    w1all[r // 2, par, c] = w1own[...]

    for copy in loads[0]:
        copy.wait()
    pack_rows(turn_to(0)[0], *groups[0][0])
    pl.semaphore_wait(barrier, sources - 1)

    def send_weights():
        for kr in range(0, n_rows, 2):
            for kc in range(n_cols):
                if kr or kc:
                    pltpu.make_async_remote_copy(
                        src_ref=w1own,
                        dst_ref=w1all.at[r // 2, par, c],
                        send_sem=wsend_sem,
                        recv_sem=wrecv_sem,
                        device_id=device(to_rs[kr], to_cs[kc]),
                        device_id_type=MESH,
                    ).start()

    def pack_and_send(t, carry):
        pl.when(t < chips - 1)(lambda: pack_rows(turn_to(t + 1)[0], *groups[0][0]))
        send_chip(0, t)
        pl.when(t == 0)(send_weights)
        return carry

    lax.fori_loop(0, chips, pack_and_send, 0)

    for g in range(1, EARLY_FROM + 1):
        pack(g)
    for chunk in range(1, len(chunks)):
        if chunk >= EARLY_FROM and chunk + 1 < len(groups):
            pack(chunk + 1)
        send_chunk(chunk)

    def wait_bytes(ref, sem):
        pltpu.make_async_copy(ref, ref, sem).wait()

    w1_bytes = recv.at[0 : sources // 2 - 1, 0, 0:5]
    wait_bytes(w1_bytes, wrecv_sem)
    wait_bytes(w1_bytes, wsend_sem)
    partner = device(r + 1 - 2 * par, c)
    w_swap = pltpu.make_async_remote_copy(
        src_ref=w1all.at[:, par],
        dst_ref=w1all.at[:, par],
        send_sem=wswap_send_sem,
        recv_sem=wswap_recv_sem,
        device_id=partner,
        device_id_type=MESH,
    )
    w_swap.start()

    def own_rows(chunk):
        rows, where, _ = chunks[chunk]
        src, dst = where(r)

        def copy(count, src_j, dst_j):
            for h in range(rows):
                recv[me, dst + h, pl.ds(dst_j, count)] = packed[src + h, pl.ds(src_j, count)]

        pl.when(at_edge)(lambda: copy(win_j - 1, tile_j * c - 1 + own_j, own_j))
        pl.when(jnp.logical_not(at_edge))(lambda: copy(win_j, tile_j * c - 1, 0))

    for chunk in range(3):
        own_rows(chunk)
    pl.when(jnp.logical_not(no_outer))(lambda: own_rows(3))

    zero_row = jnp.zeros((win_j, 2, 2 * images), BF16)
    zero_col = jnp.zeros((tile_h + 2, 2, 2 * images), BF16)

    def clear(s, carry):
        recv[s, last * (1 - par)] = zero_row
        return carry

    def clear_outer(s, carry):
        recv[s, (last - 1) * par] = zero_row
        recv[s, (last - 1) * par + 1] = zero_row
        return carry

    def clear_edge(s, carry):
        recv[s, pl.ds(3 * par, tile_h + 2), (win_j - 1) * (1 - own_j)] = zero_col
        return carry

    lax.fori_loop(0, sources, clear, 0)
    pl.when(no_outer)(lambda: (lax.fori_loop(0, sources, clear_outer, 0), None)[1])
    pl.when(at_edge)(lambda: (lax.fori_loop(0, sources, clear_edge, 0), None)[1])

    low = lax.broadcasted_iota(jnp.int32, (chans, 2 * chans), 1) < chans

    def spread(wt, u, v, dw):
        ur, vr = pltpu.roll(u, chans, 1), pltpu.roll(v, chans, 1)
        zero = jnp.zeros_like(u)
        tiles = (jnp.where(low, ur, zero), u, jnp.where(low, v, ur), jnp.where(low, zero, vr))
        for k, tile in enumerate(tiles):
            tile = tile.astype(BF16)
            for b in range(2):
                wt[dw + b, k * chans : (k + 1) * chans, b * 2 * chans : (b + 1) * 2 * chans] = tile

    def blank(wt):
        zero = jnp.zeros((4 * chans, 2 * chans), BF16)
        wt[3, :, 0 : 2 * chans] = zero
        wt[0, :, 2 * chans : 4 * chans] = zero

    for copy in params[1:]:
        copy.wait()
    blank(wt1)
    blank(wt2)
    for dw in range(3):
        w = [w2s[dh, dw].astype(F32) for dh in range(3)]
        spread(
            wt2,
            jnp.concatenate([w[1], w[0]], axis=1),
            jnp.concatenate([w[2], jnp.zeros_like(w[2])], axis=1),
            dw,
        )
    bias1[...] = jnp.concatenate([b1s[...]] * 4, axis=1)
    bias2[...] = jnp.concatenate([b2s[...]] * 4, axis=1)

    def arrived(chunk):
        def wait(count):
            wait_bytes(recv.at[0 : sources - 1, 0 : chunks[chunk][0], 0:count], recv_sem.at[chunk])

        pl.when(at_edge)(lambda: wait(win_j - 1))
        pl.when(jnp.logical_not(at_edge))(lambda: wait(win_j))

    arrived(0)
    give = tile_h - (tile_h - 3) * par
    land = tile_h + 2 - (tile_h + 1) * (1 - par)
    swap = pltpu.make_async_remote_copy(
        src_ref=recv.at[:, pl.ds(give, 2)],
        dst_ref=recv.at[:, pl.ds(land, 2)],
        send_sem=swap_send_sem,
        recv_sem=swap_recv_sem,
        device_id=partner,
        device_id_type=MESH,
    )
    swap.start()

    w_swap.wait()
    u = [w1all[:, :, :, k].reshape(chans, 2 * chans).astype(F32) for k in range(5)]
    for dw in range(3):
        v = (u[3], pltpu.roll(u[3], chans, 1), u[4])[dw]
        spread(wt1, u[dw], jnp.where(low, v, 0.0), dw)

    x_pairs, z_pairs = xmat.shape[0], ymat.shape[0]
    o_pairs = z_pairs - 1

    def nth(n, count):
        return (count - 1) * (1 - par) + n * (2 * par - 1)

    def turn_one(n, carry):
        i = nth(n, x_pairs)

        def put(j, value):
            xmat[i, j] = value

        turn(recv, i, put)
        return carry

    def first_one(n, carry):
        i = nth(n, z_pairs)
        fill = jnp.where(n == 0, 1 - par, 2)
        out_of = jnp.where(n == z_pairs - 1, jnp.where(r == 0, 0, jnp.where(r == n_rows - 1, 1, 2)), 2)
        blank_a = jnp.where(fill < 2, fill, out_of)
        first((xmat.at[i], xmat.at[i + 1]), lambda dw: wt1[dw], bias1[...], ymat.at[i], blank_a)
        return carry

    def second_one(n, carry):
        i = nth(n, o_pairs)
        second((ymat.at[i], ymat.at[i + 1]), lambda dw: wt2[dw], bias2[...], out.at[pl.ds(2 * i, 2)])
        return carry

    def stage(s, carry):
        @pl.when(s == 0)
        def _():
            swap.wait()

        for k in range(1, 4):
            there = s == k
            if k == 3:
                there = there & jnp.logical_not(no_outer)
            pl.when(there)(lambda k=k: arrived(k))

        for ends, one in ((TURNS, turn_one), (FIRSTS, first_one), (SECONDS, second_one)):
            lax.fori_loop(step(s, (0, *ends[:-1])), step(s, ends), one, 0)
        return carry

    lax.fori_loop(0, 4, stage, 0)

    per_edge = n_rows * 2
    for chunk in range(4):
        rows = chunks[chunk][0]
        n_r = n_rows - 2 if chunk == 3 else n_rows
        counts = (n_r * 2, n_r * (n_cols - 2))

        def drain(edge_n, inner_n, rows=rows, chunk=chunk):
            wait_bytes(recv.at[0:edge_n, 0:rows, 0 : win_j - 1], send_sem.at[chunk])
            wait_bytes(recv.at[0:inner_n, 0:rows, 0:win_j], send_sem.at[chunk])

        def drain_own(chunk=chunk, counts=counts, drain=drain):
            pl.when(at_edge)(lambda: drain(counts[0] - 1, counts[1]))
            pl.when(jnp.logical_not(at_edge))(lambda: drain(counts[0], counts[1] - 1))

        if chunk == 3:
            pl.when(no_outer)(lambda: drain(*counts))
            pl.when(jnp.logical_not(no_outer))(drain_own)
        else:
            drain_own()


def tail_kernel(tile, ymat, wt2, bias2, out_hbm, o_new, sem):
    par = lax.rem(lax.axis_index("model"), 2)
    rows = out_hbm.shape[0]
    o_pairs = ymat.shape[0] - 1
    late = (rows - 2) * par
    here = 2 * (1 - par)

    def start(k, carry):
        pltpu.make_async_copy(tile.at[par + k], out_hbm.at[k], sem.at[0]).start()
        return carry

    lax.fori_loop(here, here + rows - 2, start, 0)
    i = (o_pairs - 1) * par
    second((ymat.at[i], ymat.at[i + 1]), lambda dw: wt2[dw], bias2[...], o_new)
    last = pltpu.make_async_copy(o_new, out_hbm.at[pl.ds(late, 2)], sem.at[1])
    last.start()
    pltpu.make_async_copy(tile.at[0 : rows - 2], out_hbm.at[0 : rows - 2], sem.at[0]).wait()
    last.wait()


def solution(mesh):
    n_rows = mesh.shape["model"]
    n_cols = mesh.shape["cols"]

    def run_local(x_in, w_conv1, b_conv1, w_conv2, b_conv2):
        images, height, width, own_chans = x_in.shape
        sources = n_rows * n_cols
        chans = own_chans * sources
        pairs = width // 2
        tile_h, tile_j = height // n_rows, pairs // n_cols
        win_j = tile_j + 2
        x_pairs, z_pairs = (tile_h + 5) // 2, (tile_h + 3) // 2
        x_t = jnp.transpose(x_in, (1, 2, 3, 0)).reshape(n_rows // 2, 2 * tile_h, pairs, 2, own_chans, images)
        args = (x_t, w_conv1, b_conv1.reshape(1, chans), w_conv2, b_conv2.reshape(1, chans))
        hbm = pl.BlockSpec(memory_space=pltpu.HBM)
        vmem = pl.BlockSpec(memory_space=pltpu.VMEM)
        kept = (
            pltpu.VMEM((2 * (z_pairs - 1), tile_j, 2, images, chans), F32),
            pltpu.VMEM((z_pairs, win_j - 1, 2, images, 2 * chans), BF16),
            pltpu.VMEM((4, 4 * chans, 4 * chans), BF16),
            pltpu.VMEM((1, 4 * chans), F32),
        )
        state = pl.pallas_call(
            functools.partial(conv_kernel, n_rows, n_cols),
            out_shape=kept,
            in_specs=[hbm] * 5,
            out_specs=[vmem] * len(kept),
            scratch_shapes=[
                pltpu.VMEM((sources, 2 * x_pairs, win_j, own_chans, 2 * images), BF16),
                pltpu.VMEM((x_pairs, win_j, 2, images, 2 * chans), BF16),
                pltpu.VMEM((4, 4 * chans, 4 * chans), BF16),
                pltpu.VMEM((1, 4 * chans), F32),
                pltpu.VMEM((n_rows // 2, 2 * tile_h, pairs, 2, own_chans, images), BF16),
                pltpu.VMEM((height, pairs, own_chans, 2 * images), BF16),
                pltpu.VMEM((3, 3, own_chans, chans), BF16),
                pltpu.VMEM((5, own_chans, 2 * chans), BF16),
                pltpu.VMEM((n_rows // 2, 2, n_cols, 5, own_chans, 2 * chans), BF16),
                pltpu.VMEM((3, 3, chans, chans), BF16),
                pltpu.VMEM((1, chans), F32),
                pltpu.VMEM((1, chans), F32),
                pltpu.SemaphoreType.DMA((3, 2)),
                pltpu.SemaphoreType.DMA((4,)),
                pltpu.SemaphoreType.DMA((4,)),
                pltpu.SemaphoreType.DMA((4,)),
            ]
            + [pltpu.SemaphoreType.DMA] * 6,
            compiler_params=pltpu.CompilerParams(
                collective_id=0, has_side_effects=True, vmem_limit_bytes=24 << 20
            ),
            name="conv",
        )(*(pltpu.with_memory_space_constraint(a, pltpu.HBM) for a in args))
        out = pl.pallas_call(
            tail_kernel,
            out_shape=jax.ShapeDtypeStruct((tile_h, tile_j, 2, images, chans), F32),
            in_specs=[vmem] * len(kept),
            out_specs=pl.BlockSpec(memory_space=pl.ANY),
            scratch_shapes=[
                pltpu.VMEM((2, tile_j, 2, images, chans), F32),
                pltpu.SemaphoreType.DMA((2,)),
            ],
            compiler_params=pltpu.CompilerParams(vmem_limit_bytes=8 << 20),
            name="tail",
        )(*state)
        out = out.reshape(tile_h, 2 * tile_j, images, chans)
        return jnp.transpose(out, (2, 0, 1, 3))

    group = ("model", "cols")
    return jax.shard_map(
        run_local,
        mesh=mesh,
        in_specs=(P("data", None, None, group), P(None, None, group, None), P(), P(), P()),
        out_specs=P("data", "model", "cols", None),
        check_vma=False,
    )
```

```python
import functools

import jax
import jax.numpy as jnp
from jax import lax
from jax.experimental import pallas as pl
from jax.experimental.pallas import tpu as pltpu
from jax.sharding import PartitionSpec as P

MESH = pl.DeviceIdType.MESH
BF16 = jnp.bfloat16
F32 = jnp.float32
CHUNK_ROWS = (2, 3, 2)
TURNS, FIRSTS, SECONDS = (2, 4, 5, 6), (1, 3, 4, 5), (0, 2, 3, 3)
EARLY_FROM = 1
AHEAD = (1, 0)
CHIPS_ALONG = (3, 1, 2, 0)
CHIP_ORDER = tuple((other, dy) for other in (0, 1) for dy in (0, 1, -1, 2))


def turn(recv, i, put):
    sources, _, win_j, own_chans, lanes = recv.shape
    chans = sources * own_chans
    for j in range(win_j):
        top = recv[:, 2 * i, j].reshape(chans, lanes)
        under = recv[:, 2 * i + 1, j].reshape(chans, lanes)
        put(j, jnp.concatenate([top, under], axis=0).T.reshape(2, lanes // 2, 2 * chans))


def blocks(pairs, weights, count):
    acc = None
    for dw in range(4):
        parts = [view[dw // 2 : dw // 2 + count, dw % 2] for view in pairs]
        lhs = jnp.concatenate([p.reshape(count * p.shape[1], p.shape[2]) for p in parts], axis=1)
        term = jnp.dot(lhs, weights(dw), preferred_element_type=F32)
        acc = term if acc is None else acc + term
    return acc


def first(pairs, weights, bias, y_row, blank_a):
    count, _, images, lanes = y_row.shape
    c = lax.axis_index("cols")
    row = lax.rem(lax.broadcasted_iota(jnp.int32, (1, 2 * lanes), 1), lanes) // (lanes // 2)
    act = jnp.maximum(blocks(pairs, weights, count) + bias, 0.0)
    act = jnp.where(row != blank_a, act, 0.0).astype(BF16)
    for b in range(2):
        y_row[:, b] = act[:, b * lanes : (b + 1) * lanes].reshape(count, images, lanes)
    blank = jnp.zeros((images, lanes), BF16)

    @pl.when(c == 0)
    def _():
        y_row[0, 0] = blank

    @pl.when(c == lax.axis_size("cols") - 1)
    def _():
        y_row[count - 1, 1] = blank


def second(pairs, weights, bias, out_pair):
    _, count, _, images, chans = out_pair.shape
    res = blocks(pairs, weights, count) + bias
    for b in range(2):
        for a in range(2):
            at = (2 * b + a) * chans
            out_pair[a, :, b] = res[:, at : at + chans].reshape(count, images, chans)


def conv_kernel(
    n_rows,
    n_cols,
    x_hbm,
    w1_hbm,
    b1_hbm,
    w2_hbm,
    b2_hbm,
    out,
    ymat,
    wt2,
    bias2,
    recv,
    xmat,
    wt1,
    bias1,
    xs,
    packed,
    w1s,
    w1own,
    w1all,
    w2s,
    b1s,
    b2s,
    load_sem,
    par_sem,
    send_sem,
    recv_sem,
    wsend_sem,
    wrecv_sem,
    swap_send_sem,
    swap_recv_sem,
    wswap_send_sem,
    wswap_recv_sem,
):
    chip_h, pairs = xs.shape[1:3]
    images = xs.shape[-1]
    tile_h, tile_j = chip_h // 2, pairs // n_cols
    win_j = tile_j + 2
    sources = n_rows * n_cols
    r, c = lax.axis_index("model"), lax.axis_index("cols")
    par = lax.rem(r, 2)
    me = r * n_cols + c
    chans = recv.shape[0] * 2

    tops = [tile_h - sum(CHUNK_ROWS[: k + 1]) for k in range(len(CHUNK_ROWS))]
    groups = (
        ((tops[0], chip_h - tops[0]),),
        *(((k, k + n), (chip_h - k - n, chip_h - k)) for k, n in zip(tops[1:], CHUNK_ROWS[1:])),
    )
    loads = []
    for g, spans in enumerate(groups):
        loads.append(
            [
                pltpu.make_async_copy(x_hbm.at[:, lo:hi], xs.at[:, lo:hi], load_sem.at[g, n])
                for n, (lo, hi) in enumerate(spans)
            ]
        )
    for copies in loads:
        for copy in copies:
            copy.start()
    params = [
        pltpu.make_async_copy(src, dst, par_sem.at[s])
        for s, (src, dst) in enumerate(((w1_hbm, w1s), (w2_hbm, w2s), (b1_hbm, b1s), (b2_hbm, b2s)))
    ]
    for copy in params:
        copy.start()

    barrier = pltpu.get_barrier_semaphore()
    to_cs = [lax.rem(c + k, n_cols) for k in range(n_cols)]

    def device(to_r, to_c):
        return {"model": to_r, "cols": to_c}

    to_rs = [lax.rem(r + k, n_rows) for k in range(n_rows)]
    for kr, kc in sorted(
        ((kr, kc) for kr in range(n_rows) for kc in range(n_cols) if kr or kc),
        key=lambda k: (not (k[0] in (2, 3) and k[1] == 1), -(min(k[0], n_rows - k[0]) // 2 + min(k[1], n_cols - k[1]))),
    ):
        pl.semaphore_signal(barrier, inc=1, device_id=device(to_rs[kr], to_cs[kc]), device_id_type=MESH)

    ahead_r, ahead_c = AHEAD
    is_ahead = (r == ahead_r) & (c == ahead_c)

    def pack_rows(x, lo, hi):
        rows = hi - lo
        left, right = (xs[x, lo:hi, :, p].reshape(rows * pairs * 2, images) for p in range(2))
        both = jnp.concatenate([left, right], axis=1)
        packed[pl.ds(chip_h * x + lo, rows)] = both.reshape(rows, pairs, 2, 2 * images)

    def pack(g):
        for n, copy in enumerate(loads[g]):
            if (g, n) != (1, ahead_r % 2):
                copy.wait()

        def body(x, carry):
            for n, (lo, hi) in enumerate(groups[g]):
                if (g, n) == (1, ahead_r % 2):
                    pl.when(x != ahead_r // 2)(lambda lo=lo, hi=hi: pack_rows(x, lo, hi))
                else:
                    pack_rows(x, lo, hi)
            return carry

        lax.fori_loop(0, n_rows // 2, body, 0)

    last = tile_h + 4

    def rows_of(offset, count):
        def where(to_r):
            q = lax.rem(to_r, 2)
            src = tile_h * to_r + offset + (tile_h - count - 2 * offset) * q
            dst = offset + 2 + (last - count - 2 * offset - 3) * q
            return src, dst

        return where

    chunks = (
        *((n, rows_of(k, n), False) for k, n in zip(tops, CHUNK_ROWS)),
        (2, rows_of(-2, 2), True),
    )
    no_outer = (r == 0) | (r == n_rows - 1)
    at_edge = (c == 0) | (c == n_cols - 1)
    own_j = c == 0
    own_j = own_j.astype(jnp.int32)

    def send_tile(chunk, to_r, to_c, there):
        rows, where, is_outer = chunks[chunk]
        src, dst = where(to_r)
        skip = (to_c == 0).astype(jnp.int32)
        edge = (to_c == 0) | (to_c == n_cols - 1)
        if is_outer:
            there = there & (to_r > 0) & (to_r < n_rows - 1)

        def copy(count, src_j, dst_j):
            pltpu.make_async_remote_copy(
                src_ref=packed.at[pl.ds(src, rows), pl.ds(src_j, count)],
                dst_ref=recv.at[me, pl.ds(dst, rows), pl.ds(dst_j, count)],
                send_sem=send_sem.at[chunk],
                recv_sem=recv_sem.at[chunk],
                device_id=device(to_r, to_c),
                device_id_type=MESH,
            ).start()

        pl.when(there & edge)(lambda: copy(win_j - 1, tile_j * to_c - 1 + skip, skip))
        pl.when(there & jnp.logical_not(edge))(lambda: copy(win_j, tile_j * to_c - 1, 0))

    chips = n_rows // 2

    def step(t, table):
        value = jnp.int32(table[-1])
        for k, entry in enumerate(table[:-1]):
            value = jnp.where(t == k, entry, value)
        return value

    def turn_to(t):
        dx = step(t, CHIPS_ALONG)
        return lax.rem(r // 2 + dx, chips), dx

    def send_chip(chunk, t, where=None):
        x, dx = turn_to(t)
        way = 1 - 2 * lax.rem(par + t, 2)
        for other, dy in CHIP_ORDER:
            to_r = 2 * x + (1 - par if other else par)
            to_c = lax.rem(c + way * dy + n_cols, n_cols)
            there = True
            if not other and dy == 0:
                there = dx > 0
            if where is not None:
                there = there & where(to_r, to_c)
            send_tile(chunk, to_r, to_c, there)

    def send_chunk(chunk):
        early = EARLY_FROM <= chunk

        def body(t, carry):
            if chunk > EARLY_FROM:
                send_chip(chunk, t, lambda to_r, to_c: to_c > 0)
            else:
                send_chip(chunk, t, lambda to_r, to_c: (to_r != ahead_r) | (to_c != ahead_c))
            if early and chunk + 1 < len(chunks):
                x, dx = turn_to(t)
                for other in range(2):
                    to_r = 2 * x + (1 - par if other else par)
                    there = (to_r != r) | (c != 0)
                    if chunk > EARLY_FROM:
                        there = there & (to_r != ahead_r)
                    send_tile(chunk + 1, to_r, jnp.int32(0), there)
                if chunk == EARLY_FROM:
                    there = (x == ahead_r // 2) & jnp.logical_not(is_ahead)
                    send_tile(len(chunks) - 1, jnp.int32(ahead_r), jnp.int32(ahead_c), there)
            return carry

        lax.fori_loop(0, chips, body, 0)

    params[0].wait()
    for dw in range(3):
        w1own[dw] = jnp.concatenate([w1s[1, dw], w1s[0, dw]], axis=1)
    w1own[3] = jnp.concatenate([w1s[2, 0], w1s[2, 1]], axis=1)
    w1own[4] = jnp.concatenate([w1s[2, 2], jnp.zeros_like(w1s[2, 2])], axis=1)
    w1all[r // 2, par, c] = w1own[...]

    for copy in loads[0]:
        copy.wait()
    pack_rows(turn_to(0)[0], *groups[0][0])
    pl.semaphore_wait(barrier, sources - 1)

    def send_weights():
        for kr in range(0, n_rows, 2):
            for kc in range(n_cols):
                if kr or kc:
                    pltpu.make_async_remote_copy(
                        src_ref=w1own,
                        dst_ref=w1all.at[r // 2, par, c],
                        send_sem=wsend_sem,
                        recv_sem=wrecv_sem,
                        device_id=device(to_rs[kr], to_cs[kc]),
                        device_id_type=MESH,
                    ).start()

    def pack_and_send(t, carry):
        pl.when(t < chips - 1)(lambda: pack_rows(turn_to(t + 1)[0], *groups[0][0]))
        there = turn_to(t)[0] == ahead_r // 2

        @pl.when(there)
        def _():
            loads[1][ahead_r % 2].wait()
            pack_rows(ahead_r // 2, *groups[1][ahead_r % 2])

        send_chip(0, t)
        send_tile(1, jnp.int32(ahead_r), jnp.int32(ahead_c), there & jnp.logical_not(is_ahead))
        pl.when(t == 0)(send_weights)
        return carry

    lax.fori_loop(0, chips, pack_and_send, 0)

    for g in range(1, EARLY_FROM + 1):
        pack(g)
    for chunk in range(1, len(chunks)):
        if chunk >= EARLY_FROM and chunk + 1 < len(groups):
            pack(chunk + 1)
        send_chunk(chunk)

    def wait_bytes(ref, sem):
        pltpu.make_async_copy(ref, ref, sem).wait()

    w1_bytes = recv.at[0 : sources // 2 - 1, 0, 0:5]
    wait_bytes(w1_bytes, wrecv_sem)
    wait_bytes(w1_bytes, wsend_sem)
    partner = device(r + 1 - 2 * par, c)
    w_swap = pltpu.make_async_remote_copy(
        src_ref=w1all.at[:, par],
        dst_ref=w1all.at[:, par],
        send_sem=wswap_send_sem,
        recv_sem=wswap_recv_sem,
        device_id=partner,
        device_id_type=MESH,
    )
    w_swap.start()

    def own_rows(chunk):
        rows, where, _ = chunks[chunk]
        src, dst = where(r)

        def copy(count, src_j, dst_j):
            for h in range(rows):
                recv[me, dst + h, pl.ds(dst_j, count)] = packed[src + h, pl.ds(src_j, count)]

        pl.when(at_edge)(lambda: copy(win_j - 1, tile_j * c - 1 + own_j, own_j))
        pl.when(jnp.logical_not(at_edge))(lambda: copy(win_j, tile_j * c - 1, 0))

    for chunk in range(3):
        own_rows(chunk)
    pl.when(jnp.logical_not(no_outer))(lambda: own_rows(3))

    zero_row = jnp.zeros((win_j, 2, 2 * images), BF16)
    zero_col = jnp.zeros((tile_h + 2, 2, 2 * images), BF16)

    def clear(s, carry):
        recv[s, last * (1 - par)] = zero_row
        return carry

    def clear_outer(s, carry):
        recv[s, (last - 1) * par] = zero_row
        recv[s, (last - 1) * par + 1] = zero_row
        return carry

    def clear_edge(s, carry):
        recv[s, pl.ds(3 * par, tile_h + 2), (win_j - 1) * (1 - own_j)] = zero_col
        return carry

    lax.fori_loop(0, sources, clear, 0)
    pl.when(no_outer)(lambda: (lax.fori_loop(0, sources, clear_outer, 0), None)[1])
    pl.when(at_edge)(lambda: (lax.fori_loop(0, sources, clear_edge, 0), None)[1])

    low = lax.broadcasted_iota(jnp.int32, (chans, 2 * chans), 1) < chans

    def spread(wt, u, v, dw):
        ur, vr = pltpu.roll(u, chans, 1), pltpu.roll(v, chans, 1)
        zero = jnp.zeros_like(u)
        tiles = (jnp.where(low, ur, zero), u, jnp.where(low, v, ur), jnp.where(low, zero, vr))
        for k, tile in enumerate(tiles):
            tile = tile.astype(BF16)
            for b in range(2):
                wt[dw + b, k * chans : (k + 1) * chans, b * 2 * chans : (b + 1) * 2 * chans] = tile

    def blank(wt):
        zero = jnp.zeros((4 * chans, 2 * chans), BF16)
        wt[3, :, 0 : 2 * chans] = zero
        wt[0, :, 2 * chans : 4 * chans] = zero

    for copy in params[1:]:
        copy.wait()
    blank(wt1)
    blank(wt2)
    for dw in range(3):
        w = [w2s[dh, dw].astype(F32) for dh in range(3)]
        spread(
            wt2,
            jnp.concatenate([w[1], w[0]], axis=1),
            jnp.concatenate([w[2], jnp.zeros_like(w[2])], axis=1),
            dw,
        )
    bias1[...] = jnp.concatenate([b1s[...]] * 4, axis=1)
    bias2[...] = jnp.concatenate([b2s[...]] * 4, axis=1)

    def arrived(chunk):
        def wait(count):
            wait_bytes(recv.at[0 : sources - 1, 0 : chunks[chunk][0], 0:count], recv_sem.at[chunk])

        pl.when(at_edge)(lambda: wait(win_j - 1))
        pl.when(jnp.logical_not(at_edge))(lambda: wait(win_j))

    arrived(0)
    give = tile_h - (tile_h - 3) * par
    land = tile_h + 2 - (tile_h + 1) * (1 - par)
    swap = pltpu.make_async_remote_copy(
        src_ref=recv.at[:, pl.ds(give, 2)],
        dst_ref=recv.at[:, pl.ds(land, 2)],
        send_sem=swap_send_sem,
        recv_sem=swap_recv_sem,
        device_id=partner,
        device_id_type=MESH,
    )
    swap.start()

    w_swap.wait()
    u = [w1all[:, :, :, k].reshape(chans, 2 * chans).astype(F32) for k in range(5)]
    for dw in range(3):
        v = (u[3], pltpu.roll(u[3], chans, 1), u[4])[dw]
        spread(wt1, u[dw], jnp.where(low, v, 0.0), dw)

    x_pairs, z_pairs = xmat.shape[0], ymat.shape[0]
    o_pairs = z_pairs - 1

    def nth(n, count):
        return (count - 1) * (1 - par) + n * (2 * par - 1)

    def turn_one(n, carry):
        i = nth(n, x_pairs)

        def put(j, value):
            xmat[i, j] = value

        turn(recv, i, put)
        return carry

    def first_one(n, carry):
        i = nth(n, z_pairs)
        fill = jnp.where(n == 0, 1 - par, 2)
        out_of = jnp.where(n == z_pairs - 1, jnp.where(r == 0, 0, jnp.where(r == n_rows - 1, 1, 2)), 2)
        blank_a = jnp.where(fill < 2, fill, out_of)
        first((xmat.at[i], xmat.at[i + 1]), lambda dw: wt1[dw], bias1[...], ymat.at[i], blank_a)
        return carry

    def second_one(n, carry):
        i = nth(n, o_pairs)
        second((ymat.at[i], ymat.at[i + 1]), lambda dw: wt2[dw], bias2[...], out.at[pl.ds(2 * i, 2)])
        return carry

    def stage(s, carry):
        @pl.when(s == 0)
        def _():
            swap.wait()

        for k in range(1, 4):
            there = s == k
            if k == 3:
                there = there & jnp.logical_not(no_outer)
            pl.when(there)(lambda k=k: arrived(k))

        for ends, one in ((TURNS, turn_one), (FIRSTS, first_one), (SECONDS, second_one)):
            lax.fori_loop(step(s, (0, *ends[:-1])), step(s, ends), one, 0)
        return carry

    lax.fori_loop(0, 4, stage, 0)

    per_edge = n_rows * 2
    for chunk in range(4):
        rows = chunks[chunk][0]
        n_r = n_rows - 2 if chunk == 3 else n_rows
        counts = (n_r * 2, n_r * (n_cols - 2))

        def drain(edge_n, inner_n, rows=rows, chunk=chunk):
            wait_bytes(recv.at[0:edge_n, 0:rows, 0 : win_j - 1], send_sem.at[chunk])
            wait_bytes(recv.at[0:inner_n, 0:rows, 0:win_j], send_sem.at[chunk])

        def drain_own(chunk=chunk, counts=counts, drain=drain):
            pl.when(at_edge)(lambda: drain(counts[0] - 1, counts[1]))
            pl.when(jnp.logical_not(at_edge))(lambda: drain(counts[0], counts[1] - 1))

        if chunk == 3:
            pl.when(no_outer)(lambda: drain(*counts))
            pl.when(jnp.logical_not(no_outer))(drain_own)
        else:
            drain_own()


def tail_kernel(tile, ymat, wt2, bias2, out_hbm, o_new, sem):
    par = lax.rem(lax.axis_index("model"), 2)
    rows = out_hbm.shape[0]
    o_pairs = ymat.shape[0] - 1
    late = (rows - 2) * par
    here = 2 * (1 - par)

    def start(k, carry):
        pltpu.make_async_copy(tile.at[par + k], out_hbm.at[k], sem.at[0]).start()
        return carry

    lax.fori_loop(here, here + rows - 2, start, 0)
    i = (o_pairs - 1) * par
    second((ymat.at[i], ymat.at[i + 1]), lambda dw: wt2[dw], bias2[...], o_new)
    last = pltpu.make_async_copy(o_new, out_hbm.at[pl.ds(late, 2)], sem.at[1])
    last.start()
    pltpu.make_async_copy(tile.at[0 : rows - 2], out_hbm.at[0 : rows - 2], sem.at[0]).wait()
    last.wait()


def solution(mesh):
    n_rows = mesh.shape["model"]
    n_cols = mesh.shape["cols"]

    def run_local(x_in, w_conv1, b_conv1, w_conv2, b_conv2):
        images, height, width, own_chans = x_in.shape
        sources = n_rows * n_cols
        chans = own_chans * sources
        pairs = width // 2
        tile_h, tile_j = height // n_rows, pairs // n_cols
        win_j = tile_j + 2
        x_pairs, z_pairs = (tile_h + 5) // 2, (tile_h + 3) // 2
        x_t = jnp.transpose(x_in, (1, 2, 3, 0)).reshape(n_rows // 2, 2 * tile_h, pairs, 2, own_chans, images)
        args = (x_t, w_conv1, b_conv1.reshape(1, chans), w_conv2, b_conv2.reshape(1, chans))
        hbm = pl.BlockSpec(memory_space=pltpu.HBM)
        vmem = pl.BlockSpec(memory_space=pltpu.VMEM)
        kept = (
            pltpu.VMEM((2 * (z_pairs - 1), tile_j, 2, images, chans), F32),
            pltpu.VMEM((z_pairs, win_j - 1, 2, images, 2 * chans), BF16),
            pltpu.VMEM((4, 4 * chans, 4 * chans), BF16),
            pltpu.VMEM((1, 4 * chans), F32),
        )
        state = pl.pallas_call(
            functools.partial(conv_kernel, n_rows, n_cols),
            out_shape=kept,
            in_specs=[hbm] * 5,
            out_specs=[vmem] * len(kept),
            scratch_shapes=[
                pltpu.VMEM((sources, 2 * x_pairs, win_j, own_chans, 2 * images), BF16),
                pltpu.VMEM((x_pairs, win_j, 2, images, 2 * chans), BF16),
                pltpu.VMEM((4, 4 * chans, 4 * chans), BF16),
                pltpu.VMEM((1, 4 * chans), F32),
                pltpu.VMEM((n_rows // 2, 2 * tile_h, pairs, 2, own_chans, images), BF16),
                pltpu.VMEM((height, pairs, own_chans, 2 * images), BF16),
                pltpu.VMEM((3, 3, own_chans, chans), BF16),
                pltpu.VMEM((5, own_chans, 2 * chans), BF16),
                pltpu.VMEM((n_rows // 2, 2, n_cols, 5, own_chans, 2 * chans), BF16),
                pltpu.VMEM((3, 3, chans, chans), BF16),
                pltpu.VMEM((1, chans), F32),
                pltpu.VMEM((1, chans), F32),
                pltpu.SemaphoreType.DMA((3, 2)),
                pltpu.SemaphoreType.DMA((4,)),
                pltpu.SemaphoreType.DMA((4,)),
                pltpu.SemaphoreType.DMA((4,)),
            ]
            + [pltpu.SemaphoreType.DMA] * 6,
            compiler_params=pltpu.CompilerParams(
                collective_id=0, has_side_effects=True, vmem_limit_bytes=24 << 20
            ),
            name="conv",
        )(*(pltpu.with_memory_space_constraint(a, pltpu.HBM) for a in args))
        out = pl.pallas_call(
            tail_kernel,
            out_shape=jax.ShapeDtypeStruct((tile_h, tile_j, 2, images, chans), F32),
            in_specs=[vmem] * len(kept),
            out_specs=pl.BlockSpec(memory_space=pl.ANY),
            scratch_shapes=[
                pltpu.VMEM((2, tile_j, 2, images, chans), F32),
                pltpu.SemaphoreType.DMA((2,)),
            ],
            compiler_params=pltpu.CompilerParams(vmem_limit_bytes=8 << 20),
            name="tail",
        )(*state)
        out = out.reshape(tile_h, 2 * tile_j, images, chans)
        return jnp.transpose(out, (2, 0, 1, 3))

    group = ("model", "cols")
    return jax.shard_map(
        run_local,
        mesh=mesh,
        in_specs=(P("data", None, None, group), P(None, None, group, None), P(), P(), P()),
        out_specs=P("data", "model", "cols", None),
        check_vma=False,
    )
```

```python
import functools

import jax
import jax.numpy as jnp
from jax import lax
from jax.experimental import pallas as pl
from jax.experimental.pallas import tpu as pltpu
from jax.sharding import PartitionSpec as P

MESH = pl.DeviceIdType.MESH
BF16 = jnp.bfloat16
F32 = jnp.float32
CHUNK_ROWS = (2, 3, 2)
TURNS, FIRSTS, SECONDS = (2, 4, 5, 6), (1, 3, 4, 5), (0, 2, 3, 3)
EARLY_FROM = 1
AHEAD = (1, 0)
CHIPS_ALONG = (3, 1, 2, 0)
CHIP_ORDER = tuple((other, dy) for other in (0, 1) for dy in (0, 1, -1, 2))


def turn(recv, i, put):
    sources, _, win_j, own_chans, lanes = recv.shape
    chans = sources * own_chans
    for j in range(win_j):
        top = recv[:, 2 * i, j].reshape(chans, lanes)
        under = recv[:, 2 * i + 1, j].reshape(chans, lanes)
        put(j, jnp.concatenate([top, under], axis=0).T.reshape(2, lanes // 2, 2 * chans))


def blocks(pairs, weights, count):
    acc = None
    for dw in range(4):
        parts = [view[dw // 2 : dw // 2 + count, dw % 2] for view in pairs]
        lhs = jnp.concatenate([p.reshape(count * p.shape[1], p.shape[2]) for p in parts], axis=1)
        term = jnp.dot(lhs, weights(dw), preferred_element_type=F32)
        acc = term if acc is None else acc + term
    return acc


def first(pairs, weights, bias, y_row, blank_a):
    count, _, images, lanes = y_row.shape
    c = lax.axis_index("cols")
    row = lax.rem(lax.broadcasted_iota(jnp.int32, (1, 2 * lanes), 1), lanes) // (lanes // 2)
    act = jnp.maximum(blocks(pairs, weights, count) + bias, 0.0)
    act = jnp.where(row != blank_a, act, 0.0).astype(BF16)
    for b in range(2):
        y_row[:, b] = act[:, b * lanes : (b + 1) * lanes].reshape(count, images, lanes)
    blank = jnp.zeros((images, lanes), BF16)

    @pl.when(c == 0)
    def _():
        y_row[0, 0] = blank

    @pl.when(c == lax.axis_size("cols") - 1)
    def _():
        y_row[count - 1, 1] = blank


def second(pairs, weights, bias, out_pair):
    _, count, _, images, chans = out_pair.shape
    res = blocks(pairs, weights, count) + bias
    for b in range(2):
        for a in range(2):
            at = (2 * b + a) * chans
            out_pair[a, :, b] = res[:, at : at + chans].reshape(count, images, chans)


def conv_kernel(
    n_rows,
    n_cols,
    x_hbm,
    w1_hbm,
    b1_hbm,
    w2_hbm,
    b2_hbm,
    out,
    ymat,
    wt2,
    bias2,
    recv,
    xmat,
    wt1,
    bias1,
    xs,
    packed,
    w1s,
    w1own,
    w1all,
    w2s,
    b1s,
    b2s,
    load_sem,
    par_sem,
    send_sem,
    recv_sem,
    wsend_sem,
    wrecv_sem,
    swap_send_sem,
    swap_recv_sem,
    wswap_send_sem,
    wswap_recv_sem,
):
    chip_h, pairs = xs.shape[1:3]
    images = xs.shape[-1]
    tile_h, tile_j = chip_h // 2, pairs // n_cols
    win_j = tile_j + 2
    sources = n_rows * n_cols
    r, c = lax.axis_index("model"), lax.axis_index("cols")
    par = lax.rem(r, 2)
    me = r * n_cols + c
    chans = recv.shape[0] * 2

    tops = [tile_h - sum(CHUNK_ROWS[: k + 1]) for k in range(len(CHUNK_ROWS))]
    groups = (
        ((tops[0], chip_h - tops[0]),),
        *(((k, k + n), (chip_h - k - n, chip_h - k)) for k, n in zip(tops[1:], CHUNK_ROWS[1:])),
    )
    loads = []
    for g, spans in enumerate(groups):
        loads.append(
            [
                pltpu.make_async_copy(x_hbm.at[:, lo:hi], xs.at[:, lo:hi], load_sem.at[g, n])
                for n, (lo, hi) in enumerate(spans)
            ]
        )
    for copies in loads:
        for copy in copies:
            copy.start()
    params = [
        pltpu.make_async_copy(src, dst, par_sem.at[s])
        for s, (src, dst) in enumerate(((w1_hbm, w1s), (w2_hbm, w2s), (b1_hbm, b1s), (b2_hbm, b2s)))
    ]
    for copy in params:
        copy.start()

    barrier = pltpu.get_barrier_semaphore()
    to_cs = [lax.rem(c + k, n_cols) for k in range(n_cols)]

    def device(to_r, to_c):
        return {"model": to_r, "cols": to_c}

    to_rs = [lax.rem(r + k, n_rows) for k in range(n_rows)]
    for kr, kc in sorted(
        ((kr, kc) for kr in range(n_rows) for kc in range(n_cols) if kr or kc),
        key=lambda k: (k[1] not in (1, 2), k[0] not in (2, 3, 4, 5), k[1] == 2, k[0] < 4, -min(k[0], n_rows - k[0])),
    ):
        pl.semaphore_signal(barrier, inc=1, device_id=device(to_rs[kr], to_cs[kc]), device_id_type=MESH)

    ahead_r, ahead_c = AHEAD
    is_ahead = (r == ahead_r) & (c == ahead_c)

    def pack_rows(x, lo, hi):
        rows = hi - lo
        left, right = (xs[x, lo:hi, :, p].reshape(rows * pairs * 2, images) for p in range(2))
        both = jnp.concatenate([left, right], axis=1)
        packed[pl.ds(chip_h * x + lo, rows)] = both.reshape(rows, pairs, 2, 2 * images)

    def pack(g):
        for n, copy in enumerate(loads[g]):
            if (g, n) != (1, ahead_r % 2):
                copy.wait()

        def body(x, carry):
            for n, (lo, hi) in enumerate(groups[g]):
                if (g, n) == (1, ahead_r % 2):
                    pl.when(x != ahead_r // 2)(lambda lo=lo, hi=hi: pack_rows(x, lo, hi))
                else:
                    pack_rows(x, lo, hi)
            return carry

        lax.fori_loop(0, n_rows // 2, body, 0)

    last = tile_h + 4

    def rows_of(offset, count):
        def where(to_r):
            q = lax.rem(to_r, 2)
            src = tile_h * to_r + offset + (tile_h - count - 2 * offset) * q
            dst = offset + 2 + (last - count - 2 * offset - 3) * q
            return src, dst

        return where

    chunks = (
        *((n, rows_of(k, n), False) for k, n in zip(tops, CHUNK_ROWS)),
        (2, rows_of(-2, 2), True),
    )
    no_outer = (r == 0) | (r == n_rows - 1)
    at_edge = (c == 0) | (c == n_cols - 1)
    own_j = c == 0
    own_j = own_j.astype(jnp.int32)

    def send_tile(chunk, to_r, to_c, there):
        rows, where, is_outer = chunks[chunk]
        src, dst = where(to_r)
        skip = (to_c == 0).astype(jnp.int32)
        edge = (to_c == 0) | (to_c == n_cols - 1)
        if is_outer:
            there = there & (to_r > 0) & (to_r < n_rows - 1)

        def copy(count, src_j, dst_j):
            pltpu.make_async_remote_copy(
                src_ref=packed.at[pl.ds(src, rows), pl.ds(src_j, count)],
                dst_ref=recv.at[me, pl.ds(dst, rows), pl.ds(dst_j, count)],
                send_sem=send_sem.at[chunk],
                recv_sem=recv_sem.at[chunk],
                device_id=device(to_r, to_c),
                device_id_type=MESH,
            ).start()

        pl.when(there & edge)(lambda: copy(win_j - 1, tile_j * to_c - 1 + skip, skip))
        pl.when(there & jnp.logical_not(edge))(lambda: copy(win_j, tile_j * to_c - 1, 0))

    chips = n_rows // 2

    def step(t, table):
        value = jnp.int32(table[-1])
        for k, entry in enumerate(table[:-1]):
            value = jnp.where(t == k, entry, value)
        return value

    def turn_to(t):
        dx = step(t, CHIPS_ALONG)
        return lax.rem(r // 2 + dx, chips), dx

    def send_chip(chunk, t, where=None):
        x, dx = turn_to(t)
        way = 1 - 2 * lax.rem(par + t, 2)
        for other, dy in CHIP_ORDER:
            to_r = 2 * x + (1 - par if other else par)
            to_c = lax.rem(c + way * dy + n_cols, n_cols)
            there = True
            if not other and dy == 0:
                there = dx > 0
            if where is not None:
                there = there & where(to_r, to_c)
            send_tile(chunk, to_r, to_c, there)

    def send_chunk(chunk):
        early = EARLY_FROM <= chunk

        def body(t, carry):
            if chunk > EARLY_FROM:
                send_chip(chunk, t, lambda to_r, to_c: to_c > 0)
            else:
                send_chip(chunk, t, lambda to_r, to_c: (to_r != ahead_r) | (to_c != ahead_c))
            if early and chunk + 1 < len(chunks):
                x, dx = turn_to(t)
                for other in range(2):
                    to_r = 2 * x + (1 - par if other else par)
                    there = (to_r != r) | (c != 0)
                    if chunk > EARLY_FROM:
                        there = there & (to_r != ahead_r)
                    send_tile(chunk + 1, to_r, jnp.int32(0), there)
                if chunk == EARLY_FROM:
                    there = (x == ahead_r // 2) & jnp.logical_not(is_ahead)
                    send_tile(len(chunks) - 1, jnp.int32(ahead_r), jnp.int32(ahead_c), there)
            return carry

        lax.fori_loop(0, chips, body, 0)

    params[0].wait()
    for dw in range(3):
        w1own[dw] = jnp.concatenate([w1s[1, dw], w1s[0, dw]], axis=1)
    w1own[3] = jnp.concatenate([w1s[2, 0], w1s[2, 1]], axis=1)
    w1own[4] = jnp.concatenate([w1s[2, 2], jnp.zeros_like(w1s[2, 2])], axis=1)
    w1all[r // 2, par, c] = w1own[...]

    for copy in loads[0]:
        copy.wait()
    pack_rows(turn_to(0)[0], *groups[0][0])
    pl.semaphore_wait(barrier, sources - 1)

    def send_weights():
        for kr in range(0, n_rows, 2):
            for kc in range(n_cols):
                if kr or kc:
                    pltpu.make_async_remote_copy(
                        src_ref=w1own,
                        dst_ref=w1all.at[r // 2, par, c],
                        send_sem=wsend_sem,
                        recv_sem=wrecv_sem,
                        device_id=device(to_rs[kr], to_cs[kc]),
                        device_id_type=MESH,
                    ).start()

    def pack_and_send(t, carry):
        pl.when(t < chips - 1)(lambda: pack_rows(turn_to(t + 1)[0], *groups[0][0]))
        there = turn_to(t)[0] == ahead_r // 2

        @pl.when(there)
        def _():
            loads[1][ahead_r % 2].wait()
            pack_rows(ahead_r // 2, *groups[1][ahead_r % 2])

        send_chip(0, t)
        send_tile(1, jnp.int32(ahead_r), jnp.int32(ahead_c), there & jnp.logical_not(is_ahead))
        pl.when(t == 0)(send_weights)
        return carry

    lax.fori_loop(0, chips, pack_and_send, 0)

    for g in range(1, EARLY_FROM + 1):
        pack(g)
    for chunk in range(1, len(chunks)):
        if chunk >= EARLY_FROM and chunk + 1 < len(groups):
            pack(chunk + 1)
        send_chunk(chunk)

    def wait_bytes(ref, sem):
        pltpu.make_async_copy(ref, ref, sem).wait()

    w1_bytes = recv.at[0 : sources // 2 - 1, 0, 0:5]
    wait_bytes(w1_bytes, wrecv_sem)
    wait_bytes(w1_bytes, wsend_sem)
    partner = device(r + 1 - 2 * par, c)
    w_swap = pltpu.make_async_remote_copy(
        src_ref=w1all.at[:, par],
        dst_ref=w1all.at[:, par],
        send_sem=wswap_send_sem,
        recv_sem=wswap_recv_sem,
        device_id=partner,
        device_id_type=MESH,
    )
    w_swap.start()

    def own_rows(chunk):
        rows, where, _ = chunks[chunk]
        src, dst = where(r)

        def copy(count, src_j, dst_j):
            for h in range(rows):
                recv[me, dst + h, pl.ds(dst_j, count)] = packed[src + h, pl.ds(src_j, count)]

        pl.when(at_edge)(lambda: copy(win_j - 1, tile_j * c - 1 + own_j, own_j))
        pl.when(jnp.logical_not(at_edge))(lambda: copy(win_j, tile_j * c - 1, 0))

    for chunk in range(3):
        own_rows(chunk)
    pl.when(jnp.logical_not(no_outer))(lambda: own_rows(3))

    zero_row = jnp.zeros((win_j, 2, 2 * images), BF16)
    zero_col = jnp.zeros((tile_h + 2, 2, 2 * images), BF16)

    def clear(s, carry):
        recv[s, last * (1 - par)] = zero_row
        return carry

    def clear_outer(s, carry):
        recv[s, (last - 1) * par] = zero_row
        recv[s, (last - 1) * par + 1] = zero_row
        return carry

    def clear_edge(s, carry):
        recv[s, pl.ds(3 * par, tile_h + 2), (win_j - 1) * (1 - own_j)] = zero_col
        return carry

    lax.fori_loop(0, sources, clear, 0)
    pl.when(no_outer)(lambda: (lax.fori_loop(0, sources, clear_outer, 0), None)[1])
    pl.when(at_edge)(lambda: (lax.fori_loop(0, sources, clear_edge, 0), None)[1])

    low = lax.broadcasted_iota(jnp.int32, (chans, 2 * chans), 1) < chans

    def spread(wt, u, v, dw):
        ur, vr = pltpu.roll(u, chans, 1), pltpu.roll(v, chans, 1)
        zero = jnp.zeros_like(u)
        tiles = (jnp.where(low, ur, zero), u, jnp.where(low, v, ur), jnp.where(low, zero, vr))
        for k, tile in enumerate(tiles):
            tile = tile.astype(BF16)
            for b in range(2):
                wt[dw + b, k * chans : (k + 1) * chans, b * 2 * chans : (b + 1) * 2 * chans] = tile

    def blank(wt):
        zero = jnp.zeros((4 * chans, 2 * chans), BF16)
        wt[3, :, 0 : 2 * chans] = zero
        wt[0, :, 2 * chans : 4 * chans] = zero

    for copy in params[1:]:
        copy.wait()
    blank(wt1)
    blank(wt2)
    for dw in range(3):
        w = [w2s[dh, dw].astype(F32) for dh in range(3)]
        spread(
            wt2,
            jnp.concatenate([w[1], w[0]], axis=1),
            jnp.concatenate([w[2], jnp.zeros_like(w[2])], axis=1),
            dw,
        )
    bias1[...] = jnp.concatenate([b1s[...]] * 4, axis=1)
    bias2[...] = jnp.concatenate([b2s[...]] * 4, axis=1)

    def arrived(chunk):
        def wait(count):
            wait_bytes(recv.at[0 : sources - 1, 0 : chunks[chunk][0], 0:count], recv_sem.at[chunk])

        pl.when(at_edge)(lambda: wait(win_j - 1))
        pl.when(jnp.logical_not(at_edge))(lambda: wait(win_j))

    arrived(0)
    give = tile_h - (tile_h - 3) * par
    land = tile_h + 2 - (tile_h + 1) * (1 - par)
    swap = pltpu.make_async_remote_copy(
        src_ref=recv.at[:, pl.ds(give, 2)],
        dst_ref=recv.at[:, pl.ds(land, 2)],
        send_sem=swap_send_sem,
        recv_sem=swap_recv_sem,
        device_id=partner,
        device_id_type=MESH,
    )
    swap.start()

    w_swap.wait()
    u = [w1all[:, :, :, k].reshape(chans, 2 * chans).astype(F32) for k in range(5)]
    for dw in range(3):
        v = (u[3], pltpu.roll(u[3], chans, 1), u[4])[dw]
        spread(wt1, u[dw], jnp.where(low, v, 0.0), dw)

    x_pairs, z_pairs = xmat.shape[0], ymat.shape[0]
    o_pairs = z_pairs - 1

    def nth(n, count):
        return (count - 1) * (1 - par) + n * (2 * par - 1)

    def turn_one(n, carry):
        i = nth(n, x_pairs)

        def put(j, value):
            xmat[i, j] = value

        turn(recv, i, put)
        return carry

    def first_one(n, carry):
        i = nth(n, z_pairs)
        fill = jnp.where(n == 0, 1 - par, 2)
        out_of = jnp.where(n == z_pairs - 1, jnp.where(r == 0, 0, jnp.where(r == n_rows - 1, 1, 2)), 2)
        blank_a = jnp.where(fill < 2, fill, out_of)
        first((xmat.at[i], xmat.at[i + 1]), lambda dw: wt1[dw], bias1[...], ymat.at[i], blank_a)
        return carry

    def second_one(n, carry):
        i = nth(n, o_pairs)
        second((ymat.at[i], ymat.at[i + 1]), lambda dw: wt2[dw], bias2[...], out.at[pl.ds(2 * i, 2)])
        return carry

    def stage(s, carry):
        @pl.when(s == 0)
        def _():
            swap.wait()

        for k in range(1, 4):
            there = s == k
            if k == 3:
                there = there & jnp.logical_not(no_outer)
            pl.when(there)(lambda k=k: arrived(k))

        for ends, one in ((TURNS, turn_one), (FIRSTS, first_one), (SECONDS, second_one)):
            lax.fori_loop(step(s, (0, *ends[:-1])), step(s, ends), one, 0)
        return carry

    lax.fori_loop(0, 4, stage, 0)

    per_edge = n_rows * 2
    for chunk in range(4):
        rows = chunks[chunk][0]
        n_r = n_rows - 2 if chunk == 3 else n_rows
        counts = (n_r * 2, n_r * (n_cols - 2))

        def drain(edge_n, inner_n, rows=rows, chunk=chunk):
            wait_bytes(recv.at[0:edge_n, 0:rows, 0 : win_j - 1], send_sem.at[chunk])
            wait_bytes(recv.at[0:inner_n, 0:rows, 0:win_j], send_sem.at[chunk])

        def drain_own(chunk=chunk, counts=counts, drain=drain):
            pl.when(at_edge)(lambda: drain(counts[0] - 1, counts[1]))
            pl.when(jnp.logical_not(at_edge))(lambda: drain(counts[0], counts[1] - 1))

        if chunk == 3:
            pl.when(no_outer)(lambda: drain(*counts))
            pl.when(jnp.logical_not(no_outer))(drain_own)
        else:
            drain_own()


def tail_kernel(tile, ymat, wt2, bias2, out_hbm, o_new, sem):
    par = lax.rem(lax.axis_index("model"), 2)
    rows = out_hbm.shape[0]
    o_pairs = ymat.shape[0] - 1
    late = (rows - 2) * par
    here = 2 * (1 - par)

    def start(k, carry):
        pltpu.make_async_copy(tile.at[par + k], out_hbm.at[k], sem.at[0]).start()
        return carry

    lax.fori_loop(here, here + rows - 2, start, 0)
    i = (o_pairs - 1) * par
    second((ymat.at[i], ymat.at[i + 1]), lambda dw: wt2[dw], bias2[...], o_new)
    last = pltpu.make_async_copy(o_new, out_hbm.at[pl.ds(late, 2)], sem.at[1])
    last.start()
    pltpu.make_async_copy(tile.at[0 : rows - 2], out_hbm.at[0 : rows - 2], sem.at[0]).wait()
    last.wait()


def solution(mesh):
    n_rows = mesh.shape["model"]
    n_cols = mesh.shape["cols"]

    def run_local(x_in, w_conv1, b_conv1, w_conv2, b_conv2):
        images, height, width, own_chans = x_in.shape
        sources = n_rows * n_cols
        chans = own_chans * sources
        pairs = width // 2
        tile_h, tile_j = height // n_rows, pairs // n_cols
        win_j = tile_j + 2
        x_pairs, z_pairs = (tile_h + 5) // 2, (tile_h + 3) // 2
        x_t = jnp.transpose(x_in, (1, 2, 3, 0)).reshape(n_rows // 2, 2 * tile_h, pairs, 2, own_chans, images)
        args = (x_t, w_conv1, b_conv1.reshape(1, chans), w_conv2, b_conv2.reshape(1, chans))
        hbm = pl.BlockSpec(memory_space=pltpu.HBM)
        vmem = pl.BlockSpec(memory_space=pltpu.VMEM)
        kept = (
            pltpu.VMEM((2 * (z_pairs - 1), tile_j, 2, images, chans), F32),
            pltpu.VMEM((z_pairs, win_j - 1, 2, images, 2 * chans), BF16),
            pltpu.VMEM((4, 4 * chans, 4 * chans), BF16),
            pltpu.VMEM((1, 4 * chans), F32),
        )
        state = pl.pallas_call(
            functools.partial(conv_kernel, n_rows, n_cols),
            out_shape=kept,
            in_specs=[hbm] * 5,
            out_specs=[vmem] * len(kept),
            scratch_shapes=[
                pltpu.VMEM((sources, 2 * x_pairs, win_j, own_chans, 2 * images), BF16),
                pltpu.VMEM((x_pairs, win_j, 2, images, 2 * chans), BF16),
                pltpu.VMEM((4, 4 * chans, 4 * chans), BF16),
                pltpu.VMEM((1, 4 * chans), F32),
                pltpu.VMEM((n_rows // 2, 2 * tile_h, pairs, 2, own_chans, images), BF16),
                pltpu.VMEM((height, pairs, own_chans, 2 * images), BF16),
                pltpu.VMEM((3, 3, own_chans, chans), BF16),
                pltpu.VMEM((5, own_chans, 2 * chans), BF16),
                pltpu.VMEM((n_rows // 2, 2, n_cols, 5, own_chans, 2 * chans), BF16),
                pltpu.VMEM((3, 3, chans, chans), BF16),
                pltpu.VMEM((1, chans), F32),
                pltpu.VMEM((1, chans), F32),
                pltpu.SemaphoreType.DMA((3, 2)),
                pltpu.SemaphoreType.DMA((4,)),
                pltpu.SemaphoreType.DMA((4,)),
                pltpu.SemaphoreType.DMA((4,)),
            ]
            + [pltpu.SemaphoreType.DMA] * 6,
            compiler_params=pltpu.CompilerParams(
                collective_id=0, has_side_effects=True, vmem_limit_bytes=24 << 20
            ),
            name="conv",
        )(*(pltpu.with_memory_space_constraint(a, pltpu.HBM) for a in args))
        out = pl.pallas_call(
            tail_kernel,
            out_shape=jax.ShapeDtypeStruct((tile_h, tile_j, 2, images, chans), F32),
            in_specs=[vmem] * len(kept),
            out_specs=pl.BlockSpec(memory_space=pl.ANY),
            scratch_shapes=[
                pltpu.VMEM((2, tile_j, 2, images, chans), F32),
                pltpu.SemaphoreType.DMA((2,)),
            ],
            compiler_params=pltpu.CompilerParams(vmem_limit_bytes=8 << 20),
            name="tail",
        )(*state)
        out = out.reshape(tile_h, 2 * tile_j, images, chans)
        return jnp.transpose(out, (2, 0, 1, 3))

    group = ("model", "cols")
    return jax.shard_map(
        run_local,
        mesh=mesh,
        in_specs=(P("data", None, None, group), P(None, None, group, None), P(), P(), P()),
        out_specs=P("data", "model", "cols", None),
        check_vma=False,
    )
```

```python
import functools

import jax
import jax.numpy as jnp
from jax import lax
from jax.experimental import pallas as pl
from jax.experimental.pallas import tpu as pltpu
from jax.sharding import PartitionSpec as P

MESH = pl.DeviceIdType.MESH
BF16 = jnp.bfloat16
F32 = jnp.float32
CHUNK_ROWS = (2, 3, 2)
TURNS, FIRSTS, SECONDS = (2, 4, 5, 6), (1, 3, 4, 5), (0, 2, 3, 3)
EARLY_FROM = 1
AHEAD = (1, 0)
CHIPS_ALONG = (3, 1, 2, 0)
CHIP_ORDER = tuple((other, dy) for other in (0, 1) for dy in (1, -1, 0, 2))


def turn(recv, i, put):
    sources, _, win_j, own_chans, lanes = recv.shape
    chans = sources * own_chans
    for j in range(win_j):
        top = recv[:, 2 * i, j].reshape(chans, lanes)
        under = recv[:, 2 * i + 1, j].reshape(chans, lanes)
        put(j, jnp.concatenate([top, under], axis=0).T.reshape(2, lanes // 2, 2 * chans))


def blocks(pairs, weights, count):
    acc = None
    for dw in range(4):
        parts = [view[dw // 2 : dw // 2 + count, dw % 2] for view in pairs]
        lhs = jnp.concatenate([p.reshape(count * p.shape[1], p.shape[2]) for p in parts], axis=1)
        term = jnp.dot(lhs, weights(dw), preferred_element_type=F32)
        acc = term if acc is None else acc + term
    return acc


def first(pairs, weights, bias, y_row, blank_a):
    count, _, images, lanes = y_row.shape
    c = lax.axis_index("cols")
    row = lax.rem(lax.broadcasted_iota(jnp.int32, (1, 2 * lanes), 1), lanes) // (lanes // 2)
    act = jnp.maximum(blocks(pairs, weights, count) + bias, 0.0)
    act = jnp.where(row != blank_a, act, 0.0).astype(BF16)
    for b in range(2):
        y_row[:, b] = act[:, b * lanes : (b + 1) * lanes].reshape(count, images, lanes)
    blank = jnp.zeros((images, lanes), BF16)

    @pl.when(c == 0)
    def _():
        y_row[0, 0] = blank

    @pl.when(c == lax.axis_size("cols") - 1)
    def _():
        y_row[count - 1, 1] = blank


def second(pairs, weights, bias, out_pair):
    _, count, _, images, chans = out_pair.shape
    res = blocks(pairs, weights, count) + bias
    for b in range(2):
        for a in range(2):
            at = (2 * b + a) * chans
            out_pair[a, :, b] = res[:, at : at + chans].reshape(count, images, chans)


def conv_kernel(
    n_rows,
    n_cols,
    x_hbm,
    w1_hbm,
    b1_hbm,
    w2_hbm,
    b2_hbm,
    out,
    ymat,
    wt2,
    bias2,
    recv,
    xmat,
    wt1,
    bias1,
    xs,
    packed,
    w1s,
    w1own,
    w1all,
    w2s,
    b1s,
    b2s,
    load_sem,
    par_sem,
    send_sem,
    recv_sem,
    wsend_sem,
    wrecv_sem,
    swap_send_sem,
    swap_recv_sem,
    wswap_send_sem,
    wswap_recv_sem,
):
    chip_h, pairs = xs.shape[1:3]
    images = xs.shape[-1]
    tile_h, tile_j = chip_h // 2, pairs // n_cols
    win_j = tile_j + 2
    sources = n_rows * n_cols
    r, c = lax.axis_index("model"), lax.axis_index("cols")
    par = lax.rem(r, 2)
    me = r * n_cols + c
    chans = recv.shape[0] * 2

    tops = [tile_h - sum(CHUNK_ROWS[: k + 1]) for k in range(len(CHUNK_ROWS))]
    groups = (
        ((tops[0], chip_h - tops[0]),),
        *(((k, k + n), (chip_h - k - n, chip_h - k)) for k, n in zip(tops[1:], CHUNK_ROWS[1:])),
    )
    loads = []
    for g, spans in enumerate(groups):
        loads.append(
            [
                pltpu.make_async_copy(x_hbm.at[:, lo:hi], xs.at[:, lo:hi], load_sem.at[g, n])
                for n, (lo, hi) in enumerate(spans)
            ]
        )
    for copies in loads:
        for copy in copies:
            copy.start()
    params = [
        pltpu.make_async_copy(src, dst, par_sem.at[s])
        for s, (src, dst) in enumerate(((w1_hbm, w1s), (w2_hbm, w2s), (b1_hbm, b1s), (b2_hbm, b2s)))
    ]
    for copy in params:
        copy.start()

    barrier = pltpu.get_barrier_semaphore()
    to_cs = [lax.rem(c + k, n_cols) for k in range(n_cols)]

    def device(to_r, to_c):
        return {"model": to_r, "cols": to_c}

    to_rs = [lax.rem(r + k, n_rows) for k in range(n_rows)]
    for kr, kc in sorted(
        ((kr, kc) for kr in range(n_rows) for kc in range(n_cols) if kr or kc),
        key=lambda k: (not (k[0] in (2, 3) and k[1] == 1), -(min(k[0], n_rows - k[0]) // 2 + min(k[1], n_cols - k[1]))),
    ):
        pl.semaphore_signal(barrier, inc=1, device_id=device(to_rs[kr], to_cs[kc]), device_id_type=MESH)

    ahead_r, ahead_c = AHEAD
    is_ahead = (r == ahead_r) & (c == ahead_c)

    def pack_rows(x, lo, hi):
        rows = hi - lo
        left, right = (xs[x, lo:hi, :, p].reshape(rows * pairs * 2, images) for p in range(2))
        both = jnp.concatenate([left, right], axis=1)
        packed[pl.ds(chip_h * x + lo, rows)] = both.reshape(rows, pairs, 2, 2 * images)

    def pack(g):
        for n, copy in enumerate(loads[g]):
            if (g, n) != (1, ahead_r % 2):
                copy.wait()

        def body(x, carry):
            for n, (lo, hi) in enumerate(groups[g]):
                if (g, n) == (1, ahead_r % 2):
                    pl.when(x != ahead_r // 2)(lambda lo=lo, hi=hi: pack_rows(x, lo, hi))
                else:
                    pack_rows(x, lo, hi)
            return carry

        lax.fori_loop(0, n_rows // 2, body, 0)

    last = tile_h + 4

    def rows_of(offset, count):
        def where(to_r):
            q = lax.rem(to_r, 2)
            src = tile_h * to_r + offset + (tile_h - count - 2 * offset) * q
            dst = offset + 2 + (last - count - 2 * offset - 3) * q
            return src, dst

        return where

    chunks = (
        *((n, rows_of(k, n), False) for k, n in zip(tops, CHUNK_ROWS)),
        (2, rows_of(-2, 2), True),
    )
    no_outer = (r == 0) | (r == n_rows - 1)
    at_edge = (c == 0) | (c == n_cols - 1)
    own_j = c == 0
    own_j = own_j.astype(jnp.int32)

    def send_tile(chunk, to_r, to_c, there):
        rows, where, is_outer = chunks[chunk]
        src, dst = where(to_r)
        skip = (to_c == 0).astype(jnp.int32)
        edge = (to_c == 0) | (to_c == n_cols - 1)
        if is_outer:
            there = there & (to_r > 0) & (to_r < n_rows - 1)

        def copy(count, src_j, dst_j):
            pltpu.make_async_remote_copy(
                src_ref=packed.at[pl.ds(src, rows), pl.ds(src_j, count)],
                dst_ref=recv.at[me, pl.ds(dst, rows), pl.ds(dst_j, count)],
                send_sem=send_sem.at[chunk],
                recv_sem=recv_sem.at[chunk],
                device_id=device(to_r, to_c),
                device_id_type=MESH,
            ).start()

        pl.when(there & edge)(lambda: copy(win_j - 1, tile_j * to_c - 1 + skip, skip))
        pl.when(there & jnp.logical_not(edge))(lambda: copy(win_j, tile_j * to_c - 1, 0))

    chips = n_rows // 2

    def step(t, table):
        value = jnp.int32(table[-1])
        for k, entry in enumerate(table[:-1]):
            value = jnp.where(t == k, entry, value)
        return value

    def turn_to(t):
        dx = step(t, CHIPS_ALONG)
        return lax.rem(r // 2 + dx, chips), dx

    def send_chip(chunk, t, where=None):
        x, dx = turn_to(t)
        way = 1 - 2 * lax.rem(par + t, 2)
        for other, dy in CHIP_ORDER:
            to_r = 2 * x + (1 - par if other else par)
            to_c = lax.rem(c + way * dy + n_cols, n_cols)
            there = True
            if not other and dy == 0:
                there = dx > 0
            if where is not None:
                there = there & where(to_r, to_c)
            send_tile(chunk, to_r, to_c, there)

    def send_chunk(chunk):
        early = EARLY_FROM <= chunk

        def body(t, carry):
            if chunk > EARLY_FROM:
                send_chip(chunk, t, lambda to_r, to_c: to_c > 0)
            else:
                send_chip(chunk, t, lambda to_r, to_c: (to_r != ahead_r) | (to_c != ahead_c))
            if early and chunk + 1 < len(chunks):
                x, dx = turn_to(t)
                for other in range(2):
                    to_r = 2 * x + (1 - par if other else par)
                    there = (to_r != r) | (c != 0)
                    if chunk > EARLY_FROM:
                        there = there & (to_r != ahead_r)
                    send_tile(chunk + 1, to_r, jnp.int32(0), there)
                if chunk == EARLY_FROM:
                    there = (x == ahead_r // 2) & jnp.logical_not(is_ahead)
                    send_tile(len(chunks) - 1, jnp.int32(ahead_r), jnp.int32(ahead_c), there)
            return carry

        lax.fori_loop(0, chips, body, 0)

    params[0].wait()
    for dw in range(3):
        w1own[dw] = jnp.concatenate([w1s[1, dw], w1s[0, dw]], axis=1)
    w1own[3] = jnp.concatenate([w1s[2, 0], w1s[2, 1]], axis=1)
    w1own[4] = jnp.concatenate([w1s[2, 2], jnp.zeros_like(w1s[2, 2])], axis=1)
    w1all[r // 2, par, c] = w1own[...]

    for copy in loads[0]:
        copy.wait()
    pack_rows(turn_to(0)[0], *groups[0][0])
    pl.semaphore_wait(barrier, sources - 1)

    def send_weights():
        for kr in range(0, n_rows, 2):
            for kc in range(n_cols):
                if kr or kc:
                    pltpu.make_async_remote_copy(
                        src_ref=w1own,
                        dst_ref=w1all.at[r // 2, par, c],
                        send_sem=wsend_sem,
                        recv_sem=wrecv_sem,
                        device_id=device(to_rs[kr], to_cs[kc]),
                        device_id_type=MESH,
                    ).start()

    def pack_and_send(t, carry):
        pl.when(t < chips - 1)(lambda: pack_rows(turn_to(t + 1)[0], *groups[0][0]))
        there = turn_to(t)[0] == ahead_r // 2

        @pl.when(there)
        def _():
            loads[1][ahead_r % 2].wait()
            pack_rows(ahead_r // 2, *groups[1][ahead_r % 2])

        send_chip(0, t)
        send_tile(1, jnp.int32(ahead_r), jnp.int32(ahead_c), there & jnp.logical_not(is_ahead))
        pl.when(t == 0)(send_weights)
        return carry

    lax.fori_loop(0, chips, pack_and_send, 0)

    for g in range(1, EARLY_FROM + 1):
        pack(g)
    for chunk in range(1, len(chunks)):
        if chunk >= EARLY_FROM and chunk + 1 < len(groups):
            pack(chunk + 1)
        send_chunk(chunk)

    def wait_bytes(ref, sem):
        pltpu.make_async_copy(ref, ref, sem).wait()

    w1_bytes = recv.at[0 : sources // 2 - 1, 0, 0:5]
    wait_bytes(w1_bytes, wrecv_sem)
    wait_bytes(w1_bytes, wsend_sem)
    partner = device(r + 1 - 2 * par, c)
    w_swap = pltpu.make_async_remote_copy(
        src_ref=w1all.at[:, par],
        dst_ref=w1all.at[:, par],
        send_sem=wswap_send_sem,
        recv_sem=wswap_recv_sem,
        device_id=partner,
        device_id_type=MESH,
    )
    w_swap.start()

    def own_rows(chunk):
        rows, where, _ = chunks[chunk]
        src, dst = where(r)

        def copy(count, src_j, dst_j):
            for h in range(rows):
                recv[me, dst + h, pl.ds(dst_j, count)] = packed[src + h, pl.ds(src_j, count)]

        pl.when(at_edge)(lambda: copy(win_j - 1, tile_j * c - 1 + own_j, own_j))
        pl.when(jnp.logical_not(at_edge))(lambda: copy(win_j, tile_j * c - 1, 0))

    for chunk in range(3):
        own_rows(chunk)
    pl.when(jnp.logical_not(no_outer))(lambda: own_rows(3))

    zero_row = jnp.zeros((win_j, 2, 2 * images), BF16)
    zero_col = jnp.zeros((tile_h + 2, 2, 2 * images), BF16)

    def clear(s, carry):
        recv[s, last * (1 - par)] = zero_row
        return carry

    def clear_outer(s, carry):
        recv[s, (last - 1) * par] = zero_row
        recv[s, (last - 1) * par + 1] = zero_row
        return carry

    def clear_edge(s, carry):
        recv[s, pl.ds(3 * par, tile_h + 2), (win_j - 1) * (1 - own_j)] = zero_col
        return carry

    lax.fori_loop(0, sources, clear, 0)
    pl.when(no_outer)(lambda: (lax.fori_loop(0, sources, clear_outer, 0), None)[1])
    pl.when(at_edge)(lambda: (lax.fori_loop(0, sources, clear_edge, 0), None)[1])

    low = lax.broadcasted_iota(jnp.int32, (chans, 2 * chans), 1) < chans

    def spread(wt, u, v, dw):
        ur, vr = pltpu.roll(u, chans, 1), pltpu.roll(v, chans, 1)
        zero = jnp.zeros_like(u)
        tiles = (jnp.where(low, ur, zero), u, jnp.where(low, v, ur), jnp.where(low, zero, vr))
        for k, tile in enumerate(tiles):
            tile = tile.astype(BF16)
            for b in range(2):
                wt[dw + b, k * chans : (k + 1) * chans, b * 2 * chans : (b + 1) * 2 * chans] = tile

    def blank(wt):
        zero = jnp.zeros((4 * chans, 2 * chans), BF16)
        wt[3, :, 0 : 2 * chans] = zero
        wt[0, :, 2 * chans : 4 * chans] = zero

    for copy in params[1:]:
        copy.wait()
    blank(wt1)
    blank(wt2)
    for dw in range(3):
        w = [w2s[dh, dw].astype(F32) for dh in range(3)]
        spread(
            wt2,
            jnp.concatenate([w[1], w[0]], axis=1),
            jnp.concatenate([w[2], jnp.zeros_like(w[2])], axis=1),
            dw,
        )
    bias1[...] = jnp.concatenate([b1s[...]] * 4, axis=1)
    bias2[...] = jnp.concatenate([b2s[...]] * 4, axis=1)

    def arrived(chunk):
        def wait(count):
            wait_bytes(recv.at[0 : sources - 1, 0 : chunks[chunk][0], 0:count], recv_sem.at[chunk])

        pl.when(at_edge)(lambda: wait(win_j - 1))
        pl.when(jnp.logical_not(at_edge))(lambda: wait(win_j))

    arrived(0)
    give = tile_h - (tile_h - 3) * par
    land = tile_h + 2 - (tile_h + 1) * (1 - par)
    swap = pltpu.make_async_remote_copy(
        src_ref=recv.at[:, pl.ds(give, 2)],
        dst_ref=recv.at[:, pl.ds(land, 2)],
        send_sem=swap_send_sem,
        recv_sem=swap_recv_sem,
        device_id=partner,
        device_id_type=MESH,
    )
    swap.start()

    w_swap.wait()
    u = [w1all[:, :, :, k].reshape(chans, 2 * chans).astype(F32) for k in range(5)]
    for dw in range(3):
        v = (u[3], pltpu.roll(u[3], chans, 1), u[4])[dw]
        spread(wt1, u[dw], jnp.where(low, v, 0.0), dw)

    x_pairs, z_pairs = xmat.shape[0], ymat.shape[0]
    o_pairs = z_pairs - 1

    def nth(n, count):
        return (count - 1) * (1 - par) + n * (2 * par - 1)

    def turn_one(n, carry):
        i = nth(n, x_pairs)

        def put(j, value):
            xmat[i, j] = value

        turn(recv, i, put)
        return carry

    def first_one(n, carry):
        i = nth(n, z_pairs)
        fill = jnp.where(n == 0, 1 - par, 2)
        out_of = jnp.where(n == z_pairs - 1, jnp.where(r == 0, 0, jnp.where(r == n_rows - 1, 1, 2)), 2)
        blank_a = jnp.where(fill < 2, fill, out_of)
        first((xmat.at[i], xmat.at[i + 1]), lambda dw: wt1[dw], bias1[...], ymat.at[i], blank_a)
        return carry

    def second_one(n, carry):
        i = nth(n, o_pairs)
        second((ymat.at[i], ymat.at[i + 1]), lambda dw: wt2[dw], bias2[...], out.at[pl.ds(2 * i, 2)])
        return carry

    def stage(s, carry):
        @pl.when(s == 0)
        def _():
            swap.wait()

        for k in range(1, 4):
            there = s == k
            if k == 3:
                there = there & jnp.logical_not(no_outer)
            pl.when(there)(lambda k=k: arrived(k))

        for ends, one in ((TURNS, turn_one), (FIRSTS, first_one), (SECONDS, second_one)):
            lax.fori_loop(step(s, (0, *ends[:-1])), step(s, ends), one, 0)
        return carry

    lax.fori_loop(0, 4, stage, 0)

    per_edge = n_rows * 2
    for chunk in range(4):
        rows = chunks[chunk][0]
        n_r = n_rows - 2 if chunk == 3 else n_rows
        counts = (n_r * 2, n_r * (n_cols - 2))

        def drain(edge_n, inner_n, rows=rows, chunk=chunk):
            wait_bytes(recv.at[0:edge_n, 0:rows, 0 : win_j - 1], send_sem.at[chunk])
            wait_bytes(recv.at[0:inner_n, 0:rows, 0:win_j], send_sem.at[chunk])

        def drain_own(chunk=chunk, counts=counts, drain=drain):
            pl.when(at_edge)(lambda: drain(counts[0] - 1, counts[1]))
            pl.when(jnp.logical_not(at_edge))(lambda: drain(counts[0], counts[1] - 1))

        if chunk == 3:
            pl.when(no_outer)(lambda: drain(*counts))
            pl.when(jnp.logical_not(no_outer))(drain_own)
        else:
            drain_own()


def tail_kernel(tile, ymat, wt2, bias2, out_hbm, o_new, sem):
    par = lax.rem(lax.axis_index("model"), 2)
    rows = out_hbm.shape[0]
    o_pairs = ymat.shape[0] - 1
    late = (rows - 2) * par
    here = 2 * (1 - par)

    def start(k, carry):
        pltpu.make_async_copy(tile.at[par + k], out_hbm.at[k], sem.at[0]).start()
        return carry

    lax.fori_loop(here, here + rows - 2, start, 0)
    i = (o_pairs - 1) * par
    second((ymat.at[i], ymat.at[i + 1]), lambda dw: wt2[dw], bias2[...], o_new)
    last = pltpu.make_async_copy(o_new, out_hbm.at[pl.ds(late, 2)], sem.at[1])
    last.start()
    pltpu.make_async_copy(tile.at[0 : rows - 2], out_hbm.at[0 : rows - 2], sem.at[0]).wait()
    last.wait()


def solution(mesh):
    n_rows = mesh.shape["model"]
    n_cols = mesh.shape["cols"]

    def run_local(x_in, w_conv1, b_conv1, w_conv2, b_conv2):
        images, height, width, own_chans = x_in.shape
        sources = n_rows * n_cols
        chans = own_chans * sources
        pairs = width // 2
        tile_h, tile_j = height // n_rows, pairs // n_cols
        win_j = tile_j + 2
        x_pairs, z_pairs = (tile_h + 5) // 2, (tile_h + 3) // 2
        x_t = jnp.transpose(x_in, (1, 2, 3, 0)).reshape(n_rows // 2, 2 * tile_h, pairs, 2, own_chans, images)
        args = (x_t, w_conv1, b_conv1.reshape(1, chans), w_conv2, b_conv2.reshape(1, chans))
        hbm = pl.BlockSpec(memory_space=pltpu.HBM)
        vmem = pl.BlockSpec(memory_space=pltpu.VMEM)
        kept = (
            pltpu.VMEM((2 * (z_pairs - 1), tile_j, 2, images, chans), F32),
            pltpu.VMEM((z_pairs, win_j - 1, 2, images, 2 * chans), BF16),
            pltpu.VMEM((4, 4 * chans, 4 * chans), BF16),
            pltpu.VMEM((1, 4 * chans), F32),
        )
        state = pl.pallas_call(
            functools.partial(conv_kernel, n_rows, n_cols),
            out_shape=kept,
            in_specs=[hbm] * 5,
            out_specs=[vmem] * len(kept),
            scratch_shapes=[
                pltpu.VMEM((sources, 2 * x_pairs, win_j, own_chans, 2 * images), BF16),
                pltpu.VMEM((x_pairs, win_j, 2, images, 2 * chans), BF16),
                pltpu.VMEM((4, 4 * chans, 4 * chans), BF16),
                pltpu.VMEM((1, 4 * chans), F32),
                pltpu.VMEM((n_rows // 2, 2 * tile_h, pairs, 2, own_chans, images), BF16),
                pltpu.VMEM((height, pairs, own_chans, 2 * images), BF16),
                pltpu.VMEM((3, 3, own_chans, chans), BF16),
                pltpu.VMEM((5, own_chans, 2 * chans), BF16),
                pltpu.VMEM((n_rows // 2, 2, n_cols, 5, own_chans, 2 * chans), BF16),
                pltpu.VMEM((3, 3, chans, chans), BF16),
                pltpu.VMEM((1, chans), F32),
                pltpu.VMEM((1, chans), F32),
                pltpu.SemaphoreType.DMA((3, 2)),
                pltpu.SemaphoreType.DMA((4,)),
                pltpu.SemaphoreType.DMA((4,)),
                pltpu.SemaphoreType.DMA((4,)),
            ]
            + [pltpu.SemaphoreType.DMA] * 6,
            compiler_params=pltpu.CompilerParams(
                collective_id=0, has_side_effects=True, vmem_limit_bytes=24 << 20
            ),
            name="conv",
        )(*(pltpu.with_memory_space_constraint(a, pltpu.HBM) for a in args))
        out = pl.pallas_call(
            tail_kernel,
            out_shape=jax.ShapeDtypeStruct((tile_h, tile_j, 2, images, chans), F32),
            in_specs=[vmem] * len(kept),
            out_specs=pl.BlockSpec(memory_space=pl.ANY),
            scratch_shapes=[
                pltpu.VMEM((2, tile_j, 2, images, chans), F32),
                pltpu.SemaphoreType.DMA((2,)),
            ],
            compiler_params=pltpu.CompilerParams(vmem_limit_bytes=8 << 20),
            name="tail",
        )(*state)
        out = out.reshape(tile_h, 2 * tile_j, images, chans)
        return jnp.transpose(out, (2, 0, 1, 3))

    group = ("model", "cols")
    return jax.shard_map(
        run_local,
        mesh=mesh,
        in_specs=(P("data", None, None, group), P(None, None, group, None), P(), P(), P()),
        out_specs=P("data", "model", "cols", None),
        check_vma=False,
    )
```

```python
import functools

import jax
import jax.numpy as jnp
from jax import lax
from jax.experimental import pallas as pl
from jax.experimental.pallas import tpu as pltpu
from jax.sharding import PartitionSpec as P

MESH = pl.DeviceIdType.MESH
BF16 = jnp.bfloat16
F32 = jnp.float32
CHUNK_ROWS = (2, 3, 2)
TURNS, FIRSTS, SECONDS = (2, 4, 5, 6), (1, 3, 4, 5), (0, 2, 3, 3)
EARLY_FROM = 1
AHEAD = (1, 0)
CHIPS_ALONG = (3, 1, 2, 0)
CHIP_ORDER = tuple((other, dy) for other in (0, 1) for dy in (1, -1, 0, 2))


def turn(recv, i, put):
    sources, _, win_j, own_chans, lanes = recv.shape
    chans = sources * own_chans
    for j in range(win_j):
        top = recv[:, 2 * i, j].reshape(chans, lanes)
        under = recv[:, 2 * i + 1, j].reshape(chans, lanes)
        put(j, jnp.concatenate([top, under], axis=0).T.reshape(2, lanes // 2, 2 * chans))


def blocks(pairs, weights, count):
    acc = None
    for dw in range(4):
        parts = [view[dw // 2 : dw // 2 + count, dw % 2] for view in pairs]
        lhs = jnp.concatenate([p.reshape(count * p.shape[1], p.shape[2]) for p in parts], axis=1)
        term = jnp.dot(lhs, weights(dw), preferred_element_type=F32)
        acc = term if acc is None else acc + term
    return acc


def first(pairs, weights, bias, y_row, blank_a):
    count, _, images, lanes = y_row.shape
    c = lax.axis_index("cols")
    row = lax.rem(lax.broadcasted_iota(jnp.int32, (1, 2 * lanes), 1), lanes) // (lanes // 2)
    act = jnp.maximum(blocks(pairs, weights, count) + bias, 0.0)
    act = jnp.where(row != blank_a, act, 0.0).astype(BF16)
    for b in range(2):
        y_row[:, b] = act[:, b * lanes : (b + 1) * lanes].reshape(count, images, lanes)
    blank = jnp.zeros((images, lanes), BF16)

    @pl.when(c == 0)
    def _():
        y_row[0, 0] = blank

    @pl.when(c == lax.axis_size("cols") - 1)
    def _():
        y_row[count - 1, 1] = blank


def second(pairs, weights, bias, out_pair):
    _, count, _, images, chans = out_pair.shape
    res = blocks(pairs, weights, count) + bias
    for b in range(2):
        for a in range(2):
            at = (2 * b + a) * chans
            out_pair[a, :, b] = res[:, at : at + chans].reshape(count, images, chans)


def conv_kernel(
    n_rows,
    n_cols,
    x_hbm,
    w1_hbm,
    b1_hbm,
    w2_hbm,
    b2_hbm,
    out,
    ymat,
    wt2,
    bias2,
    recv,
    xmat,
    wt1,
    bias1,
    xs,
    packed,
    w1s,
    w1own,
    w1all,
    w2s,
    b1s,
    b2s,
    load_sem,
    par_sem,
    send_sem,
    recv_sem,
    wsend_sem,
    wrecv_sem,
    swap_send_sem,
    swap_recv_sem,
    wswap_send_sem,
    wswap_recv_sem,
):
    chip_h, pairs = xs.shape[1:3]
    images = xs.shape[-1]
    tile_h, tile_j = chip_h // 2, pairs // n_cols
    win_j = tile_j + 2
    sources = n_rows * n_cols
    r, c = lax.axis_index("model"), lax.axis_index("cols")
    par = lax.rem(r, 2)
    me = r * n_cols + c
    chans = recv.shape[0] * 2

    tops = [tile_h - sum(CHUNK_ROWS[: k + 1]) for k in range(len(CHUNK_ROWS))]
    groups = (
        ((tops[0], chip_h - tops[0]),),
        *(((k, k + n), (chip_h - k - n, chip_h - k)) for k, n in zip(tops[1:], CHUNK_ROWS[1:])),
    )
    loads = []
    for g, spans in enumerate(groups):
        loads.append(
            [
                pltpu.make_async_copy(x_hbm.at[:, lo:hi], xs.at[:, lo:hi], load_sem.at[g, n])
                for n, (lo, hi) in enumerate(spans)
            ]
        )
    for copies in loads:
        for copy in copies:
            copy.start()
    params = [
        pltpu.make_async_copy(src, dst, par_sem.at[s])
        for s, (src, dst) in enumerate(((w1_hbm, w1s), (w2_hbm, w2s), (b1_hbm, b1s), (b2_hbm, b2s)))
    ]
    for copy in params:
        copy.start()

    barrier = pltpu.get_barrier_semaphore()
    to_cs = [lax.rem(c + k, n_cols) for k in range(n_cols)]

    def device(to_r, to_c):
        return {"model": to_r, "cols": to_c}

    to_rs = [lax.rem(r + k, n_rows) for k in range(n_rows)]
    for kr, kc in sorted(
        ((kr, kc) for kr in range(n_rows) for kc in range(n_cols) if kr or kc),
        key=lambda k: (k[1] not in (1, 2), k[0] not in (2, 3, 4, 5), k[1] == 2, k[0] < 4, -min(k[0], n_rows - k[0])),
    ):
        pl.semaphore_signal(barrier, inc=1, device_id=device(to_rs[kr], to_cs[kc]), device_id_type=MESH)

    ahead_r, ahead_c = AHEAD
    is_ahead = (r == ahead_r) & (c == ahead_c)

    def pack_rows(x, lo, hi):
        rows = hi - lo
        left, right = (xs[x, lo:hi, :, p].reshape(rows * pairs * 2, images) for p in range(2))
        both = jnp.concatenate([left, right], axis=1)
        packed[pl.ds(chip_h * x + lo, rows)] = both.reshape(rows, pairs, 2, 2 * images)

    def pack(g):
        for n, copy in enumerate(loads[g]):
            if (g, n) != (1, ahead_r % 2):
                copy.wait()

        def body(x, carry):
            for n, (lo, hi) in enumerate(groups[g]):
                if (g, n) == (1, ahead_r % 2):
                    pl.when(x != ahead_r // 2)(lambda lo=lo, hi=hi: pack_rows(x, lo, hi))
                else:
                    pack_rows(x, lo, hi)
            return carry

        lax.fori_loop(0, n_rows // 2, body, 0)

    last = tile_h + 4

    def rows_of(offset, count):
        def where(to_r):
            q = lax.rem(to_r, 2)
            src = tile_h * to_r + offset + (tile_h - count - 2 * offset) * q
            dst = offset + 2 + (last - count - 2 * offset - 3) * q
            return src, dst

        return where

    chunks = (
        *((n, rows_of(k, n), False) for k, n in zip(tops, CHUNK_ROWS)),
        (2, rows_of(-2, 2), True),
    )
    no_outer = (r == 0) | (r == n_rows - 1)
    at_edge = (c == 0) | (c == n_cols - 1)
    own_j = c == 0
    own_j = own_j.astype(jnp.int32)

    def send_tile(chunk, to_r, to_c, there):
        rows, where, is_outer = chunks[chunk]
        src, dst = where(to_r)
        skip = (to_c == 0).astype(jnp.int32)
        edge = (to_c == 0) | (to_c == n_cols - 1)
        if is_outer:
            there = there & (to_r > 0) & (to_r < n_rows - 1)

        def copy(count, src_j, dst_j):
            pltpu.make_async_remote_copy(
                src_ref=packed.at[pl.ds(src, rows), pl.ds(src_j, count)],
                dst_ref=recv.at[me, pl.ds(dst, rows), pl.ds(dst_j, count)],
                send_sem=send_sem.at[chunk],
                recv_sem=recv_sem.at[chunk],
                device_id=device(to_r, to_c),
                device_id_type=MESH,
            ).start()

        pl.when(there & edge)(lambda: copy(win_j - 1, tile_j * to_c - 1 + skip, skip))
        pl.when(there & jnp.logical_not(edge))(lambda: copy(win_j, tile_j * to_c - 1, 0))

    chips = n_rows // 2

    def step(t, table):
        value = jnp.int32(table[-1])
        for k, entry in enumerate(table[:-1]):
            value = jnp.where(t == k, entry, value)
        return value

    def turn_to(t):
        dx = step(t, CHIPS_ALONG)
        return lax.rem(r // 2 + dx, chips), dx

    def send_chip(chunk, t, where=None):
        x, dx = turn_to(t)
        way = 1 - 2 * lax.rem(par + t, 2)
        for other, dy in CHIP_ORDER:
            to_r = 2 * x + (1 - par if other else par)
            to_c = lax.rem(c + way * dy + n_cols, n_cols)
            there = True
            if not other and dy == 0:
                there = dx > 0
            if where is not None:
                there = there & where(to_r, to_c)
            send_tile(chunk, to_r, to_c, there)

    def send_chunk(chunk):
        early = EARLY_FROM <= chunk

        def body(t, carry):
            if chunk > EARLY_FROM:
                send_chip(chunk, t, lambda to_r, to_c: to_c > 0)
            else:
                send_chip(chunk, t, lambda to_r, to_c: (to_r != ahead_r) | (to_c != ahead_c))
            if early and chunk + 1 < len(chunks):
                x, dx = turn_to(t)
                for other in range(2):
                    to_r = 2 * x + (1 - par if other else par)
                    there = (to_r != r) | (c != 0)
                    if chunk > EARLY_FROM:
                        there = there & (to_r != ahead_r)
                    send_tile(chunk + 1, to_r, jnp.int32(0), there)
                if chunk == EARLY_FROM:
                    there = (x == ahead_r // 2) & jnp.logical_not(is_ahead)
                    send_tile(len(chunks) - 1, jnp.int32(ahead_r), jnp.int32(ahead_c), there)
            return carry

        lax.fori_loop(0, chips, body, 0)

    params[0].wait()
    for dw in range(3):
        w1own[dw] = jnp.concatenate([w1s[1, dw], w1s[0, dw]], axis=1)
    w1own[3] = jnp.concatenate([w1s[2, 0], w1s[2, 1]], axis=1)
    w1own[4] = jnp.concatenate([w1s[2, 2], jnp.zeros_like(w1s[2, 2])], axis=1)
    w1all[r // 2, par, c] = w1own[...]

    for copy in loads[0]:
        copy.wait()
    pack_rows(turn_to(0)[0], *groups[0][0])
    pl.semaphore_wait(barrier, sources - 1)

    def send_weights():
        for kr in range(0, n_rows, 2):
            for kc in range(n_cols):
                if kr or kc:
                    pltpu.make_async_remote_copy(
                        src_ref=w1own,
                        dst_ref=w1all.at[r // 2, par, c],
                        send_sem=wsend_sem,
                        recv_sem=wrecv_sem,
                        device_id=device(to_rs[kr], to_cs[kc]),
                        device_id_type=MESH,
                    ).start()

    def pack_and_send(t, carry):
        pl.when(t < chips - 1)(lambda: pack_rows(turn_to(t + 1)[0], *groups[0][0]))
        there = turn_to(t)[0] == ahead_r // 2

        @pl.when(there)
        def _():
            loads[1][ahead_r % 2].wait()
            pack_rows(ahead_r // 2, *groups[1][ahead_r % 2])

        send_chip(0, t)
        send_tile(1, jnp.int32(ahead_r), jnp.int32(ahead_c), there & jnp.logical_not(is_ahead))
        pl.when(t == 0)(send_weights)
        return carry

    lax.fori_loop(0, chips, pack_and_send, 0)

    for g in range(1, EARLY_FROM + 1):
        pack(g)
    for chunk in range(1, len(chunks)):
        if chunk >= EARLY_FROM and chunk + 1 < len(groups):
            pack(chunk + 1)
        send_chunk(chunk)

    def wait_bytes(ref, sem):
        pltpu.make_async_copy(ref, ref, sem).wait()

    w1_bytes = recv.at[0 : sources // 2 - 1, 0, 0:5]
    wait_bytes(w1_bytes, wrecv_sem)
    wait_bytes(w1_bytes, wsend_sem)
    partner = device(r + 1 - 2 * par, c)
    w_swap = pltpu.make_async_remote_copy(
        src_ref=w1all.at[:, par],
        dst_ref=w1all.at[:, par],
        send_sem=wswap_send_sem,
        recv_sem=wswap_recv_sem,
        device_id=partner,
        device_id_type=MESH,
    )
    w_swap.start()

    def own_rows(chunk):
        rows, where, _ = chunks[chunk]
        src, dst = where(r)

        def copy(count, src_j, dst_j):
            for h in range(rows):
                recv[me, dst + h, pl.ds(dst_j, count)] = packed[src + h, pl.ds(src_j, count)]

        pl.when(at_edge)(lambda: copy(win_j - 1, tile_j * c - 1 + own_j, own_j))
        pl.when(jnp.logical_not(at_edge))(lambda: copy(win_j, tile_j * c - 1, 0))

    for chunk in range(3):
        own_rows(chunk)
    pl.when(jnp.logical_not(no_outer))(lambda: own_rows(3))

    zero_row = jnp.zeros((win_j, 2, 2 * images), BF16)
    zero_col = jnp.zeros((tile_h + 2, 2, 2 * images), BF16)

    def clear(s, carry):
        recv[s, last * (1 - par)] = zero_row
        return carry

    def clear_outer(s, carry):
        recv[s, (last - 1) * par] = zero_row
        recv[s, (last - 1) * par + 1] = zero_row
        return carry

    def clear_edge(s, carry):
        recv[s, pl.ds(3 * par, tile_h + 2), (win_j - 1) * (1 - own_j)] = zero_col
        return carry

    lax.fori_loop(0, sources, clear, 0)
    pl.when(no_outer)(lambda: (lax.fori_loop(0, sources, clear_outer, 0), None)[1])
    pl.when(at_edge)(lambda: (lax.fori_loop(0, sources, clear_edge, 0), None)[1])

    low = lax.broadcasted_iota(jnp.int32, (chans, 2 * chans), 1) < chans

    def spread(wt, u, v, dw):
        ur, vr = pltpu.roll(u, chans, 1), pltpu.roll(v, chans, 1)
        zero = jnp.zeros_like(u)
        tiles = (jnp.where(low, ur, zero), u, jnp.where(low, v, ur), jnp.where(low, zero, vr))
        for k, tile in enumerate(tiles):
            tile = tile.astype(BF16)
            for b in range(2):
                wt[dw + b, k * chans : (k + 1) * chans, b * 2 * chans : (b + 1) * 2 * chans] = tile

    def blank(wt):
        zero = jnp.zeros((4 * chans, 2 * chans), BF16)
        wt[3, :, 0 : 2 * chans] = zero
        wt[0, :, 2 * chans : 4 * chans] = zero

    for copy in params[1:]:
        copy.wait()
    blank(wt1)
    blank(wt2)
    for dw in range(3):
        w = [w2s[dh, dw].astype(F32) for dh in range(3)]
        spread(
            wt2,
            jnp.concatenate([w[1], w[0]], axis=1),
            jnp.concatenate([w[2], jnp.zeros_like(w[2])], axis=1),
            dw,
        )
    bias1[...] = jnp.concatenate([b1s[...]] * 4, axis=1)
    bias2[...] = jnp.concatenate([b2s[...]] * 4, axis=1)

    def arrived(chunk):
        def wait(count):
            wait_bytes(recv.at[0 : sources - 1, 0 : chunks[chunk][0], 0:count], recv_sem.at[chunk])

        pl.when(at_edge)(lambda: wait(win_j - 1))
        pl.when(jnp.logical_not(at_edge))(lambda: wait(win_j))

    arrived(0)
    give = tile_h - (tile_h - 3) * par
    land = tile_h + 2 - (tile_h + 1) * (1 - par)
    swap = pltpu.make_async_remote_copy(
        src_ref=recv.at[:, pl.ds(give, 2)],
        dst_ref=recv.at[:, pl.ds(land, 2)],
        send_sem=swap_send_sem,
        recv_sem=swap_recv_sem,
        device_id=partner,
        device_id_type=MESH,
    )
    swap.start()

    w_swap.wait()
    u = [w1all[:, :, :, k].reshape(chans, 2 * chans).astype(F32) for k in range(5)]
    for dw in range(3):
        v = (u[3], pltpu.roll(u[3], chans, 1), u[4])[dw]
        spread(wt1, u[dw], jnp.where(low, v, 0.0), dw)

    x_pairs, z_pairs = xmat.shape[0], ymat.shape[0]
    o_pairs = z_pairs - 1

    def nth(n, count):
        return (count - 1) * (1 - par) + n * (2 * par - 1)

    def turn_one(n, carry):
        i = nth(n, x_pairs)

        def put(j, value):
            xmat[i, j] = value

        turn(recv, i, put)
        return carry

    def first_one(n, carry):
        i = nth(n, z_pairs)
        fill = jnp.where(n == 0, 1 - par, 2)
        out_of = jnp.where(n == z_pairs - 1, jnp.where(r == 0, 0, jnp.where(r == n_rows - 1, 1, 2)), 2)
        blank_a = jnp.where(fill < 2, fill, out_of)
        first((xmat.at[i], xmat.at[i + 1]), lambda dw: wt1[dw], bias1[...], ymat.at[i], blank_a)
        return carry

    def second_one(n, carry):
        i = nth(n, o_pairs)
        second((ymat.at[i], ymat.at[i + 1]), lambda dw: wt2[dw], bias2[...], out.at[pl.ds(2 * i, 2)])
        return carry

    def stage(s, carry):
        @pl.when(s == 0)
        def _():
            swap.wait()

        for k in range(1, 4):
            there = s == k
            if k == 3:
                there = there & jnp.logical_not(no_outer)
            pl.when(there)(lambda k=k: arrived(k))

        for ends, one in ((TURNS, turn_one), (FIRSTS, first_one), (SECONDS, second_one)):
            lax.fori_loop(step(s, (0, *ends[:-1])), step(s, ends), one, 0)
        return carry

    lax.fori_loop(0, 4, stage, 0)

    per_edge = n_rows * 2
    for chunk in range(4):
        rows = chunks[chunk][0]
        n_r = n_rows - 2 if chunk == 3 else n_rows
        counts = (n_r * 2, n_r * (n_cols - 2))

        def drain(edge_n, inner_n, rows=rows, chunk=chunk):
            wait_bytes(recv.at[0:edge_n, 0:rows, 0 : win_j - 1], send_sem.at[chunk])
            wait_bytes(recv.at[0:inner_n, 0:rows, 0:win_j], send_sem.at[chunk])

        def drain_own(chunk=chunk, counts=counts, drain=drain):
            pl.when(at_edge)(lambda: drain(counts[0] - 1, counts[1]))
            pl.when(jnp.logical_not(at_edge))(lambda: drain(counts[0], counts[1] - 1))

        if chunk == 3:
            pl.when(no_outer)(lambda: drain(*counts))
            pl.when(jnp.logical_not(no_outer))(drain_own)
        else:
            drain_own()


def tail_kernel(tile, ymat, wt2, bias2, out_hbm, o_new, sem):
    par = lax.rem(lax.axis_index("model"), 2)
    rows = out_hbm.shape[0]
    o_pairs = ymat.shape[0] - 1
    late = (rows - 2) * par
    here = 2 * (1 - par)

    def start(k, carry):
        pltpu.make_async_copy(tile.at[par + k], out_hbm.at[k], sem.at[0]).start()
        return carry

    lax.fori_loop(here, here + rows - 2, start, 0)
    i = (o_pairs - 1) * par
    second((ymat.at[i], ymat.at[i + 1]), lambda dw: wt2[dw], bias2[...], o_new)
    last = pltpu.make_async_copy(o_new, out_hbm.at[pl.ds(late, 2)], sem.at[1])
    last.start()
    pltpu.make_async_copy(tile.at[0 : rows - 2], out_hbm.at[0 : rows - 2], sem.at[0]).wait()
    last.wait()


def solution(mesh):
    n_rows = mesh.shape["model"]
    n_cols = mesh.shape["cols"]

    def run_local(x_in, w_conv1, b_conv1, w_conv2, b_conv2):
        images, height, width, own_chans = x_in.shape
        sources = n_rows * n_cols
        chans = own_chans * sources
        pairs = width // 2
        tile_h, tile_j = height // n_rows, pairs // n_cols
        win_j = tile_j + 2
        x_pairs, z_pairs = (tile_h + 5) // 2, (tile_h + 3) // 2
        x_t = jnp.transpose(x_in, (1, 2, 3, 0)).reshape(n_rows // 2, 2 * tile_h, pairs, 2, own_chans, images)
        args = (x_t, w_conv1, b_conv1.reshape(1, chans), w_conv2, b_conv2.reshape(1, chans))
        hbm = pl.BlockSpec(memory_space=pltpu.HBM)
        vmem = pl.BlockSpec(memory_space=pltpu.VMEM)
        kept = (
            pltpu.VMEM((2 * (z_pairs - 1), tile_j, 2, images, chans), F32),
            pltpu.VMEM((z_pairs, win_j - 1, 2, images, 2 * chans), BF16),
            pltpu.VMEM((4, 4 * chans, 4 * chans), BF16),
            pltpu.VMEM((1, 4 * chans), F32),
        )
        state = pl.pallas_call(
            functools.partial(conv_kernel, n_rows, n_cols),
            out_shape=kept,
            in_specs=[hbm] * 5,
            out_specs=[vmem] * len(kept),
            scratch_shapes=[
                pltpu.VMEM((sources, 2 * x_pairs, win_j, own_chans, 2 * images), BF16),
                pltpu.VMEM((x_pairs, win_j, 2, images, 2 * chans), BF16),
                pltpu.VMEM((4, 4 * chans, 4 * chans), BF16),
                pltpu.VMEM((1, 4 * chans), F32),
                pltpu.VMEM((n_rows // 2, 2 * tile_h, pairs, 2, own_chans, images), BF16),
                pltpu.VMEM((height, pairs, own_chans, 2 * images), BF16),
                pltpu.VMEM((3, 3, own_chans, chans), BF16),
                pltpu.VMEM((5, own_chans, 2 * chans), BF16),
                pltpu.VMEM((n_rows // 2, 2, n_cols, 5, own_chans, 2 * chans), BF16),
                pltpu.VMEM((3, 3, chans, chans), BF16),
                pltpu.VMEM((1, chans), F32),
                pltpu.VMEM((1, chans), F32),
                pltpu.SemaphoreType.DMA((3, 2)),
                pltpu.SemaphoreType.DMA((4,)),
                pltpu.SemaphoreType.DMA((4,)),
                pltpu.SemaphoreType.DMA((4,)),
            ]
            + [pltpu.SemaphoreType.DMA] * 6,
            compiler_params=pltpu.CompilerParams(
                collective_id=0, has_side_effects=True, vmem_limit_bytes=24 << 20
            ),
            name="conv",
        )(*(pltpu.with_memory_space_constraint(a, pltpu.HBM) for a in args))
        out = pl.pallas_call(
            tail_kernel,
            out_shape=jax.ShapeDtypeStruct((tile_h, tile_j, 2, images, chans), F32),
            in_specs=[vmem] * len(kept),
            out_specs=pl.BlockSpec(memory_space=pl.ANY),
            scratch_shapes=[
                pltpu.VMEM((2, tile_j, 2, images, chans), F32),
                pltpu.SemaphoreType.DMA((2,)),
            ],
            compiler_params=pltpu.CompilerParams(vmem_limit_bytes=8 << 20),
            name="tail",
        )(*state)
        out = out.reshape(tile_h, 2 * tile_j, images, chans)
        return jnp.transpose(out, (2, 0, 1, 3))

    group = ("model", "cols")
    return jax.shard_map(
        run_local,
        mesh=mesh,
        in_specs=(P("data", None, None, group), P(None, None, group, None), P(), P(), P()),
        out_specs=P("data", "model", "cols", None),
        check_vma=False,
    )
```

```python
import functools

import jax
import jax.numpy as jnp
from jax import lax
from jax.experimental import pallas as pl
from jax.experimental.pallas import tpu as pltpu
from jax.sharding import PartitionSpec as P

MESH = pl.DeviceIdType.MESH
BF16 = jnp.bfloat16
F32 = jnp.float32
CHUNK_ROWS = (2, 3, 2)
TURNS, FIRSTS, SECONDS = (2, 4, 5, 6), (1, 3, 4, 5), (0, 2, 3, 3)
EARLY_FROM = 1
AHEAD = (1, 0)
CHIPS_ALONG = (1, 3, 2, 0)
CHIP_ORDER = tuple((other, dy) for other in (0, 1) for dy in (0, 1, -1, 2))


def turn(recv, i, put):
    sources, _, win_j, own_chans, lanes = recv.shape
    chans = sources * own_chans
    for j in range(win_j):
        top = recv[:, 2 * i, j].reshape(chans, lanes)
        under = recv[:, 2 * i + 1, j].reshape(chans, lanes)
        put(j, jnp.concatenate([top, under], axis=0).T.reshape(2, lanes // 2, 2 * chans))


def blocks(pairs, weights, count):
    acc = None
    for dw in range(4):
        parts = [view[dw // 2 : dw // 2 + count, dw % 2] for view in pairs]
        lhs = jnp.concatenate([p.reshape(count * p.shape[1], p.shape[2]) for p in parts], axis=1)
        term = jnp.dot(lhs, weights(dw), preferred_element_type=F32)
        acc = term if acc is None else acc + term
    return acc


def first(pairs, weights, bias, y_row, blank_a):
    count, _, images, lanes = y_row.shape
    c = lax.axis_index("cols")
    row = lax.rem(lax.broadcasted_iota(jnp.int32, (1, 2 * lanes), 1), lanes) // (lanes // 2)
    act = jnp.maximum(blocks(pairs, weights, count) + bias, 0.0)
    act = jnp.where(row != blank_a, act, 0.0).astype(BF16)
    for b in range(2):
        y_row[:, b] = act[:, b * lanes : (b + 1) * lanes].reshape(count, images, lanes)
    blank = jnp.zeros((images, lanes), BF16)

    @pl.when(c == 0)
    def _():
        y_row[0, 0] = blank

    @pl.when(c == lax.axis_size("cols") - 1)
    def _():
        y_row[count - 1, 1] = blank


def second(pairs, weights, bias, out_pair):
    _, count, _, images, chans = out_pair.shape
    res = blocks(pairs, weights, count) + bias
    for b in range(2):
        for a in range(2):
            at = (2 * b + a) * chans
            out_pair[a, :, b] = res[:, at : at + chans].reshape(count, images, chans)


def conv_kernel(
    n_rows,
    n_cols,
    x_hbm,
    w1_hbm,
    b1_hbm,
    w2_hbm,
    b2_hbm,
    out,
    ymat,
    wt2,
    bias2,
    recv,
    xmat,
    wt1,
    bias1,
    xs,
    packed,
    w1s,
    w1own,
    w1all,
    w2s,
    b1s,
    b2s,
    load_sem,
    par_sem,
    send_sem,
    recv_sem,
    wsend_sem,
    wrecv_sem,
    swap_send_sem,
    swap_recv_sem,
    wswap_send_sem,
    wswap_recv_sem,
):
    chip_h, pairs = xs.shape[1:3]
    images = xs.shape[-1]
    tile_h, tile_j = chip_h // 2, pairs // n_cols
    win_j = tile_j + 2
    sources = n_rows * n_cols
    r, c = lax.axis_index("model"), lax.axis_index("cols")
    par = lax.rem(r, 2)
    me = r * n_cols + c
    chans = recv.shape[0] * 2

    tops = [tile_h - sum(CHUNK_ROWS[: k + 1]) for k in range(len(CHUNK_ROWS))]
    groups = (
        ((tops[0], chip_h - tops[0]),),
        *(((k, k + n), (chip_h - k - n, chip_h - k)) for k, n in zip(tops[1:], CHUNK_ROWS[1:])),
    )
    loads = []
    for g, spans in enumerate(groups):
        loads.append(
            [
                pltpu.make_async_copy(x_hbm.at[:, lo:hi], xs.at[:, lo:hi], load_sem.at[g, n])
                for n, (lo, hi) in enumerate(spans)
            ]
        )
    for copies in loads:
        for copy in copies:
            copy.start()
    params = [
        pltpu.make_async_copy(src, dst, par_sem.at[s])
        for s, (src, dst) in enumerate(((w1_hbm, w1s), (w2_hbm, w2s), (b1_hbm, b1s), (b2_hbm, b2s)))
    ]
    for copy in params:
        copy.start()

    barrier = pltpu.get_barrier_semaphore()
    to_cs = [lax.rem(c + k, n_cols) for k in range(n_cols)]

    def device(to_r, to_c):
        return {"model": to_r, "cols": to_c}

    to_rs = [lax.rem(r + k, n_rows) for k in range(n_rows)]
    for kr, kc in sorted(
        ((kr, kc) for kr in range(n_rows) for kc in range(n_cols) if kr or kc),
        key=lambda k: (k[1] not in (1, 2), k[0] not in (2, 3, 4, 5), k[1] == 2, k[0] < 4, -min(k[0], n_rows - k[0])),
    ):
        pl.semaphore_signal(barrier, inc=1, device_id=device(to_rs[kr], to_cs[kc]), device_id_type=MESH)

    ahead_r, ahead_c = AHEAD
    is_ahead = (r == ahead_r) & (c == ahead_c)

    def pack_rows(x, lo, hi):
        rows = hi - lo
        left, right = (xs[x, lo:hi, :, p].reshape(rows * pairs * 2, images) for p in range(2))
        both = jnp.concatenate([left, right], axis=1)
        packed[pl.ds(chip_h * x + lo, rows)] = both.reshape(rows, pairs, 2, 2 * images)

    def pack(g):
        for n, copy in enumerate(loads[g]):
            if (g, n) != (1, ahead_r % 2):
                copy.wait()

        def body(x, carry):
            for n, (lo, hi) in enumerate(groups[g]):
                if (g, n) == (1, ahead_r % 2):
                    pl.when(x != ahead_r // 2)(lambda lo=lo, hi=hi: pack_rows(x, lo, hi))
                else:
                    pack_rows(x, lo, hi)
            return carry

        lax.fori_loop(0, n_rows // 2, body, 0)

    last = tile_h + 4

    def rows_of(offset, count):
        def where(to_r):
            q = lax.rem(to_r, 2)
            src = tile_h * to_r + offset + (tile_h - count - 2 * offset) * q
            dst = offset + 2 + (last - count - 2 * offset - 3) * q
            return src, dst

        return where

    chunks = (
        *((n, rows_of(k, n), False) for k, n in zip(tops, CHUNK_ROWS)),
        (2, rows_of(-2, 2), True),
    )
    no_outer = (r == 0) | (r == n_rows - 1)
    at_edge = (c == 0) | (c == n_cols - 1)
    own_j = c == 0
    own_j = own_j.astype(jnp.int32)

    def send_tile(chunk, to_r, to_c, there):
        rows, where, is_outer = chunks[chunk]
        src, dst = where(to_r)
        skip = (to_c == 0).astype(jnp.int32)
        edge = (to_c == 0) | (to_c == n_cols - 1)
        if is_outer:
            there = there & (to_r > 0) & (to_r < n_rows - 1)

        def copy(count, src_j, dst_j):
            pltpu.make_async_remote_copy(
                src_ref=packed.at[pl.ds(src, rows), pl.ds(src_j, count)],
                dst_ref=recv.at[me, pl.ds(dst, rows), pl.ds(dst_j, count)],
                send_sem=send_sem.at[chunk],
                recv_sem=recv_sem.at[chunk],
                device_id=device(to_r, to_c),
                device_id_type=MESH,
            ).start()

        pl.when(there & edge)(lambda: copy(win_j - 1, tile_j * to_c - 1 + skip, skip))
        pl.when(there & jnp.logical_not(edge))(lambda: copy(win_j, tile_j * to_c - 1, 0))

    chips = n_rows // 2

    def step(t, table):
        value = jnp.int32(table[-1])
        for k, entry in enumerate(table[:-1]):
            value = jnp.where(t == k, entry, value)
        return value

    def turn_to(t):
        dx = step(t, CHIPS_ALONG)
        return lax.rem(r // 2 + dx, chips), dx

    def send_chip(chunk, t, where=None):
        x, dx = turn_to(t)
        way = 1 - 2 * lax.rem(par + t, 2)
        for other, dy in CHIP_ORDER:
            to_r = 2 * x + (1 - par if other else par)
            to_c = lax.rem(c + way * dy + n_cols, n_cols)
            there = True
            if not other and dy == 0:
                there = dx > 0
            if where is not None:
                there = there & where(to_r, to_c)
            send_tile(chunk, to_r, to_c, there)

    def send_chunk(chunk):
        early = EARLY_FROM <= chunk

        def body(t, carry):
            if chunk > EARLY_FROM:
                send_chip(chunk, t, lambda to_r, to_c: to_c > 0)
            else:
                send_chip(chunk, t, lambda to_r, to_c: (to_r != ahead_r) | (to_c != ahead_c))
            if early and chunk + 1 < len(chunks):
                x, dx = turn_to(t)
                for other in range(2):
                    to_r = 2 * x + (1 - par if other else par)
                    there = (to_r != r) | (c != 0)
                    if chunk > EARLY_FROM:
                        there = there & (to_r != ahead_r)
                    send_tile(chunk + 1, to_r, jnp.int32(0), there)
                if chunk == EARLY_FROM:
                    there = (x == ahead_r // 2) & jnp.logical_not(is_ahead)
                    send_tile(len(chunks) - 1, jnp.int32(ahead_r), jnp.int32(ahead_c), there)
            return carry

        lax.fori_loop(0, chips, body, 0)

    params[0].wait()
    for dw in range(3):
        w1own[dw] = jnp.concatenate([w1s[1, dw], w1s[0, dw]], axis=1)
    w1own[3] = jnp.concatenate([w1s[2, 0], w1s[2, 1]], axis=1)
    w1own[4] = jnp.concatenate([w1s[2, 2], jnp.zeros_like(w1s[2, 2])], axis=1)
    w1all[r // 2, par, c] = w1own[...]

    for copy in loads[0]:
        copy.wait()
    pack_rows(turn_to(0)[0], *groups[0][0])
    pl.semaphore_wait(barrier, sources - 1)

    def send_weights():
        for kr in range(0, n_rows, 2):
            for kc in range(n_cols):
                if kr or kc:
                    pltpu.make_async_remote_copy(
                        src_ref=w1own,
                        dst_ref=w1all.at[r // 2, par, c],
                        send_sem=wsend_sem,
                        recv_sem=wrecv_sem,
                        device_id=device(to_rs[kr], to_cs[kc]),
                        device_id_type=MESH,
                    ).start()

    def pack_and_send(t, carry):
        pl.when(t < chips - 1)(lambda: pack_rows(turn_to(t + 1)[0], *groups[0][0]))
        there = turn_to(t)[0] == ahead_r // 2

        @pl.when(there)
        def _():
            loads[1][ahead_r % 2].wait()
            pack_rows(ahead_r // 2, *groups[1][ahead_r % 2])

        send_chip(0, t)
        send_tile(1, jnp.int32(ahead_r), jnp.int32(ahead_c), there & jnp.logical_not(is_ahead))
        pl.when(t == 0)(send_weights)
        return carry

    lax.fori_loop(0, chips, pack_and_send, 0)

    for g in range(1, EARLY_FROM + 1):
        pack(g)
    for chunk in range(1, len(chunks)):
        if chunk >= EARLY_FROM and chunk + 1 < len(groups):
            pack(chunk + 1)
        send_chunk(chunk)

    def wait_bytes(ref, sem):
        pltpu.make_async_copy(ref, ref, sem).wait()

    w1_bytes = recv.at[0 : sources // 2 - 1, 0, 0:5]
    wait_bytes(w1_bytes, wrecv_sem)
    wait_bytes(w1_bytes, wsend_sem)
    partner = device(r + 1 - 2 * par, c)
    w_swap = pltpu.make_async_remote_copy(
        src_ref=w1all.at[:, par],
        dst_ref=w1all.at[:, par],
        send_sem=wswap_send_sem,
        recv_sem=wswap_recv_sem,
        device_id=partner,
        device_id_type=MESH,
    )
    w_swap.start()

    def own_rows(chunk):
        rows, where, _ = chunks[chunk]
        src, dst = where(r)

        def copy(count, src_j, dst_j):
            for h in range(rows):
                recv[me, dst + h, pl.ds(dst_j, count)] = packed[src + h, pl.ds(src_j, count)]

        pl.when(at_edge)(lambda: copy(win_j - 1, tile_j * c - 1 + own_j, own_j))
        pl.when(jnp.logical_not(at_edge))(lambda: copy(win_j, tile_j * c - 1, 0))

    for chunk in range(3):
        own_rows(chunk)
    pl.when(jnp.logical_not(no_outer))(lambda: own_rows(3))

    zero_row = jnp.zeros((win_j, 2, 2 * images), BF16)
    zero_col = jnp.zeros((tile_h + 2, 2, 2 * images), BF16)

    def clear(s, carry):
        recv[s, last * (1 - par)] = zero_row
        return carry

    def clear_outer(s, carry):
        recv[s, (last - 1) * par] = zero_row
        recv[s, (last - 1) * par + 1] = zero_row
        return carry

    def clear_edge(s, carry):
        recv[s, pl.ds(3 * par, tile_h + 2), (win_j - 1) * (1 - own_j)] = zero_col
        return carry

    lax.fori_loop(0, sources, clear, 0)
    pl.when(no_outer)(lambda: (lax.fori_loop(0, sources, clear_outer, 0), None)[1])
    pl.when(at_edge)(lambda: (lax.fori_loop(0, sources, clear_edge, 0), None)[1])

    low = lax.broadcasted_iota(jnp.int32, (chans, 2 * chans), 1) < chans

    def spread(wt, u, v, dw):
        ur, vr = pltpu.roll(u, chans, 1), pltpu.roll(v, chans, 1)
        zero = jnp.zeros_like(u)
        tiles = (jnp.where(low, ur, zero), u, jnp.where(low, v, ur), jnp.where(low, zero, vr))
        for k, tile in enumerate(tiles):
            tile = tile.astype(BF16)
            for b in range(2):
                wt[dw + b, k * chans : (k + 1) * chans, b * 2 * chans : (b + 1) * 2 * chans] = tile

    def blank(wt):
        zero = jnp.zeros((4 * chans, 2 * chans), BF16)
        wt[3, :, 0 : 2 * chans] = zero
        wt[0, :, 2 * chans : 4 * chans] = zero

    for copy in params[1:]:
        copy.wait()
    blank(wt1)
    blank(wt2)
    for dw in range(3):
        w = [w2s[dh, dw].astype(F32) for dh in range(3)]
        spread(
            wt2,
            jnp.concatenate([w[1], w[0]], axis=1),
            jnp.concatenate([w[2], jnp.zeros_like(w[2])], axis=1),
            dw,
        )
    bias1[...] = jnp.concatenate([b1s[...]] * 4, axis=1)
    bias2[...] = jnp.concatenate([b2s[...]] * 4, axis=1)

    def arrived(chunk):
        def wait(count):
            wait_bytes(recv.at[0 : sources - 1, 0 : chunks[chunk][0], 0:count], recv_sem.at[chunk])

        pl.when(at_edge)(lambda: wait(win_j - 1))
        pl.when(jnp.logical_not(at_edge))(lambda: wait(win_j))

    arrived(0)
    give = tile_h - (tile_h - 3) * par
    land = tile_h + 2 - (tile_h + 1) * (1 - par)
    swap = pltpu.make_async_remote_copy(
        src_ref=recv.at[:, pl.ds(give, 2)],
        dst_ref=recv.at[:, pl.ds(land, 2)],
        send_sem=swap_send_sem,
        recv_sem=swap_recv_sem,
        device_id=partner,
        device_id_type=MESH,
    )
    swap.start()

    w_swap.wait()
    u = [w1all[:, :, :, k].reshape(chans, 2 * chans).astype(F32) for k in range(5)]
    for dw in range(3):
        v = (u[3], pltpu.roll(u[3], chans, 1), u[4])[dw]
        spread(wt1, u[dw], jnp.where(low, v, 0.0), dw)

    x_pairs, z_pairs = xmat.shape[0], ymat.shape[0]
    o_pairs = z_pairs - 1

    def nth(n, count):
        return (count - 1) * (1 - par) + n * (2 * par - 1)

    def turn_one(n, carry):
        i = nth(n, x_pairs)

        def put(j, value):
            xmat[i, j] = value

        turn(recv, i, put)
        return carry

    def first_one(n, carry):
        i = nth(n, z_pairs)
        fill = jnp.where(n == 0, 1 - par, 2)
        out_of = jnp.where(n == z_pairs - 1, jnp.where(r == 0, 0, jnp.where(r == n_rows - 1, 1, 2)), 2)
        blank_a = jnp.where(fill < 2, fill, out_of)
        first((xmat.at[i], xmat.at[i + 1]), lambda dw: wt1[dw], bias1[...], ymat.at[i], blank_a)
        return carry

    def second_one(n, carry):
        i = nth(n, o_pairs)
        second((ymat.at[i], ymat.at[i + 1]), lambda dw: wt2[dw], bias2[...], out.at[pl.ds(2 * i, 2)])
        return carry

    def stage(s, carry):
        @pl.when(s == 0)
        def _():
            swap.wait()

        for k in range(1, 4):
            there = s == k
            if k == 3:
                there = there & jnp.logical_not(no_outer)
            pl.when(there)(lambda k=k: arrived(k))

        for ends, one in ((TURNS, turn_one), (FIRSTS, first_one), (SECONDS, second_one)):
            lax.fori_loop(step(s, (0, *ends[:-1])), step(s, ends), one, 0)
        return carry

    lax.fori_loop(0, 4, stage, 0)

    per_edge = n_rows * 2
    for chunk in range(4):
        rows = chunks[chunk][0]
        n_r = n_rows - 2 if chunk == 3 else n_rows
        counts = (n_r * 2, n_r * (n_cols - 2))

        def drain(edge_n, inner_n, rows=rows, chunk=chunk):
            wait_bytes(recv.at[0:edge_n, 0:rows, 0 : win_j - 1], send_sem.at[chunk])
            wait_bytes(recv.at[0:inner_n, 0:rows, 0:win_j], send_sem.at[chunk])

        def drain_own(chunk=chunk, counts=counts, drain=drain):
            pl.when(at_edge)(lambda: drain(counts[0] - 1, counts[1]))
            pl.when(jnp.logical_not(at_edge))(lambda: drain(counts[0], counts[1] - 1))

        if chunk == 3:
            pl.when(no_outer)(lambda: drain(*counts))
            pl.when(jnp.logical_not(no_outer))(drain_own)
        else:
            drain_own()


def tail_kernel(tile, ymat, wt2, bias2, out_hbm, o_new, sem):
    par = lax.rem(lax.axis_index("model"), 2)
    rows = out_hbm.shape[0]
    o_pairs = ymat.shape[0] - 1
    late = (rows - 2) * par
    here = 2 * (1 - par)

    def start(k, carry):
        pltpu.make_async_copy(tile.at[par + k], out_hbm.at[k], sem.at[0]).start()
        return carry

    lax.fori_loop(here, here + rows - 2, start, 0)
    i = (o_pairs - 1) * par
    second((ymat.at[i], ymat.at[i + 1]), lambda dw: wt2[dw], bias2[...], o_new)
    last = pltpu.make_async_copy(o_new, out_hbm.at[pl.ds(late, 2)], sem.at[1])
    last.start()
    pltpu.make_async_copy(tile.at[0 : rows - 2], out_hbm.at[0 : rows - 2], sem.at[0]).wait()
    last.wait()


def solution(mesh):
    n_rows = mesh.shape["model"]
    n_cols = mesh.shape["cols"]

    def run_local(x_in, w_conv1, b_conv1, w_conv2, b_conv2):
        images, height, width, own_chans = x_in.shape
        sources = n_rows * n_cols
        chans = own_chans * sources
        pairs = width // 2
        tile_h, tile_j = height // n_rows, pairs // n_cols
        win_j = tile_j + 2
        x_pairs, z_pairs = (tile_h + 5) // 2, (tile_h + 3) // 2
        x_t = jnp.transpose(x_in, (1, 2, 3, 0)).reshape(n_rows // 2, 2 * tile_h, pairs, 2, own_chans, images)
        args = (x_t, w_conv1, b_conv1.reshape(1, chans), w_conv2, b_conv2.reshape(1, chans))
        hbm = pl.BlockSpec(memory_space=pltpu.HBM)
        vmem = pl.BlockSpec(memory_space=pltpu.VMEM)
        kept = (
            pltpu.VMEM((2 * (z_pairs - 1), tile_j, 2, images, chans), F32),
            pltpu.VMEM((z_pairs, win_j - 1, 2, images, 2 * chans), BF16),
            pltpu.VMEM((4, 4 * chans, 4 * chans), BF16),
            pltpu.VMEM((1, 4 * chans), F32),
        )
        state = pl.pallas_call(
            functools.partial(conv_kernel, n_rows, n_cols),
            out_shape=kept,
            in_specs=[hbm] * 5,
            out_specs=[vmem] * len(kept),
            scratch_shapes=[
                pltpu.VMEM((sources, 2 * x_pairs, win_j, own_chans, 2 * images), BF16),
                pltpu.VMEM((x_pairs, win_j, 2, images, 2 * chans), BF16),
                pltpu.VMEM((4, 4 * chans, 4 * chans), BF16),
                pltpu.VMEM((1, 4 * chans), F32),
                pltpu.VMEM((n_rows // 2, 2 * tile_h, pairs, 2, own_chans, images), BF16),
                pltpu.VMEM((height, pairs, own_chans, 2 * images), BF16),
                pltpu.VMEM((3, 3, own_chans, chans), BF16),
                pltpu.VMEM((5, own_chans, 2 * chans), BF16),
                pltpu.VMEM((n_rows // 2, 2, n_cols, 5, own_chans, 2 * chans), BF16),
                pltpu.VMEM((3, 3, chans, chans), BF16),
                pltpu.VMEM((1, chans), F32),
                pltpu.VMEM((1, chans), F32),
                pltpu.SemaphoreType.DMA((3, 2)),
                pltpu.SemaphoreType.DMA((4,)),
                pltpu.SemaphoreType.DMA((4,)),
                pltpu.SemaphoreType.DMA((4,)),
            ]
            + [pltpu.SemaphoreType.DMA] * 6,
            compiler_params=pltpu.CompilerParams(
                collective_id=0, has_side_effects=True, vmem_limit_bytes=24 << 20
            ),
            name="conv",
        )(*(pltpu.with_memory_space_constraint(a, pltpu.HBM) for a in args))
        out = pl.pallas_call(
            tail_kernel,
            out_shape=jax.ShapeDtypeStruct((tile_h, tile_j, 2, images, chans), F32),
            in_specs=[vmem] * len(kept),
            out_specs=pl.BlockSpec(memory_space=pl.ANY),
            scratch_shapes=[
                pltpu.VMEM((2, tile_j, 2, images, chans), F32),
                pltpu.SemaphoreType.DMA((2,)),
            ],
            compiler_params=pltpu.CompilerParams(vmem_limit_bytes=8 << 20),
            name="tail",
        )(*state)
        out = out.reshape(tile_h, 2 * tile_j, images, chans)
        return jnp.transpose(out, (2, 0, 1, 3))

    group = ("model", "cols")
    return jax.shard_map(
        run_local,
        mesh=mesh,
        in_specs=(P("data", None, None, group), P(None, None, group, None), P(), P(), P()),
        out_specs=P("data", "model", "cols", None),
        check_vma=False,
    )
```

```python
import functools

import jax
import jax.numpy as jnp
from jax import lax
from jax.experimental import pallas as pl
from jax.experimental.pallas import tpu as pltpu
from jax.sharding import PartitionSpec as P

MESH = pl.DeviceIdType.MESH
BF16 = jnp.bfloat16
F32 = jnp.float32
CHUNK_ROWS = (2, 3, 2)
TURNS, FIRSTS, SECONDS = (2, 4, 5, 6), (1, 3, 4, 5), (0, 2, 3, 3)
EARLY_FROM = 1
AHEAD = (1, 0)
CHIPS_ALONG = (3, 1, 2, 0)
CHIP_ORDER = tuple((other, dy) for other in (0, 1) for dy in (0, 1, -1, 2))


def turn(recv, i, put):
    sources, _, win_j, own_chans, lanes = recv.shape
    chans = sources * own_chans
    for j in range(win_j):
        top = recv[:, 2 * i, j].reshape(chans, lanes)
        under = recv[:, 2 * i + 1, j].reshape(chans, lanes)
        put(j, jnp.concatenate([top, under], axis=0).T.reshape(2, lanes // 2, 2 * chans))


def blocks(pairs, weights, count):
    acc = None
    for dw in range(4):
        parts = [view[dw // 2 : dw // 2 + count, dw % 2] for view in pairs]
        lhs = jnp.concatenate([p.reshape(count * p.shape[1], p.shape[2]) for p in parts], axis=1)
        term = jnp.dot(lhs, weights(dw), preferred_element_type=F32)
        acc = term if acc is None else acc + term
    return acc


def first(pairs, weights, bias, y_row, blank_a):
    count, _, images, lanes = y_row.shape
    c = lax.axis_index("cols")
    row = lax.rem(lax.broadcasted_iota(jnp.int32, (1, 2 * lanes), 1), lanes) // (lanes // 2)
    act = jnp.maximum(blocks(pairs, weights, count) + bias, 0.0)
    act = jnp.where(row != blank_a, act, 0.0).astype(BF16)
    for b in range(2):
        y_row[:, b] = act[:, b * lanes : (b + 1) * lanes].reshape(count, images, lanes)
    blank = jnp.zeros((images, lanes), BF16)

    @pl.when(c == 0)
    def _():
        y_row[0, 0] = blank

    @pl.when(c == lax.axis_size("cols") - 1)
    def _():
        y_row[count - 1, 1] = blank


def second(pairs, weights, bias, out_pair):
    _, count, _, images, chans = out_pair.shape
    res = blocks(pairs, weights, count) + bias
    for b in range(2):
        for a in range(2):
            at = (2 * b + a) * chans
            out_pair[a, :, b] = res[:, at : at + chans].reshape(count, images, chans)


def conv_kernel(
    n_rows,
    n_cols,
    x_hbm,
    w1_hbm,
    b1_hbm,
    w2_hbm,
    b2_hbm,
    out,
    ymat,
    wt2,
    bias2,
    recv,
    xmat,
    wt1,
    bias1,
    xs,
    packed,
    w1s,
    w1own,
    w1all,
    w2s,
    b1s,
    b2s,
    load_sem,
    par_sem,
    send_sem,
    recv_sem,
    wsend_sem,
    wrecv_sem,
    swap_send_sem,
    swap_recv_sem,
    wswap_send_sem,
    wswap_recv_sem,
):
    chip_h, pairs = xs.shape[1:3]
    images = xs.shape[-1]
    tile_h, tile_j = chip_h // 2, pairs // n_cols
    win_j = tile_j + 2
    sources = n_rows * n_cols
    r, c = lax.axis_index("model"), lax.axis_index("cols")
    par = lax.rem(r, 2)
    me = r * n_cols + c
    chans = recv.shape[0] * 2

    tops = [tile_h - sum(CHUNK_ROWS[: k + 1]) for k in range(len(CHUNK_ROWS))]
    groups = (
        ((tops[0], chip_h - tops[0]),),
        *(((k, k + n), (chip_h - k - n, chip_h - k)) for k, n in zip(tops[1:], CHUNK_ROWS[1:])),
    )
    loads = []
    for g, spans in enumerate(groups):
        loads.append(
            [
                pltpu.make_async_copy(x_hbm.at[:, lo:hi], xs.at[:, lo:hi], load_sem.at[g, n])
                for n, (lo, hi) in enumerate(spans)
            ]
        )
    for copies in loads:
        for copy in copies:
            copy.start()
    params = [
        pltpu.make_async_copy(src, dst, par_sem.at[s])
        for s, (src, dst) in enumerate(((w1_hbm, w1s), (w2_hbm, w2s), (b1_hbm, b1s), (b2_hbm, b2s)))
    ]
    for copy in params:
        copy.start()

    barrier = pltpu.get_barrier_semaphore()
    to_cs = [lax.rem(c + k, n_cols) for k in range(n_cols)]

    def device(to_r, to_c):
        return {"model": to_r, "cols": to_c}

    to_rs = [lax.rem(r + k, n_rows) for k in range(n_rows)]
    for kr, kc in sorted(
        ((kr, kc) for kr in range(n_rows) for kc in range(n_cols) if kr or kc),
        key=lambda k: (k[1] not in (1, 2), k[0] not in (2, 3, 4, 5), k[1] == 2, k[0] < 4, -min(k[0], n_rows - k[0])),
    ):
        pl.semaphore_signal(barrier, inc=1, device_id=device(to_rs[kr], to_cs[kc]), device_id_type=MESH)

    ahead_r, ahead_c = AHEAD
    is_ahead = (r == ahead_r) & (c == ahead_c)

    def pack_rows(x, lo, hi):
        rows = hi - lo
        left, right = (xs[x, lo:hi, :, p].reshape(rows * pairs * 2, images) for p in range(2))
        both = jnp.concatenate([left, right], axis=1)
        packed[pl.ds(chip_h * x + lo, rows)] = both.reshape(rows, pairs, 2, 2 * images)

    def pack(g):
        for n, copy in enumerate(loads[g]):
            if (g, n) != (1, ahead_r % 2):
                copy.wait()

        def body(x, carry):
            for n, (lo, hi) in enumerate(groups[g]):
                if (g, n) == (1, ahead_r % 2):
                    pl.when(x != ahead_r // 2)(lambda lo=lo, hi=hi: pack_rows(x, lo, hi))
                else:
                    pack_rows(x, lo, hi)
            return carry

        lax.fori_loop(0, n_rows // 2, body, 0)

    last = tile_h + 4

    def rows_of(offset, count):
        def where(to_r):
            q = lax.rem(to_r, 2)
            src = tile_h * to_r + offset + (tile_h - count - 2 * offset) * q
            dst = offset + 2 + (last - count - 2 * offset - 3) * q
            return src, dst

        return where

    chunks = (
        *((n, rows_of(k, n), False) for k, n in zip(tops, CHUNK_ROWS)),
        (2, rows_of(-2, 2), True),
    )
    no_outer = (r == 0) | (r == n_rows - 1)
    at_edge = (c == 0) | (c == n_cols - 1)
    own_j = c == 0
    own_j = own_j.astype(jnp.int32)

    def send_tile(chunk, to_r, to_c, there):
        rows, where, is_outer = chunks[chunk]
        src, dst = where(to_r)
        skip = (to_c == 0).astype(jnp.int32)
        edge = (to_c == 0) | (to_c == n_cols - 1)
        if is_outer:
            there = there & (to_r > 0) & (to_r < n_rows - 1)

        def copy(count, src_j, dst_j):
            pltpu.make_async_remote_copy(
                src_ref=packed.at[pl.ds(src, rows), pl.ds(src_j, count)],
                dst_ref=recv.at[me, pl.ds(dst, rows), pl.ds(dst_j, count)],
                send_sem=send_sem.at[chunk],
                recv_sem=recv_sem.at[chunk],
                device_id=device(to_r, to_c),
                device_id_type=MESH,
            ).start()

        pl.when(there & edge)(lambda: copy(win_j - 1, tile_j * to_c - 1 + skip, skip))
        pl.when(there & jnp.logical_not(edge))(lambda: copy(win_j, tile_j * to_c - 1, 0))

    chips = n_rows // 2

    def step(t, table):
        value = jnp.int32(table[-1])
        for k, entry in enumerate(table[:-1]):
            value = jnp.where(t == k, entry, value)
        return value

    def turn_to(t):
        dx = step(t, CHIPS_ALONG)
        return lax.rem(r // 2 + dx, chips), dx

    def send_chip(chunk, t, where=None):
        x, dx = turn_to(t)
        way = 1 - 2 * lax.rem(par + t, 2)
        for other, dy in CHIP_ORDER:
            to_r = 2 * x + (1 - par if other else par)
            to_c = lax.rem(c + way * dy + n_cols, n_cols)
            there = True
            if not other and dy == 0:
                there = dx > 0
            if where is not None:
                there = there & where(to_r, to_c)
            send_tile(chunk, to_r, to_c, there)

    def send_chunk(chunk):
        early = EARLY_FROM <= chunk

        def body(t, carry):
            if chunk > EARLY_FROM:
                send_chip(chunk, t, lambda to_r, to_c: to_c > 0)
            else:
                send_chip(chunk, t, lambda to_r, to_c: (to_r != ahead_r) | (to_c != ahead_c))
            if early and chunk + 1 < len(chunks):
                x, dx = turn_to(t)
                for other in range(2):
                    to_r = 2 * x + (1 - par if other else par)
                    there = (to_r != r) | (c != 0)
                    if chunk > EARLY_FROM:
                        there = there & (to_r != ahead_r)
                    send_tile(chunk + 1, to_r, jnp.int32(0), there)
                if chunk == EARLY_FROM:
                    there = (x == ahead_r // 2) & jnp.logical_not(is_ahead)
                    send_tile(len(chunks) - 1, jnp.int32(ahead_r), jnp.int32(ahead_c), there)
            return carry

        lax.fori_loop(0, chips, body, 0)

    params[0].wait()
    for dw in range(3):
        w1own[dw] = jnp.concatenate([w1s[1, dw], w1s[0, dw]], axis=1)
    w1own[3] = jnp.concatenate([w1s[2, 0], w1s[2, 1]], axis=1)
    w1own[4] = jnp.concatenate([w1s[2, 2], jnp.zeros_like(w1s[2, 2])], axis=1)
    w1all[r // 2, par, c] = w1own[...]

    for copy in loads[0]:
        copy.wait()
    pack_rows(turn_to(0)[0], *groups[0][0])
    pl.semaphore_wait(barrier, sources - 1)

    def send_weights():
        for kr in range(0, n_rows, 2):
            for kc in range(n_cols):
                if kr or kc:
                    pltpu.make_async_remote_copy(
                        src_ref=w1own,
                        dst_ref=w1all.at[r // 2, par, c],
                        send_sem=wsend_sem,
                        recv_sem=wrecv_sem,
                        device_id=device(to_rs[kr], to_cs[kc]),
                        device_id_type=MESH,
                    ).start()

    def pack_and_send(t, carry):
        pl.when(t < chips - 1)(lambda: pack_rows(turn_to(t + 1)[0], *groups[0][0]))
        there = turn_to(t)[0] == ahead_r // 2

        @pl.when(there)
        def _():
            loads[1][ahead_r % 2].wait()
            pack_rows(ahead_r // 2, *groups[1][ahead_r % 2])

        send_chip(0, t)
        send_tile(1, jnp.int32(ahead_r), jnp.int32(ahead_c), there & jnp.logical_not(is_ahead))
        pl.when(t == 1)(send_weights)
        return carry

    lax.fori_loop(0, chips, pack_and_send, 0)

    for g in range(1, EARLY_FROM + 1):
        pack(g)
    for chunk in range(1, len(chunks)):
        if chunk >= EARLY_FROM and chunk + 1 < len(groups):
            pack(chunk + 1)
        send_chunk(chunk)

    def wait_bytes(ref, sem):
        pltpu.make_async_copy(ref, ref, sem).wait()

    w1_bytes = recv.at[0 : sources // 2 - 1, 0, 0:5]
    wait_bytes(w1_bytes, wrecv_sem)
    wait_bytes(w1_bytes, wsend_sem)
    partner = device(r + 1 - 2 * par, c)
    w_swap = pltpu.make_async_remote_copy(
        src_ref=w1all.at[:, par],
        dst_ref=w1all.at[:, par],
        send_sem=wswap_send_sem,
        recv_sem=wswap_recv_sem,
        device_id=partner,
        device_id_type=MESH,
    )
    w_swap.start()

    def own_rows(chunk):
        rows, where, _ = chunks[chunk]
        src, dst = where(r)

        def copy(count, src_j, dst_j):
            for h in range(rows):
                recv[me, dst + h, pl.ds(dst_j, count)] = packed[src + h, pl.ds(src_j, count)]

        pl.when(at_edge)(lambda: copy(win_j - 1, tile_j * c - 1 + own_j, own_j))
        pl.when(jnp.logical_not(at_edge))(lambda: copy(win_j, tile_j * c - 1, 0))

    for chunk in range(3):
        own_rows(chunk)
    pl.when(jnp.logical_not(no_outer))(lambda: own_rows(3))

    zero_row = jnp.zeros((win_j, 2, 2 * images), BF16)
    zero_col = jnp.zeros((tile_h + 2, 2, 2 * images), BF16)

    def clear(s, carry):
        recv[s, last * (1 - par)] = zero_row
        return carry

    def clear_outer(s, carry):
        recv[s, (last - 1) * par] = zero_row
        recv[s, (last - 1) * par + 1] = zero_row
        return carry

    def clear_edge(s, carry):
        recv[s, pl.ds(3 * par, tile_h + 2), (win_j - 1) * (1 - own_j)] = zero_col
        return carry

    lax.fori_loop(0, sources, clear, 0)
    pl.when(no_outer)(lambda: (lax.fori_loop(0, sources, clear_outer, 0), None)[1])
    pl.when(at_edge)(lambda: (lax.fori_loop(0, sources, clear_edge, 0), None)[1])

    low = lax.broadcasted_iota(jnp.int32, (chans, 2 * chans), 1) < chans

    def spread(wt, u, v, dw):
        ur, vr = pltpu.roll(u, chans, 1), pltpu.roll(v, chans, 1)
        zero = jnp.zeros_like(u)
        tiles = (jnp.where(low, ur, zero), u, jnp.where(low, v, ur), jnp.where(low, zero, vr))
        for k, tile in enumerate(tiles):
            tile = tile.astype(BF16)
            for b in range(2):
                wt[dw + b, k * chans : (k + 1) * chans, b * 2 * chans : (b + 1) * 2 * chans] = tile

    def blank(wt):
        zero = jnp.zeros((4 * chans, 2 * chans), BF16)
        wt[3, :, 0 : 2 * chans] = zero
        wt[0, :, 2 * chans : 4 * chans] = zero

    for copy in params[1:]:
        copy.wait()
    blank(wt1)
    blank(wt2)
    for dw in range(3):
        w = [w2s[dh, dw].astype(F32) for dh in range(3)]
        spread(
            wt2,
            jnp.concatenate([w[1], w[0]], axis=1),
            jnp.concatenate([w[2], jnp.zeros_like(w[2])], axis=1),
            dw,
        )
    bias1[...] = jnp.concatenate([b1s[...]] * 4, axis=1)
    bias2[...] = jnp.concatenate([b2s[...]] * 4, axis=1)

    def arrived(chunk):
        def wait(count):
            wait_bytes(recv.at[0 : sources - 1, 0 : chunks[chunk][0], 0:count], recv_sem.at[chunk])

        pl.when(at_edge)(lambda: wait(win_j - 1))
        pl.when(jnp.logical_not(at_edge))(lambda: wait(win_j))

    arrived(0)
    give = tile_h - (tile_h - 3) * par
    land = tile_h + 2 - (tile_h + 1) * (1 - par)
    swap = pltpu.make_async_remote_copy(
        src_ref=recv.at[:, pl.ds(give, 2)],
        dst_ref=recv.at[:, pl.ds(land, 2)],
        send_sem=swap_send_sem,
        recv_sem=swap_recv_sem,
        device_id=partner,
        device_id_type=MESH,
    )
    swap.start()

    w_swap.wait()
    u = [w1all[:, :, :, k].reshape(chans, 2 * chans).astype(F32) for k in range(5)]
    for dw in range(3):
        v = (u[3], pltpu.roll(u[3], chans, 1), u[4])[dw]
        spread(wt1, u[dw], jnp.where(low, v, 0.0), dw)

    x_pairs, z_pairs = xmat.shape[0], ymat.shape[0]
    o_pairs = z_pairs - 1

    def nth(n, count):
        return (count - 1) * (1 - par) + n * (2 * par - 1)

    def turn_one(n, carry):
        i = nth(n, x_pairs)

        def put(j, value):
            xmat[i, j] = value

        turn(recv, i, put)
        return carry

    def first_one(n, carry):
        i = nth(n, z_pairs)
        fill = jnp.where(n == 0, 1 - par, 2)
        out_of = jnp.where(n == z_pairs - 1, jnp.where(r == 0, 0, jnp.where(r == n_rows - 1, 1, 2)), 2)
        blank_a = jnp.where(fill < 2, fill, out_of)
        first((xmat.at[i], xmat.at[i + 1]), lambda dw: wt1[dw], bias1[...], ymat.at[i], blank_a)
        return carry

    def second_one(n, carry):
        i = nth(n, o_pairs)
        second((ymat.at[i], ymat.at[i + 1]), lambda dw: wt2[dw], bias2[...], out.at[pl.ds(2 * i, 2)])
        return carry

    def stage(s, carry):
        @pl.when(s == 0)
        def _():
            swap.wait()

        for k in range(1, 4):
            there = s == k
            if k == 3:
                there = there & jnp.logical_not(no_outer)
            pl.when(there)(lambda k=k: arrived(k))

        for ends, one in ((TURNS, turn_one), (FIRSTS, first_one), (SECONDS, second_one)):
            lax.fori_loop(step(s, (0, *ends[:-1])), step(s, ends), one, 0)
        return carry

    lax.fori_loop(0, 4, stage, 0)

    per_edge = n_rows * 2
    for chunk in range(4):
        rows = chunks[chunk][0]
        n_r = n_rows - 2 if chunk == 3 else n_rows
        counts = (n_r * 2, n_r * (n_cols - 2))

        def drain(edge_n, inner_n, rows=rows, chunk=chunk):
            wait_bytes(recv.at[0:edge_n, 0:rows, 0 : win_j - 1], send_sem.at[chunk])
            wait_bytes(recv.at[0:inner_n, 0:rows, 0:win_j], send_sem.at[chunk])

        def drain_own(chunk=chunk, counts=counts, drain=drain):
            pl.when(at_edge)(lambda: drain(counts[0] - 1, counts[1]))
            pl.when(jnp.logical_not(at_edge))(lambda: drain(counts[0], counts[1] - 1))

        if chunk == 3:
            pl.when(no_outer)(lambda: drain(*counts))
            pl.when(jnp.logical_not(no_outer))(drain_own)
        else:
            drain_own()


def tail_kernel(tile, ymat, wt2, bias2, out_hbm, o_new, sem):
    par = lax.rem(lax.axis_index("model"), 2)
    rows = out_hbm.shape[0]
    o_pairs = ymat.shape[0] - 1
    late = (rows - 2) * par
    here = 2 * (1 - par)

    def start(k, carry):
        pltpu.make_async_copy(tile.at[par + k], out_hbm.at[k], sem.at[0]).start()
        return carry

    lax.fori_loop(here, here + rows - 2, start, 0)
    i = (o_pairs - 1) * par
    second((ymat.at[i], ymat.at[i + 1]), lambda dw: wt2[dw], bias2[...], o_new)
    last = pltpu.make_async_copy(o_new, out_hbm.at[pl.ds(late, 2)], sem.at[1])
    last.start()
    pltpu.make_async_copy(tile.at[0 : rows - 2], out_hbm.at[0 : rows - 2], sem.at[0]).wait()
    last.wait()


def solution(mesh):
    n_rows = mesh.shape["model"]
    n_cols = mesh.shape["cols"]

    def run_local(x_in, w_conv1, b_conv1, w_conv2, b_conv2):
        images, height, width, own_chans = x_in.shape
        sources = n_rows * n_cols
        chans = own_chans * sources
        pairs = width // 2
        tile_h, tile_j = height // n_rows, pairs // n_cols
        win_j = tile_j + 2
        x_pairs, z_pairs = (tile_h + 5) // 2, (tile_h + 3) // 2
        x_t = jnp.transpose(x_in, (1, 2, 3, 0)).reshape(n_rows // 2, 2 * tile_h, pairs, 2, own_chans, images)
        args = (x_t, w_conv1, b_conv1.reshape(1, chans), w_conv2, b_conv2.reshape(1, chans))
        hbm = pl.BlockSpec(memory_space=pltpu.HBM)
        vmem = pl.BlockSpec(memory_space=pltpu.VMEM)
        kept = (
            pltpu.VMEM((2 * (z_pairs - 1), tile_j, 2, images, chans), F32),
            pltpu.VMEM((z_pairs, win_j - 1, 2, images, 2 * chans), BF16),
            pltpu.VMEM((4, 4 * chans, 4 * chans), BF16),
            pltpu.VMEM((1, 4 * chans), F32),
        )
        state = pl.pallas_call(
            functools.partial(conv_kernel, n_rows, n_cols),
            out_shape=kept,
            in_specs=[hbm] * 5,
            out_specs=[vmem] * len(kept),
            scratch_shapes=[
                pltpu.VMEM((sources, 2 * x_pairs, win_j, own_chans, 2 * images), BF16),
                pltpu.VMEM((x_pairs, win_j, 2, images, 2 * chans), BF16),
                pltpu.VMEM((4, 4 * chans, 4 * chans), BF16),
                pltpu.VMEM((1, 4 * chans), F32),
                pltpu.VMEM((n_rows // 2, 2 * tile_h, pairs, 2, own_chans, images), BF16),
                pltpu.VMEM((height, pairs, own_chans, 2 * images), BF16),
                pltpu.VMEM((3, 3, own_chans, chans), BF16),
                pltpu.VMEM((5, own_chans, 2 * chans), BF16),
                pltpu.VMEM((n_rows // 2, 2, n_cols, 5, own_chans, 2 * chans), BF16),
                pltpu.VMEM((3, 3, chans, chans), BF16),
                pltpu.VMEM((1, chans), F32),
                pltpu.VMEM((1, chans), F32),
                pltpu.SemaphoreType.DMA((3, 2)),
                pltpu.SemaphoreType.DMA((4,)),
                pltpu.SemaphoreType.DMA((4,)),
                pltpu.SemaphoreType.DMA((4,)),
            ]
            + [pltpu.SemaphoreType.DMA] * 6,
            compiler_params=pltpu.CompilerParams(
                collective_id=0, has_side_effects=True, vmem_limit_bytes=24 << 20
            ),
            name="conv",
        )(*(pltpu.with_memory_space_constraint(a, pltpu.HBM) for a in args))
        out = pl.pallas_call(
            tail_kernel,
            out_shape=jax.ShapeDtypeStruct((tile_h, tile_j, 2, images, chans), F32),
            in_specs=[vmem] * len(kept),
            out_specs=pl.BlockSpec(memory_space=pl.ANY),
            scratch_shapes=[
                pltpu.VMEM((2, tile_j, 2, images, chans), F32),
                pltpu.SemaphoreType.DMA((2,)),
            ],
            compiler_params=pltpu.CompilerParams(vmem_limit_bytes=8 << 20),
            name="tail",
        )(*state)
        out = out.reshape(tile_h, 2 * tile_j, images, chans)
        return jnp.transpose(out, (2, 0, 1, 3))

    group = ("model", "cols")
    return jax.shard_map(
        run_local,
        mesh=mesh,
        in_specs=(P("data", None, None, group), P(None, None, group, None), P(), P(), P()),
        out_specs=P("data", "model", "cols", None),
        check_vma=False,
    )
```

```python
import functools

import jax
import jax.numpy as jnp
from jax import lax
from jax.experimental import pallas as pl
from jax.experimental.pallas import tpu as pltpu
from jax.sharding import PartitionSpec as P

MESH = pl.DeviceIdType.MESH
BF16 = jnp.bfloat16
F32 = jnp.float32
CHUNK_ROWS = (2, 3, 2)
TURNS, FIRSTS, SECONDS = (2, 4, 5, 6), (1, 3, 4, 5), (0, 2, 3, 3)
EARLY_FROM = 1
AHEAD = (1, 0)
CHIPS_ALONG = (3, 1, 2, 0)
CHIP_ORDER = tuple((other, dy) for other in (0, 1) for dy in (0, 1, 2, -1))


def turn(recv, i, put):
    sources, _, win_j, own_chans, lanes = recv.shape
    chans = sources * own_chans
    for j in range(win_j):
        top = recv[:, 2 * i, j].reshape(chans, lanes)
        under = recv[:, 2 * i + 1, j].reshape(chans, lanes)
        put(j, jnp.concatenate([top, under], axis=0).T.reshape(2, lanes // 2, 2 * chans))


def blocks(pairs, weights, count):
    acc = None
    for dw in range(4):
        parts = [view[dw // 2 : dw // 2 + count, dw % 2] for view in pairs]
        lhs = jnp.concatenate([p.reshape(count * p.shape[1], p.shape[2]) for p in parts], axis=1)
        term = jnp.dot(lhs, weights(dw), preferred_element_type=F32)
        acc = term if acc is None else acc + term
    return acc


def first(pairs, weights, bias, y_row, blank_a):
    count, _, images, lanes = y_row.shape
    c = lax.axis_index("cols")
    row = lax.rem(lax.broadcasted_iota(jnp.int32, (1, 2 * lanes), 1), lanes) // (lanes // 2)
    act = jnp.maximum(blocks(pairs, weights, count) + bias, 0.0)
    act = jnp.where(row != blank_a, act, 0.0).astype(BF16)
    for b in range(2):
        y_row[:, b] = act[:, b * lanes : (b + 1) * lanes].reshape(count, images, lanes)
    blank = jnp.zeros((images, lanes), BF16)

    @pl.when(c == 0)
    def _():
        y_row[0, 0] = blank

    @pl.when(c == lax.axis_size("cols") - 1)
    def _():
        y_row[count - 1, 1] = blank


def second(pairs, weights, bias, out_pair):
    _, count, _, images, chans = out_pair.shape
    res = blocks(pairs, weights, count) + bias
    for b in range(2):
        for a in range(2):
            at = (2 * b + a) * chans
            out_pair[a, :, b] = res[:, at : at + chans].reshape(count, images, chans)


def conv_kernel(
    n_rows,
    n_cols,
    x_hbm,
    w1_hbm,
    b1_hbm,
    w2_hbm,
    b2_hbm,
    out,
    ymat,
    wt2,
    bias2,
    recv,
    xmat,
    wt1,
    bias1,
    xs,
    packed,
    w1s,
    w1own,
    w1all,
    w2s,
    b1s,
    b2s,
    load_sem,
    par_sem,
    send_sem,
    recv_sem,
    wsend_sem,
    wrecv_sem,
    swap_send_sem,
    swap_recv_sem,
    wswap_send_sem,
    wswap_recv_sem,
):
    chip_h, pairs = xs.shape[1:3]
    images = xs.shape[-1]
    tile_h, tile_j = chip_h // 2, pairs // n_cols
    win_j = tile_j + 2
    sources = n_rows * n_cols
    r, c = lax.axis_index("model"), lax.axis_index("cols")
    par = lax.rem(r, 2)
    me = r * n_cols + c
    chans = recv.shape[0] * 2

    tops = [tile_h - sum(CHUNK_ROWS[: k + 1]) for k in range(len(CHUNK_ROWS))]
    groups = (
        ((tops[0], chip_h - tops[0]),),
        *(((k, k + n), (chip_h - k - n, chip_h - k)) for k, n in zip(tops[1:], CHUNK_ROWS[1:])),
    )
    loads = []
    for g, spans in enumerate(groups):
        loads.append(
            [
                pltpu.make_async_copy(x_hbm.at[:, lo:hi], xs.at[:, lo:hi], load_sem.at[g, n])
                for n, (lo, hi) in enumerate(spans)
            ]
        )
    for copies in loads:
        for copy in copies:
            copy.start()
    params = [
        pltpu.make_async_copy(src, dst, par_sem.at[s])
        for s, (src, dst) in enumerate(((w1_hbm, w1s), (w2_hbm, w2s), (b1_hbm, b1s), (b2_hbm, b2s)))
    ]
    for copy in params:
        copy.start()

    barrier = pltpu.get_barrier_semaphore()
    to_cs = [lax.rem(c + k, n_cols) for k in range(n_cols)]

    def device(to_r, to_c):
        return {"model": to_r, "cols": to_c}

    to_rs = [lax.rem(r + k, n_rows) for k in range(n_rows)]
    for kr, kc in sorted(
        ((kr, kc) for kr in range(n_rows) for kc in range(n_cols) if kr or kc),
        key=lambda k: (k[1] not in (1, 2), k[0] not in (2, 3, 4, 5), k[1] == 2, k[0] < 4, -min(k[0], n_rows - k[0])),
    ):
        pl.semaphore_signal(barrier, inc=1, device_id=device(to_rs[kr], to_cs[kc]), device_id_type=MESH)

    ahead_r, ahead_c = AHEAD
    is_ahead = (r == ahead_r) & (c == ahead_c)

    def pack_rows(x, lo, hi):
        rows = hi - lo
        left, right = (xs[x, lo:hi, :, p].reshape(rows * pairs * 2, images) for p in range(2))
        both = jnp.concatenate([left, right], axis=1)
        packed[pl.ds(chip_h * x + lo, rows)] = both.reshape(rows, pairs, 2, 2 * images)

    def pack(g):
        for n, copy in enumerate(loads[g]):
            if (g, n) != (1, ahead_r % 2):
                copy.wait()

        def body(x, carry):
            for n, (lo, hi) in enumerate(groups[g]):
                if (g, n) == (1, ahead_r % 2):
                    pl.when(x != ahead_r // 2)(lambda lo=lo, hi=hi: pack_rows(x, lo, hi))
                else:
                    pack_rows(x, lo, hi)
            return carry

        lax.fori_loop(0, n_rows // 2, body, 0)

    last = tile_h + 4

    def rows_of(offset, count):
        def where(to_r):
            q = lax.rem(to_r, 2)
            src = tile_h * to_r + offset + (tile_h - count - 2 * offset) * q
            dst = offset + 2 + (last - count - 2 * offset - 3) * q
            return src, dst

        return where

    chunks = (
        *((n, rows_of(k, n), False) for k, n in zip(tops, CHUNK_ROWS)),
        (2, rows_of(-2, 2), True),
    )
    no_outer = (r == 0) | (r == n_rows - 1)
    at_edge = (c == 0) | (c == n_cols - 1)
    own_j = c == 0
    own_j = own_j.astype(jnp.int32)

    def send_tile(chunk, to_r, to_c, there):
        rows, where, is_outer = chunks[chunk]
        src, dst = where(to_r)
        skip = (to_c == 0).astype(jnp.int32)
        edge = (to_c == 0) | (to_c == n_cols - 1)
        if is_outer:
            there = there & (to_r > 0) & (to_r < n_rows - 1)

        def copy(count, src_j, dst_j):
            pltpu.make_async_remote_copy(
                src_ref=packed.at[pl.ds(src, rows), pl.ds(src_j, count)],
                dst_ref=recv.at[me, pl.ds(dst, rows), pl.ds(dst_j, count)],
                send_sem=send_sem.at[chunk],
                recv_sem=recv_sem.at[chunk],
                device_id=device(to_r, to_c),
                device_id_type=MESH,
            ).start()

        pl.when(there & edge)(lambda: copy(win_j - 1, tile_j * to_c - 1 + skip, skip))
        pl.when(there & jnp.logical_not(edge))(lambda: copy(win_j, tile_j * to_c - 1, 0))

    chips = n_rows // 2

    def step(t, table):
        value = jnp.int32(table[-1])
        for k, entry in enumerate(table[:-1]):
            value = jnp.where(t == k, entry, value)
        return value

    def turn_to(t):
        dx = step(t, CHIPS_ALONG)
        return lax.rem(r // 2 + dx, chips), dx

    def send_chip(chunk, t, where=None):
        x, dx = turn_to(t)
        way = 1 - 2 * lax.rem(par + t, 2)
        for other, dy in CHIP_ORDER:
            to_r = 2 * x + (1 - par if other else par)
            to_c = lax.rem(c + way * dy + n_cols, n_cols)
            there = True
            if not other and dy == 0:
                there = dx > 0
            if where is not None:
                there = there & where(to_r, to_c)
            send_tile(chunk, to_r, to_c, there)

    def send_chunk(chunk):
        early = EARLY_FROM <= chunk

        def body(t, carry):
            if chunk > EARLY_FROM:
                send_chip(chunk, t, lambda to_r, to_c: to_c > 0)
            else:
                send_chip(chunk, t, lambda to_r, to_c: (to_r != ahead_r) | (to_c != ahead_c))
            if early and chunk + 1 < len(chunks):
                x, dx = turn_to(t)
                for other in range(2):
                    to_r = 2 * x + (1 - par if other else par)
                    there = (to_r != r) | (c != 0)
                    if chunk > EARLY_FROM:
                        there = there & (to_r != ahead_r)
                    send_tile(chunk + 1, to_r, jnp.int32(0), there)
                if chunk == EARLY_FROM:
                    there = (x == ahead_r // 2) & jnp.logical_not(is_ahead)
                    send_tile(len(chunks) - 1, jnp.int32(ahead_r), jnp.int32(ahead_c), there)
            return carry

        lax.fori_loop(0, chips, body, 0)

    params[0].wait()
    for dw in range(3):
        w1own[dw] = jnp.concatenate([w1s[1, dw], w1s[0, dw]], axis=1)
    w1own[3] = jnp.concatenate([w1s[2, 0], w1s[2, 1]], axis=1)
    w1own[4] = jnp.concatenate([w1s[2, 2], jnp.zeros_like(w1s[2, 2])], axis=1)
    w1all[r // 2, par, c] = w1own[...]

    for copy in loads[0]:
        copy.wait()
    pack_rows(turn_to(0)[0], *groups[0][0])
    pl.semaphore_wait(barrier, sources - 1)

    def send_weights():
        for kr in range(0, n_rows, 2):
            for kc in range(n_cols):
                if kr or kc:
                    pltpu.make_async_remote_copy(
                        src_ref=w1own,
                        dst_ref=w1all.at[r // 2, par, c],
                        send_sem=wsend_sem,
                        recv_sem=wrecv_sem,
                        device_id=device(to_rs[kr], to_cs[kc]),
                        device_id_type=MESH,
                    ).start()

    def pack_and_send(t, carry):
        pl.when(t < chips - 1)(lambda: pack_rows(turn_to(t + 1)[0], *groups[0][0]))
        there = turn_to(t)[0] == ahead_r // 2

        @pl.when(there)
        def _():
            loads[1][ahead_r % 2].wait()
            pack_rows(ahead_r // 2, *groups[1][ahead_r % 2])

        send_chip(0, t)
        send_tile(1, jnp.int32(ahead_r), jnp.int32(ahead_c), there & jnp.logical_not(is_ahead))
        pl.when(t == 0)(send_weights)
        return carry

    lax.fori_loop(0, chips, pack_and_send, 0)

    for g in range(1, EARLY_FROM + 1):
        pack(g)
    for chunk in range(1, len(chunks)):
        if chunk >= EARLY_FROM and chunk + 1 < len(groups):
            pack(chunk + 1)
        send_chunk(chunk)

    def wait_bytes(ref, sem):
        pltpu.make_async_copy(ref, ref, sem).wait()

    w1_bytes = recv.at[0 : sources // 2 - 1, 0, 0:5]
    wait_bytes(w1_bytes, wrecv_sem)
    wait_bytes(w1_bytes, wsend_sem)
    partner = device(r + 1 - 2 * par, c)
    w_swap = pltpu.make_async_remote_copy(
        src_ref=w1all.at[:, par],
        dst_ref=w1all.at[:, par],
        send_sem=wswap_send_sem,
        recv_sem=wswap_recv_sem,
        device_id=partner,
        device_id_type=MESH,
    )
    w_swap.start()

    def own_rows(chunk):
        rows, where, _ = chunks[chunk]
        src, dst = where(r)

        def copy(count, src_j, dst_j):
            for h in range(rows):
                recv[me, dst + h, pl.ds(dst_j, count)] = packed[src + h, pl.ds(src_j, count)]

        pl.when(at_edge)(lambda: copy(win_j - 1, tile_j * c - 1 + own_j, own_j))
        pl.when(jnp.logical_not(at_edge))(lambda: copy(win_j, tile_j * c - 1, 0))

    for chunk in range(3):
        own_rows(chunk)
    pl.when(jnp.logical_not(no_outer))(lambda: own_rows(3))

    zero_row = jnp.zeros((win_j, 2, 2 * images), BF16)
    zero_col = jnp.zeros((tile_h + 2, 2, 2 * images), BF16)

    def clear(s, carry):
        recv[s, last * (1 - par)] = zero_row
        return carry

    def clear_outer(s, carry):
        recv[s, (last - 1) * par] = zero_row
        recv[s, (last - 1) * par + 1] = zero_row
        return carry

    def clear_edge(s, carry):
        recv[s, pl.ds(3 * par, tile_h + 2), (win_j - 1) * (1 - own_j)] = zero_col
        return carry

    lax.fori_loop(0, sources, clear, 0)
    pl.when(no_outer)(lambda: (lax.fori_loop(0, sources, clear_outer, 0), None)[1])
    pl.when(at_edge)(lambda: (lax.fori_loop(0, sources, clear_edge, 0), None)[1])

    low = lax.broadcasted_iota(jnp.int32, (chans, 2 * chans), 1) < chans

    def spread(wt, u, v, dw):
        ur, vr = pltpu.roll(u, chans, 1), pltpu.roll(v, chans, 1)
        zero = jnp.zeros_like(u)
        tiles = (jnp.where(low, ur, zero), u, jnp.where(low, v, ur), jnp.where(low, zero, vr))
        for k, tile in enumerate(tiles):
            tile = tile.astype(BF16)
            for b in range(2):
                wt[dw + b, k * chans : (k + 1) * chans, b * 2 * chans : (b + 1) * 2 * chans] = tile

    def blank(wt):
        zero = jnp.zeros((4 * chans, 2 * chans), BF16)
        wt[3, :, 0 : 2 * chans] = zero
        wt[0, :, 2 * chans : 4 * chans] = zero

    for copy in params[1:]:
        copy.wait()
    blank(wt1)
    blank(wt2)
    for dw in range(3):
        w = [w2s[dh, dw].astype(F32) for dh in range(3)]
        spread(
            wt2,
            jnp.concatenate([w[1], w[0]], axis=1),
            jnp.concatenate([w[2], jnp.zeros_like(w[2])], axis=1),
            dw,
        )
    bias1[...] = jnp.concatenate([b1s[...]] * 4, axis=1)
    bias2[...] = jnp.concatenate([b2s[...]] * 4, axis=1)

    def arrived(chunk):
        def wait(count):
            wait_bytes(recv.at[0 : sources - 1, 0 : chunks[chunk][0], 0:count], recv_sem.at[chunk])

        pl.when(at_edge)(lambda: wait(win_j - 1))
        pl.when(jnp.logical_not(at_edge))(lambda: wait(win_j))

    arrived(0)
    give = tile_h - (tile_h - 3) * par
    land = tile_h + 2 - (tile_h + 1) * (1 - par)
    swap = pltpu.make_async_remote_copy(
        src_ref=recv.at[:, pl.ds(give, 2)],
        dst_ref=recv.at[:, pl.ds(land, 2)],
        send_sem=swap_send_sem,
        recv_sem=swap_recv_sem,
        device_id=partner,
        device_id_type=MESH,
    )
    swap.start()

    w_swap.wait()
    u = [w1all[:, :, :, k].reshape(chans, 2 * chans).astype(F32) for k in range(5)]
    for dw in range(3):
        v = (u[3], pltpu.roll(u[3], chans, 1), u[4])[dw]
        spread(wt1, u[dw], jnp.where(low, v, 0.0), dw)

    x_pairs, z_pairs = xmat.shape[0], ymat.shape[0]
    o_pairs = z_pairs - 1

    def nth(n, count):
        return (count - 1) * (1 - par) + n * (2 * par - 1)

    def turn_one(n, carry):
        i = nth(n, x_pairs)

        def put(j, value):
            xmat[i, j] = value

        turn(recv, i, put)
        return carry

    def first_one(n, carry):
        i = nth(n, z_pairs)
        fill = jnp.where(n == 0, 1 - par, 2)
        out_of = jnp.where(n == z_pairs - 1, jnp.where(r == 0, 0, jnp.where(r == n_rows - 1, 1, 2)), 2)
        blank_a = jnp.where(fill < 2, fill, out_of)
        first((xmat.at[i], xmat.at[i + 1]), lambda dw: wt1[dw], bias1[...], ymat.at[i], blank_a)
        return carry

    def second_one(n, carry):
        i = nth(n, o_pairs)
        second((ymat.at[i], ymat.at[i + 1]), lambda dw: wt2[dw], bias2[...], out.at[pl.ds(2 * i, 2)])
        return carry

    def stage(s, carry):
        @pl.when(s == 0)
        def _():
            swap.wait()

        for k in range(1, 4):
            there = s == k
            if k == 3:
                there = there & jnp.logical_not(no_outer)
            pl.when(there)(lambda k=k: arrived(k))

        for ends, one in ((TURNS, turn_one), (FIRSTS, first_one), (SECONDS, second_one)):
            lax.fori_loop(step(s, (0, *ends[:-1])), step(s, ends), one, 0)
        return carry

    lax.fori_loop(0, 4, stage, 0)

    per_edge = n_rows * 2
    for chunk in range(4):
        rows = chunks[chunk][0]
        n_r = n_rows - 2 if chunk == 3 else n_rows
        counts = (n_r * 2, n_r * (n_cols - 2))

        def drain(edge_n, inner_n, rows=rows, chunk=chunk):
            wait_bytes(recv.at[0:edge_n, 0:rows, 0 : win_j - 1], send_sem.at[chunk])
            wait_bytes(recv.at[0:inner_n, 0:rows, 0:win_j], send_sem.at[chunk])

        def drain_own(chunk=chunk, counts=counts, drain=drain):
            pl.when(at_edge)(lambda: drain(counts[0] - 1, counts[1]))
            pl.when(jnp.logical_not(at_edge))(lambda: drain(counts[0], counts[1] - 1))

        if chunk == 3:
            pl.when(no_outer)(lambda: drain(*counts))
            pl.when(jnp.logical_not(no_outer))(drain_own)
        else:
            drain_own()


def tail_kernel(tile, ymat, wt2, bias2, out_hbm, o_new, sem):
    par = lax.rem(lax.axis_index("model"), 2)
    rows = out_hbm.shape[0]
    o_pairs = ymat.shape[0] - 1
    late = (rows - 2) * par
    here = 2 * (1 - par)

    def start(k, carry):
        pltpu.make_async_copy(tile.at[par + k], out_hbm.at[k], sem.at[0]).start()
        return carry

    lax.fori_loop(here, here + rows - 2, start, 0)
    i = (o_pairs - 1) * par
    second((ymat.at[i], ymat.at[i + 1]), lambda dw: wt2[dw], bias2[...], o_new)
    last = pltpu.make_async_copy(o_new, out_hbm.at[pl.ds(late, 2)], sem.at[1])
    last.start()
    pltpu.make_async_copy(tile.at[0 : rows - 2], out_hbm.at[0 : rows - 2], sem.at[0]).wait()
    last.wait()


def solution(mesh):
    n_rows = mesh.shape["model"]
    n_cols = mesh.shape["cols"]

    def run_local(x_in, w_conv1, b_conv1, w_conv2, b_conv2):
        images, height, width, own_chans = x_in.shape
        sources = n_rows * n_cols
        chans = own_chans * sources
        pairs = width // 2
        tile_h, tile_j = height // n_rows, pairs // n_cols
        win_j = tile_j + 2
        x_pairs, z_pairs = (tile_h + 5) // 2, (tile_h + 3) // 2
        x_t = jnp.transpose(x_in, (1, 2, 3, 0)).reshape(n_rows // 2, 2 * tile_h, pairs, 2, own_chans, images)
        args = (x_t, w_conv1, b_conv1.reshape(1, chans), w_conv2, b_conv2.reshape(1, chans))
        hbm = pl.BlockSpec(memory_space=pltpu.HBM)
        vmem = pl.BlockSpec(memory_space=pltpu.VMEM)
        kept = (
            pltpu.VMEM((2 * (z_pairs - 1), tile_j, 2, images, chans), F32),
            pltpu.VMEM((z_pairs, win_j - 1, 2, images, 2 * chans), BF16),
            pltpu.VMEM((4, 4 * chans, 4 * chans), BF16),
            pltpu.VMEM((1, 4 * chans), F32),
        )
        state = pl.pallas_call(
            functools.partial(conv_kernel, n_rows, n_cols),
            out_shape=kept,
            in_specs=[hbm] * 5,
            out_specs=[vmem] * len(kept),
            scratch_shapes=[
                pltpu.VMEM((sources, 2 * x_pairs, win_j, own_chans, 2 * images), BF16),
                pltpu.VMEM((x_pairs, win_j, 2, images, 2 * chans), BF16),
                pltpu.VMEM((4, 4 * chans, 4 * chans), BF16),
                pltpu.VMEM((1, 4 * chans), F32),
                pltpu.VMEM((n_rows // 2, 2 * tile_h, pairs, 2, own_chans, images), BF16),
                pltpu.VMEM((height, pairs, own_chans, 2 * images), BF16),
                pltpu.VMEM((3, 3, own_chans, chans), BF16),
                pltpu.VMEM((5, own_chans, 2 * chans), BF16),
                pltpu.VMEM((n_rows // 2, 2, n_cols, 5, own_chans, 2 * chans), BF16),
                pltpu.VMEM((3, 3, chans, chans), BF16),
                pltpu.VMEM((1, chans), F32),
                pltpu.VMEM((1, chans), F32),
                pltpu.SemaphoreType.DMA((3, 2)),
                pltpu.SemaphoreType.DMA((4,)),
                pltpu.SemaphoreType.DMA((4,)),
                pltpu.SemaphoreType.DMA((4,)),
            ]
            + [pltpu.SemaphoreType.DMA] * 6,
            compiler_params=pltpu.CompilerParams(
                collective_id=0, has_side_effects=True, vmem_limit_bytes=24 << 20
            ),
            name="conv",
        )(*(pltpu.with_memory_space_constraint(a, pltpu.HBM) for a in args))
        out = pl.pallas_call(
            tail_kernel,
            out_shape=jax.ShapeDtypeStruct((tile_h, tile_j, 2, images, chans), F32),
            in_specs=[vmem] * len(kept),
            out_specs=pl.BlockSpec(memory_space=pl.ANY),
            scratch_shapes=[
                pltpu.VMEM((2, tile_j, 2, images, chans), F32),
                pltpu.SemaphoreType.DMA((2,)),
            ],
            compiler_params=pltpu.CompilerParams(vmem_limit_bytes=8 << 20),
            name="tail",
        )(*state)
        out = out.reshape(tile_h, 2 * tile_j, images, chans)
        return jnp.transpose(out, (2, 0, 1, 3))

    group = ("model", "cols")
    return jax.shard_map(
        run_local,
        mesh=mesh,
        in_specs=(P("data", None, None, group), P(None, None, group, None), P(), P(), P()),
        out_specs=P("data", "model", "cols", None),
        check_vma=False,
    )
```

```python
import functools

import jax
import jax.numpy as jnp
from jax import lax
from jax.experimental import pallas as pl
from jax.experimental.pallas import tpu as pltpu
from jax.sharding import PartitionSpec as P

MESH = pl.DeviceIdType.MESH
BF16 = jnp.bfloat16
F32 = jnp.float32
CHUNK_ROWS = (2, 3, 2)
TURNS, FIRSTS, SECONDS = (2, 4, 5, 6), (1, 3, 4, 5), (0, 2, 3, 3)
EARLY_FROM = 1
AHEAD = (1, 0)
CHIPS_ALONG = (3, 1, 2, 0)
CHIP_ORDER = tuple((other, dy) for other in (0, 1) for dy in (0, 1, -1, 2))


def turn(recv, i, put):
    sources, _, win_j, own_chans, lanes = recv.shape
    chans = sources * own_chans
    for j in range(win_j):
        top = recv[:, 2 * i, j].reshape(chans, lanes)
        under = recv[:, 2 * i + 1, j].reshape(chans, lanes)
        put(j, jnp.concatenate([top, under], axis=0).T.reshape(2, lanes // 2, 2 * chans))


def blocks(pairs, weights, count):
    acc = None
    for dw in range(4):
        parts = [view[dw // 2 : dw // 2 + count, dw % 2] for view in pairs]
        lhs = jnp.concatenate([p.reshape(count * p.shape[1], p.shape[2]) for p in parts], axis=1)
        term = jnp.dot(lhs, weights(dw), preferred_element_type=F32)
        acc = term if acc is None else acc + term
    return acc


def first(pairs, weights, bias, y_row, blank_a):
    count, _, images, lanes = y_row.shape
    c = lax.axis_index("cols")
    row = lax.rem(lax.broadcasted_iota(jnp.int32, (1, 2 * lanes), 1), lanes) // (lanes // 2)
    act = jnp.maximum(blocks(pairs, weights, count) + bias, 0.0)
    act = jnp.where(row != blank_a, act, 0.0).astype(BF16)
    for b in range(2):
        y_row[:, b] = act[:, b * lanes : (b + 1) * lanes].reshape(count, images, lanes)
    blank = jnp.zeros((images, lanes), BF16)

    @pl.when(c == 0)
    def _():
        y_row[0, 0] = blank

    @pl.when(c == lax.axis_size("cols") - 1)
    def _():
        y_row[count - 1, 1] = blank


def second(pairs, weights, bias, out_pair):
    _, count, _, images, chans = out_pair.shape
    res = blocks(pairs, weights, count) + bias
    for b in range(2):
        for a in range(2):
            at = (2 * b + a) * chans
            out_pair[a, :, b] = res[:, at : at + chans].reshape(count, images, chans)


def conv_kernel(
    n_rows,
    n_cols,
    x_hbm,
    w1_hbm,
    b1_hbm,
    w2_hbm,
    b2_hbm,
    out,
    ymat,
    wt2,
    bias2,
    recv,
    xmat,
    wt1,
    bias1,
    xs,
    packed,
    w1s,
    w1own,
    w1all,
    w2s,
    b1s,
    b2s,
    load_sem,
    par_sem,
    send_sem,
    recv_sem,
    wsend_sem,
    wrecv_sem,
    swap_send_sem,
    swap_recv_sem,
    wswap_send_sem,
    wswap_recv_sem,
):
    chip_h, pairs = xs.shape[1:3]
    images = xs.shape[-1]
    tile_h, tile_j = chip_h // 2, pairs // n_cols
    win_j = tile_j + 2
    sources = n_rows * n_cols
    r, c = lax.axis_index("model"), lax.axis_index("cols")
    par = lax.rem(r, 2)
    me = r * n_cols + c
    chans = recv.shape[0] * 2

    tops = [tile_h - sum(CHUNK_ROWS[: k + 1]) for k in range(len(CHUNK_ROWS))]
    groups = (
        ((tops[0], chip_h - tops[0]),),
        *(((k, k + n), (chip_h - k - n, chip_h - k)) for k, n in zip(tops[1:], CHUNK_ROWS[1:])),
    )
    loads = []
    for g, spans in enumerate(groups):
        loads.append(
            [
                pltpu.make_async_copy(x_hbm.at[:, lo:hi], xs.at[:, lo:hi], load_sem.at[g, n])
                for n, (lo, hi) in enumerate(spans)
            ]
        )
    for copies in loads:
        for copy in copies:
            copy.start()
    params = [
        pltpu.make_async_copy(src, dst, par_sem.at[s])
        for s, (src, dst) in enumerate(((w1_hbm, w1s), (w2_hbm, w2s), (b1_hbm, b1s), (b2_hbm, b2s)))
    ]
    for copy in params:
        copy.start()

    barrier = pltpu.get_barrier_semaphore()
    to_cs = [lax.rem(c + k, n_cols) for k in range(n_cols)]

    def device(to_r, to_c):
        return {"model": to_r, "cols": to_c}

    to_rs = [lax.rem(r + k, n_rows) for k in range(n_rows)]
    for kr, kc in sorted(
        ((kr, kc) for kr in range(n_rows) for kc in range(n_cols) if kr or kc),
        key=lambda k: (k[1] not in (1, 2), k[0] not in (2, 3, 4, 5), k[1] == 2, k[0] < 4, -min(k[0], n_rows - k[0])),
    ):
        pl.semaphore_signal(barrier, inc=1, device_id=device(to_rs[kr], to_cs[kc]), device_id_type=MESH)

    ahead_r, ahead_c = AHEAD
    is_ahead = (r == ahead_r) & (c == ahead_c)

    def pack_rows(x, lo, hi):
        rows = hi - lo
        left, right = (xs[x, lo:hi, :, p].reshape(rows * pairs * 2, images) for p in range(2))
        both = jnp.concatenate([left, right], axis=1)
        packed[pl.ds(chip_h * x + lo, rows)] = both.reshape(rows, pairs, 2, 2 * images)

    def pack(g):
        for n, copy in enumerate(loads[g]):
            if (g, n) != (1, ahead_r % 2):
                copy.wait()

        def body(x, carry):
            for n, (lo, hi) in enumerate(groups[g]):
                if (g, n) == (1, ahead_r % 2):
                    pl.when(x != ahead_r // 2)(lambda lo=lo, hi=hi: pack_rows(x, lo, hi))
                else:
                    pack_rows(x, lo, hi)
            return carry

        lax.fori_loop(0, n_rows // 2, body, 0)

    last = tile_h + 4

    def rows_of(offset, count):
        def where(to_r):
            q = lax.rem(to_r, 2)
            src = tile_h * to_r + offset + (tile_h - count - 2 * offset) * q
            dst = offset + 2 + (last - count - 2 * offset - 3) * q
            return src, dst

        return where

    chunks = (
        *((n, rows_of(k, n), False) for k, n in zip(tops, CHUNK_ROWS)),
        (2, rows_of(-2, 2), True),
    )
    no_outer = (r == 0) | (r == n_rows - 1)
    at_edge = (c == 0) | (c == n_cols - 1)
    own_j = c == 0
    own_j = own_j.astype(jnp.int32)

    def send_tile(chunk, to_r, to_c, there):
        rows, where, is_outer = chunks[chunk]
        src, dst = where(to_r)
        skip = (to_c == 0).astype(jnp.int32)
        edge = (to_c == 0) | (to_c == n_cols - 1)
        if is_outer:
            there = there & (to_r > 0) & (to_r < n_rows - 1)

        def copy(count, src_j, dst_j):
            pltpu.make_async_remote_copy(
                src_ref=packed.at[pl.ds(src, rows), pl.ds(src_j, count)],
                dst_ref=recv.at[me, pl.ds(dst, rows), pl.ds(dst_j, count)],
                send_sem=send_sem.at[chunk],
                recv_sem=recv_sem.at[chunk],
                device_id=device(to_r, to_c),
                device_id_type=MESH,
            ).start()

        pl.when(there & edge)(lambda: copy(win_j - 1, tile_j * to_c - 1 + skip, skip))
        pl.when(there & jnp.logical_not(edge))(lambda: copy(win_j, tile_j * to_c - 1, 0))

    chips = n_rows // 2

    def step(t, table):
        value = jnp.int32(table[-1])
        for k, entry in enumerate(table[:-1]):
            value = jnp.where(t == k, entry, value)
        return value

    def turn_to(t):
        dx = step(t, CHIPS_ALONG)
        return lax.rem(r // 2 + dx, chips), dx

    def send_chip(chunk, t, where=None):
        x, dx = turn_to(t)
        way = 1 - 2 * lax.rem(par + t, 2)
        for other, dy in CHIP_ORDER:
            to_r = 2 * x + (1 - par if other else par)
            to_c = lax.rem(c + way * dy + n_cols, n_cols)
            there = True
            if not other and dy == 0:
                there = dx > 0
            if where is not None:
                there = there & where(to_r, to_c)
            send_tile(chunk, to_r, to_c, there)

    def send_chunk(chunk):
        early = EARLY_FROM <= chunk

        def body(t, carry):
            if chunk > EARLY_FROM:
                send_chip(chunk, t, lambda to_r, to_c: to_c > 0)
            else:
                send_chip(chunk, t, lambda to_r, to_c: (to_r != ahead_r) | (to_c != ahead_c))
            if early and chunk + 1 < len(chunks):
                x, dx = turn_to(t)
                for other in range(2):
                    to_r = 2 * x + (1 - par if other else par)
                    there = (to_r != r) | (c != 0)
                    if chunk > EARLY_FROM:
                        there = there & (to_r != ahead_r)
                    send_tile(chunk + 1, to_r, jnp.int32(0), there)
                if chunk == EARLY_FROM:
                    there = (x == ahead_r // 2) & jnp.logical_not(is_ahead)
                    send_tile(len(chunks) - 1, jnp.int32(ahead_r), jnp.int32(ahead_c), there)
            return carry

        lax.fori_loop(0, chips, body, 0)

    params[0].wait()
    for dw in range(3):
        w1own[dw] = jnp.concatenate([w1s[1, dw], w1s[0, dw]], axis=1)
    w1own[3] = jnp.concatenate([w1s[2, 0], w1s[2, 1]], axis=1)
    w1own[4] = jnp.concatenate([w1s[2, 2], jnp.zeros_like(w1s[2, 2])], axis=1)
    w1all[r // 2, par, c] = w1own[...]

    for copy in loads[0]:
        copy.wait()
    pack_rows(turn_to(0)[0], *groups[0][0])
    pl.semaphore_wait(barrier, sources - 1)

    def send_weights():
        for kr in range(0, n_rows, 2):
            for kc in range(n_cols):
                if kr or kc:
                    pltpu.make_async_remote_copy(
                        src_ref=w1own,
                        dst_ref=w1all.at[r // 2, par, c],
                        send_sem=wsend_sem,
                        recv_sem=wrecv_sem,
                        device_id=device(to_rs[kr], to_cs[kc]),
                        device_id_type=MESH,
                    ).start()

    def pack_and_send(t, carry):
        pl.when(t < chips - 1)(lambda: pack_rows(turn_to(t + 1)[0], *groups[0][0]))
        there = turn_to(t)[0] == ahead_r // 2

        @pl.when(there)
        def _():
            loads[1][ahead_r % 2].wait()
            pack_rows(ahead_r // 2, *groups[1][ahead_r % 2])

        send_chip(0, t)
        send_tile(1, jnp.int32(ahead_r), jnp.int32(ahead_c), there & jnp.logical_not(is_ahead))
        pl.when(t == 1)(send_weights)
        return carry

    lax.fori_loop(0, chips, pack_and_send, 0)

    for g in range(1, EARLY_FROM + 1):
        pack(g)
    for chunk in range(1, len(chunks)):
        if chunk >= EARLY_FROM and chunk + 1 < len(groups):
            pack(chunk + 1)
        send_chunk(chunk)

    def wait_bytes(ref, sem):
        pltpu.make_async_copy(ref, ref, sem).wait()

    w1_bytes = recv.at[0 : sources // 2 - 1, 0, 0:5]
    wait_bytes(w1_bytes, wrecv_sem)
    wait_bytes(w1_bytes, wsend_sem)
    partner = device(r + 1 - 2 * par, c)
    w_swap = pltpu.make_async_remote_copy(
        src_ref=w1all.at[:, par],
        dst_ref=w1all.at[:, par],
        send_sem=wswap_send_sem,
        recv_sem=wswap_recv_sem,
        device_id=partner,
        device_id_type=MESH,
    )
    w_swap.start()

    def own_rows(chunk):
        rows, where, _ = chunks[chunk]
        src, dst = where(r)

        def copy(count, src_j, dst_j):
            for h in range(rows):
                recv[me, dst + h, pl.ds(dst_j, count)] = packed[src + h, pl.ds(src_j, count)]

        pl.when(at_edge)(lambda: copy(win_j - 1, tile_j * c - 1 + own_j, own_j))
        pl.when(jnp.logical_not(at_edge))(lambda: copy(win_j, tile_j * c - 1, 0))

    for chunk in range(3):
        own_rows(chunk)
    pl.when(jnp.logical_not(no_outer))(lambda: own_rows(3))

    zero_row = jnp.zeros((win_j, 2, 2 * images), BF16)
    zero_col = jnp.zeros((tile_h + 2, 2, 2 * images), BF16)

    def clear(s, carry):
        recv[s, last * (1 - par)] = zero_row
        return carry

    def clear_outer(s, carry):
        recv[s, (last - 1) * par] = zero_row
        recv[s, (last - 1) * par + 1] = zero_row
        return carry

    def clear_edge(s, carry):
        recv[s, pl.ds(3 * par, tile_h + 2), (win_j - 1) * (1 - own_j)] = zero_col
        return carry

    lax.fori_loop(0, sources, clear, 0)
    pl.when(no_outer)(lambda: (lax.fori_loop(0, sources, clear_outer, 0), None)[1])
    pl.when(at_edge)(lambda: (lax.fori_loop(0, sources, clear_edge, 0), None)[1])

    low = lax.broadcasted_iota(jnp.int32, (chans, 2 * chans), 1) < chans

    def spread(wt, u, v, dw):
        ur, vr = pltpu.roll(u, chans, 1), pltpu.roll(v, chans, 1)
        zero = jnp.zeros_like(u)
        tiles = (jnp.where(low, ur, zero), u, jnp.where(low, v, ur), jnp.where(low, zero, vr))
        for k, tile in enumerate(tiles):
            tile = tile.astype(BF16)
            for b in range(2):
                wt[dw + b, k * chans : (k + 1) * chans, b * 2 * chans : (b + 1) * 2 * chans] = tile

    def blank(wt):
        zero = jnp.zeros((4 * chans, 2 * chans), BF16)
        wt[3, :, 0 : 2 * chans] = zero
        wt[0, :, 2 * chans : 4 * chans] = zero

    for copy in params[1:]:
        copy.wait()
    blank(wt1)
    blank(wt2)
    for dw in range(3):
        w = [w2s[dh, dw].astype(F32) for dh in range(3)]
        spread(
            wt2,
            jnp.concatenate([w[1], w[0]], axis=1),
            jnp.concatenate([w[2], jnp.zeros_like(w[2])], axis=1),
            dw,
        )
    bias1[...] = jnp.concatenate([b1s[...]] * 4, axis=1)
    bias2[...] = jnp.concatenate([b2s[...]] * 4, axis=1)

    def arrived(chunk):
        def wait(count):
            wait_bytes(recv.at[0 : sources - 1, 0 : chunks[chunk][0], 0:count], recv_sem.at[chunk])

        pl.when(at_edge)(lambda: wait(win_j - 1))
        pl.when(jnp.logical_not(at_edge))(lambda: wait(win_j))

    arrived(0)
    give = tile_h - (tile_h - 3) * par
    land = tile_h + 2 - (tile_h + 1) * (1 - par)
    swap = pltpu.make_async_remote_copy(
        src_ref=recv.at[:, pl.ds(give, 2)],
        dst_ref=recv.at[:, pl.ds(land, 2)],
        send_sem=swap_send_sem,
        recv_sem=swap_recv_sem,
        device_id=partner,
        device_id_type=MESH,
    )
    swap.start()

    w_swap.wait()
    u = [w1all[:, :, :, k].reshape(chans, 2 * chans).astype(F32) for k in range(5)]
    for dw in range(3):
        v = (u[3], pltpu.roll(u[3], chans, 1), u[4])[dw]
        spread(wt1, u[dw], jnp.where(low, v, 0.0), dw)

    x_pairs, z_pairs = xmat.shape[0], ymat.shape[0]
    o_pairs = z_pairs - 1

    def nth(n, count):
        return (count - 1) * (1 - par) + n * (2 * par - 1)

    def turn_one(n, carry):
        i = nth(n, x_pairs)

        def put(j, value):
            xmat[i, j] = value

        turn(recv, i, put)
        return carry

    def first_one(n, carry):
        i = nth(n, z_pairs)
        fill = jnp.where(n == 0, 1 - par, 2)
        out_of = jnp.where(n == z_pairs - 1, jnp.where(r == 0, 0, jnp.where(r == n_rows - 1, 1, 2)), 2)
        blank_a = jnp.where(fill < 2, fill, out_of)
        first((xmat.at[i], xmat.at[i + 1]), lambda dw: wt1[dw], bias1[...], ymat.at[i], blank_a)
        return carry

    def second_one(n, carry):
        i = nth(n, o_pairs)
        second((ymat.at[i], ymat.at[i + 1]), lambda dw: wt2[dw], bias2[...], out.at[pl.ds(2 * i, 2)])
        return carry

    def stage(s, carry):
        @pl.when(s == 0)
        def _():
            swap.wait()

        for k in range(1, 4):
            there = s == k
            if k == 3:
                there = there & jnp.logical_not(no_outer)
            pl.when(there)(lambda k=k: arrived(k))

        for ends, one in ((TURNS, turn_one), (FIRSTS, first_one), (SECONDS, second_one)):
            lax.fori_loop(step(s, (0, *ends[:-1])), step(s, ends), one, 0)
        return carry

    lax.fori_loop(0, 4, stage, 0)

    per_edge = n_rows * 2
    for chunk in range(4):
        rows = chunks[chunk][0]
        n_r = n_rows - 2 if chunk == 3 else n_rows
        counts = (n_r * 2, n_r * (n_cols - 2))

        def drain(edge_n, inner_n, rows=rows, chunk=chunk):
            wait_bytes(recv.at[0:edge_n, 0:rows, 0 : win_j - 1], send_sem.at[chunk])
            wait_bytes(recv.at[0:inner_n, 0:rows, 0:win_j], send_sem.at[chunk])

        def drain_own(chunk=chunk, counts=counts, drain=drain):
            pl.when(at_edge)(lambda: drain(counts[0] - 1, counts[1]))
            pl.when(jnp.logical_not(at_edge))(lambda: drain(counts[0], counts[1] - 1))

        if chunk == 3:
            pl.when(no_outer)(lambda: drain(*counts))
            pl.when(jnp.logical_not(no_outer))(drain_own)
        else:
            drain_own()


def tail_kernel(tile, ymat, wt2, bias2, out_hbm, o_new, sem):
    par = lax.rem(lax.axis_index("model"), 2)
    rows = out_hbm.shape[0]
    o_pairs = ymat.shape[0] - 1
    late = (rows - 2) * par
    here = 2 * (1 - par)

    cut = out_hbm.shape[1] // 2

    def start(k, carry):
        for part in (pl.ds(0, cut), pl.ds(cut, out_hbm.shape[1] - cut)):
            pltpu.make_async_copy(tile.at[par + k, part], out_hbm.at[k, part], sem.at[0]).start()
        return carry

    lax.fori_loop(here, here + rows - 2, start, 0)
    i = (o_pairs - 1) * par
    second((ymat.at[i], ymat.at[i + 1]), lambda dw: wt2[dw], bias2[...], o_new)
    for k in range(2):
        for part in (pl.ds(0, cut), pl.ds(cut, out_hbm.shape[1] - cut)):
            pltpu.make_async_copy(o_new.at[k, part], out_hbm.at[late + k, part], sem.at[1]).start()
    pltpu.make_async_copy(tile.at[0 : rows - 2], out_hbm.at[0 : rows - 2], sem.at[0]).wait()
    pltpu.make_async_copy(o_new, out_hbm.at[pl.ds(late, 2)], sem.at[1]).wait()


def solution(mesh):
    n_rows = mesh.shape["model"]
    n_cols = mesh.shape["cols"]

    def run_local(x_in, w_conv1, b_conv1, w_conv2, b_conv2):
        images, height, width, own_chans = x_in.shape
        sources = n_rows * n_cols
        chans = own_chans * sources
        pairs = width // 2
        tile_h, tile_j = height // n_rows, pairs // n_cols
        win_j = tile_j + 2
        x_pairs, z_pairs = (tile_h + 5) // 2, (tile_h + 3) // 2
        x_t = jnp.transpose(x_in, (1, 2, 3, 0)).reshape(n_rows // 2, 2 * tile_h, pairs, 2, own_chans, images)
        args = (x_t, w_conv1, b_conv1.reshape(1, chans), w_conv2, b_conv2.reshape(1, chans))
        hbm = pl.BlockSpec(memory_space=pltpu.HBM)
        vmem = pl.BlockSpec(memory_space=pltpu.VMEM)
        kept = (
            pltpu.VMEM((2 * (z_pairs - 1), tile_j, 2, images, chans), F32),
            pltpu.VMEM((z_pairs, win_j - 1, 2, images, 2 * chans), BF16),
            pltpu.VMEM((4, 4 * chans, 4 * chans), BF16),
            pltpu.VMEM((1, 4 * chans), F32),
        )
        state = pl.pallas_call(
            functools.partial(conv_kernel, n_rows, n_cols),
            out_shape=kept,
            in_specs=[hbm] * 5,
            out_specs=[vmem] * len(kept),
            scratch_shapes=[
                pltpu.VMEM((sources, 2 * x_pairs, win_j, own_chans, 2 * images), BF16),
                pltpu.VMEM((x_pairs, win_j, 2, images, 2 * chans), BF16),
                pltpu.VMEM((4, 4 * chans, 4 * chans), BF16),
                pltpu.VMEM((1, 4 * chans), F32),
                pltpu.VMEM((n_rows // 2, 2 * tile_h, pairs, 2, own_chans, images), BF16),
                pltpu.VMEM((height, pairs, own_chans, 2 * images), BF16),
                pltpu.VMEM((3, 3, own_chans, chans), BF16),
                pltpu.VMEM((5, own_chans, 2 * chans), BF16),
                pltpu.VMEM((n_rows // 2, 2, n_cols, 5, own_chans, 2 * chans), BF16),
                pltpu.VMEM((3, 3, chans, chans), BF16),
                pltpu.VMEM((1, chans), F32),
                pltpu.VMEM((1, chans), F32),
                pltpu.SemaphoreType.DMA((3, 2)),
                pltpu.SemaphoreType.DMA((4,)),
                pltpu.SemaphoreType.DMA((4,)),
                pltpu.SemaphoreType.DMA((4,)),
            ]
            + [pltpu.SemaphoreType.DMA] * 6,
            compiler_params=pltpu.CompilerParams(
                collective_id=0, has_side_effects=True, vmem_limit_bytes=24 << 20
            ),
            name="conv",
        )(*(pltpu.with_memory_space_constraint(a, pltpu.HBM) for a in args))
        out = pl.pallas_call(
            tail_kernel,
            out_shape=jax.ShapeDtypeStruct((tile_h, tile_j, 2, images, chans), F32),
            in_specs=[vmem] * len(kept),
            out_specs=pl.BlockSpec(memory_space=pl.ANY),
            scratch_shapes=[
                pltpu.VMEM((2, tile_j, 2, images, chans), F32),
                pltpu.SemaphoreType.DMA((2,)),
            ],
            compiler_params=pltpu.CompilerParams(vmem_limit_bytes=8 << 20),
            name="tail",
        )(*state)
        out = out.reshape(tile_h, 2 * tile_j, images, chans)
        return jnp.transpose(out, (2, 0, 1, 3))

    group = ("model", "cols")
    return jax.shard_map(
        run_local,
        mesh=mesh,
        in_specs=(P("data", None, None, group), P(None, None, group, None), P(), P(), P()),
        out_specs=P("data", "model", "cols", None),
        check_vma=False,
    )
```

```python
import functools

import jax
import jax.numpy as jnp
from jax import lax
from jax.experimental import pallas as pl
from jax.experimental.pallas import tpu as pltpu
from jax.sharding import PartitionSpec as P

MESH = pl.DeviceIdType.MESH
BF16 = jnp.bfloat16
F32 = jnp.float32
CHUNK_ROWS = (2, 3, 2)
TURNS, FIRSTS, SECONDS = (2, 4, 5, 6), (1, 3, 4, 5), (0, 2, 3, 3)
EARLY_FROM = 1
AHEAD = (1, 0)
CHIPS_ALONG = (1, 3, 2, 0)
CHIP_ORDER = tuple((other, dy) for other in (0, 1) for dy in (0, 1, -1, 2))


def turn(recv, i, put):
    sources, _, win_j, own_chans, lanes = recv.shape
    chans = sources * own_chans
    for j in range(win_j):
        top = recv[:, 2 * i, j].reshape(chans, lanes)
        under = recv[:, 2 * i + 1, j].reshape(chans, lanes)
        put(j, jnp.concatenate([top, under], axis=0).T.reshape(2, lanes // 2, 2 * chans))


def blocks(pairs, weights, count):
    acc = None
    for dw in range(4):
        parts = [view[dw // 2 : dw // 2 + count, dw % 2] for view in pairs]
        lhs = jnp.concatenate([p.reshape(count * p.shape[1], p.shape[2]) for p in parts], axis=1)
        term = jnp.dot(lhs, weights(dw), preferred_element_type=F32)
        acc = term if acc is None else acc + term
    return acc


def first(pairs, weights, bias, y_row, blank_a):
    count, _, images, lanes = y_row.shape
    c = lax.axis_index("cols")
    row = lax.rem(lax.broadcasted_iota(jnp.int32, (1, 2 * lanes), 1), lanes) // (lanes // 2)
    act = jnp.maximum(blocks(pairs, weights, count) + bias, 0.0)
    act = jnp.where(row != blank_a, act, 0.0).astype(BF16)
    for b in range(2):
        y_row[:, b] = act[:, b * lanes : (b + 1) * lanes].reshape(count, images, lanes)
    blank = jnp.zeros((images, lanes), BF16)

    @pl.when(c == 0)
    def _():
        y_row[0, 0] = blank

    @pl.when(c == lax.axis_size("cols") - 1)
    def _():
        y_row[count - 1, 1] = blank


def second(pairs, weights, bias, out_pair):
    _, count, _, images, chans = out_pair.shape
    res = blocks(pairs, weights, count) + bias
    for b in range(2):
        for a in range(2):
            at = (2 * b + a) * chans
            out_pair[a, :, b] = res[:, at : at + chans].reshape(count, images, chans)


def conv_kernel(
    n_rows,
    n_cols,
    x_hbm,
    w1_hbm,
    b1_hbm,
    w2_hbm,
    b2_hbm,
    out,
    ymat,
    wt2,
    bias2,
    recv,
    xmat,
    wt1,
    bias1,
    xs,
    packed,
    w1s,
    w1own,
    w1all,
    w2s,
    b1s,
    b2s,
    load_sem,
    par_sem,
    send_sem,
    recv_sem,
    wsend_sem,
    wrecv_sem,
    swap_send_sem,
    swap_recv_sem,
    wswap_send_sem,
    wswap_recv_sem,
):
    chip_h, pairs = xs.shape[1:3]
    images = xs.shape[-1]
    tile_h, tile_j = chip_h // 2, pairs // n_cols
    win_j = tile_j + 2
    sources = n_rows * n_cols
    r, c = lax.axis_index("model"), lax.axis_index("cols")
    par = lax.rem(r, 2)
    me = r * n_cols + c
    chans = recv.shape[0] * 2

    tops = [tile_h - sum(CHUNK_ROWS[: k + 1]) for k in range(len(CHUNK_ROWS))]
    groups = (
        ((tops[0], chip_h - tops[0]),),
        *(((k, k + n), (chip_h - k - n, chip_h - k)) for k, n in zip(tops[1:], CHUNK_ROWS[1:])),
    )
    loads = []
    for g, spans in enumerate(groups):
        loads.append(
            [
                pltpu.make_async_copy(x_hbm.at[:, lo:hi], xs.at[:, lo:hi], load_sem.at[g, n])
                for n, (lo, hi) in enumerate(spans)
            ]
        )
    for copies in loads:
        for copy in copies:
            copy.start()
    params = [
        pltpu.make_async_copy(src, dst, par_sem.at[s])
        for s, (src, dst) in enumerate(((w1_hbm, w1s), (w2_hbm, w2s), (b1_hbm, b1s), (b2_hbm, b2s)))
    ]
    for copy in params:
        copy.start()

    barrier = pltpu.get_barrier_semaphore()
    to_cs = [lax.rem(c + k, n_cols) for k in range(n_cols)]

    def device(to_r, to_c):
        return {"model": to_r, "cols": to_c}

    to_rs = [lax.rem(r + k, n_rows) for k in range(n_rows)]
    for kr, kc in sorted(
        ((kr, kc) for kr in range(n_rows) for kc in range(n_cols) if kr or kc),
        key=lambda k: (k[1] not in (1, 2), k[0] not in (2, 3, 4, 5), k[1] == 2, k[0] < 4, -min(k[0], n_rows - k[0])),
    ):
        pl.semaphore_signal(barrier, inc=1, device_id=device(to_rs[kr], to_cs[kc]), device_id_type=MESH)

    ahead_r, ahead_c = AHEAD
    is_ahead = (r == ahead_r) & (c == ahead_c)

    def pack_rows(x, lo, hi):
        rows = hi - lo
        left, right = (xs[x, lo:hi, :, p].reshape(rows * pairs * 2, images) for p in range(2))
        both = jnp.concatenate([left, right], axis=1)
        packed[pl.ds(chip_h * x + lo, rows)] = both.reshape(rows, pairs, 2, 2 * images)

    def pack(g):
        for n, copy in enumerate(loads[g]):
            if (g, n) != (1, ahead_r % 2):
                copy.wait()

        def body(x, carry):
            for n, (lo, hi) in enumerate(groups[g]):
                if (g, n) == (1, ahead_r % 2):
                    pl.when(x != ahead_r // 2)(lambda lo=lo, hi=hi: pack_rows(x, lo, hi))
                else:
                    pack_rows(x, lo, hi)
            return carry

        lax.fori_loop(0, n_rows // 2, body, 0)

    last = tile_h + 4

    def rows_of(offset, count):
        def where(to_r):
            q = lax.rem(to_r, 2)
            src = tile_h * to_r + offset + (tile_h - count - 2 * offset) * q
            dst = offset + 2 + (last - count - 2 * offset - 3) * q
            return src, dst

        return where

    chunks = (
        *((n, rows_of(k, n), False) for k, n in zip(tops, CHUNK_ROWS)),
        (2, rows_of(-2, 2), True),
    )
    no_outer = (r == 0) | (r == n_rows - 1)
    at_edge = (c == 0) | (c == n_cols - 1)
    own_j = c == 0
    own_j = own_j.astype(jnp.int32)

    def send_tile(chunk, to_r, to_c, there):
        rows, where, is_outer = chunks[chunk]
        src, dst = where(to_r)
        skip = (to_c == 0).astype(jnp.int32)
        edge = (to_c == 0) | (to_c == n_cols - 1)
        if is_outer:
            there = there & (to_r > 0) & (to_r < n_rows - 1)

        def copy(count, src_j, dst_j):
            pltpu.make_async_remote_copy(
                src_ref=packed.at[pl.ds(src, rows), pl.ds(src_j, count)],
                dst_ref=recv.at[me, pl.ds(dst, rows), pl.ds(dst_j, count)],
                send_sem=send_sem.at[chunk],
                recv_sem=recv_sem.at[chunk],
                device_id=device(to_r, to_c),
                device_id_type=MESH,
            ).start()

        pl.when(there & edge)(lambda: copy(win_j - 1, tile_j * to_c - 1 + skip, skip))
        pl.when(there & jnp.logical_not(edge))(lambda: copy(win_j, tile_j * to_c - 1, 0))

    chips = n_rows // 2

    def step(t, table):
        value = jnp.int32(table[-1])
        for k, entry in enumerate(table[:-1]):
            value = jnp.where(t == k, entry, value)
        return value

    def turn_to(t):
        dx = step(t, CHIPS_ALONG)
        return lax.rem(r // 2 + dx, chips), dx

    def send_chip(chunk, t, where=None):
        x, dx = turn_to(t)
        way = 1 - 2 * lax.rem(par + t, 2)
        for other, dy in CHIP_ORDER:
            to_r = 2 * x + (1 - par if other else par)
            to_c = lax.rem(c + way * dy + n_cols, n_cols)
            there = True
            if not other and dy == 0:
                there = dx > 0
            if where is not None:
                there = there & where(to_r, to_c)
            send_tile(chunk, to_r, to_c, there)

    def send_chunk(chunk):
        early = EARLY_FROM <= chunk

        def body(t, carry):
            if chunk > EARLY_FROM:
                send_chip(chunk, t, lambda to_r, to_c: to_c > 0)
            else:
                send_chip(chunk, t, lambda to_r, to_c: (to_r != ahead_r) | (to_c != ahead_c))
            if early and chunk + 1 < len(chunks):
                x, dx = turn_to(t)
                for other in range(2):
                    to_r = 2 * x + (1 - par if other else par)
                    there = (to_r != r) | (c != 0)
                    if chunk > EARLY_FROM:
                        there = there & (to_r != ahead_r)
                    send_tile(chunk + 1, to_r, jnp.int32(0), there)
                if chunk == EARLY_FROM:
                    there = (x == ahead_r // 2) & jnp.logical_not(is_ahead)
                    send_tile(len(chunks) - 1, jnp.int32(ahead_r), jnp.int32(ahead_c), there)
            return carry

        lax.fori_loop(0, chips, body, 0)

    params[0].wait()
    for dw in range(3):
        w1own[dw] = jnp.concatenate([w1s[1, dw], w1s[0, dw]], axis=1)
    w1own[3] = jnp.concatenate([w1s[2, 0], w1s[2, 1]], axis=1)
    w1own[4] = jnp.concatenate([w1s[2, 2], jnp.zeros_like(w1s[2, 2])], axis=1)
    w1all[r // 2, par, c] = w1own[...]

    for copy in loads[0]:
        copy.wait()
    pack_rows(turn_to(0)[0], *groups[0][0])
    pl.semaphore_wait(barrier, sources - 1)

    def send_weights():
        for kr in range(0, n_rows, 2):
            for kc in range(n_cols):
                if kr or kc:
                    pltpu.make_async_remote_copy(
                        src_ref=w1own,
                        dst_ref=w1all.at[r // 2, par, c],
                        send_sem=wsend_sem,
                        recv_sem=wrecv_sem,
                        device_id=device(to_rs[kr], to_cs[kc]),
                        device_id_type=MESH,
                    ).start()

    def pack_and_send(t, carry):
        pl.when(t < chips - 1)(lambda: pack_rows(turn_to(t + 1)[0], *groups[0][0]))
        there = turn_to(t)[0] == ahead_r // 2

        @pl.when(there)
        def _():
            loads[1][ahead_r % 2].wait()
            pack_rows(ahead_r // 2, *groups[1][ahead_r % 2])

        send_chip(0, t)
        send_tile(1, jnp.int32(ahead_r), jnp.int32(ahead_c), there & jnp.logical_not(is_ahead))
        pl.when(t == 1)(send_weights)
        return carry

    lax.fori_loop(0, chips, pack_and_send, 0)

    for g in range(1, EARLY_FROM + 1):
        pack(g)
    for chunk in range(1, len(chunks)):
        if chunk >= EARLY_FROM and chunk + 1 < len(groups):
            pack(chunk + 1)
        send_chunk(chunk)

    def wait_bytes(ref, sem):
        pltpu.make_async_copy(ref, ref, sem).wait()

    w1_bytes = recv.at[0 : sources // 2 - 1, 0, 0:5]
    wait_bytes(w1_bytes, wrecv_sem)
    wait_bytes(w1_bytes, wsend_sem)
    partner = device(r + 1 - 2 * par, c)
    w_swap = pltpu.make_async_remote_copy(
        src_ref=w1all.at[:, par],
        dst_ref=w1all.at[:, par],
        send_sem=wswap_send_sem,
        recv_sem=wswap_recv_sem,
        device_id=partner,
        device_id_type=MESH,
    )
    w_swap.start()

    def own_rows(chunk):
        rows, where, _ = chunks[chunk]
        src, dst = where(r)

        def copy(count, src_j, dst_j):
            for h in range(rows):
                recv[me, dst + h, pl.ds(dst_j, count)] = packed[src + h, pl.ds(src_j, count)]

        pl.when(at_edge)(lambda: copy(win_j - 1, tile_j * c - 1 + own_j, own_j))
        pl.when(jnp.logical_not(at_edge))(lambda: copy(win_j, tile_j * c - 1, 0))

    for chunk in range(3):
        own_rows(chunk)
    pl.when(jnp.logical_not(no_outer))(lambda: own_rows(3))

    zero_row = jnp.zeros((win_j, 2, 2 * images), BF16)
    zero_col = jnp.zeros((tile_h + 2, 2, 2 * images), BF16)

    def clear(s, carry):
        recv[s, last * (1 - par)] = zero_row
        return carry

    def clear_outer(s, carry):
        recv[s, (last - 1) * par] = zero_row
        recv[s, (last - 1) * par + 1] = zero_row
        return carry

    def clear_edge(s, carry):
        recv[s, pl.ds(3 * par, tile_h + 2), (win_j - 1) * (1 - own_j)] = zero_col
        return carry

    lax.fori_loop(0, sources, clear, 0)
    pl.when(no_outer)(lambda: (lax.fori_loop(0, sources, clear_outer, 0), None)[1])
    pl.when(at_edge)(lambda: (lax.fori_loop(0, sources, clear_edge, 0), None)[1])

    low = lax.broadcasted_iota(jnp.int32, (chans, 2 * chans), 1) < chans

    def spread(wt, u, v, dw):
        ur, vr = pltpu.roll(u, chans, 1), pltpu.roll(v, chans, 1)
        zero = jnp.zeros_like(u)
        tiles = (jnp.where(low, ur, zero), u, jnp.where(low, v, ur), jnp.where(low, zero, vr))
        for k, tile in enumerate(tiles):
            tile = tile.astype(BF16)
            for b in range(2):
                wt[dw + b, k * chans : (k + 1) * chans, b * 2 * chans : (b + 1) * 2 * chans] = tile

    def blank(wt):
        zero = jnp.zeros((4 * chans, 2 * chans), BF16)
        wt[3, :, 0 : 2 * chans] = zero
        wt[0, :, 2 * chans : 4 * chans] = zero

    for copy in params[1:]:
        copy.wait()
    blank(wt1)
    blank(wt2)
    for dw in range(3):
        w = [w2s[dh, dw].astype(F32) for dh in range(3)]
        spread(
            wt2,
            jnp.concatenate([w[1], w[0]], axis=1),
            jnp.concatenate([w[2], jnp.zeros_like(w[2])], axis=1),
            dw,
        )
    bias1[...] = jnp.concatenate([b1s[...]] * 4, axis=1)
    bias2[...] = jnp.concatenate([b2s[...]] * 4, axis=1)

    def arrived(chunk):
        def wait(count):
            wait_bytes(recv.at[0 : sources - 1, 0 : chunks[chunk][0], 0:count], recv_sem.at[chunk])

        pl.when(at_edge)(lambda: wait(win_j - 1))
        pl.when(jnp.logical_not(at_edge))(lambda: wait(win_j))

    arrived(0)
    give = tile_h - (tile_h - 3) * par
    land = tile_h + 2 - (tile_h + 1) * (1 - par)
    swap = pltpu.make_async_remote_copy(
        src_ref=recv.at[:, pl.ds(give, 2)],
        dst_ref=recv.at[:, pl.ds(land, 2)],
        send_sem=swap_send_sem,
        recv_sem=swap_recv_sem,
        device_id=partner,
        device_id_type=MESH,
    )
    swap.start()

    w_swap.wait()
    u = [w1all[:, :, :, k].reshape(chans, 2 * chans).astype(F32) for k in range(5)]
    for dw in range(3):
        v = (u[3], pltpu.roll(u[3], chans, 1), u[4])[dw]
        spread(wt1, u[dw], jnp.where(low, v, 0.0), dw)

    x_pairs, z_pairs = xmat.shape[0], ymat.shape[0]
    o_pairs = z_pairs - 1

    def nth(n, count):
        return (count - 1) * (1 - par) + n * (2 * par - 1)

    def turn_one(n, carry):
        i = nth(n, x_pairs)

        def put(j, value):
            xmat[i, j] = value

        turn(recv, i, put)
        return carry

    def first_one(n, carry):
        i = nth(n, z_pairs)
        fill = jnp.where(n == 0, 1 - par, 2)
        out_of = jnp.where(n == z_pairs - 1, jnp.where(r == 0, 0, jnp.where(r == n_rows - 1, 1, 2)), 2)
        blank_a = jnp.where(fill < 2, fill, out_of)
        first((xmat.at[i], xmat.at[i + 1]), lambda dw: wt1[dw], bias1[...], ymat.at[i], blank_a)
        return carry

    def second_one(n, carry):
        i = nth(n, o_pairs)
        second((ymat.at[i], ymat.at[i + 1]), lambda dw: wt2[dw], bias2[...], out.at[pl.ds(2 * i, 2)])
        return carry

    def stage(s, carry):
        @pl.when(s == 0)
        def _():
            swap.wait()

        for k in range(1, 4):
            there = s == k
            if k == 3:
                there = there & jnp.logical_not(no_outer)
            pl.when(there)(lambda k=k: arrived(k))

        for ends, one in ((TURNS, turn_one), (FIRSTS, first_one), (SECONDS, second_one)):
            lax.fori_loop(step(s, (0, *ends[:-1])), step(s, ends), one, 0)
        return carry

    lax.fori_loop(0, 4, stage, 0)

    per_edge = n_rows * 2
    for chunk in range(4):
        rows = chunks[chunk][0]
        n_r = n_rows - 2 if chunk == 3 else n_rows
        counts = (n_r * 2, n_r * (n_cols - 2))

        def drain(edge_n, inner_n, rows=rows, chunk=chunk):
            wait_bytes(recv.at[0:edge_n, 0:rows, 0 : win_j - 1], send_sem.at[chunk])
            wait_bytes(recv.at[0:inner_n, 0:rows, 0:win_j], send_sem.at[chunk])

        def drain_own(chunk=chunk, counts=counts, drain=drain):
            pl.when(at_edge)(lambda: drain(counts[0] - 1, counts[1]))
            pl.when(jnp.logical_not(at_edge))(lambda: drain(counts[0], counts[1] - 1))

        if chunk == 3:
            pl.when(no_outer)(lambda: drain(*counts))
            pl.when(jnp.logical_not(no_outer))(drain_own)
        else:
            drain_own()


def tail_kernel(tile, ymat, wt2, bias2, out_hbm, o_new, sem):
    par = lax.rem(lax.axis_index("model"), 2)
    rows = out_hbm.shape[0]
    o_pairs = ymat.shape[0] - 1
    late = (rows - 2) * par
    here = 2 * (1 - par)

    def start(k, carry):
        pltpu.make_async_copy(tile.at[par + k], out_hbm.at[k], sem.at[0]).start()
        return carry

    lax.fori_loop(here, here + rows - 2, start, 0)
    i = (o_pairs - 1) * par
    second((ymat.at[i], ymat.at[i + 1]), lambda dw: wt2[dw], bias2[...], o_new)
    last = pltpu.make_async_copy(o_new, out_hbm.at[pl.ds(late, 2)], sem.at[1])
    last.start()
    pltpu.make_async_copy(tile.at[0 : rows - 2], out_hbm.at[0 : rows - 2], sem.at[0]).wait()
    last.wait()


def solution(mesh):
    n_rows = mesh.shape["model"]
    n_cols = mesh.shape["cols"]

    def run_local(x_in, w_conv1, b_conv1, w_conv2, b_conv2):
        images, height, width, own_chans = x_in.shape
        sources = n_rows * n_cols
        chans = own_chans * sources
        pairs = width // 2
        tile_h, tile_j = height // n_rows, pairs // n_cols
        win_j = tile_j + 2
        x_pairs, z_pairs = (tile_h + 5) // 2, (tile_h + 3) // 2
        x_t = jnp.transpose(x_in, (1, 2, 3, 0)).reshape(n_rows // 2, 2 * tile_h, pairs, 2, own_chans, images)
        args = (x_t, w_conv1, b_conv1.reshape(1, chans), w_conv2, b_conv2.reshape(1, chans))
        hbm = pl.BlockSpec(memory_space=pltpu.HBM)
        vmem = pl.BlockSpec(memory_space=pltpu.VMEM)
        kept = (
            pltpu.VMEM((2 * (z_pairs - 1), tile_j, 2, images, chans), F32),
            pltpu.VMEM((z_pairs, win_j - 1, 2, images, 2 * chans), BF16),
            pltpu.VMEM((4, 4 * chans, 4 * chans), BF16),
            pltpu.VMEM((1, 4 * chans), F32),
        )
        state = pl.pallas_call(
            functools.partial(conv_kernel, n_rows, n_cols),
            out_shape=kept,
            in_specs=[hbm] * 5,
            out_specs=[vmem] * len(kept),
            scratch_shapes=[
                pltpu.VMEM((sources, 2 * x_pairs, win_j, own_chans, 2 * images), BF16),
                pltpu.VMEM((x_pairs, win_j, 2, images, 2 * chans), BF16),
                pltpu.VMEM((4, 4 * chans, 4 * chans), BF16),
                pltpu.VMEM((1, 4 * chans), F32),
                pltpu.VMEM((n_rows // 2, 2 * tile_h, pairs, 2, own_chans, images), BF16),
                pltpu.VMEM((height, pairs, own_chans, 2 * images), BF16),
                pltpu.VMEM((3, 3, own_chans, chans), BF16),
                pltpu.VMEM((5, own_chans, 2 * chans), BF16),
                pltpu.VMEM((n_rows // 2, 2, n_cols, 5, own_chans, 2 * chans), BF16),
                pltpu.VMEM((3, 3, chans, chans), BF16),
                pltpu.VMEM((1, chans), F32),
                pltpu.VMEM((1, chans), F32),
                pltpu.SemaphoreType.DMA((3, 2)),
                pltpu.SemaphoreType.DMA((4,)),
                pltpu.SemaphoreType.DMA((4,)),
                pltpu.SemaphoreType.DMA((4,)),
            ]
            + [pltpu.SemaphoreType.DMA] * 6,
            compiler_params=pltpu.CompilerParams(
                collective_id=0, has_side_effects=True, vmem_limit_bytes=24 << 20
            ),
            name="conv",
        )(*(pltpu.with_memory_space_constraint(a, pltpu.HBM) for a in args))
        out = pl.pallas_call(
            tail_kernel,
            out_shape=jax.ShapeDtypeStruct((tile_h, tile_j, 2, images, chans), F32),
            in_specs=[vmem] * len(kept),
            out_specs=pl.BlockSpec(memory_space=pl.ANY),
            scratch_shapes=[
                pltpu.VMEM((2, tile_j, 2, images, chans), F32),
                pltpu.SemaphoreType.DMA((2,)),
            ],
            compiler_params=pltpu.CompilerParams(vmem_limit_bytes=8 << 20),
            name="tail",
        )(*state)
        out = out.reshape(tile_h, 2 * tile_j, images, chans)
        return jnp.transpose(out, (2, 0, 1, 3))

    group = ("model", "cols")
    return jax.shard_map(
        run_local,
        mesh=mesh,
        in_specs=(P("data", None, None, group), P(None, None, group, None), P(), P(), P()),
        out_specs=P("data", "model", "cols", None),
        check_vma=False,
    )
```

```python
import functools

import jax
import jax.numpy as jnp
from jax import lax
from jax.experimental import pallas as pl
from jax.experimental.pallas import tpu as pltpu
from jax.sharding import PartitionSpec as P

MESH = pl.DeviceIdType.MESH
BF16 = jnp.bfloat16
F32 = jnp.float32
CHUNK_ROWS = (2, 3, 2)
TURNS, FIRSTS, SECONDS = (2, 4, 5, 6), (1, 3, 4, 5), (0, 2, 3, 3)
EARLY_FROM = 1
AHEAD = (1, 0)
CHIPS_ALONG = (3, 1, 2, 0)
CHIP_ORDER = tuple((other, dy) for other in (0, 1) for dy in (0, 1, -1, 2))


def turn(recv, i, put):
    sources, _, win_j, own_chans, lanes = recv.shape
    chans = sources * own_chans
    for j in range(win_j):
        top = recv[:, 2 * i, j].reshape(chans, lanes)
        under = recv[:, 2 * i + 1, j].reshape(chans, lanes)
        put(j, jnp.concatenate([top, under], axis=0).T.reshape(2, lanes // 2, 2 * chans))


def blocks(pairs, weights, count):
    acc = None
    for dw in range(4):
        parts = [view[dw // 2 : dw // 2 + count, dw % 2] for view in pairs]
        lhs = jnp.concatenate([p.reshape(count * p.shape[1], p.shape[2]) for p in parts], axis=1)
        term = jnp.dot(lhs, weights(dw), preferred_element_type=F32)
        acc = term if acc is None else acc + term
    return acc


def first(pairs, weights, bias, y_row, blank_a):
    count, _, images, lanes = y_row.shape
    c = lax.axis_index("cols")
    row = lax.rem(lax.broadcasted_iota(jnp.int32, (1, 2 * lanes), 1), lanes) // (lanes // 2)
    act = jnp.maximum(blocks(pairs, weights, count) + bias, 0.0)
    act = jnp.where(row != blank_a, act, 0.0).astype(BF16)
    for b in range(2):
        y_row[:, b] = act[:, b * lanes : (b + 1) * lanes].reshape(count, images, lanes)
    blank = jnp.zeros((images, lanes), BF16)

    @pl.when(c == 0)
    def _():
        y_row[0, 0] = blank

    @pl.when(c == lax.axis_size("cols") - 1)
    def _():
        y_row[count - 1, 1] = blank


def second(pairs, weights, bias, out_pair):
    _, count, _, images, chans = out_pair.shape
    res = blocks(pairs, weights, count) + bias
    for b in range(2):
        for a in range(2):
            at = (2 * b + a) * chans
            out_pair[a, :, b] = res[:, at : at + chans].reshape(count, images, chans)


def conv_kernel(
    n_rows,
    n_cols,
    x_hbm,
    w1_hbm,
    b1_hbm,
    w2_hbm,
    b2_hbm,
    out,
    ymat,
    wt2,
    bias2,
    recv,
    xmat,
    wt1,
    bias1,
    xs,
    packed,
    w1s,
    w1own,
    w1all,
    w2s,
    b1s,
    b2s,
    load_sem,
    par_sem,
    send_sem,
    recv_sem,
    wsend_sem,
    wrecv_sem,
    swap_send_sem,
    swap_recv_sem,
    wswap_send_sem,
    wswap_recv_sem,
):
    chip_h, pairs = xs.shape[1:3]
    images = xs.shape[-1]
    tile_h, tile_j = chip_h // 2, pairs // n_cols
    win_j = tile_j + 2
    sources = n_rows * n_cols
    r, c = lax.axis_index("model"), lax.axis_index("cols")
    par = lax.rem(r, 2)
    me = r * n_cols + c
    chans = recv.shape[0] * 2

    tops = [tile_h - sum(CHUNK_ROWS[: k + 1]) for k in range(len(CHUNK_ROWS))]
    groups = (
        ((tops[0], chip_h - tops[0]),),
        *(((k, k + n), (chip_h - k - n, chip_h - k)) for k, n in zip(tops[1:], CHUNK_ROWS[1:])),
    )
    loads = []
    for g, spans in enumerate(groups):
        loads.append(
            [
                pltpu.make_async_copy(x_hbm.at[:, lo:hi], xs.at[:, lo:hi], load_sem.at[g, n])
                for n, (lo, hi) in enumerate(spans)
            ]
        )
    for copies in loads:
        for copy in copies:
            copy.start()
    params = [
        pltpu.make_async_copy(src, dst, par_sem.at[s])
        for s, (src, dst) in enumerate(((w1_hbm, w1s), (w2_hbm, w2s), (b1_hbm, b1s), (b2_hbm, b2s)))
    ]
    for copy in params:
        copy.start()

    barrier = pltpu.get_barrier_semaphore()
    to_cs = [lax.rem(c + k, n_cols) for k in range(n_cols)]

    def device(to_r, to_c):
        return {"model": to_r, "cols": to_c}

    to_rs = [lax.rem(r + k, n_rows) for k in range(n_rows)]
    for kr, kc in sorted(
        ((kr, kc) for kr in range(n_rows) for kc in range(n_cols) if kr or kc),
        key=lambda k: (k[1] not in (1, 2), k[0] not in (2, 3, 4, 5), k[1] == 2, k[0] < 4, -min(k[0], n_rows - k[0])),
    ):
        pl.semaphore_signal(barrier, inc=1, device_id=device(to_rs[kr], to_cs[kc]), device_id_type=MESH)

    ahead_r, ahead_c = AHEAD
    is_ahead = (r == ahead_r) & (c == ahead_c)

    def pack_rows(x, lo, hi):
        rows = hi - lo
        left, right = (xs[x, lo:hi, :, p].reshape(rows * pairs * 2, images) for p in range(2))
        both = jnp.concatenate([left, right], axis=1)
        packed[pl.ds(chip_h * x + lo, rows)] = both.reshape(rows, pairs, 2, 2 * images)

    def pack(g):
        for n, copy in enumerate(loads[g]):
            if (g, n) != (1, ahead_r % 2):
                copy.wait()

        def body(x, carry):
            for n, (lo, hi) in enumerate(groups[g]):
                if (g, n) == (1, ahead_r % 2):
                    pl.when(x != ahead_r // 2)(lambda lo=lo, hi=hi: pack_rows(x, lo, hi))
                else:
                    pack_rows(x, lo, hi)
            return carry

        lax.fori_loop(0, n_rows // 2, body, 0)

    last = tile_h + 4

    def rows_of(offset, count):
        def where(to_r):
            q = lax.rem(to_r, 2)
            src = tile_h * to_r + offset + (tile_h - count - 2 * offset) * q
            dst = offset + 2 + (last - count - 2 * offset - 3) * q
            return src, dst

        return where

    chunks = (
        *((n, rows_of(k, n), False) for k, n in zip(tops, CHUNK_ROWS)),
        (2, rows_of(-2, 2), True),
    )
    no_outer = (r == 0) | (r == n_rows - 1)
    at_edge = (c == 0) | (c == n_cols - 1)
    own_j = c == 0
    own_j = own_j.astype(jnp.int32)

    def send_tile(chunk, to_r, to_c, there):
        rows, where, is_outer = chunks[chunk]
        src, dst = where(to_r)
        skip = (to_c == 0).astype(jnp.int32)
        edge = (to_c == 0) | (to_c == n_cols - 1)
        if is_outer:
            there = there & (to_r > 0) & (to_r < n_rows - 1)

        def copy(count, src_j, dst_j):
            pltpu.make_async_remote_copy(
                src_ref=packed.at[pl.ds(src, rows), pl.ds(src_j, count)],
                dst_ref=recv.at[me, pl.ds(dst, rows), pl.ds(dst_j, count)],
                send_sem=send_sem.at[chunk],
                recv_sem=recv_sem.at[chunk],
                device_id=device(to_r, to_c),
                device_id_type=MESH,
            ).start()

        pl.when(there & edge)(lambda: copy(win_j - 1, tile_j * to_c - 1 + skip, skip))
        pl.when(there & jnp.logical_not(edge))(lambda: copy(win_j, tile_j * to_c - 1, 0))

    chips = n_rows // 2

    def step(t, table):
        value = jnp.int32(table[-1])
        for k, entry in enumerate(table[:-1]):
            value = jnp.where(t == k, entry, value)
        return value

    def turn_to(t):
        dx = step(t, CHIPS_ALONG)
        return lax.rem(r // 2 + dx, chips), dx

    def send_chip(chunk, t, where=None):
        x, dx = turn_to(t)
        way = 1 - 2 * lax.rem(par + t, 2)
        for other, dy in CHIP_ORDER:
            to_r = 2 * x + (1 - par if other else par)
            to_c = lax.rem(c + way * dy + n_cols, n_cols)
            there = True
            if not other and dy == 0:
                there = dx > 0
            if where is not None:
                there = there & where(to_r, to_c)
            send_tile(chunk, to_r, to_c, there)

    def send_chunk(chunk):
        early = EARLY_FROM <= chunk

        def body(t, carry):
            if chunk > EARLY_FROM:
                send_chip(chunk, t, lambda to_r, to_c: to_c > 0)
            else:
                send_chip(chunk, t, lambda to_r, to_c: (to_r != ahead_r) | (to_c != ahead_c))
            if early and chunk + 1 < len(chunks):
                x, dx = turn_to(t)
                for other in range(2):
                    to_r = 2 * x + (1 - par if other else par)
                    there = (to_r != r) | (c != 0)
                    if chunk > EARLY_FROM:
                        there = there & (to_r != ahead_r)
                    send_tile(chunk + 1, to_r, jnp.int32(0), there)
                if chunk == EARLY_FROM:
                    there = (x == ahead_r // 2) & jnp.logical_not(is_ahead)
                    send_tile(len(chunks) - 1, jnp.int32(ahead_r), jnp.int32(ahead_c), there)
            return carry

        lax.fori_loop(0, chips, body, 0)

    params[0].wait()
    for dw in range(3):
        w1own[dw] = jnp.concatenate([w1s[1, dw], w1s[0, dw]], axis=1)
    w1own[3] = jnp.concatenate([w1s[2, 0], w1s[2, 1]], axis=1)
    w1own[4] = jnp.concatenate([w1s[2, 2], jnp.zeros_like(w1s[2, 2])], axis=1)
    w1all[r // 2, par, c] = w1own[...]

    for copy in loads[0]:
        copy.wait()
    pack_rows(turn_to(0)[0], *groups[0][0])
    pl.semaphore_wait(barrier, sources - 1)

    def send_weights():
        for kr in range(0, n_rows, 2):
            for kc in range(n_cols):
                if kr or kc:
                    pltpu.make_async_remote_copy(
                        src_ref=w1own,
                        dst_ref=w1all.at[r // 2, par, c],
                        send_sem=wsend_sem,
                        recv_sem=wrecv_sem,
                        device_id=device(to_rs[kr], to_cs[kc]),
                        device_id_type=MESH,
                    ).start()

    def pack_and_send(t, carry):
        pl.when(t < chips - 1)(lambda: pack_rows(turn_to(t + 1)[0], *groups[0][0]))
        there = turn_to(t)[0] == ahead_r // 2

        @pl.when(there)
        def _():
            loads[1][ahead_r % 2].wait()
            pack_rows(ahead_r // 2, *groups[1][ahead_r % 2])

        send_chip(0, t)
        send_tile(1, jnp.int32(ahead_r), jnp.int32(ahead_c), there & jnp.logical_not(is_ahead))
        pl.when(t == 2)(send_weights)
        return carry

    lax.fori_loop(0, chips, pack_and_send, 0)

    for g in range(1, EARLY_FROM + 1):
        pack(g)
    for chunk in range(1, len(chunks)):
        if chunk >= EARLY_FROM and chunk + 1 < len(groups):
            pack(chunk + 1)
        send_chunk(chunk)

    def wait_bytes(ref, sem):
        pltpu.make_async_copy(ref, ref, sem).wait()

    w1_bytes = recv.at[0 : sources // 2 - 1, 0, 0:5]
    wait_bytes(w1_bytes, wrecv_sem)
    wait_bytes(w1_bytes, wsend_sem)
    partner = device(r + 1 - 2 * par, c)
    w_swap = pltpu.make_async_remote_copy(
        src_ref=w1all.at[:, par],
        dst_ref=w1all.at[:, par],
        send_sem=wswap_send_sem,
        recv_sem=wswap_recv_sem,
        device_id=partner,
        device_id_type=MESH,
    )
    w_swap.start()

    def own_rows(chunk):
        rows, where, _ = chunks[chunk]
        src, dst = where(r)

        def copy(count, src_j, dst_j):
            for h in range(rows):
                recv[me, dst + h, pl.ds(dst_j, count)] = packed[src + h, pl.ds(src_j, count)]

        pl.when(at_edge)(lambda: copy(win_j - 1, tile_j * c - 1 + own_j, own_j))
        pl.when(jnp.logical_not(at_edge))(lambda: copy(win_j, tile_j * c - 1, 0))

    for chunk in range(3):
        own_rows(chunk)
    pl.when(jnp.logical_not(no_outer))(lambda: own_rows(3))

    zero_row = jnp.zeros((win_j, 2, 2 * images), BF16)
    zero_col = jnp.zeros((tile_h + 2, 2, 2 * images), BF16)

    def clear(s, carry):
        recv[s, last * (1 - par)] = zero_row
        return carry

    def clear_outer(s, carry):
        recv[s, (last - 1) * par] = zero_row
        recv[s, (last - 1) * par + 1] = zero_row
        return carry

    def clear_edge(s, carry):
        recv[s, pl.ds(3 * par, tile_h + 2), (win_j - 1) * (1 - own_j)] = zero_col
        return carry

    lax.fori_loop(0, sources, clear, 0)
    pl.when(no_outer)(lambda: (lax.fori_loop(0, sources, clear_outer, 0), None)[1])
    pl.when(at_edge)(lambda: (lax.fori_loop(0, sources, clear_edge, 0), None)[1])

    low = lax.broadcasted_iota(jnp.int32, (chans, 2 * chans), 1) < chans

    def spread(wt, u, v, dw):
        ur, vr = pltpu.roll(u, chans, 1), pltpu.roll(v, chans, 1)
        zero = jnp.zeros_like(u)
        tiles = (jnp.where(low, ur, zero), u, jnp.where(low, v, ur), jnp.where(low, zero, vr))
        for k, tile in enumerate(tiles):
            tile = tile.astype(BF16)
            for b in range(2):
                wt[dw + b, k * chans : (k + 1) * chans, b * 2 * chans : (b + 1) * 2 * chans] = tile

    def blank(wt):
        zero = jnp.zeros((4 * chans, 2 * chans), BF16)
        wt[3, :, 0 : 2 * chans] = zero
        wt[0, :, 2 * chans : 4 * chans] = zero

    for copy in params[1:]:
        copy.wait()
    blank(wt1)
    blank(wt2)
    for dw in range(3):
        w = [w2s[dh, dw].astype(F32) for dh in range(3)]
        spread(
            wt2,
            jnp.concatenate([w[1], w[0]], axis=1),
            jnp.concatenate([w[2], jnp.zeros_like(w[2])], axis=1),
            dw,
        )
    bias1[...] = jnp.concatenate([b1s[...]] * 4, axis=1)
    bias2[...] = jnp.concatenate([b2s[...]] * 4, axis=1)

    def arrived(chunk):
        def wait(count):
            wait_bytes(recv.at[0 : sources - 1, 0 : chunks[chunk][0], 0:count], recv_sem.at[chunk])

        pl.when(at_edge)(lambda: wait(win_j - 1))
        pl.when(jnp.logical_not(at_edge))(lambda: wait(win_j))

    arrived(0)
    give = tile_h - (tile_h - 3) * par
    land = tile_h + 2 - (tile_h + 1) * (1 - par)
    swap = pltpu.make_async_remote_copy(
        src_ref=recv.at[:, pl.ds(give, 2)],
        dst_ref=recv.at[:, pl.ds(land, 2)],
        send_sem=swap_send_sem,
        recv_sem=swap_recv_sem,
        device_id=partner,
        device_id_type=MESH,
    )
    swap.start()

    w_swap.wait()
    u = [w1all[:, :, :, k].reshape(chans, 2 * chans).astype(F32) for k in range(5)]
    for dw in range(3):
        v = (u[3], pltpu.roll(u[3], chans, 1), u[4])[dw]
        spread(wt1, u[dw], jnp.where(low, v, 0.0), dw)

    x_pairs, z_pairs = xmat.shape[0], ymat.shape[0]
    o_pairs = z_pairs - 1

    def nth(n, count):
        return (count - 1) * (1 - par) + n * (2 * par - 1)

    def turn_one(n, carry):
        i = nth(n, x_pairs)

        def put(j, value):
            xmat[i, j] = value

        turn(recv, i, put)
        return carry

    def first_one(n, carry):
        i = nth(n, z_pairs)
        fill = jnp.where(n == 0, 1 - par, 2)
        out_of = jnp.where(n == z_pairs - 1, jnp.where(r == 0, 0, jnp.where(r == n_rows - 1, 1, 2)), 2)
        blank_a = jnp.where(fill < 2, fill, out_of)
        first((xmat.at[i], xmat.at[i + 1]), lambda dw: wt1[dw], bias1[...], ymat.at[i], blank_a)
        return carry

    def second_one(n, carry):
        i = nth(n, o_pairs)
        second((ymat.at[i], ymat.at[i + 1]), lambda dw: wt2[dw], bias2[...], out.at[pl.ds(2 * i, 2)])
        return carry

    def stage(s, carry):
        @pl.when(s == 0)
        def _():
            swap.wait()

        for k in range(1, 4):
            there = s == k
            if k == 3:
                there = there & jnp.logical_not(no_outer)
            pl.when(there)(lambda k=k: arrived(k))

        for ends, one in ((TURNS, turn_one), (FIRSTS, first_one), (SECONDS, second_one)):
            lax.fori_loop(step(s, (0, *ends[:-1])), step(s, ends), one, 0)
        return carry

    lax.fori_loop(0, 4, stage, 0)

    per_edge = n_rows * 2
    for chunk in range(4):
        rows = chunks[chunk][0]
        n_r = n_rows - 2 if chunk == 3 else n_rows
        counts = (n_r * 2, n_r * (n_cols - 2))

        def drain(edge_n, inner_n, rows=rows, chunk=chunk):
            wait_bytes(recv.at[0:edge_n, 0:rows, 0 : win_j - 1], send_sem.at[chunk])
            wait_bytes(recv.at[0:inner_n, 0:rows, 0:win_j], send_sem.at[chunk])

        def drain_own(chunk=chunk, counts=counts, drain=drain):
            pl.when(at_edge)(lambda: drain(counts[0] - 1, counts[1]))
            pl.when(jnp.logical_not(at_edge))(lambda: drain(counts[0], counts[1] - 1))

        if chunk == 3:
            pl.when(no_outer)(lambda: drain(*counts))
            pl.when(jnp.logical_not(no_outer))(drain_own)
        else:
            drain_own()


def tail_kernel(tile, ymat, wt2, bias2, out_hbm, o_new, sem):
    par = lax.rem(lax.axis_index("model"), 2)
    rows = out_hbm.shape[0]
    o_pairs = ymat.shape[0] - 1
    late = (rows - 2) * par
    here = 2 * (1 - par)

    def start(k, carry):
        pltpu.make_async_copy(tile.at[par + k], out_hbm.at[k], sem.at[0]).start()
        return carry

    lax.fori_loop(here, here + rows - 2, start, 0)
    i = (o_pairs - 1) * par
    second((ymat.at[i], ymat.at[i + 1]), lambda dw: wt2[dw], bias2[...], o_new)
    last = pltpu.make_async_copy(o_new, out_hbm.at[pl.ds(late, 2)], sem.at[1])
    last.start()
    pltpu.make_async_copy(tile.at[0 : rows - 2], out_hbm.at[0 : rows - 2], sem.at[0]).wait()
    last.wait()


def solution(mesh):
    n_rows = mesh.shape["model"]
    n_cols = mesh.shape["cols"]

    def run_local(x_in, w_conv1, b_conv1, w_conv2, b_conv2):
        images, height, width, own_chans = x_in.shape
        sources = n_rows * n_cols
        chans = own_chans * sources
        pairs = width // 2
        tile_h, tile_j = height // n_rows, pairs // n_cols
        win_j = tile_j + 2
        x_pairs, z_pairs = (tile_h + 5) // 2, (tile_h + 3) // 2
        x_t = jnp.transpose(x_in, (1, 2, 3, 0)).reshape(n_rows // 2, 2 * tile_h, pairs, 2, own_chans, images)
        args = (x_t, w_conv1, b_conv1.reshape(1, chans), w_conv2, b_conv2.reshape(1, chans))
        hbm = pl.BlockSpec(memory_space=pltpu.HBM)
        vmem = pl.BlockSpec(memory_space=pltpu.VMEM)
        kept = (
            pltpu.VMEM((2 * (z_pairs - 1), tile_j, 2, images, chans), F32),
            pltpu.VMEM((z_pairs, win_j - 1, 2, images, 2 * chans), BF16),
            pltpu.VMEM((4, 4 * chans, 4 * chans), BF16),
            pltpu.VMEM((1, 4 * chans), F32),
        )
        state = pl.pallas_call(
            functools.partial(conv_kernel, n_rows, n_cols),
            out_shape=kept,
            in_specs=[hbm] * 5,
            out_specs=[vmem] * len(kept),
            scratch_shapes=[
                pltpu.VMEM((sources, 2 * x_pairs, win_j, own_chans, 2 * images), BF16),
                pltpu.VMEM((x_pairs, win_j, 2, images, 2 * chans), BF16),
                pltpu.VMEM((4, 4 * chans, 4 * chans), BF16),
                pltpu.VMEM((1, 4 * chans), F32),
                pltpu.VMEM((n_rows // 2, 2 * tile_h, pairs, 2, own_chans, images), BF16),
                pltpu.VMEM((height, pairs, own_chans, 2 * images), BF16),
                pltpu.VMEM((3, 3, own_chans, chans), BF16),
                pltpu.VMEM((5, own_chans, 2 * chans), BF16),
                pltpu.VMEM((n_rows // 2, 2, n_cols, 5, own_chans, 2 * chans), BF16),
                pltpu.VMEM((3, 3, chans, chans), BF16),
                pltpu.VMEM((1, chans), F32),
                pltpu.VMEM((1, chans), F32),
                pltpu.SemaphoreType.DMA((3, 2)),
                pltpu.SemaphoreType.DMA((4,)),
                pltpu.SemaphoreType.DMA((4,)),
                pltpu.SemaphoreType.DMA((4,)),
            ]
            + [pltpu.SemaphoreType.DMA] * 6,
            compiler_params=pltpu.CompilerParams(
                collective_id=0, has_side_effects=True, vmem_limit_bytes=24 << 20
            ),
            name="conv",
        )(*(pltpu.with_memory_space_constraint(a, pltpu.HBM) for a in args))
        out = pl.pallas_call(
            tail_kernel,
            out_shape=jax.ShapeDtypeStruct((tile_h, tile_j, 2, images, chans), F32),
            in_specs=[vmem] * len(kept),
            out_specs=pl.BlockSpec(memory_space=pl.ANY),
            scratch_shapes=[
                pltpu.VMEM((2, tile_j, 2, images, chans), F32),
                pltpu.SemaphoreType.DMA((2,)),
            ],
            compiler_params=pltpu.CompilerParams(vmem_limit_bytes=8 << 20),
            name="tail",
        )(*state)
        out = out.reshape(tile_h, 2 * tile_j, images, chans)
        return jnp.transpose(out, (2, 0, 1, 3))

    group = ("model", "cols")
    return jax.shard_map(
        run_local,
        mesh=mesh,
        in_specs=(P("data", None, None, group), P(None, None, group, None), P(), P(), P()),
        out_specs=P("data", "model", "cols", None),
        check_vma=False,
    )
```

```python
import functools

import jax
import jax.numpy as jnp
from jax import lax
from jax.experimental import pallas as pl
from jax.experimental.pallas import tpu as pltpu
from jax.sharding import PartitionSpec as P

MESH = pl.DeviceIdType.MESH
BF16 = jnp.bfloat16
F32 = jnp.float32
CHUNK_ROWS = (2, 3, 2)
TURNS, FIRSTS, SECONDS = (2, 4, 5, 6), (1, 3, 4, 5), (0, 2, 3, 3)
EARLY_FROM = 1
AHEAD = (1, 0)
CHIPS_ALONG = (3, 1, 2, 0)
CHIP_ORDER = tuple((other, dy) for other in (0, 1) for dy in (0, 1, 2, -1))


def turn(recv, i, put):
    sources, _, win_j, own_chans, lanes = recv.shape
    chans = sources * own_chans
    for j in range(win_j):
        top = recv[:, 2 * i, j].reshape(chans, lanes)
        under = recv[:, 2 * i + 1, j].reshape(chans, lanes)
        put(j, jnp.concatenate([top, under], axis=0).T.reshape(2, lanes // 2, 2 * chans))


def blocks(pairs, weights, count):
    acc = None
    for dw in range(4):
        parts = [view[dw // 2 : dw // 2 + count, dw % 2] for view in pairs]
        lhs = jnp.concatenate([p.reshape(count * p.shape[1], p.shape[2]) for p in parts], axis=1)
        term = jnp.dot(lhs, weights(dw), preferred_element_type=F32)
        acc = term if acc is None else acc + term
    return acc


def first(pairs, weights, bias, y_row, blank_a):
    count, _, images, lanes = y_row.shape
    c = lax.axis_index("cols")
    row = lax.rem(lax.broadcasted_iota(jnp.int32, (1, 2 * lanes), 1), lanes) // (lanes // 2)
    act = jnp.maximum(blocks(pairs, weights, count) + bias, 0.0)
    act = jnp.where(row != blank_a, act, 0.0).astype(BF16)
    for b in range(2):
        y_row[:, b] = act[:, b * lanes : (b + 1) * lanes].reshape(count, images, lanes)
    blank = jnp.zeros((images, lanes), BF16)

    @pl.when(c == 0)
    def _():
        y_row[0, 0] = blank

    @pl.when(c == lax.axis_size("cols") - 1)
    def _():
        y_row[count - 1, 1] = blank


def second(pairs, weights, bias, out_pair):
    _, count, _, images, chans = out_pair.shape
    res = blocks(pairs, weights, count) + bias
    for b in range(2):
        for a in range(2):
            at = (2 * b + a) * chans
            out_pair[a, :, b] = res[:, at : at + chans].reshape(count, images, chans)


def conv_kernel(
    n_rows,
    n_cols,
    x_hbm,
    w1_hbm,
    b1_hbm,
    w2_hbm,
    b2_hbm,
    out,
    ymat,
    wt2,
    bias2,
    recv,
    xmat,
    wt1,
    bias1,
    xs,
    packed,
    w1s,
    w1own,
    w1all,
    w2s,
    b1s,
    b2s,
    load_sem,
    par_sem,
    send_sem,
    recv_sem,
    wsend_sem,
    wrecv_sem,
    swap_send_sem,
    swap_recv_sem,
    wswap_send_sem,
    wswap_recv_sem,
):
    chip_h, pairs = xs.shape[1:3]
    images = xs.shape[-1]
    tile_h, tile_j = chip_h // 2, pairs // n_cols
    win_j = tile_j + 2
    sources = n_rows * n_cols
    r, c = lax.axis_index("model"), lax.axis_index("cols")
    par = lax.rem(r, 2)
    me = r * n_cols + c
    chans = recv.shape[0] * 2

    tops = [tile_h - sum(CHUNK_ROWS[: k + 1]) for k in range(len(CHUNK_ROWS))]
    groups = (
        ((tops[0], chip_h - tops[0]),),
        *(((k, k + n), (chip_h - k - n, chip_h - k)) for k, n in zip(tops[1:], CHUNK_ROWS[1:])),
    )
    loads = []
    for g, spans in enumerate(groups):
        loads.append(
            [
                pltpu.make_async_copy(x_hbm.at[:, lo:hi], xs.at[:, lo:hi], load_sem.at[g, n])
                for n, (lo, hi) in enumerate(spans)
            ]
        )
    for copies in loads:
        for copy in copies:
            copy.start()
    params = [
        pltpu.make_async_copy(src, dst, par_sem.at[s])
        for s, (src, dst) in enumerate(((w1_hbm, w1s), (w2_hbm, w2s), (b1_hbm, b1s), (b2_hbm, b2s)))
    ]
    for copy in params:
        copy.start()

    barrier = pltpu.get_barrier_semaphore()
    to_cs = [lax.rem(c + k, n_cols) for k in range(n_cols)]

    def device(to_r, to_c):
        return {"model": to_r, "cols": to_c}

    to_rs = [lax.rem(r + k, n_rows) for k in range(n_rows)]
    for kr, kc in sorted(
        ((kr, kc) for kr in range(n_rows) for kc in range(n_cols) if kr or kc),
        key=lambda k: (k[1] not in (1, 2), k[0] not in (2, 3, 4, 5), k[1] == 2, k[0] < 4, -min(k[0], n_rows - k[0])),
    ):
        pl.semaphore_signal(barrier, inc=1, device_id=device(to_rs[kr], to_cs[kc]), device_id_type=MESH)

    ahead_r, ahead_c = AHEAD
    is_ahead = (r == ahead_r) & (c == ahead_c)

    def pack_rows(x, lo, hi):
        rows = hi - lo
        left, right = (xs[x, lo:hi, :, p].reshape(rows * pairs * 2, images) for p in range(2))
        both = jnp.concatenate([left, right], axis=1)
        packed[pl.ds(chip_h * x + lo, rows)] = both.reshape(rows, pairs, 2, 2 * images)

    def pack(g):
        for n, copy in enumerate(loads[g]):
            if (g, n) != (1, ahead_r % 2):
                copy.wait()

        def body(x, carry):
            for n, (lo, hi) in enumerate(groups[g]):
                if (g, n) == (1, ahead_r % 2):
                    pl.when(x != ahead_r // 2)(lambda lo=lo, hi=hi: pack_rows(x, lo, hi))
                else:
                    pack_rows(x, lo, hi)
            return carry

        lax.fori_loop(0, n_rows // 2, body, 0)

    last = tile_h + 4

    def rows_of(offset, count):
        def where(to_r):
            q = lax.rem(to_r, 2)
            src = tile_h * to_r + offset + (tile_h - count - 2 * offset) * q
            dst = offset + 2 + (last - count - 2 * offset - 3) * q
            return src, dst

        return where

    chunks = (
        *((n, rows_of(k, n), False) for k, n in zip(tops, CHUNK_ROWS)),
        (2, rows_of(-2, 2), True),
    )
    no_outer = (r == 0) | (r == n_rows - 1)
    at_edge = (c == 0) | (c == n_cols - 1)
    own_j = c == 0
    own_j = own_j.astype(jnp.int32)

    def send_tile(chunk, to_r, to_c, there):
        rows, where, is_outer = chunks[chunk]
        src, dst = where(to_r)
        skip = (to_c == 0).astype(jnp.int32)
        edge = (to_c == 0) | (to_c == n_cols - 1)
        if is_outer:
            there = there & (to_r > 0) & (to_r < n_rows - 1)

        def copy(count, src_j, dst_j):
            pltpu.make_async_remote_copy(
                src_ref=packed.at[pl.ds(src, rows), pl.ds(src_j, count)],
                dst_ref=recv.at[me, pl.ds(dst, rows), pl.ds(dst_j, count)],
                send_sem=send_sem.at[chunk],
                recv_sem=recv_sem.at[chunk],
                device_id=device(to_r, to_c),
                device_id_type=MESH,
            ).start()

        pl.when(there & edge)(lambda: copy(win_j - 1, tile_j * to_c - 1 + skip, skip))
        pl.when(there & jnp.logical_not(edge))(lambda: copy(win_j, tile_j * to_c - 1, 0))

    chips = n_rows // 2

    def step(t, table):
        value = jnp.int32(table[-1])
        for k, entry in enumerate(table[:-1]):
            value = jnp.where(t == k, entry, value)
        return value

    def turn_to(t):
        dx = step(t, CHIPS_ALONG)
        return lax.rem(r // 2 + dx, chips), dx

    def send_chip(chunk, t, where=None):
        x, dx = turn_to(t)
        way = 1 - 2 * lax.rem(par + t, 2)
        for other, dy in CHIP_ORDER:
            to_r = 2 * x + (1 - par if other else par)
            to_c = lax.rem(c + way * dy + n_cols, n_cols)
            there = True
            if not other and dy == 0:
                there = dx > 0
            if where is not None:
                there = there & where(to_r, to_c)
            send_tile(chunk, to_r, to_c, there)

    def send_chunk(chunk):
        early = EARLY_FROM <= chunk

        def body(t, carry):
            if chunk > EARLY_FROM:
                send_chip(chunk, t, lambda to_r, to_c: to_c > 0)
            else:
                send_chip(chunk, t, lambda to_r, to_c: (to_r != ahead_r) | (to_c != ahead_c))
            if early and chunk + 1 < len(chunks):
                x, dx = turn_to(t)
                for other in range(2):
                    to_r = 2 * x + (1 - par if other else par)
                    there = (to_r != r) | (c != 0)
                    if chunk > EARLY_FROM:
                        there = there & (to_r != ahead_r)
                    send_tile(chunk + 1, to_r, jnp.int32(0), there)
                if chunk == EARLY_FROM:
                    there = (x == ahead_r // 2) & jnp.logical_not(is_ahead)
                    send_tile(len(chunks) - 1, jnp.int32(ahead_r), jnp.int32(ahead_c), there)
            return carry

        lax.fori_loop(0, chips, body, 0)

    params[0].wait()
    for dw in range(3):
        w1own[dw] = jnp.concatenate([w1s[1, dw], w1s[0, dw]], axis=1)
    w1own[3] = jnp.concatenate([w1s[2, 0], w1s[2, 1]], axis=1)
    w1own[4] = jnp.concatenate([w1s[2, 2], jnp.zeros_like(w1s[2, 2])], axis=1)
    w1all[r // 2, par, c] = w1own[...]

    for copy in loads[0]:
        copy.wait()
    pack_rows(turn_to(0)[0], *groups[0][0])
    pl.semaphore_wait(barrier, sources - 1)

    def send_weights():
        for kr in range(0, n_rows, 2):
            for kc in range(n_cols):
                if kr or kc:
                    pltpu.make_async_remote_copy(
                        src_ref=w1own,
                        dst_ref=w1all.at[r // 2, par, c],
                        send_sem=wsend_sem,
                        recv_sem=wrecv_sem,
                        device_id=device(to_rs[kr], to_cs[kc]),
                        device_id_type=MESH,
                    ).start()

    def pack_and_send(t, carry):
        pl.when(t < chips - 1)(lambda: pack_rows(turn_to(t + 1)[0], *groups[0][0]))
        there = turn_to(t)[0] == ahead_r // 2

        @pl.when(there)
        def _():
            loads[1][ahead_r % 2].wait()
            pack_rows(ahead_r // 2, *groups[1][ahead_r % 2])

        send_chip(0, t)
        send_tile(1, jnp.int32(ahead_r), jnp.int32(ahead_c), there & jnp.logical_not(is_ahead))
        pl.when(t == 1)(send_weights)
        return carry

    lax.fori_loop(0, chips, pack_and_send, 0)

    for g in range(1, EARLY_FROM + 1):
        pack(g)
    for chunk in range(1, len(chunks)):
        if chunk >= EARLY_FROM and chunk + 1 < len(groups):
            pack(chunk + 1)
        send_chunk(chunk)

    def wait_bytes(ref, sem):
        pltpu.make_async_copy(ref, ref, sem).wait()

    w1_bytes = recv.at[0 : sources // 2 - 1, 0, 0:5]
    wait_bytes(w1_bytes, wrecv_sem)
    wait_bytes(w1_bytes, wsend_sem)
    partner = device(r + 1 - 2 * par, c)
    w_swap = pltpu.make_async_remote_copy(
        src_ref=w1all.at[:, par],
        dst_ref=w1all.at[:, par],
        send_sem=wswap_send_sem,
        recv_sem=wswap_recv_sem,
        device_id=partner,
        device_id_type=MESH,
    )
    w_swap.start()

    def own_rows(chunk):
        rows, where, _ = chunks[chunk]
        src, dst = where(r)

        def copy(count, src_j, dst_j):
            for h in range(rows):
                recv[me, dst + h, pl.ds(dst_j, count)] = packed[src + h, pl.ds(src_j, count)]

        pl.when(at_edge)(lambda: copy(win_j - 1, tile_j * c - 1 + own_j, own_j))
        pl.when(jnp.logical_not(at_edge))(lambda: copy(win_j, tile_j * c - 1, 0))

    for chunk in range(3):
        own_rows(chunk)
    pl.when(jnp.logical_not(no_outer))(lambda: own_rows(3))

    zero_row = jnp.zeros((win_j, 2, 2 * images), BF16)
    zero_col = jnp.zeros((tile_h + 2, 2, 2 * images), BF16)

    def clear(s, carry):
        recv[s, last * (1 - par)] = zero_row
        return carry

    def clear_outer(s, carry):
        recv[s, (last - 1) * par] = zero_row
        recv[s, (last - 1) * par + 1] = zero_row
        return carry

    def clear_edge(s, carry):
        recv[s, pl.ds(3 * par, tile_h + 2), (win_j - 1) * (1 - own_j)] = zero_col
        return carry

    lax.fori_loop(0, sources, clear, 0)
    pl.when(no_outer)(lambda: (lax.fori_loop(0, sources, clear_outer, 0), None)[1])
    pl.when(at_edge)(lambda: (lax.fori_loop(0, sources, clear_edge, 0), None)[1])

    low = lax.broadcasted_iota(jnp.int32, (chans, 2 * chans), 1) < chans

    def spread(wt, u, v, dw):
        ur, vr = pltpu.roll(u, chans, 1), pltpu.roll(v, chans, 1)
        zero = jnp.zeros_like(u)
        tiles = (jnp.where(low, ur, zero), u, jnp.where(low, v, ur), jnp.where(low, zero, vr))
        for k, tile in enumerate(tiles):
            tile = tile.astype(BF16)
            for b in range(2):
                wt[dw + b, k * chans : (k + 1) * chans, b * 2 * chans : (b + 1) * 2 * chans] = tile

    def blank(wt):
        zero = jnp.zeros((4 * chans, 2 * chans), BF16)
        wt[3, :, 0 : 2 * chans] = zero
        wt[0, :, 2 * chans : 4 * chans] = zero

    for copy in params[1:]:
        copy.wait()
    blank(wt1)
    blank(wt2)
    for dw in range(3):
        w = [w2s[dh, dw].astype(F32) for dh in range(3)]
        spread(
            wt2,
            jnp.concatenate([w[1], w[0]], axis=1),
            jnp.concatenate([w[2], jnp.zeros_like(w[2])], axis=1),
            dw,
        )
    bias1[...] = jnp.concatenate([b1s[...]] * 4, axis=1)
    bias2[...] = jnp.concatenate([b2s[...]] * 4, axis=1)

    def arrived(chunk):
        def wait(count):
            wait_bytes(recv.at[0 : sources - 1, 0 : chunks[chunk][0], 0:count], recv_sem.at[chunk])

        pl.when(at_edge)(lambda: wait(win_j - 1))
        pl.when(jnp.logical_not(at_edge))(lambda: wait(win_j))

    arrived(0)
    give = tile_h - (tile_h - 3) * par
    land = tile_h + 2 - (tile_h + 1) * (1 - par)
    swap = pltpu.make_async_remote_copy(
        src_ref=recv.at[:, pl.ds(give, 2)],
        dst_ref=recv.at[:, pl.ds(land, 2)],
        send_sem=swap_send_sem,
        recv_sem=swap_recv_sem,
        device_id=partner,
        device_id_type=MESH,
    )
    swap.start()

    w_swap.wait()
    u = [w1all[:, :, :, k].reshape(chans, 2 * chans).astype(F32) for k in range(5)]
    for dw in range(3):
        v = (u[3], pltpu.roll(u[3], chans, 1), u[4])[dw]
        spread(wt1, u[dw], jnp.where(low, v, 0.0), dw)

    x_pairs, z_pairs = xmat.shape[0], ymat.shape[0]
    o_pairs = z_pairs - 1

    def nth(n, count):
        return (count - 1) * (1 - par) + n * (2 * par - 1)

    def turn_one(n, carry):
        i = nth(n, x_pairs)

        def put(j, value):
            xmat[i, j] = value

        turn(recv, i, put)
        return carry

    def first_one(n, carry):
        i = nth(n, z_pairs)
        fill = jnp.where(n == 0, 1 - par, 2)
        out_of = jnp.where(n == z_pairs - 1, jnp.where(r == 0, 0, jnp.where(r == n_rows - 1, 1, 2)), 2)
        blank_a = jnp.where(fill < 2, fill, out_of)
        first((xmat.at[i], xmat.at[i + 1]), lambda dw: wt1[dw], bias1[...], ymat.at[i], blank_a)
        return carry

    def second_one(n, carry):
        i = nth(n, o_pairs)
        second((ymat.at[i], ymat.at[i + 1]), lambda dw: wt2[dw], bias2[...], out.at[pl.ds(2 * i, 2)])
        return carry

    def stage(s, carry):
        @pl.when(s == 0)
        def _():
            swap.wait()

        for k in range(1, 4):
            there = s == k
            if k == 3:
                there = there & jnp.logical_not(no_outer)
            pl.when(there)(lambda k=k: arrived(k))

        for ends, one in ((TURNS, turn_one), (FIRSTS, first_one), (SECONDS, second_one)):
            lax.fori_loop(step(s, (0, *ends[:-1])), step(s, ends), one, 0)
        return carry

    lax.fori_loop(0, 4, stage, 0)

    per_edge = n_rows * 2
    for chunk in range(4):
        rows = chunks[chunk][0]
        n_r = n_rows - 2 if chunk == 3 else n_rows
        counts = (n_r * 2, n_r * (n_cols - 2))

        def drain(edge_n, inner_n, rows=rows, chunk=chunk):
            wait_bytes(recv.at[0:edge_n, 0:rows, 0 : win_j - 1], send_sem.at[chunk])
            wait_bytes(recv.at[0:inner_n, 0:rows, 0:win_j], send_sem.at[chunk])

        def drain_own(chunk=chunk, counts=counts, drain=drain):
            pl.when(at_edge)(lambda: drain(counts[0] - 1, counts[1]))
            pl.when(jnp.logical_not(at_edge))(lambda: drain(counts[0], counts[1] - 1))

        if chunk == 3:
            pl.when(no_outer)(lambda: drain(*counts))
            pl.when(jnp.logical_not(no_outer))(drain_own)
        else:
            drain_own()


def tail_kernel(tile, ymat, wt2, bias2, out_hbm, o_new, sem):
    par = lax.rem(lax.axis_index("model"), 2)
    rows = out_hbm.shape[0]
    o_pairs = ymat.shape[0] - 1
    late = (rows - 2) * par
    here = 2 * (1 - par)

    cut = out_hbm.shape[1] // 2

    def start(k, carry):
        for part in (pl.ds(0, cut), pl.ds(cut, out_hbm.shape[1] - cut)):
            pltpu.make_async_copy(tile.at[par + k, part], out_hbm.at[k, part], sem.at[0]).start()
        return carry

    lax.fori_loop(here, here + rows - 2, start, 0)
    i = (o_pairs - 1) * par
    second((ymat.at[i], ymat.at[i + 1]), lambda dw: wt2[dw], bias2[...], o_new)
    for k in range(2):
        for part in (pl.ds(0, cut), pl.ds(cut, out_hbm.shape[1] - cut)):
            pltpu.make_async_copy(o_new.at[k, part], out_hbm.at[late + k, part], sem.at[1]).start()
    pltpu.make_async_copy(tile.at[0 : rows - 2], out_hbm.at[0 : rows - 2], sem.at[0]).wait()
    pltpu.make_async_copy(o_new, out_hbm.at[pl.ds(late, 2)], sem.at[1]).wait()


def solution(mesh):
    n_rows = mesh.shape["model"]
    n_cols = mesh.shape["cols"]

    def run_local(x_in, w_conv1, b_conv1, w_conv2, b_conv2):
        images, height, width, own_chans = x_in.shape
        sources = n_rows * n_cols
        chans = own_chans * sources
        pairs = width // 2
        tile_h, tile_j = height // n_rows, pairs // n_cols
        win_j = tile_j + 2
        x_pairs, z_pairs = (tile_h + 5) // 2, (tile_h + 3) // 2
        x_t = jnp.transpose(x_in, (1, 2, 3, 0)).reshape(n_rows // 2, 2 * tile_h, pairs, 2, own_chans, images)
        args = (x_t, w_conv1, b_conv1.reshape(1, chans), w_conv2, b_conv2.reshape(1, chans))
        hbm = pl.BlockSpec(memory_space=pltpu.HBM)
        vmem = pl.BlockSpec(memory_space=pltpu.VMEM)
        kept = (
            pltpu.VMEM((2 * (z_pairs - 1), tile_j, 2, images, chans), F32),
            pltpu.VMEM((z_pairs, win_j - 1, 2, images, 2 * chans), BF16),
            pltpu.VMEM((4, 4 * chans, 4 * chans), BF16),
            pltpu.VMEM((1, 4 * chans), F32),
        )
        state = pl.pallas_call(
            functools.partial(conv_kernel, n_rows, n_cols),
            out_shape=kept,
            in_specs=[hbm] * 5,
            out_specs=[vmem] * len(kept),
            scratch_shapes=[
                pltpu.VMEM((sources, 2 * x_pairs, win_j, own_chans, 2 * images), BF16),
                pltpu.VMEM((x_pairs, win_j, 2, images, 2 * chans), BF16),
                pltpu.VMEM((4, 4 * chans, 4 * chans), BF16),
                pltpu.VMEM((1, 4 * chans), F32),
                pltpu.VMEM((n_rows // 2, 2 * tile_h, pairs, 2, own_chans, images), BF16),
                pltpu.VMEM((height, pairs, own_chans, 2 * images), BF16),
                pltpu.VMEM((3, 3, own_chans, chans), BF16),
                pltpu.VMEM((5, own_chans, 2 * chans), BF16),
                pltpu.VMEM((n_rows // 2, 2, n_cols, 5, own_chans, 2 * chans), BF16),
                pltpu.VMEM((3, 3, chans, chans), BF16),
                pltpu.VMEM((1, chans), F32),
                pltpu.VMEM((1, chans), F32),
                pltpu.SemaphoreType.DMA((3, 2)),
                pltpu.SemaphoreType.DMA((4,)),
                pltpu.SemaphoreType.DMA((4,)),
                pltpu.SemaphoreType.DMA((4,)),
            ]
            + [pltpu.SemaphoreType.DMA] * 6,
            compiler_params=pltpu.CompilerParams(
                collective_id=0, has_side_effects=True, vmem_limit_bytes=24 << 20
            ),
            name="conv",
        )(*(pltpu.with_memory_space_constraint(a, pltpu.HBM) for a in args))
        out = pl.pallas_call(
            tail_kernel,
            out_shape=jax.ShapeDtypeStruct((tile_h, tile_j, 2, images, chans), F32),
            in_specs=[vmem] * len(kept),
            out_specs=pl.BlockSpec(memory_space=pl.ANY),
            scratch_shapes=[
                pltpu.VMEM((2, tile_j, 2, images, chans), F32),
                pltpu.SemaphoreType.DMA((2,)),
            ],
            compiler_params=pltpu.CompilerParams(vmem_limit_bytes=8 << 20),
            name="tail",
        )(*state)
        out = out.reshape(tile_h, 2 * tile_j, images, chans)
        return jnp.transpose(out, (2, 0, 1, 3))

    group = ("model", "cols")
    return jax.shard_map(
        run_local,
        mesh=mesh,
        in_specs=(P("data", None, None, group), P(None, None, group, None), P(), P(), P()),
        out_specs=P("data", "model", "cols", None),
        check_vma=False,
    )
```

```python
import functools

import jax
import jax.numpy as jnp
from jax import lax
from jax.experimental import pallas as pl
from jax.experimental.pallas import tpu as pltpu
from jax.sharding import PartitionSpec as P

MESH = pl.DeviceIdType.MESH
BF16 = jnp.bfloat16
F32 = jnp.float32
CHUNK_ROWS = (2, 3, 2)
TURNS, FIRSTS, SECONDS = (2, 4, 5, 6), (1, 3, 4, 5), (0, 2, 3, 3)
EARLY_FROM = 1
AHEAD = (1, 0)
CHIPS_ALONG = (3, 1, 2, 0)
CHIP_ORDER = tuple((other, dy) for other in (0, 1) for dy in (0, 1, -1, 2))


def turn(recv, i, put):
    sources, _, win_j, own_chans, lanes = recv.shape
    chans = sources * own_chans
    for j in range(win_j):
        top = recv[:, 2 * i, j].reshape(chans, lanes)
        under = recv[:, 2 * i + 1, j].reshape(chans, lanes)
        put(j, jnp.concatenate([top, under], axis=0).T.reshape(2, lanes // 2, 2 * chans))


def blocks(pairs, weights, count):
    acc = None
    for dw in range(4):
        parts = [view[dw // 2 : dw // 2 + count, dw % 2] for view in pairs]
        lhs = jnp.concatenate([p.reshape(count * p.shape[1], p.shape[2]) for p in parts], axis=1)
        term = jnp.dot(lhs, weights(dw), preferred_element_type=F32)
        acc = term if acc is None else acc + term
    return acc


def first(pairs, weights, bias, y_row, blank_a):
    count, _, images, lanes = y_row.shape
    c = lax.axis_index("cols")
    row = lax.rem(lax.broadcasted_iota(jnp.int32, (1, 2 * lanes), 1), lanes) // (lanes // 2)
    act = jnp.maximum(blocks(pairs, weights, count) + bias, 0.0)
    act = jnp.where(row != blank_a, act, 0.0).astype(BF16)
    for b in range(2):
        y_row[:, b] = act[:, b * lanes : (b + 1) * lanes].reshape(count, images, lanes)
    blank = jnp.zeros((images, lanes), BF16)

    @pl.when(c == 0)
    def _():
        y_row[0, 0] = blank

    @pl.when(c == lax.axis_size("cols") - 1)
    def _():
        y_row[count - 1, 1] = blank


def second(pairs, weights, bias, out_pair):
    _, count, _, images, chans = out_pair.shape
    res = blocks(pairs, weights, count) + bias
    for b in range(2):
        for a in range(2):
            at = (2 * b + a) * chans
            out_pair[a, :, b] = res[:, at : at + chans].reshape(count, images, chans)


def conv_kernel(
    n_rows,
    n_cols,
    x_hbm,
    w1_hbm,
    b1_hbm,
    w2_hbm,
    b2_hbm,
    out,
    ymat,
    wt2,
    bias2,
    recv,
    xmat,
    wt1,
    bias1,
    xs,
    packed,
    w1s,
    w1own,
    w1all,
    w2s,
    b1s,
    b2s,
    load_sem,
    par_sem,
    send_sem,
    recv_sem,
    wsend_sem,
    wrecv_sem,
    swap_send_sem,
    swap_recv_sem,
    wswap_send_sem,
    wswap_recv_sem,
):
    chip_h, pairs = xs.shape[1:3]
    images = xs.shape[-1]
    tile_h, tile_j = chip_h // 2, pairs // n_cols
    win_j = tile_j + 2
    sources = n_rows * n_cols
    r, c = lax.axis_index("model"), lax.axis_index("cols")
    par = lax.rem(r, 2)
    me = r * n_cols + c
    chans = recv.shape[0] * 2

    tops = [tile_h - sum(CHUNK_ROWS[: k + 1]) for k in range(len(CHUNK_ROWS))]
    groups = (
        ((tops[0], chip_h - tops[0]),),
        *(((k, k + n), (chip_h - k - n, chip_h - k)) for k, n in zip(tops[1:], CHUNK_ROWS[1:])),
    )
    loads = []
    for g, spans in enumerate(groups):
        loads.append(
            [
                pltpu.make_async_copy(x_hbm.at[:, lo:hi], xs.at[:, lo:hi], load_sem.at[g, n])
                for n, (lo, hi) in enumerate(spans)
            ]
        )
    for copies in loads:
        for copy in copies:
            copy.start()
    params = [
        pltpu.make_async_copy(src, dst, par_sem.at[s])
        for s, (src, dst) in enumerate(((w1_hbm, w1s), (w2_hbm, w2s), (b1_hbm, b1s), (b2_hbm, b2s)))
    ]
    for copy in params:
        copy.start()

    barrier = pltpu.get_barrier_semaphore()
    to_cs = [lax.rem(c + k, n_cols) for k in range(n_cols)]

    def device(to_r, to_c):
        return {"model": to_r, "cols": to_c}

    to_rs = [lax.rem(r + k, n_rows) for k in range(n_rows)]
    for kr, kc in sorted(
        ((kr, kc) for kr in range(n_rows) for kc in range(n_cols) if kr or kc),
        key=lambda k: (k[1] not in (1, 2), k[0] not in (2, 3, 4, 5), k[1] == 2, k[0] < 4, -min(k[0], n_rows - k[0])),
    ):
        pl.semaphore_signal(barrier, inc=1, device_id=device(to_rs[kr], to_cs[kc]), device_id_type=MESH)

    ahead_r, ahead_c = AHEAD
    is_ahead = (r == ahead_r) & (c == ahead_c)

    def pack_rows(x, lo, hi):
        rows = hi - lo
        left, right = (xs[x, lo:hi, :, p].reshape(rows * pairs * 2, images) for p in range(2))
        both = jnp.concatenate([left, right], axis=1)
        packed[pl.ds(chip_h * x + lo, rows)] = both.reshape(rows, pairs, 2, 2 * images)

    def pack(g):
        for n, copy in enumerate(loads[g]):
            if (g, n) != (1, ahead_r % 2):
                copy.wait()

        def body(x, carry):
            for n, (lo, hi) in enumerate(groups[g]):
                if (g, n) == (1, ahead_r % 2):
                    pl.when(x != ahead_r // 2)(lambda lo=lo, hi=hi: pack_rows(x, lo, hi))
                else:
                    pack_rows(x, lo, hi)
            return carry

        lax.fori_loop(0, n_rows // 2, body, 0)

    last = tile_h + 4

    def rows_of(offset, count):
        def where(to_r):
            q = lax.rem(to_r, 2)
            src = tile_h * to_r + offset + (tile_h - count - 2 * offset) * q
            dst = offset + 2 + (last - count - 2 * offset - 3) * q
            return src, dst

        return where

    chunks = (
        *((n, rows_of(k, n), False) for k, n in zip(tops, CHUNK_ROWS)),
        (2, rows_of(-2, 2), True),
    )
    no_outer = (r == 0) | (r == n_rows - 1)
    at_edge = (c == 0) | (c == n_cols - 1)
    own_j = c == 0
    own_j = own_j.astype(jnp.int32)

    def send_tile(chunk, to_r, to_c, there):
        rows, where, is_outer = chunks[chunk]
        src, dst = where(to_r)
        skip = (to_c == 0).astype(jnp.int32)
        edge = (to_c == 0) | (to_c == n_cols - 1)
        if is_outer:
            there = there & (to_r > 0) & (to_r < n_rows - 1)

        def copy(count, src_j, dst_j):
            pltpu.make_async_remote_copy(
                src_ref=packed.at[pl.ds(src, rows), pl.ds(src_j, count)],
                dst_ref=recv.at[me, pl.ds(dst, rows), pl.ds(dst_j, count)],
                send_sem=send_sem.at[chunk],
                recv_sem=recv_sem.at[chunk],
                device_id=device(to_r, to_c),
                device_id_type=MESH,
            ).start()

        pl.when(there & edge)(lambda: copy(win_j - 1, tile_j * to_c - 1 + skip, skip))
        pl.when(there & jnp.logical_not(edge))(lambda: copy(win_j, tile_j * to_c - 1, 0))

    chips = n_rows // 2

    def step(t, table):
        value = jnp.int32(table[-1])
        for k, entry in enumerate(table[:-1]):
            value = jnp.where(t == k, entry, value)
        return value

    def turn_to(t):
        dx = step(t, CHIPS_ALONG)
        return lax.rem(r // 2 + dx, chips), dx

    def send_chip(chunk, t, where=None):
        x, dx = turn_to(t)
        way = 1 - 2 * lax.rem(par + t, 2)
        for other, dy in CHIP_ORDER:
            to_r = 2 * x + (1 - par if other else par)
            to_c = lax.rem(c + way * dy + n_cols, n_cols)
            there = True
            if not other and dy == 0:
                there = dx > 0
            if where is not None:
                there = there & where(to_r, to_c)
            send_tile(chunk, to_r, to_c, there)

    def send_chunk(chunk):
        early = EARLY_FROM <= chunk

        def body(t, carry):
            if chunk > EARLY_FROM:
                send_chip(chunk, t, lambda to_r, to_c: to_c > 0)
            else:
                send_chip(chunk, t, lambda to_r, to_c: (to_r != ahead_r) | (to_c != ahead_c))
            if early and chunk + 1 < len(chunks):
                x, dx = turn_to(t)
                for other in range(2):
                    to_r = 2 * x + (1 - par if other else par)
                    there = (to_r != r) | (c != 0)
                    if chunk > EARLY_FROM:
                        there = there & (to_r != ahead_r)
                    send_tile(chunk + 1, to_r, jnp.int32(0), there)
                if chunk == EARLY_FROM:
                    there = (x == ahead_r // 2) & jnp.logical_not(is_ahead)
                    send_tile(len(chunks) - 1, jnp.int32(ahead_r), jnp.int32(ahead_c), there)
            return carry

        lax.fori_loop(0, chips, body, 0)

    params[0].wait()
    for dw in range(3):
        w1own[dw] = jnp.concatenate([w1s[1, dw], w1s[0, dw]], axis=1)
    w1own[3] = jnp.concatenate([w1s[2, 0], w1s[2, 1]], axis=1)
    w1own[4] = jnp.concatenate([w1s[2, 2], jnp.zeros_like(w1s[2, 2])], axis=1)
    w1all[r // 2, par, c] = w1own[...]

    for copy in loads[0]:
        copy.wait()
    pack_rows(turn_to(0)[0], *groups[0][0])
    pl.semaphore_wait(barrier, sources - 1)

    def send_weights():
        def body(k, carry):
            to_r = lax.rem(r + 2 * k, n_rows)
            for kc in range(n_cols):

                def copy(kc=kc):
                    pltpu.make_async_remote_copy(
                        src_ref=w1own,
                        dst_ref=w1all.at[r // 2, par, c],
                        send_sem=wsend_sem,
                        recv_sem=wrecv_sem,
                        device_id=device(to_r, to_cs[kc]),
                        device_id_type=MESH,
                    ).start()

                pl.when(k < chips)(copy) if kc == 0 else copy()
            return carry

        lax.fori_loop(1, chips + 1, body, 0)

    def pack_and_send(t, carry):
        pl.when(t < chips - 1)(lambda: pack_rows(turn_to(t + 1)[0], *groups[0][0]))
        there = turn_to(t)[0] == ahead_r // 2

        @pl.when(there)
        def _():
            loads[1][ahead_r % 2].wait()
            pack_rows(ahead_r // 2, *groups[1][ahead_r % 2])

        send_chip(0, t)
        send_tile(1, jnp.int32(ahead_r), jnp.int32(ahead_c), there & jnp.logical_not(is_ahead))
        pl.when(t == 1)(send_weights)
        return carry

    lax.fori_loop(0, chips, pack_and_send, 0)

    for g in range(1, EARLY_FROM + 1):
        pack(g)
    for chunk in range(1, len(chunks)):
        if chunk >= EARLY_FROM and chunk + 1 < len(groups):
            pack(chunk + 1)
        send_chunk(chunk)

    def wait_bytes(ref, sem):
        pltpu.make_async_copy(ref, ref, sem).wait()

    w1_bytes = recv.at[0 : sources // 2 - 1, 0, 0:5]
    wait_bytes(w1_bytes, wrecv_sem)
    wait_bytes(w1_bytes, wsend_sem)
    partner = device(r + 1 - 2 * par, c)
    w_swap = pltpu.make_async_remote_copy(
        src_ref=w1all.at[:, par],
        dst_ref=w1all.at[:, par],
        send_sem=wswap_send_sem,
        recv_sem=wswap_recv_sem,
        device_id=partner,
        device_id_type=MESH,
    )
    w_swap.start()

    def own_rows(chunk):
        rows, where, _ = chunks[chunk]
        src, dst = where(r)

        def copy(count, src_j, dst_j):
            for h in range(rows):
                recv[me, dst + h, pl.ds(dst_j, count)] = packed[src + h, pl.ds(src_j, count)]

        pl.when(at_edge)(lambda: copy(win_j - 1, tile_j * c - 1 + own_j, own_j))
        pl.when(jnp.logical_not(at_edge))(lambda: copy(win_j, tile_j * c - 1, 0))

    for chunk in range(3):
        own_rows(chunk)
    pl.when(jnp.logical_not(no_outer))(lambda: own_rows(3))

    zero_row = jnp.zeros((win_j, 2, 2 * images), BF16)
    zero_col = jnp.zeros((tile_h + 2, 2, 2 * images), BF16)

    def clear(s, carry):
        recv[s, last * (1 - par)] = zero_row
        return carry

    def clear_outer(s, carry):
        recv[s, (last - 1) * par] = zero_row
        recv[s, (last - 1) * par + 1] = zero_row
        return carry

    def clear_edge(s, carry):
        recv[s, pl.ds(3 * par, tile_h + 2), (win_j - 1) * (1 - own_j)] = zero_col
        return carry

    lax.fori_loop(0, sources, clear, 0)
    pl.when(no_outer)(lambda: (lax.fori_loop(0, sources, clear_outer, 0), None)[1])
    pl.when(at_edge)(lambda: (lax.fori_loop(0, sources, clear_edge, 0), None)[1])

    low = lax.broadcasted_iota(jnp.int32, (chans, 2 * chans), 1) < chans

    def spread(wt, u, v, dw):
        ur, vr = pltpu.roll(u, chans, 1), pltpu.roll(v, chans, 1)
        zero = jnp.zeros_like(u)
        tiles = (jnp.where(low, ur, zero), u, jnp.where(low, v, ur), jnp.where(low, zero, vr))
        for k, tile in enumerate(tiles):
            tile = tile.astype(BF16)
            for b in range(2):
                wt[dw + b, k * chans : (k + 1) * chans, b * 2 * chans : (b + 1) * 2 * chans] = tile

    def blank(wt):
        zero = jnp.zeros((4 * chans, 2 * chans), BF16)
        wt[3, :, 0 : 2 * chans] = zero
        wt[0, :, 2 * chans : 4 * chans] = zero

    for copy in params[1:]:
        copy.wait()
    blank(wt1)
    blank(wt2)
    for dw in range(3):
        w = [w2s[dh, dw].astype(F32) for dh in range(3)]
        spread(
            wt2,
            jnp.concatenate([w[1], w[0]], axis=1),
            jnp.concatenate([w[2], jnp.zeros_like(w[2])], axis=1),
            dw,
        )
    bias1[...] = jnp.concatenate([b1s[...]] * 4, axis=1)
    bias2[...] = jnp.concatenate([b2s[...]] * 4, axis=1)

    def arrived(chunk):
        def wait(count):
            wait_bytes(recv.at[0 : sources - 1, 0 : chunks[chunk][0], 0:count], recv_sem.at[chunk])

        pl.when(at_edge)(lambda: wait(win_j - 1))
        pl.when(jnp.logical_not(at_edge))(lambda: wait(win_j))

    arrived(0)
    give = tile_h - (tile_h - 3) * par
    land = tile_h + 2 - (tile_h + 1) * (1 - par)
    swap = pltpu.make_async_remote_copy(
        src_ref=recv.at[:, pl.ds(give, 2)],
        dst_ref=recv.at[:, pl.ds(land, 2)],
        send_sem=swap_send_sem,
        recv_sem=swap_recv_sem,
        device_id=partner,
        device_id_type=MESH,
    )
    swap.start()

    w_swap.wait()
    u = [w1all[:, :, :, k].reshape(chans, 2 * chans).astype(F32) for k in range(5)]
    for dw in range(3):
        v = (u[3], pltpu.roll(u[3], chans, 1), u[4])[dw]
        spread(wt1, u[dw], jnp.where(low, v, 0.0), dw)

    x_pairs, z_pairs = xmat.shape[0], ymat.shape[0]
    o_pairs = z_pairs - 1

    def nth(n, count):
        return (count - 1) * (1 - par) + n * (2 * par - 1)

    def turn_one(n, carry):
        i = nth(n, x_pairs)

        def put(j, value):
            xmat[i, j] = value

        turn(recv, i, put)
        return carry

    def first_one(n, carry):
        i = nth(n, z_pairs)
        fill = jnp.where(n == 0, 1 - par, 2)
        out_of = jnp.where(n == z_pairs - 1, jnp.where(r == 0, 0, jnp.where(r == n_rows - 1, 1, 2)), 2)
        blank_a = jnp.where(fill < 2, fill, out_of)
        first((xmat.at[i], xmat.at[i + 1]), lambda dw: wt1[dw], bias1[...], ymat.at[i], blank_a)
        return carry

    def second_one(n, carry):
        i = nth(n, o_pairs)
        second((ymat.at[i], ymat.at[i + 1]), lambda dw: wt2[dw], bias2[...], out.at[pl.ds(2 * i, 2)])
        return carry

    def stage(s, carry):
        @pl.when(s == 0)
        def _():
            swap.wait()

        for k in range(1, 4):
            there = s == k
            if k == 3:
                there = there & jnp.logical_not(no_outer)
            pl.when(there)(lambda k=k: arrived(k))

        for ends, one in ((TURNS, turn_one), (FIRSTS, first_one), (SECONDS, second_one)):
            lax.fori_loop(step(s, (0, *ends[:-1])), step(s, ends), one, 0)
        return carry

    lax.fori_loop(0, 4, stage, 0)

    per_edge = n_rows * 2
    for chunk in range(4):
        rows = chunks[chunk][0]
        n_r = n_rows - 2 if chunk == 3 else n_rows
        counts = (n_r * 2, n_r * (n_cols - 2))

        def drain(edge_n, inner_n, rows=rows, chunk=chunk):
            wait_bytes(recv.at[0:edge_n, 0:rows, 0 : win_j - 1], send_sem.at[chunk])
            wait_bytes(recv.at[0:inner_n, 0:rows, 0:win_j], send_sem.at[chunk])

        def drain_own(chunk=chunk, counts=counts, drain=drain):
            pl.when(at_edge)(lambda: drain(counts[0] - 1, counts[1]))
            pl.when(jnp.logical_not(at_edge))(lambda: drain(counts[0], counts[1] - 1))

        if chunk == 3:
            pl.when(no_outer)(lambda: drain(*counts))
            pl.when(jnp.logical_not(no_outer))(drain_own)
        else:
            drain_own()


def tail_kernel(tile, ymat, wt2, bias2, out_hbm, o_new, sem):
    par = lax.rem(lax.axis_index("model"), 2)
    rows = out_hbm.shape[0]
    o_pairs = ymat.shape[0] - 1
    late = (rows - 2) * par
    here = 2 * (1 - par)

    cut = out_hbm.shape[1] // 2

    def start(k, carry):
        for part in (pl.ds(0, cut), pl.ds(cut, out_hbm.shape[1] - cut)):
            pltpu.make_async_copy(tile.at[par + k, part], out_hbm.at[k, part], sem.at[0]).start()
        return carry

    lax.fori_loop(here, here + rows - 2, start, 0)
    i = (o_pairs - 1) * par
    second((ymat.at[i], ymat.at[i + 1]), lambda dw: wt2[dw], bias2[...], o_new)
    for k in range(2):
        for part in (pl.ds(0, cut), pl.ds(cut, out_hbm.shape[1] - cut)):
            pltpu.make_async_copy(o_new.at[k, part], out_hbm.at[late + k, part], sem.at[1]).start()
    pltpu.make_async_copy(tile.at[0 : rows - 2], out_hbm.at[0 : rows - 2], sem.at[0]).wait()
    pltpu.make_async_copy(o_new, out_hbm.at[pl.ds(late, 2)], sem.at[1]).wait()


def solution(mesh):
    n_rows = mesh.shape["model"]
    n_cols = mesh.shape["cols"]

    def run_local(x_in, w_conv1, b_conv1, w_conv2, b_conv2):
        images, height, width, own_chans = x_in.shape
        sources = n_rows * n_cols
        chans = own_chans * sources
        pairs = width // 2
        tile_h, tile_j = height // n_rows, pairs // n_cols
        win_j = tile_j + 2
        x_pairs, z_pairs = (tile_h + 5) // 2, (tile_h + 3) // 2
        x_t = jnp.transpose(x_in, (1, 2, 3, 0)).reshape(n_rows // 2, 2 * tile_h, pairs, 2, own_chans, images)
        args = (x_t, w_conv1, b_conv1.reshape(1, chans), w_conv2, b_conv2.reshape(1, chans))
        hbm = pl.BlockSpec(memory_space=pltpu.HBM)
        vmem = pl.BlockSpec(memory_space=pltpu.VMEM)
        kept = (
            pltpu.VMEM((2 * (z_pairs - 1), tile_j, 2, images, chans), F32),
            pltpu.VMEM((z_pairs, win_j - 1, 2, images, 2 * chans), BF16),
            pltpu.VMEM((4, 4 * chans, 4 * chans), BF16),
            pltpu.VMEM((1, 4 * chans), F32),
        )
        state = pl.pallas_call(
            functools.partial(conv_kernel, n_rows, n_cols),
            out_shape=kept,
            in_specs=[hbm] * 5,
            out_specs=[vmem] * len(kept),
            scratch_shapes=[
                pltpu.VMEM((sources, 2 * x_pairs, win_j, own_chans, 2 * images), BF16),
                pltpu.VMEM((x_pairs, win_j, 2, images, 2 * chans), BF16),
                pltpu.VMEM((4, 4 * chans, 4 * chans), BF16),
                pltpu.VMEM((1, 4 * chans), F32),
                pltpu.VMEM((n_rows // 2, 2 * tile_h, pairs, 2, own_chans, images), BF16),
                pltpu.VMEM((height, pairs, own_chans, 2 * images), BF16),
                pltpu.VMEM((3, 3, own_chans, chans), BF16),
                pltpu.VMEM((5, own_chans, 2 * chans), BF16),
                pltpu.VMEM((n_rows // 2, 2, n_cols, 5, own_chans, 2 * chans), BF16),
                pltpu.VMEM((3, 3, chans, chans), BF16),
                pltpu.VMEM((1, chans), F32),
                pltpu.VMEM((1, chans), F32),
                pltpu.SemaphoreType.DMA((3, 2)),
                pltpu.SemaphoreType.DMA((4,)),
                pltpu.SemaphoreType.DMA((4,)),
                pltpu.SemaphoreType.DMA((4,)),
            ]
            + [pltpu.SemaphoreType.DMA] * 6,
            compiler_params=pltpu.CompilerParams(
                collective_id=0, has_side_effects=True, vmem_limit_bytes=24 << 20
            ),
            name="conv",
        )(*(pltpu.with_memory_space_constraint(a, pltpu.HBM) for a in args))
        out = pl.pallas_call(
            tail_kernel,
            out_shape=jax.ShapeDtypeStruct((tile_h, tile_j, 2, images, chans), F32),
            in_specs=[vmem] * len(kept),
            out_specs=pl.BlockSpec(memory_space=pl.ANY),
            scratch_shapes=[
                pltpu.VMEM((2, tile_j, 2, images, chans), F32),
                pltpu.SemaphoreType.DMA((2,)),
            ],
            compiler_params=pltpu.CompilerParams(vmem_limit_bytes=8 << 20),
            name="tail",
        )(*state)
        out = out.reshape(tile_h, 2 * tile_j, images, chans)
        return jnp.transpose(out, (2, 0, 1, 3))

    group = ("model", "cols")
    return jax.shard_map(
        run_local,
        mesh=mesh,
        in_specs=(P("data", None, None, group), P(None, None, group, None), P(), P(), P()),
        out_specs=P("data", "model", "cols", None),
        check_vma=False,
    )
```

```python
import functools

import jax
import jax.numpy as jnp
from jax import lax
from jax.experimental import pallas as pl
from jax.experimental.pallas import tpu as pltpu
from jax.sharding import PartitionSpec as P

MESH = pl.DeviceIdType.MESH
BF16 = jnp.bfloat16
F32 = jnp.float32
CHUNK_ROWS = (2, 3, 2)
TURNS, FIRSTS, SECONDS = (2, 4, 5, 6), (1, 3, 4, 5), (0, 2, 3, 3)
EARLY_FROM = 1
AHEAD = (1, 0)
CHIPS_ALONG = (3, 1, 0, 2)
CHIP_ORDER = tuple((other, dy) for other in (0, 1) for dy in (0, 1, -1, 2))


def turn(recv, i, put):
    sources, _, win_j, own_chans, lanes = recv.shape
    chans = sources * own_chans
    for j in range(win_j):
        top = recv[:, 2 * i, j].reshape(chans, lanes)
        under = recv[:, 2 * i + 1, j].reshape(chans, lanes)
        put(j, jnp.concatenate([top, under], axis=0).T.reshape(2, lanes // 2, 2 * chans))


def blocks(pairs, weights, count):
    acc = None
    for dw in range(4):
        parts = [view[dw // 2 : dw // 2 + count, dw % 2] for view in pairs]
        lhs = jnp.concatenate([p.reshape(count * p.shape[1], p.shape[2]) for p in parts], axis=1)
        term = jnp.dot(lhs, weights(dw), preferred_element_type=F32)
        acc = term if acc is None else acc + term
    return acc


def first(pairs, weights, bias, y_row, blank_a):
    count, _, images, lanes = y_row.shape
    c = lax.axis_index("cols")
    row = lax.rem(lax.broadcasted_iota(jnp.int32, (1, 2 * lanes), 1), lanes) // (lanes // 2)
    act = jnp.maximum(blocks(pairs, weights, count) + bias, 0.0)
    act = jnp.where(row != blank_a, act, 0.0).astype(BF16)
    for b in range(2):
        y_row[:, b] = act[:, b * lanes : (b + 1) * lanes].reshape(count, images, lanes)
    blank = jnp.zeros((images, lanes), BF16)

    @pl.when(c == 0)
    def _():
        y_row[0, 0] = blank

    @pl.when(c == lax.axis_size("cols") - 1)
    def _():
        y_row[count - 1, 1] = blank


def second(pairs, weights, bias, out_pair):
    _, count, _, images, chans = out_pair.shape
    res = blocks(pairs, weights, count) + bias
    for b in range(2):
        for a in range(2):
            at = (2 * b + a) * chans
            out_pair[a, :, b] = res[:, at : at + chans].reshape(count, images, chans)


def conv_kernel(
    n_rows,
    n_cols,
    x_hbm,
    w1_hbm,
    b1_hbm,
    w2_hbm,
    b2_hbm,
    out,
    ymat,
    wt2,
    bias2,
    recv,
    xmat,
    wt1,
    bias1,
    xs,
    packed,
    w1s,
    w1own,
    w1all,
    w2s,
    b1s,
    b2s,
    load_sem,
    par_sem,
    send_sem,
    recv_sem,
    wsend_sem,
    wrecv_sem,
    swap_send_sem,
    swap_recv_sem,
    wswap_send_sem,
    wswap_recv_sem,
):
    chip_h, pairs = xs.shape[1:3]
    images = xs.shape[-1]
    tile_h, tile_j = chip_h // 2, pairs // n_cols
    win_j = tile_j + 2
    sources = n_rows * n_cols
    r, c = lax.axis_index("model"), lax.axis_index("cols")
    par = lax.rem(r, 2)
    me = r * n_cols + c
    chans = recv.shape[0] * 2

    tops = [tile_h - sum(CHUNK_ROWS[: k + 1]) for k in range(len(CHUNK_ROWS))]
    groups = (
        ((tops[0], chip_h - tops[0]),),
        *(((k, k + n), (chip_h - k - n, chip_h - k)) for k, n in zip(tops[1:], CHUNK_ROWS[1:])),
    )
    loads = []
    for g, spans in enumerate(groups):
        loads.append(
            [
                pltpu.make_async_copy(x_hbm.at[:, lo:hi], xs.at[:, lo:hi], load_sem.at[g, n])
                for n, (lo, hi) in enumerate(spans)
            ]
        )
    for copies in loads:
        for copy in copies:
            copy.start()
    params = [
        pltpu.make_async_copy(src, dst, par_sem.at[s])
        for s, (src, dst) in enumerate(((w1_hbm, w1s), (w2_hbm, w2s), (b1_hbm, b1s), (b2_hbm, b2s)))
    ]
    for copy in params:
        copy.start()

    barrier = pltpu.get_barrier_semaphore()
    to_cs = [lax.rem(c + k, n_cols) for k in range(n_cols)]

    def device(to_r, to_c):
        return {"model": to_r, "cols": to_c}

    to_rs = [lax.rem(r + k, n_rows) for k in range(n_rows)]
    for kr, kc in sorted(
        ((kr, kc) for kr in range(n_rows) for kc in range(n_cols) if kr or kc),
        key=lambda k: (k[1] not in (1, 2), k[0] not in (2, 3, 4, 5), k[1] == 2, k[0] < 4, -min(k[0], n_rows - k[0])),
    ):
        pl.semaphore_signal(barrier, inc=1, device_id=device(to_rs[kr], to_cs[kc]), device_id_type=MESH)

    ahead_r, ahead_c = AHEAD
    is_ahead = (r == ahead_r) & (c == ahead_c)

    def pack_rows(x, lo, hi):
        rows = hi - lo
        left, right = (xs[x, lo:hi, :, p].reshape(rows * pairs * 2, images) for p in range(2))
        both = jnp.concatenate([left, right], axis=1)
        packed[pl.ds(chip_h * x + lo, rows)] = both.reshape(rows, pairs, 2, 2 * images)

    def pack(g):
        for n, copy in enumerate(loads[g]):
            if (g, n) != (1, ahead_r % 2):
                copy.wait()

        def body(x, carry):
            for n, (lo, hi) in enumerate(groups[g]):
                if (g, n) == (1, ahead_r % 2):
                    pl.when(x != ahead_r // 2)(lambda lo=lo, hi=hi: pack_rows(x, lo, hi))
                else:
                    pack_rows(x, lo, hi)
            return carry

        lax.fori_loop(0, n_rows // 2, body, 0)

    last = tile_h + 4

    def rows_of(offset, count):
        def where(to_r):
            q = lax.rem(to_r, 2)
            src = tile_h * to_r + offset + (tile_h - count - 2 * offset) * q
            dst = offset + 2 + (last - count - 2 * offset - 3) * q
            return src, dst

        return where

    chunks = (
        *((n, rows_of(k, n), False) for k, n in zip(tops, CHUNK_ROWS)),
        (2, rows_of(-2, 2), True),
    )
    no_outer = (r == 0) | (r == n_rows - 1)
    at_edge = (c == 0) | (c == n_cols - 1)
    own_j = c == 0
    own_j = own_j.astype(jnp.int32)

    def send_tile(chunk, to_r, to_c, there):
        rows, where, is_outer = chunks[chunk]
        src, dst = where(to_r)
        skip = (to_c == 0).astype(jnp.int32)
        edge = (to_c == 0) | (to_c == n_cols - 1)
        if is_outer:
            there = there & (to_r > 0) & (to_r < n_rows - 1)

        def copy(count, src_j, dst_j):
            pltpu.make_async_remote_copy(
                src_ref=packed.at[pl.ds(src, rows), pl.ds(src_j, count)],
                dst_ref=recv.at[me, pl.ds(dst, rows), pl.ds(dst_j, count)],
                send_sem=send_sem.at[chunk],
                recv_sem=recv_sem.at[chunk],
                device_id=device(to_r, to_c),
                device_id_type=MESH,
            ).start()

        pl.when(there & edge)(lambda: copy(win_j - 1, tile_j * to_c - 1 + skip, skip))
        pl.when(there & jnp.logical_not(edge))(lambda: copy(win_j, tile_j * to_c - 1, 0))

    chips = n_rows // 2

    def step(t, table):
        value = jnp.int32(table[-1])
        for k, entry in enumerate(table[:-1]):
            value = jnp.where(t == k, entry, value)
        return value

    def turn_to(t):
        dx = step(t, CHIPS_ALONG)
        return lax.rem(r // 2 + dx, chips), dx

    def send_chip(chunk, t, where=None):
        x, dx = turn_to(t)
        way = 1 - 2 * lax.rem(par + t, 2)
        for other, dy in CHIP_ORDER:
            to_r = 2 * x + (1 - par if other else par)
            to_c = lax.rem(c + way * dy + n_cols, n_cols)
            there = True
            if not other and dy == 0:
                there = dx > 0
            if where is not None:
                there = there & where(to_r, to_c)
            send_tile(chunk, to_r, to_c, there)

    def send_chunk(chunk):
        early = EARLY_FROM <= chunk

        def body(t, carry):
            if chunk > EARLY_FROM:
                send_chip(chunk, t, lambda to_r, to_c: to_c > 0)
            else:
                send_chip(chunk, t, lambda to_r, to_c: (to_r != ahead_r) | (to_c != ahead_c))
            if early and chunk + 1 < len(chunks):
                x, dx = turn_to(t)
                for other in range(2):
                    to_r = 2 * x + (1 - par if other else par)
                    there = (to_r != r) | (c != 0)
                    if chunk > EARLY_FROM:
                        there = there & (to_r != ahead_r)
                    send_tile(chunk + 1, to_r, jnp.int32(0), there)
                if chunk == EARLY_FROM:
                    there = (x == ahead_r // 2) & jnp.logical_not(is_ahead)
                    send_tile(len(chunks) - 1, jnp.int32(ahead_r), jnp.int32(ahead_c), there)
            return carry

        lax.fori_loop(0, chips, body, 0)

    params[0].wait()
    for dw in range(3):
        w1own[dw] = jnp.concatenate([w1s[1, dw], w1s[0, dw]], axis=1)
    w1own[3] = jnp.concatenate([w1s[2, 0], w1s[2, 1]], axis=1)
    w1own[4] = jnp.concatenate([w1s[2, 2], jnp.zeros_like(w1s[2, 2])], axis=1)
    w1all[r // 2, par, c] = w1own[...]

    for copy in loads[0]:
        copy.wait()
    pack_rows(turn_to(0)[0], *groups[0][0])
    pl.semaphore_wait(barrier, sources - 1)

    def send_weights():
        for kr in range(0, n_rows, 2):
            for kc in range(n_cols):
                if kr or kc:
                    pltpu.make_async_remote_copy(
                        src_ref=w1own,
                        dst_ref=w1all.at[r // 2, par, c],
                        send_sem=wsend_sem,
                        recv_sem=wrecv_sem,
                        device_id=device(to_rs[kr], to_cs[kc]),
                        device_id_type=MESH,
                    ).start()

    def pack_and_send(t, carry):
        pl.when(t < chips - 1)(lambda: pack_rows(turn_to(t + 1)[0], *groups[0][0]))
        there = turn_to(t)[0] == ahead_r // 2

        @pl.when(there)
        def _():
            loads[1][ahead_r % 2].wait()
            pack_rows(ahead_r // 2, *groups[1][ahead_r % 2])

        send_chip(0, t)
        send_tile(1, jnp.int32(ahead_r), jnp.int32(ahead_c), there & jnp.logical_not(is_ahead))
        pl.when(t == 1)(send_weights)
        return carry

    lax.fori_loop(0, chips, pack_and_send, 0)

    for g in range(1, EARLY_FROM + 1):
        pack(g)
    for chunk in range(1, len(chunks)):
        if chunk >= EARLY_FROM and chunk + 1 < len(groups):
            pack(chunk + 1)
        send_chunk(chunk)

    def wait_bytes(ref, sem):
        pltpu.make_async_copy(ref, ref, sem).wait()

    w1_bytes = recv.at[0 : sources // 2 - 1, 0, 0:5]
    wait_bytes(w1_bytes, wrecv_sem)
    wait_bytes(w1_bytes, wsend_sem)
    partner = device(r + 1 - 2 * par, c)
    w_swap = pltpu.make_async_remote_copy(
        src_ref=w1all.at[:, par],
        dst_ref=w1all.at[:, par],
        send_sem=wswap_send_sem,
        recv_sem=wswap_recv_sem,
        device_id=partner,
        device_id_type=MESH,
    )
    w_swap.start()

    def own_rows(chunk):
        rows, where, _ = chunks[chunk]
        src, dst = where(r)

        def copy(count, src_j, dst_j):
            for h in range(rows):
                recv[me, dst + h, pl.ds(dst_j, count)] = packed[src + h, pl.ds(src_j, count)]

        pl.when(at_edge)(lambda: copy(win_j - 1, tile_j * c - 1 + own_j, own_j))
        pl.when(jnp.logical_not(at_edge))(lambda: copy(win_j, tile_j * c - 1, 0))

    for chunk in range(3):
        own_rows(chunk)
    pl.when(jnp.logical_not(no_outer))(lambda: own_rows(3))

    zero_row = jnp.zeros((win_j, 2, 2 * images), BF16)
    zero_col = jnp.zeros((tile_h + 2, 2, 2 * images), BF16)

    def clear(s, carry):
        recv[s, last * (1 - par)] = zero_row
        return carry

    def clear_outer(s, carry):
        recv[s, (last - 1) * par] = zero_row
        recv[s, (last - 1) * par + 1] = zero_row
        return carry

    def clear_edge(s, carry):
        recv[s, pl.ds(3 * par, tile_h + 2), (win_j - 1) * (1 - own_j)] = zero_col
        return carry

    lax.fori_loop(0, sources, clear, 0)
    pl.when(no_outer)(lambda: (lax.fori_loop(0, sources, clear_outer, 0), None)[1])
    pl.when(at_edge)(lambda: (lax.fori_loop(0, sources, clear_edge, 0), None)[1])

    low = lax.broadcasted_iota(jnp.int32, (chans, 2 * chans), 1) < chans

    def spread(wt, u, v, dw):
        ur, vr = pltpu.roll(u, chans, 1), pltpu.roll(v, chans, 1)
        zero = jnp.zeros_like(u)
        tiles = (jnp.where(low, ur, zero), u, jnp.where(low, v, ur), jnp.where(low, zero, vr))
        for k, tile in enumerate(tiles):
            tile = tile.astype(BF16)
            for b in range(2):
                wt[dw + b, k * chans : (k + 1) * chans, b * 2 * chans : (b + 1) * 2 * chans] = tile

    def blank(wt):
        zero = jnp.zeros((4 * chans, 2 * chans), BF16)
        wt[3, :, 0 : 2 * chans] = zero
        wt[0, :, 2 * chans : 4 * chans] = zero

    for copy in params[1:]:
        copy.wait()
    blank(wt1)
    blank(wt2)
    for dw in range(3):
        w = [w2s[dh, dw].astype(F32) for dh in range(3)]
        spread(
            wt2,
            jnp.concatenate([w[1], w[0]], axis=1),
            jnp.concatenate([w[2], jnp.zeros_like(w[2])], axis=1),
            dw,
        )
    bias1[...] = jnp.concatenate([b1s[...]] * 4, axis=1)
    bias2[...] = jnp.concatenate([b2s[...]] * 4, axis=1)

    def arrived(chunk):
        def wait(count):
            wait_bytes(recv.at[0 : sources - 1, 0 : chunks[chunk][0], 0:count], recv_sem.at[chunk])

        pl.when(at_edge)(lambda: wait(win_j - 1))
        pl.when(jnp.logical_not(at_edge))(lambda: wait(win_j))

    arrived(0)
    give = tile_h - (tile_h - 3) * par
    land = tile_h + 2 - (tile_h + 1) * (1 - par)
    swap = pltpu.make_async_remote_copy(
        src_ref=recv.at[:, pl.ds(give, 2)],
        dst_ref=recv.at[:, pl.ds(land, 2)],
        send_sem=swap_send_sem,
        recv_sem=swap_recv_sem,
        device_id=partner,
        device_id_type=MESH,
    )
    swap.start()

    w_swap.wait()
    u = [w1all[:, :, :, k].reshape(chans, 2 * chans).astype(F32) for k in range(5)]
    for dw in range(3):
        v = (u[3], pltpu.roll(u[3], chans, 1), u[4])[dw]
        spread(wt1, u[dw], jnp.where(low, v, 0.0), dw)

    x_pairs, z_pairs = xmat.shape[0], ymat.shape[0]
    o_pairs = z_pairs - 1

    def nth(n, count):
        return (count - 1) * (1 - par) + n * (2 * par - 1)

    def turn_one(n, carry):
        i = nth(n, x_pairs)

        def put(j, value):
            xmat[i, j] = value

        turn(recv, i, put)
        return carry

    def first_one(n, carry):
        i = nth(n, z_pairs)
        fill = jnp.where(n == 0, 1 - par, 2)
        out_of = jnp.where(n == z_pairs - 1, jnp.where(r == 0, 0, jnp.where(r == n_rows - 1, 1, 2)), 2)
        blank_a = jnp.where(fill < 2, fill, out_of)
        first((xmat.at[i], xmat.at[i + 1]), lambda dw: wt1[dw], bias1[...], ymat.at[i], blank_a)
        return carry

    def second_one(n, carry):
        i = nth(n, o_pairs)
        second((ymat.at[i], ymat.at[i + 1]), lambda dw: wt2[dw], bias2[...], out.at[pl.ds(2 * i, 2)])
        return carry

    def stage(s, carry):
        @pl.when(s == 0)
        def _():
            swap.wait()

        for k in range(1, 4):
            there = s == k
            if k == 3:
                there = there & jnp.logical_not(no_outer)
            pl.when(there)(lambda k=k: arrived(k))

        for ends, one in ((TURNS, turn_one), (FIRSTS, first_one), (SECONDS, second_one)):
            lax.fori_loop(step(s, (0, *ends[:-1])), step(s, ends), one, 0)
        return carry

    lax.fori_loop(0, 4, stage, 0)

    per_edge = n_rows * 2
    for chunk in range(4):
        rows = chunks[chunk][0]
        n_r = n_rows - 2 if chunk == 3 else n_rows
        counts = (n_r * 2, n_r * (n_cols - 2))

        def drain(edge_n, inner_n, rows=rows, chunk=chunk):
            wait_bytes(recv.at[0:edge_n, 0:rows, 0 : win_j - 1], send_sem.at[chunk])
            wait_bytes(recv.at[0:inner_n, 0:rows, 0:win_j], send_sem.at[chunk])

        def drain_own(chunk=chunk, counts=counts, drain=drain):
            pl.when(at_edge)(lambda: drain(counts[0] - 1, counts[1]))
            pl.when(jnp.logical_not(at_edge))(lambda: drain(counts[0], counts[1] - 1))

        if chunk == 3:
            pl.when(no_outer)(lambda: drain(*counts))
            pl.when(jnp.logical_not(no_outer))(drain_own)
        else:
            drain_own()


def tail_kernel(tile, ymat, wt2, bias2, out_hbm, o_new, sem):
    par = lax.rem(lax.axis_index("model"), 2)
    rows = out_hbm.shape[0]
    o_pairs = ymat.shape[0] - 1
    late = (rows - 2) * par
    here = 2 * (1 - par)

    cut = out_hbm.shape[1] // 2

    def start(k, carry):
        for part in (pl.ds(0, cut), pl.ds(cut, out_hbm.shape[1] - cut)):
            pltpu.make_async_copy(tile.at[par + k, part], out_hbm.at[k, part], sem.at[0]).start()
        return carry

    lax.fori_loop(here, here + rows - 2, start, 0)
    i = (o_pairs - 1) * par
    second((ymat.at[i], ymat.at[i + 1]), lambda dw: wt2[dw], bias2[...], o_new)
    for k in range(2):
        for part in (pl.ds(0, cut), pl.ds(cut, out_hbm.shape[1] - cut)):
            pltpu.make_async_copy(o_new.at[k, part], out_hbm.at[late + k, part], sem.at[1]).start()
    pltpu.make_async_copy(tile.at[0 : rows - 2], out_hbm.at[0 : rows - 2], sem.at[0]).wait()
    pltpu.make_async_copy(o_new, out_hbm.at[pl.ds(late, 2)], sem.at[1]).wait()


def solution(mesh):
    n_rows = mesh.shape["model"]
    n_cols = mesh.shape["cols"]

    def run_local(x_in, w_conv1, b_conv1, w_conv2, b_conv2):
        images, height, width, own_chans = x_in.shape
        sources = n_rows * n_cols
        chans = own_chans * sources
        pairs = width // 2
        tile_h, tile_j = height // n_rows, pairs // n_cols
        win_j = tile_j + 2
        x_pairs, z_pairs = (tile_h + 5) // 2, (tile_h + 3) // 2
        x_t = jnp.transpose(x_in, (1, 2, 3, 0)).reshape(n_rows // 2, 2 * tile_h, pairs, 2, own_chans, images)
        args = (x_t, w_conv1, b_conv1.reshape(1, chans), w_conv2, b_conv2.reshape(1, chans))
        hbm = pl.BlockSpec(memory_space=pltpu.HBM)
        vmem = pl.BlockSpec(memory_space=pltpu.VMEM)
        kept = (
            pltpu.VMEM((2 * (z_pairs - 1), tile_j, 2, images, chans), F32),
            pltpu.VMEM((z_pairs, win_j - 1, 2, images, 2 * chans), BF16),
            pltpu.VMEM((4, 4 * chans, 4 * chans), BF16),
            pltpu.VMEM((1, 4 * chans), F32),
        )
        state = pl.pallas_call(
            functools.partial(conv_kernel, n_rows, n_cols),
            out_shape=kept,
            in_specs=[hbm] * 5,
            out_specs=[vmem] * len(kept),
            scratch_shapes=[
                pltpu.VMEM((sources, 2 * x_pairs, win_j, own_chans, 2 * images), BF16),
                pltpu.VMEM((x_pairs, win_j, 2, images, 2 * chans), BF16),
                pltpu.VMEM((4, 4 * chans, 4 * chans), BF16),
                pltpu.VMEM((1, 4 * chans), F32),
                pltpu.VMEM((n_rows // 2, 2 * tile_h, pairs, 2, own_chans, images), BF16),
                pltpu.VMEM((height, pairs, own_chans, 2 * images), BF16),
                pltpu.VMEM((3, 3, own_chans, chans), BF16),
                pltpu.VMEM((5, own_chans, 2 * chans), BF16),
                pltpu.VMEM((n_rows // 2, 2, n_cols, 5, own_chans, 2 * chans), BF16),
                pltpu.VMEM((3, 3, chans, chans), BF16),
                pltpu.VMEM((1, chans), F32),
                pltpu.VMEM((1, chans), F32),
                pltpu.SemaphoreType.DMA((3, 2)),
                pltpu.SemaphoreType.DMA((4,)),
                pltpu.SemaphoreType.DMA((4,)),
                pltpu.SemaphoreType.DMA((4,)),
            ]
            + [pltpu.SemaphoreType.DMA] * 6,
            compiler_params=pltpu.CompilerParams(
                collective_id=0, has_side_effects=True, vmem_limit_bytes=24 << 20
            ),
            name="conv",
        )(*(pltpu.with_memory_space_constraint(a, pltpu.HBM) for a in args))
        out = pl.pallas_call(
            tail_kernel,
            out_shape=jax.ShapeDtypeStruct((tile_h, tile_j, 2, images, chans), F32),
            in_specs=[vmem] * len(kept),
            out_specs=pl.BlockSpec(memory_space=pl.ANY),
            scratch_shapes=[
                pltpu.VMEM((2, tile_j, 2, images, chans), F32),
                pltpu.SemaphoreType.DMA((2,)),
            ],
            compiler_params=pltpu.CompilerParams(vmem_limit_bytes=8 << 20),
            name="tail",
        )(*state)
        out = out.reshape(tile_h, 2 * tile_j, images, chans)
        return jnp.transpose(out, (2, 0, 1, 3))

    group = ("model", "cols")
    return jax.shard_map(
        run_local,
        mesh=mesh,
        in_specs=(P("data", None, None, group), P(None, None, group, None), P(), P(), P()),
        out_specs=P("data", "model", "cols", None),
        check_vma=False,
    )
```

```python
import functools

import jax
import jax.numpy as jnp
from jax import lax
from jax.experimental import pallas as pl
from jax.experimental.pallas import tpu as pltpu
from jax.sharding import PartitionSpec as P

MESH = pl.DeviceIdType.MESH
BF16 = jnp.bfloat16
F32 = jnp.float32
CHUNK_ROWS = (2, 3, 2)
TURNS, FIRSTS, SECONDS = (2, 4, 5, 6), (1, 3, 4, 5), (0, 2, 3, 3)
EARLY_FROM = 1
AHEAD = (1, 0)
CHIPS_ALONG = (3, 1, 2, 0)
CHIP_ORDER = tuple((other, dy) for other in (0, 1) for dy in (0, -1, 1, 2))


def turn(recv, i, put):
    sources, _, win_j, own_chans, lanes = recv.shape
    chans = sources * own_chans
    for j in range(win_j):
        top = recv[:, 2 * i, j].reshape(chans, lanes)
        under = recv[:, 2 * i + 1, j].reshape(chans, lanes)
        put(j, jnp.concatenate([top, under], axis=0).T.reshape(2, lanes // 2, 2 * chans))


def blocks(pairs, weights, count):
    acc = None
    for dw in range(4):
        parts = [view[dw // 2 : dw // 2 + count, dw % 2] for view in pairs]
        lhs = jnp.concatenate([p.reshape(count * p.shape[1], p.shape[2]) for p in parts], axis=1)
        term = jnp.dot(lhs, weights(dw), preferred_element_type=F32)
        acc = term if acc is None else acc + term
    return acc


def first(pairs, weights, bias, y_row, blank_a):
    count, _, images, lanes = y_row.shape
    c = lax.axis_index("cols")
    row = lax.rem(lax.broadcasted_iota(jnp.int32, (1, 2 * lanes), 1), lanes) // (lanes // 2)
    act = jnp.maximum(blocks(pairs, weights, count) + bias, 0.0)
    act = jnp.where(row != blank_a, act, 0.0).astype(BF16)
    for b in range(2):
        y_row[:, b] = act[:, b * lanes : (b + 1) * lanes].reshape(count, images, lanes)
    blank = jnp.zeros((images, lanes), BF16)

    @pl.when(c == 0)
    def _():
        y_row[0, 0] = blank

    @pl.when(c == lax.axis_size("cols") - 1)
    def _():
        y_row[count - 1, 1] = blank


def second(pairs, weights, bias, out_pair):
    _, count, _, images, chans = out_pair.shape
    res = blocks(pairs, weights, count) + bias
    for b in range(2):
        for a in range(2):
            at = (2 * b + a) * chans
            out_pair[a, :, b] = res[:, at : at + chans].reshape(count, images, chans)


def conv_kernel(
    n_rows,
    n_cols,
    x_hbm,
    w1_hbm,
    b1_hbm,
    w2_hbm,
    b2_hbm,
    out,
    ymat,
    wt2,
    bias2,
    recv,
    xmat,
    wt1,
    bias1,
    xs,
    packed,
    w1s,
    w1own,
    w1all,
    w2s,
    b1s,
    b2s,
    load_sem,
    par_sem,
    send_sem,
    recv_sem,
    wsend_sem,
    wrecv_sem,
    swap_send_sem,
    swap_recv_sem,
    wswap_send_sem,
    wswap_recv_sem,
):
    chip_h, pairs = xs.shape[1:3]
    images = xs.shape[-1]
    tile_h, tile_j = chip_h // 2, pairs // n_cols
    win_j = tile_j + 2
    sources = n_rows * n_cols
    r, c = lax.axis_index("model"), lax.axis_index("cols")
    par = lax.rem(r, 2)
    me = r * n_cols + c
    chans = recv.shape[0] * 2

    tops = [tile_h - sum(CHUNK_ROWS[: k + 1]) for k in range(len(CHUNK_ROWS))]
    groups = (
        ((tops[0], chip_h - tops[0]),),
        *(((k, k + n), (chip_h - k - n, chip_h - k)) for k, n in zip(tops[1:], CHUNK_ROWS[1:])),
    )
    loads = []
    for g, spans in enumerate(groups):
        loads.append(
            [
                pltpu.make_async_copy(x_hbm.at[:, lo:hi], xs.at[:, lo:hi], load_sem.at[g, n])
                for n, (lo, hi) in enumerate(spans)
            ]
        )
    for copies in loads:
        for copy in copies:
            copy.start()
    params = [
        pltpu.make_async_copy(src, dst, par_sem.at[s])
        for s, (src, dst) in enumerate(((w1_hbm, w1s), (w2_hbm, w2s), (b1_hbm, b1s), (b2_hbm, b2s)))
    ]
    for copy in params:
        copy.start()

    barrier = pltpu.get_barrier_semaphore()
    to_cs = [lax.rem(c + k, n_cols) for k in range(n_cols)]

    def device(to_r, to_c):
        return {"model": to_r, "cols": to_c}

    to_rs = [lax.rem(r + k, n_rows) for k in range(n_rows)]
    for kr, kc in sorted(
        ((kr, kc) for kr in range(n_rows) for kc in range(n_cols) if kr or kc),
        key=lambda k: (k[1] not in (1, 2), k[0] not in (2, 3, 4, 5), k[1] == 2, k[0] < 4, -min(k[0], n_rows - k[0])),
    ):
        pl.semaphore_signal(barrier, inc=1, device_id=device(to_rs[kr], to_cs[kc]), device_id_type=MESH)

    ahead_r, ahead_c = AHEAD
    is_ahead = (r == ahead_r) & (c == ahead_c)

    def pack_rows(x, lo, hi):
        rows = hi - lo
        left, right = (xs[x, lo:hi, :, p].reshape(rows * pairs * 2, images) for p in range(2))
        both = jnp.concatenate([left, right], axis=1)
        packed[pl.ds(chip_h * x + lo, rows)] = both.reshape(rows, pairs, 2, 2 * images)

    def pack(g):
        for n, copy in enumerate(loads[g]):
            if (g, n) != (1, ahead_r % 2):
                copy.wait()

        def body(x, carry):
            for n, (lo, hi) in enumerate(groups[g]):
                if (g, n) == (1, ahead_r % 2):
                    pl.when(x != ahead_r // 2)(lambda lo=lo, hi=hi: pack_rows(x, lo, hi))
                else:
                    pack_rows(x, lo, hi)
            return carry

        lax.fori_loop(0, n_rows // 2, body, 0)

    last = tile_h + 4

    def rows_of(offset, count):
        def where(to_r):
            q = lax.rem(to_r, 2)
            src = tile_h * to_r + offset + (tile_h - count - 2 * offset) * q
            dst = offset + 2 + (last - count - 2 * offset - 3) * q
            return src, dst

        return where

    chunks = (
        *((n, rows_of(k, n), False) for k, n in zip(tops, CHUNK_ROWS)),
        (2, rows_of(-2, 2), True),
    )
    no_outer = (r == 0) | (r == n_rows - 1)
    at_edge = (c == 0) | (c == n_cols - 1)
    own_j = c == 0
    own_j = own_j.astype(jnp.int32)

    def send_tile(chunk, to_r, to_c, there):
        rows, where, is_outer = chunks[chunk]
        src, dst = where(to_r)
        skip = (to_c == 0).astype(jnp.int32)
        edge = (to_c == 0) | (to_c == n_cols - 1)
        if is_outer:
            there = there & (to_r > 0) & (to_r < n_rows - 1)

        def copy(count, src_j, dst_j):
            pltpu.make_async_remote_copy(
                src_ref=packed.at[pl.ds(src, rows), pl.ds(src_j, count)],
                dst_ref=recv.at[me, pl.ds(dst, rows), pl.ds(dst_j, count)],
                send_sem=send_sem.at[chunk],
                recv_sem=recv_sem.at[chunk],
                device_id=device(to_r, to_c),
                device_id_type=MESH,
            ).start()

        pl.when(there & edge)(lambda: copy(win_j - 1, tile_j * to_c - 1 + skip, skip))
        pl.when(there & jnp.logical_not(edge))(lambda: copy(win_j, tile_j * to_c - 1, 0))

    chips = n_rows // 2

    def step(t, table):
        value = jnp.int32(table[-1])
        for k, entry in enumerate(table[:-1]):
            value = jnp.where(t == k, entry, value)
        return value

    def turn_to(t):
        dx = step(t, CHIPS_ALONG)
        return lax.rem(r // 2 + dx, chips), dx

    def send_chip(chunk, t, where=None):
        x, dx = turn_to(t)
        way = 1 - 2 * lax.rem(par + t, 2)
        for other, dy in CHIP_ORDER:
            to_r = 2 * x + (1 - par if other else par)
            to_c = lax.rem(c + way * dy + n_cols, n_cols)
            there = True
            if not other and dy == 0:
                there = dx > 0
            if where is not None:
                there = there & where(to_r, to_c)
            send_tile(chunk, to_r, to_c, there)

    def send_chunk(chunk):
        early = EARLY_FROM <= chunk

        def body(t, carry):
            if chunk > EARLY_FROM:
                send_chip(chunk, t, lambda to_r, to_c: to_c > 0)
            else:
                send_chip(chunk, t, lambda to_r, to_c: (to_r != ahead_r) | (to_c != ahead_c))
            if early and chunk + 1 < len(chunks):
                x, dx = turn_to(t)
                for other in range(2):
                    to_r = 2 * x + (1 - par if other else par)
                    there = (to_r != r) | (c != 0)
                    if chunk > EARLY_FROM:
                        there = there & (to_r != ahead_r)
                    send_tile(chunk + 1, to_r, jnp.int32(0), there)
                if chunk == EARLY_FROM:
                    there = (x == ahead_r // 2) & jnp.logical_not(is_ahead)
                    send_tile(len(chunks) - 1, jnp.int32(ahead_r), jnp.int32(ahead_c), there)
            return carry

        lax.fori_loop(0, chips, body, 0)

    params[0].wait()
    for dw in range(3):
        w1own[dw] = jnp.concatenate([w1s[1, dw], w1s[0, dw]], axis=1)
    w1own[3] = jnp.concatenate([w1s[2, 0], w1s[2, 1]], axis=1)
    w1own[4] = jnp.concatenate([w1s[2, 2], jnp.zeros_like(w1s[2, 2])], axis=1)
    w1all[r // 2, par, c] = w1own[...]

    for copy in loads[0]:
        copy.wait()
    pack_rows(turn_to(0)[0], *groups[0][0])
    pl.semaphore_wait(barrier, sources - 1)

    def send_weights():
        for kr in range(0, n_rows, 2):
            for kc in range(n_cols):
                if kr or kc:
                    pltpu.make_async_remote_copy(
                        src_ref=w1own,
                        dst_ref=w1all.at[r // 2, par, c],
                        send_sem=wsend_sem,
                        recv_sem=wrecv_sem,
                        device_id=device(to_rs[kr], to_cs[kc]),
                        device_id_type=MESH,
                    ).start()

    def pack_and_send(t, carry):
        pl.when(t < chips - 1)(lambda: pack_rows(turn_to(t + 1)[0], *groups[0][0]))
        there = turn_to(t)[0] == ahead_r // 2

        @pl.when(there)
        def _():
            loads[1][ahead_r % 2].wait()
            pack_rows(ahead_r // 2, *groups[1][ahead_r % 2])

        send_chip(0, t)
        send_tile(1, jnp.int32(ahead_r), jnp.int32(ahead_c), there & jnp.logical_not(is_ahead))
        pl.when(t == 1)(send_weights)
        return carry

    lax.fori_loop(0, chips, pack_and_send, 0)

    for g in range(1, EARLY_FROM + 1):
        pack(g)
    for chunk in range(1, len(chunks)):
        if chunk >= EARLY_FROM and chunk + 1 < len(groups):
            pack(chunk + 1)
        send_chunk(chunk)

    def wait_bytes(ref, sem):
        pltpu.make_async_copy(ref, ref, sem).wait()

    w1_bytes = recv.at[0 : sources // 2 - 1, 0, 0:5]
    wait_bytes(w1_bytes, wrecv_sem)
    wait_bytes(w1_bytes, wsend_sem)
    partner = device(r + 1 - 2 * par, c)
    w_swap = pltpu.make_async_remote_copy(
        src_ref=w1all.at[:, par],
        dst_ref=w1all.at[:, par],
        send_sem=wswap_send_sem,
        recv_sem=wswap_recv_sem,
        device_id=partner,
        device_id_type=MESH,
    )
    w_swap.start()

    def own_rows(chunk):
        rows, where, _ = chunks[chunk]
        src, dst = where(r)

        def copy(count, src_j, dst_j):
            for h in range(rows):
                recv[me, dst + h, pl.ds(dst_j, count)] = packed[src + h, pl.ds(src_j, count)]

        pl.when(at_edge)(lambda: copy(win_j - 1, tile_j * c - 1 + own_j, own_j))
        pl.when(jnp.logical_not(at_edge))(lambda: copy(win_j, tile_j * c - 1, 0))

    for chunk in range(3):
        own_rows(chunk)
    pl.when(jnp.logical_not(no_outer))(lambda: own_rows(3))

    zero_row = jnp.zeros((win_j, 2, 2 * images), BF16)
    zero_col = jnp.zeros((tile_h + 2, 2, 2 * images), BF16)

    def clear(s, carry):
        recv[s, last * (1 - par)] = zero_row
        return carry

    def clear_outer(s, carry):
        recv[s, (last - 1) * par] = zero_row
        recv[s, (last - 1) * par + 1] = zero_row
        return carry

    def clear_edge(s, carry):
        recv[s, pl.ds(3 * par, tile_h + 2), (win_j - 1) * (1 - own_j)] = zero_col
        return carry

    lax.fori_loop(0, sources, clear, 0)
    pl.when(no_outer)(lambda: (lax.fori_loop(0, sources, clear_outer, 0), None)[1])
    pl.when(at_edge)(lambda: (lax.fori_loop(0, sources, clear_edge, 0), None)[1])

    low = lax.broadcasted_iota(jnp.int32, (chans, 2 * chans), 1) < chans

    def spread(wt, u, v, dw):
        ur, vr = pltpu.roll(u, chans, 1), pltpu.roll(v, chans, 1)
        zero = jnp.zeros_like(u)
        tiles = (jnp.where(low, ur, zero), u, jnp.where(low, v, ur), jnp.where(low, zero, vr))
        for k, tile in enumerate(tiles):
            tile = tile.astype(BF16)
            for b in range(2):
                wt[dw + b, k * chans : (k + 1) * chans, b * 2 * chans : (b + 1) * 2 * chans] = tile

    def blank(wt):
        zero = jnp.zeros((4 * chans, 2 * chans), BF16)
        wt[3, :, 0 : 2 * chans] = zero
        wt[0, :, 2 * chans : 4 * chans] = zero

    for copy in params[1:]:
        copy.wait()
    blank(wt1)
    blank(wt2)
    for dw in range(3):
        w = [w2s[dh, dw].astype(F32) for dh in range(3)]
        spread(
            wt2,
            jnp.concatenate([w[1], w[0]], axis=1),
            jnp.concatenate([w[2], jnp.zeros_like(w[2])], axis=1),
            dw,
        )
    bias1[...] = jnp.concatenate([b1s[...]] * 4, axis=1)
    bias2[...] = jnp.concatenate([b2s[...]] * 4, axis=1)

    def arrived(chunk):
        def wait(count):
            wait_bytes(recv.at[0 : sources - 1, 0 : chunks[chunk][0], 0:count], recv_sem.at[chunk])

        pl.when(at_edge)(lambda: wait(win_j - 1))
        pl.when(jnp.logical_not(at_edge))(lambda: wait(win_j))

    arrived(0)
    give = tile_h - (tile_h - 3) * par
    land = tile_h + 2 - (tile_h + 1) * (1 - par)
    swap = pltpu.make_async_remote_copy(
        src_ref=recv.at[:, pl.ds(give, 2)],
        dst_ref=recv.at[:, pl.ds(land, 2)],
        send_sem=swap_send_sem,
        recv_sem=swap_recv_sem,
        device_id=partner,
        device_id_type=MESH,
    )
    swap.start()

    w_swap.wait()
    u = [w1all[:, :, :, k].reshape(chans, 2 * chans).astype(F32) for k in range(5)]
    for dw in range(3):
        v = (u[3], pltpu.roll(u[3], chans, 1), u[4])[dw]
        spread(wt1, u[dw], jnp.where(low, v, 0.0), dw)

    x_pairs, z_pairs = xmat.shape[0], ymat.shape[0]
    o_pairs = z_pairs - 1

    def nth(n, count):
        return (count - 1) * (1 - par) + n * (2 * par - 1)

    def turn_one(n, carry):
        i = nth(n, x_pairs)

        def put(j, value):
            xmat[i, j] = value

        turn(recv, i, put)
        return carry

    def first_one(n, carry):
        i = nth(n, z_pairs)
        fill = jnp.where(n == 0, 1 - par, 2)
        out_of = jnp.where(n == z_pairs - 1, jnp.where(r == 0, 0, jnp.where(r == n_rows - 1, 1, 2)), 2)
        blank_a = jnp.where(fill < 2, fill, out_of)
        first((xmat.at[i], xmat.at[i + 1]), lambda dw: wt1[dw], bias1[...], ymat.at[i], blank_a)
        return carry

    def second_one(n, carry):
        i = nth(n, o_pairs)
        second((ymat.at[i], ymat.at[i + 1]), lambda dw: wt2[dw], bias2[...], out.at[pl.ds(2 * i, 2)])
        return carry

    def stage(s, carry):
        @pl.when(s == 0)
        def _():
            swap.wait()

        for k in range(1, 4):
            there = s == k
            if k == 3:
                there = there & jnp.logical_not(no_outer)
            pl.when(there)(lambda k=k: arrived(k))

        for ends, one in ((TURNS, turn_one), (FIRSTS, first_one), (SECONDS, second_one)):
            lax.fori_loop(step(s, (0, *ends[:-1])), step(s, ends), one, 0)
        return carry

    lax.fori_loop(0, 4, stage, 0)

    per_edge = n_rows * 2
    for chunk in range(4):
        rows = chunks[chunk][0]
        n_r = n_rows - 2 if chunk == 3 else n_rows
        counts = (n_r * 2, n_r * (n_cols - 2))

        def drain(edge_n, inner_n, rows=rows, chunk=chunk):
            wait_bytes(recv.at[0:edge_n, 0:rows, 0 : win_j - 1], send_sem.at[chunk])
            wait_bytes(recv.at[0:inner_n, 0:rows, 0:win_j], send_sem.at[chunk])

        def drain_own(chunk=chunk, counts=counts, drain=drain):
            pl.when(at_edge)(lambda: drain(counts[0] - 1, counts[1]))
            pl.when(jnp.logical_not(at_edge))(lambda: drain(counts[0], counts[1] - 1))

        if chunk == 3:
            pl.when(no_outer)(lambda: drain(*counts))
            pl.when(jnp.logical_not(no_outer))(drain_own)
        else:
            drain_own()


def tail_kernel(tile, ymat, wt2, bias2, out_hbm, o_new, sem):
    par = lax.rem(lax.axis_index("model"), 2)
    rows = out_hbm.shape[0]
    o_pairs = ymat.shape[0] - 1
    late = (rows - 2) * par
    here = 2 * (1 - par)

    cut = out_hbm.shape[1] // 2

    def start(k, carry):
        for part in (pl.ds(0, cut), pl.ds(cut, out_hbm.shape[1] - cut)):
            pltpu.make_async_copy(tile.at[par + k, part], out_hbm.at[k, part], sem.at[0]).start()
        return carry

    lax.fori_loop(here, here + rows - 2, start, 0)
    i = (o_pairs - 1) * par
    second((ymat.at[i], ymat.at[i + 1]), lambda dw: wt2[dw], bias2[...], o_new)
    for k in range(2):
        for part in (pl.ds(0, cut), pl.ds(cut, out_hbm.shape[1] - cut)):
            pltpu.make_async_copy(o_new.at[k, part], out_hbm.at[late + k, part], sem.at[1]).start()
    pltpu.make_async_copy(tile.at[0 : rows - 2], out_hbm.at[0 : rows - 2], sem.at[0]).wait()
    pltpu.make_async_copy(o_new, out_hbm.at[pl.ds(late, 2)], sem.at[1]).wait()


def solution(mesh):
    n_rows = mesh.shape["model"]
    n_cols = mesh.shape["cols"]

    def run_local(x_in, w_conv1, b_conv1, w_conv2, b_conv2):
        images, height, width, own_chans = x_in.shape
        sources = n_rows * n_cols
        chans = own_chans * sources
        pairs = width // 2
        tile_h, tile_j = height // n_rows, pairs // n_cols
        win_j = tile_j + 2
        x_pairs, z_pairs = (tile_h + 5) // 2, (tile_h + 3) // 2
        x_t = jnp.transpose(x_in, (1, 2, 3, 0)).reshape(n_rows // 2, 2 * tile_h, pairs, 2, own_chans, images)
        args = (x_t, w_conv1, b_conv1.reshape(1, chans), w_conv2, b_conv2.reshape(1, chans))
        hbm = pl.BlockSpec(memory_space=pltpu.HBM)
        vmem = pl.BlockSpec(memory_space=pltpu.VMEM)
        kept = (
            pltpu.VMEM((2 * (z_pairs - 1), tile_j, 2, images, chans), F32),
            pltpu.VMEM((z_pairs, win_j - 1, 2, images, 2 * chans), BF16),
            pltpu.VMEM((4, 4 * chans, 4 * chans), BF16),
            pltpu.VMEM((1, 4 * chans), F32),
        )
        state = pl.pallas_call(
            functools.partial(conv_kernel, n_rows, n_cols),
            out_shape=kept,
            in_specs=[hbm] * 5,
            out_specs=[vmem] * len(kept),
            scratch_shapes=[
                pltpu.VMEM((sources, 2 * x_pairs, win_j, own_chans, 2 * images), BF16),
                pltpu.VMEM((x_pairs, win_j, 2, images, 2 * chans), BF16),
                pltpu.VMEM((4, 4 * chans, 4 * chans), BF16),
                pltpu.VMEM((1, 4 * chans), F32),
                pltpu.VMEM((n_rows // 2, 2 * tile_h, pairs, 2, own_chans, images), BF16),
                pltpu.VMEM((height, pairs, own_chans, 2 * images), BF16),
                pltpu.VMEM((3, 3, own_chans, chans), BF16),
                pltpu.VMEM((5, own_chans, 2 * chans), BF16),
                pltpu.VMEM((n_rows // 2, 2, n_cols, 5, own_chans, 2 * chans), BF16),
                pltpu.VMEM((3, 3, chans, chans), BF16),
                pltpu.VMEM((1, chans), F32),
                pltpu.VMEM((1, chans), F32),
                pltpu.SemaphoreType.DMA((3, 2)),
                pltpu.SemaphoreType.DMA((4,)),
                pltpu.SemaphoreType.DMA((4,)),
                pltpu.SemaphoreType.DMA((4,)),
            ]
            + [pltpu.SemaphoreType.DMA] * 6,
            compiler_params=pltpu.CompilerParams(
                collective_id=0, has_side_effects=True, vmem_limit_bytes=24 << 20
            ),
            name="conv",
        )(*(pltpu.with_memory_space_constraint(a, pltpu.HBM) for a in args))
        out = pl.pallas_call(
            tail_kernel,
            out_shape=jax.ShapeDtypeStruct((tile_h, tile_j, 2, images, chans), F32),
            in_specs=[vmem] * len(kept),
            out_specs=pl.BlockSpec(memory_space=pl.ANY),
            scratch_shapes=[
                pltpu.VMEM((2, tile_j, 2, images, chans), F32),
                pltpu.SemaphoreType.DMA((2,)),
            ],
            compiler_params=pltpu.CompilerParams(vmem_limit_bytes=8 << 20),
            name="tail",
        )(*state)
        out = out.reshape(tile_h, 2 * tile_j, images, chans)
        return jnp.transpose(out, (2, 0, 1, 3))

    group = ("model", "cols")
    return jax.shard_map(
        run_local,
        mesh=mesh,
        in_specs=(P("data", None, None, group), P(None, None, group, None), P(), P(), P()),
        out_specs=P("data", "model", "cols", None),
        check_vma=False,
    )
```

```python
import functools

import jax
import jax.numpy as jnp
from jax import lax
from jax.experimental import pallas as pl
from jax.experimental.pallas import tpu as pltpu
from jax.sharding import PartitionSpec as P

MESH = pl.DeviceIdType.MESH
BF16 = jnp.bfloat16
F32 = jnp.float32
CHUNK_ROWS = (2, 3, 2)
TURNS, FIRSTS, SECONDS = (2, 4, 5, 6), (1, 3, 4, 5), (0, 2, 3, 3)
EARLY_FROM = 1
AHEAD = (1, 0)
CHIPS_ALONG = (3, 1, 2, 0)
CHIP_ORDER = tuple((other, dy) for other in (0, 1) for dy in (0, 1, -1, 2))


def turn(recv, i, put):
    sources, _, win_j, own_chans, lanes = recv.shape
    chans = sources * own_chans
    for j in range(win_j):
        top = recv[:, 2 * i, j].reshape(chans, lanes)
        under = recv[:, 2 * i + 1, j].reshape(chans, lanes)
        put(j, jnp.concatenate([top, under], axis=0).T.reshape(2, lanes // 2, 2 * chans))


def blocks(pairs, weights, count):
    acc = None
    for dw in range(4):
        parts = [view[dw // 2 : dw // 2 + count, dw % 2] for view in pairs]
        lhs = jnp.concatenate([p.reshape(count * p.shape[1], p.shape[2]) for p in parts], axis=1)
        term = jnp.dot(lhs, weights(dw), preferred_element_type=F32)
        acc = term if acc is None else acc + term
    return acc


def first(pairs, weights, bias, y_row, blank_a):
    count, _, images, lanes = y_row.shape
    c = lax.axis_index("cols")
    row = lax.rem(lax.broadcasted_iota(jnp.int32, (1, 2 * lanes), 1), lanes) // (lanes // 2)
    act = jnp.maximum(blocks(pairs, weights, count) + bias, 0.0)
    act = jnp.where(row != blank_a, act, 0.0).astype(BF16)
    for b in range(2):
        y_row[:, b] = act[:, b * lanes : (b + 1) * lanes].reshape(count, images, lanes)
    blank = jnp.zeros((images, lanes), BF16)

    @pl.when(c == 0)
    def _():
        y_row[0, 0] = blank

    @pl.when(c == lax.axis_size("cols") - 1)
    def _():
        y_row[count - 1, 1] = blank


def second(pairs, weights, bias, out_pair):
    _, count, _, images, chans = out_pair.shape
    res = blocks(pairs, weights, count) + bias
    for b in range(2):
        for a in range(2):
            at = (2 * b + a) * chans
            out_pair[a, :, b] = res[:, at : at + chans].reshape(count, images, chans)


def conv_kernel(
    n_rows,
    n_cols,
    x_hbm,
    w1_hbm,
    b1_hbm,
    w2_hbm,
    b2_hbm,
    out,
    ymat,
    wt2,
    bias2,
    recv,
    xmat,
    wt1,
    bias1,
    xs,
    packed,
    w1s,
    w1own,
    w1all,
    w2s,
    b1s,
    b2s,
    load_sem,
    par_sem,
    send_sem,
    recv_sem,
    wsend_sem,
    wrecv_sem,
    swap_send_sem,
    swap_recv_sem,
    wswap_send_sem,
    wswap_recv_sem,
):
    chip_h, pairs = xs.shape[1:3]
    images = xs.shape[-1]
    tile_h, tile_j = chip_h // 2, pairs // n_cols
    win_j = tile_j + 2
    sources = n_rows * n_cols
    r, c = lax.axis_index("model"), lax.axis_index("cols")
    par = lax.rem(r, 2)
    me = r * n_cols + c
    chans = recv.shape[0] * 2

    tops = [tile_h - sum(CHUNK_ROWS[: k + 1]) for k in range(len(CHUNK_ROWS))]
    groups = (
        ((tops[0], chip_h - tops[0]),),
        *(((k, k + n), (chip_h - k - n, chip_h - k)) for k, n in zip(tops[1:], CHUNK_ROWS[1:])),
    )
    loads = []
    for g, spans in enumerate(groups):
        loads.append(
            [
                pltpu.make_async_copy(x_hbm.at[:, lo:hi], xs.at[:, lo:hi], load_sem.at[g, n])
                for n, (lo, hi) in enumerate(spans)
            ]
        )
    for copies in loads:
        for copy in copies:
            copy.start()
    params = [
        pltpu.make_async_copy(src, dst, par_sem.at[s])
        for s, (src, dst) in enumerate(((w1_hbm, w1s), (w2_hbm, w2s), (b1_hbm, b1s), (b2_hbm, b2s)))
    ]
    for copy in params:
        copy.start()

    barrier = pltpu.get_barrier_semaphore()
    to_cs = [lax.rem(c + k, n_cols) for k in range(n_cols)]

    def device(to_r, to_c):
        return {"model": to_r, "cols": to_c}

    to_rs = [lax.rem(r + k, n_rows) for k in range(n_rows)]
    for kr, kc in sorted(
        ((kr, kc) for kr in range(n_rows) for kc in range(n_cols) if kr or kc),
        key=lambda k: (k[1] not in (1, 2), k[0] not in (2, 3, 4, 5), k[1] == 2, k[0] < 4, -min(k[0], n_rows - k[0])),
    ):
        pl.semaphore_signal(barrier, inc=1, device_id=device(to_rs[kr], to_cs[kc]), device_id_type=MESH)

    ahead_r, ahead_c = AHEAD
    is_ahead = (r == ahead_r) & (c == ahead_c)

    def pack_rows(x, lo, hi):
        rows = hi - lo
        left, right = (xs[x, lo:hi, :, p].reshape(rows * pairs * 2, images) for p in range(2))
        both = jnp.concatenate([left, right], axis=1)
        packed[pl.ds(chip_h * x + lo, rows)] = both.reshape(rows, pairs, 2, 2 * images)

    def pack(g):
        for n, copy in enumerate(loads[g]):
            if (g, n) != (1, ahead_r % 2):
                copy.wait()

        def body(x, carry):
            for n, (lo, hi) in enumerate(groups[g]):
                if (g, n) == (1, ahead_r % 2):
                    pl.when(x != ahead_r // 2)(lambda lo=lo, hi=hi: pack_rows(x, lo, hi))
                else:
                    pack_rows(x, lo, hi)
            return carry

        lax.fori_loop(0, n_rows // 2, body, 0)

    last = tile_h + 4

    def rows_of(offset, count):
        def where(to_r):
            q = lax.rem(to_r, 2)
            src = tile_h * to_r + offset + (tile_h - count - 2 * offset) * q
            dst = offset + 2 + (last - count - 2 * offset - 3) * q
            return src, dst

        return where

    chunks = (
        *((n, rows_of(k, n), False) for k, n in zip(tops, CHUNK_ROWS)),
        (2, rows_of(-2, 2), True),
    )
    no_outer = (r == 0) | (r == n_rows - 1)
    at_edge = (c == 0) | (c == n_cols - 1)
    own_j = c == 0
    own_j = own_j.astype(jnp.int32)

    def send_tile(chunk, to_r, to_c, there):
        rows, where, is_outer = chunks[chunk]
        src, dst = where(to_r)
        skip = (to_c == 0).astype(jnp.int32)
        edge = (to_c == 0) | (to_c == n_cols - 1)
        if is_outer:
            there = there & (to_r > 0) & (to_r < n_rows - 1)

        def copy(count, src_j, dst_j):
            pltpu.make_async_remote_copy(
                src_ref=packed.at[pl.ds(src, rows), pl.ds(src_j, count)],
                dst_ref=recv.at[me, pl.ds(dst, rows), pl.ds(dst_j, count)],
                send_sem=send_sem.at[chunk],
                recv_sem=recv_sem.at[chunk],
                device_id=device(to_r, to_c),
                device_id_type=MESH,
            ).start()

        pl.when(there & edge)(lambda: copy(win_j - 1, tile_j * to_c - 1 + skip, skip))
        pl.when(there & jnp.logical_not(edge))(lambda: copy(win_j, tile_j * to_c - 1, 0))

    chips = n_rows // 2

    def step(t, table):
        value = jnp.int32(table[-1])
        for k, entry in enumerate(table[:-1]):
            value = jnp.where(t == k, entry, value)
        return value

    def turn_to(t):
        dx = step(t, CHIPS_ALONG)
        return lax.rem(r // 2 + dx, chips), dx

    def send_chip(chunk, t, where=None):
        x, dx = turn_to(t)
        way = 1 - 2 * lax.rem(par + t, 2)
        for other, dy in CHIP_ORDER:
            to_r = 2 * x + (1 - par if other else par)
            to_c = lax.rem(c + way * dy + n_cols, n_cols)
            there = True
            if not other and dy == 0:
                there = dx > 0
            if where is not None:
                there = there & where(to_r, to_c)
            send_tile(chunk, to_r, to_c, there)

    def send_chunk(chunk):
        early = EARLY_FROM <= chunk

        def body(t, carry):
            if chunk > EARLY_FROM:
                send_chip(chunk, t, lambda to_r, to_c: to_c > 0)
            else:
                send_chip(chunk, t, lambda to_r, to_c: (to_r != ahead_r) | (to_c != ahead_c))
            if early and chunk + 1 < len(chunks):
                x, dx = turn_to(t)
                for other in range(2):
                    to_r = 2 * x + (1 - par if other else par)
                    there = (to_r != r) | (c != 0)
                    if chunk > EARLY_FROM:
                        there = there & (to_r != ahead_r)
                    send_tile(chunk + 1, to_r, jnp.int32(0), there)
                if chunk == EARLY_FROM:
                    there = (x == ahead_r // 2) & jnp.logical_not(is_ahead)
                    send_tile(len(chunks) - 1, jnp.int32(ahead_r), jnp.int32(ahead_c), there)
            return carry

        lax.fori_loop(0, chips, body, 0)

    params[0].wait()
    for dw in range(3):
        w1own[dw] = jnp.concatenate([w1s[1, dw], w1s[0, dw]], axis=1)
    w1own[3] = jnp.concatenate([w1s[2, 0], w1s[2, 1]], axis=1)
    w1own[4] = jnp.concatenate([w1s[2, 2], jnp.zeros_like(w1s[2, 2])], axis=1)
    w1all[r // 2, par, c] = w1own[...]

    for copy in loads[0]:
        copy.wait()
    pack_rows(turn_to(0)[0], *groups[0][0])
    pl.semaphore_wait(barrier, sources - 1)

    def send_weights():
        for kr in range(0, n_rows, 2):
            for kc in range(n_cols):
                if kr or kc:
                    pltpu.make_async_remote_copy(
                        src_ref=w1own,
                        dst_ref=w1all.at[r // 2, par, c],
                        send_sem=wsend_sem,
                        recv_sem=wrecv_sem,
                        device_id=device(to_rs[kr], to_cs[kc]),
                        device_id_type=MESH,
                    ).start()

    def pack_and_send(t, carry):
        pl.when(t < chips - 1)(lambda: pack_rows(turn_to(t + 1)[0], *groups[0][0]))
        there = turn_to(t)[0] == ahead_r // 2

        @pl.when(there)
        def _():
            loads[1][ahead_r % 2].wait()
            pack_rows(ahead_r // 2, *groups[1][ahead_r % 2])

        send_chip(0, t)
        send_tile(1, jnp.int32(ahead_r), jnp.int32(ahead_c), there & jnp.logical_not(is_ahead))
        pl.when(t == 1)(send_weights)
        return carry

    lax.fori_loop(0, chips, pack_and_send, 0)

    for g in range(1, EARLY_FROM + 1):
        pack(g)
    for chunk in range(1, len(chunks)):
        if chunk >= EARLY_FROM and chunk + 1 < len(groups):
            pack(chunk + 1)
        send_chunk(chunk)

    def wait_bytes(ref, sem):
        pltpu.make_async_copy(ref, ref, sem).wait()

    w1_bytes = recv.at[0 : sources // 2 - 1, 0, 0:5]
    wait_bytes(w1_bytes, wrecv_sem)
    wait_bytes(w1_bytes, wsend_sem)
    partner = device(r + 1 - 2 * par, c)
    w_swap = pltpu.make_async_remote_copy(
        src_ref=w1all.at[:, par],
        dst_ref=w1all.at[:, par],
        send_sem=wswap_send_sem,
        recv_sem=wswap_recv_sem,
        device_id=partner,
        device_id_type=MESH,
    )
    w_swap.start()

    def own_rows(chunk):
        rows, where, _ = chunks[chunk]
        src, dst = where(r)

        def copy(count, src_j, dst_j):
            for h in range(rows):
                recv[me, dst + h, pl.ds(dst_j, count)] = packed[src + h, pl.ds(src_j, count)]

        pl.when(at_edge)(lambda: copy(win_j - 1, tile_j * c - 1 + own_j, own_j))
        pl.when(jnp.logical_not(at_edge))(lambda: copy(win_j, tile_j * c - 1, 0))

    for chunk in range(3):
        own_rows(chunk)
    pl.when(jnp.logical_not(no_outer))(lambda: own_rows(3))

    zero_row = jnp.zeros((win_j, 2, 2 * images), BF16)
    zero_col = jnp.zeros((tile_h + 2, 2, 2 * images), BF16)

    def clear(s, carry):
        recv[s, last * (1 - par)] = zero_row
        return carry

    def clear_outer(s, carry):
        recv[s, (last - 1) * par] = zero_row
        recv[s, (last - 1) * par + 1] = zero_row
        return carry

    def clear_edge(s, carry):
        recv[s, pl.ds(3 * par, tile_h + 2), (win_j - 1) * (1 - own_j)] = zero_col
        return carry

    lax.fori_loop(0, sources, clear, 0)
    pl.when(no_outer)(lambda: (lax.fori_loop(0, sources, clear_outer, 0), None)[1])
    pl.when(at_edge)(lambda: (lax.fori_loop(0, sources, clear_edge, 0), None)[1])

    low = lax.broadcasted_iota(jnp.int32, (chans, 2 * chans), 1) < chans

    def spread(wt, u, v, dw):
        ur, vr = pltpu.roll(u, chans, 1), pltpu.roll(v, chans, 1)
        zero = jnp.zeros_like(u)
        tiles = (jnp.where(low, ur, zero), u, jnp.where(low, v, ur), jnp.where(low, zero, vr))
        for k, tile in enumerate(tiles):
            tile = tile.astype(BF16)
            for b in range(2):
                wt[dw + b, k * chans : (k + 1) * chans, b * 2 * chans : (b + 1) * 2 * chans] = tile

    def blank(wt):
        zero = jnp.zeros((4 * chans, 2 * chans), BF16)
        wt[3, :, 0 : 2 * chans] = zero
        wt[0, :, 2 * chans : 4 * chans] = zero

    for copy in params[1:]:
        copy.wait()
    blank(wt1)
    blank(wt2)
    for dw in range(3):
        w = [w2s[dh, dw].astype(F32) for dh in range(3)]
        spread(
            wt2,
            jnp.concatenate([w[1], w[0]], axis=1),
            jnp.concatenate([w[2], jnp.zeros_like(w[2])], axis=1),
            dw,
        )
    bias1[...] = jnp.concatenate([b1s[...]] * 4, axis=1)
    bias2[...] = jnp.concatenate([b2s[...]] * 4, axis=1)

    def arrived(chunk):
        def wait(count):
            wait_bytes(recv.at[0 : sources - 1, 0 : chunks[chunk][0], 0:count], recv_sem.at[chunk])

        pl.when(at_edge)(lambda: wait(win_j - 1))
        pl.when(jnp.logical_not(at_edge))(lambda: wait(win_j))

    arrived(0)
    give = tile_h - (tile_h - 3) * par
    land = tile_h + 2 - (tile_h + 1) * (1 - par)
    swap = pltpu.make_async_remote_copy(
        src_ref=recv.at[:, pl.ds(give, 2)],
        dst_ref=recv.at[:, pl.ds(land, 2)],
        send_sem=swap_send_sem,
        recv_sem=swap_recv_sem,
        device_id=partner,
        device_id_type=MESH,
    )
    swap.start()

    w_swap.wait()
    u = [w1all[:, :, :, k].reshape(chans, 2 * chans).astype(F32) for k in range(5)]
    for dw in range(3):
        v = (u[3], pltpu.roll(u[3], chans, 1), u[4])[dw]
        spread(wt1, u[dw], jnp.where(low, v, 0.0), dw)

    x_pairs, z_pairs = xmat.shape[0], ymat.shape[0]
    o_pairs = z_pairs - 1

    def nth(n, count):
        return (count - 1) * (1 - par) + n * (2 * par - 1)

    def turn_one(n, carry):
        i = nth(n, x_pairs)

        def put(j, value):
            xmat[i, j] = value

        turn(recv, i, put)
        return carry

    def first_one(n, carry):
        i = nth(n, z_pairs)
        fill = jnp.where(n == 0, 1 - par, 2)
        out_of = jnp.where(n == z_pairs - 1, jnp.where(r == 0, 0, jnp.where(r == n_rows - 1, 1, 2)), 2)
        blank_a = jnp.where(fill < 2, fill, out_of)
        first((xmat.at[i], xmat.at[i + 1]), lambda dw: wt1[dw], bias1[...], ymat.at[i], blank_a)
        return carry

    def second_one(n, carry):
        i = nth(n, o_pairs)
        second((ymat.at[i], ymat.at[i + 1]), lambda dw: wt2[dw], bias2[...], out.at[pl.ds(2 * i, 2)])
        return carry

    def stage(s, carry):
        @pl.when(s == 0)
        def _():
            swap.wait()

        for k in range(1, 4):
            there = s == k
            if k == 3:
                there = there & jnp.logical_not(no_outer)
            pl.when(there)(lambda k=k: arrived(k))

        for ends, one in ((TURNS, turn_one), (FIRSTS, first_one), (SECONDS, second_one)):
            lax.fori_loop(step(s, (0, *ends[:-1])), step(s, ends), one, 0)
        return carry

    lax.fori_loop(0, 4, stage, 0)

    per_edge = n_rows * 2
    for chunk in range(4):
        rows = chunks[chunk][0]
        n_r = n_rows - 2 if chunk == 3 else n_rows
        counts = (n_r * 2, n_r * (n_cols - 2))

        def drain(edge_n, inner_n, rows=rows, chunk=chunk):
            wait_bytes(recv.at[0:edge_n, 0:rows, 0 : win_j - 1], send_sem.at[chunk])
            wait_bytes(recv.at[0:inner_n, 0:rows, 0:win_j], send_sem.at[chunk])

        def drain_own(chunk=chunk, counts=counts, drain=drain):
            pl.when(at_edge)(lambda: drain(counts[0] - 1, counts[1]))
            pl.when(jnp.logical_not(at_edge))(lambda: drain(counts[0], counts[1] - 1))

        if chunk == 3:
            pl.when(no_outer)(lambda: drain(*counts))
            pl.when(jnp.logical_not(no_outer))(drain_own)
        else:
            drain_own()


def tail_kernel(tile, ymat, wt2, bias2, out_hbm, o_new, sem):
    par = lax.rem(lax.axis_index("model"), 2)
    rows = out_hbm.shape[0]
    o_pairs = ymat.shape[0] - 1
    late = (rows - 2) * par
    here = 2 * (1 - par)

    width = out_hbm.shape[1]
    parts = [pl.ds(j, min(2, width - j)) for j in range(0, width, 2)]

    def start(k, carry):
        for part in parts:
            pltpu.make_async_copy(tile.at[par + k, part], out_hbm.at[k, part], sem.at[0]).start()
        return carry

    lax.fori_loop(here, here + rows - 2, start, 0)
    i = (o_pairs - 1) * par
    second((ymat.at[i], ymat.at[i + 1]), lambda dw: wt2[dw], bias2[...], o_new)
    for k in range(2):
        for part in parts:
            pltpu.make_async_copy(o_new.at[k, part], out_hbm.at[late + k, part], sem.at[1]).start()
    pltpu.make_async_copy(tile.at[0 : rows - 2], out_hbm.at[0 : rows - 2], sem.at[0]).wait()
    pltpu.make_async_copy(o_new, out_hbm.at[pl.ds(late, 2)], sem.at[1]).wait()


def solution(mesh):
    n_rows = mesh.shape["model"]
    n_cols = mesh.shape["cols"]

    def run_local(x_in, w_conv1, b_conv1, w_conv2, b_conv2):
        images, height, width, own_chans = x_in.shape
        sources = n_rows * n_cols
        chans = own_chans * sources
        pairs = width // 2
        tile_h, tile_j = height // n_rows, pairs // n_cols
        win_j = tile_j + 2
        x_pairs, z_pairs = (tile_h + 5) // 2, (tile_h + 3) // 2
        x_t = jnp.transpose(x_in, (1, 2, 3, 0)).reshape(n_rows // 2, 2 * tile_h, pairs, 2, own_chans, images)
        args = (x_t, w_conv1, b_conv1.reshape(1, chans), w_conv2, b_conv2.reshape(1, chans))
        hbm = pl.BlockSpec(memory_space=pltpu.HBM)
        vmem = pl.BlockSpec(memory_space=pltpu.VMEM)
        kept = (
            pltpu.VMEM((2 * (z_pairs - 1), tile_j, 2, images, chans), F32),
            pltpu.VMEM((z_pairs, win_j - 1, 2, images, 2 * chans), BF16),
            pltpu.VMEM((4, 4 * chans, 4 * chans), BF16),
            pltpu.VMEM((1, 4 * chans), F32),
        )
        state = pl.pallas_call(
            functools.partial(conv_kernel, n_rows, n_cols),
            out_shape=kept,
            in_specs=[hbm] * 5,
            out_specs=[vmem] * len(kept),
            scratch_shapes=[
                pltpu.VMEM((sources, 2 * x_pairs, win_j, own_chans, 2 * images), BF16),
                pltpu.VMEM((x_pairs, win_j, 2, images, 2 * chans), BF16),
                pltpu.VMEM((4, 4 * chans, 4 * chans), BF16),
                pltpu.VMEM((1, 4 * chans), F32),
                pltpu.VMEM((n_rows // 2, 2 * tile_h, pairs, 2, own_chans, images), BF16),
                pltpu.VMEM((height, pairs, own_chans, 2 * images), BF16),
                pltpu.VMEM((3, 3, own_chans, chans), BF16),
                pltpu.VMEM((5, own_chans, 2 * chans), BF16),
                pltpu.VMEM((n_rows // 2, 2, n_cols, 5, own_chans, 2 * chans), BF16),
                pltpu.VMEM((3, 3, chans, chans), BF16),
                pltpu.VMEM((1, chans), F32),
                pltpu.VMEM((1, chans), F32),
                pltpu.SemaphoreType.DMA((3, 2)),
                pltpu.SemaphoreType.DMA((4,)),
                pltpu.SemaphoreType.DMA((4,)),
                pltpu.SemaphoreType.DMA((4,)),
            ]
            + [pltpu.SemaphoreType.DMA] * 6,
            compiler_params=pltpu.CompilerParams(
                collective_id=0, has_side_effects=True, vmem_limit_bytes=24 << 20
            ),
            name="conv",
        )(*(pltpu.with_memory_space_constraint(a, pltpu.HBM) for a in args))
        out = pl.pallas_call(
            tail_kernel,
            out_shape=jax.ShapeDtypeStruct((tile_h, tile_j, 2, images, chans), F32),
            in_specs=[vmem] * len(kept),
            out_specs=pl.BlockSpec(memory_space=pl.ANY),
            scratch_shapes=[
                pltpu.VMEM((2, tile_j, 2, images, chans), F32),
                pltpu.SemaphoreType.DMA((2,)),
            ],
            compiler_params=pltpu.CompilerParams(vmem_limit_bytes=8 << 20),
            name="tail",
        )(*state)
        out = out.reshape(tile_h, 2 * tile_j, images, chans)
        return jnp.transpose(out, (2, 0, 1, 3))

    group = ("model", "cols")
    return jax.shard_map(
        run_local,
        mesh=mesh,
        in_specs=(P("data", None, None, group), P(None, None, group, None), P(), P(), P()),
        out_specs=P("data", "model", "cols", None),
        check_vma=False,
    )
```

```python
import functools

import jax
import jax.numpy as jnp
from jax import lax
from jax.experimental import pallas as pl
from jax.experimental.pallas import tpu as pltpu
from jax.sharding import PartitionSpec as P

MESH = pl.DeviceIdType.MESH
BF16 = jnp.bfloat16
F32 = jnp.float32
CHUNK_ROWS = (2, 3, 2)
TURNS, FIRSTS, SECONDS = (2, 4, 5, 6), (1, 3, 4, 5), (0, 2, 3, 3)
EARLY_FROM = 1
AHEAD = (1, 0)
CHIPS_ALONG = (3, 1, 2, 0)
CHIP_ORDER = tuple((other, dy) for other in (0, 1) for dy in (0, 1, -1, 2))


def turn(recv, i, put):
    sources, _, win_j, own_chans, lanes = recv.shape
    chans = sources * own_chans
    for j in range(win_j):
        top = recv[:, 2 * i, j].reshape(chans, lanes)
        under = recv[:, 2 * i + 1, j].reshape(chans, lanes)
        put(j, jnp.concatenate([top, under], axis=0).T.reshape(2, lanes // 2, 2 * chans))


def blocks(pairs, weights, count):
    acc = None
    for dw in range(4):
        parts = [view[dw // 2 : dw // 2 + count, dw % 2] for view in pairs]
        lhs = jnp.concatenate([p.reshape(count * p.shape[1], p.shape[2]) for p in parts], axis=1)
        term = jnp.dot(lhs, weights(dw), preferred_element_type=F32)
        acc = term if acc is None else acc + term
    return acc


def first(pairs, weights, bias, y_row, blank_a):
    count, _, images, lanes = y_row.shape
    c = lax.axis_index("cols")
    row = lax.rem(lax.broadcasted_iota(jnp.int32, (1, 2 * lanes), 1), lanes) // (lanes // 2)
    act = jnp.maximum(blocks(pairs, weights, count) + bias, 0.0)
    act = jnp.where(row != blank_a, act, 0.0).astype(BF16)
    for b in range(2):
        y_row[:, b] = act[:, b * lanes : (b + 1) * lanes].reshape(count, images, lanes)
    blank = jnp.zeros((images, lanes), BF16)

    @pl.when(c == 0)
    def _():
        y_row[0, 0] = blank

    @pl.when(c == lax.axis_size("cols") - 1)
    def _():
        y_row[count - 1, 1] = blank


def second(pairs, weights, bias, out_pair):
    _, count, _, images, chans = out_pair.shape
    res = blocks(pairs, weights, count) + bias
    for b in range(2):
        for a in range(2):
            at = (2 * b + a) * chans
            out_pair[a, :, b] = res[:, at : at + chans].reshape(count, images, chans)


def conv_kernel(
    n_rows,
    n_cols,
    x_hbm,
    w1_hbm,
    b1_hbm,
    w2_hbm,
    b2_hbm,
    out,
    ymat,
    wt2,
    bias2,
    recv,
    xmat,
    wt1,
    bias1,
    xs,
    packed,
    w1s,
    w1own,
    w1all,
    w2s,
    b1s,
    b2s,
    load_sem,
    par_sem,
    send_sem,
    recv_sem,
    wsend_sem,
    wrecv_sem,
    swap_send_sem,
    swap_recv_sem,
    wswap_send_sem,
    wswap_recv_sem,
):
    chip_h, pairs = xs.shape[1:3]
    images = xs.shape[-1]
    tile_h, tile_j = chip_h // 2, pairs // n_cols
    win_j = tile_j + 2
    sources = n_rows * n_cols
    r, c = lax.axis_index("model"), lax.axis_index("cols")
    par = lax.rem(r, 2)
    me = r * n_cols + c
    chans = recv.shape[0] * 2

    tops = [tile_h - sum(CHUNK_ROWS[: k + 1]) for k in range(len(CHUNK_ROWS))]
    groups = (
        ((tops[0], chip_h - tops[0]),),
        *(((k, k + n), (chip_h - k - n, chip_h - k)) for k, n in zip(tops[1:], CHUNK_ROWS[1:])),
    )
    loads = []
    for g, spans in enumerate(groups):
        loads.append(
            [
                pltpu.make_async_copy(x_hbm.at[:, lo:hi], xs.at[:, lo:hi], load_sem.at[g, n])
                for n, (lo, hi) in enumerate(spans)
            ]
        )
    for copies in loads:
        for copy in copies:
            copy.start()
    params = [
        pltpu.make_async_copy(src, dst, par_sem.at[s])
        for s, (src, dst) in enumerate(((w1_hbm, w1s), (w2_hbm, w2s), (b1_hbm, b1s), (b2_hbm, b2s)))
    ]
    for copy in params:
        copy.start()

    barrier = pltpu.get_barrier_semaphore()
    to_cs = [lax.rem(c + k, n_cols) for k in range(n_cols)]

    def device(to_r, to_c):
        return {"model": to_r, "cols": to_c}

    to_rs = [lax.rem(r + k, n_rows) for k in range(n_rows)]
    for kr, kc in sorted(
        ((kr, kc) for kr in range(n_rows) for kc in range(n_cols) if kr or kc),
        key=lambda k: (k[1] not in (1, 2), k[0] not in (2, 3, 4, 5), k[1] == 2, k[0] < 4, -min(k[0], n_rows - k[0])),
    ):
        pl.semaphore_signal(barrier, inc=1, device_id=device(to_rs[kr], to_cs[kc]), device_id_type=MESH)

    ahead_r, ahead_c = AHEAD
    is_ahead = (r == ahead_r) & (c == ahead_c)

    def pack_rows(x, lo, hi):
        rows = hi - lo
        left, right = (xs[x, lo:hi, :, p].reshape(rows * pairs * 2, images) for p in range(2))
        both = jnp.concatenate([left, right], axis=1)
        packed[pl.ds(chip_h * x + lo, rows)] = both.reshape(rows, pairs, 2, 2 * images)

    def pack(g):
        for n, copy in enumerate(loads[g]):
            if (g, n) != (1, ahead_r % 2):
                copy.wait()

        def body(x, carry):
            for n, (lo, hi) in enumerate(groups[g]):
                if (g, n) == (1, ahead_r % 2):
                    pl.when(x != ahead_r // 2)(lambda lo=lo, hi=hi: pack_rows(x, lo, hi))
                else:
                    pack_rows(x, lo, hi)
            return carry

        lax.fori_loop(0, n_rows // 2, body, 0)

    last = tile_h + 4

    def rows_of(offset, count):
        def where(to_r):
            q = lax.rem(to_r, 2)
            src = tile_h * to_r + offset + (tile_h - count - 2 * offset) * q
            dst = offset + 2 + (last - count - 2 * offset - 3) * q
            return src, dst

        return where

    chunks = (
        *((n, rows_of(k, n), False) for k, n in zip(tops, CHUNK_ROWS)),
        (2, rows_of(-2, 2), True),
    )
    no_outer = (r == 0) | (r == n_rows - 1)
    at_edge = (c == 0) | (c == n_cols - 1)
    own_j = c == 0
    own_j = own_j.astype(jnp.int32)

    def send_tile(chunk, to_r, to_c, there):
        rows, where, is_outer = chunks[chunk]
        src, dst = where(to_r)
        skip = (to_c == 0).astype(jnp.int32)
        edge = (to_c == 0) | (to_c == n_cols - 1)
        if is_outer:
            there = there & (to_r > 0) & (to_r < n_rows - 1)

        def copy(count, src_j, dst_j):
            pltpu.make_async_remote_copy(
                src_ref=packed.at[pl.ds(src, rows), pl.ds(src_j, count)],
                dst_ref=recv.at[me, pl.ds(dst, rows), pl.ds(dst_j, count)],
                send_sem=send_sem.at[chunk],
                recv_sem=recv_sem.at[chunk],
                device_id=device(to_r, to_c),
                device_id_type=MESH,
            ).start()

        pl.when(there & edge)(lambda: copy(win_j - 1, tile_j * to_c - 1 + skip, skip))
        pl.when(there & jnp.logical_not(edge))(lambda: copy(win_j, tile_j * to_c - 1, 0))

    chips = n_rows // 2

    def step(t, table):
        value = jnp.int32(table[-1])
        for k, entry in enumerate(table[:-1]):
            value = jnp.where(t == k, entry, value)
        return value

    def turn_to(t):
        dx = step(t, CHIPS_ALONG)
        return lax.rem(r // 2 + dx, chips), dx

    def send_chip(chunk, t, where=None):
        x, dx = turn_to(t)
        way = 1 - 2 * lax.rem(par + t, 2)
        for other, dy in CHIP_ORDER:
            to_r = 2 * x + (1 - par if other else par)
            to_c = lax.rem(c + way * dy + n_cols, n_cols)
            there = True
            if not other and dy == 0:
                there = dx > 0
            if where is not None:
                there = there & where(to_r, to_c)
            send_tile(chunk, to_r, to_c, there)

    def send_chunk(chunk):
        early = EARLY_FROM <= chunk

        def body(t, carry):
            if chunk > EARLY_FROM:
                send_chip(chunk, t, lambda to_r, to_c: to_c > 0)
            else:
                send_chip(chunk, t, lambda to_r, to_c: (to_r != ahead_r) | (to_c != ahead_c))
            if early and chunk + 1 < len(chunks):
                x, dx = turn_to(t)
                for other in range(2):
                    to_r = 2 * x + (1 - par if other else par)
                    there = (to_r != r) | (c != 0)
                    if chunk > EARLY_FROM:
                        there = there & (to_r != ahead_r)
                    send_tile(chunk + 1, to_r, jnp.int32(0), there)
                if chunk == EARLY_FROM:
                    there = (x == ahead_r // 2) & jnp.logical_not(is_ahead)
                    send_tile(len(chunks) - 1, jnp.int32(ahead_r), jnp.int32(ahead_c), there)
            return carry

        lax.fori_loop(0, chips, body, 0)

    params[0].wait()
    for dw in range(3):
        w1own[dw] = jnp.concatenate([w1s[1, dw], w1s[0, dw]], axis=1)
    w1own[3] = jnp.concatenate([w1s[2, 0], w1s[2, 1]], axis=1)
    w1own[4] = jnp.concatenate([w1s[2, 2], jnp.zeros_like(w1s[2, 2])], axis=1)
    w1all[r // 2, par, c] = w1own[...]

    for copy in loads[0]:
        copy.wait()
    pack_rows(turn_to(0)[0], *groups[0][0])
    pl.semaphore_wait(barrier, sources - 1)

    def send_weights():
        for kr in range(0, n_rows, 2):
            for kc in range(n_cols):
                if kr or kc:
                    pltpu.make_async_remote_copy(
                        src_ref=w1own,
                        dst_ref=w1all.at[r // 2, par, c],
                        send_sem=wsend_sem,
                        recv_sem=wrecv_sem,
                        device_id=device(to_rs[kr], to_cs[kc]),
                        device_id_type=MESH,
                    ).start()

    def pack_and_send(t, carry):
        pl.when(t < chips - 1)(lambda: pack_rows(turn_to(t + 1)[0], *groups[0][0]))
        there = turn_to(t)[0] == ahead_r // 2

        @pl.when(there)
        def _():
            loads[1][ahead_r % 2].wait()
            pack_rows(ahead_r // 2, *groups[1][ahead_r % 2])

        send_chip(0, t)
        send_tile(1, jnp.int32(ahead_r), jnp.int32(ahead_c), there & jnp.logical_not(is_ahead))
        pl.when(t == 1)(send_weights)
        return carry

    lax.fori_loop(0, chips, pack_and_send, 0)

    for g in range(1, EARLY_FROM + 1):
        pack(g)
    for chunk in range(1, len(chunks)):
        if chunk >= EARLY_FROM and chunk + 1 < len(groups):
            pack(chunk + 1)
        send_chunk(chunk)

    def wait_bytes(ref, sem):
        pltpu.make_async_copy(ref, ref, sem).wait()

    w1_bytes = recv.at[0 : sources // 2 - 1, 0, 0:5]
    wait_bytes(w1_bytes, wrecv_sem)
    wait_bytes(w1_bytes, wsend_sem)
    partner = device(r + 1 - 2 * par, c)
    w_swap = pltpu.make_async_remote_copy(
        src_ref=w1all.at[:, par],
        dst_ref=w1all.at[:, par],
        send_sem=wswap_send_sem,
        recv_sem=wswap_recv_sem,
        device_id=partner,
        device_id_type=MESH,
    )
    w_swap.start()

    def own_rows(chunk):
        rows, where, _ = chunks[chunk]
        src, dst = where(r)

        def copy(count, src_j, dst_j):
            for h in range(rows):
                recv[me, dst + h, pl.ds(dst_j, count)] = packed[src + h, pl.ds(src_j, count)]

        pl.when(at_edge)(lambda: copy(win_j - 1, tile_j * c - 1 + own_j, own_j))
        pl.when(jnp.logical_not(at_edge))(lambda: copy(win_j, tile_j * c - 1, 0))

    for chunk in range(3):
        own_rows(chunk)
    pl.when(jnp.logical_not(no_outer))(lambda: own_rows(3))

    zero_row = jnp.zeros((win_j, 2, 2 * images), BF16)
    zero_col = jnp.zeros((tile_h + 2, 2, 2 * images), BF16)

    def clear(s, carry):
        recv[s, last * (1 - par)] = zero_row
        return carry

    def clear_outer(s, carry):
        recv[s, (last - 1) * par] = zero_row
        recv[s, (last - 1) * par + 1] = zero_row
        return carry

    def clear_edge(s, carry):
        recv[s, pl.ds(3 * par, tile_h + 2), (win_j - 1) * (1 - own_j)] = zero_col
        return carry

    lax.fori_loop(0, sources, clear, 0)
    pl.when(no_outer)(lambda: (lax.fori_loop(0, sources, clear_outer, 0), None)[1])
    pl.when(at_edge)(lambda: (lax.fori_loop(0, sources, clear_edge, 0), None)[1])

    low = lax.broadcasted_iota(jnp.int32, (chans, 2 * chans), 1) < chans

    def spread(wt, u, v, dw):
        ur, vr = pltpu.roll(u, chans, 1), pltpu.roll(v, chans, 1)
        zero = jnp.zeros_like(u)
        tiles = (jnp.where(low, ur, zero), u, jnp.where(low, v, ur), jnp.where(low, zero, vr))
        for k, tile in enumerate(tiles):
            tile = tile.astype(BF16)
            for b in range(2):
                wt[dw + b, k * chans : (k + 1) * chans, b * 2 * chans : (b + 1) * 2 * chans] = tile

    def blank(wt):
        zero = jnp.zeros((4 * chans, 2 * chans), BF16)
        wt[3, :, 0 : 2 * chans] = zero
        wt[0, :, 2 * chans : 4 * chans] = zero

    for copy in params[1:]:
        copy.wait()
    blank(wt1)
    blank(wt2)
    for dw in range(3):
        w = [w2s[dh, dw].astype(F32) for dh in range(3)]
        spread(
            wt2,
            jnp.concatenate([w[1], w[0]], axis=1),
            jnp.concatenate([w[2], jnp.zeros_like(w[2])], axis=1),
            dw,
        )
    bias1[...] = jnp.concatenate([b1s[...]] * 4, axis=1)
    bias2[...] = jnp.concatenate([b2s[...]] * 4, axis=1)

    def arrived(chunk):
        def wait(count):
            wait_bytes(recv.at[0 : sources - 1, 0 : chunks[chunk][0], 0:count], recv_sem.at[chunk])

        pl.when(at_edge)(lambda: wait(win_j - 1))
        pl.when(jnp.logical_not(at_edge))(lambda: wait(win_j))

    arrived(0)
    give = tile_h - (tile_h - 3) * par
    land = tile_h + 2 - (tile_h + 1) * (1 - par)
    swap = pltpu.make_async_remote_copy(
        src_ref=recv.at[:, pl.ds(give, 2)],
        dst_ref=recv.at[:, pl.ds(land, 2)],
        send_sem=swap_send_sem,
        recv_sem=swap_recv_sem,
        device_id=partner,
        device_id_type=MESH,
    )
    swap.start()

    w_swap.wait()
    u = [w1all[:, :, :, k].reshape(chans, 2 * chans).astype(F32) for k in range(5)]
    for dw in range(3):
        v = (u[3], pltpu.roll(u[3], chans, 1), u[4])[dw]
        spread(wt1, u[dw], jnp.where(low, v, 0.0), dw)

    x_pairs, z_pairs = xmat.shape[0], ymat.shape[0]
    o_pairs = z_pairs - 1

    def nth(n, count):
        return (count - 1) * (1 - par) + n * (2 * par - 1)

    def turn_one(n, carry):
        i = nth(n, x_pairs)

        def put(j, value):
            xmat[i, j] = value

        turn(recv, i, put)
        return carry

    def first_one(n, carry):
        i = nth(n, z_pairs)
        fill = jnp.where(n == 0, 1 - par, 2)
        out_of = jnp.where(n == z_pairs - 1, jnp.where(r == 0, 0, jnp.where(r == n_rows - 1, 1, 2)), 2)
        blank_a = jnp.where(fill < 2, fill, out_of)
        first((xmat.at[i], xmat.at[i + 1]), lambda dw: wt1[dw], bias1[...], ymat.at[i], blank_a)
        return carry

    def second_one(n, carry):
        i = nth(n, o_pairs)
        second((ymat.at[i], ymat.at[i + 1]), lambda dw: wt2[dw], bias2[...], out.at[pl.ds(2 * i, 2)])
        return carry

    def stage(s, carry):
        @pl.when(s == 0)
        def _():
            swap.wait()

        for k in range(1, 4):
            there = s == k
            if k == 3:
                there = there & jnp.logical_not(no_outer)
            pl.when(there)(lambda k=k: arrived(k))

        for ends, one in ((TURNS, turn_one), (FIRSTS, first_one), (SECONDS, second_one)):
            lax.fori_loop(step(s, (0, *ends[:-1])), step(s, ends), one, 0)
        return carry

    lax.fori_loop(0, 4, stage, 0)

    per_edge = n_rows * 2
    for chunk in range(4):
        rows = chunks[chunk][0]
        n_r = n_rows - 2 if chunk == 3 else n_rows
        counts = (n_r * 2, n_r * (n_cols - 2))

        def drain(edge_n, inner_n, rows=rows, chunk=chunk):
            wait_bytes(recv.at[0:edge_n, 0:rows, 0 : win_j - 1], send_sem.at[chunk])
            wait_bytes(recv.at[0:inner_n, 0:rows, 0:win_j], send_sem.at[chunk])

        def drain_own(chunk=chunk, counts=counts, drain=drain):
            pl.when(at_edge)(lambda: drain(counts[0] - 1, counts[1]))
            pl.when(jnp.logical_not(at_edge))(lambda: drain(counts[0], counts[1] - 1))

        if chunk == 3:
            pl.when(no_outer)(lambda: drain(*counts))
            pl.when(jnp.logical_not(no_outer))(drain_own)
        else:
            drain_own()


def tail_kernel(tile, ymat, wt2, bias2, out_hbm, o_new, sem):
    par = lax.rem(lax.axis_index("model"), 2)
    rows = out_hbm.shape[0]
    o_pairs = ymat.shape[0] - 1
    late = (rows - 2) * par
    here = 2 * (1 - par)

    width = out_hbm.shape[1]
    parts = [pl.ds(j, 1) for j in range(width)]

    def start(k, carry):
        for part in parts:
            pltpu.make_async_copy(tile.at[par + k, part], out_hbm.at[k, part], sem.at[0]).start()
        return carry

    lax.fori_loop(here, here + rows - 2, start, 0)
    i = (o_pairs - 1) * par
    second((ymat.at[i], ymat.at[i + 1]), lambda dw: wt2[dw], bias2[...], o_new)
    for k in range(2):
        for part in parts:
            pltpu.make_async_copy(o_new.at[k, part], out_hbm.at[late + k, part], sem.at[1]).start()
    pltpu.make_async_copy(tile.at[0 : rows - 2], out_hbm.at[0 : rows - 2], sem.at[0]).wait()
    pltpu.make_async_copy(o_new, out_hbm.at[pl.ds(late, 2)], sem.at[1]).wait()


def solution(mesh):
    n_rows = mesh.shape["model"]
    n_cols = mesh.shape["cols"]

    def run_local(x_in, w_conv1, b_conv1, w_conv2, b_conv2):
        images, height, width, own_chans = x_in.shape
        sources = n_rows * n_cols
        chans = own_chans * sources
        pairs = width // 2
        tile_h, tile_j = height // n_rows, pairs // n_cols
        win_j = tile_j + 2
        x_pairs, z_pairs = (tile_h + 5) // 2, (tile_h + 3) // 2
        x_t = jnp.transpose(x_in, (1, 2, 3, 0)).reshape(n_rows // 2, 2 * tile_h, pairs, 2, own_chans, images)
        args = (x_t, w_conv1, b_conv1.reshape(1, chans), w_conv2, b_conv2.reshape(1, chans))
        hbm = pl.BlockSpec(memory_space=pltpu.HBM)
        vmem = pl.BlockSpec(memory_space=pltpu.VMEM)
        kept = (
            pltpu.VMEM((2 * (z_pairs - 1), tile_j, 2, images, chans), F32),
            pltpu.VMEM((z_pairs, win_j - 1, 2, images, 2 * chans), BF16),
            pltpu.VMEM((4, 4 * chans, 4 * chans), BF16),
            pltpu.VMEM((1, 4 * chans), F32),
        )
        state = pl.pallas_call(
            functools.partial(conv_kernel, n_rows, n_cols),
            out_shape=kept,
            in_specs=[hbm] * 5,
            out_specs=[vmem] * len(kept),
            scratch_shapes=[
                pltpu.VMEM((sources, 2 * x_pairs, win_j, own_chans, 2 * images), BF16),
                pltpu.VMEM((x_pairs, win_j, 2, images, 2 * chans), BF16),
                pltpu.VMEM((4, 4 * chans, 4 * chans), BF16),
                pltpu.VMEM((1, 4 * chans), F32),
                pltpu.VMEM((n_rows // 2, 2 * tile_h, pairs, 2, own_chans, images), BF16),
                pltpu.VMEM((height, pairs, own_chans, 2 * images), BF16),
                pltpu.VMEM((3, 3, own_chans, chans), BF16),
                pltpu.VMEM((5, own_chans, 2 * chans), BF16),
                pltpu.VMEM((n_rows // 2, 2, n_cols, 5, own_chans, 2 * chans), BF16),
                pltpu.VMEM((3, 3, chans, chans), BF16),
                pltpu.VMEM((1, chans), F32),
                pltpu.VMEM((1, chans), F32),
                pltpu.SemaphoreType.DMA((3, 2)),
                pltpu.SemaphoreType.DMA((4,)),
                pltpu.SemaphoreType.DMA((4,)),
                pltpu.SemaphoreType.DMA((4,)),
            ]
            + [pltpu.SemaphoreType.DMA] * 6,
            compiler_params=pltpu.CompilerParams(
                collective_id=0, has_side_effects=True, vmem_limit_bytes=24 << 20
            ),
            name="conv",
        )(*(pltpu.with_memory_space_constraint(a, pltpu.HBM) for a in args))
        out = pl.pallas_call(
            tail_kernel,
            out_shape=jax.ShapeDtypeStruct((tile_h, tile_j, 2, images, chans), F32),
            in_specs=[vmem] * len(kept),
            out_specs=pl.BlockSpec(memory_space=pl.ANY),
            scratch_shapes=[
                pltpu.VMEM((2, tile_j, 2, images, chans), F32),
                pltpu.SemaphoreType.DMA((2,)),
            ],
            compiler_params=pltpu.CompilerParams(vmem_limit_bytes=8 << 20),
            name="tail",
        )(*state)
        out = out.reshape(tile_h, 2 * tile_j, images, chans)
        return jnp.transpose(out, (2, 0, 1, 3))

    group = ("model", "cols")
    return jax.shard_map(
        run_local,
        mesh=mesh,
        in_specs=(P("data", None, None, group), P(None, None, group, None), P(), P(), P()),
        out_specs=P("data", "model", "cols", None),
        check_vma=False,
    )
```

```python
import functools

import jax
import jax.numpy as jnp
from jax import lax
from jax.experimental import pallas as pl
from jax.experimental.pallas import tpu as pltpu
from jax.sharding import PartitionSpec as P

MESH = pl.DeviceIdType.MESH
BF16 = jnp.bfloat16
F32 = jnp.float32
CHUNK_ROWS = (2, 3, 2)
TURNS, FIRSTS, SECONDS = (2, 4, 5, 6), (1, 3, 4, 5), (0, 2, 3, 3)
EARLY_FROM = 1
AHEAD = (1, 0)
CHIPS_ALONG = (3, 1, 2, 0)
CHIP_ORDER = tuple((other, dy) for other in (0, 1) for dy in (0, 1, -1, 2))


def turn(recv, i, put):
    sources, _, win_j, own_chans, lanes = recv.shape
    chans = sources * own_chans
    for j in range(win_j):
        top = recv[:, 2 * i, j].reshape(chans, lanes)
        under = recv[:, 2 * i + 1, j].reshape(chans, lanes)
        put(j, jnp.concatenate([top, under], axis=0).T.reshape(2, lanes // 2, 2 * chans))


def blocks(pairs, weights, count):
    acc = None
    for dw in range(4):
        parts = [view[dw // 2 : dw // 2 + count, dw % 2] for view in pairs]
        lhs = jnp.concatenate([p.reshape(count * p.shape[1], p.shape[2]) for p in parts], axis=1)
        term = jnp.dot(lhs, weights(dw), preferred_element_type=F32)
        acc = term if acc is None else acc + term
    return acc


def first(pairs, weights, bias, y_row, blank_a):
    count, _, images, lanes = y_row.shape
    c = lax.axis_index("cols")
    row = lax.rem(lax.broadcasted_iota(jnp.int32, (1, 2 * lanes), 1), lanes) // (lanes // 2)
    act = jnp.maximum(blocks(pairs, weights, count) + bias, 0.0)
    act = jnp.where(row != blank_a, act, 0.0).astype(BF16)
    for b in range(2):
        y_row[:, b] = act[:, b * lanes : (b + 1) * lanes].reshape(count, images, lanes)
    blank = jnp.zeros((images, lanes), BF16)

    @pl.when(c == 0)
    def _():
        y_row[0, 0] = blank

    @pl.when(c == lax.axis_size("cols") - 1)
    def _():
        y_row[count - 1, 1] = blank


def second(pairs, weights, bias, out_pair):
    _, count, _, images, chans = out_pair.shape
    res = blocks(pairs, weights, count) + bias
    for b in range(2):
        for a in range(2):
            at = (2 * b + a) * chans
            out_pair[a, :, b] = res[:, at : at + chans].reshape(count, images, chans)


def conv_kernel(
    n_rows,
    n_cols,
    x_hbm,
    w1_hbm,
    b1_hbm,
    w2_hbm,
    b2_hbm,
    out,
    ymat,
    wt2,
    bias2,
    recv,
    xmat,
    wt1,
    bias1,
    xs,
    packed,
    w1s,
    w1own,
    w1all,
    w2s,
    b1s,
    b2s,
    load_sem,
    par_sem,
    send_sem,
    recv_sem,
    wsend_sem,
    wrecv_sem,
    swap_send_sem,
    swap_recv_sem,
    wswap_send_sem,
    wswap_recv_sem,
):
    chip_h, pairs = xs.shape[1:3]
    images = xs.shape[-1]
    tile_h, tile_j = chip_h // 2, pairs // n_cols
    win_j = tile_j + 2
    sources = n_rows * n_cols
    r, c = lax.axis_index("model"), lax.axis_index("cols")
    par = lax.rem(r, 2)
    me = r * n_cols + c
    chans = recv.shape[0] * 2

    tops = [tile_h - sum(CHUNK_ROWS[: k + 1]) for k in range(len(CHUNK_ROWS))]
    groups = (
        ((tops[0], chip_h - tops[0]),),
        *(((k, k + n), (chip_h - k - n, chip_h - k)) for k, n in zip(tops[1:], CHUNK_ROWS[1:])),
    )
    loads = []
    for g, spans in enumerate(groups):
        loads.append(
            [
                pltpu.make_async_copy(x_hbm.at[:, lo:hi], xs.at[:, lo:hi], load_sem.at[g, n])
                for n, (lo, hi) in enumerate(spans)
            ]
        )
    for copies in loads:
        for copy in copies:
            copy.start()
    params = [
        pltpu.make_async_copy(src, dst, par_sem.at[s])
        for s, (src, dst) in enumerate(((w1_hbm, w1s), (w2_hbm, w2s), (b1_hbm, b1s), (b2_hbm, b2s)))
    ]
    for copy in params:
        copy.start()

    barrier = pltpu.get_barrier_semaphore()
    to_cs = [lax.rem(c + k, n_cols) for k in range(n_cols)]

    def device(to_r, to_c):
        return {"model": to_r, "cols": to_c}

    to_rs = [lax.rem(r + k, n_rows) for k in range(n_rows)]
    for kr, kc in sorted(
        ((kr, kc) for kr in range(n_rows) for kc in range(n_cols) if kr or kc),
        key=lambda k: (k[1] not in (1, 2), k[0] not in (2, 3, 4, 5), k[1] == 2, k[0] < 4, -min(k[0], n_rows - k[0])),
    ):
        pl.semaphore_signal(barrier, inc=1, device_id=device(to_rs[kr], to_cs[kc]), device_id_type=MESH)

    ahead_r, ahead_c = AHEAD
    is_ahead = (r == ahead_r) & (c == ahead_c)

    def pack_rows(x, lo, hi):
        rows = hi - lo
        left, right = (xs[x, lo:hi, :, p].reshape(rows * pairs * 2, images) for p in range(2))
        both = jnp.concatenate([left, right], axis=1)
        packed[pl.ds(chip_h * x + lo, rows)] = both.reshape(rows, pairs, 2, 2 * images)

    def pack(g):
        for n, copy in enumerate(loads[g]):
            if (g, n) != (1, ahead_r % 2):
                copy.wait()

        def body(x, carry):
            for n, (lo, hi) in enumerate(groups[g]):
                if (g, n) == (1, ahead_r % 2):
                    pl.when(x != ahead_r // 2)(lambda lo=lo, hi=hi: pack_rows(x, lo, hi))
                else:
                    pack_rows(x, lo, hi)
            return carry

        lax.fori_loop(0, n_rows // 2, body, 0)

    last = tile_h + 4

    def rows_of(offset, count):
        def where(to_r):
            q = lax.rem(to_r, 2)
            src = tile_h * to_r + offset + (tile_h - count - 2 * offset) * q
            dst = offset + 2 + (last - count - 2 * offset - 3) * q
            return src, dst

        return where

    chunks = (
        *((n, rows_of(k, n), False) for k, n in zip(tops, CHUNK_ROWS)),
        (2, rows_of(-2, 2), True),
    )
    no_outer = (r == 0) | (r == n_rows - 1)
    at_edge = (c == 0) | (c == n_cols - 1)
    own_j = c == 0
    own_j = own_j.astype(jnp.int32)

    def send_tile(chunk, to_r, to_c, there):
        rows, where, is_outer = chunks[chunk]
        src, dst = where(to_r)
        skip = (to_c == 0).astype(jnp.int32)
        edge = (to_c == 0) | (to_c == n_cols - 1)
        if is_outer:
            there = there & (to_r > 0) & (to_r < n_rows - 1)

        def copy(count, src_j, dst_j):
            pltpu.make_async_remote_copy(
                src_ref=packed.at[pl.ds(src, rows), pl.ds(src_j, count)],
                dst_ref=recv.at[me, pl.ds(dst, rows), pl.ds(dst_j, count)],
                send_sem=send_sem.at[chunk],
                recv_sem=recv_sem.at[chunk],
                device_id=device(to_r, to_c),
                device_id_type=MESH,
            ).start()

        pl.when(there & edge)(lambda: copy(win_j - 1, tile_j * to_c - 1 + skip, skip))
        pl.when(there & jnp.logical_not(edge))(lambda: copy(win_j, tile_j * to_c - 1, 0))

    chips = n_rows // 2

    def step(t, table):
        value = jnp.int32(table[-1])
        for k, entry in enumerate(table[:-1]):
            value = jnp.where(t == k, entry, value)
        return value

    def turn_to(t):
        dx = step(t, CHIPS_ALONG)
        return lax.rem(r // 2 + dx, chips), dx

    def send_chip(chunk, t, where=None):
        x, dx = turn_to(t)
        way = 1 - 2 * lax.rem(par + t, 2)
        for other, dy in CHIP_ORDER:
            to_r = 2 * x + (1 - par if other else par)
            to_c = lax.rem(c + way * dy + n_cols, n_cols)
            there = True
            if not other and dy == 0:
                there = dx > 0
            if where is not None:
                there = there & where(to_r, to_c)
            send_tile(chunk, to_r, to_c, there)

    def send_chunk(chunk):
        early = EARLY_FROM <= chunk

        def body(t, carry):
            if chunk > EARLY_FROM:
                send_chip(chunk, t, lambda to_r, to_c: to_c > 0)
            else:
                send_chip(chunk, t, lambda to_r, to_c: (to_r != ahead_r) | (to_c != ahead_c))
            if early and chunk + 1 < len(chunks):
                x, dx = turn_to(t)
                for other in range(2):
                    to_r = 2 * x + (1 - par if other else par)
                    there = (to_r != r) | (c != 0)
                    if chunk > EARLY_FROM:
                        there = there & (to_r != ahead_r)
                    send_tile(chunk + 1, to_r, jnp.int32(0), there)
                if chunk == EARLY_FROM:
                    there = (x == ahead_r // 2) & jnp.logical_not(is_ahead)
                    send_tile(len(chunks) - 1, jnp.int32(ahead_r), jnp.int32(ahead_c), there)
            return carry

        lax.fori_loop(0, chips, body, 0)

    params[0].wait()
    for dw in range(3):
        w1own[dw] = jnp.concatenate([w1s[1, dw], w1s[0, dw]], axis=1)
    w1own[3] = jnp.concatenate([w1s[2, 0], w1s[2, 1]], axis=1)
    w1own[4] = jnp.concatenate([w1s[2, 2], jnp.zeros_like(w1s[2, 2])], axis=1)
    w1all[r // 2, par, c] = w1own[...]

    for copy in loads[0]:
        copy.wait()
    pack_rows(turn_to(0)[0], *groups[0][0])
    pl.semaphore_wait(barrier, sources - 1)

    def send_weights():
        for kr in range(0, n_rows, 2):
            for kc in range(n_cols):
                if kr or kc:
                    pltpu.make_async_remote_copy(
                        src_ref=w1own,
                        dst_ref=w1all.at[r // 2, par, c],
                        send_sem=wsend_sem,
                        recv_sem=wrecv_sem,
                        device_id=device(to_rs[kr], to_cs[kc]),
                        device_id_type=MESH,
                    ).start()

    def pack_and_send(t, carry):
        pl.when(t < chips - 1)(lambda: pack_rows(turn_to(t + 1)[0], *groups[0][0]))
        there = turn_to(t)[0] == ahead_r // 2

        @pl.when(there)
        def _():
            loads[1][ahead_r % 2].wait()
            pack_rows(ahead_r // 2, *groups[1][ahead_r % 2])

        send_chip(0, t)
        send_tile(1, jnp.int32(ahead_r), jnp.int32(ahead_c), there & jnp.logical_not(is_ahead))
        pl.when(t == 1)(send_weights)
        return carry

    lax.fori_loop(0, chips, pack_and_send, 0)

    for g in range(1, EARLY_FROM + 1):
        pack(g)
    for chunk in range(1, len(chunks)):
        if chunk >= EARLY_FROM and chunk + 1 < len(groups):
            pack(chunk + 1)
        send_chunk(chunk)

    def wait_bytes(ref, sem):
        pltpu.make_async_copy(ref, ref, sem).wait()

    w1_bytes = recv.at[0 : sources // 2 - 1, 0, 0:5]
    wait_bytes(w1_bytes, wrecv_sem)
    wait_bytes(w1_bytes, wsend_sem)
    partner = device(r + 1 - 2 * par, c)
    w_swap = pltpu.make_async_remote_copy(
        src_ref=w1all.at[:, par],
        dst_ref=w1all.at[:, par],
        send_sem=wswap_send_sem,
        recv_sem=wswap_recv_sem,
        device_id=partner,
        device_id_type=MESH,
    )
    w_swap.start()

    def own_rows(chunk):
        rows, where, _ = chunks[chunk]
        src, dst = where(r)

        def copy(count, src_j, dst_j):
            for h in range(rows):
                recv[me, dst + h, pl.ds(dst_j, count)] = packed[src + h, pl.ds(src_j, count)]

        pl.when(at_edge)(lambda: copy(win_j - 1, tile_j * c - 1 + own_j, own_j))
        pl.when(jnp.logical_not(at_edge))(lambda: copy(win_j, tile_j * c - 1, 0))

    for chunk in range(3):
        own_rows(chunk)
    pl.when(jnp.logical_not(no_outer))(lambda: own_rows(3))

    zero_row = jnp.zeros((win_j, 2, 2 * images), BF16)
    zero_col = jnp.zeros((tile_h + 2, 2, 2 * images), BF16)

    def clear(s, carry):
        recv[s, last * (1 - par)] = zero_row
        return carry

    def clear_outer(s, carry):
        recv[s, (last - 1) * par] = zero_row
        recv[s, (last - 1) * par + 1] = zero_row
        return carry

    def clear_edge(s, carry):
        recv[s, pl.ds(3 * par, tile_h + 2), (win_j - 1) * (1 - own_j)] = zero_col
        return carry

    lax.fori_loop(0, sources, clear, 0)
    pl.when(no_outer)(lambda: (lax.fori_loop(0, sources, clear_outer, 0), None)[1])
    pl.when(at_edge)(lambda: (lax.fori_loop(0, sources, clear_edge, 0), None)[1])

    low = lax.broadcasted_iota(jnp.int32, (chans, 2 * chans), 1) < chans

    def spread(wt, u, v, dw):
        ur, vr = pltpu.roll(u, chans, 1), pltpu.roll(v, chans, 1)
        zero = jnp.zeros_like(u)
        tiles = (jnp.where(low, ur, zero), u, jnp.where(low, v, ur), jnp.where(low, zero, vr))
        for k, tile in enumerate(tiles):
            tile = tile.astype(BF16)
            for b in range(2):
                wt[dw + b, k * chans : (k + 1) * chans, b * 2 * chans : (b + 1) * 2 * chans] = tile

    def blank(wt):
        zero = jnp.zeros((4 * chans, 2 * chans), BF16)
        wt[3, :, 0 : 2 * chans] = zero
        wt[0, :, 2 * chans : 4 * chans] = zero

    for copy in params[1:]:
        copy.wait()
    blank(wt1)
    blank(wt2)
    for dw in range(3):
        w = [w2s[dh, dw].astype(F32) for dh in range(3)]
        spread(
            wt2,
            jnp.concatenate([w[1], w[0]], axis=1),
            jnp.concatenate([w[2], jnp.zeros_like(w[2])], axis=1),
            dw,
        )
    bias1[...] = jnp.concatenate([b1s[...]] * 4, axis=1)
    bias2[...] = jnp.concatenate([b2s[...]] * 4, axis=1)

    def arrived(chunk):
        def wait(count):
            wait_bytes(recv.at[0 : sources - 1, 0 : chunks[chunk][0], 0:count], recv_sem.at[chunk])

        pl.when(at_edge)(lambda: wait(win_j - 1))
        pl.when(jnp.logical_not(at_edge))(lambda: wait(win_j))

    arrived(0)
    give = tile_h - (tile_h - 3) * par
    land = tile_h + 2 - (tile_h + 1) * (1 - par)
    swap = pltpu.make_async_remote_copy(
        src_ref=recv.at[:, pl.ds(give, 2)],
        dst_ref=recv.at[:, pl.ds(land, 2)],
        send_sem=swap_send_sem,
        recv_sem=swap_recv_sem,
        device_id=partner,
        device_id_type=MESH,
    )
    swap.start()

    w_swap.wait()
    u = [w1all[:, :, :, k].reshape(chans, 2 * chans).astype(F32) for k in range(5)]
    for dw in range(3):
        v = (u[3], pltpu.roll(u[3], chans, 1), u[4])[dw]
        spread(wt1, u[dw], jnp.where(low, v, 0.0), dw)

    x_pairs, z_pairs = xmat.shape[0], ymat.shape[0]
    o_pairs = z_pairs - 1

    def nth(n, count):
        return (count - 1) * (1 - par) + n * (2 * par - 1)

    def turn_one(n, carry):
        i = nth(n, x_pairs)

        def put(j, value):
            xmat[i, j] = value

        turn(recv, i, put)
        return carry

    def first_one(n, carry):
        i = nth(n, z_pairs)
        fill = jnp.where(n == 0, 1 - par, 2)
        out_of = jnp.where(n == z_pairs - 1, jnp.where(r == 0, 0, jnp.where(r == n_rows - 1, 1, 2)), 2)
        blank_a = jnp.where(fill < 2, fill, out_of)
        first((xmat.at[i], xmat.at[i + 1]), lambda dw: wt1[dw], bias1[...], ymat.at[i], blank_a)
        return carry

    def second_one(n, carry):
        i = nth(n, o_pairs)
        second((ymat.at[i], ymat.at[i + 1]), lambda dw: wt2[dw], bias2[...], out.at[pl.ds(2 * i, 2)])
        return carry

    def stage(s, carry):
        @pl.when(s == 0)
        def _():
            swap.wait()

        for k in range(1, 4):
            there = s == k
            if k == 3:
                there = there & jnp.logical_not(no_outer)
            pl.when(there)(lambda k=k: arrived(k))

        for ends, one in ((TURNS, turn_one), (FIRSTS, first_one), (SECONDS, second_one)):
            lax.fori_loop(step(s, (0, *ends[:-1])), step(s, ends), one, 0)
        return carry

    lax.fori_loop(0, 4, stage, 0)

    per_edge = n_rows * 2
    for chunk in range(4):
        rows = chunks[chunk][0]
        n_r = n_rows - 2 if chunk == 3 else n_rows
        counts = (n_r * 2, n_r * (n_cols - 2))

        def drain(edge_n, inner_n, rows=rows, chunk=chunk):
            wait_bytes(recv.at[0:edge_n, 0:rows, 0 : win_j - 1], send_sem.at[chunk])
            wait_bytes(recv.at[0:inner_n, 0:rows, 0:win_j], send_sem.at[chunk])

        def drain_own(chunk=chunk, counts=counts, drain=drain):
            pl.when(at_edge)(lambda: drain(counts[0] - 1, counts[1]))
            pl.when(jnp.logical_not(at_edge))(lambda: drain(counts[0], counts[1] - 1))

        if chunk == 3:
            pl.when(no_outer)(lambda: drain(*counts))
            pl.when(jnp.logical_not(no_outer))(drain_own)
        else:
            drain_own()


def tail_kernel(tile, ymat, wt2, bias2, out_hbm, o_new, sem):
    par = lax.rem(lax.axis_index("model"), 2)
    rows = out_hbm.shape[0]
    o_pairs = ymat.shape[0] - 1
    late = (rows - 2) * par
    here = 2 * (1 - par)

    width = out_hbm.shape[1]
    parts = [(pl.ds(j, 1), pl.ds(b, 1)) for j in range(width) for b in range(2)]

    def start(k, carry):
        for part in parts:
            pltpu.make_async_copy(tile.at[(par + k, *part)], out_hbm.at[(k, *part)], sem.at[0]).start()
        return carry

    lax.fori_loop(here, here + rows - 2, start, 0)
    i = (o_pairs - 1) * par
    second((ymat.at[i], ymat.at[i + 1]), lambda dw: wt2[dw], bias2[...], o_new)
    for k in range(2):
        for part in parts:
            pltpu.make_async_copy(o_new.at[(k, *part)], out_hbm.at[(late + k, *part)], sem.at[1]).start()
    pltpu.make_async_copy(tile.at[0 : rows - 2], out_hbm.at[0 : rows - 2], sem.at[0]).wait()
    pltpu.make_async_copy(o_new, out_hbm.at[pl.ds(late, 2)], sem.at[1]).wait()


def solution(mesh):
    n_rows = mesh.shape["model"]
    n_cols = mesh.shape["cols"]

    def run_local(x_in, w_conv1, b_conv1, w_conv2, b_conv2):
        images, height, width, own_chans = x_in.shape
        sources = n_rows * n_cols
        chans = own_chans * sources
        pairs = width // 2
        tile_h, tile_j = height // n_rows, pairs // n_cols
        win_j = tile_j + 2
        x_pairs, z_pairs = (tile_h + 5) // 2, (tile_h + 3) // 2
        x_t = jnp.transpose(x_in, (1, 2, 3, 0)).reshape(n_rows // 2, 2 * tile_h, pairs, 2, own_chans, images)
        args = (x_t, w_conv1, b_conv1.reshape(1, chans), w_conv2, b_conv2.reshape(1, chans))
        hbm = pl.BlockSpec(memory_space=pltpu.HBM)
        vmem = pl.BlockSpec(memory_space=pltpu.VMEM)
        kept = (
            pltpu.VMEM((2 * (z_pairs - 1), tile_j, 2, images, chans), F32),
            pltpu.VMEM((z_pairs, win_j - 1, 2, images, 2 * chans), BF16),
            pltpu.VMEM((4, 4 * chans, 4 * chans), BF16),
            pltpu.VMEM((1, 4 * chans), F32),
        )
        state = pl.pallas_call(
            functools.partial(conv_kernel, n_rows, n_cols),
            out_shape=kept,
            in_specs=[hbm] * 5,
            out_specs=[vmem] * len(kept),
            scratch_shapes=[
                pltpu.VMEM((sources, 2 * x_pairs, win_j, own_chans, 2 * images), BF16),
                pltpu.VMEM((x_pairs, win_j, 2, images, 2 * chans), BF16),
                pltpu.VMEM((4, 4 * chans, 4 * chans), BF16),
                pltpu.VMEM((1, 4 * chans), F32),
                pltpu.VMEM((n_rows // 2, 2 * tile_h, pairs, 2, own_chans, images), BF16),
                pltpu.VMEM((height, pairs, own_chans, 2 * images), BF16),
                pltpu.VMEM((3, 3, own_chans, chans), BF16),
                pltpu.VMEM((5, own_chans, 2 * chans), BF16),
                pltpu.VMEM((n_rows // 2, 2, n_cols, 5, own_chans, 2 * chans), BF16),
                pltpu.VMEM((3, 3, chans, chans), BF16),
                pltpu.VMEM((1, chans), F32),
                pltpu.VMEM((1, chans), F32),
                pltpu.SemaphoreType.DMA((3, 2)),
                pltpu.SemaphoreType.DMA((4,)),
                pltpu.SemaphoreType.DMA((4,)),
                pltpu.SemaphoreType.DMA((4,)),
            ]
            + [pltpu.SemaphoreType.DMA] * 6,
            compiler_params=pltpu.CompilerParams(
                collective_id=0, has_side_effects=True, vmem_limit_bytes=24 << 20
            ),
            name="conv",
        )(*(pltpu.with_memory_space_constraint(a, pltpu.HBM) for a in args))
        out = pl.pallas_call(
            tail_kernel,
            out_shape=jax.ShapeDtypeStruct((tile_h, tile_j, 2, images, chans), F32),
            in_specs=[vmem] * len(kept),
            out_specs=pl.BlockSpec(memory_space=pl.ANY),
            scratch_shapes=[
                pltpu.VMEM((2, tile_j, 2, images, chans), F32),
                pltpu.SemaphoreType.DMA((2,)),
            ],
            compiler_params=pltpu.CompilerParams(vmem_limit_bytes=8 << 20),
            name="tail",
        )(*state)
        out = out.reshape(tile_h, 2 * tile_j, images, chans)
        return jnp.transpose(out, (2, 0, 1, 3))

    group = ("model", "cols")
    return jax.shard_map(
        run_local,
        mesh=mesh,
        in_specs=(P("data", None, None, group), P(None, None, group, None), P(), P(), P()),
        out_specs=P("data", "model", "cols", None),
        check_vma=False,
    )
```
